32 devices in a mesh: rep: 4 (over z), ep: 8 (over y, x, core).
Axes of the slice: x: 2, y: 2, z: 4, core: 2. Of those that a mesh axis runs over, the one named last changes fastest.
Arguments:
- tokens: bfloat16 [32, 256, 2048], P('rep', 'ep'), may hold values from -6 to 6
- cotangent: bfloat16 [32, 256, 2048], P('rep', 'ep'), may hold values from -6 to 6
- gate_weights: bfloat16 [32, 256, 8], P('rep', 'ep'), may hold values from 0.049804688 to 0.25
- expert_ids: int32 [32, 256, 8], P('rep', 'ep'), may hold values from 0 to 15, all different within a row; in each aligned block of 256 rows (0 to 255, 256 to 511, ..., all dimensions but the last counted through in order) at most 144 rows name the same one
- seq_lengths: int32 [32], P(('rep', 'ep')), may hold values from 1 to 256, 5120 in all
- query_weight: bfloat16 [2048, 2048], P('ep'), may hold values from -0.125 to 0.125
- key_weight: bfloat16 [2048, 2048], P('ep'), may hold values from -0.125 to 0.125
- value_weight: bfloat16 [2048, 2048], P('ep'), may hold values from -0.125 to 0.125
- output_weight: bfloat16 [2048, 2048], P('ep'), may hold values from -0.75 to 0.75
- attn_gain: bfloat16 [2048], P('ep'), may hold values from 0.25 to 1.75
- ffn_gain: bfloat16 [2048], P('ep'), may hold values from 0.25 to 1.75
- query_gain: bfloat16 [128], P('ep'), may hold values from 0.25 to 1.75
- key_gain: bfloat16 [128], P('ep'), may hold values from 0.25 to 1.75
- expert_in: bfloat16 [16, 2048, 2048], P('ep'), may hold values from -0.125 to 0.125
- expert_out: bfloat16 [16, 1024, 2048], P('ep'), may hold values from -0.5 to 0.5
Outputs:
- result: bfloat16 [32, 256, 2048], P('rep', 'ep')
- token_grad: bfloat16 [32, 256, 2048], P('rep', 'ep')
- query_weight_grad: float32 [2048, 2048], P('ep')
- key_weight_grad: float32 [2048, 2048], P('ep')
- value_weight_grad: float32 [2048, 2048], P('ep')
- output_weight_grad: float32 [2048, 2048], P('ep')
- attn_gain_grad: float32 [2048], P('ep')
- ffn_gain_grad: float32 [2048], P('ep')
- query_gain_grad: float32 [128], P('ep')
- key_gain_grad: float32 [128], P('ep')
- expert_in_grad: float32 [16, 2048, 2048], P('ep', 'rep')
- expert_out_grad: float32 [16, 1024, 2048], P('ep', 'rep')
The draws below stay inside these ranges and needn't reach their ends.
Inputs may be any that keep to these rules, and one draw needn't show every extreme that they name: `expert_ids`: each token names 8 different experts; within the 256 token slots of one sequence no expert is named more than 144 times, and some expert of some sequence is named exactly 144 times. `seq_lengths`: some sequence is full, with exactly 256 live tokens; live tokens come first in a sequence.
All inputs are finite; a program needn't handle non-finite values. No bound on the sum of `seq_lengths` on one device may be relied on, other than what follows from the above.
Results may differ from the reference program's by a relative error of at most 0.028.
Values may be sent and summed in bfloat16 or wider, within the bound.
A program may use at most 320 MiB of HBM per device.

```python
import math
import jax
import jax.numpy as jnp
import numpy as np
from jax import lax

WIDTH = 2048
HEADS = 16
HEAD_DIM = 128
EXPERT_HIDDEN = 1024
TOP = 8
SEQ_LEN = 256
ATTN_WIDTH = 2048
EXPERTS = 16
SEQS = 32
CAPACITY = 144


def levels(key, extent, split, least, largest):
    level = 1.0
    for position, parts in split:
        heights = jax.random.uniform(jax.random.fold_in(jax.random.fold_in(key, 6), position), (parts,), jnp.float32, least / len(split), largest / len(split))
        level = level * jnp.repeat(jnp.exp(heights), extent[position] // parts).reshape((-1,) + (1,) * (len(extent) - 1 - position))
    return level


def profile(number_of, total, bound, skew):
    portions = [(1 << 20) // math.isqrt(grade ** skew) + 1 for grade in range(2, number_of + 1)]
    spare, holding = total - bound - (number_of - 1), [1] * (number_of - 1)
    while spare > 0:
        candidates = [i for i in range(number_of - 1) if holding[i] < bound]
        mass, left = sum([portions[i] for i in candidates]), spare
        for i in candidates:
            more = min(bound - holding[i], max(1, left * portions[i] // mass), spare)
            holding[i] = holding[i] + more
            spare = spare - more
    return np.array([bound] + holding)


def uneven(own_key, amount, total, bound, skew):
    if amount == 2:
        one = jax.random.randint(own_key, (), max(1, total - bound), min(bound, total - 1) + 1)
        return jnp.stack([one, total - one])
    tallies = jnp.asarray(profile(amount, total, bound, skew), jnp.int32)
    twos = (amount - 1) // 2
    source_of, sink = tallies[1:1 + 2 * twos:2], tallies[2:2 + 2 * twos:2]
    slack = jnp.minimum(source_of - 1, bound - sink)
    moved = jax.random.randint(jax.random.fold_in(own_key, 1), (twos,), 0, 1 << 20) % (slack + 1)
    tallies = tallies.at[1:1 + 2 * twos:2].set(source_of - moved).at[2:2 + 2 * twos:2].set(sink + moved)
    return tallies[jax.random.permutation(jax.random.fold_in(own_key, 2), amount)]


def shared_out(key, own, number, rows, count, top, limit, slope):
    order = jax.random.permutation(key, count)
    crowded, usual = shares(count, rows * top, limit, slope, True), shares(count, rows * top, limit, slope, False)
    places = jnp.arange(count)

    def named(tallies, turn):
        used = int((tallies > 0).sum())
        fixed = max(1, used // 4)
        moved = fixed + (places - fixed + turn * (used - fixed)) % max(1, count - fixed)
        return jnp.zeros((count,), jnp.int32).at[order[jnp.where(places < fixed, places, moved)]].set(jnp.asarray(tallies, jnp.int32))

    tallies = jnp.where(number % 4 == 0, named(crowded, number // 4), named(usual, number - number // 4 - 1))
    mixed = jax.random.permutation(jax.random.fold_in(own, 3), count)
    source_of, taker = mixed[0:count // 2 * 2:2], mixed[1:count // 2 * 2:2]
    slack = jnp.minimum(tallies[source_of] - 1, limit - tallies[taker]) // 2
    slack = jnp.where((source_of == order[0]) | (taker == order[0]) | (tallies[taker] == 0), 0, jnp.maximum(slack, 0))
    moved = jax.random.randint(jax.random.fold_in(own, 4), (count // 2,), 0, 1 << 20) % (slack + 1)
    tallies = tallies.at[source_of].add(-moved).at[taker].add(moved)
    items = jnp.searchsorted(jnp.cumsum(tallies), jnp.arange(rows * top), side="right").astype(jnp.int32)
    grid = items.reshape(top, rows).T
    grid = grid[jax.random.permutation(jax.random.fold_in(own, 1), rows)]
    turn = jax.random.randint(jax.random.fold_in(own, 2), (rows, 1), 0, top)
    return jnp.take_along_axis(grid, (jnp.arange(top)[None, :] + turn) % top, axis=1)


def shares(amount, total, reach, skew, full):
    weights = [(1 << 20) // math.isqrt(grade ** skew) + 1 for grade in range(1, amount + 1)]
    largest = reach if full else min(reach, max(-(-total // amount), total * weights[0] // sum(weights)))
    least = 1 if total - largest >= amount - 1 else 0
    given, spare = [largest] + [least] * (amount - 1), total - largest - least * (amount - 1)
    while spare > 0:
        free = [i for i in range(1, amount) if given[i] < largest] or [i for i in range(1, amount) if given[i] < reach]
        pool, budget = sum([weights[i] for i in free]), spare
        for i in free:
            extra = min(reach - given[i], max(1, budget * weights[i] // pool), spare)
            given[i] = given[i] + extra
            spare = spare - extra
    return np.array(given)


def bell_draw(stream_key, dims, spread, most, cuts=(), kind=jnp.bfloat16):
    gain = levels(stream_key, dims, cuts, -0.22, 0.18) if cuts else 1.0
    entries = jax.random.normal(stream_key, dims, jnp.float32) * spread * gain
    return jnp.minimum(jnp.maximum(entries, -most), most).astype(kind)


def setup_inputs(seed: int = 0) -> dict:
    key_of = jax.random.split(jax.random.key(seed), 16)
    tokens = bell_draw(key_of[0], (SEQS, SEQ_LEN, WIDTH), 1.0, 6.0, ((0, 4), (1, 8)))
    cotangent = bell_draw(key_of[1], (SEQS, SEQ_LEN, WIDTH), 1.0, 6.0, ((0, 4), (1, 8)))
    gate_weights = jnp.clip(0.049804688 + 0.20019531 * jax.random.uniform(key_of[2], (SEQS, SEQ_LEN, TOP), jnp.float32) ** levels(key_of[2], (SEQS, SEQ_LEN, TOP), ((0, 4), (1, 8)), -0.2, 0.2), 0.049804688, 0.25).astype(jnp.bfloat16)
    expert_ids_keys = jax.random.split(jax.random.fold_in(key_of[3], 1), SEQS * SEQ_LEN // SEQ_LEN)
    expert_ids_turns = jax.random.permutation(jax.random.fold_in(key_of[3], 3), SEQS * SEQ_LEN // SEQ_LEN)
    expert_ids = jax.vmap(lambda own, number: shared_out(jax.random.fold_in(key_of[3], 2), own, number, SEQ_LEN, EXPERTS, TOP, CAPACITY, 1))(expert_ids_keys, expert_ids_turns).reshape((SEQS, SEQ_LEN, TOP))
    seq_lengths = uneven(key_of[4], SEQS, SEQS * SEQ_LEN * 5 // 8, SEQ_LEN, 2).astype(jnp.int32)
    query_weight = bell_draw(key_of[5], (WIDTH, ATTN_WIDTH), WIDTH ** -0.5, 0.125, ((0, 8),))
    key_weight = bell_draw(key_of[6], (WIDTH, ATTN_WIDTH), WIDTH ** -0.5, 0.125, ((0, 8),))
    value_weight = bell_draw(key_of[7], (WIDTH, ATTN_WIDTH), WIDTH ** -0.5, 0.125, ((0, 8),))
    output_weight = bell_draw(key_of[8], (ATTN_WIDTH, WIDTH), (ATTN_WIDTH // 32) ** -0.5, 0.75, ((0, 8),))
    attn_gain = jnp.clip(1.0 + 0.15 * jax.random.normal(key_of[9], (WIDTH,), jnp.float32), 0.25, 1.75).astype(jnp.bfloat16)
    ffn_gain = jnp.clip(1.0 + 0.15 * jax.random.normal(key_of[10], (WIDTH,), jnp.float32), 0.25, 1.75).astype(jnp.bfloat16)
    query_gain = jnp.clip(1.0 + 0.15 * jax.random.normal(key_of[11], (HEAD_DIM,), jnp.float32), 0.25, 1.75).astype(jnp.bfloat16)
    key_gain = jnp.clip(1.0 + 0.15 * jax.random.normal(key_of[12], (HEAD_DIM,), jnp.float32), 0.25, 1.75).astype(jnp.bfloat16)
    expert_in = bell_draw(key_of[13], (EXPERTS, WIDTH, 2 * EXPERT_HIDDEN), WIDTH ** -0.5, 0.125, ((0, 8),))
    expert_out = bell_draw(key_of[14], (EXPERTS, EXPERT_HIDDEN, WIDTH), (EXPERT_HIDDEN // 8) ** -0.5, 0.5, ((0, 8),))
    return dict(tokens=tokens, cotangent=cotangent, gate_weights=gate_weights, expert_ids=expert_ids, seq_lengths=seq_lengths, query_weight=query_weight, key_weight=key_weight, value_weight=value_weight, output_weight=output_weight, attn_gain=attn_gain, ffn_gain=ffn_gain, query_gain=query_gain, key_gain=key_gain, expert_in=expert_in, expert_out=expert_out)


@jax.custom_vjp
def low(v):
    return lax.optimization_barrier(v.astype(jnp.bfloat16)).astype(jnp.float32)

@jax.custom_vjp
def low_back(v):
    return v

def low_keep(v):
    return (low(v), None)

def low_pass(kept, grad):
    return (grad,)

def back_keep(v):
    return (v, None)

def back_low(kept, grad):
    return (low(grad),)
low.defvjp(low_keep, low_pass)
low_back.defvjp(back_keep, back_low)
epsilon = 1e-06
rope_base = 50000.0
highest = lax.Precision.HIGHEST

def rms_norm(values, gain_vector):
    return values * lax.rsqrt(lax.optimization_barrier(jnp.mean(values * values, axis=-1, keepdims=True)) + epsilon) * gain_vector

def rotary_tables(length, head_width):
    half_width = head_width // 2
    frequency = rope_base ** (-(jnp.arange(half_width, dtype=jnp.float32) * (2.0 / head_width)))
    angles = jnp.arange(length, dtype=jnp.float32)[:, None] * frequency[None, :]
    angles = jnp.concatenate([angles, angles], axis=-1)
    return (jnp.cos(angles)[:, None, :], jnp.sin(angles)[:, None, :])

def rotate(values, cos_table, sin_table):
    half_width = values.shape[-1] // 2
    turned = jnp.concatenate([-values[..., half_width:], values[..., :half_width]], axis=-1)
    return values * cos_table + turned * sin_table

def slot_index(expert_ids, experts, capacity):
    flat_ids = expert_ids.reshape(-1).astype(jnp.int32)
    choose = (flat_ids[:, None] == jnp.arange(experts, dtype=jnp.int32)[None, :]).astype(jnp.int32)
    before = jnp.cumsum(choose, axis=0) - choose
    ranking = lax.optimization_barrier(jnp.sum(before * choose, axis=1))
    return (flat_ids * capacity + ranking).astype(jnp.int32)

def layer(hidden_in, query_weight, key_weight, value_weight, output_weight, attn_gain, ffn_gain, query_gain, key_gain, expert_in, expert_out, combine_weight, destination, living):
    length = hidden_in.shape[0]
    cos_table, sin_table = rotary_tables(length, HEAD_DIM)
    score_scale = HEAD_DIM ** (-0.5)
    normed = low(rms_norm(hidden_in, attn_gain))
    queries = low_back(jnp.dot(normed, query_weight, precision=highest)).reshape(length, HEADS, HEAD_DIM)
    keys_pre = low_back(jnp.dot(normed, key_weight, precision=highest)).reshape(length, HEADS, HEAD_DIM)
    values = low(low_back(jnp.dot(normed, value_weight, precision=highest))).reshape(length, HEADS, HEAD_DIM)
    query_rot = low(rotate(rms_norm(queries, query_gain), cos_table, sin_table))
    key_rot = low(rotate(rms_norm(keys_pre, key_gain), cos_table, sin_table))
    scores = low_back(jnp.einsum('qhd,khd->hqk', query_rot, key_rot, precision=highest) * score_scale)
    scores = jnp.where(living[None, None, :] > 0.5, scores, -1000000000.0)
    attention = low(jax.nn.softmax(scores, axis=-1))
    context = low(low_back(jnp.einsum('hqk,khd->qhd', attention, values, precision=highest))).reshape(length, ATTN_WIDTH)
    attended = low_back(jnp.dot(context, output_weight, precision=highest)) * living[:, None]
    middle = hidden_in + attended
    mixed_in = low(rms_norm(middle, ffn_gain))
    copies = low_back(jnp.broadcast_to(mixed_in[:, None, :], (length, TOP, WIDTH)).reshape(length * TOP, WIDTH))
    buffer = jnp.zeros((EXPERTS * CAPACITY, WIDTH), jnp.float32).at[destination].set(copies)
    buffer = buffer.reshape(EXPERTS, CAPACITY, WIDTH)
    gate_up = low_back(jnp.einsum('ecd,edf->ecf', buffer, expert_in, precision=highest))
    activated = low(jax.nn.silu(gate_up[..., :EXPERT_HIDDEN]) * gate_up[..., EXPERT_HIDDEN:])
    produced = low(low_back(jnp.einsum('ecf,efd->ecd', activated, expert_out, precision=highest)))
    gathered = produced.reshape(EXPERTS * CAPACITY, WIDTH)[destination].reshape(length, TOP, WIDTH)
    return middle + lax.optimization_barrier(jnp.sum(combine_weight[:, :, None] * gathered, axis=1))

def reference(tokens, cotangent, gate_weights, expert_ids, seq_lengths, query_weight, key_weight, value_weight, output_weight, attn_gain, ffn_gain, query_gain, key_gain, expert_in, expert_out):
    params = (query_weight, key_weight, value_weight, output_weight, attn_gain, ffn_gain, query_gain, key_gain, expert_in, expert_out)
    params = tuple((member.astype(jnp.float32) for member in params))
    positions = jnp.arange(SEQ_LEN, dtype=jnp.int32)

    def one_sequence(running, pieces):
        seq_tokens, seq_cot, seq_gates, seq_ids, seq_len = pieces
        living = (positions < seq_len).astype(jnp.float32)
        combine_weight = seq_gates.astype(jnp.float32) * living[:, None]
        destination = slot_index(seq_ids, EXPERTS, CAPACITY)

        def forward(hidden_in, *weights):
            return layer(hidden_in, *weights, combine_weight, destination, living)
        outcome, pull_back = jax.vjp(forward, seq_tokens.astype(jnp.float32), *params)
        grads_all = pull_back(seq_cot.astype(jnp.float32))
        running = tuple((total_part + grad_part for total_part, grad_part in zip(running, grads_all[1:])))
        return (running, (outcome.astype(jnp.bfloat16), grads_all[0].astype(jnp.bfloat16)))
    zeros_all = tuple((jnp.zeros(member.shape, jnp.float32) for member in params))
    sums, (outputs, input_grads) = lax.scan(one_sequence, zeros_all, (tokens, cotangent, gate_weights, expert_ids, seq_lengths))
    return (outputs, input_grads, sums[0], sums[1], sums[2], sums[3], sums[4], sums[5], sums[6], sums[7], sums[8], sums[9])
```

```python
import jax
import jax.numpy as jnp
from jax import lax
from jax.experimental import pallas as pl
from jax.experimental.pallas import tpu as pltpu
from jax.sharding import PartitionSpec as P

HEAD_DIM = 128
EPS = 1e-06
ROPE_BASE = 50000.0
MESH = pl.DeviceIdType.MESH
F32 = jnp.float32
BF16 = jnp.bfloat16


def sds(shape, dtype):
    return jax.ShapeDtypeStruct(shape, dtype)


VM = pl.BlockSpec(memory_space=pltpu.VMEM)
AN = pl.BlockSpec(memory_space=pl.ANY)


def inverse_rms(v):
    return lax.rsqrt(jnp.mean(v * v, axis=-1, keepdims=True) + EPS)


def rms_back(v, r, ug):
    return r * ug - v * (r * r * r * jnp.mean(ug * v, axis=-1, keepdims=True))


def mix_rows(total, tok, living, gain):
    middle = tok.astype(F32) + living * total
    mixed = middle * inverse_rms(middle) * gain
    return middle, mixed.astype(BF16)


def ffn_back_rows(mixed_grad, middle, cot, living, gain):
    r = inverse_rms(middle)
    middle_grad = cot.astype(F32) + rms_back(middle, r, mixed_grad * gain)
    return middle_grad, (living * middle_grad).astype(BF16), mixed_grad * middle * r


def attn_back_rows(normed_grad, tok, middle_grad, gain):
    v = tok.astype(F32)
    r = inverse_rms(v)
    return (middle_grad + rms_back(v, r, normed_grad * gain)).astype(BF16), normed_grad * v * r


class Place:
    def __init__(self):
        me = lax.axis_index("ep")
        core, x, y = lax.rem(me, 2), lax.rem(me // 2, 2), me // 4
        self.rep = lax.axis_index("rep")
        self.me = me
        self.sb = me + 1 - 2 * core
        self.dx = 2 - 4 * x
        self.dy = 4 - 8 * y
        self.xn = me + self.dx
        self.yn = me + self.dy
        self.dg = me + self.dx + self.dy

    def push(self, src, dst, send, recv, dev):
        return pltpu.make_async_remote_copy(
            src_ref=src, dst_ref=dst, send_sem=send, recv_sem=recv, device_id=(self.rep, dev), device_id_type=MESH
        )

    def peers(self):
        sb, dx, dy = self.sb, self.dx, self.dy
        return (self.xn, self.yn, self.dg, sb, sb + dx, sb + dy, sb + dx + dy)

    def greet(self, peers):
        barrier = pltpu.get_barrier_semaphore()
        for peer in peers:
            pl.semaphore_signal(barrier, inc=1, device_id=(self.rep, peer), device_id_type=MESH)
        pl.semaphore_wait(barrier, len(peers))


class Gather:
    sems = 3

    def __init__(self, at, own, full, ssem, rsem, lsem):
        self.at, self.own, self.full, self.ssem, self.rsem, self.lsem = at, own, full, ssem, rsem, lsem
        self.rows = own.shape[1]

    @staticmethod
    def scratch(seqs):
        return [pltpu.SemaphoreType.DMA((7, seqs)), pltpu.SemaphoreType.DMA((8, seqs)), pltpu.SemaphoreType.DMA((seqs,))]

    def block(self, s, dev):
        return self.full.at[s, pl.ds(pl.multiple_of(dev * self.rows, self.rows), self.rows)]

    def copy(self, s, dev, kind, slot, to, src=None):
        block = self.block(s, dev)
        return self.at.push(block if src is None else src, block, self.ssem.at[kind, s], self.rsem.at[slot, s], to)

    def start(self, s):
        at, own = self.at, self.own.at[s]
        self.copy(s, at.me, 0, 2, at.xn, own).start()
        self.copy(s, at.me, 1, 4, at.yn, own).start()
        self.copy(s, at.me, 2, 1, at.sb, own).start()
        pltpu.make_async_copy(own, self.block(s, at.me), self.lsem.at[s]).start()

    def relay(self, s, by_y):
        at = self.at
        self.copy(s, at.xn, 0, 2, at.xn).wait_recv()
        if by_y:
            self.copy(s, at.xn, 3, 6, at.yn).start()
        self.copy(s, at.xn, 4, 3, at.sb).start()
        self.copy(s, at.yn, 1, 4, at.yn).wait_recv()
        if not by_y:
            self.copy(s, at.yn, 3, 6, at.xn).start()
        self.copy(s, at.yn, 5, 5, at.sb).start()

    def relay_far(self, s):
        at = self.at
        self.copy(s, at.dg, 3, 6, at.yn).wait_recv()
        self.copy(s, at.dg, 6, 7, at.sb).start()

    def finish(self, s):
        at = self.at
        for dev, slot in ((at.sb, 1), (at.sb + at.dx, 3), (at.sb + at.dy, 5), (at.sb + at.dx + at.dy, 7)):
            self.copy(s, dev, 0, slot, at.sb).wait_recv()
        for kind in range(7):
            self.copy(s, at.me, kind, 0, at.sb).wait_send()
        pltpu.make_async_copy(self.own.at[s], self.block(s, at.me), self.lsem.at[s]).wait()


def gather_tail(seqs, gather):
    def relay(i, _):
        gather.relay(2 * i, True)
        gather.relay(2 * i + 1, False)
        return 0

    def far(s, _):
        gather.relay_far(s)
        return 0

    def finish(s, _):
        gather.finish(s)
        return 0

    lax.fori_loop(0, seqs // 2, relay, 0)
    lax.fori_loop(0, seqs, far, 0)
    lax.fori_loop(0, seqs, finish, 0)


class Reduce:
    def __init__(self, at, part, held, x1, y1, x2, y2, hs, hr, d1s, d1r, d2s, d2r):
        self.at, self.part, self.held = at, part, held
        self.x1, self.y1, self.x2, self.y2 = x1, y1, x2, y2
        self.hs, self.hr, self.d1s, self.d1r, self.d2s, self.d2r = hs, hr, d1s, d1r, d2s, d2r
        self.half = part.shape[2] // 2

    @staticmethod
    def scratch(part):
        s, _, t, d = part.shape
        dma = pltpu.SemaphoreType.DMA
        return [
            pltpu.VMEM((s, 4, t, d), BF16),
            pltpu.VMEM((s, t // 2, d), BF16),
            pltpu.VMEM((s, t // 2, d), BF16),
            pltpu.VMEM((s, t, d), BF16),
            pltpu.VMEM((s, t, d), BF16),
            dma((4, s)),
            dma((4, s)),
            dma((2, s)),
            dma((2, s)),
            dma((2, s)),
            dma((2, s)),
        ]

    sems = 11

    def core_copy(self, s, k):
        at = self.at
        dest = (at.sb, at.sb + at.dx, at.sb + at.dy, at.sb + at.dx + at.dy)[k]
        return at.push(self.part.at[s, dest], self.held.at[s, k], self.hs.at[k, s], self.hr.at[k, s], at.sb)

    def first(self, s, k):
        at, h = self.at, self.half
        src = self.held.at[s, 3, pl.ds(k * h, h)]
        return at.push(src, (self.x1, self.y1)[k].at[s], self.d1s.at[k, s], self.d1r.at[k, s], (at.xn, at.yn)[k])

    def second(self, s, k):
        at = self.at
        src = self.held.at[s, 1 + k]
        return at.push(src, (self.x2, self.y2)[k].at[s], self.d2s.at[k, s], self.d2r.at[k, s], (at.xn, at.yn)[k])

    def start(self, s):
        for k in (3, 1, 2, 0):
            self.core_copy(s, k).start()

    def hop1(self, s):
        self.core_copy(s, 3).wait_recv()
        self.held[s, 3] = (self.held[s, 3].astype(F32) + self.part[s, self.at.dg].astype(F32)).astype(BF16)
        self.first(s, 0).start()
        self.first(s, 1).start()

    def hop2(self, s):
        h = self.half
        for k, dest, extra, rows, rest in (
            (0, self.at.xn, self.y1, pl.ds(h, h), pl.ds(0, h)),
            (1, self.at.yn, self.x1, pl.ds(0, h), pl.ds(h, h)),
        ):
            self.core_copy(s, 1 + k).wait_recv()
            self.first(s, 1 - k).wait_recv()
            held, part = self.held.at[s, 1 + k], self.part.at[s, dest]
            held[rows] = (held[rows].astype(F32) + part[rows].astype(F32) + extra[s].astype(F32)).astype(BF16)
            held[rest] = (held[rest].astype(F32) + part[rest].astype(F32)).astype(BF16)
            self.second(s, k).start()

    def total(self, s):
        self.core_copy(s, 0).wait_recv()
        self.second(s, 0).wait_recv()
        self.second(s, 1).wait_recv()
        return (
            self.part[s, self.at.me].astype(F32)
            + self.held[s, 0].astype(F32)
            + self.x2[s].astype(F32)
            + self.y2[s].astype(F32)
        )

    def finish(self, s):
        for k in range(4):
            self.core_copy(s, k).wait_send()
        for k in range(2):
            self.first(s, k).wait_send()
            self.second(s, k).wait_send()


def each(n, *steps):
    def run(s, _):
        for step in steps:
            step(s)
        return 0

    lax.fori_loop(0, n, run, 0)


COMM = dict(has_side_effects=True, vmem_limit_bytes=60 << 20)


def front_kernel(tok, wq, wk, wv, pk, full, weights, packets, tok_v, *sems):
    at = Place()
    gather = Gather(at, tok, full, *sems[:3])
    wsend, wrecv, psend, precv, local = sems[3:]
    seqs = tok.shape[0]
    block, width = wq.shape[0], weights.shape[2]
    at.greet(at.peers())
    each(seqs, gather.start)
    mine = pl.ds(pl.multiple_of(at.me * block, block), block)

    def weight_copy(m, j, dev):
        cols = pl.ds(pl.multiple_of(dev * width, width), width)
        return at.push((wq, wk, wv)[j].at[:, cols], weights.at[j, mine], wsend.at[m, j], wrecv.at[m, j], dev)

    def packet_copy(m, dev):
        return at.push(pk, packets.at[at.me], psend.at[m], precv.at[m], dev)

    own_cols = pl.ds(pl.multiple_of(at.me * width, width), width)
    own = [pltpu.make_async_copy(w.at[:, own_cols], weights.at[j, mine], local.at[j]) for j, w in enumerate((wq, wk, wv))]
    own.append(pltpu.make_async_copy(pk, packets.at[at.me], local.at[3]))
    for copy in own:
        copy.start()
    for m, dev in enumerate(at.peers()):
        packet_copy(m, dev).start()
    for m, dev in enumerate(at.peers()):
        for j in range(3):
            weight_copy(m, j, dev).start()
    gather_tail(seqs, gather)
    for m, dev in enumerate(at.peers()):
        packet_copy(m, dev).wait()
        for j in range(3):
            weight_copy(m, j, dev).wait()
    for copy in own:
        copy.wait()


def front(tokens, wq, wk, wv, packet):
    seqs, rows, width = tokens.shape
    ep = lax.axis_size("ep")
    cols = wq.shape[1] // ep
    if ep != 8:
        full = lax.all_gather(tokens, "ep", axis=1, tiled=True)
        weights = [lax.all_to_all(w, "ep", split_axis=1, concat_axis=0, tiled=True) for w in (wq, wk, wv)]
        return full, jnp.stack(weights), lax.all_gather(packet, "ep", axis=0)
    dma = pltpu.SemaphoreType.DMA
    return pl.pallas_call(
        front_kernel,
        out_shape=(
            sds((seqs, rows * ep, width), BF16),
            sds((3, wq.shape[0] * ep, cols), BF16),
            sds((ep,) + packet.shape, F32),
        ),
        in_specs=[VM] * 5,
        out_specs=(AN, AN, AN),
        scratch_shapes=[pltpu.VMEM((8, 128), F32)]
        + Gather.scratch(seqs)
        + [dma((7, 3)), dma((7, 3)), dma((7,)), dma((7,)), dma((4,))],
        compiler_params=pltpu.CompilerParams(collective_id=1, **COMM),
        name="front",
    )(tokens, wq, wk, wv, packet)


def mix_kernel(part, tok, living, gain, middle, full, own, *scratch):
    at = Place()
    seqs = tok.shape[0]
    reduce = Reduce(at, part, *scratch[: Reduce.sems])
    gather = Gather(at, own, full, *scratch[Reduce.sems :])
    at.greet((at.xn, at.yn, at.sb))
    each(seqs, reduce.start)
    each(seqs, reduce.hop1)
    each(seqs, reduce.hop2)

    def rows(s):
        mid, mixed = mix_rows(reduce.total(s), tok[s], living[s], gain[...])
        middle[s] = mid
        own[s] = mixed
        gather.start(s)

    each(seqs, rows)
    gather_tail(seqs, gather)
    each(seqs, reduce.finish)


def mix(part, tokens, living, gain):
    seqs, rows, width = tokens.shape
    ep = lax.axis_size("ep")
    if ep != 8:
        total = lax.psum_scatter(part, "ep", scatter_dimension=1, tiled=True).astype(F32)
        middle, mixed = mix_rows(total, tokens, living, gain)
        return middle, lax.all_gather(mixed, "ep", axis=1, tiled=True)
    part = part.reshape(seqs, ep, rows, width)
    return pl.pallas_call(
        mix_kernel,
        out_shape=(sds(tokens.shape, F32), sds((seqs, rows * ep, width), BF16)),
        in_specs=[VM] * 4,
        out_specs=(VM, AN),
        scratch_shapes=[pltpu.VMEM(tokens.shape, BF16)] + Reduce.scratch(part) + Gather.scratch(seqs),
        compiler_params=pltpu.CompilerParams(collective_id=2, **COMM),
        name="mix",
    )(part, tokens, living, gain)


def back_kernel(gpart, opart, middle, cot, living, gain, result, mgrad, ggrad, full, own, *scratch):
    at = Place()
    seqs = cot.shape[0]
    n = Reduce.sems
    rg = Reduce(at, gpart, *scratch[:n])
    ro = Reduce(at, opart, *scratch[n : 2 * n])
    gather = Gather(at, own, full, *scratch[2 * n :])
    at.greet((at.xn, at.yn, at.sb))
    each(seqs, rg.start)
    each(seqs, ro.start)
    each(seqs, rg.hop1)
    each(seqs, rg.hop2)
    ggrad[...] = jnp.zeros_like(ggrad)

    def rows(s):
        mg, ag, back = ffn_back_rows(rg.total(s), middle[s], cot[s], living[s], gain[...])
        mgrad[s] = mg
        own[s] = ag
        ggrad[...] += jnp.sum(back, axis=0, keepdims=True)
        gather.start(s)

    each(seqs, rows)
    gather_tail(seqs, gather)
    each(seqs, ro.hop1)
    each(seqs, ro.hop2)

    def out(s):
        result[s] = (middle[s] + ro.total(s)).astype(BF16)

    each(seqs, out)
    each(seqs, rg.finish, ro.finish)


def back(gpart, opart, middle, cot, living, gain):
    seqs, rows, width = cot.shape
    ep = lax.axis_size("ep")
    if ep != 8:
        mixed_grad = lax.psum_scatter(gpart, "ep", scatter_dimension=1, tiled=True).astype(F32)
        moe = lax.psum_scatter(opart, "ep", scatter_dimension=1, tiled=True).astype(F32)
        mg, ag, backs = ffn_back_rows(mixed_grad, middle, cot, living, gain)
        full = lax.all_gather(ag, "ep", axis=1, tiled=True)
        return (middle + moe).astype(BF16), mg, jnp.sum(backs, axis=(0, 1))[None], full
    gpart, opart = (p.reshape(seqs, ep, rows, width) for p in (gpart, opart))
    return pl.pallas_call(
        back_kernel,
        out_shape=(
            sds(cot.shape, BF16),
            sds(cot.shape, F32),
            sds((1, width), F32),
            sds((seqs, rows * ep, width), BF16),
        ),
        in_specs=[VM] * 6,
        out_specs=(VM, VM, VM, AN),
        scratch_shapes=[pltpu.VMEM(cot.shape, BF16)] + 2 * Reduce.scratch(gpart) + Gather.scratch(seqs),
        compiler_params=pltpu.CompilerParams(collective_id=3, **COMM),
        name="back",
    )(gpart, opart, middle, cot, living, gain)


def final_kernel(part, wgrad, tok, mgrad, gain, tgrad, ggrad, wrows, *scratch):
    at = Place()
    seqs = tok.shape[0]
    n = Reduce.sems
    reduce = Reduce(at, part, *scratch[:n])
    wsend, wrecv, local = scratch[n:]
    width = wgrad.shape[2]
    block = wrows.shape[1]
    at.greet(at.peers())
    cols = pl.ds(pl.multiple_of(at.me * width, width), width)

    def weight_copy(m, dev):
        rows = pl.ds(pl.multiple_of(dev * block, block), block)
        return at.push(wgrad.at[:, rows], wrows.at[:, :, cols], wsend.at[m], wrecv.at[m], dev)

    mine = pl.ds(pl.multiple_of(at.me * block, block), block)
    own = pltpu.make_async_copy(wgrad.at[:, mine], wrows.at[:, :, cols], local)
    own.start()
    for m, dev in enumerate(at.peers()):
        weight_copy(m, dev).start()
    each(seqs, reduce.start)
    each(seqs, reduce.hop1)
    each(seqs, reduce.hop2)
    ggrad[...] = jnp.zeros_like(ggrad)

    def rows(s):
        tg, back = attn_back_rows(reduce.total(s), tok[s], mgrad[s], gain[...])
        tgrad[s] = tg
        ggrad[...] += jnp.sum(back, axis=0, keepdims=True)

    each(seqs, rows)
    each(seqs, reduce.finish)
    for m, dev in enumerate(at.peers()):
        weight_copy(m, dev).wait()
    own.wait()


def final(part, wgrad, tokens, mgrad, gain):
    seqs, rows, width = tokens.shape
    ep = lax.axis_size("ep")
    if ep != 8:
        normed_grad = lax.psum_scatter(part, "ep", scatter_dimension=1, tiled=True).astype(F32)
        tg, backs = attn_back_rows(normed_grad, tokens, mgrad, gain)
        wrows = lax.all_to_all(wgrad, "ep", split_axis=1, concat_axis=2, tiled=True)
        return tg, jnp.sum(backs, axis=(0, 1))[None], wrows
    part = part.reshape(seqs, ep, rows, width)
    dma = pltpu.SemaphoreType.DMA
    return pl.pallas_call(
        final_kernel,
        out_shape=(
            sds(tokens.shape, BF16),
            sds((1, width), F32),
            sds((3, wgrad.shape[1] // ep, wgrad.shape[2] * ep), BF16),
        ),
        in_specs=[VM] * 5,
        out_specs=(VM, VM, AN),
        scratch_shapes=Reduce.scratch(part) + [dma((7,)), dma((7,)), dma],
        compiler_params=pltpu.CompilerParams(collective_id=4, **COMM),
        name="final",
    )(part, wgrad, tokens, mgrad, gain)


def dot(a, b, ca, cb):
    return lax.dot_general(a, b, (((ca,), (cb,)), ((), ())), preferred_element_type=F32)


def rope(v, cos, sin_turn):
    return v * cos + pltpu.roll(v, HEAD_DIM // 2, 1) * sin_turn


def probabilities(q, k, length):
    scores = dot(q, k, 1, 1) * HEAD_DIM**-0.5
    column = lax.broadcasted_iota(jnp.int32, scores.shape, 1)
    scores = jnp.where(column < length, scores, -1e9)
    p = jnp.exp(scores - jnp.max(scores, axis=-1, keepdims=True))
    return p * (1.0 / jnp.sum(p, axis=-1, keepdims=True))


def attend_kernel(lens, tok, w, wo, gain, qg, kg, cos, sin, normed, pre, low, ctx, part):
    length = lens[pl.program_id(0)]
    v = tok[0].astype(F32)
    x = (v * inverse_rms(v) * gain[...]).astype(BF16)
    normed[0] = x
    q_pre, k_pre = dot(x, w[0], 1, 0), dot(x, w[1], 1, 0)
    value = dot(x, w[2], 1, 0).astype(BF16)
    pre[0, 0], pre[1, 0] = q_pre, k_pre
    low[2, 0] = value
    for h in range(q_pre.shape[1] // HEAD_DIM):
        cols = slice(h * HEAD_DIM, (h + 1) * HEAD_DIM)
        rot = []
        for i, (u, g) in enumerate(((q_pre[:, cols], qg[...]), (k_pre[:, cols], kg[...]))):
            rot.append(rope(u * inverse_rms(u) * g, cos[...], sin[...]).astype(BF16))
            low[i, 0, :, cols] = rot[i]
        attention = probabilities(rot[0], rot[1], length).astype(BF16)
        ctx[0, :, cols] = dot(attention, value[:, cols], 1, 0).astype(BF16)
    part[0] = dot(ctx[0], wo[...], 1, 0).astype(BF16)


def attend(full, weights, wo, gain, qg, kg, cos, sin, lens):
    seqs, length, width = full.shape
    cols = weights.shape[2]
    row = lambda i, *_: (i, 0, 0)
    row2 = lambda i, *_: (0, i, 0, 0)
    two = lambda i, *_: (0, 0)
    return pl.pallas_call(
        attend_kernel,
        out_shape=(
            sds(full.shape, BF16),
            sds((2, seqs, length, cols), F32),
            sds((3, seqs, length, cols), BF16),
            sds((seqs, length, cols), BF16),
            sds(full.shape, BF16),
        ),
        grid_spec=pltpu.PrefetchScalarGridSpec(
            num_scalar_prefetch=1,
            grid=(seqs,),
            in_specs=[
                pl.BlockSpec((1, length, width), row),
                pl.BlockSpec(weights.shape, lambda i, *_: (0, 0, 0)),
                pl.BlockSpec(wo.shape, two),
                pl.BlockSpec((1, width), two),
                pl.BlockSpec((1, HEAD_DIM), two),
                pl.BlockSpec((1, HEAD_DIM), two),
                pl.BlockSpec((length, HEAD_DIM), two),
                pl.BlockSpec((length, HEAD_DIM), two),
            ],
            out_specs=(
                pl.BlockSpec((1, length, width), row),
                pl.BlockSpec((2, 1, length, cols), row2),
                pl.BlockSpec((3, 1, length, cols), row2),
                pl.BlockSpec((1, length, cols), row),
                pl.BlockSpec((1, length, width), row),
            ),
        ),
        compiler_params=pltpu.CompilerParams(dimension_semantics=("arbitrary",), vmem_limit_bytes=60 << 20),
        cost_estimate=pl.CostEstimate(flops=10**10, bytes_accessed=4 * 10**7, transcendentals=10**6),
        name="attend",
    )(lens, full, weights, wo, gain, qg, kg, cos, sin)


def attend_back_kernel(
    lens, agrad, normed, pre, low, ctx, w, wo, qg, kg, cos, sin, part, wgrad, wograd, gains, wacc, woacc
):
    s = pl.program_id(0)
    length = lens[s]

    @pl.when(s == 0)
    def _():
        wacc[...] = jnp.zeros_like(wacc)
        woacc[...] = jnp.zeros_like(woacc)
        gains[...] = jnp.zeros_like(gains)

    ag = agrad[0]
    woacc[...] += dot(ctx[0], ag, 0, 0)
    cg_all = dot(ag, wo[...], 1, 1).astype(BF16)
    scale = HEAD_DIM**-0.5
    half = HEAD_DIM // 2
    grads = ([], [], [])
    for h in range(cg_all.shape[1] // HEAD_DIM):
        cols = slice(h * HEAD_DIM, (h + 1) * HEAD_DIM)
        q, k, value, cg = low[0, 0, :, cols], low[1, 0, :, cols], low[2, 0, :, cols], cg_all[:, cols]
        attention = probabilities(q, k, length)
        grads[2].append(dot(attention.astype(BF16), cg, 0, 0).astype(BF16))
        pg = dot(cg, value, 1, 1)
        sg = (attention * (pg - jnp.sum(attention * pg, axis=-1, keepdims=True))).astype(BF16)
        for i, (rot_grad, g) in enumerate(((dot(sg, k, 1, 0), qg[...]), (dot(sg, q, 0, 0), kg[...]))):
            wgt = rot_grad * scale
            u = wgt * cos[...] + pltpu.roll(wgt * sin[...], half, 1)
            v = pre[i, 0, :, cols]
            r = inverse_rms(v)
            grads[i].append(rms_back(v, r, u * g).astype(BF16))
            gains[i : i + 1] += jnp.sum(u * v * r, axis=0, keepdims=True)
    total = None
    for i in range(3):
        g = grads[i][0] if len(grads[i]) == 1 else jnp.concatenate(grads[i], axis=1)
        wacc[i] += dot(normed[0], g, 0, 0)
        piece = dot(g, w[i], 1, 1)
        total = piece if total is None else total + piece
    part[0] = total.astype(BF16)

    @pl.when(s == pl.num_programs(0) - 1)
    def _():
        wgrad[...] = wacc[...].astype(BF16)
        wograd[...] = woacc[...].astype(BF16)


def attend_back(agrad, normed, pre, low, ctx, weights, wo, qg, kg, cos, sin, lens):
    seqs, length, width = agrad.shape
    cols = weights.shape[2]
    row = lambda i, *_: (i, 0, 0)
    row2 = lambda i, *_: (0, i, 0, 0)
    two = lambda i, *_: (0, 0)
    three = lambda i, *_: (0, 0, 0)
    return pl.pallas_call(
        attend_back_kernel,
        out_shape=(
            sds(agrad.shape, BF16),
            sds(weights.shape, BF16),
            sds(wo.shape, BF16),
            sds((8, HEAD_DIM), F32),
        ),
        grid_spec=pltpu.PrefetchScalarGridSpec(
            num_scalar_prefetch=1,
            grid=(seqs,),
            in_specs=[
                pl.BlockSpec((1, length, width), row),
                pl.BlockSpec((1, length, width), row),
                pl.BlockSpec((2, 1, length, cols), row2),
                pl.BlockSpec((3, 1, length, cols), row2),
                pl.BlockSpec((1, length, cols), row),
                pl.BlockSpec(weights.shape, three),
                pl.BlockSpec(wo.shape, two),
                pl.BlockSpec((1, HEAD_DIM), two),
                pl.BlockSpec((1, HEAD_DIM), two),
                pl.BlockSpec((length, HEAD_DIM), two),
                pl.BlockSpec((length, HEAD_DIM), two),
            ],
            out_specs=(
                pl.BlockSpec((1, length, width), row),
                pl.BlockSpec(weights.shape, three),
                pl.BlockSpec(wo.shape, two),
                pl.BlockSpec((8, HEAD_DIM), two),
            ),
            scratch_shapes=[pltpu.VMEM(weights.shape, F32), pltpu.VMEM(wo.shape, F32)],
        ),
        compiler_params=pltpu.CompilerParams(dimension_semantics=("arbitrary",), vmem_limit_bytes=60 << 20),
        cost_estimate=pl.CostEstimate(flops=2 * 10**10, bytes_accessed=4 * 10**7, transcendentals=10**6),
        name="attend_back",
    )(lens, agrad, normed, pre, low, ctx, weights, wo, qg, kg, cos, sin)


def shards(
    tokens, cotangent, gate_weights, expert_ids, seq_lengths, query_weight, key_weight, value_weight,
    output_weight, attn_gain, ffn_gain, query_gain, key_gain, expert_in, expert_out,
):
    ep = lax.axis_size("ep")
    me = lax.axis_index("ep")
    seqs, rows, width = tokens.shape
    length = rows * ep
    top = gate_weights.shape[2]
    local = expert_in.shape[0]
    hidden = expert_out.shape[1]
    experts = local * ep
    capacity = length * top * 9 // (8 * experts)

    pairs = jnp.concatenate(
        [expert_ids.astype(F32).transpose(0, 2, 1), gate_weights.astype(F32).transpose(0, 2, 1)], axis=1
    ).reshape(-1, 128)
    gains = jnp.concatenate([attn_gain, ffn_gain]).astype(F32).reshape(-1, 128)
    few = jnp.concatenate([query_gain.astype(F32), key_gain.astype(F32), seq_lengths.astype(F32)])
    few = jnp.pad(few, (0, 128 - few.shape[0]))[None]
    packet = jnp.concatenate([pairs, gains, few], axis=0)
    packet = jnp.pad(packet, ((0, -packet.shape[0] % 8), (0, 0)))

    full, weights, packets = front(tokens, query_weight, key_weight, value_weight, packet)
    cot_full = lax.all_gather(cotangent, "ep", axis=1, tiled=True)

    n = pairs.shape[0]
    g = gains.shape[0] // 2
    gain_attn = packets[:, n : n + g].reshape(1, width)
    gain_ffn = packets[:, n + g : n + 2 * g].reshape(1, width)
    q = query_gain.shape[0]
    gain_query = packets[:, n + 2 * g, :q].reshape(1, HEAD_DIM)
    gain_key = packets[:, n + 2 * g, q : 2 * q].reshape(1, HEAD_DIM)
    lens = packets[:, n + 2 * g, 2 * q].astype(jnp.int32)
    table = packets[:, :n].reshape(ep, seqs, 2 * top, rows).transpose(1, 2, 0, 3).reshape(seqs, 2 * top, length)
    positions = jnp.arange(length, dtype=jnp.int32)
    live = (positions[None] < lens[:, None]).astype(F32)
    living = lax.dynamic_slice_in_dim(live, me * rows, rows, axis=1)[..., None]

    half = HEAD_DIM // 2
    frequency = ROPE_BASE ** (-(jnp.arange(half, dtype=F32) * (2.0 / HEAD_DIM)))
    angles = positions.astype(F32)[:, None] * frequency[None, :]
    cos = jnp.concatenate([jnp.cos(angles)] * 2, axis=-1)
    sin = jnp.concatenate([-jnp.sin(angles), jnp.sin(angles)], axis=-1)

    normed, pre, low, ctx, part = attend(
        full, weights, output_weight, gain_attn, gain_query, gain_key, cos, sin, lens
    )
    middle, mixed = mix(part, tokens, living, gain_ffn)

    mine = (me * local + jnp.arange(local)).astype(F32)
    chosen = (table[None, :, :top] == mine[:, None, None, None]).astype(F32)
    hit = jnp.sum(chosen, axis=2) * live[None]
    weight = jnp.sum(chosen * table[None, :, top:], axis=2) * live[None]
    before = (positions[:, None] < positions[None, :]).astype(BF16)
    rank = jnp.dot(hit.astype(BF16), before, preferred_element_type=F32)
    slot = jnp.where(hit > 0.5, rank, -1.0)
    place = slot[:, :, None, :] == jnp.arange(capacity, dtype=F32)[None, None, :, None]
    pick = place.astype(BF16)
    weighted = jnp.where(place, weight[:, :, None, :], 0.0).astype(BF16)

    def ein(spec, a, b):
        return jnp.einsum(spec, a, b, preferred_element_type=F32)

    slots = seqs * capacity
    arrived = ein("jsrt,std->jsrd", pick, mixed).astype(BF16).reshape(local, slots, width)
    arrived_grad = ein("jsrt,std->jsrd", weighted, cot_full).astype(BF16).reshape(local, slots, width)
    in_grads, out_grads, acts, dgus = [], [], [], []
    token = None
    for j in range(local):
        x, dy = arrived[j], arrived_grad[j]
        if token is not None:
            x, dy, _ = lax.optimization_barrier((x, dy, token))
        gate_up = jnp.dot(x, expert_in[j], preferred_element_type=F32)
        dact = dot(dy, expert_out[j], 1, 1)
        gate, up = gate_up[:, :hidden], gate_up[:, hidden:]
        sig = jax.nn.sigmoid(gate)
        act = (gate * sig * up).astype(BF16)
        dgu = jnp.concatenate(
            [dact * up * sig * (1.0 + gate * (1.0 - sig)), dact * gate * sig], axis=1
        ).astype(BF16)
        out_grad = dot(act, dy, 0, 0).astype(BF16)
        in_grad = dot(x, dgu, 0, 0).astype(BF16)
        out_grad, in_grad, act, dgu = lax.optimization_barrier((out_grad, in_grad, act, dgu))
        token = act
        out_grads.append(lax.psum_scatter(out_grad, "rep", scatter_dimension=0, tiled=True))
        in_grads.append(lax.psum_scatter(in_grad, "rep", scatter_dimension=0, tiled=True))
        acts.append(act)
        dgus.append(dgu)
    out_parts = [jnp.dot(a, expert_out[j], preferred_element_type=F32).astype(BF16) for j, a in enumerate(acts)]
    grad_parts = [dot(d, expert_in[j], 1, 1).astype(BF16) for j, d in enumerate(dgus)]
    stack = lambda parts: jnp.stack(parts).reshape(local, seqs, capacity, width)
    grad_part = ein("jsrt,jsrd->std", pick, stack(grad_parts)).astype(BF16)
    out_part = ein("jsrt,jsrd->std", weighted, stack(out_parts)).astype(BF16)

    result, mgrad, ffn_back, agrad = back(grad_part, out_part, middle, cotangent, living, gain_ffn)
    npart, wgrad, wograd, qk_back = attend_back(
        agrad, normed, pre, low, ctx, weights, output_weight, gain_query, gain_key, cos, sin, lens
    )
    token_grad, attn_back, wrows = final(npart, wgrad, tokens, mgrad, gain_attn)
    sums = lax.psum((wrows, wograd), "rep")
    small = jnp.concatenate([attn_back[0], ffn_back[0], qk_back[0], qk_back[1]])
    small = lax.psum(small, ("rep", "ep"))

    def share(vector):
        return lax.dynamic_slice_in_dim(vector, me * (vector.shape[0] // ep), vector.shape[0] // ep)

    return (
        result,
        token_grad,
        sums[0][0].astype(F32),
        sums[0][1].astype(F32),
        sums[0][2].astype(F32),
        sums[1].astype(F32),
        share(small[:width]),
        share(small[width : 2 * width]),
        share(small[2 * width : 2 * width + HEAD_DIM]),
        share(small[2 * width + HEAD_DIM :]),
        jnp.stack(in_grads).astype(F32),
        jnp.stack(out_grads).astype(F32),
    )


def solution(mesh):
    seq = P("rep", "ep", None)
    row, gain, expert = P("ep", None), P("ep"), P("ep", None, None)
    split = P("ep", "rep", None)

    return jax.shard_map(
        shards,
        mesh=mesh,
        in_specs=(seq, seq, seq, seq, P(("rep", "ep")), row, row, row, row, gain, gain, gain, gain, expert, expert),
        out_specs=(seq, seq, row, row, row, row, gain, gain, gain, gain, split, split),
        check_vma=False,
    )
```

```python
import functools

import jax
import jax.numpy as jnp
from jax import lax
from jax.experimental import pallas as pl
from jax.experimental.pallas import tpu as pltpu
from jax.sharding import PartitionSpec as P

HEAD_DIM = 128
EPS = 1e-06
ROPE_BASE = 50000.0
MESH = pl.DeviceIdType.MESH
F32 = jnp.float32
BF16 = jnp.bfloat16


def sds(shape, dtype):
    return jax.ShapeDtypeStruct(shape, dtype)


VM = pl.BlockSpec(memory_space=pltpu.VMEM)
AN = pl.BlockSpec(memory_space=pl.ANY)


def inverse_rms(v):
    return lax.rsqrt(jnp.mean(v * v, axis=-1, keepdims=True) + EPS)


def rms_back(v, r, ug):
    return r * ug - v * (r * r * r * jnp.mean(ug * v, axis=-1, keepdims=True))


def mix_rows(total, tok, living, gain):
    middle = tok.astype(F32) + living * total
    mixed = middle * inverse_rms(middle) * gain
    return middle, mixed.astype(BF16)


def ffn_back_rows(mixed_grad, middle, cot, living, gain):
    r = inverse_rms(middle)
    middle_grad = cot.astype(F32) + rms_back(middle, r, mixed_grad * gain)
    return middle_grad, (living * middle_grad).astype(BF16), mixed_grad * middle * r


def attn_back_rows(normed_grad, tok, middle_grad, gain):
    v = tok.astype(F32)
    r = inverse_rms(v)
    return (middle_grad + rms_back(v, r, normed_grad * gain)).astype(BF16), normed_grad * v * r


class Place:
    def __init__(self):
        me = lax.axis_index("ep")
        core, x, y = lax.rem(me, 2), lax.rem(me // 2, 2), me // 4
        self.rep = lax.axis_index("rep")
        self.me = me
        self.sb = me + 1 - 2 * core
        self.dx = 2 - 4 * x
        self.dy = 4 - 8 * y
        self.xn = me + self.dx
        self.yn = me + self.dy
        self.dg = me + self.dx + self.dy

    def push(self, src, dst, send, recv, dev):
        return pltpu.make_async_remote_copy(
            src_ref=src, dst_ref=dst, send_sem=send, recv_sem=recv, device_id=(self.rep, dev), device_id_type=MESH
        )

    def peers(self):
        sb, dx, dy = self.sb, self.dx, self.dy
        return (self.xn, self.yn, self.dg, sb, sb + dx, sb + dy, sb + dx + dy)

    def greet(self, peers):
        barrier = pltpu.get_barrier_semaphore()
        for peer in peers:
            pl.semaphore_signal(barrier, inc=1, device_id=(self.rep, peer), device_id_type=MESH)
        pl.semaphore_wait(barrier, len(peers))


class Gather:
    sems = 3

    def __init__(self, at, own, full, ssem, rsem, lsem):
        self.at, self.own, self.full, self.ssem, self.rsem, self.lsem = at, own, full, ssem, rsem, lsem
        self.rows = own.shape[1]

    @staticmethod
    def scratch(seqs):
        return [pltpu.SemaphoreType.DMA((7, seqs)), pltpu.SemaphoreType.DMA((8, seqs)), pltpu.SemaphoreType.DMA((seqs,))]

    def block(self, s, dev):
        return self.full.at[s, pl.ds(pl.multiple_of(dev * self.rows, self.rows), self.rows)]

    def copy(self, s, dev, kind, slot, to, src=None):
        block = self.block(s, dev)
        return self.at.push(block if src is None else src, block, self.ssem.at[kind, s], self.rsem.at[slot, s], to)

    def start(self, s):
        at, own = self.at, self.own.at[s]
        self.copy(s, at.me, 0, 2, at.xn, own).start()
        self.copy(s, at.me, 1, 4, at.yn, own).start()
        self.copy(s, at.me, 2, 1, at.sb, own).start()
        pltpu.make_async_copy(own, self.block(s, at.me), self.lsem.at[s]).start()

    def relay(self, s, by_y):
        at = self.at
        self.copy(s, at.xn, 0, 2, at.xn).wait_recv()
        if by_y:
            self.copy(s, at.xn, 3, 6, at.yn).start()
        self.copy(s, at.xn, 4, 3, at.sb).start()
        self.copy(s, at.yn, 1, 4, at.yn).wait_recv()
        if not by_y:
            self.copy(s, at.yn, 3, 6, at.xn).start()
        self.copy(s, at.yn, 5, 5, at.sb).start()

    def relay_far(self, s):
        at = self.at
        self.copy(s, at.dg, 3, 6, at.yn).wait_recv()
        self.copy(s, at.dg, 6, 7, at.sb).start()

    def finish(self, s):
        at = self.at
        for dev, slot in ((at.sb, 1), (at.sb + at.dx, 3), (at.sb + at.dy, 5), (at.sb + at.dx + at.dy, 7)):
            self.copy(s, dev, 0, slot, at.sb).wait_recv()
        for kind in range(7):
            self.copy(s, at.me, kind, 0, at.sb).wait_send()
        pltpu.make_async_copy(self.own.at[s], self.block(s, at.me), self.lsem.at[s]).wait()


def gather_tail(seqs, gather):
    def relay(i, _):
        gather.relay(2 * i, True)
        gather.relay(2 * i + 1, False)
        return 0

    def far(s, _):
        gather.relay_far(s)
        return 0

    def finish(s, _):
        gather.finish(s)
        return 0

    lax.fori_loop(0, seqs // 2, relay, 0)
    lax.fori_loop(0, seqs, far, 0)
    lax.fori_loop(0, seqs, finish, 0)


class Reduce:
    def __init__(self, at, part, held, x1, y1, x2, y2, hs, hr, d1s, d1r, d2s, d2r):
        self.at, self.part, self.held = at, part, held
        self.x1, self.y1, self.x2, self.y2 = x1, y1, x2, y2
        self.hs, self.hr, self.d1s, self.d1r, self.d2s, self.d2r = hs, hr, d1s, d1r, d2s, d2r
        self.half = part.shape[2] // 2

    @staticmethod
    def scratch(part):
        s, _, t, d = part.shape
        dma = pltpu.SemaphoreType.DMA
        return [
            pltpu.VMEM((s, 4, t, d), BF16),
            pltpu.VMEM((s, t // 2, d), BF16),
            pltpu.VMEM((s, t // 2, d), BF16),
            pltpu.VMEM((s, t, d), BF16),
            pltpu.VMEM((s, t, d), BF16),
            dma((4, s)),
            dma((4, s)),
            dma((2, s)),
            dma((2, s)),
            dma((2, s)),
            dma((2, s)),
        ]

    sems = 11

    def core_copy(self, s, k):
        at = self.at
        dest = (at.sb, at.sb + at.dx, at.sb + at.dy, at.sb + at.dx + at.dy)[k]
        return at.push(self.part.at[s, dest], self.held.at[s, k], self.hs.at[k, s], self.hr.at[k, s], at.sb)

    def first(self, s, k):
        at, h = self.at, self.half
        src = self.held.at[s, 3, pl.ds(k * h, h)]
        return at.push(src, (self.x1, self.y1)[k].at[s], self.d1s.at[k, s], self.d1r.at[k, s], (at.xn, at.yn)[k])

    def second(self, s, k):
        at = self.at
        src = self.held.at[s, 1 + k]
        return at.push(src, (self.x2, self.y2)[k].at[s], self.d2s.at[k, s], self.d2r.at[k, s], (at.xn, at.yn)[k])

    def start(self, s):
        for k in (3, 1, 2, 0):
            self.core_copy(s, k).start()

    def hop1(self, s):
        self.core_copy(s, 3).wait_recv()
        self.held[s, 3] = (self.held[s, 3].astype(F32) + self.part[s, self.at.dg].astype(F32)).astype(BF16)
        self.first(s, 0).start()
        self.first(s, 1).start()

    def hop2(self, s):
        h = self.half
        for k, dest, extra, rows, rest in (
            (0, self.at.xn, self.y1, pl.ds(h, h), pl.ds(0, h)),
            (1, self.at.yn, self.x1, pl.ds(0, h), pl.ds(h, h)),
        ):
            self.core_copy(s, 1 + k).wait_recv()
            self.first(s, 1 - k).wait_recv()
            held, part = self.held.at[s, 1 + k], self.part.at[s, dest]
            held[rows] = (held[rows].astype(F32) + part[rows].astype(F32) + extra[s].astype(F32)).astype(BF16)
            held[rest] = (held[rest].astype(F32) + part[rest].astype(F32)).astype(BF16)
            self.second(s, k).start()

    def total(self, s):
        self.core_copy(s, 0).wait_recv()
        self.second(s, 0).wait_recv()
        self.second(s, 1).wait_recv()
        return (
            self.part[s, self.at.me].astype(F32)
            + self.held[s, 0].astype(F32)
            + self.x2[s].astype(F32)
            + self.y2[s].astype(F32)
        )

    def finish(self, s):
        for k in range(4):
            self.core_copy(s, k).wait_send()
        for k in range(2):
            self.first(s, k).wait_send()
            self.second(s, k).wait_send()


def each(n, *steps):
    def run(s, _):
        for step in steps:
            step(s)
        return 0

    lax.fori_loop(0, n, run, 0)


COMM = dict(has_side_effects=True, vmem_limit_bytes=60 << 20)


def front_kernel(tok, wq, wk, wv, pk, full, weights, packets, tok_v, *sems):
    at = Place()
    gather = Gather(at, tok, full, *sems[:3])
    wsend, wrecv, psend, precv, local = sems[3:]
    seqs = tok.shape[0]
    block, width = wq.shape[0], weights.shape[2]
    at.greet(at.peers())
    each(seqs, gather.start)
    mine = pl.ds(pl.multiple_of(at.me * block, block), block)

    def weight_copy(m, j, dev):
        cols = pl.ds(pl.multiple_of(dev * width, width), width)
        return at.push((wq, wk, wv)[j].at[:, cols], weights.at[j, mine], wsend.at[m, j], wrecv.at[m, j], dev)

    def packet_copy(m, dev):
        return at.push(pk, packets.at[at.me], psend.at[m], precv.at[m], dev)

    own_cols = pl.ds(pl.multiple_of(at.me * width, width), width)
    own = [pltpu.make_async_copy(w.at[:, own_cols], weights.at[j, mine], local.at[j]) for j, w in enumerate((wq, wk, wv))]
    own.append(pltpu.make_async_copy(pk, packets.at[at.me], local.at[3]))
    for copy in own:
        copy.start()
    for m, dev in enumerate(at.peers()):
        packet_copy(m, dev).start()
    for m, dev in enumerate(at.peers()):
        for j in range(3):
            weight_copy(m, j, dev).start()
    gather_tail(seqs, gather)
    for m, dev in enumerate(at.peers()):
        packet_copy(m, dev).wait()
        for j in range(3):
            weight_copy(m, j, dev).wait()
    for copy in own:
        copy.wait()


def front(tokens, wq, wk, wv, packet):
    seqs, rows, width = tokens.shape
    ep = lax.axis_size("ep")
    cols = wq.shape[1] // ep
    if ep != 8:
        full = lax.all_gather(tokens, "ep", axis=1, tiled=True)
        weights = [lax.all_to_all(w, "ep", split_axis=1, concat_axis=0, tiled=True) for w in (wq, wk, wv)]
        return full, jnp.stack(weights), lax.all_gather(packet, "ep", axis=0)
    dma = pltpu.SemaphoreType.DMA
    return pl.pallas_call(
        front_kernel,
        out_shape=(
            sds((seqs, rows * ep, width), BF16),
            sds((3, wq.shape[0] * ep, cols), BF16),
            sds((ep,) + packet.shape, F32),
        ),
        in_specs=[VM] * 5,
        out_specs=(AN, AN, AN),
        scratch_shapes=[pltpu.VMEM((8, 128), F32)]
        + Gather.scratch(seqs)
        + [dma((7, 3)), dma((7, 3)), dma((7,)), dma((7,)), dma((4,))],
        compiler_params=pltpu.CompilerParams(collective_id=1, **COMM),
        name="front",
    )(tokens, wq, wk, wv, packet)


def mix_kernel(part, tok, living, gain, middle, full, own, *scratch):
    at = Place()
    seqs = tok.shape[0]
    reduce = Reduce(at, part, *scratch[: Reduce.sems])
    gather = Gather(at, own, full, *scratch[Reduce.sems :])
    at.greet((at.xn, at.yn, at.sb))
    each(seqs, reduce.start)
    each(seqs, reduce.hop1)
    each(seqs, reduce.hop2)

    def rows(s):
        mid, mixed = mix_rows(reduce.total(s), tok[s], living[s], gain[...])
        middle[s] = mid
        own[s] = mixed
        gather.start(s)

    each(seqs, rows)
    gather_tail(seqs, gather)
    each(seqs, reduce.finish)


def mix(part, tokens, living, gain):
    seqs, rows, width = tokens.shape
    ep = lax.axis_size("ep")
    if ep != 8:
        total = lax.psum_scatter(part, "ep", scatter_dimension=1, tiled=True).astype(F32)
        middle, mixed = mix_rows(total, tokens, living, gain)
        return middle, lax.all_gather(mixed, "ep", axis=1, tiled=True)
    part = part.reshape(seqs, ep, rows, width)
    return pl.pallas_call(
        mix_kernel,
        out_shape=(sds(tokens.shape, F32), sds((seqs, rows * ep, width), BF16)),
        in_specs=[VM] * 4,
        out_specs=(VM, AN),
        scratch_shapes=[pltpu.VMEM(tokens.shape, BF16)] + Reduce.scratch(part) + Gather.scratch(seqs),
        compiler_params=pltpu.CompilerParams(collective_id=2, **COMM),
        name="mix",
    )(part, tokens, living, gain)


def back_kernel(gpart, opart, middle, cot, living, gain, result, mgrad, ggrad, full, own, *scratch):
    at = Place()
    seqs = cot.shape[0]
    n = Reduce.sems
    rg = Reduce(at, gpart, *scratch[:n])
    ro = Reduce(at, opart, *scratch[n : 2 * n])
    gather = Gather(at, own, full, *scratch[2 * n :])
    at.greet((at.xn, at.yn, at.sb))
    each(seqs, rg.start)
    each(seqs, ro.start)
    each(seqs, rg.hop1)
    each(seqs, rg.hop2)
    ggrad[...] = jnp.zeros_like(ggrad)

    def rows(s):
        mg, ag, back = ffn_back_rows(rg.total(s), middle[s], cot[s], living[s], gain[...])
        mgrad[s] = mg
        own[s] = ag
        ggrad[...] += jnp.sum(back, axis=0, keepdims=True)
        gather.start(s)

    each(seqs, rows)
    gather_tail(seqs, gather)
    each(seqs, ro.hop1)
    each(seqs, ro.hop2)

    def out(s):
        result[s] = (middle[s] + ro.total(s)).astype(BF16)

    each(seqs, out)
    each(seqs, rg.finish, ro.finish)


def back(gpart, opart, middle, cot, living, gain):
    seqs, rows, width = cot.shape
    ep = lax.axis_size("ep")
    if ep != 8:
        mixed_grad = lax.psum_scatter(gpart, "ep", scatter_dimension=1, tiled=True).astype(F32)
        moe = lax.psum_scatter(opart, "ep", scatter_dimension=1, tiled=True).astype(F32)
        mg, ag, backs = ffn_back_rows(mixed_grad, middle, cot, living, gain)
        full = lax.all_gather(ag, "ep", axis=1, tiled=True)
        return (middle + moe).astype(BF16), mg, jnp.sum(backs, axis=(0, 1))[None], full
    gpart, opart = (p.reshape(seqs, ep, rows, width) for p in (gpart, opart))
    return pl.pallas_call(
        back_kernel,
        out_shape=(
            sds(cot.shape, BF16),
            sds(cot.shape, F32),
            sds((1, width), F32),
            sds((seqs, rows * ep, width), BF16),
        ),
        in_specs=[VM] * 6,
        out_specs=(VM, VM, VM, AN),
        scratch_shapes=[pltpu.VMEM(cot.shape, BF16)] + 2 * Reduce.scratch(gpart) + Gather.scratch(seqs),
        compiler_params=pltpu.CompilerParams(collective_id=3, **COMM),
        name="back",
    )(gpart, opart, middle, cot, living, gain)


def final_kernel(part, wgrad, tok, mgrad, gain, others, tgrad, small, wrows, ggrad, parcel, landed, *scratch):
    at = Place()
    seqs = tok.shape[0]
    n = Reduce.sems
    reduce = Reduce(at, part, *scratch[:n])
    wsend, wrecv, local, gsend, grecv = scratch[n:]
    width = wgrad.shape[2]
    block = wrows.shape[1]
    at.greet(at.peers())
    cols = pl.ds(pl.multiple_of(at.me * width, width), width)

    def weight_copy(m, dev):
        rows = pl.ds(pl.multiple_of(dev * block, block), block)
        return at.push(wgrad.at[:, rows], wrows.at[:, :, cols], wsend.at[m], wrecv.at[m], dev)

    mine = pl.ds(pl.multiple_of(at.me * block, block), block)
    own = pltpu.make_async_copy(wgrad.at[:, mine], wrows.at[:, :, cols], local)
    own.start()
    for m, dev in enumerate(at.peers()):
        weight_copy(m, dev).start()
    each(seqs, reduce.start)
    each(seqs, reduce.hop1)
    each(seqs, reduce.hop2)
    ggrad[...] = jnp.zeros_like(ggrad)

    def rows(s):
        tg, back = attn_back_rows(reduce.total(s), tok[s], mgrad[s], gain[...])
        tgrad[s] = tg
        ggrad[...] += jnp.sum(back, axis=0, keepdims=True)

    each(seqs, rows)

    parcel[...] = jnp.zeros_like(parcel)
    devices = parcel.shape[0]
    rows_of = ggrad.shape[1] // (128 * devices)
    for dev in range(devices):
        for k in range(rows_of):
            lanes = pl.ds((dev * rows_of + k) * 128, 128)
            parcel[dev, k : k + 1] = ggrad[:, lanes]
            parcel[dev, rows_of + k : rows_of + k + 1] = others[0:1, lanes]
        parcel[dev, 2 * rows_of : 2 * rows_of + 2] = others[1:3, 0:128]

    def parcel_copy(m, dev):
        return at.push(parcel.at[dev], landed.at[m], gsend.at[m], grecv.at[m], dev)

    for m, dev in enumerate(at.peers()):
        parcel_copy(m, dev).start()
    total = parcel[at.me]
    for m, dev in enumerate(at.peers()):
        parcel_copy(m, dev).wait_recv()
        total = total + landed[m]
    small[...] = total
    each(seqs, reduce.finish)
    for m, dev in enumerate(at.peers()):
        weight_copy(m, dev).wait()
        parcel_copy(m, dev).wait_send()
    own.wait()


def final(part, wgrad, tokens, mgrad, gain, ffn_back, qk_back):
    seqs, rows, width = tokens.shape
    ep = lax.axis_size("ep")
    if ep != 8:
        normed_grad = lax.psum_scatter(part, "ep", scatter_dimension=1, tiled=True).astype(F32)
        tg, backs = attn_back_rows(normed_grad, tokens, mgrad, gain)
        wrows = lax.all_to_all(wgrad, "ep", split_axis=1, concat_axis=2, tiled=True)
        share = width // ep
        small = jnp.concatenate([jnp.sum(backs, axis=(0, 1)), ffn_back[0], qk_back[0], qk_back[1]])
        small = lax.psum(small, "ep")
        mine = lax.axis_index("ep") * share
        cut = [lax.dynamic_slice_in_dim(small, k * width + mine, share).reshape(-1, 128) for k in range(2)]
        small = jnp.concatenate(cut + [small[2 * width :].reshape(2, HEAD_DIM)], axis=0)
        return tg, jnp.pad(small, ((0, 8 - small.shape[0]), (0, 0))), wrows
    others = jnp.concatenate([ffn_back, jnp.pad(qk_back[:2], ((0, 0), (0, width - HEAD_DIM)))], axis=0)
    part = part.reshape(seqs, ep, rows, width)
    dma = pltpu.SemaphoreType.DMA
    return pl.pallas_call(
        final_kernel,
        out_shape=(
            sds(tokens.shape, BF16),
            sds((8, 128), F32),
            sds((3, wgrad.shape[1] // ep, wgrad.shape[2] * ep), BF16),
        ),
        in_specs=[VM] * 6,
        out_specs=(VM, VM, AN),
        scratch_shapes=[pltpu.VMEM((1, width), F32), pltpu.VMEM((ep, 8, 128), F32), pltpu.VMEM((7, 8, 128), F32)]
        + Reduce.scratch(part)
        + [dma((7,)), dma((7,)), dma, dma((7,)), dma((7,))],
        compiler_params=pltpu.CompilerParams(collective_id=4, **COMM),
        name="final",
    )(part, wgrad, tokens, mgrad, gain, others)


def line_kernel(own, small, out, small_out, right, left, landed, rs, rr, ls, lr, gs, gr, hs, hr, ss, sr):
    z = lax.axis_index("rep")
    ep = lax.axis_index("ep")
    count = 4
    halves = own.shape[2]
    chunks = own.shape[0] * halves

    def part(ref, c, q):
        return ref.at[c // halves, q, lax.rem(c, halves)]

    def push(src, dst, send, recv, dev):
        return pltpu.make_async_remote_copy(
            src_ref=src, dst_ref=dst, send_sem=send, recv_sem=recv, device_id=(dev, ep), device_id_type=MESH
        )

    barrier = pltpu.get_barrier_semaphore()
    others = [lax.rem(z + k, count) for k in range(1, count)]
    for dev in others:
        pl.semaphore_signal(barrier, inc=1, device_id=(dev, ep), device_id_type=MESH)
    pl.semaphore_wait(barrier, count - 1)

    def small_copy(k):
        return push(small, landed.at[k], ss.at[k], sr.at[k], others[k])

    for k in range(count - 1):
        small_copy(k).start()

    def to_right(c, q):
        return push(part(right, c, q), part(right, c, q), rs.at[c, q], rr.at[c, q], z + 1)

    def to_left(c, q):
        return push(part(left, c, q), part(left, c, q), ls.at[c, q], lr.at[c, q], z - 1)

    def give_right(c, q):
        return push(part(out, c, q), part(out, c, q), gs.at[c, q], gr.at[c, q], z + 1)

    def give_left(c, q):
        return push(part(out, c, q), part(out, c, q), hs.at[c, q], hr.at[c, q], z - 1)

    def load(ref, c, q):
        return part(ref, c, q)[...].astype(F32)

    def add(held, c, q, first):
        @pl.when(first)
        def _():
            part(held, c, q)[...] = part(own, c, q)[...]

        @pl.when(jnp.logical_not(first))
        def _():
            part(held, c, q)[...] = (load(held, c, q) + load(own, c, q)).astype(BF16)

    def walk(c):
        for step in range(count - 1):
            q = count - 1 - step

            @pl.when(z < q)
            def _():
                @pl.when(z > 0)
                def _():
                    to_right(c, q).wait_recv()

                add(right, c, q, z == 0)
                to_right(c, q).start()

            @pl.when(z > step)
            def _():
                @pl.when(z < count - 1)
                def _():
                    to_left(c, step).wait_recv()

                add(left, c, step, z == count - 1)
                to_left(c, step).start()


    def total(c):
        @pl.when(z > 0)
        def _():
            to_right(c, z).wait_recv()

        @pl.when(z < count - 1)
        def _():
            to_left(c, z).wait_recv()

        @pl.when(z == 0)
        def _():
            part(out, c, z)[...] = (load(own, c, z) + load(left, c, z)).astype(BF16)

        @pl.when(z == count - 1)
        def _():
            part(out, c, z)[...] = (load(own, c, z) + load(right, c, z)).astype(BF16)

        @pl.when(jnp.logical_and(z > 0, z < count - 1))
        def _():
            part(out, c, z)[...] = (load(own, c, z) + load(left, c, z) + load(right, c, z)).astype(BF16)

        @pl.when(z < count - 1)
        def _():
            give_right(c, z).start()

        @pl.when(z > 0)
        def _():
            give_left(c, z).start()


    def spread(c):
        for d in range(1, count):

            @pl.when(z >= d)
            def _():
                give_right(c, z - d).wait_recv()

                @pl.when(z < count - 1)
                def _():
                    give_right(c, z - d).start()

            @pl.when(z + d < count)
            def _():
                give_left(c, z + d).wait_recv()

                @pl.when(z > 0)
                def _():
                    give_left(c, z + d).start()

    def run(c, _):
        @pl.when(c < chunks)
        def _():
            walk(c)

        @pl.when(jnp.logical_and(c >= 1, c < chunks + 1))
        def _():
            total(c - 1)

        @pl.when(c >= 2)
        def _():
            spread(c - 2)

        return 0

    lax.fori_loop(0, chunks + 2, run, 0)

    def finish(c):
        for q in range(count):

            @pl.when(z < q)
            def _():
                to_right(c, q).wait_send()

            @pl.when(z > q)
            def _():
                to_left(c, q).wait_send()

            @pl.when(jnp.logical_and(q <= z, z < count - 1))
            def _():
                give_right(c, q).wait_send()

            @pl.when(jnp.logical_and(q >= z, z > 0))
            def _():
                give_left(c, q).wait_send()

    each(chunks, finish)
    total_small = small[...]
    for k in range(count - 1):
        small_copy(k).wait()
        total_small = total_small + landed[k]
    small_out[...] = total_small


def line_sum(big, small):
    if lax.axis_size("rep") != 4 or lax.axis_size("ep") != 8:
        return lax.psum(big, "rep"), lax.psum(small, "rep")
    count, rows, cols = big.shape
    own = big.reshape(count, 4, 2, rows // 8, cols)
    chunks = 2 * count
    dma = pltpu.SemaphoreType.DMA
    out, small = pl.pallas_call(
        line_kernel,
        out_shape=(sds(own.shape, BF16), sds(small.shape, F32)),
        in_specs=[VM, VM],
        out_specs=(VM, VM),
        scratch_shapes=[
            pltpu.VMEM(own.shape, BF16),
            pltpu.VMEM(own.shape, BF16),
            pltpu.VMEM((3,) + small.shape, F32),
        ]
        + [dma((chunks, 4))] * 8
        + [dma((3,))] * 2,
        compiler_params=pltpu.CompilerParams(collective_id=5, has_side_effects=True, vmem_limit_bytes=40 << 20),
        name="line_sum",
    )(own, small)
    return out.reshape(big.shape), small


def dot(a, b, ca, cb):
    return lax.dot_general(a, b, (((ca,), (cb,)), ((), ())), preferred_element_type=F32)


def rope(v, cos, sin_turn):
    return v * cos + pltpu.roll(v, HEAD_DIM // 2, 1) * sin_turn


def probabilities(q, k, length):
    scores = dot(q, k, 1, 1) * HEAD_DIM**-0.5
    column = lax.broadcasted_iota(jnp.int32, scores.shape, 1)
    scores = jnp.where(column < length, scores, -1e9)
    p = jnp.exp(scores - jnp.max(scores, axis=-1, keepdims=True))
    return p * (1.0 / jnp.sum(p, axis=-1, keepdims=True))


def attend_kernel(lens, tok, w, wo, gain, qg, kg, cos, sin, normed, pre, low, ctx, part):
    length = lens[pl.program_id(0)]
    v = tok[0].astype(F32)
    x = (v * inverse_rms(v) * gain[...]).astype(BF16)
    normed[0] = x
    q_pre, k_pre = dot(x, w[0], 1, 0), dot(x, w[1], 1, 0)
    value = dot(x, w[2], 1, 0).astype(BF16)
    pre[0, 0], pre[1, 0] = q_pre, k_pre
    low[2, 0] = value
    for h in range(q_pre.shape[1] // HEAD_DIM):
        cols = slice(h * HEAD_DIM, (h + 1) * HEAD_DIM)
        rot = []
        for i, (u, g) in enumerate(((q_pre[:, cols], qg[...]), (k_pre[:, cols], kg[...]))):
            rot.append(rope(u * inverse_rms(u) * g, cos[...], sin[...]).astype(BF16))
            low[i, 0, :, cols] = rot[i]
        attention = probabilities(rot[0], rot[1], length).astype(BF16)
        ctx[0, :, cols] = dot(attention, value[:, cols], 1, 0).astype(BF16)
    part[0] = dot(ctx[0], wo[...], 1, 0).astype(BF16)


def attend(full, weights, wo, gain, qg, kg, cos, sin, lens):
    seqs, length, width = full.shape
    cols = weights.shape[2]
    row = lambda i, *_: (i, 0, 0)
    row2 = lambda i, *_: (0, i, 0, 0)
    two = lambda i, *_: (0, 0)
    return pl.pallas_call(
        attend_kernel,
        out_shape=(
            sds(full.shape, BF16),
            sds((2, seqs, length, cols), F32),
            sds((3, seqs, length, cols), BF16),
            sds((seqs, length, cols), BF16),
            sds(full.shape, BF16),
        ),
        grid_spec=pltpu.PrefetchScalarGridSpec(
            num_scalar_prefetch=1,
            grid=(seqs,),
            in_specs=[
                pl.BlockSpec((1, length, width), row),
                pl.BlockSpec(weights.shape, lambda i, *_: (0, 0, 0)),
                pl.BlockSpec(wo.shape, two),
                pl.BlockSpec((1, width), two),
                pl.BlockSpec((1, HEAD_DIM), two),
                pl.BlockSpec((1, HEAD_DIM), two),
                pl.BlockSpec((length, HEAD_DIM), two),
                pl.BlockSpec((length, HEAD_DIM), two),
            ],
            out_specs=(
                pl.BlockSpec((1, length, width), row),
                pl.BlockSpec((2, 1, length, cols), row2),
                pl.BlockSpec((3, 1, length, cols), row2),
                pl.BlockSpec((1, length, cols), row),
                pl.BlockSpec((1, length, width), row),
            ),
        ),
        compiler_params=pltpu.CompilerParams(dimension_semantics=("arbitrary",), vmem_limit_bytes=60 << 20),
        cost_estimate=pl.CostEstimate(flops=10**10, bytes_accessed=4 * 10**7, transcendentals=10**6),
        name="attend",
    )(lens, full, weights, wo, gain, qg, kg, cos, sin)


def attend_back_kernel(
    lens, agrad, normed, pre, low, ctx, w, wo, qg, kg, cos, sin, part, wgrad, wograd, gains, wacc, woacc
):
    s = pl.program_id(0)
    length = lens[s]

    @pl.when(s == 0)
    def _():
        wacc[...] = jnp.zeros_like(wacc)
        woacc[...] = jnp.zeros_like(woacc)
        gains[...] = jnp.zeros_like(gains)

    ag = agrad[0]
    woacc[...] += dot(ctx[0], ag, 0, 0)
    cg_all = dot(ag, wo[...], 1, 1).astype(BF16)
    scale = HEAD_DIM**-0.5
    half = HEAD_DIM // 2
    grads = ([], [], [])
    for h in range(cg_all.shape[1] // HEAD_DIM):
        cols = slice(h * HEAD_DIM, (h + 1) * HEAD_DIM)
        q, k, value, cg = low[0, 0, :, cols], low[1, 0, :, cols], low[2, 0, :, cols], cg_all[:, cols]
        attention = probabilities(q, k, length)
        grads[2].append(dot(attention.astype(BF16), cg, 0, 0).astype(BF16))
        pg = dot(cg, value, 1, 1)
        sg = (attention * (pg - jnp.sum(attention * pg, axis=-1, keepdims=True))).astype(BF16)
        for i, (rot_grad, g) in enumerate(((dot(sg, k, 1, 0), qg[...]), (dot(sg, q, 0, 0), kg[...]))):
            wgt = rot_grad * scale
            u = wgt * cos[...] + pltpu.roll(wgt * sin[...], half, 1)
            v = pre[i, 0, :, cols]
            r = inverse_rms(v)
            grads[i].append(rms_back(v, r, u * g).astype(BF16))
            gains[i : i + 1] += jnp.sum(u * v * r, axis=0, keepdims=True)
    total = None
    for i in range(3):
        g = grads[i][0] if len(grads[i]) == 1 else jnp.concatenate(grads[i], axis=1)
        wacc[i] += dot(normed[0], g, 0, 0)
        piece = dot(g, w[i], 1, 1)
        total = piece if total is None else total + piece
    part[0] = total.astype(BF16)

    @pl.when(s == pl.num_programs(0) - 1)
    def _():
        wgrad[...] = wacc[...].astype(BF16)
        wograd[...] = woacc[...].astype(BF16)


def attend_back(agrad, normed, pre, low, ctx, weights, wo, qg, kg, cos, sin, lens):
    seqs, length, width = agrad.shape
    cols = weights.shape[2]
    row = lambda i, *_: (i, 0, 0)
    row2 = lambda i, *_: (0, i, 0, 0)
    two = lambda i, *_: (0, 0)
    three = lambda i, *_: (0, 0, 0)
    return pl.pallas_call(
        attend_back_kernel,
        out_shape=(
            sds(agrad.shape, BF16),
            sds(weights.shape, BF16),
            sds(wo.shape, BF16),
            sds((8, HEAD_DIM), F32),
        ),
        grid_spec=pltpu.PrefetchScalarGridSpec(
            num_scalar_prefetch=1,
            grid=(seqs,),
            in_specs=[
                pl.BlockSpec((1, length, width), row),
                pl.BlockSpec((1, length, width), row),
                pl.BlockSpec((2, 1, length, cols), row2),
                pl.BlockSpec((3, 1, length, cols), row2),
                pl.BlockSpec((1, length, cols), row),
                pl.BlockSpec(weights.shape, three),
                pl.BlockSpec(wo.shape, two),
                pl.BlockSpec((1, HEAD_DIM), two),
                pl.BlockSpec((1, HEAD_DIM), two),
                pl.BlockSpec((length, HEAD_DIM), two),
                pl.BlockSpec((length, HEAD_DIM), two),
            ],
            out_specs=(
                pl.BlockSpec((1, length, width), row),
                pl.BlockSpec(weights.shape, three),
                pl.BlockSpec(wo.shape, two),
                pl.BlockSpec((8, HEAD_DIM), two),
            ),
            scratch_shapes=[pltpu.VMEM(weights.shape, F32), pltpu.VMEM(wo.shape, F32)],
        ),
        compiler_params=pltpu.CompilerParams(dimension_semantics=("arbitrary",), vmem_limit_bytes=60 << 20),
        cost_estimate=pl.CostEstimate(flops=2 * 10**10, bytes_accessed=4 * 10**7, transcendentals=10**6),
        name="attend_back",
    )(lens, agrad, normed, pre, low, ctx, weights, wo, qg, kg, cos, sin)


BLOCK = 256


def pack_rows(seqs, capacity):
    return -(-seqs * capacity // BLOCK) * BLOCK + BLOCK


def expert_kernel(
    capacity, top, j, number, lens, mixed, cot, table, w_in, w_out, slots, starts, act, dgu, out_grad, in_grad,
    x, dy, wi, wo, acts, dgus, acc, stage, wsem, ssem, rsem,
):
    s = pl.program_id(0)
    seqs = pl.num_programs(0)
    length, width = mixed.shape[1:]
    hidden = wo.shape[0]
    loads = [pltpu.make_async_copy(w_in.at[j], wi, wsem.at[0]), pltpu.make_async_copy(w_out.at[j], wo, wsem.at[1])]

    @pl.when(s == 0)
    def _():
        for copy in loads:
            copy.start()
        starts[0] = 0

    tab = table[0].astype(F32)
    lane = lax.broadcasted_iota(jnp.int32, tab.shape, 1)
    row = lax.broadcasted_iota(jnp.int32, tab.shape, 0)
    chosen = jnp.logical_and(jnp.logical_and(tab == number[0].astype(F32), lane < top), row < lens[s])
    chosen = jnp.where(chosen, 1.0, 0.0)
    hit = jnp.sum(chosen, axis=1, keepdims=True)
    weight = jnp.sum(chosen * pltpu.roll(tab, 128 - top, 1), axis=1, keepdims=True)
    later = lax.broadcasted_iota(jnp.int32, (length, length), 0)
    earlier = lax.broadcasted_iota(jnp.int32, (length, length), 1)
    before = jnp.where(earlier < later, 1.0, 0.0).astype(BF16)
    rank = dot(before, jnp.broadcast_to(hit, (length, 128)).astype(BF16), 1, 0)
    slot = jnp.where(hit > 0.5, rank, -1.0)
    slots[0] = jnp.where(lane < 64, slot, weight)
    column = lax.broadcasted_iota(jnp.int32, (length, capacity), 1).astype(F32)
    place = slot[:, 0:1] == column
    start = pl.multiple_of(starts[s], 16)
    span = pl.ds(start, capacity)
    x[span] = dot(jnp.where(place, 1.0, 0.0).astype(BF16), mixed[0], 0, 0).astype(BF16)
    dy[span] = dot(jnp.where(place, weight, 0.0).astype(BF16), cot[0], 0, 0).astype(BF16)
    count = jnp.sum(hit).astype(jnp.int32)
    starts[s + 1] = start + (count + 15) // 16 * 16

    @pl.when(s == seqs - 1)
    def _():
        total = starts[seqs]
        tail = pl.ds(pl.multiple_of(start + capacity, 16), BLOCK)
        x[tail] = jnp.zeros((BLOCK, width), BF16)
        dy[tail] = jnp.zeros((BLOCK, width), BF16)
        blocks = (total + BLOCK - 1) // BLOCK
        for copy in loads:
            copy.wait()
        part = min(hidden, 512)

        def forward(b, _):
            rows = pl.ds(pl.multiple_of(b * BLOCK, BLOCK), BLOCK)
            for h in range(hidden // part):
                gcols, ucols = pl.ds(h * part, part), pl.ds(hidden + h * part, part)
                gate = dot(x[rows], wi[:, gcols], 1, 0)
                up = dot(x[rows], wi[:, ucols], 1, 0)
                dact = dot(dy[rows], wo[gcols], 1, 1)
                sig = 1.0 / (1.0 + jnp.exp(-gate))
                silu = gate * sig
                acts[rows, gcols] = (silu * up).astype(BF16)
                dgus[rows, gcols] = (dact * up * sig * (1.0 + gate * (1.0 - sig))).astype(BF16)
                dgus[rows, ucols] = (dact * silu).astype(BF16)
            return 0

        lax.fori_loop(0, blocks, forward, 0)
        saves = [pltpu.make_async_copy(acts, act, rsem.at[0]), pltpu.make_async_copy(dgus, dgu, rsem.at[1])]
        for copy in saves:
            copy.start()

        tr, tc = acc.shape

        def grads(left, right, result, first):
            down, across = result.shape[0] // tr, result.shape[1] // tc

            def tile(t, _):
                rt, ct = t // across, lax.rem(t, across)
                left_cols = pl.ds(pl.multiple_of(rt * tr, tr), tr)
                right_cols = pl.ds(pl.multiple_of(ct * tc, tc), tc)

                def step(b, _):
                    rows = pl.ds(pl.multiple_of(b * BLOCK, BLOCK), BLOCK)
                    piece = dot(left[rows, left_cols], right[rows, right_cols], 0, 0)

                    @pl.when(b == 0)
                    def _():
                        acc[...] = piece

                    @pl.when(b > 0)
                    def _():
                        acc[...] += piece

                    return 0

                @pl.when(blocks == 0)
                def _():
                    acc[...] = jnp.zeros_like(acc)

                lax.fori_loop(0, blocks, step, 0)
                k = lax.rem(t, 2)
                out = pltpu.make_async_copy(stage.at[k], result.at[left_cols, right_cols], ssem.at[k])

                @pl.when(jnp.logical_or(t >= 2, not first))
                def _():
                    out.wait()

                stage[k] = acc[...].astype(BF16)
                out.start()
                return 0

            lax.fori_loop(0, down * across, tile, 0)

        grads(acts, dy, out_grad, True)
        grads(x, dgus, in_grad, False)
        for k in range(2):
            pltpu.make_async_copy(stage.at[k], in_grad.at[pl.ds(0, tr), pl.ds(0, tc)], ssem.at[k]).wait()
        for copy in saves:
            copy.wait()


def expert_pass(j, number, lens, mixed, cot, w_in, w_out, capacity, top):
    seqs, length, width = mixed.shape
    hidden = w_out.shape[1]
    rows = pack_rows(seqs, capacity)
    dma = pltpu.SemaphoreType.DMA
    kernel = functools.partial(expert_kernel, capacity, top, j)
    seq = lambda i, *_: (i, 0, 0)
    return pl.pallas_call(
        kernel,
        out_shape=(
            sds((seqs, length, 128), F32),
            sds((seqs + 1,), jnp.int32),
            sds((rows, hidden), BF16),
            sds((rows, 2 * hidden), BF16),
            sds((hidden, width), BF16),
            sds((width, 2 * hidden), BF16),
        ),
        grid_spec=pltpu.PrefetchScalarGridSpec(
            num_scalar_prefetch=2,
            grid=(seqs,),
            in_specs=[
                pl.BlockSpec((1, length, width), seq),
                pl.BlockSpec((1, length, width), seq),
                pl.BlockSpec((1, length, 128), lambda i, *_: (i, 0, width // 128)),
                AN,
                AN,
            ],
            out_specs=(
                pl.BlockSpec((1, length, 128), seq),
                pl.BlockSpec(memory_space=pltpu.SMEM),
                AN,
                AN,
                AN,
                AN,
            ),
            scratch_shapes=[
                pltpu.VMEM((rows, width), BF16),
                pltpu.VMEM((rows, width), BF16),
                pltpu.VMEM(w_in.shape[1:], BF16),
                pltpu.VMEM(w_out.shape[1:], BF16),
                pltpu.VMEM((rows, hidden), BF16),
                pltpu.VMEM((rows, 2 * hidden), BF16),
                pltpu.VMEM((min(hidden, 512), min(width, 1024)), F32),
                pltpu.VMEM((2, min(hidden, 512), min(width, 1024)), BF16),
                dma((2,)),
                dma((2,)),
                dma((2,)),
            ],
        ),
        compiler_params=pltpu.CompilerParams(dimension_semantics=("arbitrary",), vmem_limit_bytes=60 << 20),
        cost_estimate=pl.CostEstimate(flops=25 * 10**9, bytes_accessed=6 * 10**7, transcendentals=10**6),
        name="expert_pass",
    )(number, lens, mixed, cot, cot, w_in, w_out)


def tail_kernel(starts, act, dgu, w_in, w_out, produced, dx):
    @pl.when(pl.program_id(0) * BLOCK < starts[starts.shape[0] - 1])
    def _():
        produced[...] = dot(act[...], w_out[...], 1, 0).astype(BF16)
        dx[...] = dot(dgu[...], w_in[...], 1, 1).astype(BF16)


def expert_tail(j, starts, act, dgu, w_in, w_out):
    rows, hidden = act.shape
    width = w_in.shape[1]
    last = starts.shape[0] - 1
    block = lambda i, st: (jnp.maximum(jnp.minimum(i, (st[last] + BLOCK - 1) // BLOCK - 1), 0), 0)
    return pl.pallas_call(
        tail_kernel,
        out_shape=(sds((rows, width), BF16), sds((rows, width), BF16)),
        grid_spec=pltpu.PrefetchScalarGridSpec(
            num_scalar_prefetch=1,
            grid=(rows // BLOCK - 1,),
            in_specs=[
                pl.BlockSpec((BLOCK, hidden), block),
                pl.BlockSpec((BLOCK, 2 * hidden), block),
                pl.BlockSpec((None,) + w_in.shape[1:], lambda i, *_: (j, 0, 0)),
                pl.BlockSpec((None,) + w_out.shape[1:], lambda i, *_: (j, 0, 0)),
            ],
            out_specs=(pl.BlockSpec((BLOCK, width), block), pl.BlockSpec((BLOCK, width), block)),
        ),
        compiler_params=pltpu.CompilerParams(dimension_semantics=("arbitrary",), vmem_limit_bytes=60 << 20),
        cost_estimate=pl.CostEstimate(flops=12 * 10**9, bytes_accessed=3 * 10**7, transcendentals=0),
        name="expert_tail",
    )(starts, act, dgu, w_in, w_out)


def combine_kernel(capacity, local, *refs):
    s = pl.program_id(0)
    starts = refs[:local]
    slots = refs[local : 2 * local]
    produced = refs[2 * local : 3 * local]
    dx = refs[3 * local : 4 * local]
    out_part, grad_part = refs[4 * local :]
    out_sum, grad_sum = None, None
    for j in range(local):
        length = slots[j].shape[1]
        column = lax.broadcasted_iota(jnp.int32, (length, capacity), 1).astype(F32)
        place = slots[j][0, :, 0:1] == column
        span = pl.ds(pl.multiple_of(starts[j][s], 16), capacity)
        held = lax.broadcasted_iota(jnp.int32, (capacity, 1), 0) < starts[j][s + 1] - starts[j][s]
        rows = jnp.where(held, produced[j][span], 0.0).astype(BF16)
        grads = jnp.where(held, dx[j][span], 0.0).astype(BF16)
        out = dot(jnp.where(place, slots[j][0, :, 64:65], 0.0).astype(BF16), rows, 1, 0)
        grad = dot(jnp.where(place, 1.0, 0.0).astype(BF16), grads, 1, 0)
        out_sum = out if out_sum is None else out_sum + out
        grad_sum = grad if grad_sum is None else grad_sum + grad
    out_part[0] = out_sum.astype(BF16)
    grad_part[0] = grad_sum.astype(BF16)


def combine(starts, slots, produced, dx, capacity):
    local = len(starts)
    seqs, length, _ = slots[0].shape
    width = produced[0].shape[1]
    seq = lambda i, *_: (i, 0, 0)
    two = lambda i, *_: (0, 0)
    rows = pl.BlockSpec(produced[0].shape, two)
    return pl.pallas_call(
        functools.partial(combine_kernel, capacity, local),
        out_shape=(sds((seqs, length, width), BF16), sds((seqs, length, width), BF16)),
        grid_spec=pltpu.PrefetchScalarGridSpec(
            num_scalar_prefetch=local,
            grid=(seqs,),
            in_specs=[pl.BlockSpec((1, length, 128), seq)] * local + [rows] * (2 * local),
            out_specs=(pl.BlockSpec((1, length, width), seq), pl.BlockSpec((1, length, width), seq)),
        ),
        compiler_params=pltpu.CompilerParams(dimension_semantics=("arbitrary",), vmem_limit_bytes=60 << 20),
        cost_estimate=pl.CostEstimate(flops=3 * 10**9, bytes_accessed=4 * 10**7, transcendentals=0),
        name="combine",
    )(*starts, *slots, *produced, *dx)


def shards(
    tokens, cotangent, gate_weights, expert_ids, seq_lengths, query_weight, key_weight, value_weight,
    output_weight, attn_gain, ffn_gain, query_gain, key_gain, expert_in, expert_out,
):
    ep = lax.axis_size("ep")
    me = lax.axis_index("ep")
    _, rows, width = tokens.shape
    length = rows * ep
    top = gate_weights.shape[2]
    local = expert_in.shape[0]
    experts = local * ep
    capacity = -(-(length * top * 9 // (8 * experts)) // 16) * 16

    gains = jnp.concatenate([attn_gain, ffn_gain]).astype(F32).reshape(-1, 128)
    few = jnp.concatenate([query_gain.astype(F32), key_gain.astype(F32), seq_lengths.astype(F32)])
    few = jnp.pad(few, (0, 128 - few.shape[0]))[None]
    packet = jnp.concatenate([gains, few], axis=0)
    packet = jnp.pad(packet, ((0, -packet.shape[0] % 8), (0, 0)))

    full, weights, packets = front(tokens, query_weight, key_weight, value_weight, packet)
    routes = jnp.concatenate([expert_ids.astype(BF16), gate_weights], axis=-1)
    routes = jnp.pad(routes, ((0, 0), (0, 0), (0, 128 - 2 * top)))
    cot_full = lax.all_gather(jnp.concatenate([cotangent, routes], axis=-1), "ep", axis=1, tiled=True)

    n = 0
    g = gains.shape[0] // 2
    gain_attn = packets[:, n : n + g].reshape(1, width)
    gain_ffn = packets[:, n + g : n + 2 * g].reshape(1, width)
    q = query_gain.shape[0]
    gain_query = packets[:, n + 2 * g, :q].reshape(1, HEAD_DIM)
    gain_key = packets[:, n + 2 * g, q : 2 * q].reshape(1, HEAD_DIM)
    lens = packets[:, n + 2 * g, 2 * q].astype(jnp.int32)
    positions = jnp.arange(length, dtype=jnp.int32)
    live = (positions[None] < lens[:, None]).astype(F32)
    living = lax.dynamic_slice_in_dim(live, me * rows, rows, axis=1)[..., None]

    half = HEAD_DIM // 2
    frequency = ROPE_BASE ** (-(jnp.arange(half, dtype=F32) * (2.0 / HEAD_DIM)))
    angles = positions.astype(F32)[:, None] * frequency[None, :]
    cos = jnp.concatenate([jnp.cos(angles)] * 2, axis=-1)
    sin = jnp.concatenate([-jnp.sin(angles), jnp.sin(angles)], axis=-1)

    normed, pre, low, ctx, part = attend(
        full, weights, output_weight, gain_attn, gain_query, gain_key, cos, sin, lens
    )
    middle, mixed = mix(part, tokens, living, gain_ffn)

    in_grads, out_grads, passes = [], [], []
    for j in range(local):
        number = (me * local + j).astype(jnp.int32)[None]
        if passes:
            number, _ = lax.optimization_barrier((number, passes[-1][1]))
        slots, starts, act, dgu, out_grad, in_grad = expert_pass(
            j, number, lens, mixed, cot_full, expert_in, expert_out, capacity, top
        )
        passes.append((slots, starts, act, dgu))
        out_grads.append(lax.psum_scatter(out_grad, "rep", scatter_dimension=0, tiled=True))
        in_grads.append(lax.psum_scatter(in_grad, "rep", scatter_dimension=0, tiled=True))
    tails = [
        expert_tail(j, starts, act, dgu, expert_in, expert_out)
        for j, (slots, starts, act, dgu) in enumerate(passes)
    ]
    out_part, grad_part = combine(
        [p[1] for p in passes], [p[0] for p in passes], [t[0] for t in tails], [t[1] for t in tails], capacity
    )
    result, mgrad, ffn_back, agrad = back(grad_part, out_part, middle, cotangent, living, gain_ffn)
    npart, wgrad, wograd, qk_back = attend_back(
        agrad, normed, pre, low, ctx, weights, output_weight, gain_query, gain_key, cos, sin, lens
    )
    token_grad, small, wrows = final(npart, wgrad, tokens, mgrad, gain_attn, ffn_back, qk_back)
    sums, small = line_sum(jnp.concatenate([wrows, wograd[None]], axis=0), small)
    share = g

    def head_share(vector):
        return lax.dynamic_slice_in_dim(vector, me * (HEAD_DIM // ep), HEAD_DIM // ep)

    return (
        result,
        token_grad,
        sums[0].astype(F32),
        sums[1].astype(F32),
        sums[2].astype(F32),
        sums[3].astype(F32),
        small[:share].reshape(-1),
        small[share : 2 * share].reshape(-1),
        head_share(small[2 * share]),
        head_share(small[2 * share + 1]),
        jnp.stack(in_grads).astype(F32),
        jnp.stack(out_grads).astype(F32),
    )


def solution(mesh):
    seq = P("rep", "ep", None)
    row, gain, expert = P("ep", None), P("ep"), P("ep", None, None)
    split = P("ep", "rep", None)

    return jax.shard_map(
        shards,
        mesh=mesh,
        in_specs=(seq, seq, seq, seq, P(("rep", "ep")), row, row, row, row, gain, gain, gain, gain, expert, expert),
        out_specs=(seq, seq, row, row, row, row, gain, gain, gain, gain, split, split),
        check_vma=False,
    )
```

```python
import functools

import jax
import jax.numpy as jnp
from jax import lax
from jax.experimental import pallas as pl
from jax.experimental.pallas import tpu as pltpu
from jax.sharding import PartitionSpec as P

HEAD_DIM = 128
EPS = 1e-06
ROPE_BASE = 50000.0
MESH = pl.DeviceIdType.MESH
F32 = jnp.float32
BF16 = jnp.bfloat16


def sds(shape, dtype):
    return jax.ShapeDtypeStruct(shape, dtype)


VM = pl.BlockSpec(memory_space=pltpu.VMEM)
AN = pl.BlockSpec(memory_space=pl.ANY)


def inverse_rms(v):
    return lax.rsqrt(jnp.mean(v * v, axis=-1, keepdims=True) + EPS)


def rms_back(v, r, ug):
    return r * ug - v * (r * r * r * jnp.mean(ug * v, axis=-1, keepdims=True))


def mix_rows(total, tok, living, gain):
    middle = tok.astype(F32) + living * total
    mixed = middle * inverse_rms(middle) * gain
    return middle, mixed.astype(BF16)


def ffn_back_rows(mixed_grad, middle, cot, living, gain):
    r = inverse_rms(middle)
    middle_grad = cot.astype(F32) + rms_back(middle, r, mixed_grad * gain)
    return middle_grad, (living * middle_grad).astype(BF16), mixed_grad * middle * r


def attn_back_rows(normed_grad, tok, middle_grad, gain):
    v = tok.astype(F32)
    r = inverse_rms(v)
    return (middle_grad + rms_back(v, r, normed_grad * gain)).astype(BF16), normed_grad * v * r


class Place:
    def __init__(self):
        me = lax.axis_index("ep")
        core, x, y = lax.rem(me, 2), lax.rem(me // 2, 2), me // 4
        self.rep = lax.axis_index("rep")
        self.me = me
        self.sb = me + 1 - 2 * core
        self.dx = 2 - 4 * x
        self.dy = 4 - 8 * y
        self.xn = me + self.dx
        self.yn = me + self.dy
        self.dg = me + self.dx + self.dy

    def push(self, src, dst, send, recv, dev):
        return pltpu.make_async_remote_copy(
            src_ref=src, dst_ref=dst, send_sem=send, recv_sem=recv, device_id=(self.rep, dev), device_id_type=MESH
        )

    def peers(self):
        sb, dx, dy = self.sb, self.dx, self.dy
        return (self.xn, self.yn, self.dg, sb, sb + dx, sb + dy, sb + dx + dy)

    def greet(self, peers):
        barrier = pltpu.get_barrier_semaphore()
        for peer in peers:
            pl.semaphore_signal(barrier, inc=1, device_id=(self.rep, peer), device_id_type=MESH)
        pl.semaphore_wait(barrier, len(peers))


class Gather:
    sems = 3

    def __init__(self, at, own, full, ssem, rsem, lsem):
        self.at, self.own, self.full, self.ssem, self.rsem, self.lsem = at, own, full, ssem, rsem, lsem
        self.rows = own.shape[1]

    @staticmethod
    def scratch(seqs):
        return [pltpu.SemaphoreType.DMA((7, seqs)), pltpu.SemaphoreType.DMA((8, seqs)), pltpu.SemaphoreType.DMA((seqs,))]

    def block(self, s, dev):
        return self.full.at[s, pl.ds(pl.multiple_of(dev * self.rows, self.rows), self.rows)]

    def copy(self, s, dev, kind, slot, to, src=None):
        block = self.block(s, dev)
        return self.at.push(block if src is None else src, block, self.ssem.at[kind, s], self.rsem.at[slot, s], to)

    def start(self, s):
        at, own = self.at, self.own.at[s]
        self.copy(s, at.me, 0, 2, at.xn, own).start()
        self.copy(s, at.me, 1, 4, at.yn, own).start()
        self.copy(s, at.me, 2, 1, at.sb, own).start()
        pltpu.make_async_copy(own, self.block(s, at.me), self.lsem.at[s]).start()

    def relay(self, s, by_y):
        at = self.at
        self.copy(s, at.xn, 0, 2, at.xn).wait_recv()
        if by_y:
            self.copy(s, at.xn, 3, 6, at.yn).start()
        self.copy(s, at.xn, 4, 3, at.sb).start()
        self.copy(s, at.yn, 1, 4, at.yn).wait_recv()
        if not by_y:
            self.copy(s, at.yn, 3, 6, at.xn).start()
        self.copy(s, at.yn, 5, 5, at.sb).start()

    def relay_far(self, s):
        at = self.at
        self.copy(s, at.dg, 3, 6, at.yn).wait_recv()
        self.copy(s, at.dg, 6, 7, at.sb).start()

    def finish(self, s):
        at = self.at
        for dev, slot in ((at.sb, 1), (at.sb + at.dx, 3), (at.sb + at.dy, 5), (at.sb + at.dx + at.dy, 7)):
            self.copy(s, dev, 0, slot, at.sb).wait_recv()
        for kind in range(7):
            self.copy(s, at.me, kind, 0, at.sb).wait_send()
        pltpu.make_async_copy(self.own.at[s], self.block(s, at.me), self.lsem.at[s]).wait()


def gather_tail(seqs, gather):
    def relay(i, _):
        gather.relay(2 * i, True)
        gather.relay(2 * i + 1, False)
        return 0

    def far(s, _):
        gather.relay_far(s)
        return 0

    def finish(s, _):
        gather.finish(s)
        return 0

    lax.fori_loop(0, seqs // 2, relay, 0)
    lax.fori_loop(0, seqs, far, 0)
    lax.fori_loop(0, seqs, finish, 0)


class Reduce:
    def __init__(self, at, part, held, x1, y1, x2, y2, hs, hr, d1s, d1r, d2s, d2r):
        self.at, self.part, self.held = at, part, held
        self.x1, self.y1, self.x2, self.y2 = x1, y1, x2, y2
        self.hs, self.hr, self.d1s, self.d1r, self.d2s, self.d2r = hs, hr, d1s, d1r, d2s, d2r
        self.half = part.shape[2] // 2

    @staticmethod
    def scratch(part):
        s, _, t, d = part.shape
        dma = pltpu.SemaphoreType.DMA
        return [
            pltpu.VMEM((s, 4, t, d), BF16),
            pltpu.VMEM((s, t // 2, d), BF16),
            pltpu.VMEM((s, t // 2, d), BF16),
            pltpu.VMEM((s, t, d), BF16),
            pltpu.VMEM((s, t, d), BF16),
            dma((4, s)),
            dma((4, s)),
            dma((2, s)),
            dma((2, s)),
            dma((2, s)),
            dma((2, s)),
        ]

    sems = 11

    def core_copy(self, s, k):
        at = self.at
        dest = (at.sb, at.sb + at.dx, at.sb + at.dy, at.sb + at.dx + at.dy)[k]
        return at.push(self.part.at[s, dest], self.held.at[s, k], self.hs.at[k, s], self.hr.at[k, s], at.sb)

    def first(self, s, k):
        at, h = self.at, self.half
        src = self.held.at[s, 3, pl.ds(k * h, h)]
        return at.push(src, (self.x1, self.y1)[k].at[s], self.d1s.at[k, s], self.d1r.at[k, s], (at.xn, at.yn)[k])

    def second(self, s, k):
        at = self.at
        src = self.held.at[s, 1 + k]
        return at.push(src, (self.x2, self.y2)[k].at[s], self.d2s.at[k, s], self.d2r.at[k, s], (at.xn, at.yn)[k])

    def start(self, s):
        for k in (3, 1, 2, 0):
            self.core_copy(s, k).start()

    def hop1(self, s):
        self.core_copy(s, 3).wait_recv()
        self.held[s, 3] = (self.held[s, 3].astype(F32) + self.part[s, self.at.dg].astype(F32)).astype(BF16)
        self.first(s, 0).start()
        self.first(s, 1).start()

    def hop2(self, s):
        h = self.half
        for k, dest, extra, rows, rest in (
            (0, self.at.xn, self.y1, pl.ds(h, h), pl.ds(0, h)),
            (1, self.at.yn, self.x1, pl.ds(0, h), pl.ds(h, h)),
        ):
            self.core_copy(s, 1 + k).wait_recv()
            self.first(s, 1 - k).wait_recv()
            held, part = self.held.at[s, 1 + k], self.part.at[s, dest]
            held[rows] = (held[rows].astype(F32) + part[rows].astype(F32) + extra[s].astype(F32)).astype(BF16)
            held[rest] = (held[rest].astype(F32) + part[rest].astype(F32)).astype(BF16)
            self.second(s, k).start()

    def total(self, s):
        self.core_copy(s, 0).wait_recv()
        self.second(s, 0).wait_recv()
        self.second(s, 1).wait_recv()
        return (
            self.part[s, self.at.me].astype(F32)
            + self.held[s, 0].astype(F32)
            + self.x2[s].astype(F32)
            + self.y2[s].astype(F32)
        )

    def finish(self, s):
        for k in range(4):
            self.core_copy(s, k).wait_send()
        for k in range(2):
            self.first(s, k).wait_send()
            self.second(s, k).wait_send()


def each(n, *steps):
    def run(s, _):
        for step in steps:
            step(s)
        return 0

    lax.fori_loop(0, n, run, 0)


COMM = dict(has_side_effects=True, vmem_limit_bytes=60 << 20)


def front_kernel(tok, wq, wk, wv, pk, full, weights, packets, tok_v, *sems):
    at = Place()
    gather = Gather(at, tok, full, *sems[:3])
    wsend, wrecv, psend, precv, local = sems[3:]
    seqs = tok.shape[0]
    block, width = wq.shape[0], weights.shape[2]
    at.greet(at.peers())
    each(seqs, gather.start)
    mine = pl.ds(pl.multiple_of(at.me * block, block), block)

    def weight_copy(m, j, dev):
        cols = pl.ds(pl.multiple_of(dev * width, width), width)
        return at.push((wq, wk, wv)[j].at[:, cols], weights.at[j, mine], wsend.at[m, j], wrecv.at[m, j], dev)

    def packet_copy(m, dev):
        return at.push(pk, packets.at[at.me], psend.at[m], precv.at[m], dev)

    own_cols = pl.ds(pl.multiple_of(at.me * width, width), width)
    own = [pltpu.make_async_copy(w.at[:, own_cols], weights.at[j, mine], local.at[j]) for j, w in enumerate((wq, wk, wv))]
    own.append(pltpu.make_async_copy(pk, packets.at[at.me], local.at[3]))
    for copy in own:
        copy.start()
    for m, dev in enumerate(at.peers()):
        packet_copy(m, dev).start()
    for m, dev in enumerate(at.peers()):
        for j in range(3):
            weight_copy(m, j, dev).start()
    gather_tail(seqs, gather)
    for m, dev in enumerate(at.peers()):
        packet_copy(m, dev).wait()
        for j in range(3):
            weight_copy(m, j, dev).wait()
    for copy in own:
        copy.wait()


def front(tokens, wq, wk, wv, packet):
    seqs, rows, width = tokens.shape
    ep = lax.axis_size("ep")
    cols = wq.shape[1] // ep
    if ep != 8:
        full = lax.all_gather(tokens, "ep", axis=1, tiled=True)
        weights = [lax.all_to_all(w, "ep", split_axis=1, concat_axis=0, tiled=True) for w in (wq, wk, wv)]
        return full, jnp.stack(weights), lax.all_gather(packet, "ep", axis=0)
    dma = pltpu.SemaphoreType.DMA
    return pl.pallas_call(
        front_kernel,
        out_shape=(
            sds((seqs, rows * ep, width), BF16),
            sds((3, wq.shape[0] * ep, cols), BF16),
            sds((ep,) + packet.shape, F32),
        ),
        in_specs=[VM] * 5,
        out_specs=(AN, AN, AN),
        scratch_shapes=[pltpu.VMEM((8, 128), F32)]
        + Gather.scratch(seqs)
        + [dma((7, 3)), dma((7, 3)), dma((7,)), dma((7,)), dma((4,))],
        compiler_params=pltpu.CompilerParams(collective_id=1, **COMM),
        name="front",
    )(tokens, wq, wk, wv, packet)


def mix_kernel(part, tok, living, gain, middle, full, own, *scratch):
    at = Place()
    seqs = tok.shape[0]
    reduce = Reduce(at, part, *scratch[: Reduce.sems])
    gather = Gather(at, own, full, *scratch[Reduce.sems :])
    at.greet((at.xn, at.yn, at.sb))
    each(seqs, reduce.start)
    each(seqs, reduce.hop1)
    each(seqs, reduce.hop2)

    def rows(s):
        mid, mixed = mix_rows(reduce.total(s), tok[s], living[s], gain[...])
        middle[s] = mid
        own[s] = mixed
        gather.start(s)

    each(seqs, rows)
    gather_tail(seqs, gather)
    each(seqs, reduce.finish)


def mix(part, tokens, living, gain):
    seqs, rows, width = tokens.shape
    ep = lax.axis_size("ep")
    if ep != 8:
        total = lax.psum_scatter(part, "ep", scatter_dimension=1, tiled=True).astype(F32)
        middle, mixed = mix_rows(total, tokens, living, gain)
        return middle, lax.all_gather(mixed, "ep", axis=1, tiled=True)
    part = part.reshape(seqs, ep, rows, width)
    return pl.pallas_call(
        mix_kernel,
        out_shape=(sds(tokens.shape, F32), sds((seqs, rows * ep, width), BF16)),
        in_specs=[VM] * 4,
        out_specs=(VM, AN),
        scratch_shapes=[pltpu.VMEM(tokens.shape, BF16)] + Reduce.scratch(part) + Gather.scratch(seqs),
        compiler_params=pltpu.CompilerParams(collective_id=2, **COMM),
        name="mix",
    )(part, tokens, living, gain)


def back_kernel(gpart, opart, middle, cot, living, gain, result, mgrad, ggrad, full, own, *scratch):
    at = Place()
    seqs = cot.shape[0]
    n = Reduce.sems
    rg = Reduce(at, gpart, *scratch[:n])
    ro = Reduce(at, opart, *scratch[n : 2 * n])
    gather = Gather(at, own, full, *scratch[2 * n :])
    at.greet((at.xn, at.yn, at.sb))
    each(seqs, rg.start)
    each(seqs, ro.start)
    each(seqs, rg.hop1)
    each(seqs, rg.hop2)
    ggrad[...] = jnp.zeros_like(ggrad)

    def rows(s):
        mg, ag, back = ffn_back_rows(rg.total(s), middle[s], cot[s], living[s], gain[...])
        mgrad[s] = mg
        own[s] = ag
        ggrad[...] += jnp.sum(back, axis=0, keepdims=True)
        gather.start(s)

    each(seqs, rows)
    gather_tail(seqs, gather)
    each(seqs, ro.hop1)
    each(seqs, ro.hop2)

    def out(s):
        result[s] = (middle[s] + ro.total(s)).astype(BF16)

    each(seqs, out)
    each(seqs, rg.finish, ro.finish)


def back(gpart, opart, middle, cot, living, gain):
    seqs, rows, width = cot.shape
    ep = lax.axis_size("ep")
    if ep != 8:
        mixed_grad = lax.psum_scatter(gpart, "ep", scatter_dimension=1, tiled=True).astype(F32)
        moe = lax.psum_scatter(opart, "ep", scatter_dimension=1, tiled=True).astype(F32)
        mg, ag, backs = ffn_back_rows(mixed_grad, middle, cot, living, gain)
        full = lax.all_gather(ag, "ep", axis=1, tiled=True)
        return (middle + moe).astype(BF16), mg, jnp.sum(backs, axis=(0, 1))[None], full
    gpart, opart = (p.reshape(seqs, ep, rows, width) for p in (gpart, opart))
    return pl.pallas_call(
        back_kernel,
        out_shape=(
            sds(cot.shape, BF16),
            sds(cot.shape, F32),
            sds((1, width), F32),
            sds((seqs, rows * ep, width), BF16),
        ),
        in_specs=[VM] * 6,
        out_specs=(VM, VM, VM, AN),
        scratch_shapes=[pltpu.VMEM(cot.shape, BF16)] + 2 * Reduce.scratch(gpart) + Gather.scratch(seqs),
        compiler_params=pltpu.CompilerParams(collective_id=3, **COMM),
        name="back",
    )(gpart, opart, middle, cot, living, gain)


def final_kernel(part, wgrad, tok, mgrad, gain, others, tgrad, small, wrows, ggrad, parcel, landed, *scratch):
    at = Place()
    seqs = tok.shape[0]
    n = Reduce.sems
    reduce = Reduce(at, part, *scratch[:n])
    wsend, wrecv, local, gsend, grecv = scratch[n:]
    width = wgrad.shape[2]
    block = wrows.shape[1]
    at.greet(at.peers())
    cols = pl.ds(pl.multiple_of(at.me * width, width), width)

    def weight_copy(m, dev):
        rows = pl.ds(pl.multiple_of(dev * block, block), block)
        return at.push(wgrad.at[:, rows], wrows.at[:, :, cols], wsend.at[m], wrecv.at[m], dev)

    mine = pl.ds(pl.multiple_of(at.me * block, block), block)
    own = pltpu.make_async_copy(wgrad.at[:, mine], wrows.at[:, :, cols], local)
    own.start()
    for m, dev in enumerate(at.peers()):
        weight_copy(m, dev).start()
    each(seqs, reduce.start)
    each(seqs, reduce.hop1)
    each(seqs, reduce.hop2)
    ggrad[...] = jnp.zeros_like(ggrad)

    def rows(s):
        tg, back = attn_back_rows(reduce.total(s), tok[s], mgrad[s], gain[...])
        tgrad[s] = tg
        ggrad[...] += jnp.sum(back, axis=0, keepdims=True)

    each(seqs, rows)

    parcel[...] = jnp.zeros_like(parcel)
    devices = parcel.shape[0]
    rows_of = ggrad.shape[1] // (128 * devices)
    for dev in range(devices):
        for k in range(rows_of):
            lanes = pl.ds((dev * rows_of + k) * 128, 128)
            parcel[dev, k : k + 1] = ggrad[:, lanes]
            parcel[dev, rows_of + k : rows_of + k + 1] = others[0:1, lanes]
        parcel[dev, 2 * rows_of : 2 * rows_of + 2] = others[1:3, 0:128]

    def parcel_copy(m, dev):
        return at.push(parcel.at[dev], landed.at[m], gsend.at[m], grecv.at[m], dev)

    for m, dev in enumerate(at.peers()):
        parcel_copy(m, dev).start()
    total = parcel[at.me]
    for m, dev in enumerate(at.peers()):
        parcel_copy(m, dev).wait_recv()
        total = total + landed[m]
    small[...] = total
    each(seqs, reduce.finish)
    for m, dev in enumerate(at.peers()):
        weight_copy(m, dev).wait()
        parcel_copy(m, dev).wait_send()
    own.wait()


def final(part, wgrad, tokens, mgrad, gain, ffn_back, qk_back):
    seqs, rows, width = tokens.shape
    ep = lax.axis_size("ep")
    if ep != 8:
        normed_grad = lax.psum_scatter(part, "ep", scatter_dimension=1, tiled=True).astype(F32)
        tg, backs = attn_back_rows(normed_grad, tokens, mgrad, gain)
        wrows = lax.all_to_all(wgrad, "ep", split_axis=1, concat_axis=2, tiled=True)
        share = width // ep
        small = jnp.concatenate([jnp.sum(backs, axis=(0, 1)), ffn_back[0], qk_back[0], qk_back[1]])
        small = lax.psum(small, "ep")
        mine = lax.axis_index("ep") * share
        cut = [lax.dynamic_slice_in_dim(small, k * width + mine, share).reshape(-1, 128) for k in range(2)]
        small = jnp.concatenate(cut + [small[2 * width :].reshape(2, HEAD_DIM)], axis=0)
        return tg, jnp.pad(small, ((0, 8 - small.shape[0]), (0, 0))), wrows
    others = jnp.concatenate([ffn_back, jnp.pad(qk_back[:2], ((0, 0), (0, width - HEAD_DIM)))], axis=0)
    part = part.reshape(seqs, ep, rows, width)
    dma = pltpu.SemaphoreType.DMA
    return pl.pallas_call(
        final_kernel,
        out_shape=(
            sds(tokens.shape, BF16),
            sds((8, 128), F32),
            sds((3, wgrad.shape[1] // ep, wgrad.shape[2] * ep), BF16),
        ),
        in_specs=[VM] * 6,
        out_specs=(VM, VM, AN),
        scratch_shapes=[pltpu.VMEM((1, width), F32), pltpu.VMEM((ep, 8, 128), F32), pltpu.VMEM((7, 8, 128), F32)]
        + Reduce.scratch(part)
        + [dma((7,)), dma((7,)), dma, dma((7,)), dma((7,))],
        compiler_params=pltpu.CompilerParams(collective_id=4, **COMM),
        name="final",
    )(part, wgrad, tokens, mgrad, gain, others)


def line_kernel(own, small, out, small_out, held, met, landed, os, or_, ps, pr, qs, qr, fs, fr, ss, sr):
    z = lax.axis_index("rep")
    ep = lax.axis_index("ep")
    chunks = own.shape[0]

    def push(src, dst, send, recv, dev):
        return pltpu.make_async_remote_copy(
            src_ref=src, dst_ref=dst, send_sem=send, recv_sem=recv, device_id=(dev, ep), device_id_type=MESH
        )

    barrier = pltpu.get_barrier_semaphore()
    others = [lax.rem(z + k, 4) for k in range(1, 4)]
    for dev in others:
        pl.semaphore_signal(barrier, inc=1, device_id=(dev, ep), device_id_type=MESH)
    pl.semaphore_wait(barrier, 3)
    inner = jnp.logical_and(z > 0, z < 3)
    middle, partner, outer = 1 + z // 3, 3 - z, 3 * (z - 1)

    def inward(c):
        return push(own.at[c], held.at[c], os.at[c], or_.at[c], middle)

    def across(c):
        return push(held.at[c], met.at[c], ps.at[c], pr.at[c], partner)

    def share(c):
        return push(out.at[c], out.at[c], qs.at[c], qr.at[c], partner)

    def outward(c):
        return push(out.at[c], out.at[c], fs.at[c], fr.at[c], outer)

    def small_copy(k):
        return push(small, landed.at[k], ss.at[k], sr.at[k], others[k])

    for k in range(3):
        small_copy(k).start()

    @pl.when(jnp.logical_not(inner))
    def _():
        each(chunks, lambda c: inward(c).start())
        each(chunks, lambda c: outward(c).wait_recv())
        each(chunks, lambda c: inward(c).wait_send())

    def mine(c):
        return 1 + lax.rem(c, 2) == z

    @pl.when(inner)
    def _():
        def run(c, _):
            @pl.when(c < chunks)
            def _():
                inward(c).wait_recv()
                held[c] = (held[c].astype(F32) + own[c].astype(F32)).astype(BF16)

                @pl.when(jnp.logical_not(mine(c)))
                def _():
                    across(c).start()

            b = c - 1

            @pl.when(jnp.logical_and(jnp.logical_and(c >= 1, c < chunks + 1), mine(c + 1)))
            def _():
                across(b).wait_recv()
                out[b] = (held[b].astype(F32) + met[b].astype(F32)).astype(BF16)
                share(b).start()
                outward(b).start()

            a = c - 2

            @pl.when(jnp.logical_and(c >= 2, jnp.logical_not(mine(c))))
            def _():
                share(a).wait_recv()
                outward(a).start()

            return 0

        lax.fori_loop(0, chunks + 2, run, 0)

        def finish(c):
            outward(c).wait_send()

            @pl.when(mine(c))
            def _():
                share(c).wait_send()

            @pl.when(jnp.logical_not(mine(c)))
            def _():
                across(c).wait_send()

        each(chunks, finish)

    total = small[...]
    for k in range(3):
        small_copy(k).wait()
        total = total + landed[k]
    small_out[...] = total


def line_sum(big, small):
    if lax.axis_size("rep") != 4 or lax.axis_size("ep") != 8:
        return lax.psum(big, "rep"), lax.psum(small, "rep")
    count, rows, cols = big.shape
    chunks = 16
    own = big.reshape(chunks, count * rows // chunks, cols)
    dma = pltpu.SemaphoreType.DMA
    out, small = pl.pallas_call(
        line_kernel,
        out_shape=(sds(own.shape, BF16), sds(small.shape, F32)),
        in_specs=[VM, VM],
        out_specs=(VM, VM),
        scratch_shapes=[
            pltpu.VMEM(own.shape, BF16),
            pltpu.VMEM(own.shape, BF16),
            pltpu.VMEM((3,) + small.shape, F32),
        ]
        + [dma((chunks,))] * 8
        + [dma((3,))] * 2,
        compiler_params=pltpu.CompilerParams(collective_id=5, has_side_effects=True, vmem_limit_bytes=40 << 20),
        name="line_sum",
    )(own, small)
    return out.reshape(big.shape), small


def dot(a, b, ca, cb):
    return lax.dot_general(a, b, (((ca,), (cb,)), ((), ())), preferred_element_type=F32)


def rope(v, cos, sin_turn):
    return v * cos + pltpu.roll(v, HEAD_DIM // 2, 1) * sin_turn


def probabilities(q, k, length):
    scores = dot(q, k, 1, 1) * HEAD_DIM**-0.5
    column = lax.broadcasted_iota(jnp.int32, scores.shape, 1)
    scores = jnp.where(column < length, scores, -1e9)
    p = jnp.exp(scores - jnp.max(scores, axis=-1, keepdims=True))
    return p * (1.0 / jnp.sum(p, axis=-1, keepdims=True))


def attend_kernel(lens, tok, w, wo, gain, qg, kg, cos, sin, normed, pre, low, ctx, part):
    length = lens[pl.program_id(0)]
    v = tok[0].astype(F32)
    x = (v * inverse_rms(v) * gain[...]).astype(BF16)
    normed[0] = x
    q_pre, k_pre = dot(x, w[0], 1, 0), dot(x, w[1], 1, 0)
    value = dot(x, w[2], 1, 0).astype(BF16)
    pre[0, 0], pre[1, 0] = q_pre, k_pre
    low[2, 0] = value
    for h in range(q_pre.shape[1] // HEAD_DIM):
        cols = slice(h * HEAD_DIM, (h + 1) * HEAD_DIM)
        rot = []
        for i, (u, g) in enumerate(((q_pre[:, cols], qg[...]), (k_pre[:, cols], kg[...]))):
            rot.append(rope(u * inverse_rms(u) * g, cos[...], sin[...]).astype(BF16))
            low[i, 0, :, cols] = rot[i]
        attention = probabilities(rot[0], rot[1], length).astype(BF16)
        ctx[0, :, cols] = dot(attention, value[:, cols], 1, 0).astype(BF16)
    part[0] = dot(ctx[0], wo[...], 1, 0).astype(BF16)


def attend(full, weights, wo, gain, qg, kg, cos, sin, lens):
    seqs, length, width = full.shape
    cols = weights.shape[2]
    row = lambda i, *_: (i, 0, 0)
    row2 = lambda i, *_: (0, i, 0, 0)
    two = lambda i, *_: (0, 0)
    return pl.pallas_call(
        attend_kernel,
        out_shape=(
            sds(full.shape, BF16),
            sds((2, seqs, length, cols), F32),
            sds((3, seqs, length, cols), BF16),
            sds((seqs, length, cols), BF16),
            sds(full.shape, BF16),
        ),
        grid_spec=pltpu.PrefetchScalarGridSpec(
            num_scalar_prefetch=1,
            grid=(seqs,),
            in_specs=[
                pl.BlockSpec((1, length, width), row),
                pl.BlockSpec(weights.shape, lambda i, *_: (0, 0, 0)),
                pl.BlockSpec(wo.shape, two),
                pl.BlockSpec((1, width), two),
                pl.BlockSpec((1, HEAD_DIM), two),
                pl.BlockSpec((1, HEAD_DIM), two),
                pl.BlockSpec((length, HEAD_DIM), two),
                pl.BlockSpec((length, HEAD_DIM), two),
            ],
            out_specs=(
                pl.BlockSpec((1, length, width), row),
                pl.BlockSpec((2, 1, length, cols), row2),
                pl.BlockSpec((3, 1, length, cols), row2),
                pl.BlockSpec((1, length, cols), row),
                pl.BlockSpec((1, length, width), row),
            ),
        ),
        compiler_params=pltpu.CompilerParams(dimension_semantics=("arbitrary",), vmem_limit_bytes=60 << 20),
        cost_estimate=pl.CostEstimate(flops=10**10, bytes_accessed=4 * 10**7, transcendentals=10**6),
        name="attend",
    )(lens, full, weights, wo, gain, qg, kg, cos, sin)


def attend_back_kernel(
    lens, agrad, normed, pre, low, ctx, w, wo, qg, kg, cos, sin, part, wgrad, wograd, gains, wacc, woacc
):
    s = pl.program_id(0)
    length = lens[s]

    @pl.when(s == 0)
    def _():
        wacc[...] = jnp.zeros_like(wacc)
        woacc[...] = jnp.zeros_like(woacc)
        gains[...] = jnp.zeros_like(gains)

    ag = agrad[0]
    woacc[...] += dot(ctx[0], ag, 0, 0)
    cg_all = dot(ag, wo[...], 1, 1).astype(BF16)
    scale = HEAD_DIM**-0.5
    half = HEAD_DIM // 2
    grads = ([], [], [])
    for h in range(cg_all.shape[1] // HEAD_DIM):
        cols = slice(h * HEAD_DIM, (h + 1) * HEAD_DIM)
        q, k, value, cg = low[0, 0, :, cols], low[1, 0, :, cols], low[2, 0, :, cols], cg_all[:, cols]
        attention = probabilities(q, k, length)
        grads[2].append(dot(attention.astype(BF16), cg, 0, 0).astype(BF16))
        pg = dot(cg, value, 1, 1)
        sg = (attention * (pg - jnp.sum(attention * pg, axis=-1, keepdims=True))).astype(BF16)
        for i, (rot_grad, g) in enumerate(((dot(sg, k, 1, 0), qg[...]), (dot(sg, q, 0, 0), kg[...]))):
            wgt = rot_grad * scale
            u = wgt * cos[...] + pltpu.roll(wgt * sin[...], half, 1)
            v = pre[i, 0, :, cols]
            r = inverse_rms(v)
            grads[i].append(rms_back(v, r, u * g).astype(BF16))
            gains[i : i + 1] += jnp.sum(u * v * r, axis=0, keepdims=True)
    total = None
    for i in range(3):
        g = grads[i][0] if len(grads[i]) == 1 else jnp.concatenate(grads[i], axis=1)
        wacc[i] += dot(normed[0], g, 0, 0)
        piece = dot(g, w[i], 1, 1)
        total = piece if total is None else total + piece
    part[0] = total.astype(BF16)

    @pl.when(s == pl.num_programs(0) - 1)
    def _():
        wgrad[...] = wacc[...].astype(BF16)
        wograd[...] = woacc[...].astype(BF16)


def attend_back(agrad, normed, pre, low, ctx, weights, wo, qg, kg, cos, sin, lens):
    seqs, length, width = agrad.shape
    cols = weights.shape[2]
    row = lambda i, *_: (i, 0, 0)
    row2 = lambda i, *_: (0, i, 0, 0)
    two = lambda i, *_: (0, 0)
    three = lambda i, *_: (0, 0, 0)
    return pl.pallas_call(
        attend_back_kernel,
        out_shape=(
            sds(agrad.shape, BF16),
            sds(weights.shape, BF16),
            sds(wo.shape, BF16),
            sds((8, HEAD_DIM), F32),
        ),
        grid_spec=pltpu.PrefetchScalarGridSpec(
            num_scalar_prefetch=1,
            grid=(seqs,),
            in_specs=[
                pl.BlockSpec((1, length, width), row),
                pl.BlockSpec((1, length, width), row),
                pl.BlockSpec((2, 1, length, cols), row2),
                pl.BlockSpec((3, 1, length, cols), row2),
                pl.BlockSpec((1, length, cols), row),
                pl.BlockSpec(weights.shape, three),
                pl.BlockSpec(wo.shape, two),
                pl.BlockSpec((1, HEAD_DIM), two),
                pl.BlockSpec((1, HEAD_DIM), two),
                pl.BlockSpec((length, HEAD_DIM), two),
                pl.BlockSpec((length, HEAD_DIM), two),
            ],
            out_specs=(
                pl.BlockSpec((1, length, width), row),
                pl.BlockSpec(weights.shape, three),
                pl.BlockSpec(wo.shape, two),
                pl.BlockSpec((8, HEAD_DIM), two),
            ),
            scratch_shapes=[pltpu.VMEM(weights.shape, F32), pltpu.VMEM(wo.shape, F32)],
        ),
        compiler_params=pltpu.CompilerParams(dimension_semantics=("arbitrary",), vmem_limit_bytes=60 << 20),
        cost_estimate=pl.CostEstimate(flops=2 * 10**10, bytes_accessed=4 * 10**7, transcendentals=10**6),
        name="attend_back",
    )(lens, agrad, normed, pre, low, ctx, weights, wo, qg, kg, cos, sin)


BLOCK = 256
TILE = (512, 2048)


def pack_rows(seqs, capacity):
    return -(-seqs * capacity // BLOCK) * BLOCK + BLOCK


def expert_kernel(
    capacity, top, j, number, lens, mixed, cot, table, w_in, w_out, slots, starts, act, dgu, out_grad, in_grad,
    x, dy, wi, wo, acts, dgus, acc, stage, wsem, ssem, rsem,
):
    s = pl.program_id(0)
    seqs = pl.num_programs(0)
    length, width = mixed.shape[1:]
    hidden = wo.shape[0]
    loads = [pltpu.make_async_copy(w_in.at[j], wi, wsem.at[0]), pltpu.make_async_copy(w_out.at[j], wo, wsem.at[1])]

    @pl.when(s == 0)
    def _():
        for copy in loads:
            copy.start()
        starts[0] = 0

    tab = table[0].astype(F32)
    lane = lax.broadcasted_iota(jnp.int32, tab.shape, 1)
    row = lax.broadcasted_iota(jnp.int32, tab.shape, 0)
    chosen = jnp.logical_and(jnp.logical_and(tab == number[0].astype(F32), lane < top), row < lens[s])
    gates = jnp.where(chosen, pltpu.roll(tab, 128 - top, 1), 0.0).astype(BF16)
    chosen = jnp.where(chosen, 1.0, 0.0).astype(BF16)
    ones = jnp.ones((8, 128), BF16)
    hit = dot(ones, chosen, 1, 1)
    weight = dot(ones, gates, 1, 1)
    earlier = lax.broadcasted_iota(jnp.int32, (length, length), 0)
    later = lax.broadcasted_iota(jnp.int32, (length, length), 1)
    before = jnp.where(earlier < later, 1.0, 0.0).astype(BF16)
    rank = dot(hit.astype(BF16), before, 1, 0)
    slot = jnp.where(hit > 0.5, rank, -1.0)
    slots[0, 0:8] = slot
    slots[0, 8:16] = weight
    column = lax.broadcasted_iota(jnp.int32, (capacity, length), 0).astype(F32)
    place = column == slot[0:1]
    start = pl.multiple_of(starts[s], 16)
    span = pl.ds(start, capacity)
    x[span] = dot(jnp.where(place, 1.0, 0.0).astype(BF16), mixed[0], 1, 0).astype(BF16)
    dy[span] = dot(jnp.where(place, weight[0:1], 0.0).astype(BF16), cot[0], 1, 0).astype(BF16)
    count = jnp.sum(hit[0:1]).astype(jnp.int32)
    starts[s + 1] = start + (count + 15) // 16 * 16

    @pl.when(s == seqs - 1)
    def _():
        total = starts[seqs]
        tail = pl.ds(pl.multiple_of(start + capacity, 16), BLOCK)
        x[tail] = jnp.zeros((BLOCK, width), BF16)
        dy[tail] = jnp.zeros((BLOCK, width), BF16)
        blocks = (total + BLOCK - 1) // BLOCK
        for copy in loads:
            copy.wait()
        part = min(hidden, 512)

        def forward(b, _):
            rows = pl.ds(pl.multiple_of(b * BLOCK, BLOCK), BLOCK)
            for h in range(hidden // part):
                gcols, ucols = pl.ds(h * part, part), pl.ds(hidden + h * part, part)
                gate = dot(x[rows], wi[:, gcols], 1, 0)
                up = dot(x[rows], wi[:, ucols], 1, 0)
                dact = dot(dy[rows], wo[gcols], 1, 1)
                sig = 1.0 / (1.0 + jnp.exp(-gate))
                silu = gate * sig
                acts[rows, gcols] = (silu * up).astype(BF16)
                dgus[rows, gcols] = (dact * up * sig * (1.0 + gate * (1.0 - sig))).astype(BF16)
                dgus[rows, ucols] = (dact * silu).astype(BF16)
            return 0

        lax.fori_loop(0, blocks, forward, 0)
        saves = [pltpu.make_async_copy(acts, act, rsem.at[0]), pltpu.make_async_copy(dgus, dgu, rsem.at[1])]
        for copy in saves:
            copy.start()

        tr, tc = acc.shape

        def grads(left, right, result, first):
            down, across = result.shape[0] // tr, result.shape[1] // tc

            def tile(t, _):
                rt, ct = t // across, lax.rem(t, across)
                left_cols = pl.ds(pl.multiple_of(rt * tr, tr), tr)
                right_cols = pl.ds(pl.multiple_of(ct * tc, tc), tc)

                def step(b, _):
                    rows = pl.ds(pl.multiple_of(b * BLOCK, BLOCK), BLOCK)
                    piece = dot(left[rows, left_cols], right[rows, right_cols], 0, 0)

                    @pl.when(b == 0)
                    def _():
                        acc[...] = piece

                    @pl.when(b > 0)
                    def _():
                        acc[...] += piece

                    return 0

                @pl.when(blocks == 0)
                def _():
                    acc[...] = jnp.zeros_like(acc)

                lax.fori_loop(0, blocks, step, 0)
                k = lax.rem(t, 2)
                out = pltpu.make_async_copy(stage.at[k], result.at[left_cols, right_cols], ssem.at[k])

                @pl.when(jnp.logical_or(t >= 2, not first))
                def _():
                    out.wait()

                stage[k] = acc[...].astype(BF16)
                out.start()
                return 0

            lax.fori_loop(0, down * across, tile, 0)

        grads(acts, dy, out_grad, True)
        grads(x, dgus, in_grad, False)
        for k in range(2):
            pltpu.make_async_copy(stage.at[k], in_grad.at[pl.ds(0, tr), pl.ds(0, tc)], ssem.at[k]).wait()
        for copy in saves:
            copy.wait()


def expert_pass(j, number, lens, mixed, cot, w_in, w_out, capacity, top):
    seqs, length, width = mixed.shape
    hidden = w_out.shape[1]
    rows = pack_rows(seqs, capacity)
    dma = pltpu.SemaphoreType.DMA
    kernel = functools.partial(expert_kernel, capacity, top, j)
    seq = lambda i, *_: (i, 0, 0)
    return pl.pallas_call(
        kernel,
        out_shape=(
            sds((seqs, 16, length), F32),
            sds((seqs + 1,), jnp.int32),
            sds((rows, hidden), BF16),
            sds((rows, 2 * hidden), BF16),
            sds((hidden, width), BF16),
            sds((width, 2 * hidden), BF16),
        ),
        grid_spec=pltpu.PrefetchScalarGridSpec(
            num_scalar_prefetch=2,
            grid=(seqs,),
            in_specs=[
                pl.BlockSpec((1, length, width), seq),
                pl.BlockSpec((1, length, width), seq),
                pl.BlockSpec((1, length, 128), lambda i, *_: (i, 0, width // 128)),
                AN,
                AN,
            ],
            out_specs=(
                pl.BlockSpec((1, 16, length), seq),
                pl.BlockSpec(memory_space=pltpu.SMEM),
                AN,
                AN,
                AN,
                AN,
            ),
            scratch_shapes=[
                pltpu.VMEM((rows, width), BF16),
                pltpu.VMEM((rows, width), BF16),
                pltpu.VMEM(w_in.shape[1:], BF16),
                pltpu.VMEM(w_out.shape[1:], BF16),
                pltpu.VMEM((rows, hidden), BF16),
                pltpu.VMEM((rows, 2 * hidden), BF16),
                pltpu.VMEM(TILE, F32),
                pltpu.VMEM((2,) + TILE, BF16),
                dma((2,)),
                dma((2,)),
                dma((2,)),
            ],
        ),
        compiler_params=pltpu.CompilerParams(dimension_semantics=("arbitrary",), vmem_limit_bytes=60 << 20),
        cost_estimate=pl.CostEstimate(flops=25 * 10**9, bytes_accessed=6 * 10**7, transcendentals=10**6),
        name="expert_pass",
    )(number, lens, mixed, cot, cot, w_in, w_out)


def tail_kernel(starts, act, dgu, w_in, w_out, produced, dx):
    @pl.when(pl.program_id(0) * BLOCK < starts[starts.shape[0] - 1])
    def _():
        produced[...] = dot(act[...], w_out[...], 1, 0).astype(BF16)
        dx[...] = dot(dgu[...], w_in[...], 1, 1).astype(BF16)


def expert_tail(j, starts, act, dgu, w_in, w_out):
    rows, hidden = act.shape
    width = w_in.shape[1]
    last = starts.shape[0] - 1
    block = lambda i, st: (jnp.maximum(jnp.minimum(i, (st[last] + BLOCK - 1) // BLOCK - 1), 0), 0)
    return pl.pallas_call(
        tail_kernel,
        out_shape=(sds((rows, width), BF16), sds((rows, width), BF16)),
        grid_spec=pltpu.PrefetchScalarGridSpec(
            num_scalar_prefetch=1,
            grid=(rows // BLOCK - 1,),
            in_specs=[
                pl.BlockSpec((BLOCK, hidden), block),
                pl.BlockSpec((BLOCK, 2 * hidden), block),
                pl.BlockSpec((None,) + w_in.shape[1:], lambda i, *_: (j, 0, 0)),
                pl.BlockSpec((None,) + w_out.shape[1:], lambda i, *_: (j, 0, 0)),
            ],
            out_specs=(pl.BlockSpec((BLOCK, width), block), pl.BlockSpec((BLOCK, width), block)),
        ),
        compiler_params=pltpu.CompilerParams(dimension_semantics=("arbitrary",), vmem_limit_bytes=60 << 20),
        cost_estimate=pl.CostEstimate(flops=12 * 10**9, bytes_accessed=3 * 10**7, transcendentals=0),
        name="expert_tail",
    )(starts, act, dgu, w_in, w_out)


def combine_kernel(capacity, local, *refs):
    s = pl.program_id(0)
    starts = refs[:local]
    slots = refs[local : 2 * local]
    produced = refs[2 * local : 3 * local]
    dx = refs[3 * local : 4 * local]
    out_part, grad_part = refs[4 * local :]
    out_sum, grad_sum = None, None
    for j in range(local):
        length = slots[j].shape[2]
        column = lax.broadcasted_iota(jnp.int32, (capacity, length), 0).astype(F32)
        place = column == slots[j][0, 0:1]
        span = pl.ds(pl.multiple_of(starts[j][s], 16), capacity)
        held = lax.broadcasted_iota(jnp.int32, (capacity, 1), 0) < starts[j][s + 1] - starts[j][s]
        rows = jnp.where(held, produced[j][span], 0.0).astype(BF16)
        grads = jnp.where(held, dx[j][span], 0.0).astype(BF16)
        out = dot(jnp.where(place, slots[j][0, 8:9], 0.0).astype(BF16), rows, 0, 0)
        grad = dot(jnp.where(place, 1.0, 0.0).astype(BF16), grads, 0, 0)
        out_sum = out if out_sum is None else out_sum + out
        grad_sum = grad if grad_sum is None else grad_sum + grad
    out_part[0] = out_sum.astype(BF16)
    grad_part[0] = grad_sum.astype(BF16)


def combine(starts, slots, produced, dx, capacity):
    local = len(starts)
    seqs, _, length = slots[0].shape
    width = produced[0].shape[1]
    seq = lambda i, *_: (i, 0, 0)
    two = lambda i, *_: (0, 0)
    rows = pl.BlockSpec(produced[0].shape, two)
    return pl.pallas_call(
        functools.partial(combine_kernel, capacity, local),
        out_shape=(sds((seqs, length, width), BF16), sds((seqs, length, width), BF16)),
        grid_spec=pltpu.PrefetchScalarGridSpec(
            num_scalar_prefetch=local,
            grid=(seqs,),
            in_specs=[pl.BlockSpec((1, 16, length), seq)] * local + [rows] * (2 * local),
            out_specs=(pl.BlockSpec((1, length, width), seq), pl.BlockSpec((1, length, width), seq)),
        ),
        compiler_params=pltpu.CompilerParams(dimension_semantics=("arbitrary",), vmem_limit_bytes=60 << 20),
        cost_estimate=pl.CostEstimate(flops=3 * 10**9, bytes_accessed=4 * 10**7, transcendentals=0),
        name="combine",
    )(*starts, *slots, *produced, *dx)


def shards(
    tokens, cotangent, gate_weights, expert_ids, seq_lengths, query_weight, key_weight, value_weight,
    output_weight, attn_gain, ffn_gain, query_gain, key_gain, expert_in, expert_out,
):
    ep = lax.axis_size("ep")
    me = lax.axis_index("ep")
    _, rows, width = tokens.shape
    length = rows * ep
    top = gate_weights.shape[2]
    local = expert_in.shape[0]
    experts = local * ep
    capacity = -(-(length * top * 9 // (8 * experts)) // 16) * 16

    gains = jnp.concatenate([attn_gain, ffn_gain]).astype(F32).reshape(-1, 128)
    few = jnp.concatenate([query_gain.astype(F32), key_gain.astype(F32), seq_lengths.astype(F32)])
    few = jnp.pad(few, (0, 128 - few.shape[0]))[None]
    packet = jnp.concatenate([gains, few], axis=0)
    packet = jnp.pad(packet, ((0, -packet.shape[0] % 8), (0, 0)))

    full, weights, packets = front(tokens, query_weight, key_weight, value_weight, packet)
    routes = jnp.concatenate([expert_ids.astype(BF16), gate_weights], axis=-1)
    routes = jnp.pad(routes, ((0, 0), (0, 0), (0, 128 - 2 * top)))
    cot_full = lax.all_gather(jnp.concatenate([cotangent, routes], axis=-1), "ep", axis=1, tiled=True)

    n = 0
    g = gains.shape[0] // 2
    gain_attn = packets[:, n : n + g].reshape(1, width)
    gain_ffn = packets[:, n + g : n + 2 * g].reshape(1, width)
    q = query_gain.shape[0]
    gain_query = packets[:, n + 2 * g, :q].reshape(1, HEAD_DIM)
    gain_key = packets[:, n + 2 * g, q : 2 * q].reshape(1, HEAD_DIM)
    lens = packets[:, n + 2 * g, 2 * q].astype(jnp.int32)
    positions = jnp.arange(length, dtype=jnp.int32)
    live = (positions[None] < lens[:, None]).astype(F32)
    living = lax.dynamic_slice_in_dim(live, me * rows, rows, axis=1)[..., None]

    half = HEAD_DIM // 2
    frequency = ROPE_BASE ** (-(jnp.arange(half, dtype=F32) * (2.0 / HEAD_DIM)))
    angles = positions.astype(F32)[:, None] * frequency[None, :]
    cos = jnp.concatenate([jnp.cos(angles)] * 2, axis=-1)
    sin = jnp.concatenate([-jnp.sin(angles), jnp.sin(angles)], axis=-1)

    normed, pre, low, ctx, part = attend(
        full, weights, output_weight, gain_attn, gain_query, gain_key, cos, sin, lens
    )
    middle, mixed = mix(part, tokens, living, gain_ffn)

    in_grads, out_grads, passes = [], [], []
    for j in range(local):
        number = (me * local + j).astype(jnp.int32)[None]
        if passes:
            number, _ = lax.optimization_barrier((number, passes[-1][1]))
        slots, starts, act, dgu, out_grad, in_grad = expert_pass(
            j, number, lens, mixed, cot_full, expert_in, expert_out, capacity, top
        )
        passes.append((slots, starts, act, dgu))
        out_grads.append(lax.psum_scatter(out_grad, "rep", scatter_dimension=0, tiled=True))
        in_grads.append(lax.psum_scatter(in_grad, "rep", scatter_dimension=0, tiled=True))
    tails = [
        expert_tail(j, starts, act, dgu, expert_in, expert_out)
        for j, (slots, starts, act, dgu) in enumerate(passes)
    ]
    out_part, grad_part = combine(
        [p[1] for p in passes], [p[0] for p in passes], [t[0] for t in tails], [t[1] for t in tails], capacity
    )
    result, mgrad, ffn_back, agrad = back(grad_part, out_part, middle, cotangent, living, gain_ffn)
    npart, wgrad, wograd, qk_back = attend_back(
        agrad, normed, pre, low, ctx, weights, output_weight, gain_query, gain_key, cos, sin, lens
    )
    token_grad, small, wrows = final(npart, wgrad, tokens, mgrad, gain_attn, ffn_back, qk_back)
    sums, small = line_sum(jnp.concatenate([wrows, wograd[None]], axis=0), small)
    share = g

    def head_share(vector):
        return lax.dynamic_slice_in_dim(vector, me * (HEAD_DIM // ep), HEAD_DIM // ep)

    return (
        result,
        token_grad,
        sums[0].astype(F32),
        sums[1].astype(F32),
        sums[2].astype(F32),
        sums[3].astype(F32),
        small[:share].reshape(-1),
        small[share : 2 * share].reshape(-1),
        head_share(small[2 * share]),
        head_share(small[2 * share + 1]),
        jnp.stack(in_grads).astype(F32),
        jnp.stack(out_grads).astype(F32),
    )


def solution(mesh):
    seq = P("rep", "ep", None)
    row, gain, expert = P("ep", None), P("ep"), P("ep", None, None)
    split = P("ep", "rep", None)

    return jax.shard_map(
        shards,
        mesh=mesh,
        in_specs=(seq, seq, seq, seq, P(("rep", "ep")), row, row, row, row, gain, gain, gain, gain, expert, expert),
        out_specs=(seq, seq, row, row, row, row, gain, gain, gain, gain, split, split),
        check_vma=False,
    )
```

```python
import functools

import jax
import jax.numpy as jnp
from jax import lax
from jax.experimental import pallas as pl
from jax.experimental.pallas import tpu as pltpu
from jax.sharding import PartitionSpec as P

HEAD_DIM = 128
EPS = 1e-06
ROPE_BASE = 50000.0
MESH = pl.DeviceIdType.MESH
F32 = jnp.float32
BF16 = jnp.bfloat16


def sds(shape, dtype):
    return jax.ShapeDtypeStruct(shape, dtype)


VM = pl.BlockSpec(memory_space=pltpu.VMEM)
AN = pl.BlockSpec(memory_space=pl.ANY)


def inverse_rms(v):
    return lax.rsqrt(jnp.mean(v * v, axis=-1, keepdims=True) + EPS)


def rms_back(v, r, ug):
    return r * ug - v * (r * r * r * jnp.mean(ug * v, axis=-1, keepdims=True))


def mix_rows(total, tok, living, gain):
    middle = tok.astype(F32) + living * total
    mixed = middle * inverse_rms(middle) * gain
    return middle, mixed.astype(BF16)


def ffn_back_rows(mixed_grad, middle, cot, living, gain):
    r = inverse_rms(middle)
    middle_grad = cot.astype(F32) + rms_back(middle, r, mixed_grad * gain)
    return middle_grad, (living * middle_grad).astype(BF16), mixed_grad * middle * r


def attn_back_rows(normed_grad, tok, middle_grad, gain):
    v = tok.astype(F32)
    r = inverse_rms(v)
    return (middle_grad + rms_back(v, r, normed_grad * gain)).astype(BF16), normed_grad * v * r


class Place:
    def __init__(self):
        me = lax.axis_index("ep")
        core, x, y = lax.rem(me, 2), lax.rem(me // 2, 2), me // 4
        self.rep = lax.axis_index("rep")
        self.me = me
        self.sb = me + 1 - 2 * core
        self.dx = 2 - 4 * x
        self.dy = 4 - 8 * y
        self.xn = me + self.dx
        self.yn = me + self.dy
        self.dg = me + self.dx + self.dy

    def push(self, src, dst, send, recv, dev):
        return pltpu.make_async_remote_copy(
            src_ref=src, dst_ref=dst, send_sem=send, recv_sem=recv, device_id=(self.rep, dev), device_id_type=MESH
        )

    def peers(self):
        sb, dx, dy = self.sb, self.dx, self.dy
        return (self.xn, self.yn, self.dg, sb, sb + dx, sb + dy, sb + dx + dy)

    def greet(self, peers):
        barrier = pltpu.get_barrier_semaphore()
        for peer in peers:
            pl.semaphore_signal(barrier, inc=1, device_id=(self.rep, peer), device_id_type=MESH)
        pl.semaphore_wait(barrier, len(peers))


class Gather:
    sems = 3

    def __init__(self, at, own, full, ssem, rsem, lsem):
        self.at, self.own, self.full, self.ssem, self.rsem, self.lsem = at, own, full, ssem, rsem, lsem
        self.rows = own.shape[1]

    @staticmethod
    def scratch(seqs):
        return [pltpu.SemaphoreType.DMA((7, seqs)), pltpu.SemaphoreType.DMA((8, seqs)), pltpu.SemaphoreType.DMA((seqs,))]

    def block(self, s, dev):
        return self.full.at[s, pl.ds(pl.multiple_of(dev * self.rows, self.rows), self.rows)]

    def copy(self, s, dev, kind, slot, to, src=None):
        block = self.block(s, dev)
        return self.at.push(block if src is None else src, block, self.ssem.at[kind, s], self.rsem.at[slot, s], to)

    def start(self, s):
        at, own = self.at, self.own.at[s]
        self.copy(s, at.me, 0, 2, at.xn, own).start()
        self.copy(s, at.me, 1, 4, at.yn, own).start()
        self.copy(s, at.me, 2, 1, at.sb, own).start()
        pltpu.make_async_copy(own, self.block(s, at.me), self.lsem.at[s]).start()

    def relay(self, s, by_y):
        at = self.at
        self.copy(s, at.xn, 0, 2, at.xn).wait_recv()
        if by_y:
            self.copy(s, at.xn, 3, 6, at.yn).start()
        self.copy(s, at.xn, 4, 3, at.sb).start()
        self.copy(s, at.yn, 1, 4, at.yn).wait_recv()
        if not by_y:
            self.copy(s, at.yn, 3, 6, at.xn).start()
        self.copy(s, at.yn, 5, 5, at.sb).start()

    def relay_far(self, s):
        at = self.at
        self.copy(s, at.dg, 3, 6, at.yn).wait_recv()
        self.copy(s, at.dg, 6, 7, at.sb).start()

    def finish(self, s):
        at = self.at
        for dev, slot in ((at.sb, 1), (at.sb + at.dx, 3), (at.sb + at.dy, 5), (at.sb + at.dx + at.dy, 7)):
            self.copy(s, dev, 0, slot, at.sb).wait_recv()
        for kind in range(7):
            self.copy(s, at.me, kind, 0, at.sb).wait_send()
        pltpu.make_async_copy(self.own.at[s], self.block(s, at.me), self.lsem.at[s]).wait()


def gather_tail(seqs, gather):
    def relay(i, _):
        gather.relay(2 * i, True)
        gather.relay(2 * i + 1, False)
        return 0

    def far(s, _):
        gather.relay_far(s)
        return 0

    def finish(s, _):
        gather.finish(s)
        return 0

    lax.fori_loop(0, seqs // 2, relay, 0)
    lax.fori_loop(0, seqs, far, 0)
    lax.fori_loop(0, seqs, finish, 0)


class Reduce:
    def __init__(self, at, part, held, x1, y1, x2, y2, hs, hr, d1s, d1r, d2s, d2r):
        self.at, self.part, self.held = at, part, held
        self.x1, self.y1, self.x2, self.y2 = x1, y1, x2, y2
        self.hs, self.hr, self.d1s, self.d1r, self.d2s, self.d2r = hs, hr, d1s, d1r, d2s, d2r
        self.half = part.shape[2] // 2

    @staticmethod
    def scratch(part):
        s, _, t, d = part.shape
        dma = pltpu.SemaphoreType.DMA
        return [
            pltpu.VMEM((s, 4, t, d), BF16),
            pltpu.VMEM((s, t // 2, d), BF16),
            pltpu.VMEM((s, t // 2, d), BF16),
            pltpu.VMEM((s, t, d), BF16),
            pltpu.VMEM((s, t, d), BF16),
            dma((4, s)),
            dma((4, s)),
            dma((2, s)),
            dma((2, s)),
            dma((2, s)),
            dma((2, s)),
        ]

    sems = 11

    def core_copy(self, s, k):
        at = self.at
        dest = (at.sb, at.sb + at.dx, at.sb + at.dy, at.sb + at.dx + at.dy)[k]
        return at.push(self.part.at[s, dest], self.held.at[s, k], self.hs.at[k, s], self.hr.at[k, s], at.sb)

    def first(self, s, k):
        at, h = self.at, self.half
        src = self.held.at[s, 3, pl.ds(k * h, h)]
        return at.push(src, (self.x1, self.y1)[k].at[s], self.d1s.at[k, s], self.d1r.at[k, s], (at.xn, at.yn)[k])

    def second(self, s, k):
        at = self.at
        src = self.held.at[s, 1 + k]
        return at.push(src, (self.x2, self.y2)[k].at[s], self.d2s.at[k, s], self.d2r.at[k, s], (at.xn, at.yn)[k])

    def start(self, s):
        for k in (3, 1, 2, 0):
            self.core_copy(s, k).start()

    def hop1(self, s):
        self.core_copy(s, 3).wait_recv()
        self.held[s, 3] = (self.held[s, 3].astype(F32) + self.part[s, self.at.dg].astype(F32)).astype(BF16)
        self.first(s, 0).start()
        self.first(s, 1).start()

    def hop2(self, s):
        h = self.half
        for k, dest, extra, rows, rest in (
            (0, self.at.xn, self.y1, pl.ds(h, h), pl.ds(0, h)),
            (1, self.at.yn, self.x1, pl.ds(0, h), pl.ds(h, h)),
        ):
            self.core_copy(s, 1 + k).wait_recv()
            self.first(s, 1 - k).wait_recv()
            held, part = self.held.at[s, 1 + k], self.part.at[s, dest]
            held[rows] = (held[rows].astype(F32) + part[rows].astype(F32) + extra[s].astype(F32)).astype(BF16)
            held[rest] = (held[rest].astype(F32) + part[rest].astype(F32)).astype(BF16)
            self.second(s, k).start()

    def total(self, s):
        self.core_copy(s, 0).wait_recv()
        self.second(s, 0).wait_recv()
        self.second(s, 1).wait_recv()
        return (
            self.part[s, self.at.me].astype(F32)
            + self.held[s, 0].astype(F32)
            + self.x2[s].astype(F32)
            + self.y2[s].astype(F32)
        )

    def finish(self, s):
        for k in range(4):
            self.core_copy(s, k).wait_send()
        for k in range(2):
            self.first(s, k).wait_send()
            self.second(s, k).wait_send()


def each(n, *steps):
    def run(s, _):
        for step in steps:
            step(s)
        return 0

    lax.fori_loop(0, n, run, 0)


COMM = dict(has_side_effects=True, vmem_limit_bytes=60 << 20)


def front_kernel(tok, wq, wk, wv, pk, full, weights, packets, tok_v, *sems):
    at = Place()
    gather = Gather(at, tok, full, *sems[:3])
    wsend, wrecv, psend, precv, local = sems[3:]
    seqs = tok.shape[0]
    block, width = wq.shape[0], weights.shape[2]
    at.greet(at.peers())
    each(seqs, gather.start)
    mine = pl.ds(pl.multiple_of(at.me * block, block), block)

    def weight_copy(m, j, dev):
        cols = pl.ds(pl.multiple_of(dev * width, width), width)
        return at.push((wq, wk, wv)[j].at[:, cols], weights.at[j, mine], wsend.at[m, j], wrecv.at[m, j], dev)

    def packet_copy(m, dev):
        return at.push(pk, packets.at[at.me], psend.at[m], precv.at[m], dev)

    own_cols = pl.ds(pl.multiple_of(at.me * width, width), width)
    own = [pltpu.make_async_copy(w.at[:, own_cols], weights.at[j, mine], local.at[j]) for j, w in enumerate((wq, wk, wv))]
    own.append(pltpu.make_async_copy(pk, packets.at[at.me], local.at[3]))
    for copy in own:
        copy.start()
    for m, dev in enumerate(at.peers()):
        packet_copy(m, dev).start()
    for m, dev in enumerate(at.peers()):
        for j in range(3):
            weight_copy(m, j, dev).start()
    gather_tail(seqs, gather)
    for m, dev in enumerate(at.peers()):
        packet_copy(m, dev).wait()
        for j in range(3):
            weight_copy(m, j, dev).wait()
    for copy in own:
        copy.wait()


def front(tokens, wq, wk, wv, packet):
    seqs, rows, width = tokens.shape
    ep = lax.axis_size("ep")
    cols = wq.shape[1] // ep
    if ep != 8:
        full = lax.all_gather(tokens, "ep", axis=1, tiled=True)
        weights = [lax.all_to_all(w, "ep", split_axis=1, concat_axis=0, tiled=True) for w in (wq, wk, wv)]
        return full, jnp.stack(weights), lax.all_gather(packet, "ep", axis=0)
    dma = pltpu.SemaphoreType.DMA
    return pl.pallas_call(
        front_kernel,
        out_shape=(
            sds((seqs, rows * ep, width), BF16),
            sds((3, wq.shape[0] * ep, cols), BF16),
            sds((ep,) + packet.shape, F32),
        ),
        in_specs=[VM] * 5,
        out_specs=(AN, AN, AN),
        scratch_shapes=[pltpu.VMEM((8, 128), F32)]
        + Gather.scratch(seqs)
        + [dma((7, 3)), dma((7, 3)), dma((7,)), dma((7,)), dma((4,))],
        compiler_params=pltpu.CompilerParams(collective_id=1, **COMM),
        name="front",
    )(tokens, wq, wk, wv, packet)


def mix_kernel(part, tok, living, gain, middle, full, own, *scratch):
    at = Place()
    seqs = tok.shape[0]
    reduce = Reduce(at, part, *scratch[: Reduce.sems])
    gather = Gather(at, own, full, *scratch[Reduce.sems :])
    at.greet((at.xn, at.yn, at.sb))
    each(seqs, reduce.start)
    each(seqs, reduce.hop1)
    each(seqs, reduce.hop2)

    def rows(s):
        mid, mixed = mix_rows(reduce.total(s), tok[s], living[s], gain[...])
        middle[s] = mid
        own[s] = mixed
        gather.start(s)

    each(seqs, rows)
    gather_tail(seqs, gather)
    each(seqs, reduce.finish)


def mix(part, tokens, living, gain):
    seqs, rows, width = tokens.shape
    ep = lax.axis_size("ep")
    if ep != 8:
        total = lax.psum_scatter(part, "ep", scatter_dimension=1, tiled=True).astype(F32)
        middle, mixed = mix_rows(total, tokens, living, gain)
        return middle, lax.all_gather(mixed, "ep", axis=1, tiled=True)
    part = part.reshape(seqs, ep, rows, width)
    return pl.pallas_call(
        mix_kernel,
        out_shape=(sds(tokens.shape, F32), sds((seqs, rows * ep, width), BF16)),
        in_specs=[VM] * 4,
        out_specs=(VM, AN),
        scratch_shapes=[pltpu.VMEM(tokens.shape, BF16)] + Reduce.scratch(part) + Gather.scratch(seqs),
        compiler_params=pltpu.CompilerParams(collective_id=2, **COMM),
        name="mix",
    )(part, tokens, living, gain)


def back_kernel(gpart, middle, cot, living, gain, mgrad, ggrad, full, own, *scratch):
    at = Place()
    seqs = cot.shape[0]
    n = Reduce.sems
    rg = Reduce(at, gpart, *scratch[:n])
    gather = Gather(at, own, full, *scratch[n:])
    at.greet((at.xn, at.yn, at.sb))
    each(seqs, rg.start)
    each(seqs, rg.hop1)
    each(seqs, rg.hop2)
    ggrad[...] = jnp.zeros_like(ggrad)

    def rows(s):
        mg, ag, back = ffn_back_rows(rg.total(s), middle[s], cot[s], living[s], gain[...])
        mgrad[s] = mg
        own[s] = ag
        ggrad[...] += jnp.sum(back, axis=0, keepdims=True)
        gather.start(s)

    each(seqs, rows)
    gather_tail(seqs, gather)
    each(seqs, rg.finish)


def back(gpart, middle, cot, living, gain):
    seqs, rows, width = cot.shape
    ep = lax.axis_size("ep")
    if ep != 8:
        mixed_grad = lax.psum_scatter(gpart, "ep", scatter_dimension=1, tiled=True).astype(F32)
        mg, ag, backs = ffn_back_rows(mixed_grad, middle, cot, living, gain)
        full = lax.all_gather(ag, "ep", axis=1, tiled=True)
        return mg, jnp.sum(backs, axis=(0, 1))[None], full
    gpart = gpart.reshape(seqs, ep, rows, width)
    return pl.pallas_call(
        back_kernel,
        out_shape=(
            sds(cot.shape, F32),
            sds((1, width), F32),
            sds((seqs, rows * ep, width), BF16),
        ),
        in_specs=[VM] * 5,
        out_specs=(VM, VM, AN),
        scratch_shapes=[pltpu.VMEM(cot.shape, BF16)] + Reduce.scratch(gpart) + Gather.scratch(seqs),
        compiler_params=pltpu.CompilerParams(collective_id=3, **COMM),
        name="back",
    )(gpart, middle, cot, living, gain)


def final_kernel(part, wgrad, tok, mgrad, gain, others, tgrad, small, wrows, ggrad, parcel, landed, *scratch):
    at = Place()
    seqs = tok.shape[0]
    n = Reduce.sems
    reduce = Reduce(at, part, *scratch[:n])
    wsend, wrecv, local, gsend, grecv = scratch[n:]
    width = wgrad.shape[2]
    block = wrows.shape[1]
    at.greet(at.peers())
    cols = pl.ds(pl.multiple_of(at.me * width, width), width)

    def weight_copy(m, dev):
        rows = pl.ds(pl.multiple_of(dev * block, block), block)
        return at.push(wgrad.at[:, rows], wrows.at[:, :, cols], wsend.at[m], wrecv.at[m], dev)

    mine = pl.ds(pl.multiple_of(at.me * block, block), block)
    own = pltpu.make_async_copy(wgrad.at[:, mine], wrows.at[:, :, cols], local)
    own.start()
    for m, dev in enumerate(at.peers()):
        weight_copy(m, dev).start()
    each(seqs, reduce.start)
    each(seqs, reduce.hop1)
    each(seqs, reduce.hop2)
    ggrad[...] = jnp.zeros_like(ggrad)

    def rows(s):
        tg, back = attn_back_rows(reduce.total(s), tok[s], mgrad[s], gain[...])
        tgrad[s] = tg
        ggrad[...] += jnp.sum(back, axis=0, keepdims=True)

    each(seqs, rows)

    parcel[...] = jnp.zeros_like(parcel)
    devices = parcel.shape[0]
    rows_of = ggrad.shape[1] // (128 * devices)
    for dev in range(devices):
        for k in range(rows_of):
            lanes = pl.ds((dev * rows_of + k) * 128, 128)
            parcel[dev, k : k + 1] = ggrad[:, lanes]
            parcel[dev, rows_of + k : rows_of + k + 1] = others[0:1, lanes]
        parcel[dev, 2 * rows_of : 2 * rows_of + 2] = others[1:3, 0:128]

    def parcel_copy(m, dev):
        return at.push(parcel.at[dev], landed.at[m], gsend.at[m], grecv.at[m], dev)

    for m, dev in enumerate(at.peers()):
        parcel_copy(m, dev).start()
    total = parcel[at.me]
    for m, dev in enumerate(at.peers()):
        parcel_copy(m, dev).wait_recv()
        total = total + landed[m]
    small[...] = total
    each(seqs, reduce.finish)
    for m, dev in enumerate(at.peers()):
        weight_copy(m, dev).wait()
        parcel_copy(m, dev).wait_send()
    own.wait()


def final(part, wgrad, tokens, mgrad, gain, ffn_back, qk_back):
    seqs, rows, width = tokens.shape
    ep = lax.axis_size("ep")
    if ep != 8:
        normed_grad = lax.psum_scatter(part, "ep", scatter_dimension=1, tiled=True).astype(F32)
        tg, backs = attn_back_rows(normed_grad, tokens, mgrad, gain)
        wrows = lax.all_to_all(wgrad, "ep", split_axis=1, concat_axis=2, tiled=True)
        share = width // ep
        small = jnp.concatenate([jnp.sum(backs, axis=(0, 1)), ffn_back[0], qk_back[0], qk_back[1]])
        small = lax.psum(small, "ep")
        mine = lax.axis_index("ep") * share
        cut = [lax.dynamic_slice_in_dim(small, k * width + mine, share).reshape(-1, 128) for k in range(2)]
        small = jnp.concatenate(cut + [small[2 * width :].reshape(2, HEAD_DIM)], axis=0)
        return tg, jnp.pad(small, ((0, 8 - small.shape[0]), (0, 0))), wrows
    others = jnp.concatenate([ffn_back, jnp.pad(qk_back[:2], ((0, 0), (0, width - HEAD_DIM)))], axis=0)
    part = part.reshape(seqs, ep, rows, width)
    dma = pltpu.SemaphoreType.DMA
    return pl.pallas_call(
        final_kernel,
        out_shape=(
            sds(tokens.shape, BF16),
            sds((8, 128), F32),
            sds((3, wgrad.shape[1] // ep, wgrad.shape[2] * ep), BF16),
        ),
        in_specs=[VM] * 6,
        out_specs=(VM, VM, AN),
        scratch_shapes=[pltpu.VMEM((1, width), F32), pltpu.VMEM((ep, 8, 128), F32), pltpu.VMEM((7, 8, 128), F32)]
        + Reduce.scratch(part)
        + [dma((7,)), dma((7,)), dma, dma((7,)), dma((7,))],
        compiler_params=pltpu.CompilerParams(collective_id=4, **COMM),
        name="final",
    )(part, wgrad, tokens, mgrad, gain, others)


def line_kernel(
    own, small, opart, mid_rows, out, small_out, result, held, met, landed, os, or_, ps, pr, qs, qr, fs, fr, ss, sr, *scratch
):
    at = Place()
    reduce = Reduce(at, opart, *scratch)
    seqs = opart.shape[0]
    z = lax.axis_index("rep")
    ep = lax.axis_index("ep")
    chunks = own.shape[0]

    def push(src, dst, send, recv, dev):
        return pltpu.make_async_remote_copy(
            src_ref=src, dst_ref=dst, send_sem=send, recv_sem=recv, device_id=(dev, ep), device_id_type=MESH
        )

    barrier = pltpu.get_barrier_semaphore()
    others = [lax.rem(z + k, 4) for k in range(1, 4)]
    for dev in others:
        pl.semaphore_signal(barrier, inc=1, device_id=(dev, ep), device_id_type=MESH)
    for dev in (at.xn, at.yn, at.sb):
        pl.semaphore_signal(barrier, inc=1, device_id=(z, dev), device_id_type=MESH)
    pl.semaphore_wait(barrier, 6)
    inner = jnp.logical_and(z > 0, z < 3)
    middle, partner, outer = 1 + z // 3, 3 - z, 3 * (z - 1)

    def inward(c):
        return push(own.at[c], held.at[c], os.at[c], or_.at[c], middle)

    def across(c):
        return push(held.at[c], met.at[c], ps.at[c], pr.at[c], partner)

    def share(c):
        return push(out.at[c], out.at[c], qs.at[c], qr.at[c], partner)

    def outward(c):
        return push(out.at[c], out.at[c], fs.at[c], fr.at[c], outer)

    def small_copy(k):
        return push(small, landed.at[k], ss.at[k], sr.at[k], others[k])

    def out_rows(s):
        result[s] = (mid_rows[s] + reduce.total(s)).astype(BF16)

    for k in range(3):
        small_copy(k).start()

    @pl.when(jnp.logical_not(inner))
    def _():
        each(chunks, lambda c: inward(c).start())
        each(seqs, reduce.start)
        each(seqs, reduce.hop1)
        each(seqs, reduce.hop2)
        each(seqs, out_rows)
        each(chunks, lambda c: outward(c).wait_recv())
        each(chunks, lambda c: inward(c).wait_send())

    def mine(c):
        return 1 + lax.rem(c, 2) == z

    @pl.when(inner)
    def _():
        each(seqs, reduce.start)
        half = seqs // 2

        def run(c, _):
            for step, lag in ((reduce.hop1, 0), (reduce.hop2, half), (out_rows, 2 * half)):

                @pl.when(jnp.logical_and(c >= lag, c < seqs + lag))
                def _():
                    step(c - lag)

            @pl.when(c < chunks)
            def _():
                inward(c).wait_recv()
                held[c] = (held[c].astype(F32) + own[c].astype(F32)).astype(BF16)

                @pl.when(jnp.logical_not(mine(c)))
                def _():
                    across(c).start()

            b = c - 1

            @pl.when(jnp.logical_and(jnp.logical_and(c >= 1, c < chunks + 1), mine(c + 1)))
            def _():
                across(b).wait_recv()
                out[b] = (held[b].astype(F32) + met[b].astype(F32)).astype(BF16)
                share(b).start()
                outward(b).start()

            a = c - 2

            @pl.when(jnp.logical_and(c >= 2, jnp.logical_not(mine(c))))
            def _():
                share(a).wait_recv()
                outward(a).start()

            return 0

        lax.fori_loop(0, chunks + 2, run, 0)

        def finish(c):
            outward(c).wait_send()

            @pl.when(mine(c))
            def _():
                share(c).wait_send()

            @pl.when(jnp.logical_not(mine(c)))
            def _():
                across(c).wait_send()

        each(chunks, finish)

    each(seqs, reduce.finish)
    total = small[...]
    for k in range(3):
        small_copy(k).wait()
        total = total + landed[k]
    small_out[...] = total


def line_sum(big, small, opart, middle):
    if lax.axis_size("rep") != 4 or lax.axis_size("ep") != 8:
        moe = lax.psum_scatter(opart, "ep", scatter_dimension=1, tiled=True).astype(F32)
        return lax.psum(big, "rep"), lax.psum(small, "rep"), (middle + moe).astype(BF16)
    seqs, tokens, width = middle.shape
    opart = opart.reshape(seqs, 8, tokens, width)
    assert 2 * seqs <= 18
    count, rows, cols = big.shape
    chunks = 16
    own = big.reshape(chunks, count * rows // chunks, cols)
    dma = pltpu.SemaphoreType.DMA
    out, small, result = pl.pallas_call(
        line_kernel,
        out_shape=(sds(own.shape, BF16), sds(small.shape, F32), sds(middle.shape, BF16)),
        in_specs=[VM] * 4,
        out_specs=(VM, VM, VM),
        scratch_shapes=[
            pltpu.VMEM(own.shape, BF16),
            pltpu.VMEM(own.shape, BF16),
            pltpu.VMEM((3,) + small.shape, F32),
        ]
        + [dma((chunks,))] * 8
        + [dma((3,))] * 2
        + Reduce.scratch(opart),
        compiler_params=pltpu.CompilerParams(collective_id=5, **COMM),
        name="line_sum",
    )(own, small, opart, middle)
    return out.reshape(big.shape), small, result


def dot(a, b, ca, cb):
    return lax.dot_general(a, b, (((ca,), (cb,)), ((), ())), preferred_element_type=F32)


def rope(v, cos, sin_turn):
    return v * cos + pltpu.roll(v, HEAD_DIM // 2, 1) * sin_turn


def probabilities(q, k, length):
    scores = dot(q, k, 1, 1) * HEAD_DIM**-0.5
    column = lax.broadcasted_iota(jnp.int32, scores.shape, 1)
    scores = jnp.where(column < length, scores, -1e9)
    p = jnp.exp(scores - jnp.max(scores, axis=-1, keepdims=True))
    return p * (1.0 / jnp.sum(p, axis=-1, keepdims=True))


def attend_kernel(lens, tok, w, wo, gain, qg, kg, cos, sin, normed, pre, low, ctx, part):
    length = lens[pl.program_id(0)]
    v = tok[0].astype(F32)
    x = (v * inverse_rms(v) * gain[...]).astype(BF16)
    normed[0] = x
    q_pre, k_pre = dot(x, w[0], 1, 0), dot(x, w[1], 1, 0)
    value = dot(x, w[2], 1, 0).astype(BF16)
    pre[0, 0], pre[1, 0] = q_pre, k_pre
    low[2, 0] = value
    for h in range(q_pre.shape[1] // HEAD_DIM):
        cols = slice(h * HEAD_DIM, (h + 1) * HEAD_DIM)
        rot = []
        for i, (u, g) in enumerate(((q_pre[:, cols], qg[...]), (k_pre[:, cols], kg[...]))):
            rot.append(rope(u * inverse_rms(u) * g, cos[...], sin[...]).astype(BF16))
            low[i, 0, :, cols] = rot[i]
        attention = probabilities(rot[0], rot[1], length).astype(BF16)
        ctx[0, :, cols] = dot(attention, value[:, cols], 1, 0).astype(BF16)
    part[0] = dot(ctx[0], wo[...], 1, 0).astype(BF16)


def attend(full, weights, wo, gain, qg, kg, cos, sin, lens):
    seqs, length, width = full.shape
    cols = weights.shape[2]
    row = lambda i, *_: (i, 0, 0)
    row2 = lambda i, *_: (0, i, 0, 0)
    two = lambda i, *_: (0, 0)
    return pl.pallas_call(
        attend_kernel,
        out_shape=(
            sds(full.shape, BF16),
            sds((2, seqs, length, cols), F32),
            sds((3, seqs, length, cols), BF16),
            sds((seqs, length, cols), BF16),
            sds(full.shape, BF16),
        ),
        grid_spec=pltpu.PrefetchScalarGridSpec(
            num_scalar_prefetch=1,
            grid=(seqs,),
            in_specs=[
                pl.BlockSpec((1, length, width), row),
                pl.BlockSpec(weights.shape, lambda i, *_: (0, 0, 0)),
                pl.BlockSpec(wo.shape, two),
                pl.BlockSpec((1, width), two),
                pl.BlockSpec((1, HEAD_DIM), two),
                pl.BlockSpec((1, HEAD_DIM), two),
                pl.BlockSpec((length, HEAD_DIM), two),
                pl.BlockSpec((length, HEAD_DIM), two),
            ],
            out_specs=(
                pl.BlockSpec((1, length, width), row),
                pl.BlockSpec((2, 1, length, cols), row2),
                pl.BlockSpec((3, 1, length, cols), row2),
                pl.BlockSpec((1, length, cols), row),
                pl.BlockSpec((1, length, width), row),
            ),
        ),
        compiler_params=pltpu.CompilerParams(dimension_semantics=("arbitrary",), vmem_limit_bytes=60 << 20),
        cost_estimate=pl.CostEstimate(flops=10**10, bytes_accessed=4 * 10**7, transcendentals=10**6),
        name="attend",
    )(lens, full, weights, wo, gain, qg, kg, cos, sin)


def attend_back_kernel(
    lens, agrad, normed, pre, low, ctx, w, wo, qg, kg, cos, sin, part, wgrad, wograd, gains, wacc, woacc
):
    s = pl.program_id(0)
    length = lens[s]

    @pl.when(s == 0)
    def _():
        wacc[...] = jnp.zeros_like(wacc)
        woacc[...] = jnp.zeros_like(woacc)
        gains[...] = jnp.zeros_like(gains)

    ag = agrad[0]
    woacc[...] += dot(ctx[0], ag, 0, 0)
    cg_all = dot(ag, wo[...], 1, 1).astype(BF16)
    scale = HEAD_DIM**-0.5
    half = HEAD_DIM // 2
    grads = ([], [], [])
    for h in range(cg_all.shape[1] // HEAD_DIM):
        cols = slice(h * HEAD_DIM, (h + 1) * HEAD_DIM)
        q, k, value, cg = low[0, 0, :, cols], low[1, 0, :, cols], low[2, 0, :, cols], cg_all[:, cols]
        attention = probabilities(q, k, length)
        grads[2].append(dot(attention.astype(BF16), cg, 0, 0).astype(BF16))
        pg = dot(cg, value, 1, 1)
        sg = (attention * (pg - jnp.sum(attention * pg, axis=-1, keepdims=True))).astype(BF16)
        for i, (rot_grad, g) in enumerate(((dot(sg, k, 1, 0), qg[...]), (dot(sg, q, 0, 0), kg[...]))):
            wgt = rot_grad * scale
            u = wgt * cos[...] + pltpu.roll(wgt * sin[...], half, 1)
            v = pre[i, 0, :, cols]
            r = inverse_rms(v)
            grads[i].append(rms_back(v, r, u * g).astype(BF16))
            gains[i : i + 1] += jnp.sum(u * v * r, axis=0, keepdims=True)
    total = None
    for i in range(3):
        g = grads[i][0] if len(grads[i]) == 1 else jnp.concatenate(grads[i], axis=1)
        wacc[i] += dot(normed[0], g, 0, 0)
        piece = dot(g, w[i], 1, 1)
        total = piece if total is None else total + piece
    part[0] = total.astype(BF16)

    @pl.when(s == pl.num_programs(0) - 1)
    def _():
        wgrad[...] = wacc[...].astype(BF16)
        wograd[...] = woacc[...].astype(BF16)


def attend_back(agrad, normed, pre, low, ctx, weights, wo, qg, kg, cos, sin, lens):
    seqs, length, width = agrad.shape
    cols = weights.shape[2]
    row = lambda i, *_: (i, 0, 0)
    row2 = lambda i, *_: (0, i, 0, 0)
    two = lambda i, *_: (0, 0)
    three = lambda i, *_: (0, 0, 0)
    return pl.pallas_call(
        attend_back_kernel,
        out_shape=(
            sds(agrad.shape, BF16),
            sds(weights.shape, BF16),
            sds(wo.shape, BF16),
            sds((8, HEAD_DIM), F32),
        ),
        grid_spec=pltpu.PrefetchScalarGridSpec(
            num_scalar_prefetch=1,
            grid=(seqs,),
            in_specs=[
                pl.BlockSpec((1, length, width), row),
                pl.BlockSpec((1, length, width), row),
                pl.BlockSpec((2, 1, length, cols), row2),
                pl.BlockSpec((3, 1, length, cols), row2),
                pl.BlockSpec((1, length, cols), row),
                pl.BlockSpec(weights.shape, three),
                pl.BlockSpec(wo.shape, two),
                pl.BlockSpec((1, HEAD_DIM), two),
                pl.BlockSpec((1, HEAD_DIM), two),
                pl.BlockSpec((length, HEAD_DIM), two),
                pl.BlockSpec((length, HEAD_DIM), two),
            ],
            out_specs=(
                pl.BlockSpec((1, length, width), row),
                pl.BlockSpec(weights.shape, three),
                pl.BlockSpec(wo.shape, two),
                pl.BlockSpec((8, HEAD_DIM), two),
            ),
            scratch_shapes=[pltpu.VMEM(weights.shape, F32), pltpu.VMEM(wo.shape, F32)],
        ),
        compiler_params=pltpu.CompilerParams(dimension_semantics=("arbitrary",), vmem_limit_bytes=60 << 20),
        cost_estimate=pl.CostEstimate(flops=2 * 10**10, bytes_accessed=4 * 10**7, transcendentals=10**6),
        name="attend_back",
    )(lens, agrad, normed, pre, low, ctx, weights, wo, qg, kg, cos, sin)


BLOCK = 256


def pack_rows(seqs, capacity):
    return -(-seqs * capacity // BLOCK) * BLOCK + BLOCK


def packed_slots(number, table, length_live, top):
    tab = table.astype(F32)
    length = tab.shape[0]
    lane = lax.broadcasted_iota(jnp.int32, tab.shape, 1)
    row = lax.broadcasted_iota(jnp.int32, tab.shape, 0)
    chosen = jnp.logical_and(jnp.logical_and(tab == number, lane < top), row < length_live)
    gates = jnp.where(chosen, pltpu.roll(tab, 128 - top, 1), 0.0).astype(BF16)
    chosen = jnp.where(chosen, 1.0, 0.0).astype(BF16)
    ones = jnp.ones((8, 128), BF16)
    hit = dot(ones, chosen, 1, 1)
    weight = dot(ones, gates, 1, 1)
    earlier = lax.broadcasted_iota(jnp.int32, (length, length), 0)
    later = lax.broadcasted_iota(jnp.int32, (length, length), 1)
    rank = dot(hit.astype(BF16), jnp.where(earlier < later, 1.0, 0.0).astype(BF16), 1, 0)
    return jnp.where(hit > 0.5, rank, -1.0), weight, jnp.sum(hit[0:1]).astype(jnp.int32)


def forward_blocks(blocks, x, dy, wi, wo, acts, dgus):
    hidden = wo.shape[0]
    part = min(hidden, 512)

    def forward(b, _):
        rows = pl.ds(pl.multiple_of(b * BLOCK, BLOCK), BLOCK)
        for h in range(hidden // part):
            gcols, ucols = pl.ds(h * part, part), pl.ds(hidden + h * part, part)
            gate = dot(x[rows], wi[:, gcols], 1, 0)
            up = dot(x[rows], wi[:, ucols], 1, 0)
            dact = dot(dy[rows], wo[gcols], 1, 1)
            sig = 1.0 / (1.0 + jnp.exp(-gate))
            silu = gate * sig
            acts[rows, gcols] = (silu * up).astype(BF16)
            dgus[rows, gcols] = (dact * up * sig * (1.0 + gate * (1.0 - sig))).astype(BF16)
            dgus[rows, ucols] = (dact * silu).astype(BF16)
        return 0

    lax.fori_loop(0, blocks, forward, 0)


def gradient_tiles(blocks, left, right, result, acc, stage, ssem, busy):
    tr, tc = acc.shape
    down, across = result.shape[0] // tr, result.shape[1] // tc

    def tile(t, _):
        rt, ct = t // across, lax.rem(t, across)
        left_cols = pl.ds(pl.multiple_of(rt * tr, tr), tr)
        right_cols = pl.ds(pl.multiple_of(ct * tc, tc), tc)

        def step(b, _):
            rows = pl.ds(pl.multiple_of(b * BLOCK, BLOCK), BLOCK)
            piece = dot(left[rows, left_cols], right[rows, right_cols], 0, 0)

            @pl.when(b == 0)
            def _():
                acc[...] = piece

            @pl.when(b > 0)
            def _():
                acc[...] += piece

            return 0

        @pl.when(blocks == 0)
        def _():
            acc[...] = jnp.zeros_like(acc)

        lax.fori_loop(0, blocks, step, 0)
        k = lax.rem(t, 2)
        out = pltpu.make_async_copy(stage.at[k], result.at[left_cols, right_cols], ssem.at[k])

        @pl.when(jnp.logical_or(t >= 2, busy))
        def _():
            out.wait()

        stage[k] = acc[...].astype(BF16)
        out.start()
        return 0

    lax.fori_loop(0, down * across, tile, 0)


def drain_tiles(result, acc, stage, ssem):
    tr, tc = acc.shape
    for k in range(2):
        pltpu.make_async_copy(stage.at[k], result.at[pl.ds(0, tr), pl.ds(0, tc)], ssem.at[k]).wait()


def first_kernel(
    capacity, top, number, lens, mixed, cot, table, w_in, w_out,
    slots0, slots1, starts, act, dgu, x_all, dy_all, out_grad,
    x, dy, wi, wo, acts, dgus, acc, stage, wsem, ssem, rsem,
):
    s = pl.program_id(0)
    seqs = pl.num_programs(0)
    width = mixed.shape[2]
    loads = [pltpu.make_async_copy(w_in.at[0], wi, wsem.at[0]), pltpu.make_async_copy(w_out.at[0], wo, wsem.at[1])]

    @pl.when(s == 0)
    def _():
        for copy in loads:
            copy.start()
        starts[0, 0] = 0
        starts[1, 0] = 0

    spread, gate_spread, spans = [], [], []
    for j, slots in enumerate((slots0, slots1)):
        slot, weight, count = packed_slots((number[0] + j).astype(F32), table[0], lens[s], top)
        slots[0, 0:8] = slot
        slots[0, 8:16] = weight
        place = lax.broadcasted_iota(jnp.int32, (capacity, slot.shape[1]), 0).astype(F32) == slot[0:1]
        spread.append(jnp.where(place, 1.0, 0.0).astype(BF16))
        gate_spread.append(jnp.where(place, weight[0:1], 0.0).astype(BF16))
        start = pl.multiple_of(starts[j, s], 16)
        spans.append(pl.ds(start, capacity))
        starts[j, s + 1] = start + (count + 15) // 16 * 16
    for target, source, weights in ((x, mixed, spread), (dy, cot, gate_spread)):
        packed = dot(jnp.concatenate(weights, axis=0), source[0], 1, 0).astype(BF16)
        for j in range(2):
            target[j, spans[j]] = packed[j * capacity : (j + 1) * capacity]

    @pl.when(s == seqs - 1)
    def _():
        for j in range(2):
            tail = pl.ds(pl.multiple_of(starts[j, s] + capacity, 16), BLOCK)
            x[j, tail] = jnp.zeros((BLOCK, width), BF16)
            dy[j, tail] = jnp.zeros((BLOCK, width), BF16)
        saves = [pltpu.make_async_copy(x, x_all, rsem.at[0]), pltpu.make_async_copy(dy.at[1], dy_all, rsem.at[1])]
        for copy in saves:
            copy.start()
        blocks = (starts[0, seqs] + BLOCK - 1) // BLOCK
        for copy in loads:
            copy.wait()
        forward_blocks(blocks, x.at[0], dy.at[0], wi, wo, acts, dgus)
        saves += [pltpu.make_async_copy(acts, act, rsem.at[2]), pltpu.make_async_copy(dgus, dgu, rsem.at[3])]
        for copy in saves[2:]:
            copy.start()
        gradient_tiles(blocks, acts, dy.at[0], out_grad, acc, stage, ssem, False)
        drain_tiles(out_grad, acc, stage, ssem)
        for copy in saves:
            copy.wait()


def expert_first(number, lens, mixed, cot, w_in, w_out, capacity, top):
    seqs, length, width = mixed.shape
    hidden = w_out.shape[1]
    rows = pack_rows(seqs, capacity)
    dma = pltpu.SemaphoreType.DMA
    seq = lambda i, *_: (i, 0, 0)
    slot_spec = pl.BlockSpec((1, 16, length), seq)
    return pl.pallas_call(
        functools.partial(first_kernel, capacity, top),
        out_shape=(
            sds((seqs, 16, length), F32),
            sds((seqs, 16, length), F32),
            sds((2, seqs + 1), jnp.int32),
            sds((rows, hidden), BF16),
            sds((rows, 2 * hidden), BF16),
            sds((2, rows, width), BF16),
            sds((rows, width), BF16),
            sds((hidden, width), BF16),
        ),
        grid_spec=pltpu.PrefetchScalarGridSpec(
            num_scalar_prefetch=2,
            grid=(seqs,),
            in_specs=[
                pl.BlockSpec((1, length, width), seq),
                pl.BlockSpec((1, length, width), seq),
                pl.BlockSpec((1, length, 128), lambda i, *_: (i, 0, width // 128)),
                AN,
                AN,
            ],
            out_specs=(slot_spec, slot_spec, pl.BlockSpec(memory_space=pltpu.SMEM), AN, AN, AN, AN, AN),
            scratch_shapes=[
                pltpu.VMEM((2, rows, width), BF16),
                pltpu.VMEM((2, rows, width), BF16),
                pltpu.VMEM(w_in.shape[1:], BF16),
                pltpu.VMEM(w_out.shape[1:], BF16),
                pltpu.VMEM((rows, hidden), BF16),
                pltpu.VMEM((rows, 2 * hidden), BF16),
                pltpu.VMEM((512, 1024), F32),
                pltpu.VMEM((2, 512, 1024), BF16),
                dma((2,)),
                dma((2,)),
                dma((4,)),
            ],
        ),
        compiler_params=pltpu.CompilerParams(dimension_semantics=("arbitrary",), vmem_limit_bytes=62 << 20),
        cost_estimate=pl.CostEstimate(flops=2 * 10**10, bytes_accessed=6 * 10**7, transcendentals=10**6),
        name="expert_first",
    )(number, lens, mixed, cot, cot, w_in, w_out)


def in_grad_kernel(starts, x_all, dgu, in_grad, x, dgus, acc, stage, lsem, ssem):
    blocks = (starts[0, starts.shape[1] - 1] + BLOCK - 1) // BLOCK

    def load(b):
        rows = pl.ds(pl.multiple_of(b * BLOCK, BLOCK), BLOCK)
        return (
            pltpu.make_async_copy(x_all.at[0, rows], x.at[rows], lsem.at[0, b]),
            pltpu.make_async_copy(dgu.at[rows], dgus.at[rows], lsem.at[1, b]),
        )

    def run(b, action):
        for copy in load(b):
            getattr(copy, action)()
        return 0

    lax.fori_loop(0, blocks, lambda b, _: run(b, "start"), 0)
    lax.fori_loop(0, blocks, lambda b, _: run(b, "wait"), 0)
    gradient_tiles(blocks, x, dgus, in_grad, acc, stage, ssem, False)
    drain_tiles(in_grad, acc, stage, ssem)


def first_in_grad(starts, x_all, dgu):
    rows, width = x_all.shape[1:]
    dma = pltpu.SemaphoreType.DMA
    return pl.pallas_call(
        in_grad_kernel,
        out_shape=sds((width, dgu.shape[1]), BF16),
        grid_spec=pltpu.PrefetchScalarGridSpec(
            num_scalar_prefetch=1,
            grid=(1,),
            in_specs=[AN, AN],
            out_specs=AN,
            scratch_shapes=[
                pltpu.VMEM((rows, width), BF16),
                pltpu.VMEM(dgu.shape, BF16),
                pltpu.VMEM((512, 2048), F32),
                pltpu.VMEM((2, 512, 2048), BF16),
                dma((2, rows // BLOCK)),
                dma((2,)),
            ],
        ),
        compiler_params=pltpu.CompilerParams(dimension_semantics=("arbitrary",), vmem_limit_bytes=60 << 20),
        cost_estimate=pl.CostEstimate(flops=10**10, bytes_accessed=2 * 10**7, transcendentals=0),
        name="first_in_grad",
    )(starts, x_all, dgu)


def second_kernel(
    starts, x_all, dy_all, w_in, w_out, act, dgu, out_grad, in_grad,
    x, dy, wi, wo, acts, dgus, acc, stage, wsem, lsem, ssem, rsem,
):
    blocks = (starts[1, starts.shape[1] - 1] + BLOCK - 1) // BLOCK
    loads = [pltpu.make_async_copy(w_in.at[1], wi, wsem.at[0]), pltpu.make_async_copy(w_out.at[1], wo, wsem.at[1])]

    def load(b, action):
        rows = pl.ds(pl.multiple_of(b * BLOCK, BLOCK), BLOCK)
        for copy in (
            pltpu.make_async_copy(x_all.at[1, rows], x.at[rows], lsem.at[0, b]),
            pltpu.make_async_copy(dy_all.at[rows], dy.at[rows], lsem.at[1, b]),
        ):
            getattr(copy, action)()
        return 0

    for copy in loads:
        copy.start()
    lax.fori_loop(0, blocks, lambda b, _: load(b, "start"), 0)
    for copy in loads:
        copy.wait()
    lax.fori_loop(0, blocks, lambda b, _: load(b, "wait"), 0)
    forward_blocks(blocks, x, dy, wi, wo, acts, dgus)
    saves = [pltpu.make_async_copy(acts, act, rsem.at[0]), pltpu.make_async_copy(dgus, dgu, rsem.at[1])]
    for copy in saves:
        copy.start()
    gradient_tiles(blocks, x, dgus, in_grad, acc, stage, ssem, False)
    gradient_tiles(blocks, acts, dy, out_grad, acc, stage, ssem, True)
    drain_tiles(out_grad, acc, stage, ssem)
    for copy in saves:
        copy.wait()


def expert_second(starts, x_all, dy_all, w_in, w_out):
    rows, width = dy_all.shape
    hidden = w_out.shape[1]
    dma = pltpu.SemaphoreType.DMA
    return pl.pallas_call(
        second_kernel,
        out_shape=(
            sds((rows, hidden), BF16),
            sds((rows, 2 * hidden), BF16),
            sds((hidden, width), BF16),
            sds((width, 2 * hidden), BF16),
        ),
        grid_spec=pltpu.PrefetchScalarGridSpec(
            num_scalar_prefetch=1,
            grid=(1,),
            in_specs=[AN] * 4,
            out_specs=(AN, AN, AN, AN),
            scratch_shapes=[
                pltpu.VMEM((rows, width), BF16),
                pltpu.VMEM((rows, width), BF16),
                pltpu.VMEM(w_in.shape[1:], BF16),
                pltpu.VMEM(w_out.shape[1:], BF16),
                pltpu.VMEM((rows, hidden), BF16),
                pltpu.VMEM((rows, 2 * hidden), BF16),
                pltpu.VMEM((512, 2048), F32),
                pltpu.VMEM((2, 512, 2048), BF16),
                dma((2,)),
                dma((2, rows // BLOCK)),
                dma((2,)),
                dma((2,)),
            ],
        ),
        compiler_params=pltpu.CompilerParams(dimension_semantics=("arbitrary",), vmem_limit_bytes=60 << 20),
        cost_estimate=pl.CostEstimate(flops=25 * 10**9, bytes_accessed=6 * 10**7, transcendentals=10**6),
        name="expert_second",
    )(starts, x_all, dy_all, w_in, w_out)


def tail_kernel(j, starts, act, dgu, w_in, w_out, produced, dx):
    @pl.when(pl.program_id(0) * BLOCK < starts[j, starts.shape[1] - 1])
    def _():
        produced[...] = dot(act[...], w_out[...], 1, 0).astype(BF16)
        dx[...] = dot(dgu[...], w_in[...], 1, 1).astype(BF16)


def expert_tail(j, starts, act, dgu, w_in, w_out):
    rows, hidden = act.shape
    width = w_in.shape[1]
    last = starts.shape[1] - 1
    block = lambda i, st: (jnp.maximum(jnp.minimum(i, (st[j, last] + BLOCK - 1) // BLOCK - 1), 0), 0)
    return pl.pallas_call(
        functools.partial(tail_kernel, j),
        out_shape=(sds((rows, width), BF16), sds((rows, width), BF16)),
        grid_spec=pltpu.PrefetchScalarGridSpec(
            num_scalar_prefetch=1,
            grid=(rows // BLOCK - 1,),
            in_specs=[
                pl.BlockSpec((BLOCK, hidden), block),
                pl.BlockSpec((BLOCK, 2 * hidden), block),
                pl.BlockSpec((None,) + w_in.shape[1:], lambda i, *_: (j, 0, 0)),
                pl.BlockSpec((None,) + w_out.shape[1:], lambda i, *_: (j, 0, 0)),
            ],
            out_specs=(pl.BlockSpec((BLOCK, width), block), pl.BlockSpec((BLOCK, width), block)),
        ),
        compiler_params=pltpu.CompilerParams(dimension_semantics=("arbitrary",), vmem_limit_bytes=60 << 20),
        cost_estimate=pl.CostEstimate(flops=12 * 10**9, bytes_accessed=3 * 10**7, transcendentals=0),
        name="expert_tail",
    )(starts, act, dgu, w_in, w_out)


def combine_kernel(capacity, local, *refs):
    s = pl.program_id(0)
    starts = refs[0]
    slots = refs[1 : 1 + local]
    produced = refs[1 + local : 1 + 2 * local]
    dx = refs[1 + 2 * local : 1 + 3 * local]
    out_part, grad_part = refs[1 + 3 * local :]
    out_sum, grad_sum = None, None
    for j in range(local):
        length = slots[j].shape[2]
        column = lax.broadcasted_iota(jnp.int32, (capacity, length), 0).astype(F32)
        place = column == slots[j][0, 0:1]
        span = pl.ds(pl.multiple_of(starts[j, s], 16), capacity)
        held = lax.broadcasted_iota(jnp.int32, (capacity, 1), 0) < starts[j, s + 1] - starts[j, s]
        rows = jnp.where(held, produced[j][span], 0.0).astype(BF16)
        grads = jnp.where(held, dx[j][span], 0.0).astype(BF16)
        out = dot(jnp.where(place, slots[j][0, 8:9], 0.0).astype(BF16), rows, 0, 0)
        grad = dot(jnp.where(place, 1.0, 0.0).astype(BF16), grads, 0, 0)
        out_sum = out if out_sum is None else out_sum + out
        grad_sum = grad if grad_sum is None else grad_sum + grad
    out_part[0] = out_sum.astype(BF16)
    grad_part[0] = grad_sum.astype(BF16)


def combine(starts, slots, produced, dx, capacity):
    local = len(slots)
    seqs, _, length = slots[0].shape
    width = produced[0].shape[1]
    seq = lambda i, *_: (i, 0, 0)
    two = lambda i, *_: (0, 0)
    rows = pl.BlockSpec(produced[0].shape, two)
    return pl.pallas_call(
        functools.partial(combine_kernel, capacity, local),
        out_shape=(sds((seqs, length, width), BF16), sds((seqs, length, width), BF16)),
        grid_spec=pltpu.PrefetchScalarGridSpec(
            num_scalar_prefetch=1,
            grid=(seqs,),
            in_specs=[pl.BlockSpec((1, 16, length), seq)] * local + [rows] * (2 * local),
            out_specs=(pl.BlockSpec((1, length, width), seq), pl.BlockSpec((1, length, width), seq)),
        ),
        compiler_params=pltpu.CompilerParams(dimension_semantics=("arbitrary",), vmem_limit_bytes=60 << 20),
        cost_estimate=pl.CostEstimate(flops=3 * 10**9, bytes_accessed=4 * 10**7, transcendentals=0),
        name="combine",
    )(starts, *slots, *produced, *dx)


def shards(
    tokens, cotangent, gate_weights, expert_ids, seq_lengths, query_weight, key_weight, value_weight,
    output_weight, attn_gain, ffn_gain, query_gain, key_gain, expert_in, expert_out,
):
    ep = lax.axis_size("ep")
    me = lax.axis_index("ep")
    _, rows, width = tokens.shape
    length = rows * ep
    top = gate_weights.shape[2]
    local = expert_in.shape[0]
    experts = local * ep
    capacity = -(-(length * top * 9 // (8 * experts)) // 16) * 16

    gains = jnp.concatenate([attn_gain, ffn_gain]).astype(F32).reshape(-1, 128)
    few = jnp.concatenate([query_gain.astype(F32), key_gain.astype(F32), seq_lengths.astype(F32)])
    few = jnp.pad(few, (0, 128 - few.shape[0]))[None]
    packet = jnp.concatenate([gains, few], axis=0)
    packet = jnp.pad(packet, ((0, -packet.shape[0] % 8), (0, 0)))

    full, weights, packets = front(tokens, query_weight, key_weight, value_weight, packet)
    routes = jnp.concatenate([expert_ids.astype(BF16), gate_weights], axis=-1)
    routes = jnp.pad(routes, ((0, 0), (0, 0), (0, 128 - 2 * top)))
    routed, packets = lax.optimization_barrier((jnp.concatenate([cotangent, routes], axis=-1), packets))
    cot_full = lax.all_gather(routed, "ep", axis=1, tiled=True)

    n = 0
    g = gains.shape[0] // 2
    gain_attn = packets[:, n : n + g].reshape(1, width)
    gain_ffn = packets[:, n + g : n + 2 * g].reshape(1, width)
    q = query_gain.shape[0]
    gain_query = packets[:, n + 2 * g, :q].reshape(1, HEAD_DIM)
    gain_key = packets[:, n + 2 * g, q : 2 * q].reshape(1, HEAD_DIM)
    lens = packets[:, n + 2 * g, 2 * q].astype(jnp.int32)
    positions = jnp.arange(length, dtype=jnp.int32)
    live = (positions[None] < lens[:, None]).astype(F32)
    living = lax.dynamic_slice_in_dim(live, me * rows, rows, axis=1)[..., None]

    half = HEAD_DIM // 2
    frequency = ROPE_BASE ** (-(jnp.arange(half, dtype=F32) * (2.0 / HEAD_DIM)))
    angles = positions.astype(F32)[:, None] * frequency[None, :]
    cos = jnp.concatenate([jnp.cos(angles)] * 2, axis=-1)
    sin = jnp.concatenate([-jnp.sin(angles), jnp.sin(angles)], axis=-1)

    normed, pre, low, ctx, part = attend(
        full, weights, output_weight, gain_attn, gain_query, gain_key, cos, sin, lens
    )
    middle, mixed = mix(part, tokens, living, gain_ffn)

    number = (me * local).astype(jnp.int32)[None]
    slots0, slots1, starts, act0, dgu0, x_all, dy_all, out_grad0 = expert_first(
        number, lens, mixed, cot_full, expert_in, expert_out, capacity, top
    )

    def over_rep(value):
        return lax.psum_scatter(value, "rep", scatter_dimension=0, tiled=True)

    out0 = over_rep(out_grad0)
    in_grad0 = first_in_grad(starts, x_all, dgu0)
    in0 = over_rep(in_grad0)
    x_all, _ = lax.optimization_barrier((x_all, in_grad0))
    act1, dgu1, out_grad1, in_grad1 = expert_second(starts, x_all, dy_all, expert_in, expert_out)
    in1 = over_rep(in_grad1)
    out1 = over_rep(out_grad1)
    produced0, dx0 = expert_tail(0, starts, act0, dgu0, expert_in, expert_out)
    produced1, dx1 = expert_tail(1, starts, act1, dgu1, expert_in, expert_out)
    out_part, grad_part = combine(starts, (slots0, slots1), (produced0, produced1), (dx0, dx1), capacity)

    mgrad, ffn_back, agrad = back(grad_part, middle, cotangent, living, gain_ffn)
    npart, wgrad, wograd, qk_back = attend_back(
        agrad, normed, pre, low, ctx, weights, output_weight, gain_query, gain_key, cos, sin, lens
    )
    token_grad, small, wrows = final(npart, wgrad, tokens, mgrad, gain_attn, ffn_back, qk_back)
    sums, small, result = line_sum(jnp.concatenate([wrows, wograd[None]], axis=0), small, out_part, middle)
    share = g

    def head_share(vector):
        return lax.dynamic_slice_in_dim(vector, me * (HEAD_DIM // ep), HEAD_DIM // ep)

    return (
        result,
        token_grad,
        sums[0].astype(F32),
        sums[1].astype(F32),
        sums[2].astype(F32),
        sums[3].astype(F32),
        small[:share].reshape(-1),
        small[share : 2 * share].reshape(-1),
        head_share(small[2 * share]),
        head_share(small[2 * share + 1]),
        jnp.stack([in0, in1]).astype(F32),
        jnp.stack([out0, out1]).astype(F32),
    )


def solution(mesh):
    seq = P("rep", "ep", None)
    row, gain, expert = P("ep", None), P("ep"), P("ep", None, None)
    split = P("ep", "rep", None)

    return jax.shard_map(
        shards,
        mesh=mesh,
        in_specs=(seq, seq, seq, seq, P(("rep", "ep")), row, row, row, row, gain, gain, gain, gain, expert, expert),
        out_specs=(seq, seq, row, row, row, row, gain, gain, gain, gain, split, split),
        check_vma=False,
    )
```

```python
import functools

import jax
import jax.numpy as jnp
import numpy as np
from jax import lax
from jax.experimental import pallas as pl
from jax.experimental.pallas import tpu as pltpu
from jax.sharding import PartitionSpec as P

HEAD_DIM = 128
EPS = 1e-06
ROPE_BASE = 50000.0
MESH = pl.DeviceIdType.MESH
F32 = jnp.float32
BF16 = jnp.bfloat16


def sds(shape, dtype):
    return jax.ShapeDtypeStruct(shape, dtype)


VM = pl.BlockSpec(memory_space=pltpu.VMEM)
AN = pl.BlockSpec(memory_space=pl.ANY)


def inverse_rms(v):
    return lax.rsqrt(jnp.mean(v * v, axis=-1, keepdims=True) + EPS)


def rms_back(v, r, ug):
    return r * ug - v * (r * r * r * jnp.mean(ug * v, axis=-1, keepdims=True))


def mix_rows(total, tok, living, gain):
    middle = tok.astype(F32) + living * total
    mixed = middle * inverse_rms(middle) * gain
    return middle, mixed.astype(BF16)


def ffn_back_rows(mixed_grad, middle, cot, living, gain):
    r = inverse_rms(middle)
    middle_grad = cot.astype(F32) + rms_back(middle, r, mixed_grad * gain)
    return middle_grad, (living * middle_grad).astype(BF16), mixed_grad * middle * r


def attn_back_rows(normed_grad, tok, middle_grad, gain):
    v = tok.astype(F32)
    r = inverse_rms(v)
    return (middle_grad + rms_back(v, r, normed_grad * gain)).astype(BF16), normed_grad * v * r


def seq_len(small, s):
    lane = lax.broadcasted_iota(jnp.int32, (1, 128), 1)
    return jnp.sum(jnp.where(lane == s, small[2:3, :], 0.0), axis=1, keepdims=True)


def live_rows(small, s, me, rows):
    place = (lax.broadcasted_iota(jnp.int32, (rows, 1), 0) + me * rows).astype(F32)
    return jnp.where(place < seq_len(small, s), 1.0, 0.0)


class Place:
    def __init__(self):
        me = lax.axis_index("ep")
        core, x, y = lax.rem(me, 2), lax.rem(me // 2, 2), me // 4
        self.rep = lax.axis_index("rep")
        self.me = me
        self.sb = me + 1 - 2 * core
        self.dx = 2 - 4 * x
        self.dy = 4 - 8 * y
        self.xn = me + self.dx
        self.yn = me + self.dy
        self.dg = me + self.dx + self.dy

    def push(self, src, dst, send, recv, dev):
        return pltpu.make_async_remote_copy(
            src_ref=src, dst_ref=dst, send_sem=send, recv_sem=recv, device_id=(self.rep, dev), device_id_type=MESH
        )

    def peers(self):
        sb, dx, dy = self.sb, self.dx, self.dy
        return (self.xn, self.yn, self.dg, sb, sb + dx, sb + dy, sb + dx + dy)

    def greet(self, peers):
        barrier = pltpu.get_barrier_semaphore()
        for peer in peers:
            pl.semaphore_signal(barrier, inc=1, device_id=(self.rep, peer), device_id_type=MESH)
        pl.semaphore_wait(barrier, len(peers))


class Gather:
    sems = 3

    def __init__(self, at, own, full, ssem, rsem, lsem):
        self.at, self.own, self.full, self.ssem, self.rsem, self.lsem = at, own, full, ssem, rsem, lsem
        self.rows = own.shape[1]

    @staticmethod
    def scratch(seqs):
        return [pltpu.SemaphoreType.DMA((7, seqs)), pltpu.SemaphoreType.DMA((8, seqs)), pltpu.SemaphoreType.DMA((seqs,))]

    def block(self, s, dev):
        return self.full.at[s, pl.ds(pl.multiple_of(dev * self.rows, self.rows), self.rows)]

    def copy(self, s, dev, kind, slot, to, src=None):
        block = self.block(s, dev)
        return self.at.push(block if src is None else src, block, self.ssem.at[kind, s], self.rsem.at[slot, s], to)

    def start(self, s):
        at, own = self.at, self.own.at[s]
        self.copy(s, at.me, 0, 2, at.xn, own).start()
        self.copy(s, at.me, 1, 4, at.yn, own).start()
        self.copy(s, at.me, 2, 1, at.sb, own).start()
        pltpu.make_async_copy(own, self.block(s, at.me), self.lsem.at[s]).start()

    def relay(self, s, by_y):
        at = self.at
        self.copy(s, at.xn, 0, 2, at.xn).wait_recv()
        if by_y:
            self.copy(s, at.xn, 3, 6, at.yn).start()
        self.copy(s, at.xn, 4, 3, at.sb).start()
        self.copy(s, at.yn, 1, 4, at.yn).wait_recv()
        if not by_y:
            self.copy(s, at.yn, 3, 6, at.xn).start()
        self.copy(s, at.yn, 5, 5, at.sb).start()

    def relay_far(self, s):
        at = self.at
        self.copy(s, at.dg, 3, 6, at.yn).wait_recv()
        self.copy(s, at.dg, 6, 7, at.sb).start()

    def finish(self, s):
        at = self.at
        for dev, slot in ((at.sb, 1), (at.sb + at.dx, 3), (at.sb + at.dy, 5), (at.sb + at.dx + at.dy, 7)):
            self.copy(s, dev, 0, slot, at.sb).wait_recv()
        for kind in range(7):
            self.copy(s, at.me, kind, 0, at.sb).wait_send()
        pltpu.make_async_copy(self.own.at[s], self.block(s, at.me), self.lsem.at[s]).wait()


def gather_tail(seqs, gather):
    def relay(i, _):
        gather.relay(2 * i, True)
        gather.relay(2 * i + 1, False)
        return 0

    def far(s, _):
        gather.relay_far(s)
        return 0

    def finish(s, _):
        gather.finish(s)
        return 0

    lax.fori_loop(0, seqs // 2, relay, 0)
    lax.fori_loop(0, seqs, far, 0)
    lax.fori_loop(0, seqs, finish, 0)


class Reduce:
    def __init__(self, at, part, held, x1, y1, x2, y2, hs, hr, d1s, d1r, d2s, d2r):
        self.at, self.part, self.held = at, part, held
        self.x1, self.y1, self.x2, self.y2 = x1, y1, x2, y2
        self.hs, self.hr, self.d1s, self.d1r, self.d2s, self.d2r = hs, hr, d1s, d1r, d2s, d2r
        self.half = part.shape[2] // 2

    @staticmethod
    def scratch(part):
        s, _, t, d = part.shape
        dma = pltpu.SemaphoreType.DMA
        return [
            pltpu.VMEM((s, 4, t, d), BF16),
            pltpu.VMEM((s, t // 2, d), BF16),
            pltpu.VMEM((s, t // 2, d), BF16),
            pltpu.VMEM((s, t, d), BF16),
            pltpu.VMEM((s, t, d), BF16),
            dma((4, s)),
            dma((4, s)),
            dma((2, s)),
            dma((2, s)),
            dma((2, s)),
            dma((2, s)),
        ]

    sems = 11

    def core_copy(self, s, k):
        at = self.at
        dest = (at.sb, at.sb + at.dx, at.sb + at.dy, at.sb + at.dx + at.dy)[k]
        return at.push(self.part.at[s, dest], self.held.at[s, k], self.hs.at[k, s], self.hr.at[k, s], at.sb)

    def first(self, s, k):
        at, h = self.at, self.half
        src = self.held.at[s, 3, pl.ds(k * h, h)]
        return at.push(src, (self.x1, self.y1)[k].at[s], self.d1s.at[k, s], self.d1r.at[k, s], (at.xn, at.yn)[k])

    def second(self, s, k):
        at = self.at
        src = self.held.at[s, 1 + k]
        return at.push(src, (self.x2, self.y2)[k].at[s], self.d2s.at[k, s], self.d2r.at[k, s], (at.xn, at.yn)[k])

    def start(self, s):
        for k in (3, 1, 2, 0):
            self.core_copy(s, k).start()

    def hop1(self, s):
        self.core_copy(s, 3).wait_recv()
        self.held[s, 3] = (self.held[s, 3].astype(F32) + self.part[s, self.at.dg].astype(F32)).astype(BF16)
        self.first(s, 0).start()
        self.first(s, 1).start()

    def hop2(self, s):
        h = self.half
        for k, dest, extra, rows, rest in (
            (0, self.at.xn, self.y1, pl.ds(h, h), pl.ds(0, h)),
            (1, self.at.yn, self.x1, pl.ds(0, h), pl.ds(h, h)),
        ):
            self.core_copy(s, 1 + k).wait_recv()
            self.first(s, 1 - k).wait_recv()
            held, part = self.held.at[s, 1 + k], self.part.at[s, dest]
            held[rows] = (held[rows].astype(F32) + part[rows].astype(F32) + extra[s].astype(F32)).astype(BF16)
            held[rest] = (held[rest].astype(F32) + part[rest].astype(F32)).astype(BF16)
            self.second(s, k).start()

    def total(self, s):
        self.core_copy(s, 0).wait_recv()
        self.second(s, 0).wait_recv()
        self.second(s, 1).wait_recv()
        return (
            self.part[s, self.at.me].astype(F32)
            + self.held[s, 0].astype(F32)
            + self.x2[s].astype(F32)
            + self.y2[s].astype(F32)
        )

    def finish(self, s):
        for k in range(4):
            self.core_copy(s, k).wait_send()
        for k in range(2):
            self.first(s, k).wait_send()
            self.second(s, k).wait_send()


def each(n, *steps):
    def run(s, _):
        for step in steps:
            step(s)
        return 0

    lax.fori_loop(0, n, run, 0)


COMM = dict(has_side_effects=True, vmem_limit_bytes=60 << 20)


def front_kernel(
    tok, cot, ids, gates, wq, wk, wv, pk, full, weights, routed, gains, small,
    packets, gsend, grecv, glocal, wsend, wrecv, psend, precv, rsend, rrecv, lsend, lrecv, local,
):
    at = Place()
    z = at.rep
    gather = Gather(at, tok, full, gsend, grecv, glocal)
    seqs, _, width = tok.shape
    top = ids.shape[1]
    block, cols = wq.shape[0], weights.shape[2]
    quarter = block // 4
    peers = at.peers()
    barrier = pltpu.get_barrier_semaphore()
    line = [lax.rem(z + k, 4) for k in range(1, 4)]
    for dev in line:
        pl.semaphore_signal(barrier, inc=1, device_id=(dev, at.me), device_id_type=MESH)
    for dev in peers:
        pl.semaphore_signal(barrier, inc=1, device_id=(z, dev), device_id_type=MESH)
    pl.semaphore_wait(barrier, 10)

    def packet_copy(m, dev):
        return at.push(pk, packets.at[at.me], psend.at[m], precv.at[m], dev)

    def weight_copy(m, j, dev):
        theirs = pl.ds(pl.multiple_of(dev * cols, cols), cols)
        src = (wq, wk, wv)[j].at[pl.ds(pl.multiple_of(z * quarter, quarter), quarter), theirs]
        dst = weights.at[j, pl.ds(pl.multiple_of(at.me * block + z * quarter, quarter), quarter)]
        return at.push(src, dst, wsend.at[m, j], wrecv.at[m, j], dev)

    def weight_landed(m, j, dev):
        dst = weights.at[j, pl.ds(pl.multiple_of(dev * block + z * quarter, quarter), quarter)]
        return at.push(dst, dst, wsend.at[m, j], wrecv.at[m, j], dev)

    def walk(m, q, right):
        part = weights.at[:, pl.ds(pl.multiple_of(peers[m] * block + q * quarter, quarter), quarter)]
        send, recv, dev = (rsend, rrecv, z + 1) if right else (lsend, lrecv, z - 1)
        return pltpu.make_async_remote_copy(
            src_ref=part, dst_ref=part, send_sem=send.at[m, q], recv_sem=recv.at[m, q],
            device_id=(dev, at.me), device_id_type=MESH,
        )

    for m, dev in enumerate(peers):
        packet_copy(m, dev).start()
        for j in range(3):
            weight_copy(m, j, dev).start()
    each(seqs, gather.start)
    own_cols = pl.ds(pl.multiple_of(at.me * cols, cols), cols)
    mine = pl.ds(pl.multiple_of(at.me * block, block), block)
    own = [pltpu.make_async_copy(w.at[:, own_cols], weights.at[j, mine], local.at[j]) for j, w in enumerate((wq, wk, wv))]
    for copy in own:
        copy.start()

    place = lax.broadcasted_iota(jnp.int32, (top, 128), 0)
    lane = lax.broadcasted_iota(jnp.int32, (top, 128), 1)
    first = jnp.where(lane == place, 1.0, 0.0).astype(BF16)
    second = jnp.where(lane == place + top, 1.0, 0.0).astype(BF16)

    def join(s):
        routed[s, :, 0:width] = cot[s]
        table = dot(ids[s].astype(F32).astype(BF16), first, 0, 0) + dot(gates[s], second, 0, 0)
        routed[s, :, width : width + 128] = table.astype(BF16)

    each(seqs, join)

    for m, dev in enumerate(peers):
        for j in range(3):
            weight_landed(m, j, dev).wait_recv()

        @pl.when(z < 3)
        def _():
            walk(m, z, True).start()

        @pl.when(z > 0)
        def _():
            walk(m, z, False).start()

    def pass_on(d):
        @pl.when(z - d >= 0)
        def _():
            for m in range(7):
                walk(m, z - d, True).wait_recv()

                @pl.when(z < 3)
                def _():
                    walk(m, z - d, True).start()

        @pl.when(z + d <= 3)
        def _():
            for m in range(7):
                walk(m, z + d, False).wait_recv()

                @pl.when(z > 0)
                def _():
                    walk(m, z + d, False).start()

    def relay(i, _):
        gather.relay(2 * i, True)
        gather.relay(2 * i + 1, False)
        return 0

    pairs = seqs // 2
    lax.fori_loop(0, pairs // 2, relay, 0)
    pass_on(1)
    lax.fori_loop(pairs // 2, pairs, relay, 0)
    pass_on(2)
    each(seqs, gather.relay_far)
    for m, dev in enumerate(peers):
        packet_copy(m, dev).wait_recv()
    packets[at.me] = pk[...]
    devices = packets.shape[0]
    share = width // (128 * devices)
    heads = HEAD_DIM // devices
    gains[...] = jnp.zeros_like(gains)
    small[...] = jnp.zeros_like(small)
    for o in range(devices):
        for k in range(share):
            lanes = pl.ds((o * share + k) * 128, 128)
            gains[0:1, lanes] = packets[o, k : k + 1]
            gains[1:2, lanes] = packets[o, share + k : share + k + 1]
        base = 2 * share
        small[0:1] += pltpu.roll(packets[o, base : base + 1], o * heads, 1)
        small[1:2] += pltpu.roll(packets[o, base + 1 : base + 2], o * heads, 1)
        small[2:3] += pltpu.roll(packets[o, base + 2 : base + 3], o, 1)
    each(seqs, gather.finish)
    pass_on(3)

    def sent(q, going, right):
        @pl.when(going)
        def _():
            for m in range(7):
                walk(m, q, right).wait_send()

    for q in range(4):
        sent(q, jnp.logical_and(q <= z, z < 3), True)
        sent(q, jnp.logical_and(q >= z, z > 0), False)
    for m, dev in enumerate(peers):
        packet_copy(m, dev).wait_send()
        for j in range(3):
            weight_copy(m, j, dev).wait_send()
    for copy in own:
        copy.wait()


def front(tokens, cotangent, ids, gates, wq, wk, wv, packet):
    seqs, rows, width = tokens.shape
    ep = lax.axis_size("ep")
    cols = wq.shape[1] // ep
    top = ids.shape[1]
    if ep != 8 or lax.axis_size("rep") != 4:
        full = lax.all_gather(tokens, "ep", axis=1, tiled=True)
        weights = [lax.all_to_all(w, "ep", split_axis=1, concat_axis=0, tiled=True) for w in (wq, wk, wv)]
        routes = jnp.concatenate([ids.astype(BF16), gates], axis=1).transpose(0, 2, 1)
        routes = jnp.pad(routes, ((0, 0), (0, 0), (0, 128 - 2 * top)))
        packets = lax.all_gather(packet, "ep", axis=0)
        share, heads = width // (128 * ep), HEAD_DIM // ep
        gains = jnp.stack([packets[:, :share].reshape(width), packets[:, share : 2 * share].reshape(width)])
        lens = jnp.pad(packets[:, 2 * share + 2, 0], (0, 128 - ep))
        few = [packets[:, 2 * share + k, :heads].reshape(HEAD_DIM) for k in range(2)] + [lens]
        return (
            full, jnp.stack(weights), jnp.concatenate([cotangent, routes], axis=-1),
            jnp.pad(gains, ((0, 6), (0, 0))), jnp.pad(jnp.stack(few), ((0, 5), (0, 0))),
        )
    dma = pltpu.SemaphoreType.DMA
    return pl.pallas_call(
        front_kernel,
        out_shape=(
            sds((seqs, rows * ep, width), BF16),
            sds((3, wq.shape[0] * ep, cols), BF16),
            sds((seqs, rows, width + 128), BF16),
            sds((8, width), F32),
            sds((8, 128), F32),
        ),
        in_specs=[VM] * 8,
        out_specs=(AN, AN, VM, VM, VM),
        scratch_shapes=[pltpu.VMEM((ep,) + packet.shape, F32)]
        + Gather.scratch(seqs)
        + [dma((7, 3)), dma((7, 3)), dma((7,)), dma((7,))]
        + [dma((7, 4))] * 4
        + [dma((3,))],
        compiler_params=pltpu.CompilerParams(collective_id=1, **COMM),
        name="front",
    )(tokens, cotangent, ids, gates, wq, wk, wv, packet)


def plain_living(small, seqs, rows):
    place = (jnp.arange(rows) + lax.axis_index("ep") * rows).astype(F32)
    return (place[None] < small[2, :seqs, None]).astype(F32)[..., None]


def mix_kernel(part, tok, small, gains, middle, full, own, *scratch):
    at = Place()
    seqs = tok.shape[0]
    reduce = Reduce(at, part, *scratch[: Reduce.sems])
    gather = Gather(at, own, full, *scratch[Reduce.sems :])
    at.greet((at.xn, at.yn, at.sb))
    each(seqs, reduce.start)
    each(seqs, reduce.hop1)
    each(seqs, reduce.hop2)

    def rows(s):
        living = live_rows(small, s, at.me, tok.shape[1])
        mid, mixed = mix_rows(reduce.total(s), tok[s], living, gains[1:2])
        middle[s] = mid
        own[s] = mixed
        gather.start(s)

    each(seqs, rows)
    gather_tail(seqs, gather)
    each(seqs, reduce.finish)


def mix(part, tokens, small, gains):
    seqs, rows, width = tokens.shape
    ep = lax.axis_size("ep")
    if ep != 8:
        total = lax.psum_scatter(part, "ep", scatter_dimension=1, tiled=True).astype(F32)
        middle, mixed = mix_rows(total, tokens, plain_living(small, seqs, rows), gains[1])
        return middle, lax.all_gather(mixed, "ep", axis=1, tiled=True)
    part = part.reshape(seqs, ep, rows, width)
    return pl.pallas_call(
        mix_kernel,
        out_shape=(sds(tokens.shape, F32), sds((seqs, rows * ep, width), BF16)),
        in_specs=[VM] * 4,
        out_specs=(VM, AN),
        scratch_shapes=[pltpu.VMEM(tokens.shape, BF16)] + Reduce.scratch(part) + Gather.scratch(seqs),
        compiler_params=pltpu.CompilerParams(collective_id=2, **COMM),
        name="mix",
    )(part, tokens, small, gains)


def back_kernel(gpart, middle, cot, small, gains, mgrad, ggrad, full, own, *scratch):
    at = Place()
    seqs = cot.shape[0]
    n = Reduce.sems
    rg = Reduce(at, gpart, *scratch[:n])
    gather = Gather(at, own, full, *scratch[n:])
    at.greet((at.xn, at.yn, at.sb))
    each(seqs, rg.start)
    each(seqs, rg.hop1)
    each(seqs, rg.hop2)
    ggrad[...] = jnp.zeros_like(ggrad)

    def rows(s):
        living = live_rows(small, s, at.me, cot.shape[1])
        mg, ag, back = ffn_back_rows(rg.total(s), middle[s], cot[s], living, gains[1:2])
        mgrad[s] = mg
        own[s] = ag
        ggrad[...] += jnp.sum(back, axis=0, keepdims=True)
        gather.start(s)

    each(seqs, rows)
    gather_tail(seqs, gather)
    each(seqs, rg.finish)


def back(gpart, middle, cot, small, gains):
    seqs, rows, width = cot.shape
    ep = lax.axis_size("ep")
    if ep != 8:
        mixed_grad = lax.psum_scatter(gpart, "ep", scatter_dimension=1, tiled=True).astype(F32)
        mg, ag, backs = ffn_back_rows(mixed_grad, middle, cot, plain_living(small, seqs, rows), gains[1])
        full = lax.all_gather(ag, "ep", axis=1, tiled=True)
        return mg, jnp.sum(backs, axis=(0, 1))[None], full
    gpart = gpart.reshape(seqs, ep, rows, width)
    return pl.pallas_call(
        back_kernel,
        out_shape=(
            sds(cot.shape, F32),
            sds((1, width), F32),
            sds((seqs, rows * ep, width), BF16),
        ),
        in_specs=[VM] * 5,
        out_specs=(VM, VM, AN),
        scratch_shapes=[pltpu.VMEM(cot.shape, BF16)] + Reduce.scratch(gpart) + Gather.scratch(seqs),
        compiler_params=pltpu.CompilerParams(collective_id=3, **COMM),
        name="back",
    )(gpart, middle, cot, small, gains)


def final_kernel(part, wgrad, tok, mgrad, gains, others, tgrad, small, wrows, ggrad, parcel, landed, *scratch):
    at = Place()
    seqs = tok.shape[0]
    n = Reduce.sems
    reduce = Reduce(at, part, *scratch[:n])
    wsend, wrecv, local, gsend, grecv = scratch[n:]
    width = wgrad.shape[2]
    block = wrows.shape[1]
    at.greet(at.peers())
    cols = pl.ds(pl.multiple_of(at.me * width, width), width)

    def weight_copy(m, dev):
        rows = pl.ds(pl.multiple_of(dev * block, block), block)
        return at.push(wgrad.at[:, rows], wrows.at[:, :, cols], wsend.at[m], wrecv.at[m], dev)

    mine = pl.ds(pl.multiple_of(at.me * block, block), block)
    own = pltpu.make_async_copy(wgrad.at[:, mine], wrows.at[:, :, cols], local)
    own.start()
    for m, dev in enumerate(at.peers()):
        weight_copy(m, dev).start()
    each(seqs, reduce.start)
    each(seqs, reduce.hop1)
    each(seqs, reduce.hop2)
    ggrad[...] = jnp.zeros_like(ggrad)

    def rows(s):
        tg, back = attn_back_rows(reduce.total(s), tok[s], mgrad[s], gains[0:1])
        tgrad[s] = tg
        ggrad[...] += jnp.sum(back, axis=0, keepdims=True)

    each(seqs, rows)

    parcel[...] = jnp.zeros_like(parcel)
    devices = parcel.shape[0]
    rows_of = ggrad.shape[1] // (128 * devices)
    for dev in range(devices):
        for k in range(rows_of):
            lanes = pl.ds((dev * rows_of + k) * 128, 128)
            parcel[dev, k : k + 1] = ggrad[:, lanes]
            parcel[dev, rows_of + k : rows_of + k + 1] = others[0:1, lanes]
        parcel[dev, 2 * rows_of : 2 * rows_of + 2] = others[1:3, 0:128]

    def parcel_copy(m, dev):
        return at.push(parcel.at[dev], landed.at[m], gsend.at[m], grecv.at[m], dev)

    for m, dev in enumerate(at.peers()):
        parcel_copy(m, dev).start()
    total = parcel[at.me]
    for m, dev in enumerate(at.peers()):
        parcel_copy(m, dev).wait_recv()
        total = total + landed[m]
    small[...] = total
    each(seqs, reduce.finish)
    for m, dev in enumerate(at.peers()):
        weight_copy(m, dev).wait()
        parcel_copy(m, dev).wait_send()
    own.wait()


def final(part, wgrad, tokens, mgrad, gains, ffn_back, qk_back):
    seqs, rows, width = tokens.shape
    ep = lax.axis_size("ep")
    if ep != 8:
        normed_grad = lax.psum_scatter(part, "ep", scatter_dimension=1, tiled=True).astype(F32)
        tg, backs = attn_back_rows(normed_grad, tokens, mgrad, gains[0])
        wrows = lax.all_to_all(wgrad, "ep", split_axis=1, concat_axis=2, tiled=True)
        share = width // ep
        small = jnp.concatenate([jnp.sum(backs, axis=(0, 1)), ffn_back[0], qk_back[0], qk_back[1]])
        small = lax.psum(small, "ep")
        mine = lax.axis_index("ep") * share
        cut = [lax.dynamic_slice_in_dim(small, k * width + mine, share).reshape(-1, 128) for k in range(2)]
        small = jnp.concatenate(cut + [small[2 * width :].reshape(2, HEAD_DIM)], axis=0)
        return tg, jnp.pad(small, ((0, 8 - small.shape[0]), (0, 0))), wrows
    others = jnp.concatenate([ffn_back, jnp.pad(qk_back[:2], ((0, 0), (0, width - HEAD_DIM)))], axis=0)
    part = part.reshape(seqs, ep, rows, width)
    dma = pltpu.SemaphoreType.DMA
    return pl.pallas_call(
        final_kernel,
        out_shape=(
            sds(tokens.shape, BF16),
            sds((8, 128), F32),
            sds((3, wgrad.shape[1] // ep, wgrad.shape[2] * ep), BF16),
        ),
        in_specs=[VM] * 6,
        out_specs=(VM, VM, AN),
        scratch_shapes=[pltpu.VMEM((1, width), F32), pltpu.VMEM((ep, 8, 128), F32), pltpu.VMEM((7, 8, 128), F32)]
        + Reduce.scratch(part)
        + [dma((7,)), dma((7,)), dma, dma((7,)), dma((7,))],
        compiler_params=pltpu.CompilerParams(collective_id=4, **COMM),
        name="final",
    )(part, wgrad, tokens, mgrad, gains, others)


def line_kernel(
    own, small, opart, mid_rows, out, small_out, result, held, met, landed, os, or_, ps, pr, qs, qr, fs, fr, ss, sr, *scratch
):
    at = Place()
    reduce = Reduce(at, opart, *scratch)
    seqs = opart.shape[0]
    z = lax.axis_index("rep")
    ep = lax.axis_index("ep")
    chunks = own.shape[0]

    def push(src, dst, send, recv, dev):
        return pltpu.make_async_remote_copy(
            src_ref=src, dst_ref=dst, send_sem=send, recv_sem=recv, device_id=(dev, ep), device_id_type=MESH
        )

    barrier = pltpu.get_barrier_semaphore()
    others = [lax.rem(z + k, 4) for k in range(1, 4)]
    for dev in others:
        pl.semaphore_signal(barrier, inc=1, device_id=(dev, ep), device_id_type=MESH)
    for dev in (at.xn, at.yn, at.sb):
        pl.semaphore_signal(barrier, inc=1, device_id=(z, dev), device_id_type=MESH)
    pl.semaphore_wait(barrier, 6)
    inner = jnp.logical_and(z > 0, z < 3)
    middle, partner, outer = 1 + z // 3, 3 - z, 3 * (z - 1)

    def inward(c):
        return push(own.at[c], held.at[c], os.at[c], or_.at[c], middle)

    def across(c):
        return push(held.at[c], met.at[c], ps.at[c], pr.at[c], partner)

    def share(c):
        return push(out.at[c], out.at[c], qs.at[c], qr.at[c], partner)

    def outward(c):
        return push(out.at[c], out.at[c], fs.at[c], fr.at[c], outer)

    def small_copy(k):
        return push(small, landed.at[k], ss.at[k], sr.at[k], others[k])

    def out_rows(s):
        result[s] = (mid_rows[s] + reduce.total(s)).astype(BF16)

    for k in range(3):
        small_copy(k).start()

    @pl.when(jnp.logical_not(inner))
    def _():
        each(chunks, lambda c: inward(c).start())
        each(seqs, reduce.start)
        each(seqs, reduce.hop1)
        each(seqs, reduce.hop2)
        each(seqs, out_rows)
        each(chunks, lambda c: outward(c).wait_recv())
        each(chunks, lambda c: inward(c).wait_send())

    def mine(c):
        return 1 + lax.rem(c, 2) == z

    @pl.when(inner)
    def _():
        each(seqs, reduce.start)
        half = seqs // 2

        def run(c, _):
            for step, lag in ((reduce.hop1, 0), (reduce.hop2, half), (out_rows, 2 * half)):

                @pl.when(jnp.logical_and(c >= lag, c < seqs + lag))
                def _():
                    step(c - lag)

            @pl.when(c < chunks)
            def _():
                inward(c).wait_recv()
                held[c] = (held[c].astype(F32) + own[c].astype(F32)).astype(BF16)

                @pl.when(jnp.logical_not(mine(c)))
                def _():
                    across(c).start()

            b = c - 1

            @pl.when(jnp.logical_and(jnp.logical_and(c >= 1, c < chunks + 1), mine(c + 1)))
            def _():
                across(b).wait_recv()
                out[b] = (held[b].astype(F32) + met[b].astype(F32)).astype(BF16)
                share(b).start()
                outward(b).start()

            a = c - 2

            @pl.when(jnp.logical_and(c >= 2, jnp.logical_not(mine(c))))
            def _():
                share(a).wait_recv()
                outward(a).start()

            return 0

        lax.fori_loop(0, chunks + 2, run, 0)

        def finish(c):
            outward(c).wait_send()

            @pl.when(mine(c))
            def _():
                share(c).wait_send()

            @pl.when(jnp.logical_not(mine(c)))
            def _():
                across(c).wait_send()

        each(chunks, finish)

    each(seqs, reduce.finish)
    total = small[...]
    for k in range(3):
        small_copy(k).wait()
        total = total + landed[k]
    small_out[...] = total


def line_sum(big, small, opart, middle):
    if lax.axis_size("rep") != 4 or lax.axis_size("ep") != 8:
        moe = lax.psum_scatter(opart, "ep", scatter_dimension=1, tiled=True).astype(F32)
        return lax.psum(big, "rep"), lax.psum(small, "rep"), (middle + moe).astype(BF16)
    seqs, tokens, width = middle.shape
    opart = opart.reshape(seqs, 8, tokens, width)
    assert 2 * seqs <= 18
    count, rows, cols = big.shape
    chunks = 16
    own = big.reshape(chunks, count * rows // chunks, cols)
    dma = pltpu.SemaphoreType.DMA
    out, small, result = pl.pallas_call(
        line_kernel,
        out_shape=(sds(own.shape, BF16), sds(small.shape, F32), sds(middle.shape, BF16)),
        in_specs=[VM] * 4,
        out_specs=(VM, VM, VM),
        scratch_shapes=[
            pltpu.VMEM(own.shape, BF16),
            pltpu.VMEM(own.shape, BF16),
            pltpu.VMEM((3,) + small.shape, F32),
        ]
        + [dma((chunks,))] * 8
        + [dma((3,))] * 2
        + Reduce.scratch(opart),
        compiler_params=pltpu.CompilerParams(collective_id=5, **COMM),
        name="line_sum",
    )(own, small, opart, middle)
    return out.reshape(big.shape), small, result


def dot(a, b, ca, cb):
    return lax.dot_general(a, b, (((ca,), (cb,)), ((), ())), preferred_element_type=F32)


def rope(v, cos, sin_turn):
    return v * cos + pltpu.roll(v, HEAD_DIM // 2, 1) * sin_turn


def probabilities(q, k, length):
    scores = dot(q, k, 1, 1) * HEAD_DIM**-0.5
    column = lax.broadcasted_iota(jnp.int32, (1, scores.shape[1]), 1).astype(F32)
    scores = jnp.where(column < length, scores, -1e9)
    p = jnp.exp(scores - jnp.max(scores, axis=-1, keepdims=True))
    return p * (1.0 / jnp.sum(p, axis=-1, keepdims=True))


def attend_kernel(tok, w, wo, gains, small, cos, sin, normed, pre, low, ctx, part):
    length = seq_len(small, pl.program_id(0))
    v = tok[0].astype(F32)
    x = (v * inverse_rms(v) * gains[0:1]).astype(BF16)
    normed[0] = x
    q_pre, k_pre = dot(x, w[0], 1, 0), dot(x, w[1], 1, 0)
    value = dot(x, w[2], 1, 0).astype(BF16)
    pre[0, 0], pre[1, 0] = q_pre, k_pre
    low[2, 0] = value
    for h in range(q_pre.shape[1] // HEAD_DIM):
        cols = slice(h * HEAD_DIM, (h + 1) * HEAD_DIM)
        rot = []
        for i, (u, g) in enumerate(((q_pre[:, cols], small[0:1]), (k_pre[:, cols], small[1:2]))):
            rot.append(rope(u * inverse_rms(u) * g, cos[...], sin[...]).astype(BF16))
            low[i, 0, :, cols] = rot[i]
        attention = probabilities(rot[0], rot[1], length).astype(BF16)
        ctx[0, :, cols] = dot(attention, value[:, cols], 1, 0).astype(BF16)
    part[0] = dot(ctx[0], wo[...], 1, 0).astype(BF16)


def attend(full, weights, wo, gains, small, cos, sin):
    seqs, length, width = full.shape
    cols = weights.shape[2]
    row = lambda i, *_: (i, 0, 0)
    row2 = lambda i, *_: (0, i, 0, 0)
    two = lambda i, *_: (0, 0)
    return pl.pallas_call(
        attend_kernel,
        out_shape=(
            sds(full.shape, BF16),
            sds((2, seqs, length, cols), F32),
            sds((3, seqs, length, cols), BF16),
            sds((seqs, length, cols), BF16),
            sds(full.shape, BF16),
        ),
        grid_spec=pltpu.PrefetchScalarGridSpec(
            num_scalar_prefetch=0,
            grid=(seqs,),
            in_specs=[
                pl.BlockSpec((1, length, width), row),
                pl.BlockSpec(weights.shape, lambda i, *_: (0, 0, 0)),
                pl.BlockSpec(wo.shape, two),
                pl.BlockSpec((8, width), two),
                pl.BlockSpec((8, 128), two),
                pl.BlockSpec((length, HEAD_DIM), two),
                pl.BlockSpec((length, HEAD_DIM), two),
            ],
            out_specs=(
                pl.BlockSpec((1, length, width), row),
                pl.BlockSpec((2, 1, length, cols), row2),
                pl.BlockSpec((3, 1, length, cols), row2),
                pl.BlockSpec((1, length, cols), row),
                pl.BlockSpec((1, length, width), row),
            ),
        ),
        compiler_params=pltpu.CompilerParams(dimension_semantics=("arbitrary",), vmem_limit_bytes=60 << 20),
        cost_estimate=pl.CostEstimate(flops=10**10, bytes_accessed=4 * 10**7, transcendentals=10**6),
        name="attend",
    )(full, weights, wo, gains, small, cos, sin)


def attend_back_kernel(
    agrad, normed, pre, low, ctx, w, wo, small, cos, sin, part, wgrad, wograd, gains, wacc, woacc
):
    s = pl.program_id(0)
    length = seq_len(small, s)

    @pl.when(s == 0)
    def _():
        wacc[...] = jnp.zeros_like(wacc)
        woacc[...] = jnp.zeros_like(woacc)
        gains[...] = jnp.zeros_like(gains)

    ag = agrad[0]
    woacc[...] += dot(ctx[0], ag, 0, 0)
    cg_all = dot(ag, wo[...], 1, 1).astype(BF16)
    scale = HEAD_DIM**-0.5
    half = HEAD_DIM // 2
    grads = ([], [], [])
    for h in range(cg_all.shape[1] // HEAD_DIM):
        cols = slice(h * HEAD_DIM, (h + 1) * HEAD_DIM)
        q, k, value, cg = low[0, 0, :, cols], low[1, 0, :, cols], low[2, 0, :, cols], cg_all[:, cols]
        attention = probabilities(q, k, length)
        grads[2].append(dot(attention.astype(BF16), cg, 0, 0).astype(BF16))
        pg = dot(cg, value, 1, 1)
        sg = (attention * (pg - jnp.sum(attention * pg, axis=-1, keepdims=True))).astype(BF16)
        for i, (rot_grad, g) in enumerate(((dot(sg, k, 1, 0), small[0:1]), (dot(sg, q, 0, 0), small[1:2]))):
            wgt = rot_grad * scale
            u = wgt * cos[...] + pltpu.roll(wgt * sin[...], half, 1)
            v = pre[i, 0, :, cols]
            r = inverse_rms(v)
            grads[i].append(rms_back(v, r, u * g).astype(BF16))
            gains[i : i + 1] += jnp.sum(u * v * r, axis=0, keepdims=True)
    total = None
    for i in range(3):
        g = grads[i][0] if len(grads[i]) == 1 else jnp.concatenate(grads[i], axis=1)
        wacc[i] += dot(normed[0], g, 0, 0)
        piece = dot(g, w[i], 1, 1)
        total = piece if total is None else total + piece
    part[0] = total.astype(BF16)

    @pl.when(s == pl.num_programs(0) - 1)
    def _():
        wgrad[...] = wacc[...].astype(BF16)
        wograd[...] = woacc[...].astype(BF16)


def attend_back(agrad, normed, pre, low, ctx, weights, wo, small, cos, sin):
    seqs, length, width = agrad.shape
    cols = weights.shape[2]
    row = lambda i, *_: (i, 0, 0)
    row2 = lambda i, *_: (0, i, 0, 0)
    two = lambda i, *_: (0, 0)
    three = lambda i, *_: (0, 0, 0)
    return pl.pallas_call(
        attend_back_kernel,
        out_shape=(
            sds(agrad.shape, BF16),
            sds(weights.shape, BF16),
            sds(wo.shape, BF16),
            sds((8, HEAD_DIM), F32),
        ),
        grid_spec=pltpu.PrefetchScalarGridSpec(
            num_scalar_prefetch=0,
            grid=(seqs,),
            in_specs=[
                pl.BlockSpec((1, length, width), row),
                pl.BlockSpec((1, length, width), row),
                pl.BlockSpec((2, 1, length, cols), row2),
                pl.BlockSpec((3, 1, length, cols), row2),
                pl.BlockSpec((1, length, cols), row),
                pl.BlockSpec(weights.shape, three),
                pl.BlockSpec(wo.shape, two),
                pl.BlockSpec((8, 128), two),
                pl.BlockSpec((length, HEAD_DIM), two),
                pl.BlockSpec((length, HEAD_DIM), two),
            ],
            out_specs=(
                pl.BlockSpec((1, length, width), row),
                pl.BlockSpec(weights.shape, three),
                pl.BlockSpec(wo.shape, two),
                pl.BlockSpec((8, HEAD_DIM), two),
            ),
            scratch_shapes=[pltpu.VMEM(weights.shape, F32), pltpu.VMEM(wo.shape, F32)],
        ),
        compiler_params=pltpu.CompilerParams(dimension_semantics=("arbitrary",), vmem_limit_bytes=60 << 20),
        cost_estimate=pl.CostEstimate(flops=2 * 10**10, bytes_accessed=4 * 10**7, transcendentals=10**6),
        name="attend_back",
    )(agrad, normed, pre, low, ctx, weights, wo, small, cos, sin)


BLOCK = 256


def pack_rows(seqs, capacity):
    return -(-seqs * capacity // BLOCK) * BLOCK


def packed_slots(number, table, length_live, top):
    tab = table.astype(F32)
    length = tab.shape[0]
    lane = lax.broadcasted_iota(jnp.int32, tab.shape, 1)
    row = lax.broadcasted_iota(jnp.int32, (length, 1), 0).astype(F32)
    chosen = jnp.logical_and(jnp.logical_and(tab == number, lane < top), row < length_live)
    gates = jnp.where(chosen, pltpu.roll(tab, 128 - top, 1), 0.0).astype(BF16)
    chosen = jnp.where(chosen, 1.0, 0.0).astype(BF16)
    ones = jnp.ones((8, 128), BF16)
    hit = dot(ones, chosen, 1, 1)
    weight = dot(ones, gates, 1, 1)
    earlier = lax.broadcasted_iota(jnp.int32, (length, length), 0)
    later = lax.broadcasted_iota(jnp.int32, (length, length), 1)
    rank = dot(hit.astype(BF16), jnp.where(earlier < later, 1.0, 0.0).astype(BF16), 1, 0)
    return jnp.where(hit > 0.5, rank, -1.0), weight, jnp.sum(hit[0:1]).astype(jnp.int32)


def forward_blocks(blocks, x, dy, wi, wo, acts, dgus):
    hidden = wo.shape[0]
    part = min(hidden, 512)

    def forward(b, _):
        rows = pl.ds(pl.multiple_of(b * BLOCK, BLOCK), BLOCK)
        for h in range(hidden // part):
            gcols, ucols = pl.ds(h * part, part), pl.ds(hidden + h * part, part)
            gate = dot(x[rows], wi[:, gcols], 1, 0)
            up = dot(x[rows], wi[:, ucols], 1, 0)
            dact = dot(dy[rows], wo[gcols], 1, 1)
            sig = 1.0 / (1.0 + jnp.exp(-gate))
            silu = gate * sig
            acts[rows, gcols] = (silu * up).astype(BF16)
            dgus[rows, gcols] = (dact * up * sig * (1.0 + gate * (1.0 - sig))).astype(BF16)
            dgus[rows, ucols] = (dact * silu).astype(BF16)
        return 0

    lax.fori_loop(0, blocks, forward, 0)


def gradient_tiles(blocks, left, right, result, acc, stage, ssem, busy):
    tr, tc = acc.shape
    down, across = result.shape[0] // tr, result.shape[1] // tc

    def tile(t, _):
        rt, ct = t // across, lax.rem(t, across)
        left_cols = pl.ds(pl.multiple_of(rt * tr, tr), tr)
        right_cols = pl.ds(pl.multiple_of(ct * tc, tc), tc)

        def step(b, _):
            rows = pl.ds(pl.multiple_of(b * BLOCK, BLOCK), BLOCK)
            piece = dot(left[rows, left_cols], right[rows, right_cols], 0, 0)

            @pl.when(b == 0)
            def _():
                acc[...] = piece

            @pl.when(b > 0)
            def _():
                acc[...] += piece

            return 0

        @pl.when(blocks == 0)
        def _():
            acc[...] = jnp.zeros_like(acc)

        lax.fori_loop(0, blocks, step, 0)
        k = lax.rem(t, 2)
        out = pltpu.make_async_copy(stage.at[k], result.at[left_cols, right_cols], ssem.at[k])

        @pl.when(jnp.logical_or(t >= 2, busy))
        def _():
            out.wait()

        stage[k] = acc[...].astype(BF16)
        out.start()
        return 0

    lax.fori_loop(0, down * across, tile, 0)


def drain_tiles(result, acc, stage, ssem):
    tr, tc = acc.shape
    for k in range(2):
        pltpu.make_async_copy(stage.at[k], result.at[pl.ds(0, tr), pl.ds(0, tc)], ssem.at[k]).wait()


def first_kernel(
    capacity, top, number, mixed, cot, table, small, w_in, w_out,
    slots0, slots1, starts, act, dgu, x_all, dy_all, out_grad,
    x, dy, wi, wo, acts, dgus, acc, stage, wsem, ssem, rsem,
):
    step = pl.program_id(0)
    steps = pl.num_programs(0)
    together = mixed.shape[0]
    seqs = steps * together
    width = mixed.shape[2]
    loads = [pltpu.make_async_copy(w_in.at[0], wi, wsem.at[0]), pltpu.make_async_copy(w_out.at[0], wo, wsem.at[1])]

    @pl.when(step == 0)
    def _():
        for copy in loads:
            copy.start()
        starts[0, 0] = 0
        starts[1, 0] = 0

    packed = []
    for k in range(together):
        spread, gate_spread, counts = [], [], []
        for j, slots in enumerate((slots0, slots1)):
            slot, weight, count = packed_slots(
                (number[0] + j).astype(F32), table[k], seq_len(small, step * together + k), top
            )
            slots[k, 0:8] = slot
            slots[k, 8:16] = weight
            place = lax.broadcasted_iota(jnp.int32, (capacity, slot.shape[1]), 0).astype(F32) == slot[0:1]
            spread.append(jnp.where(place, 1.0, 0.0).astype(BF16))
            gate_spread.append(jnp.where(place, weight[0:1], 0.0).astype(BF16))
            counts.append(count)
        packed.append(
            (
                counts,
                dot(jnp.concatenate(spread, axis=0), mixed[k], 1, 0).astype(BF16),
                dot(jnp.concatenate(gate_spread, axis=0), cot[k], 1, 0).astype(BF16),
            )
        )
    for k, (counts, x_rows, dy_rows) in enumerate(packed):
        s = step * together + k
        for j in range(2):
            start = pl.multiple_of(starts[j, s], 16)
            x[j, pl.ds(start, capacity)] = x_rows[j * capacity : (j + 1) * capacity]
            dy[j, pl.ds(start, capacity)] = dy_rows[j * capacity : (j + 1) * capacity]
            starts[j, s + 1] = start + (counts[j] + 15) // 16 * 16

    @pl.when(step == steps - 1)
    def _():
        for j in range(2):
            past = (starts[j, seqs - 1] + capacity) // 16
            end = (starts[j, seqs] + BLOCK - 1) // BLOCK * (BLOCK // 16)

            def clear(i, _):
                rows = pl.ds(pl.multiple_of(i * 16, 16), 16)
                x[j, rows] = jnp.zeros((16, width), BF16)
                dy[j, rows] = jnp.zeros((16, width), BF16)
                return 0

            lax.fori_loop(past, end, clear, 0)
        saves = [pltpu.make_async_copy(x, x_all, rsem.at[0]), pltpu.make_async_copy(dy.at[1], dy_all, rsem.at[1])]
        for copy in saves:
            copy.start()
        blocks = (starts[0, seqs] + BLOCK - 1) // BLOCK
        for copy in loads:
            copy.wait()
        forward_blocks(blocks, x.at[0], dy.at[0], wi, wo, acts, dgus)
        saves += [pltpu.make_async_copy(acts, act, rsem.at[2]), pltpu.make_async_copy(dgus, dgu, rsem.at[3])]
        for copy in saves[2:]:
            copy.start()
        gradient_tiles(blocks, acts, dy.at[0], out_grad, acc, stage, ssem, False)
        drain_tiles(out_grad, acc, stage, ssem)
        for copy in saves:
            copy.wait()


def expert_first(number, mixed, cot, small, w_in, w_out, capacity, top):
    seqs, length, width = mixed.shape
    hidden = w_out.shape[1]
    rows = pack_rows(seqs, capacity)
    dma = pltpu.SemaphoreType.DMA
    seq = lambda i, *_: (i, 0, 0)
    together = 2
    slot_spec = pl.BlockSpec((together, 16, length), seq)
    return pl.pallas_call(
        functools.partial(first_kernel, capacity, top),
        out_shape=(
            sds((seqs, 16, length), F32),
            sds((seqs, 16, length), F32),
            sds((2, seqs + 1), jnp.int32),
            sds((rows, hidden), BF16),
            sds((rows, 2 * hidden), BF16),
            sds((2, rows, width), BF16),
            sds((rows, width), BF16),
            sds((hidden, width), BF16),
        ),
        grid_spec=pltpu.PrefetchScalarGridSpec(
            num_scalar_prefetch=1,
            grid=(seqs // together,),
            in_specs=[
                pl.BlockSpec((together, length, width), seq),
                pl.BlockSpec((together, length, width), seq),
                pl.BlockSpec((together, length, 128), lambda i, *_: (i, 0, width // 128)),
                pl.BlockSpec((8, 128), lambda i, *_: (0, 0)),
                AN,
                AN,
            ],
            out_specs=(slot_spec, slot_spec, pl.BlockSpec(memory_space=pltpu.SMEM), AN, AN, AN, AN, AN),
            scratch_shapes=[
                pltpu.VMEM((2, rows, width), BF16),
                pltpu.VMEM((2, rows, width), BF16),
                pltpu.VMEM(w_in.shape[1:], BF16),
                pltpu.VMEM(w_out.shape[1:], BF16),
                pltpu.VMEM((rows, hidden), BF16),
                pltpu.VMEM((rows, 2 * hidden), BF16),
                pltpu.VMEM((256, 1024), F32),
                pltpu.VMEM((2, 256, 1024), BF16),
                dma((2,)),
                dma((2,)),
                dma((4,)),
            ],
        ),
        compiler_params=pltpu.CompilerParams(dimension_semantics=("arbitrary",), vmem_limit_bytes=63 << 20),
        cost_estimate=pl.CostEstimate(flops=2 * 10**10, bytes_accessed=6 * 10**7, transcendentals=10**6),
        name="expert_first",
    )(number, mixed, cot, cot, small, w_in, w_out)


def in_grad_kernel(starts, x_all, dgu, in_grad, x, dgus, acc, stage, lsem, ssem):
    blocks = (starts[0, starts.shape[1] - 1] + BLOCK - 1) // BLOCK

    def load(b):
        rows = pl.ds(pl.multiple_of(b * BLOCK, BLOCK), BLOCK)
        return (
            pltpu.make_async_copy(x_all.at[0, rows], x.at[rows], lsem.at[0, b]),
            pltpu.make_async_copy(dgu.at[rows], dgus.at[rows], lsem.at[1, b]),
        )

    def run(b, action):
        for copy in load(b):
            getattr(copy, action)()
        return 0

    lax.fori_loop(0, blocks, lambda b, _: run(b, "start"), 0)
    lax.fori_loop(0, blocks, lambda b, _: run(b, "wait"), 0)
    gradient_tiles(blocks, x, dgus, in_grad, acc, stage, ssem, False)
    drain_tiles(in_grad, acc, stage, ssem)


def first_in_grad(starts, x_all, dgu):
    rows, width = x_all.shape[1:]
    dma = pltpu.SemaphoreType.DMA
    return pl.pallas_call(
        in_grad_kernel,
        out_shape=sds((width, dgu.shape[1]), BF16),
        grid_spec=pltpu.PrefetchScalarGridSpec(
            num_scalar_prefetch=1,
            grid=(1,),
            in_specs=[AN, AN],
            out_specs=AN,
            scratch_shapes=[
                pltpu.VMEM((rows, width), BF16),
                pltpu.VMEM(dgu.shape, BF16),
                pltpu.VMEM((512, 2048), F32),
                pltpu.VMEM((2, 512, 2048), BF16),
                dma((2, rows // BLOCK)),
                dma((2,)),
            ],
        ),
        compiler_params=pltpu.CompilerParams(dimension_semantics=("arbitrary",), vmem_limit_bytes=60 << 20),
        cost_estimate=pl.CostEstimate(flops=10**10, bytes_accessed=2 * 10**7, transcendentals=0),
        name="first_in_grad",
    )(starts, x_all, dgu)


def second_kernel(
    starts, x_all, dy_all, w_in, w_out, act, dgu, out_grad, in_grad,
    x, dy, wi, wo, acts, dgus, acc, stage, wsem, lsem, ssem, rsem,
):
    blocks = (starts[1, starts.shape[1] - 1] + BLOCK - 1) // BLOCK
    loads = [pltpu.make_async_copy(w_in.at[1], wi, wsem.at[0]), pltpu.make_async_copy(w_out.at[1], wo, wsem.at[1])]

    def load(b, action):
        rows = pl.ds(pl.multiple_of(b * BLOCK, BLOCK), BLOCK)
        for copy in (
            pltpu.make_async_copy(x_all.at[1, rows], x.at[rows], lsem.at[0, b]),
            pltpu.make_async_copy(dy_all.at[rows], dy.at[rows], lsem.at[1, b]),
        ):
            getattr(copy, action)()
        return 0

    for copy in loads:
        copy.start()
    lax.fori_loop(0, blocks, lambda b, _: load(b, "start"), 0)
    for copy in loads:
        copy.wait()
    lax.fori_loop(0, blocks, lambda b, _: load(b, "wait"), 0)
    forward_blocks(blocks, x, dy, wi, wo, acts, dgus)
    saves = [pltpu.make_async_copy(acts, act, rsem.at[0]), pltpu.make_async_copy(dgus, dgu, rsem.at[1])]
    for copy in saves:
        copy.start()
    gradient_tiles(blocks, x, dgus, in_grad, acc, stage, ssem, False)
    gradient_tiles(blocks, acts, dy, out_grad, acc, stage, ssem, True)
    drain_tiles(out_grad, acc, stage, ssem)
    for copy in saves:
        copy.wait()


def expert_second(starts, x_all, dy_all, w_in, w_out):
    rows, width = dy_all.shape
    hidden = w_out.shape[1]
    dma = pltpu.SemaphoreType.DMA
    return pl.pallas_call(
        second_kernel,
        out_shape=(
            sds((rows, hidden), BF16),
            sds((rows, 2 * hidden), BF16),
            sds((hidden, width), BF16),
            sds((width, 2 * hidden), BF16),
        ),
        grid_spec=pltpu.PrefetchScalarGridSpec(
            num_scalar_prefetch=1,
            grid=(1,),
            in_specs=[AN] * 4,
            out_specs=(AN, AN, AN, AN),
            scratch_shapes=[
                pltpu.VMEM((rows, width), BF16),
                pltpu.VMEM((rows, width), BF16),
                pltpu.VMEM(w_in.shape[1:], BF16),
                pltpu.VMEM(w_out.shape[1:], BF16),
                pltpu.VMEM((rows, hidden), BF16),
                pltpu.VMEM((rows, 2 * hidden), BF16),
                pltpu.VMEM((512, 2048), F32),
                pltpu.VMEM((2, 512, 2048), BF16),
                dma((2,)),
                dma((2, rows // BLOCK)),
                dma((2,)),
                dma((2,)),
            ],
        ),
        compiler_params=pltpu.CompilerParams(dimension_semantics=("arbitrary",), vmem_limit_bytes=60 << 20),
        cost_estimate=pl.CostEstimate(flops=25 * 10**9, bytes_accessed=6 * 10**7, transcendentals=10**6),
        name="expert_second",
    )(starts, x_all, dy_all, w_in, w_out)


def tail_kernel(j, starts, act, dgu, w_in, w_out, produced, dx):
    @pl.when(pl.program_id(0) * BLOCK < starts[j, starts.shape[1] - 1])
    def _():
        produced[...] = dot(act[...], w_out[...], 1, 0).astype(BF16)
        dx[...] = dot(dgu[...], w_in[...], 1, 1).astype(BF16)


def expert_tail(j, starts, act, dgu, w_in, w_out):
    rows, hidden = act.shape
    width = w_in.shape[1]
    last = starts.shape[1] - 1
    block = lambda i, st: (jnp.maximum(jnp.minimum(i, (st[j, last] + BLOCK - 1) // BLOCK - 1), 0), 0)
    return pl.pallas_call(
        functools.partial(tail_kernel, j),
        out_shape=(sds((rows, width), BF16), sds((rows, width), BF16)),
        grid_spec=pltpu.PrefetchScalarGridSpec(
            num_scalar_prefetch=1,
            grid=(rows // BLOCK,),
            in_specs=[
                pl.BlockSpec((BLOCK, hidden), block),
                pl.BlockSpec((BLOCK, 2 * hidden), block),
                pl.BlockSpec((None,) + w_in.shape[1:], lambda i, *_: (j, 0, 0)),
                pl.BlockSpec((None,) + w_out.shape[1:], lambda i, *_: (j, 0, 0)),
            ],
            out_specs=(pl.BlockSpec((BLOCK, width), block), pl.BlockSpec((BLOCK, width), block)),
        ),
        compiler_params=pltpu.CompilerParams(dimension_semantics=("arbitrary",), vmem_limit_bytes=60 << 20),
        cost_estimate=pl.CostEstimate(flops=12 * 10**9, bytes_accessed=3 * 10**7, transcendentals=0),
        name="expert_tail",
    )(starts, act, dgu, w_in, w_out)


def combine_kernel(capacity, local, *refs):
    s = pl.program_id(0)
    starts = refs[0]
    slots = refs[1 : 1 + local]
    produced = refs[1 + local : 1 + 2 * local]
    dx = refs[1 + 2 * local : 1 + 3 * local]
    out_part, grad_part = refs[1 + 3 * local :]
    out_sum, grad_sum = None, None
    for j in range(local):
        length = slots[j].shape[2]
        column = lax.broadcasted_iota(jnp.int32, (capacity, length), 0).astype(F32)
        place = column == slots[j][0, 0:1]
        span = pl.ds(pl.multiple_of(starts[j, s], 16), capacity)
        held = lax.broadcasted_iota(jnp.int32, (capacity, 1), 0) < starts[j, s + 1] - starts[j, s]
        rows = jnp.where(held, produced[j][span], 0.0).astype(BF16)
        grads = jnp.where(held, dx[j][span], 0.0).astype(BF16)
        out = dot(jnp.where(place, slots[j][0, 8:9], 0.0).astype(BF16), rows, 0, 0)
        grad = dot(jnp.where(place, 1.0, 0.0).astype(BF16), grads, 0, 0)
        out_sum = out if out_sum is None else out_sum + out
        grad_sum = grad if grad_sum is None else grad_sum + grad
    out_part[0] = out_sum.astype(BF16)
    grad_part[0] = grad_sum.astype(BF16)


def combine(starts, slots, produced, dx, capacity):
    local = len(slots)
    seqs, _, length = slots[0].shape
    width = produced[0].shape[1]
    seq = lambda i, *_: (i, 0, 0)
    two = lambda i, *_: (0, 0)
    rows = pl.BlockSpec(produced[0].shape, two)
    return pl.pallas_call(
        functools.partial(combine_kernel, capacity, local),
        out_shape=(sds((seqs, length, width), BF16), sds((seqs, length, width), BF16)),
        grid_spec=pltpu.PrefetchScalarGridSpec(
            num_scalar_prefetch=1,
            grid=(seqs,),
            in_specs=[pl.BlockSpec((1, 16, length), seq)] * local + [rows] * (2 * local),
            out_specs=(pl.BlockSpec((1, length, width), seq), pl.BlockSpec((1, length, width), seq)),
        ),
        compiler_params=pltpu.CompilerParams(dimension_semantics=("arbitrary",), vmem_limit_bytes=60 << 20),
        cost_estimate=pl.CostEstimate(flops=3 * 10**9, bytes_accessed=4 * 10**7, transcendentals=0),
        name="combine",
    )(starts, *slots, *produced, *dx)


def shards(
    tokens, cotangent, gate_weights, expert_ids, seq_lengths, query_weight, key_weight, value_weight,
    output_weight, attn_gain, ffn_gain, query_gain, key_gain, expert_in, expert_out,
):
    ep = lax.axis_size("ep")
    me = lax.axis_index("ep")
    _, rows, _ = tokens.shape
    length = rows * ep
    top = gate_weights.shape[2]
    local = expert_in.shape[0]
    experts = local * ep
    capacity = -(-(length * top * 9 // (8 * experts)) // 16) * 16

    gains = jnp.concatenate([attn_gain, ffn_gain]).astype(F32).reshape(-1, 128)
    few = [query_gain.astype(F32), key_gain.astype(F32), seq_lengths.astype(F32)]
    few = jnp.stack([jnp.pad(v, (0, 128 - v.shape[0])) for v in few])
    packet = jnp.concatenate([gains, few], axis=0)
    packet = jnp.pad(packet, ((0, -packet.shape[0] % 8), (0, 0)))
    share = gains.shape[0] // 2

    full, weights, routed, gains, small_in = front(
        tokens, cotangent, expert_ids.transpose(0, 2, 1), gate_weights.transpose(0, 2, 1),
        query_weight, key_weight, value_weight, packet,
    )
    cot_full = lax.all_gather(routed, "ep", axis=1, tiled=True)

    half = HEAD_DIM // 2
    frequency = ROPE_BASE ** (-(np.arange(half, dtype=np.float32) * np.float32(2.0 / HEAD_DIM)))
    angles = np.arange(length, dtype=np.float32)[:, None] * frequency.astype(np.float32)[None, :]
    cos = jnp.asarray(np.concatenate([np.cos(angles)] * 2, axis=-1), F32)
    sin = jnp.asarray(np.concatenate([-np.sin(angles), np.sin(angles)], axis=-1), F32)

    normed, pre, low, ctx, part = attend(full, weights, output_weight, gains, small_in, cos, sin)
    middle, mixed = mix(part, tokens, small_in, gains)

    number = (me * local).astype(jnp.int32)[None]
    slots0, slots1, starts, act0, dgu0, x_all, dy_all, out_grad0 = expert_first(
        number, mixed, cot_full, small_in, expert_in, expert_out, capacity, top
    )

    def over_rep(value):
        return lax.psum_scatter(value, "rep", scatter_dimension=0, tiled=True)

    out0 = over_rep(out_grad0)
    in_grad0 = first_in_grad(starts, x_all, dgu0)
    in0 = over_rep(in_grad0)
    x_all, _ = lax.optimization_barrier((x_all, in_grad0))
    act1, dgu1, out_grad1, in_grad1 = expert_second(starts, x_all, dy_all, expert_in, expert_out)
    in1 = over_rep(in_grad1)
    out1 = over_rep(out_grad1)
    produced0, dx0 = expert_tail(0, starts, act0, dgu0, expert_in, expert_out)
    produced1, dx1 = expert_tail(1, starts, act1, dgu1, expert_in, expert_out)
    out_part, grad_part = combine(starts, (slots0, slots1), (produced0, produced1), (dx0, dx1), capacity)

    mgrad, ffn_back, agrad = back(grad_part, middle, cotangent, small_in, gains)
    npart, wgrad, wograd, qk_back = attend_back(
        agrad, normed, pre, low, ctx, weights, output_weight, small_in, cos, sin
    )
    token_grad, small, wrows = final(npart, wgrad, tokens, mgrad, gains, ffn_back, qk_back)
    big = jnp.concatenate([wrows, wograd[None]], axis=0)

    def widen(into, value, j):
        return lax.dynamic_update_slice(into, value.astype(F32)[None], (j, 0, 0))

    in_all = widen(jnp.zeros((local,) + in0.shape, F32), in0, 0)
    out_all = widen(jnp.zeros((local,) + out0.shape, F32), out0, 0)
    big, in_all, out_all = lax.optimization_barrier((big, in_all, out_all))
    sums, small, result = line_sum(big, small, out_part, middle)

    def head_share(vector):
        return lax.dynamic_slice_in_dim(vector, me * (HEAD_DIM // ep), HEAD_DIM // ep)

    return (
        result,
        token_grad,
        sums[0].astype(F32),
        sums[1].astype(F32),
        sums[2].astype(F32),
        sums[3].astype(F32),
        small[:share].reshape(-1),
        small[share : 2 * share].reshape(-1),
        head_share(small[2 * share]),
        head_share(small[2 * share + 1]),
        widen(in_all, in1, 1),
        widen(out_all, out1, 1),
    )


def solution(mesh):
    seq = P("rep", "ep", None)
    row, gain, expert = P("ep", None), P("ep"), P("ep", None, None)
    split = P("ep", "rep", None)

    return jax.shard_map(
        shards,
        mesh=mesh,
        in_specs=(seq, seq, seq, seq, P(("rep", "ep")), row, row, row, row, gain, gain, gain, gain, expert, expert),
        out_specs=(seq, seq, row, row, row, row, gain, gain, gain, gain, split, split),
        check_vma=False,
    )
```

```python
import functools

import jax
import jax.numpy as jnp
import numpy as np
from jax import lax
from jax.experimental import pallas as pl
from jax.experimental.pallas import tpu as pltpu
from jax.sharding import PartitionSpec as P

HEAD_DIM = 128
EPS = 1e-06
ROPE_BASE = 50000.0
MESH = pl.DeviceIdType.MESH
F32 = jnp.float32
BF16 = jnp.bfloat16


def sds(shape, dtype):
    return jax.ShapeDtypeStruct(shape, dtype)


VM = pl.BlockSpec(memory_space=pltpu.VMEM)
AN = pl.BlockSpec(memory_space=pl.ANY)


def inverse_rms(v):
    return lax.rsqrt(jnp.mean(v * v, axis=-1, keepdims=True) + EPS)


def rms_back(v, r, ug):
    return r * ug - v * (r * r * r * jnp.mean(ug * v, axis=-1, keepdims=True))


def mix_rows(total, tok, living, gain):
    middle = tok.astype(F32) + living * total
    mixed = middle * inverse_rms(middle) * gain
    return middle, mixed.astype(BF16)


def ffn_back_rows(mixed_grad, middle, cot, living, gain):
    r = inverse_rms(middle)
    middle_grad = cot.astype(F32) + rms_back(middle, r, mixed_grad * gain)
    return middle_grad, (living * middle_grad).astype(BF16), mixed_grad * middle * r


def attn_back_rows(normed_grad, tok, middle_grad, gain):
    v = tok.astype(F32)
    r = inverse_rms(v)
    return (middle_grad + rms_back(v, r, normed_grad * gain)).astype(BF16), normed_grad * v * r


def seq_len(small, s):
    lane = lax.broadcasted_iota(jnp.int32, (1, 128), 1)
    return jnp.sum(jnp.where(lane == s, small[2:3, :], 0.0), axis=1, keepdims=True)


def live_rows(small, s, me, rows):
    place = (lax.broadcasted_iota(jnp.int32, (rows, 1), 0) + me * rows).astype(F32)
    return jnp.where(place < seq_len(small, s), 1.0, 0.0)


class Place:
    def __init__(self):
        me = lax.axis_index("ep")
        core, x, y = lax.rem(me, 2), lax.rem(me // 2, 2), me // 4
        self.rep = lax.axis_index("rep")
        self.me = me
        self.sb = me + 1 - 2 * core
        self.dx = 2 - 4 * x
        self.dy = 4 - 8 * y
        self.xn = me + self.dx
        self.yn = me + self.dy
        self.dg = me + self.dx + self.dy

    def push(self, src, dst, send, recv, dev):
        return pltpu.make_async_remote_copy(
            src_ref=src, dst_ref=dst, send_sem=send, recv_sem=recv, device_id=(self.rep, dev), device_id_type=MESH
        )

    def peers(self):
        sb, dx, dy = self.sb, self.dx, self.dy
        return (self.xn, self.yn, self.dg, sb, sb + dx, sb + dy, sb + dx + dy)

    def greet(self, peers):
        barrier = pltpu.get_barrier_semaphore()
        for peer in peers:
            pl.semaphore_signal(barrier, inc=1, device_id=(self.rep, peer), device_id_type=MESH)
        pl.semaphore_wait(barrier, len(peers))


class Gather:
    sems = 3

    def __init__(self, at, own, full, ssem, rsem, lsem):
        self.at, self.own, self.full, self.ssem, self.rsem, self.lsem = at, own, full, ssem, rsem, lsem
        self.rows = own.shape[1]

    @staticmethod
    def scratch(seqs):
        return [pltpu.SemaphoreType.DMA((7, seqs)), pltpu.SemaphoreType.DMA((8, seqs)), pltpu.SemaphoreType.DMA((seqs,))]

    def block(self, s, dev):
        return self.full.at[s, pl.ds(pl.multiple_of(dev * self.rows, self.rows), self.rows)]

    def copy(self, s, dev, kind, slot, to, src=None):
        block = self.block(s, dev)
        return self.at.push(block if src is None else src, block, self.ssem.at[kind, s], self.rsem.at[slot, s], to)

    def start(self, s):
        at, own = self.at, self.own.at[s]
        self.copy(s, at.me, 0, 2, at.xn, own).start()
        self.copy(s, at.me, 1, 4, at.yn, own).start()
        self.copy(s, at.me, 2, 1, at.sb, own).start()
        pltpu.make_async_copy(own, self.block(s, at.me), self.lsem.at[s]).start()

    def relay(self, s, by_y):
        at = self.at
        self.copy(s, at.xn, 0, 2, at.xn).wait_recv()
        if by_y:
            self.copy(s, at.xn, 3, 6, at.yn).start()
        self.copy(s, at.xn, 4, 3, at.sb).start()
        self.copy(s, at.yn, 1, 4, at.yn).wait_recv()
        if not by_y:
            self.copy(s, at.yn, 3, 6, at.xn).start()
        self.copy(s, at.yn, 5, 5, at.sb).start()

    def relay_far(self, s):
        at = self.at
        self.copy(s, at.dg, 3, 6, at.yn).wait_recv()
        self.copy(s, at.dg, 6, 7, at.sb).start()

    def finish(self, s):
        at = self.at
        for dev, slot in ((at.sb, 1), (at.sb + at.dx, 3), (at.sb + at.dy, 5), (at.sb + at.dx + at.dy, 7)):
            self.copy(s, dev, 0, slot, at.sb).wait_recv()
        for kind in range(7):
            self.copy(s, at.me, kind, 0, at.sb).wait_send()
        pltpu.make_async_copy(self.own.at[s], self.block(s, at.me), self.lsem.at[s]).wait()


def gather_tail(seqs, gather):
    def relay(i, _):
        gather.relay(2 * i, True)
        gather.relay(2 * i + 1, False)
        return 0

    def far(s, _):
        gather.relay_far(s)
        return 0

    def finish(s, _):
        gather.finish(s)
        return 0

    lax.fori_loop(0, seqs // 2, relay, 0)
    lax.fori_loop(0, seqs, far, 0)
    lax.fori_loop(0, seqs, finish, 0)


class Reduce:
    def __init__(self, at, part, held, mine, x1, y1, x2, y2, ms, hs, hr, d1s, d1r, d2s, d2r):
        self.at, self.part, self.held, self.mine = at, part, held, mine
        self.x1, self.y1, self.x2, self.y2 = x1, y1, x2, y2
        self.ms, self.hs, self.hr, self.d1s, self.d1r, self.d2s, self.d2r = ms, hs, hr, d1s, d1r, d2s, d2r
        self.half = part.shape[2] // 2

    @staticmethod
    def scratch(part):
        s, _, t, d = part.shape
        dma = pltpu.SemaphoreType.DMA
        return [
            pltpu.VMEM((s, 4, t, d), BF16),
            pltpu.VMEM((s, 4, t, d), BF16),
            pltpu.VMEM((s, t // 2, d), BF16),
            pltpu.VMEM((s, t // 2, d), BF16),
            pltpu.VMEM((s, t, d), BF16),
            pltpu.VMEM((s, t, d), BF16),
            dma((4, s)),
            dma((4, s)),
            dma((4, s)),
            dma((2, s)),
            dma((2, s)),
            dma((2, s)),
            dma((2, s)),
        ]

    sems = 13

    def core_copy(self, s, k):
        at = self.at
        dest = (at.sb, at.sb + at.dx, at.sb + at.dy, at.sb + at.dx + at.dy)[k]
        return at.push(self.part.at[s, dest], self.held.at[s, k], self.hs.at[k, s], self.hr.at[k, s], at.sb)

    def load(self, s, k):
        at = self.at
        dest = (at.me, at.xn, at.yn, at.dg)[k]
        return pltpu.make_async_copy(self.part.at[s, dest], self.mine.at[s, k], self.ms.at[k, s])

    def first(self, s, k):
        at, h = self.at, self.half
        src = self.held.at[s, 3, pl.ds(k * h, h)]
        return at.push(src, (self.x1, self.y1)[k].at[s], self.d1s.at[k, s], self.d1r.at[k, s], (at.xn, at.yn)[k])

    def second(self, s, k):
        at = self.at
        src = self.held.at[s, 1 + k]
        return at.push(src, (self.x2, self.y2)[k].at[s], self.d2s.at[k, s], self.d2r.at[k, s], (at.xn, at.yn)[k])

    def start(self, s):
        for k in (3, 1, 2, 0):
            self.core_copy(s, k).start()
            self.load(s, k).start()

    def hop1(self, s):
        self.core_copy(s, 3).wait_recv()
        self.load(s, 3).wait()
        self.held[s, 3] = (self.held[s, 3].astype(F32) + self.mine[s, 3].astype(F32)).astype(BF16)
        self.first(s, 0).start()
        self.first(s, 1).start()

    def hop2(self, s):
        h = self.half
        for k, extra, rows, rest in (
            (0, self.y1, pl.ds(h, h), pl.ds(0, h)),
            (1, self.x1, pl.ds(0, h), pl.ds(h, h)),
        ):
            self.core_copy(s, 1 + k).wait_recv()
            self.load(s, 1 + k).wait()
            self.first(s, 1 - k).wait_recv()
            held, mine = self.held.at[s, 1 + k], self.mine.at[s, 1 + k]
            held[rows] = (held[rows].astype(F32) + mine[rows].astype(F32) + extra[s].astype(F32)).astype(BF16)
            held[rest] = (held[rest].astype(F32) + mine[rest].astype(F32)).astype(BF16)
            self.second(s, k).start()

    def total(self, s):
        self.core_copy(s, 0).wait_recv()
        self.load(s, 0).wait()
        self.second(s, 0).wait_recv()
        self.second(s, 1).wait_recv()
        return (
            self.mine[s, 0].astype(F32)
            + self.held[s, 0].astype(F32)
            + self.x2[s].astype(F32)
            + self.y2[s].astype(F32)
        )

    def finish(self, s):
        for k in range(4):
            self.core_copy(s, k).wait_send()
        for k in range(2):
            self.first(s, k).wait_send()
            self.second(s, k).wait_send()


def each(n, *steps):
    def run(s, _):
        for step in steps:
            step(s)
        return 0

    lax.fori_loop(0, n, run, 0)


COMM = dict(has_side_effects=True, vmem_limit_bytes=60 << 20)


def front_kernel(
    tok, cot, ids, gates, wq, wk, wv, pk, full, weights, routed, gains, small,
    packets, gsend, grecv, glocal, wsend, wrecv, psend, precv, rsend, rrecv, lsend, lrecv, local,
):
    at = Place()
    z = at.rep
    gather = Gather(at, tok, full, gsend, grecv, glocal)
    seqs, _, width = tok.shape
    top = ids.shape[1]
    block, cols = wq.shape[0], weights.shape[2]
    quarter = block // 4
    peers = at.peers()
    barrier = pltpu.get_barrier_semaphore()
    line = [lax.rem(z + k, 4) for k in range(1, 4)]
    for dev in line:
        pl.semaphore_signal(barrier, inc=1, device_id=(dev, at.me), device_id_type=MESH)
    for dev in peers:
        pl.semaphore_signal(barrier, inc=1, device_id=(z, dev), device_id_type=MESH)
    pl.semaphore_wait(barrier, 10)

    def packet_copy(m, dev):
        return at.push(pk, packets.at[at.me], psend.at[m], precv.at[m], dev)

    def weight_copy(m, j, dev):
        theirs = pl.ds(pl.multiple_of(dev * cols, cols), cols)
        src = (wq, wk, wv)[j].at[pl.ds(pl.multiple_of(z * quarter, quarter), quarter), theirs]
        dst = weights.at[j, pl.ds(pl.multiple_of(at.me * block + z * quarter, quarter), quarter)]
        return at.push(src, dst, wsend.at[m, j], wrecv.at[m, j], dev)

    def weight_landed(m, j, dev):
        dst = weights.at[j, pl.ds(pl.multiple_of(dev * block + z * quarter, quarter), quarter)]
        return at.push(dst, dst, wsend.at[m, j], wrecv.at[m, j], dev)

    def walk(m, q, right):
        part = weights.at[:, pl.ds(pl.multiple_of(peers[m] * block + q * quarter, quarter), quarter)]
        send, recv, dev = (rsend, rrecv, z + 1) if right else (lsend, lrecv, z - 1)
        return pltpu.make_async_remote_copy(
            src_ref=part, dst_ref=part, send_sem=send.at[m, q], recv_sem=recv.at[m, q],
            device_id=(dev, at.me), device_id_type=MESH,
        )

    for m, dev in enumerate(peers):
        packet_copy(m, dev).start()
        for j in range(3):
            weight_copy(m, j, dev).start()
    each(seqs, gather.start)
    own_cols = pl.ds(pl.multiple_of(at.me * cols, cols), cols)
    mine = pl.ds(pl.multiple_of(at.me * block, block), block)
    own = [pltpu.make_async_copy(w.at[:, own_cols], weights.at[j, mine], local.at[j]) for j, w in enumerate((wq, wk, wv))]
    for copy in own:
        copy.start()

    place = lax.broadcasted_iota(jnp.int32, (top, 128), 0)
    lane = lax.broadcasted_iota(jnp.int32, (top, 128), 1)
    first = jnp.where(lane == place, 1.0, 0.0).astype(BF16)
    second = jnp.where(lane == place + top, 1.0, 0.0).astype(BF16)

    def join(s):
        routed[s, :, 0:width] = cot[s]
        table = dot(ids[s].astype(F32).astype(BF16), first, 0, 0) + dot(gates[s], second, 0, 0)
        routed[s, :, width : width + 128] = table.astype(BF16)

    each(seqs, join)

    for m, dev in enumerate(peers):
        for j in range(3):
            weight_landed(m, j, dev).wait_recv()

        @pl.when(z < 3)
        def _():
            walk(m, z, True).start()

        @pl.when(z > 0)
        def _():
            walk(m, z, False).start()

    def pass_on(d):
        @pl.when(z - d >= 0)
        def _():
            for m in range(7):
                walk(m, z - d, True).wait_recv()

                @pl.when(z < 3)
                def _():
                    walk(m, z - d, True).start()

        @pl.when(z + d <= 3)
        def _():
            for m in range(7):
                walk(m, z + d, False).wait_recv()

                @pl.when(z > 0)
                def _():
                    walk(m, z + d, False).start()

    def relay(i, _):
        gather.relay(2 * i, True)
        gather.relay(2 * i + 1, False)
        return 0

    pairs = seqs // 2
    lax.fori_loop(0, pairs // 2, relay, 0)
    pass_on(1)
    lax.fori_loop(pairs // 2, pairs, relay, 0)
    pass_on(2)
    each(seqs, gather.relay_far)
    for m, dev in enumerate(peers):
        packet_copy(m, dev).wait_recv()
    packets[at.me] = pk[...]
    devices = packets.shape[0]
    share = width // (128 * devices)
    heads = HEAD_DIM // devices
    gains[...] = jnp.zeros_like(gains)
    small[...] = jnp.zeros_like(small)
    for o in range(devices):
        for k in range(share):
            lanes = pl.ds((o * share + k) * 128, 128)
            gains[0:1, lanes] = packets[o, k : k + 1]
            gains[1:2, lanes] = packets[o, share + k : share + k + 1]
        base = 2 * share
        small[0:1] += pltpu.roll(packets[o, base : base + 1], o * heads, 1)
        small[1:2] += pltpu.roll(packets[o, base + 1 : base + 2], o * heads, 1)
        small[2:3] += pltpu.roll(packets[o, base + 2 : base + 3], o, 1)
    each(seqs, gather.finish)
    pass_on(3)

    def sent(q, going, right):
        @pl.when(going)
        def _():
            for m in range(7):
                walk(m, q, right).wait_send()

    for q in range(4):
        sent(q, jnp.logical_and(q <= z, z < 3), True)
        sent(q, jnp.logical_and(q >= z, z > 0), False)
    for m, dev in enumerate(peers):
        packet_copy(m, dev).wait_send()
        for j in range(3):
            weight_copy(m, j, dev).wait_send()
    for copy in own:
        copy.wait()


def front(tokens, cotangent, ids, gates, wq, wk, wv, packet):
    seqs, rows, width = tokens.shape
    ep = lax.axis_size("ep")
    cols = wq.shape[1] // ep
    top = ids.shape[1]
    if ep != 8 or lax.axis_size("rep") != 4:
        full = lax.all_gather(tokens, "ep", axis=1, tiled=True)
        weights = [lax.all_to_all(w, "ep", split_axis=1, concat_axis=0, tiled=True) for w in (wq, wk, wv)]
        routes = jnp.concatenate([ids.astype(BF16), gates], axis=1).transpose(0, 2, 1)
        routes = jnp.pad(routes, ((0, 0), (0, 0), (0, 128 - 2 * top)))
        packets = lax.all_gather(packet, "ep", axis=0)
        share, heads = width // (128 * ep), HEAD_DIM // ep
        gains = jnp.stack([packets[:, :share].reshape(width), packets[:, share : 2 * share].reshape(width)])
        lens = jnp.pad(packets[:, 2 * share + 2, 0], (0, 128 - ep))
        few = [packets[:, 2 * share + k, :heads].reshape(HEAD_DIM) for k in range(2)] + [lens]
        return (
            full, jnp.stack(weights), jnp.concatenate([cotangent, routes], axis=-1),
            jnp.pad(gains, ((0, 6), (0, 0))), jnp.pad(jnp.stack(few), ((0, 5), (0, 0))),
        )
    dma = pltpu.SemaphoreType.DMA
    return pl.pallas_call(
        front_kernel,
        out_shape=(
            sds((seqs, rows * ep, width), BF16),
            sds((3, wq.shape[0] * ep, cols), BF16),
            sds((seqs, rows, width + 128), BF16),
            sds((8, width), F32),
            sds((8, 128), F32),
        ),
        in_specs=[VM] * 8,
        out_specs=(AN, AN, VM, VM, VM),
        scratch_shapes=[pltpu.VMEM((ep,) + packet.shape, F32)]
        + Gather.scratch(seqs)
        + [dma((7, 3)), dma((7, 3)), dma((7,)), dma((7,))]
        + [dma((7, 4))] * 4
        + [dma((3,))],
        compiler_params=pltpu.CompilerParams(collective_id=1, **COMM),
        name="front",
    )(tokens, cotangent, ids, gates, wq, wk, wv, packet)


def plain_living(small, seqs, rows):
    place = (jnp.arange(rows) + lax.axis_index("ep") * rows).astype(F32)
    return (place[None] < small[2, :seqs, None]).astype(F32)[..., None]


def mix_kernel(part, tok, small, gains, middle, full, own, *scratch):
    at = Place()
    seqs = tok.shape[0]
    reduce = Reduce(at, part, *scratch[: Reduce.sems])
    gather = Gather(at, own, full, *scratch[Reduce.sems :])
    at.greet((at.xn, at.yn, at.sb))
    each(seqs, reduce.start)
    each(seqs, reduce.hop1)
    each(seqs, reduce.hop2)

    def rows(s):
        living = live_rows(small, s, at.me, tok.shape[1])
        mid, mixed = mix_rows(reduce.total(s), tok[s], living, gains[1:2])
        middle[s] = mid
        own[s] = mixed
        gather.start(s)

    each(seqs, rows)
    gather_tail(seqs, gather)
    each(seqs, reduce.finish)


def mix(part, tokens, small, gains):
    seqs, rows, width = tokens.shape
    ep = lax.axis_size("ep")
    if ep != 8:
        total = lax.psum_scatter(part, "ep", scatter_dimension=1, tiled=True).astype(F32)
        middle, mixed = mix_rows(total, tokens, plain_living(small, seqs, rows), gains[1])
        return middle, lax.all_gather(mixed, "ep", axis=1, tiled=True)
    part = part.reshape(seqs, ep, rows, width)
    return pl.pallas_call(
        mix_kernel,
        out_shape=(sds(tokens.shape, F32), sds((seqs, rows * ep, width), BF16)),
        in_specs=[AN] + [VM] * 3,
        out_specs=(VM, AN),
        scratch_shapes=[pltpu.VMEM(tokens.shape, BF16)] + Reduce.scratch(part) + Gather.scratch(seqs),
        compiler_params=pltpu.CompilerParams(collective_id=2, **COMM),
        name="mix",
    )(part, tokens, small, gains)


def back_kernel(gpart, middle, cot, small, gains, mgrad, ggrad, full, own, *scratch):
    at = Place()
    seqs = cot.shape[0]
    n = Reduce.sems
    rg = Reduce(at, gpart, *scratch[:n])
    gather = Gather(at, own, full, *scratch[n:])
    at.greet((at.xn, at.yn, at.sb))
    each(seqs, rg.start)
    each(seqs, rg.hop1)
    each(seqs, rg.hop2)
    ggrad[...] = jnp.zeros_like(ggrad)

    def rows(s):
        living = live_rows(small, s, at.me, cot.shape[1])
        mg, ag, back = ffn_back_rows(rg.total(s), middle[s], cot[s], living, gains[1:2])
        mgrad[s] = mg
        own[s] = ag
        ggrad[...] += jnp.sum(back, axis=0, keepdims=True)
        gather.start(s)

    each(seqs, rows)
    gather_tail(seqs, gather)
    each(seqs, rg.finish)


def back(gpart, middle, cot, small, gains):
    seqs, rows, width = cot.shape
    ep = lax.axis_size("ep")
    if ep != 8:
        mixed_grad = lax.psum_scatter(gpart, "ep", scatter_dimension=1, tiled=True).astype(F32)
        mg, ag, backs = ffn_back_rows(mixed_grad, middle, cot, plain_living(small, seqs, rows), gains[1])
        full = lax.all_gather(ag, "ep", axis=1, tiled=True)
        return mg, jnp.sum(backs, axis=(0, 1))[None], full
    gpart = gpart.reshape(seqs, ep, rows, width)
    return pl.pallas_call(
        back_kernel,
        out_shape=(
            sds(cot.shape, F32),
            sds((1, width), F32),
            sds((seqs, rows * ep, width), BF16),
        ),
        in_specs=[AN] + [VM] * 4,
        out_specs=(VM, VM, AN),
        scratch_shapes=[pltpu.VMEM(cot.shape, BF16)] + Reduce.scratch(gpart) + Gather.scratch(seqs),
        compiler_params=pltpu.CompilerParams(collective_id=3, **COMM),
        name="back",
    )(gpart, middle, cot, small, gains)


def finish_kernel(
    wgrad, wograd, npart, opart, tok, middle, mgrad, gains, others,
    out, small_out, result, tgrad,
    own, held, met, ggrad, parcel, landed, spare,
    wsend, wrecv, local, gsend, grecv, os, or_, ps, pr, qs, qr, fs, fr, ss, sr, *scratch,
):
    at = Place()
    z, me = at.rep, at.me
    n = Reduce.sems
    normed_sum = Reduce(at, npart, *scratch[:n])
    result_sum = Reduce(at, opart, *scratch[n:])
    seqs = tok.shape[0]
    parts, pieces = own.shape[:2]
    chunks = parts * pieces
    width = wgrad.shape[3]
    peers = at.peers()
    barrier = pltpu.get_barrier_semaphore()
    line = [lax.rem(z + k, 4) for k in range(1, 4)]
    for dev in line:
        pl.semaphore_signal(barrier, inc=1, device_id=(dev, me), device_id_type=MESH)
    for dev in peers:
        pl.semaphore_signal(barrier, inc=1, device_id=(z, dev), device_id_type=MESH)
    pl.semaphore_wait(barrier, 10)
    inner = jnp.logical_and(z > 0, z < 3)
    outer_end, partner, outer = 1 + z // 3, 3 - z, 3 * (z - 1)
    cols = pl.ds(pl.multiple_of(me * width, width), width)

    def column_copy(m, j, dev):
        rows = pl.ds(pl.multiple_of(dev * pieces, pieces), pieces)
        return at.push(wgrad.at[j, rows], own.at[1 + j, :, :, cols], wsend.at[m, j], wrecv.at[m, j], dev)

    mine_rows = pl.ds(pl.multiple_of(me * pieces, pieces), pieces)
    locals_ = [pltpu.make_async_copy(wgrad.at[j, mine_rows], own.at[1 + j, :, :, cols], local.at[j]) for j in range(3)]
    locals_.append(pltpu.make_async_copy(wograd, own.at[0], local.at[3]))
    for copy in locals_:
        copy.start()
    for j in range(3):
        for m, dev in enumerate(peers):
            column_copy(m, j, dev).start()
    each(seqs, normed_sum.start)
    each(seqs, result_sum.start)
    ggrad[...] = jnp.zeros_like(ggrad)

    def piece(ref, c):
        return ref.at[c // pieces, lax.rem(c, pieces)]

    def line_push(src, dst, send, recv, dev):
        return pltpu.make_async_remote_copy(
            src_ref=src, dst_ref=dst, send_sem=send, recv_sem=recv, device_id=(dev, me), device_id_type=MESH
        )

    def inward(c):
        return line_push(piece(own, c), piece(held, c), os.at[c], or_.at[c], outer_end)

    def across(c):
        return line_push(piece(held, c), met.at[c // 2], ps.at[c], pr.at[c], partner)

    def share(c):
        return line_push(piece(out, c), piece(out, c), qs.at[c], qr.at[c], partner)

    def outward(c):
        return line_push(piece(out, c), piece(out, c), fs.at[c], fr.at[c], outer)

    def mine(c):
        return 1 + lax.rem(c, 2) == z

    def ready(part):
        for j in range(parts):

            @pl.when(part == j)
            def _():
                locals_[(3, 0, 1, 2)[j]].wait()
                if j > 0:
                    for m, dev in enumerate(peers):
                        column_copy(m, j - 1, dev).wait_recv()

    def step(c):
        @pl.when(lax.rem(c, pieces) == 0)
        def _():
            ready(c // pieces)

        @pl.when(jnp.logical_not(inner))
        def _():
            inward(c).start()

        @pl.when(inner)
        def _():
            inward(c).wait_recv()
            here = piece(held, c)
            here[...] = (here[...].astype(F32) + piece(own, c)[...].astype(F32)).astype(BF16)

            @pl.when(jnp.logical_not(mine(c)))
            def _():
                across(c).start()

    def settle(c):
        @pl.when(jnp.logical_and(inner, mine(c)))
        def _():
            across(c).wait_recv()
            piece(out, c)[...] = (piece(held, c)[...].astype(F32) + met[c // 2].astype(F32)).astype(BF16)
            share(c).start()
            outward(c).start()

    def forward(c):
        @pl.when(jnp.logical_and(inner, jnp.logical_not(mine(c))))
        def _():
            share(c).wait_recv()
            outward(c).start()

    def token_rows(s):
        tg, back = attn_back_rows(normed_sum.total(s), tok[s], mgrad[s], gains[0:1])
        tgrad[s] = tg
        ggrad[...] += jnp.sum(back, axis=0, keepdims=True)

    def out_rows(s):
        result[s] = (middle[s] + result_sum.total(s)).astype(BF16)

    jobs = (
        (step, 0, chunks), (settle, 1, chunks), (forward, 2, chunks),
        (normed_sum.hop1, 2, seqs), (normed_sum.hop2, 6, seqs), (token_rows, 10, seqs),
        (result_sum.hop1, 6, seqs), (result_sum.hop2, 10, seqs), (out_rows, 14, seqs),
    )

    def tick(i, _):
        for job, lag, count in jobs:

            @pl.when(jnp.logical_and(i >= lag, i < lag + count))
            def _():
                job(i - lag)

        return 0

    lax.fori_loop(0, max(lag + count for _, lag, count in jobs), tick, 0)

    parcel[...] = jnp.zeros_like(parcel)
    devices = parcel.shape[0]
    rows_of = ggrad.shape[1] // (128 * devices)
    for dev in range(devices):
        for k in range(rows_of):
            lanes = pl.ds((dev * rows_of + k) * 128, 128)
            parcel[dev, k : k + 1] = ggrad[:, lanes]
            parcel[dev, rows_of + k : rows_of + k + 1] = others[0:1, lanes]
        parcel[dev, 2 * rows_of : 2 * rows_of + 2] = others[1:3, 0:128]

    def parcel_copy(m, dev):
        return at.push(parcel.at[dev], landed.at[m], gsend.at[m], grecv.at[m], dev)

    for m, dev in enumerate(peers):
        parcel_copy(m, dev).start()
    total = parcel[me]
    for m, dev in enumerate(peers):
        parcel_copy(m, dev).wait_recv()
        total = total + landed[m]
    spare[0] = total

    def small_copy(k):
        return line_push(spare.at[0], spare.at[1 + k], ss.at[k], sr.at[k], line[k])

    for k in range(3):
        small_copy(k).start()

    @pl.when(jnp.logical_not(inner))
    def _():
        each(chunks, lambda c: outward(c).wait_recv())
        each(chunks, lambda c: inward(c).wait_send())

    @pl.when(inner)
    def _():
        def sent(c):
            outward(c).wait_send()

            @pl.when(mine(c))
            def _():
                share(c).wait_send()

            @pl.when(jnp.logical_not(mine(c)))
            def _():
                across(c).wait_send()

        each(chunks, sent)

    each(seqs, normed_sum.finish, result_sum.finish)
    for m, dev in enumerate(peers):
        parcel_copy(m, dev).wait_send()
        for j in range(3):
            column_copy(m, j, dev).wait_send()
    total = spare[0]
    for k in range(3):
        small_copy(k).wait()
        total = total + spare[1 + k]
    small_out[...] = total


def finish(wgrad, wograd, npart, opart, tokens, middle, mgrad, gains, ffn_back, qk_back):
    seqs, rows, width = tokens.shape
    ep = lax.axis_size("ep")
    if ep != 8 or lax.axis_size("rep") != 4:
        normed_grad = lax.psum_scatter(npart, "ep", scatter_dimension=1, tiled=True).astype(F32)
        moe = lax.psum_scatter(opart, "ep", scatter_dimension=1, tiled=True).astype(F32)
        tg, backs = attn_back_rows(normed_grad, tokens, mgrad, gains[0])
        wrows = lax.all_to_all(wgrad, "ep", split_axis=1, concat_axis=2, tiled=True)
        share = width // ep
        small = jnp.concatenate([jnp.sum(backs, axis=(0, 1)), ffn_back[0], qk_back[0], qk_back[1]])
        small = lax.psum(small, ("ep", "rep"))
        mine = lax.axis_index("ep") * share
        cut = [lax.dynamic_slice_in_dim(small, k * width + mine, share).reshape(-1, 128) for k in range(2)]
        small = jnp.concatenate(cut + [small[2 * width :].reshape(2, HEAD_DIM)], axis=0)
        big = lax.psum(jnp.concatenate([wograd[None], wrows], axis=0), "rep")
        return big, jnp.pad(small, ((0, 8 - small.shape[0]), (0, 0))), (middle + moe).astype(BF16), tg
    others = jnp.concatenate([ffn_back, jnp.pad(qk_back[:2], ((0, 0), (0, width - HEAD_DIM)))], axis=0)
    npart, opart = (p.reshape(seqs, ep, rows, width) for p in (npart, opart))
    pieces = 4
    block = wograd.shape[0] // pieces
    wgrad = wgrad.reshape(3, wgrad.shape[1] // block, block, wgrad.shape[2])
    wograd = wograd.reshape(pieces, block, width)
    whole = (4, pieces, block, width)
    dma = pltpu.SemaphoreType.DMA
    chunks = 4 * pieces
    out, small, result, tgrad = pl.pallas_call(
        finish_kernel,
        out_shape=(sds(whole, BF16), sds((8, 128), F32), sds(tokens.shape, BF16), sds(tokens.shape, BF16)),
        in_specs=[VM, VM, AN, AN] + [VM] * 5,
        out_specs=(VM, VM, VM, VM),
        scratch_shapes=[
            pltpu.VMEM(whole, BF16),
            pltpu.VMEM(whole, BF16),
            pltpu.VMEM((chunks // 2, block, width), BF16),
            pltpu.VMEM((1, width), F32),
            pltpu.VMEM((ep, 8, 128), F32),
            pltpu.VMEM((7, 8, 128), F32),
            pltpu.VMEM((4, 8, 128), F32),
        ]
        + [dma((7, 3)), dma((7, 3)), dma((4,)), dma((7,)), dma((7,))]
        + [dma((chunks,))] * 8
        + [dma((3,))] * 2
        + 2 * Reduce.scratch(npart),
        compiler_params=pltpu.CompilerParams(collective_id=4, has_side_effects=True, vmem_limit_bytes=61 << 20),
        name="finish",
    )(wgrad, wograd, npart, opart, tokens, middle, mgrad, gains, others)
    return out.reshape(4, pieces * block, width), small, result, tgrad


def dot(a, b, ca, cb):
    return lax.dot_general(a, b, (((ca,), (cb,)), ((), ())), preferred_element_type=F32)


def rope(v, cos, sin_turn):
    return v * cos + pltpu.roll(v, HEAD_DIM // 2, 1) * sin_turn


def probabilities(q, k, length):
    scores = dot(q, k, 1, 1) * HEAD_DIM**-0.5
    column = lax.broadcasted_iota(jnp.int32, (1, scores.shape[1]), 1).astype(F32)
    scores = jnp.where(column < length, scores, -1e9)
    p = jnp.exp(scores - jnp.max(scores, axis=-1, keepdims=True))
    return p * (1.0 / jnp.sum(p, axis=-1, keepdims=True))


def attend_kernel(tok, w, wo, gains, small, cos, sin, normed, pre, low, ctx, part):
    length = seq_len(small, pl.program_id(0))
    v = tok[0].astype(F32)
    x = (v * inverse_rms(v) * gains[0:1]).astype(BF16)
    normed[0] = x
    q_pre, k_pre = dot(x, w[0], 1, 0), dot(x, w[1], 1, 0)
    value = dot(x, w[2], 1, 0).astype(BF16)
    pre[0, 0], pre[1, 0] = q_pre, k_pre
    low[2, 0] = value
    for h in range(q_pre.shape[1] // HEAD_DIM):
        cols = slice(h * HEAD_DIM, (h + 1) * HEAD_DIM)
        rot = []
        for i, (u, g) in enumerate(((q_pre[:, cols], small[0:1]), (k_pre[:, cols], small[1:2]))):
            rot.append(rope(u * inverse_rms(u) * g, cos[...], sin[...]).astype(BF16))
            low[i, 0, :, cols] = rot[i]
        attention = probabilities(rot[0], rot[1], length).astype(BF16)
        ctx[0, :, cols] = dot(attention, value[:, cols], 1, 0).astype(BF16)
    part[0] = dot(ctx[0], wo[...], 1, 0).astype(BF16)


def attend(full, weights, wo, gains, small, cos, sin):
    seqs, length, width = full.shape
    cols = weights.shape[2]
    row = lambda i, *_: (i, 0, 0)
    row2 = lambda i, *_: (0, i, 0, 0)
    two = lambda i, *_: (0, 0)
    return pl.pallas_call(
        attend_kernel,
        out_shape=(
            sds(full.shape, BF16),
            sds((2, seqs, length, cols), F32),
            sds((3, seqs, length, cols), BF16),
            sds((seqs, length, cols), BF16),
            sds(full.shape, BF16),
        ),
        grid_spec=pltpu.PrefetchScalarGridSpec(
            num_scalar_prefetch=0,
            grid=(seqs,),
            in_specs=[
                pl.BlockSpec((1, length, width), row),
                pl.BlockSpec(weights.shape, lambda i, *_: (0, 0, 0)),
                pl.BlockSpec(wo.shape, two),
                pl.BlockSpec((8, width), two),
                pl.BlockSpec((8, 128), two),
                pl.BlockSpec((length, HEAD_DIM), two),
                pl.BlockSpec((length, HEAD_DIM), two),
            ],
            out_specs=(
                pl.BlockSpec((1, length, width), row),
                pl.BlockSpec((2, 1, length, cols), row2),
                pl.BlockSpec((3, 1, length, cols), row2),
                pl.BlockSpec((1, length, cols), row),
                pl.BlockSpec((1, length, width), row),
            ),
        ),
        compiler_params=pltpu.CompilerParams(dimension_semantics=("arbitrary",), vmem_limit_bytes=60 << 20),
        cost_estimate=pl.CostEstimate(flops=10**10, bytes_accessed=4 * 10**7, transcendentals=10**6),
        name="attend",
    )(full, weights, wo, gains, small, cos, sin)


def attend_back_kernel(
    agrad, normed, pre, low, ctx, w, wo, small, cos, sin, part, wgrad, wograd, gains, wacc, woacc
):
    s = pl.program_id(0)
    length = seq_len(small, s)

    @pl.when(s == 0)
    def _():
        wacc[...] = jnp.zeros_like(wacc)
        woacc[...] = jnp.zeros_like(woacc)
        gains[...] = jnp.zeros_like(gains)

    ag = agrad[0]
    woacc[...] += dot(ctx[0], ag, 0, 0)
    cg_all = dot(ag, wo[...], 1, 1).astype(BF16)
    scale = HEAD_DIM**-0.5
    half = HEAD_DIM // 2
    grads = ([], [], [])
    for h in range(cg_all.shape[1] // HEAD_DIM):
        cols = slice(h * HEAD_DIM, (h + 1) * HEAD_DIM)
        q, k, value, cg = low[0, 0, :, cols], low[1, 0, :, cols], low[2, 0, :, cols], cg_all[:, cols]
        attention = probabilities(q, k, length)
        grads[2].append(dot(attention.astype(BF16), cg, 0, 0).astype(BF16))
        pg = dot(cg, value, 1, 1)
        sg = (attention * (pg - jnp.sum(attention * pg, axis=-1, keepdims=True))).astype(BF16)
        for i, (rot_grad, g) in enumerate(((dot(sg, k, 1, 0), small[0:1]), (dot(sg, q, 0, 0), small[1:2]))):
            wgt = rot_grad * scale
            u = wgt * cos[...] + pltpu.roll(wgt * sin[...], half, 1)
            v = pre[i, 0, :, cols]
            r = inverse_rms(v)
            grads[i].append(rms_back(v, r, u * g).astype(BF16))
            gains[i : i + 1] += jnp.sum(u * v * r, axis=0, keepdims=True)
    total = None
    for i in range(3):
        g = grads[i][0] if len(grads[i]) == 1 else jnp.concatenate(grads[i], axis=1)
        wacc[i] += dot(normed[0], g, 0, 0)
        piece = dot(g, w[i], 1, 1)
        total = piece if total is None else total + piece
    part[0] = total.astype(BF16)

    @pl.when(s == pl.num_programs(0) - 1)
    def _():
        wgrad[...] = wacc[...].astype(BF16)
        wograd[...] = woacc[...].astype(BF16)


def attend_back(agrad, normed, pre, low, ctx, weights, wo, small, cos, sin):
    seqs, length, width = agrad.shape
    cols = weights.shape[2]
    row = lambda i, *_: (i, 0, 0)
    row2 = lambda i, *_: (0, i, 0, 0)
    two = lambda i, *_: (0, 0)
    three = lambda i, *_: (0, 0, 0)
    return pl.pallas_call(
        attend_back_kernel,
        out_shape=(
            sds(agrad.shape, BF16),
            sds(weights.shape, BF16),
            sds(wo.shape, BF16),
            sds((8, HEAD_DIM), F32),
        ),
        grid_spec=pltpu.PrefetchScalarGridSpec(
            num_scalar_prefetch=0,
            grid=(seqs,),
            in_specs=[
                pl.BlockSpec((1, length, width), row),
                pl.BlockSpec((1, length, width), row),
                pl.BlockSpec((2, 1, length, cols), row2),
                pl.BlockSpec((3, 1, length, cols), row2),
                pl.BlockSpec((1, length, cols), row),
                pl.BlockSpec(weights.shape, three),
                pl.BlockSpec(wo.shape, two),
                pl.BlockSpec((8, 128), two),
                pl.BlockSpec((length, HEAD_DIM), two),
                pl.BlockSpec((length, HEAD_DIM), two),
            ],
            out_specs=(
                pl.BlockSpec((1, length, width), row),
                pl.BlockSpec(weights.shape, three),
                pl.BlockSpec(wo.shape, two),
                pl.BlockSpec((8, HEAD_DIM), two),
            ),
            scratch_shapes=[pltpu.VMEM(weights.shape, F32), pltpu.VMEM(wo.shape, F32)],
        ),
        compiler_params=pltpu.CompilerParams(dimension_semantics=("arbitrary",), vmem_limit_bytes=60 << 20),
        cost_estimate=pl.CostEstimate(flops=2 * 10**10, bytes_accessed=4 * 10**7, transcendentals=10**6),
        name="attend_back",
    )(agrad, normed, pre, low, ctx, weights, wo, small, cos, sin)


BLOCK = 256


def pack_rows(seqs, capacity):
    return -(-seqs * capacity // BLOCK) * BLOCK


def packed_slots(number, table, length_live, top):
    tab = table.astype(F32)
    length = tab.shape[0]
    lane = lax.broadcasted_iota(jnp.int32, tab.shape, 1)
    row = lax.broadcasted_iota(jnp.int32, (length, 1), 0).astype(F32)
    chosen = jnp.logical_and(jnp.logical_and(tab == number, lane < top), row < length_live)
    gates = jnp.where(chosen, pltpu.roll(tab, 128 - top, 1), 0.0).astype(BF16)
    chosen = jnp.where(chosen, 1.0, 0.0).astype(BF16)
    ones = jnp.ones((8, 128), BF16)
    hit = dot(ones, chosen, 1, 1)
    weight = dot(ones, gates, 1, 1)
    earlier = lax.broadcasted_iota(jnp.int32, (length, length), 0)
    later = lax.broadcasted_iota(jnp.int32, (length, length), 1)
    rank = dot(hit.astype(BF16), jnp.where(earlier < later, 1.0, 0.0).astype(BF16), 1, 0)
    return jnp.where(hit > 0.5, rank, -1.0), weight, jnp.sum(hit[0:1]).astype(jnp.int32)


def forward_blocks(blocks, x, dy, wi, wo, acts, dgus):
    hidden = wo.shape[0]
    part = min(hidden, 512)

    def forward(b, _):
        rows = pl.ds(pl.multiple_of(b * BLOCK, BLOCK), BLOCK)
        for h in range(hidden // part):
            gcols, ucols = pl.ds(h * part, part), pl.ds(hidden + h * part, part)
            gate = dot(x[rows], wi[:, gcols], 1, 0)
            up = dot(x[rows], wi[:, ucols], 1, 0)
            dact = dot(dy[rows], wo[gcols], 1, 1)
            sig = 1.0 / (1.0 + jnp.exp(-gate))
            silu = gate * sig
            acts[rows, gcols] = (silu * up).astype(BF16)
            dgus[rows, gcols] = (dact * up * sig * (1.0 + gate * (1.0 - sig))).astype(BF16)
            dgus[rows, ucols] = (dact * silu).astype(BF16)
        return 0

    lax.fori_loop(0, blocks, forward, 0)


def gradient_tiles(blocks, left, right, result, acc, stage, ssem, busy):
    tr, tc = acc.shape
    down, across = result.shape[0] // tr, result.shape[1] // tc

    def tile(t, _):
        rt, ct = t // across, lax.rem(t, across)
        left_cols = pl.ds(pl.multiple_of(rt * tr, tr), tr)
        right_cols = pl.ds(pl.multiple_of(ct * tc, tc), tc)

        def step(b, _):
            rows = pl.ds(pl.multiple_of(b * BLOCK, BLOCK), BLOCK)
            piece = dot(left[rows, left_cols], right[rows, right_cols], 0, 0)

            @pl.when(b == 0)
            def _():
                acc[...] = piece

            @pl.when(b > 0)
            def _():
                acc[...] += piece

            return 0

        @pl.when(blocks == 0)
        def _():
            acc[...] = jnp.zeros_like(acc)

        lax.fori_loop(0, blocks, step, 0)
        k = lax.rem(t, 2)
        out = pltpu.make_async_copy(stage.at[k], result.at[left_cols, right_cols], ssem.at[k])

        @pl.when(jnp.logical_or(t >= 2, busy))
        def _():
            out.wait()

        stage[k] = acc[...].astype(BF16)
        out.start()
        return 0

    lax.fori_loop(0, down * across, tile, 0)


def drain_tiles(result, acc, stage, ssem):
    tr, tc = acc.shape
    for k in range(2):
        pltpu.make_async_copy(stage.at[k], result.at[pl.ds(0, tr), pl.ds(0, tc)], ssem.at[k]).wait()


def first_kernel(
    capacity, top, number, mixed, cot, table, small, w_in, w_out,
    slots0, slots1, starts, act, dgu, x_all, dy_all, out_grad,
    x, dy, wi, wo, acts, dgus, acc, stage, wsem, ssem, rsem,
):
    step = pl.program_id(0)
    steps = pl.num_programs(0)
    together = mixed.shape[0]
    seqs = steps * together
    width = mixed.shape[2]
    loads = [pltpu.make_async_copy(w_in.at[0], wi, wsem.at[0]), pltpu.make_async_copy(w_out.at[0], wo, wsem.at[1])]

    @pl.when(step == 0)
    def _():
        for copy in loads:
            copy.start()
        starts[0, 0] = 0
        starts[1, 0] = 0

    packed = []
    for k in range(together):
        spread, gate_spread, counts = [], [], []
        for j, slots in enumerate((slots0, slots1)):
            slot, weight, count = packed_slots(
                (number[0] + j).astype(F32), table[k], seq_len(small, step * together + k), top
            )
            slots[k, 0:8] = slot
            slots[k, 8:16] = weight
            place = lax.broadcasted_iota(jnp.int32, (capacity, slot.shape[1]), 0).astype(F32) == slot[0:1]
            spread.append(jnp.where(place, 1.0, 0.0).astype(BF16))
            gate_spread.append(jnp.where(place, weight[0:1], 0.0).astype(BF16))
            counts.append(count)
        packed.append(
            (
                counts,
                dot(jnp.concatenate(spread, axis=0), mixed[k], 1, 0).astype(BF16),
                dot(jnp.concatenate(gate_spread, axis=0), cot[k], 1, 0).astype(BF16),
            )
        )
    for k, (counts, x_rows, dy_rows) in enumerate(packed):
        s = step * together + k
        for j in range(2):
            start = pl.multiple_of(starts[j, s], 16)
            x[j, pl.ds(start, capacity)] = x_rows[j * capacity : (j + 1) * capacity]
            dy[j, pl.ds(start, capacity)] = dy_rows[j * capacity : (j + 1) * capacity]
            starts[j, s + 1] = start + (counts[j] + 15) // 16 * 16

    @pl.when(step == steps - 1)
    def _():
        for j in range(2):
            past = (starts[j, seqs - 1] + capacity) // 16
            end = (starts[j, seqs] + BLOCK - 1) // BLOCK * (BLOCK // 16)

            def clear(i, _):
                rows = pl.ds(pl.multiple_of(i * 16, 16), 16)
                x[j, rows] = jnp.zeros((16, width), BF16)
                dy[j, rows] = jnp.zeros((16, width), BF16)
                return 0

            lax.fori_loop(past, end, clear, 0)
        saves = [pltpu.make_async_copy(x, x_all, rsem.at[0]), pltpu.make_async_copy(dy.at[1], dy_all, rsem.at[1])]
        for copy in saves:
            copy.start()
        blocks = (starts[0, seqs] + BLOCK - 1) // BLOCK
        for copy in loads:
            copy.wait()
        forward_blocks(blocks, x.at[0], dy.at[0], wi, wo, acts, dgus)
        saves += [pltpu.make_async_copy(acts, act, rsem.at[2]), pltpu.make_async_copy(dgus, dgu, rsem.at[3])]
        for copy in saves[2:]:
            copy.start()
        gradient_tiles(blocks, acts, dy.at[0], out_grad, acc, stage, ssem, False)
        drain_tiles(out_grad, acc, stage, ssem)
        for copy in saves:
            copy.wait()


def expert_first(number, mixed, cot, small, w_in, w_out, capacity, top):
    seqs, length, width = mixed.shape
    hidden = w_out.shape[1]
    rows = pack_rows(seqs, capacity)
    dma = pltpu.SemaphoreType.DMA
    seq = lambda i, *_: (i, 0, 0)
    together = 2
    slot_spec = pl.BlockSpec((together, 16, length), seq)
    return pl.pallas_call(
        functools.partial(first_kernel, capacity, top),
        out_shape=(
            sds((seqs, 16, length), F32),
            sds((seqs, 16, length), F32),
            sds((2, seqs + 1), jnp.int32),
            sds((rows, hidden), BF16),
            sds((rows, 2 * hidden), BF16),
            sds((2, rows, width), BF16),
            sds((rows, width), BF16),
            sds((hidden, width), BF16),
        ),
        grid_spec=pltpu.PrefetchScalarGridSpec(
            num_scalar_prefetch=1,
            grid=(seqs // together,),
            in_specs=[
                pl.BlockSpec((together, length, width), seq),
                pl.BlockSpec((together, length, width), seq),
                pl.BlockSpec((together, length, 128), lambda i, *_: (i, 0, width // 128)),
                pl.BlockSpec((8, 128), lambda i, *_: (0, 0)),
                AN,
                AN,
            ],
            out_specs=(slot_spec, slot_spec, pl.BlockSpec(memory_space=pltpu.SMEM), AN, AN, AN, AN, AN),
            scratch_shapes=[
                pltpu.VMEM((2, rows, width), BF16),
                pltpu.VMEM((2, rows, width), BF16),
                pltpu.VMEM(w_in.shape[1:], BF16),
                pltpu.VMEM(w_out.shape[1:], BF16),
                pltpu.VMEM((rows, hidden), BF16),
                pltpu.VMEM((rows, 2 * hidden), BF16),
                pltpu.VMEM((256, 1024), F32),
                pltpu.VMEM((2, 256, 1024), BF16),
                dma((2,)),
                dma((2,)),
                dma((4,)),
            ],
        ),
        compiler_params=pltpu.CompilerParams(dimension_semantics=("arbitrary",), vmem_limit_bytes=63 << 20),
        cost_estimate=pl.CostEstimate(flops=2 * 10**10, bytes_accessed=6 * 10**7, transcendentals=10**6),
        name="expert_first",
    )(number, mixed, cot, cot, small, w_in, w_out)


def in_grad_kernel(starts, x_all, dgu, in_grad, x, dgus, acc, stage, lsem, ssem):
    blocks = (starts[0, starts.shape[1] - 1] + BLOCK - 1) // BLOCK

    def load(b):
        rows = pl.ds(pl.multiple_of(b * BLOCK, BLOCK), BLOCK)
        return (
            pltpu.make_async_copy(x_all.at[0, rows], x.at[rows], lsem.at[0, b]),
            pltpu.make_async_copy(dgu.at[rows], dgus.at[rows], lsem.at[1, b]),
        )

    def run(b, action):
        for copy in load(b):
            getattr(copy, action)()
        return 0

    lax.fori_loop(0, blocks, lambda b, _: run(b, "start"), 0)
    lax.fori_loop(0, blocks, lambda b, _: run(b, "wait"), 0)
    gradient_tiles(blocks, x, dgus, in_grad, acc, stage, ssem, False)
    drain_tiles(in_grad, acc, stage, ssem)


def first_in_grad(starts, x_all, dgu):
    rows, width = x_all.shape[1:]
    dma = pltpu.SemaphoreType.DMA
    return pl.pallas_call(
        in_grad_kernel,
        out_shape=sds((width, dgu.shape[1]), BF16),
        grid_spec=pltpu.PrefetchScalarGridSpec(
            num_scalar_prefetch=1,
            grid=(1,),
            in_specs=[AN, AN],
            out_specs=AN,
            scratch_shapes=[
                pltpu.VMEM((rows, width), BF16),
                pltpu.VMEM(dgu.shape, BF16),
                pltpu.VMEM((512, 2048), F32),
                pltpu.VMEM((2, 512, 2048), BF16),
                dma((2, rows // BLOCK)),
                dma((2,)),
            ],
        ),
        compiler_params=pltpu.CompilerParams(dimension_semantics=("arbitrary",), vmem_limit_bytes=60 << 20),
        cost_estimate=pl.CostEstimate(flops=10**10, bytes_accessed=2 * 10**7, transcendentals=0),
        name="first_in_grad",
    )(starts, x_all, dgu)


def second_kernel(
    starts, x_all, dy_all, w_in, w_out, act, dgu, out_grad, in_grad,
    x, dy, wi, wo, acts, dgus, acc, stage, wsem, lsem, ssem, rsem,
):
    blocks = (starts[1, starts.shape[1] - 1] + BLOCK - 1) // BLOCK
    loads = [pltpu.make_async_copy(w_in.at[1], wi, wsem.at[0]), pltpu.make_async_copy(w_out.at[1], wo, wsem.at[1])]

    def load(b, action):
        rows = pl.ds(pl.multiple_of(b * BLOCK, BLOCK), BLOCK)
        for copy in (
            pltpu.make_async_copy(x_all.at[1, rows], x.at[rows], lsem.at[0, b]),
            pltpu.make_async_copy(dy_all.at[rows], dy.at[rows], lsem.at[1, b]),
        ):
            getattr(copy, action)()
        return 0

    for copy in loads:
        copy.start()
    lax.fori_loop(0, blocks, lambda b, _: load(b, "start"), 0)
    for copy in loads:
        copy.wait()
    lax.fori_loop(0, blocks, lambda b, _: load(b, "wait"), 0)
    forward_blocks(blocks, x, dy, wi, wo, acts, dgus)
    saves = [pltpu.make_async_copy(acts, act, rsem.at[0]), pltpu.make_async_copy(dgus, dgu, rsem.at[1])]
    for copy in saves:
        copy.start()
    gradient_tiles(blocks, x, dgus, in_grad, acc, stage, ssem, False)
    gradient_tiles(blocks, acts, dy, out_grad, acc, stage, ssem, True)
    drain_tiles(out_grad, acc, stage, ssem)
    for copy in saves:
        copy.wait()


def expert_second(starts, x_all, dy_all, w_in, w_out):
    rows, width = dy_all.shape
    hidden = w_out.shape[1]
    dma = pltpu.SemaphoreType.DMA
    return pl.pallas_call(
        second_kernel,
        out_shape=(
            sds((rows, hidden), BF16),
            sds((rows, 2 * hidden), BF16),
            sds((hidden, width), BF16),
            sds((width, 2 * hidden), BF16),
        ),
        grid_spec=pltpu.PrefetchScalarGridSpec(
            num_scalar_prefetch=1,
            grid=(1,),
            in_specs=[AN] * 4,
            out_specs=(AN, AN, AN, AN),
            scratch_shapes=[
                pltpu.VMEM((rows, width), BF16),
                pltpu.VMEM((rows, width), BF16),
                pltpu.VMEM(w_in.shape[1:], BF16),
                pltpu.VMEM(w_out.shape[1:], BF16),
                pltpu.VMEM((rows, hidden), BF16),
                pltpu.VMEM((rows, 2 * hidden), BF16),
                pltpu.VMEM((512, 2048), F32),
                pltpu.VMEM((2, 512, 2048), BF16),
                dma((2,)),
                dma((2, rows // BLOCK)),
                dma((2,)),
                dma((2,)),
            ],
        ),
        compiler_params=pltpu.CompilerParams(dimension_semantics=("arbitrary",), vmem_limit_bytes=60 << 20),
        cost_estimate=pl.CostEstimate(flops=25 * 10**9, bytes_accessed=6 * 10**7, transcendentals=10**6),
        name="expert_second",
    )(starts, x_all, dy_all, w_in, w_out)


def tail_kernel(j, starts, act, dgu, w_in, w_out, produced, dx):
    @pl.when(pl.program_id(0) * BLOCK < starts[j, starts.shape[1] - 1])
    def _():
        produced[...] = dot(act[...], w_out[...], 1, 0).astype(BF16)
        dx[...] = dot(dgu[...], w_in[...], 1, 1).astype(BF16)


def expert_tail(j, starts, act, dgu, w_in, w_out):
    rows, hidden = act.shape
    width = w_in.shape[1]
    last = starts.shape[1] - 1
    block = lambda i, st: (jnp.maximum(jnp.minimum(i, (st[j, last] + BLOCK - 1) // BLOCK - 1), 0), 0)
    return pl.pallas_call(
        functools.partial(tail_kernel, j),
        out_shape=(sds((rows, width), BF16), sds((rows, width), BF16)),
        grid_spec=pltpu.PrefetchScalarGridSpec(
            num_scalar_prefetch=1,
            grid=(rows // BLOCK,),
            in_specs=[
                pl.BlockSpec((BLOCK, hidden), block),
                pl.BlockSpec((BLOCK, 2 * hidden), block),
                pl.BlockSpec((None,) + w_in.shape[1:], lambda i, *_: (j, 0, 0)),
                pl.BlockSpec((None,) + w_out.shape[1:], lambda i, *_: (j, 0, 0)),
            ],
            out_specs=(pl.BlockSpec((BLOCK, width), block), pl.BlockSpec((BLOCK, width), block)),
        ),
        compiler_params=pltpu.CompilerParams(dimension_semantics=("arbitrary",), vmem_limit_bytes=60 << 20),
        cost_estimate=pl.CostEstimate(flops=12 * 10**9, bytes_accessed=3 * 10**7, transcendentals=0),
        name="expert_tail",
    )(starts, act, dgu, w_in, w_out)


def combine_kernel(capacity, local, *refs):
    s = pl.program_id(0)
    starts = refs[0]
    slots = refs[1 : 1 + local]
    produced = refs[1 + local : 1 + 2 * local]
    dx = refs[1 + 2 * local : 1 + 3 * local]
    out_part, grad_part = refs[1 + 3 * local :]
    out_sum, grad_sum = None, None
    for j in range(local):
        length = slots[j].shape[2]
        column = lax.broadcasted_iota(jnp.int32, (capacity, length), 0).astype(F32)
        place = column == slots[j][0, 0:1]
        span = pl.ds(pl.multiple_of(starts[j, s], 16), capacity)
        held = lax.broadcasted_iota(jnp.int32, (capacity, 1), 0) < starts[j, s + 1] - starts[j, s]
        rows = jnp.where(held, produced[j][span], 0.0).astype(BF16)
        grads = jnp.where(held, dx[j][span], 0.0).astype(BF16)
        out = dot(jnp.where(place, slots[j][0, 8:9], 0.0).astype(BF16), rows, 0, 0)
        grad = dot(jnp.where(place, 1.0, 0.0).astype(BF16), grads, 0, 0)
        out_sum = out if out_sum is None else out_sum + out
        grad_sum = grad if grad_sum is None else grad_sum + grad
    out_part[0] = out_sum.astype(BF16)
    grad_part[0] = grad_sum.astype(BF16)


def combine(starts, slots, produced, dx, capacity):
    local = len(slots)
    seqs, _, length = slots[0].shape
    width = produced[0].shape[1]
    seq = lambda i, *_: (i, 0, 0)
    two = lambda i, *_: (0, 0)
    rows = pl.BlockSpec(produced[0].shape, two)
    return pl.pallas_call(
        functools.partial(combine_kernel, capacity, local),
        out_shape=(sds((seqs, length, width), BF16), sds((seqs, length, width), BF16)),
        grid_spec=pltpu.PrefetchScalarGridSpec(
            num_scalar_prefetch=1,
            grid=(seqs,),
            in_specs=[pl.BlockSpec((1, 16, length), seq)] * local + [rows] * (2 * local),
            out_specs=(pl.BlockSpec((1, length, width), seq), pl.BlockSpec((1, length, width), seq)),
        ),
        compiler_params=pltpu.CompilerParams(dimension_semantics=("arbitrary",), vmem_limit_bytes=60 << 20),
        cost_estimate=pl.CostEstimate(flops=3 * 10**9, bytes_accessed=4 * 10**7, transcendentals=0),
        name="combine",
    )(starts, *slots, *produced, *dx)


def shards(
    tokens, cotangent, gate_weights, expert_ids, seq_lengths, query_weight, key_weight, value_weight,
    output_weight, attn_gain, ffn_gain, query_gain, key_gain, expert_in, expert_out,
):
    ep = lax.axis_size("ep")
    me = lax.axis_index("ep")
    _, rows, _ = tokens.shape
    length = rows * ep
    top = gate_weights.shape[2]
    local = expert_in.shape[0]
    experts = local * ep
    capacity = -(-(length * top * 9 // (8 * experts)) // 16) * 16

    gains = jnp.concatenate([attn_gain, ffn_gain]).astype(F32).reshape(-1, 128)
    few = [query_gain.astype(F32), key_gain.astype(F32), seq_lengths.astype(F32)]
    few = jnp.stack([jnp.pad(v, (0, 128 - v.shape[0])) for v in few])
    packet = jnp.concatenate([gains, few], axis=0)
    packet = jnp.pad(packet, ((0, -packet.shape[0] % 8), (0, 0)))
    share = gains.shape[0] // 2

    full, weights, routed, gains, small_in = front(
        tokens, cotangent, expert_ids.transpose(0, 2, 1), gate_weights.transpose(0, 2, 1),
        query_weight, key_weight, value_weight, packet,
    )
    cot_full = lax.all_gather(routed, "ep", axis=1, tiled=True)

    half = HEAD_DIM // 2
    frequency = ROPE_BASE ** (-(np.arange(half, dtype=np.float32) * np.float32(2.0 / HEAD_DIM)))
    angles = np.arange(length, dtype=np.float32)[:, None] * frequency.astype(np.float32)[None, :]
    cos = jnp.asarray(np.concatenate([np.cos(angles)] * 2, axis=-1), F32)
    sin = jnp.asarray(np.concatenate([-np.sin(angles), np.sin(angles)], axis=-1), F32)

    normed, pre, low, ctx, part = attend(full, weights, output_weight, gains, small_in, cos, sin)
    middle, mixed = mix(part, tokens, small_in, gains)

    number = (me * local).astype(jnp.int32)[None]
    slots0, slots1, starts, act0, dgu0, x_all, dy_all, out_grad0 = expert_first(
        number, mixed, cot_full, small_in, expert_in, expert_out, capacity, top
    )

    def over_rep(value):
        return lax.psum_scatter(value, "rep", scatter_dimension=0, tiled=True)

    out0 = over_rep(out_grad0)
    in_grad0 = first_in_grad(starts, x_all, dgu0)
    in0 = over_rep(in_grad0)
    x_all, _ = lax.optimization_barrier((x_all, in_grad0))
    act1, dgu1, out_grad1, in_grad1 = expert_second(starts, x_all, dy_all, expert_in, expert_out)
    in1 = over_rep(in_grad1)
    out1 = over_rep(out_grad1)
    produced0, dx0 = expert_tail(0, starts, act0, dgu0, expert_in, expert_out)
    produced1, dx1 = expert_tail(1, starts, act1, dgu1, expert_in, expert_out)
    out_part, grad_part = combine(starts, (slots0, slots1), (produced0, produced1), (dx0, dx1), capacity)

    mgrad, ffn_back, agrad = back(grad_part, middle, cotangent, small_in, gains)
    npart, wgrad, wograd, qk_back = attend_back(
        agrad, normed, pre, low, ctx, weights, output_weight, small_in, cos, sin
    )

    def widen(into, value, j):
        return lax.dynamic_update_slice(into, value.astype(F32)[None], (j, 0, 0))

    in_all = widen(jnp.zeros((local,) + in0.shape, F32), in0, 0)
    out_all = widen(jnp.zeros((local,) + out0.shape, F32), out0, 0)
    npart, in_all, out_all = lax.optimization_barrier((npart, in_all, out_all))
    sums, small, result, token_grad = finish(
        wgrad, wograd, npart, out_part, tokens, middle, mgrad, gains, ffn_back, qk_back
    )

    def head_share(vector):
        return lax.dynamic_slice_in_dim(vector, me * (HEAD_DIM // ep), HEAD_DIM // ep)

    return (
        result,
        token_grad,
        sums[1].astype(F32),
        sums[2].astype(F32),
        sums[3].astype(F32),
        sums[0].astype(F32),
        small[:share].reshape(-1),
        small[share : 2 * share].reshape(-1),
        head_share(small[2 * share]),
        head_share(small[2 * share + 1]),
        widen(in_all, in1, 1),
        widen(out_all, out1, 1),
    )


def solution(mesh):
    seq = P("rep", "ep", None)
    row, gain, expert = P("ep", None), P("ep"), P("ep", None, None)
    split = P("ep", "rep", None)

    return jax.shard_map(
        shards,
        mesh=mesh,
        in_specs=(seq, seq, seq, seq, P(("rep", "ep")), row, row, row, row, gain, gain, gain, gain, expert, expert),
        out_specs=(seq, seq, row, row, row, row, gain, gain, gain, gain, split, split),
        check_vma=False,
    )
```

```python
import functools

import jax
import jax.numpy as jnp
import numpy as np
from jax import lax
from jax.experimental import pallas as pl
from jax.experimental.pallas import tpu as pltpu
from jax.sharding import PartitionSpec as P

HEAD_DIM = 128
EPS = 1e-06
ROPE_BASE = 50000.0
MESH = pl.DeviceIdType.MESH
F32 = jnp.float32
BF16 = jnp.bfloat16


def sds(shape, dtype):
    return jax.ShapeDtypeStruct(shape, dtype)


VM = pl.BlockSpec(memory_space=pltpu.VMEM)
AN = pl.BlockSpec(memory_space=pl.ANY)


def inverse_rms(v):
    return lax.rsqrt(jnp.mean(v * v, axis=-1, keepdims=True) + EPS)


def rms_back(v, r, ug):
    return r * ug - v * (r * r * r * jnp.mean(ug * v, axis=-1, keepdims=True))


def mix_rows(total, tok, living, gain):
    middle = tok.astype(F32) + living * total
    mixed = middle * inverse_rms(middle) * gain
    return middle, mixed.astype(BF16)


def ffn_back_rows(mixed_grad, middle, cot, living, gain):
    r = inverse_rms(middle)
    middle_grad = cot.astype(F32) + rms_back(middle, r, mixed_grad * gain)
    return middle_grad, (living * middle_grad).astype(BF16), mixed_grad * middle * r


def attn_back_rows(normed_grad, tok, middle_grad, gain):
    v = tok.astype(F32)
    r = inverse_rms(v)
    return (middle_grad + rms_back(v, r, normed_grad * gain)).astype(BF16), normed_grad * v * r


def seq_len(small, s):
    lane = lax.broadcasted_iota(jnp.int32, (1, 128), 1)
    return jnp.sum(jnp.where(lane == s, small[2:3, :], 0.0), axis=1, keepdims=True)


def live_rows(small, s, me, rows):
    place = (lax.broadcasted_iota(jnp.int32, (rows, 1), 0) + me * rows).astype(F32)
    return jnp.where(place < seq_len(small, s), 1.0, 0.0)


class Place:
    def __init__(self):
        me = lax.axis_index("ep")
        core, x, y = lax.rem(me, 2), lax.rem(me // 2, 2), me // 4
        self.rep = lax.axis_index("rep")
        self.me = me
        self.sb = me + 1 - 2 * core
        self.dx = 2 - 4 * x
        self.dy = 4 - 8 * y
        self.xn = me + self.dx
        self.yn = me + self.dy
        self.dg = me + self.dx + self.dy

    def push(self, src, dst, send, recv, dev):
        return pltpu.make_async_remote_copy(
            src_ref=src, dst_ref=dst, send_sem=send, recv_sem=recv, device_id=(self.rep, dev), device_id_type=MESH
        )

    def peers(self):
        sb, dx, dy = self.sb, self.dx, self.dy
        return (self.xn, self.yn, self.dg, sb, sb + dx, sb + dy, sb + dx + dy)

    def greet(self, peers):
        barrier = pltpu.get_barrier_semaphore()
        for peer in peers:
            pl.semaphore_signal(barrier, inc=1, device_id=(self.rep, peer), device_id_type=MESH)
        pl.semaphore_wait(barrier, len(peers))


class Gather:
    sems = 3

    def __init__(self, at, own, full, ssem, rsem, lsem):
        self.at, self.own, self.full, self.ssem, self.rsem, self.lsem = at, own, full, ssem, rsem, lsem
        self.rows = own.shape[1]

    @staticmethod
    def scratch(seqs):
        return [pltpu.SemaphoreType.DMA((7, seqs)), pltpu.SemaphoreType.DMA((8, seqs)), pltpu.SemaphoreType.DMA((seqs,))]

    def block(self, s, dev):
        return self.full.at[s, pl.ds(pl.multiple_of(dev * self.rows, self.rows), self.rows)]

    def copy(self, s, dev, kind, slot, to, src=None):
        block = self.block(s, dev)
        return self.at.push(block if src is None else src, block, self.ssem.at[kind, s], self.rsem.at[slot, s], to)

    def start(self, s):
        at, own = self.at, self.own.at[s]
        self.copy(s, at.me, 0, 2, at.xn, own).start()
        self.copy(s, at.me, 1, 4, at.yn, own).start()
        self.copy(s, at.me, 2, 1, at.sb, own).start()
        pltpu.make_async_copy(own, self.block(s, at.me), self.lsem.at[s]).start()

    def relay(self, s, by_y):
        at = self.at
        self.copy(s, at.xn, 0, 2, at.xn).wait_recv()
        if by_y:
            self.copy(s, at.xn, 3, 6, at.yn).start()
        self.copy(s, at.xn, 4, 3, at.sb).start()
        self.copy(s, at.yn, 1, 4, at.yn).wait_recv()
        if not by_y:
            self.copy(s, at.yn, 3, 6, at.xn).start()
        self.copy(s, at.yn, 5, 5, at.sb).start()

    def relay_far(self, s):
        at = self.at
        self.copy(s, at.dg, 3, 6, at.yn).wait_recv()
        self.copy(s, at.dg, 6, 7, at.sb).start()

    def finish(self, s):
        at = self.at
        for dev, slot in ((at.sb, 1), (at.sb + at.dx, 3), (at.sb + at.dy, 5), (at.sb + at.dx + at.dy, 7)):
            self.copy(s, dev, 0, slot, at.sb).wait_recv()
        for kind in range(7):
            self.copy(s, at.me, kind, 0, at.sb).wait_send()
        pltpu.make_async_copy(self.own.at[s], self.block(s, at.me), self.lsem.at[s]).wait()


def gather_tail(gather, low, high):
    def relay(i, _):
        gather.relay(low + 2 * i, True)
        gather.relay(low + 2 * i + 1, False)
        return 0

    lax.fori_loop(0, (high - low) // 2, relay, 0)
    each(high, gather.relay_far, low=low)
    each(high, gather.finish, low=low)


class Reduce:
    def __init__(self, at, part, held, mine, x1, y1, x2, y2, ms, hs, hr, d1s, d1r, d2s, d2r):
        self.at, self.part, self.held, self.mine = at, part, held, mine
        self.x1, self.y1, self.x2, self.y2 = x1, y1, x2, y2
        self.ms, self.hs, self.hr, self.d1s, self.d1r, self.d2s, self.d2r = ms, hs, hr, d1s, d1r, d2s, d2r
        self.half = part.shape[2] // 2

    @staticmethod
    def scratch(part):
        s, _, t, d = part.shape
        dma = pltpu.SemaphoreType.DMA
        return [
            pltpu.VMEM((s, 4, t, d), BF16),
            pltpu.VMEM((s, 4, t, d), BF16),
            pltpu.VMEM((s, t // 2, d), BF16),
            pltpu.VMEM((s, t // 2, d), BF16),
            pltpu.VMEM((s, t, d), BF16),
            pltpu.VMEM((s, t, d), BF16),
            dma((4, s)),
            dma((4, s)),
            dma((4, s)),
            dma((2, s)),
            dma((2, s)),
            dma((2, s)),
            dma((2, s)),
        ]

    sems = 13

    def core_copy(self, s, k):
        at = self.at
        dest = (at.sb, at.sb + at.dx, at.sb + at.dy, at.sb + at.dx + at.dy)[k]
        return at.push(self.part.at[s, dest], self.held.at[s, k], self.hs.at[k, s], self.hr.at[k, s], at.sb)

    def load(self, s, k):
        at = self.at
        dest = (at.me, at.xn, at.yn, at.dg)[k]
        return pltpu.make_async_copy(self.part.at[s, dest], self.mine.at[s, k], self.ms.at[k, s])

    def first(self, s, k):
        at, h = self.at, self.half
        src = self.held.at[s, 3, pl.ds(k * h, h)]
        return at.push(src, (self.x1, self.y1)[k].at[s], self.d1s.at[k, s], self.d1r.at[k, s], (at.xn, at.yn)[k])

    def second(self, s, k):
        at = self.at
        src = self.held.at[s, 1 + k]
        return at.push(src, (self.x2, self.y2)[k].at[s], self.d2s.at[k, s], self.d2r.at[k, s], (at.xn, at.yn)[k])

    def start(self, s):
        for k in (3, 1, 2, 0):
            self.core_copy(s, k).start()
            self.load(s, k).start()

    def hop1(self, s):
        self.core_copy(s, 3).wait_recv()
        self.load(s, 3).wait()
        self.held[s, 3] = (self.held[s, 3].astype(F32) + self.mine[s, 3].astype(F32)).astype(BF16)
        self.first(s, 0).start()
        self.first(s, 1).start()

    def hop2(self, s):
        h = self.half
        for k, extra, rows, rest in (
            (0, self.y1, pl.ds(h, h), pl.ds(0, h)),
            (1, self.x1, pl.ds(0, h), pl.ds(h, h)),
        ):
            self.core_copy(s, 1 + k).wait_recv()
            self.load(s, 1 + k).wait()
            self.first(s, 1 - k).wait_recv()
            held, mine = self.held.at[s, 1 + k], self.mine.at[s, 1 + k]
            held[rows] = (held[rows].astype(F32) + mine[rows].astype(F32) + extra[s].astype(F32)).astype(BF16)
            held[rest] = (held[rest].astype(F32) + mine[rest].astype(F32)).astype(BF16)
            self.second(s, k).start()

    def total(self, s):
        self.core_copy(s, 0).wait_recv()
        self.load(s, 0).wait()
        self.second(s, 0).wait_recv()
        self.second(s, 1).wait_recv()
        return (
            self.mine[s, 0].astype(F32)
            + self.held[s, 0].astype(F32)
            + self.x2[s].astype(F32)
            + self.y2[s].astype(F32)
        )

    def finish(self, s):
        for k in range(4):
            self.core_copy(s, k).wait_send()
        for k in range(2):
            self.first(s, k).wait_send()
            self.second(s, k).wait_send()


def each(n, *steps, low=0):
    def run(s, _):
        for step in steps:
            step(s)
        return 0

    lax.fori_loop(low, n, run, 0)


COMM = dict(has_side_effects=True, vmem_limit_bytes=60 << 20)


def front_kernel(
    tok, cot, ids, gates, wq, wk, wv, pk, full, weights, cot_full, gains, small,
    packets, own, gsend, grecv, glocal, csend, crecv, clocal,
    wsend, wrecv, psend, precv, rsend, rrecv, lsend, lrecv, local,
):
    at = Place()
    z = at.rep
    gather = Gather(at, own, full, gsend, grecv, glocal)
    cot_gather = Gather(at, cot, cot_full, csend, crecv, clocal)
    seqs, _, width = tok.shape
    top = ids.shape[1]
    block, cols = wq.shape[0], weights.shape[2]
    quarter = block // 4
    peers = at.peers()
    barrier = pltpu.get_barrier_semaphore()
    line = [lax.rem(z + k, 4) for k in range(1, 4)]
    for dev in line:
        pl.semaphore_signal(barrier, inc=1, device_id=(dev, at.me), device_id_type=MESH)
    for dev in peers:
        pl.semaphore_signal(barrier, inc=1, device_id=(z, dev), device_id_type=MESH)
    pl.semaphore_wait(barrier, 10)

    def packet_copy(m, dev):
        return at.push(pk, packets.at[at.me], psend.at[m], precv.at[m], dev)

    def weight_copy(m, j, dev):
        theirs = pl.ds(pl.multiple_of(dev * cols, cols), cols)
        src = (wq, wk, wv)[j].at[pl.ds(pl.multiple_of(z * quarter, quarter), quarter), theirs]
        dst = weights.at[j, pl.ds(pl.multiple_of(at.me * block + z * quarter, quarter), quarter)]
        return at.push(src, dst, wsend.at[m, j], wrecv.at[m, j], dev)

    def weight_landed(m, j, dev):
        dst = weights.at[j, pl.ds(pl.multiple_of(dev * block + z * quarter, quarter), quarter)]
        return at.push(dst, dst, wsend.at[m, j], wrecv.at[m, j], dev)

    def walk(m, q, right):
        part = weights.at[:, pl.ds(pl.multiple_of(peers[m] * block + q * quarter, quarter), quarter)]
        send, recv, dev = (rsend, rrecv, z + 1) if right else (lsend, lrecv, z - 1)
        return pltpu.make_async_remote_copy(
            src_ref=part, dst_ref=part, send_sem=send.at[m, q], recv_sem=recv.at[m, q],
            device_id=(dev, at.me), device_id_type=MESH,
        )

    for m, dev in enumerate(peers):
        packet_copy(m, dev).start()
        for j in range(3):
            weight_copy(m, j, dev).start()

    place = lax.broadcasted_iota(jnp.int32, (top, 128), 0)
    lane = lax.broadcasted_iota(jnp.int32, (top, 128), 1)
    first = jnp.where(lane == place, 1.0, 0.0).astype(BF16)
    second = jnp.where(lane == place + top, 1.0, 0.0).astype(BF16)

    def join(s):
        own[s, :, 0:width] = tok[s]
        table = dot(ids[s].astype(F32).astype(BF16), first, 0, 0) + dot(gates[s], second, 0, 0)
        own[s, :, width : width + 128] = table.astype(BF16)

    each(seqs, join)
    each(seqs, gather.start)
    own_cols = pl.ds(pl.multiple_of(at.me * cols, cols), cols)
    mine = pl.ds(pl.multiple_of(at.me * block, block), block)
    own_weights = [
        pltpu.make_async_copy(w.at[:, own_cols], weights.at[j, mine], local.at[j]) for j, w in enumerate((wq, wk, wv))
    ]
    for copy in own_weights:
        copy.start()
    early = seqs // 2
    each(early, cot_gather.start)

    for m, dev in enumerate(peers):
        for j in range(3):
            weight_landed(m, j, dev).wait_recv()

        @pl.when(z < 3)
        def _():
            walk(m, z, True).start()

        @pl.when(z > 0)
        def _():
            walk(m, z, False).start()

    def pass_on(d):
        @pl.when(z - d >= 0)
        def _():
            for m in range(7):
                walk(m, z - d, True).wait_recv()

                @pl.when(z < 3)
                def _():
                    walk(m, z - d, True).start()

        @pl.when(z + d <= 3)
        def _():
            for m in range(7):
                walk(m, z + d, False).wait_recv()

                @pl.when(z > 0)
                def _():
                    walk(m, z + d, False).start()

    def relay(i, _):
        gather.relay(2 * i, True)
        gather.relay(2 * i + 1, False)
        return 0

    def cot_relay(i, _):
        cot_gather.relay(2 * i, True)
        cot_gather.relay(2 * i + 1, False)
        return 0

    pairs = seqs // 2
    lax.fori_loop(0, pairs // 2, relay, 0)
    pass_on(1)
    lax.fori_loop(pairs // 2, pairs, relay, 0)
    pass_on(2)
    lax.fori_loop(0, early // 2, cot_relay, 0)
    each(seqs, gather.relay_far)
    each(early, cot_gather.relay_far)
    for m, dev in enumerate(peers):
        packet_copy(m, dev).wait_recv()
    packets[at.me] = pk[...]
    devices = packets.shape[0]
    share = width // (128 * devices)
    heads = HEAD_DIM // devices
    gains[...] = jnp.zeros_like(gains)
    small[...] = jnp.zeros_like(small)
    for o in range(devices):
        for k in range(share):
            lanes = pl.ds((o * share + k) * 128, 128)
            gains[0:1, lanes] = packets[o, k : k + 1]
            gains[1:2, lanes] = packets[o, share + k : share + k + 1]
        base = 2 * share
        small[0:1] += pltpu.roll(packets[o, base : base + 1], o * heads, 1)
        small[1:2] += pltpu.roll(packets[o, base + 1 : base + 2], o * heads, 1)
        small[2:3] += pltpu.roll(packets[o, base + 2 : base + 3], o, 1)
    each(seqs, gather.finish)
    each(early, cot_gather.finish)
    pass_on(3)

    def sent(q, going, right):
        @pl.when(going)
        def _():
            for m in range(7):
                walk(m, q, right).wait_send()

    for q in range(4):
        sent(q, jnp.logical_and(q <= z, z < 3), True)
        sent(q, jnp.logical_and(q >= z, z > 0), False)
    for m, dev in enumerate(peers):
        packet_copy(m, dev).wait_send()
        for j in range(3):
            weight_copy(m, j, dev).wait_send()
    for copy in own_weights:
        copy.wait()


def front(tokens, cotangent, ids, gates, wq, wk, wv, packet):
    seqs, rows, width = tokens.shape
    ep = lax.axis_size("ep")
    cols = wq.shape[1] // ep
    top = ids.shape[1]
    if ep != 8 or lax.axis_size("rep") != 4:
        routes = jnp.concatenate([ids.astype(BF16), gates], axis=1).transpose(0, 2, 1)
        routes = jnp.pad(routes, ((0, 0), (0, 0), (0, 128 - 2 * top)))
        full = lax.all_gather(jnp.concatenate([tokens, routes], axis=-1), "ep", axis=1, tiled=True)
        weights = [lax.all_to_all(w, "ep", split_axis=1, concat_axis=0, tiled=True) for w in (wq, wk, wv)]
        packets = lax.all_gather(packet, "ep", axis=0)
        share, heads = width // (128 * ep), HEAD_DIM // ep
        gains = jnp.stack([packets[:, :share].reshape(width), packets[:, share : 2 * share].reshape(width)])
        lens = jnp.pad(packets[:, 2 * share + 2, 0], (0, 128 - ep))
        few = [packets[:, 2 * share + k, :heads].reshape(HEAD_DIM) for k in range(2)] + [lens]
        return (
            full, jnp.stack(weights), lax.all_gather(cotangent, "ep", axis=1, tiled=True),
            jnp.pad(gains, ((0, 6), (0, 0))), jnp.pad(jnp.stack(few), ((0, 5), (0, 0))),
        )
    dma = pltpu.SemaphoreType.DMA
    return pl.pallas_call(
        front_kernel,
        out_shape=(
            sds((seqs, rows * ep, width + 128), BF16),
            sds((3, wq.shape[0] * ep, cols), BF16),
            sds((seqs, rows * ep, width), BF16),
            sds((8, width), F32),
            sds((8, 128), F32),
        ),
        in_specs=[VM] * 8,
        out_specs=(AN, AN, AN, VM, VM),
        scratch_shapes=[pltpu.VMEM((ep,) + packet.shape, F32), pltpu.VMEM((seqs, rows, width + 128), BF16)]
        + Gather.scratch(seqs)
        + Gather.scratch(seqs)
        + [dma((7, 3)), dma((7, 3)), dma((7,)), dma((7,))]
        + [dma((7, 4))] * 4
        + [dma((3,))],
        compiler_params=pltpu.CompilerParams(collective_id=1, **COMM),
        name="front",
    )(tokens, cotangent, ids, gates, wq, wk, wv, packet)


def plain_living(small, seqs, rows):
    place = (jnp.arange(rows) + lax.axis_index("ep") * rows).astype(F32)
    return (place[None] < small[2, :seqs, None]).astype(F32)[..., None]


def mix(part, tokens, small, gains):
    seqs, rows, _ = tokens.shape
    total = lax.psum_scatter(part, "ep", scatter_dimension=1, tiled=True).astype(F32)
    middle, mixed = mix_rows(total, tokens, plain_living(small, seqs, rows), gains[1])
    return middle, lax.all_gather(mixed, "ep", axis=1, tiled=True)


def back_kernel(gpart, middle, cot, small, gains, mgrad, ggrad, full, own, *scratch):
    at = Place()
    seqs = cot.shape[0]
    n = Reduce.sems
    rg = Reduce(at, gpart, *scratch[:n])
    gather = Gather(at, own, full, *scratch[n:])
    at.greet((at.xn, at.yn, at.sb))
    each(seqs, rg.start)
    each(seqs, rg.hop1)
    each(seqs, rg.hop2)
    ggrad[...] = jnp.zeros_like(ggrad)

    def rows(s):
        living = live_rows(small, s, at.me, cot.shape[1])
        mg, ag, back = ffn_back_rows(rg.total(s), middle[s], cot[s], living, gains[1:2])
        mgrad[s] = mg
        own[s] = ag
        ggrad[...] += jnp.sum(back, axis=0, keepdims=True)
        gather.start(s)

    each(seqs, rows)
    gather_tail(gather, 0, seqs)
    each(seqs, rg.finish)


def back(gpart, middle, cot, small, gains):
    seqs, rows, width = cot.shape
    ep = lax.axis_size("ep")
    if ep != 8:
        mixed_grad = lax.psum_scatter(gpart, "ep", scatter_dimension=1, tiled=True).astype(F32)
        mg, ag, backs = ffn_back_rows(mixed_grad, middle, cot, plain_living(small, seqs, rows), gains[1])
        full = lax.all_gather(ag, "ep", axis=1, tiled=True)
        return mg, jnp.sum(backs, axis=(0, 1))[None], full
    gpart = gpart.reshape(seqs, ep, rows, width)
    return pl.pallas_call(
        back_kernel,
        out_shape=(
            sds(cot.shape, F32),
            sds((1, width), F32),
            sds((seqs, rows * ep, width), BF16),
        ),
        in_specs=[AN] + [VM] * 4,
        out_specs=(VM, VM, AN),
        scratch_shapes=[pltpu.VMEM(cot.shape, BF16)] + Reduce.scratch(gpart) + Gather.scratch(seqs),
        compiler_params=pltpu.CompilerParams(collective_id=3, **COMM),
        name="back",
    )(gpart, middle, cot, small, gains)


def finish_kernel(
    wgrad, wograd, npart, opart, tok, middle, mgrad, gains, others,
    out, small_out, result, tgrad,
    own, held, met, ggrad, parcel, landed, spare,
    wsend, wrecv, local, gsend, grecv, os, or_, ps, pr, qs, qr, fs, fr, ss, sr, *scratch,
):
    at = Place()
    z, me = at.rep, at.me
    n = Reduce.sems
    normed_sum = Reduce(at, npart, *scratch[:n])
    result_sum = Reduce(at, opart, *scratch[n:])
    seqs = tok.shape[0]
    parts, pieces = own.shape[:2]
    chunks = parts * pieces
    width = wgrad.shape[3]
    peers = at.peers()
    barrier = pltpu.get_barrier_semaphore()
    line = [lax.rem(z + k, 4) for k in range(1, 4)]
    for dev in line:
        pl.semaphore_signal(barrier, inc=1, device_id=(dev, me), device_id_type=MESH)
    for dev in peers:
        pl.semaphore_signal(barrier, inc=1, device_id=(z, dev), device_id_type=MESH)
    pl.semaphore_wait(barrier, 10)
    inner = jnp.logical_and(z > 0, z < 3)
    outer_end, partner, outer = 1 + z // 3, 3 - z, 3 * (z - 1)
    cols = pl.ds(pl.multiple_of(me * width, width), width)

    def column_copy(m, j, dev):
        rows = pl.ds(pl.multiple_of(dev * pieces, pieces), pieces)
        return at.push(wgrad.at[j, rows], own.at[1 + j, :, :, cols], wsend.at[m, j], wrecv.at[m, j], dev)

    mine_rows = pl.ds(pl.multiple_of(me * pieces, pieces), pieces)
    locals_ = [pltpu.make_async_copy(wgrad.at[j, mine_rows], own.at[1 + j, :, :, cols], local.at[j]) for j in range(3)]
    locals_.append(pltpu.make_async_copy(wograd, own.at[0], local.at[3]))
    for copy in locals_:
        copy.start()
    for j in range(3):
        for m, dev in enumerate(peers):
            column_copy(m, j, dev).start()
    each(seqs, normed_sum.start)
    each(seqs, result_sum.start)
    ggrad[...] = jnp.zeros_like(ggrad)

    def piece(ref, c):
        return ref.at[c // pieces, lax.rem(c, pieces)]

    def line_push(src, dst, send, recv, dev):
        return pltpu.make_async_remote_copy(
            src_ref=src, dst_ref=dst, send_sem=send, recv_sem=recv, device_id=(dev, me), device_id_type=MESH
        )

    def inward(c):
        return line_push(piece(own, c), piece(held, c), os.at[c], or_.at[c], outer_end)

    def across(c):
        return line_push(piece(held, c), met.at[c // 2], ps.at[c], pr.at[c], partner)

    def share(c):
        return line_push(piece(out, c), piece(out, c), qs.at[c], qr.at[c], partner)

    def outward(c):
        return line_push(piece(out, c), piece(out, c), fs.at[c], fr.at[c], outer)

    def mine(c):
        return 1 + lax.rem(c, 2) == z

    def ready(part):
        for j in range(parts):

            @pl.when(part == j)
            def _():
                locals_[(3, 0, 1, 2)[j]].wait()
                if j > 0:
                    for m, dev in enumerate(peers):
                        column_copy(m, j - 1, dev).wait_recv()

    def step(c):
        @pl.when(lax.rem(c, pieces) == 0)
        def _():
            ready(c // pieces)

        @pl.when(jnp.logical_not(inner))
        def _():
            inward(c).start()

        @pl.when(inner)
        def _():
            inward(c).wait_recv()
            here = piece(held, c)
            here[...] = (here[...].astype(F32) + piece(own, c)[...].astype(F32)).astype(BF16)

            @pl.when(jnp.logical_not(mine(c)))
            def _():
                across(c).start()

    def settle(c):
        @pl.when(jnp.logical_and(inner, mine(c)))
        def _():
            across(c).wait_recv()
            piece(out, c)[...] = (piece(held, c)[...].astype(F32) + met[c // 2].astype(F32)).astype(BF16)
            share(c).start()
            outward(c).start()

    def forward(c):
        @pl.when(jnp.logical_and(inner, jnp.logical_not(mine(c))))
        def _():
            share(c).wait_recv()
            outward(c).start()

    def token_rows(s):
        tg, back = attn_back_rows(normed_sum.total(s), tok[s], mgrad[s], gains[0:1])
        tgrad[s] = tg
        ggrad[...] += jnp.sum(back, axis=0, keepdims=True)

    def out_rows(s):
        result[s] = (middle[s] + result_sum.total(s)).astype(BF16)

    jobs = (
        (step, 0, chunks), (settle, 1, chunks), (forward, 2, chunks),
        (normed_sum.hop1, 2, seqs), (normed_sum.hop2, 6, seqs), (token_rows, 10, seqs),
        (result_sum.hop1, 6, seqs), (result_sum.hop2, 10, seqs), (out_rows, 14, seqs),
    )

    def tick(i, _):
        for job, lag, count in jobs:

            @pl.when(jnp.logical_and(i >= lag, i < lag + count))
            def _():
                job(i - lag)

        return 0

    lax.fori_loop(0, max(lag + count for _, lag, count in jobs), tick, 0)

    parcel[...] = jnp.zeros_like(parcel)
    devices = parcel.shape[0]
    rows_of = ggrad.shape[1] // (128 * devices)
    for dev in range(devices):
        for k in range(rows_of):
            lanes = pl.ds((dev * rows_of + k) * 128, 128)
            parcel[dev, k : k + 1] = ggrad[:, lanes]
            parcel[dev, rows_of + k : rows_of + k + 1] = others[0:1, lanes]
        parcel[dev, 2 * rows_of : 2 * rows_of + 2] = others[1:3, 0:128]

    def parcel_copy(m, dev):
        return at.push(parcel.at[dev], landed.at[m], gsend.at[m], grecv.at[m], dev)

    for m, dev in enumerate(peers):
        parcel_copy(m, dev).start()
    total = parcel[me]
    for m, dev in enumerate(peers):
        parcel_copy(m, dev).wait_recv()
        total = total + landed[m]
    spare[0] = total

    def small_copy(k):
        return line_push(spare.at[0], spare.at[1 + k], ss.at[k], sr.at[k], line[k])

    for k in range(3):
        small_copy(k).start()

    @pl.when(jnp.logical_not(inner))
    def _():
        each(chunks, lambda c: outward(c).wait_recv())
        each(chunks, lambda c: inward(c).wait_send())

    @pl.when(inner)
    def _():
        def sent(c):
            outward(c).wait_send()

            @pl.when(mine(c))
            def _():
                share(c).wait_send()

            @pl.when(jnp.logical_not(mine(c)))
            def _():
                across(c).wait_send()

        each(chunks, sent)

    each(seqs, normed_sum.finish, result_sum.finish)
    for m, dev in enumerate(peers):
        parcel_copy(m, dev).wait_send()
        for j in range(3):
            column_copy(m, j, dev).wait_send()
    total = spare[0]
    for k in range(3):
        small_copy(k).wait()
        total = total + spare[1 + k]
    small_out[...] = total


def finish(wgrad, wograd, npart, opart, tokens, middle, mgrad, gains, ffn_back, qk_back):
    seqs, rows, width = tokens.shape
    ep = lax.axis_size("ep")
    if ep != 8 or lax.axis_size("rep") != 4:
        normed_grad = lax.psum_scatter(npart, "ep", scatter_dimension=1, tiled=True).astype(F32)
        moe = lax.psum_scatter(opart, "ep", scatter_dimension=1, tiled=True).astype(F32)
        tg, backs = attn_back_rows(normed_grad, tokens, mgrad, gains[0])
        wrows = lax.all_to_all(wgrad, "ep", split_axis=1, concat_axis=2, tiled=True)
        share = width // ep
        small = jnp.concatenate([jnp.sum(backs, axis=(0, 1)), ffn_back[0], qk_back[0], qk_back[1]])
        small = lax.psum(small, ("ep", "rep"))
        mine = lax.axis_index("ep") * share
        cut = [lax.dynamic_slice_in_dim(small, k * width + mine, share).reshape(-1, 128) for k in range(2)]
        small = jnp.concatenate(cut + [small[2 * width :].reshape(2, HEAD_DIM)], axis=0)
        big = lax.psum(jnp.concatenate([wograd[None], wrows], axis=0), "rep")
        return big, jnp.pad(small, ((0, 8 - small.shape[0]), (0, 0))), (middle + moe).astype(BF16), tg
    others = jnp.concatenate([ffn_back, jnp.pad(qk_back[:2], ((0, 0), (0, width - HEAD_DIM)))], axis=0)
    npart, opart = (p.reshape(seqs, ep, rows, width) for p in (npart, opart))
    pieces = 4
    block = wograd.shape[0] // pieces
    wgrad = wgrad.reshape(3, wgrad.shape[1] // block, block, wgrad.shape[2])
    wograd = wograd.reshape(pieces, block, width)
    whole = (4, pieces, block, width)
    dma = pltpu.SemaphoreType.DMA
    chunks = 4 * pieces
    out, small, result, tgrad = pl.pallas_call(
        finish_kernel,
        out_shape=(sds(whole, BF16), sds((8, 128), F32), sds(tokens.shape, BF16), sds(tokens.shape, BF16)),
        in_specs=[VM, VM, AN, AN] + [VM] * 5,
        out_specs=(VM, VM, VM, VM),
        scratch_shapes=[
            pltpu.VMEM(whole, BF16),
            pltpu.VMEM(whole, BF16),
            pltpu.VMEM((chunks // 2, block, width), BF16),
            pltpu.VMEM((1, width), F32),
            pltpu.VMEM((ep, 8, 128), F32),
            pltpu.VMEM((7, 8, 128), F32),
            pltpu.VMEM((4, 8, 128), F32),
        ]
        + [dma((7, 3)), dma((7, 3)), dma((4,)), dma((7,)), dma((7,))]
        + [dma((chunks,))] * 8
        + [dma((3,))] * 2
        + 2 * Reduce.scratch(npart),
        compiler_params=pltpu.CompilerParams(collective_id=4, has_side_effects=True, vmem_limit_bytes=61 << 20),
        name="finish",
    )(wgrad, wograd, npart, opart, tokens, middle, mgrad, gains, others)
    return out.reshape(4, pieces * block, width), small, result, tgrad


def dot(a, b, ca, cb):
    return lax.dot_general(a, b, (((ca,), (cb,)), ((), ())), preferred_element_type=F32)


def rope(v, cos, sin_turn):
    return v * cos + pltpu.roll(v, HEAD_DIM // 2, 1) * sin_turn


def probabilities(q, k, length):
    scores = dot(q, k, 1, 1) * HEAD_DIM**-0.5
    column = lax.broadcasted_iota(jnp.int32, (1, scores.shape[1]), 1).astype(F32)
    scores = jnp.where(column < length, scores, -1e9)
    p = jnp.exp(scores - jnp.max(scores, axis=-1, keepdims=True))
    return p * (1.0 / jnp.sum(p, axis=-1, keepdims=True))


def packed_slots(number, table, length_live, top):
    tab = table.astype(F32)
    length = tab.shape[0]
    lane = lax.broadcasted_iota(jnp.int32, tab.shape, 1)
    row = lax.broadcasted_iota(jnp.int32, (length, 1), 0).astype(F32)
    chosen = jnp.logical_and(jnp.logical_and(tab == number, lane < top), row < length_live)
    gates = jnp.where(chosen, pltpu.roll(tab, 128 - top, 1), 0.0).astype(BF16)
    chosen = jnp.where(chosen, 1.0, 0.0).astype(BF16)
    ones = jnp.ones((8, 128), BF16)
    hit = dot(ones, chosen, 1, 1)
    weight = dot(ones, gates, 1, 1)
    earlier = lax.broadcasted_iota(jnp.int32, (length, length), 0)
    later = lax.broadcasted_iota(jnp.int32, (length, length), 1)
    rank = dot(hit.astype(BF16), jnp.where(earlier < later, 1.0, 0.0).astype(BF16), 1, 0)
    return jnp.where(hit > 0.5, rank, -1.0), weight, jnp.sum(hit[0:1], axis=1, keepdims=True)


def attend_rows(top, number, s, block, w, wo, gains, small, cos, sin, normed, pre, low, ctx, part, slots, starts):
    width = normed.shape[1]
    length = seq_len(small, s)
    v = block[:, 0:width].astype(F32)
    x = (v * inverse_rms(v) * gains[0:1]).astype(BF16)
    normed[...] = x
    q_pre, k_pre = dot(x, w[0], 1, 0), dot(x, w[1], 1, 0)
    value = dot(x, w[2], 1, 0).astype(BF16)
    pre[0], pre[1] = q_pre, k_pre
    low[2] = value
    for h in range(q_pre.shape[1] // HEAD_DIM):
        cols = slice(h * HEAD_DIM, (h + 1) * HEAD_DIM)
        rot = []
        for i, (u, g) in enumerate(((q_pre[:, cols], small[0:1]), (k_pre[:, cols], small[1:2]))):
            rot.append(rope(u * inverse_rms(u) * g, cos[...], sin[...]).astype(BF16))
            low[i, :, cols] = rot[i]
        attention = probabilities(rot[0], rot[1], length).astype(BF16)
        ctx[:, cols] = dot(attention, value[:, cols], 1, 0).astype(BF16)
    part[...] = dot(ctx[...], wo[...], 1, 0).astype(BF16).reshape(part.shape)
    table = block[:, width : width + 128]
    lane = lax.broadcasted_iota(jnp.int32, (1, 128), 1)
    for j, ref in enumerate(slots):
        slot, weight, count = packed_slots(number + j, table, length, top)
        ref[0:8] = slot
        ref[8:16] = weight
        row = starts[j : j + 1]
        after = jnp.sum(jnp.where(lane == s, row, 0.0), axis=1, keepdims=True) + 16.0 * jnp.floor((count + 15.0) * 0.0625)
        starts[j : j + 1] = jnp.where(lane == s + 1, after, row)


def attend_kernel(top, number, full, w, wo, gains, small, cos, sin, normed, pre, low, ctx, part, slots0, slots1, starts):
    s = pl.program_id(0)

    @pl.when(s == 0)
    def _():
        starts[...] = jnp.zeros_like(starts)

    attend_rows(
        top, number[0].astype(F32), s, full.at[0], w, wo, gains, small, cos, sin,
        normed.at[0], pre.at[:, 0], low.at[:, 0], ctx.at[0], part.at[0], (slots0.at[0], slots1.at[0]), starts,
    )


def attend(top, number, full, weights, wo, gains, small, cos, sin):
    seqs, length, wide = full.shape
    width = wide - 128
    cols = weights.shape[2]
    row = lambda i, *_: (i, 0, 0)
    row2 = lambda i, *_: (0, i, 0, 0)
    two = lambda i, *_: (0, 0)
    slot = pl.BlockSpec((1, 16, length), row)
    return pl.pallas_call(
        functools.partial(attend_kernel, top),
        out_shape=(
            sds((seqs, length, width), BF16),
            sds((2, seqs, length, cols), F32),
            sds((3, seqs, length, cols), BF16),
            sds((seqs, length, cols), BF16),
            sds((seqs, length, width), BF16),
            sds((seqs, 16, length), F32),
            sds((seqs, 16, length), F32),
            sds((8, 128), F32),
        ),
        grid_spec=pltpu.PrefetchScalarGridSpec(
            num_scalar_prefetch=1,
            grid=(seqs,),
            in_specs=[
                pl.BlockSpec((1, length, wide), row),
                pl.BlockSpec(weights.shape, lambda i, *_: (0, 0, 0)),
                pl.BlockSpec(wo.shape, two),
                pl.BlockSpec((8, width), two),
                pl.BlockSpec((8, 128), two),
                pl.BlockSpec((length, HEAD_DIM), two),
                pl.BlockSpec((length, HEAD_DIM), two),
            ],
            out_specs=(
                pl.BlockSpec((1, length, width), row),
                pl.BlockSpec((2, 1, length, cols), row2),
                pl.BlockSpec((3, 1, length, cols), row2),
                pl.BlockSpec((1, length, cols), row),
                pl.BlockSpec((1, length, width), row),
                slot,
                slot,
                pl.BlockSpec((8, 128), two),
            ),
        ),
        compiler_params=pltpu.CompilerParams(dimension_semantics=("arbitrary",), vmem_limit_bytes=60 << 20),
        cost_estimate=pl.CostEstimate(flops=10**10, bytes_accessed=4 * 10**7, transcendentals=10**6),
        name="attend",
    )(number, full, weights, wo, gains, small, cos, sin)


def attend_mix_kernel(
    top, local, full, w, wo, gains, small, cos, sin, tok, cot, _cot_early,
    normed, pre, low, ctx, middle, mixed, cot_full, slots0, slots1, starts,
    own, blocks, nbuf, pbuf, lbuf, cbuf, part, begins, tsem, ssem, *scratch,
):
    at = Place()
    seqs = tok.shape[0]
    n = Reduce.sems
    reduce = Reduce(at, part, *scratch[:n])
    gather = Gather(at, own, mixed, *scratch[n : n + 3])
    cot_gather = Gather(at, cot, cot_full, *scratch[n + 3 :])
    number = (at.me * local).astype(F32)
    early = seqs // 2
    at.greet((at.xn, at.yn, at.sb))
    each(seqs, cot_gather.start, low=early)
    begins[...] = jnp.zeros_like(begins)

    def load(s):
        return pltpu.make_async_copy(full.at[s], blocks.at[lax.rem(s, 2)], tsem.at[lax.rem(s, 2)])

    def stores(s):
        k = lax.rem(s, 2)
        pairs = ((nbuf.at[k], normed.at[s]), (pbuf.at[k], pre.at[:, s]), (lbuf.at[k], low.at[:, s]), (cbuf.at[k], ctx.at[s]))
        return [pltpu.make_async_copy(src, dst, ssem.at[i, k]) for i, (src, dst) in enumerate(pairs)]

    load(0).start()

    def sequence(s):
        k = lax.rem(s, 2)
        load(s).wait()

        @pl.when(s + 1 < seqs)
        def _():
            load(s + 1).start()

        @pl.when(s >= 2)
        def _():
            for copy in stores(s - 2):
                copy.wait()

        attend_rows(
            top, number, s, blocks.at[k], w, wo, gains, small, cos, sin,
            nbuf.at[k], pbuf.at[k], lbuf.at[k], cbuf.at[k], part.at[s], (slots0.at[s], slots1.at[s]), begins,
        )
        for copy in stores(s):
            copy.start()
        reduce.start(s)

    def rows(s):
        living = live_rows(small, s, at.me, tok.shape[1])
        mid, out = mix_rows(reduce.total(s), tok[s], living, gains[1:2])
        middle[s] = mid
        own[s] = out
        gather.start(s)

    def cot_pair(p):
        @pl.when(lax.rem(p, 2) == 0)
        def _():
            cot_gather.relay(early + p, True)
            cot_gather.relay(early + p + 1, False)

    jobs = (
        (sequence, 0, seqs), (reduce.hop1, 1, seqs), (cot_pair, 3, early), (reduce.hop2, 3, seqs),
        (lambda s: cot_gather.relay_far(early + s), 7, early), (rows, 5, seqs),
    )

    def tick(i, _):
        for job, lag, count in jobs:

            @pl.when(jnp.logical_and(i >= lag, i < lag + count))
            def _():
                job(i - lag)

        return 0

    lax.fori_loop(0, max(lag + count for _, lag, count in jobs), tick, 0)
    starts[...] = begins[...].astype(jnp.int32)
    each(seqs, cot_gather.finish, low=early)
    gather_tail(gather, 0, seqs)
    for s in (seqs - 2, seqs - 1):
        for copy in stores(s):
            copy.wait()
    each(seqs, reduce.finish)


def attend_mix(top, local, full, weights, wo, gains, small, cos, sin, tokens, cotangent, cot_early):
    seqs, rows, width = tokens.shape
    length = full.shape[1]
    cols = weights.shape[2]
    part = sds((seqs, 8, rows, width), BF16)
    dma = pltpu.SemaphoreType.DMA
    return pl.pallas_call(
        functools.partial(attend_mix_kernel, top, local),
        out_shape=(
            sds((seqs, length, width), BF16),
            sds((2, seqs, length, cols), F32),
            sds((3, seqs, length, cols), BF16),
            sds((seqs, length, cols), BF16),
            sds(tokens.shape, F32),
            sds((seqs, length, width), BF16),
            sds((seqs, length, width), BF16),
            sds((seqs, 16, length), F32),
            sds((seqs, 16, length), F32),
            sds((8, 128), jnp.int32),
        ),
        in_specs=[AN] + [VM] * 8 + [AN],
        out_specs=(AN, AN, AN, AN, VM, AN, AN, VM, VM, VM),
        input_output_aliases={9: 6},
        scratch_shapes=[
            pltpu.VMEM(tokens.shape, BF16),
            pltpu.VMEM((2,) + full.shape[1:], BF16),
            pltpu.VMEM((2, length, width), BF16),
            pltpu.VMEM((2, 2, length, cols), F32),
            pltpu.VMEM((2, 3, length, cols), BF16),
            pltpu.VMEM((2, length, cols), BF16),
            pltpu.VMEM(part.shape, BF16),
            pltpu.VMEM((8, 128), F32),
            dma((2,)),
            dma((4, 2)),
        ]
        + Reduce.scratch(part)
        + Gather.scratch(seqs)
        + Gather.scratch(seqs),
        compiler_params=pltpu.CompilerParams(collective_id=2, **COMM),
        name="attend_mix",
    )(full, weights, wo, gains, small, cos, sin, tokens, cotangent, cot_early)


def attend_back_kernel(
    agrad, normed, pre, low, ctx, w, wo, small, cos, sin, part, wgrad, wograd, gains, wacc, woacc
):
    s = pl.program_id(0)
    length = seq_len(small, s)

    @pl.when(s == 0)
    def _():
        wacc[...] = jnp.zeros_like(wacc)
        woacc[...] = jnp.zeros_like(woacc)
        gains[...] = jnp.zeros_like(gains)

    ag = agrad[0]
    woacc[...] += dot(ctx[0], ag, 0, 0)
    cg_all = dot(ag, wo[...], 1, 1).astype(BF16)
    scale = HEAD_DIM**-0.5
    half = HEAD_DIM // 2
    grads = ([], [], [])
    for h in range(cg_all.shape[1] // HEAD_DIM):
        cols = slice(h * HEAD_DIM, (h + 1) * HEAD_DIM)
        q, k, value, cg = low[0, 0, :, cols], low[1, 0, :, cols], low[2, 0, :, cols], cg_all[:, cols]
        attention = probabilities(q, k, length)
        grads[2].append(dot(attention.astype(BF16), cg, 0, 0).astype(BF16))
        pg = dot(cg, value, 1, 1)
        sg = (attention * (pg - jnp.sum(attention * pg, axis=-1, keepdims=True))).astype(BF16)
        for i, (rot_grad, g) in enumerate(((dot(sg, k, 1, 0), small[0:1]), (dot(sg, q, 0, 0), small[1:2]))):
            wgt = rot_grad * scale
            u = wgt * cos[...] + pltpu.roll(wgt * sin[...], half, 1)
            v = pre[i, 0, :, cols]
            r = inverse_rms(v)
            grads[i].append(rms_back(v, r, u * g).astype(BF16))
            gains[i : i + 1] += jnp.sum(u * v * r, axis=0, keepdims=True)
    total = None
    for i in range(3):
        g = grads[i][0] if len(grads[i]) == 1 else jnp.concatenate(grads[i], axis=1)
        wacc[i] += dot(normed[0], g, 0, 0)
        piece = dot(g, w[i], 1, 1)
        total = piece if total is None else total + piece
    part[0] = total.astype(BF16)

    @pl.when(s == pl.num_programs(0) - 1)
    def _():
        wgrad[...] = wacc[...].astype(BF16)
        wograd[...] = woacc[...].astype(BF16)


def attend_back(agrad, normed, pre, low, ctx, weights, wo, small, cos, sin):
    seqs, length, width = agrad.shape
    cols = weights.shape[2]
    row = lambda i, *_: (i, 0, 0)
    row2 = lambda i, *_: (0, i, 0, 0)
    two = lambda i, *_: (0, 0)
    three = lambda i, *_: (0, 0, 0)
    return pl.pallas_call(
        attend_back_kernel,
        out_shape=(
            sds(agrad.shape, BF16),
            sds(weights.shape, BF16),
            sds(wo.shape, BF16),
            sds((8, HEAD_DIM), F32),
        ),
        grid_spec=pltpu.PrefetchScalarGridSpec(
            num_scalar_prefetch=0,
            grid=(seqs,),
            in_specs=[
                pl.BlockSpec((1, length, width), row),
                pl.BlockSpec((1, length, width), row),
                pl.BlockSpec((2, 1, length, cols), row2),
                pl.BlockSpec((3, 1, length, cols), row2),
                pl.BlockSpec((1, length, cols), row),
                pl.BlockSpec(weights.shape, three),
                pl.BlockSpec(wo.shape, two),
                pl.BlockSpec((8, 128), two),
                pl.BlockSpec((length, HEAD_DIM), two),
                pl.BlockSpec((length, HEAD_DIM), two),
            ],
            out_specs=(
                pl.BlockSpec((1, length, width), row),
                pl.BlockSpec(weights.shape, three),
                pl.BlockSpec(wo.shape, two),
                pl.BlockSpec((8, HEAD_DIM), two),
            ),
            scratch_shapes=[pltpu.VMEM(weights.shape, F32), pltpu.VMEM(wo.shape, F32)],
        ),
        compiler_params=pltpu.CompilerParams(dimension_semantics=("arbitrary",), vmem_limit_bytes=60 << 20),
        cost_estimate=pl.CostEstimate(flops=2 * 10**10, bytes_accessed=4 * 10**7, transcendentals=10**6),
        name="attend_back",
    )(agrad, normed, pre, low, ctx, weights, wo, small, cos, sin)


BLOCK = 256


def pack_rows(seqs, capacity):
    return -(-seqs * capacity // BLOCK) * BLOCK


def forward_blocks(blocks, x, dy, wi, wo, acts, dgus):
    hidden = wo.shape[0]
    part = min(hidden, 512)

    def forward(b, _):
        rows = pl.ds(pl.multiple_of(b * BLOCK, BLOCK), BLOCK)
        for h in range(hidden // part):
            gcols, ucols = pl.ds(h * part, part), pl.ds(hidden + h * part, part)
            gate = dot(x[rows], wi[:, gcols], 1, 0)
            up = dot(x[rows], wi[:, ucols], 1, 0)
            dact = dot(dy[rows], wo[gcols], 1, 1)
            sig = 1.0 / (1.0 + jnp.exp(-gate))
            silu = gate * sig
            acts[rows, gcols] = (silu * up).astype(BF16)
            dgus[rows, gcols] = (dact * up * sig * (1.0 + gate * (1.0 - sig))).astype(BF16)
            dgus[rows, ucols] = (dact * silu).astype(BF16)
        return 0

    lax.fori_loop(0, blocks, forward, 0)


def gradient_tiles(blocks, left, right, result, acc, stage, ssem, busy):
    tr, tc = acc.shape
    down, across = result.shape[0] // tr, result.shape[1] // tc

    def tile(t, _):
        rt, ct = t // across, lax.rem(t, across)
        left_cols = pl.ds(pl.multiple_of(rt * tr, tr), tr)
        right_cols = pl.ds(pl.multiple_of(ct * tc, tc), tc)

        def step(b, _):
            rows = pl.ds(pl.multiple_of(b * BLOCK, BLOCK), BLOCK)
            piece = dot(left[rows, left_cols], right[rows, right_cols], 0, 0)

            @pl.when(b == 0)
            def _():
                acc[...] = piece

            @pl.when(b > 0)
            def _():
                acc[...] += piece

            return 0

        @pl.when(blocks == 0)
        def _():
            acc[...] = jnp.zeros_like(acc)

        lax.fori_loop(0, blocks, step, 0)
        k = lax.rem(t, 2)
        out = pltpu.make_async_copy(stage.at[k], result.at[left_cols, right_cols], ssem.at[k])

        @pl.when(jnp.logical_or(t >= 2, busy))
        def _():
            out.wait()

        stage[k] = acc[...].astype(BF16)
        out.start()
        return 0

    lax.fori_loop(0, down * across, tile, 0)


def drain_tiles(result, acc, stage, ssem):
    tr, tc = acc.shape
    for k in range(2):
        pltpu.make_async_copy(stage.at[k], result.at[pl.ds(0, tr), pl.ds(0, tc)], ssem.at[k]).wait()


def first_kernel(
    capacity, starts, mixed, cot, slots0, slots1, w_in, w_out,
    act, dgu, x_all, dy_all, out_grad,
    x, dy, wi, wo, acts, dgus, acc, stage, wsem, ssem, rsem,
):
    step = pl.program_id(0)
    steps = pl.num_programs(0)
    together = mixed.shape[0]
    seqs = steps * together
    width = mixed.shape[2]
    loads = [pltpu.make_async_copy(w_in.at[0], wi, wsem.at[0]), pltpu.make_async_copy(w_out.at[0], wo, wsem.at[1])]

    @pl.when(step == 0)
    def _():
        for copy in loads:
            copy.start()

    packed = []
    for k in range(together):
        spread, gate_spread = [], []
        for slots in (slots0, slots1):
            column = lax.broadcasted_iota(jnp.int32, (capacity, slots.shape[2]), 0).astype(F32)
            place = column == slots[k, 0:1]
            spread.append(jnp.where(place, 1.0, 0.0).astype(BF16))
            gate_spread.append(jnp.where(place, slots[k, 8:9], 0.0).astype(BF16))
        packed.append(
            (
                dot(jnp.concatenate(spread, axis=0), mixed[k], 1, 0).astype(BF16),
                dot(jnp.concatenate(gate_spread, axis=0), cot[k], 1, 0).astype(BF16),
            )
        )
    for k, (x_rows, dy_rows) in enumerate(packed):
        s = step * together + k
        for j in range(2):
            start = pl.multiple_of(starts[j, s], 16)
            x[j, pl.ds(start, capacity)] = x_rows[j * capacity : (j + 1) * capacity]
            dy[j, pl.ds(start, capacity)] = dy_rows[j * capacity : (j + 1) * capacity]

    @pl.when(step == steps - 1)
    def _():
        for j in range(2):
            past = (starts[j, seqs - 1] + capacity) // 16
            end = (starts[j, seqs] + BLOCK - 1) // BLOCK * (BLOCK // 16)

            def clear(i, _):
                rows = pl.ds(pl.multiple_of(i * 16, 16), 16)
                x[j, rows] = jnp.zeros((16, width), BF16)
                dy[j, rows] = jnp.zeros((16, width), BF16)
                return 0

            lax.fori_loop(past, end, clear, 0)
        saves = [pltpu.make_async_copy(x, x_all, rsem.at[0]), pltpu.make_async_copy(dy.at[1], dy_all, rsem.at[1])]
        for copy in saves:
            copy.start()
        blocks = (starts[0, seqs] + BLOCK - 1) // BLOCK
        for copy in loads:
            copy.wait()
        forward_blocks(blocks, x.at[0], dy.at[0], wi, wo, acts, dgus)
        saves += [pltpu.make_async_copy(acts, act, rsem.at[2]), pltpu.make_async_copy(dgus, dgu, rsem.at[3])]
        for copy in saves[2:]:
            copy.start()
        gradient_tiles(blocks, acts, dy.at[0], out_grad, acc, stage, ssem, False)
        drain_tiles(out_grad, acc, stage, ssem)
        for copy in saves:
            copy.wait()


def expert_first(starts, mixed, cot, slots, w_in, w_out, capacity):
    seqs, length, width = mixed.shape
    hidden = w_out.shape[1]
    rows = pack_rows(seqs, capacity)
    dma = pltpu.SemaphoreType.DMA
    seq = lambda i, *_: (i, 0, 0)
    together = 2
    slot_spec = pl.BlockSpec((together, 16, length), seq)
    return pl.pallas_call(
        functools.partial(first_kernel, capacity),
        out_shape=(
            sds((rows, hidden), BF16),
            sds((rows, 2 * hidden), BF16),
            sds((2, rows, width), BF16),
            sds((rows, width), BF16),
            sds((hidden, width), BF16),
        ),
        grid_spec=pltpu.PrefetchScalarGridSpec(
            num_scalar_prefetch=1,
            grid=(seqs // together,),
            in_specs=[
                pl.BlockSpec((together, length, width), seq),
                pl.BlockSpec((together, length, width), seq),
                slot_spec,
                slot_spec,
                AN,
                AN,
            ],
            out_specs=(AN, AN, AN, AN, AN),
            scratch_shapes=[
                pltpu.VMEM((2, rows, width), BF16),
                pltpu.VMEM((2, rows, width), BF16),
                pltpu.VMEM(w_in.shape[1:], BF16),
                pltpu.VMEM(w_out.shape[1:], BF16),
                pltpu.VMEM((rows, hidden), BF16),
                pltpu.VMEM((rows, 2 * hidden), BF16),
                pltpu.VMEM((256, 1024), F32),
                pltpu.VMEM((2, 256, 1024), BF16),
                dma((2,)),
                dma((2,)),
                dma((4,)),
            ],
        ),
        compiler_params=pltpu.CompilerParams(dimension_semantics=("arbitrary",), vmem_limit_bytes=63 << 20),
        cost_estimate=pl.CostEstimate(flops=2 * 10**10, bytes_accessed=6 * 10**7, transcendentals=10**6),
        name="expert_first",
    )(starts, mixed, cot, *slots, w_in, w_out)


def in_grad_kernel(seqs, starts, x_all, dgu, in_grad, x, dgus, acc, stage, lsem, ssem):
    blocks = (starts[0, seqs] + BLOCK - 1) // BLOCK

    def load(b):
        rows = pl.ds(pl.multiple_of(b * BLOCK, BLOCK), BLOCK)
        return (
            pltpu.make_async_copy(x_all.at[0, rows], x.at[rows], lsem.at[0, b]),
            pltpu.make_async_copy(dgu.at[rows], dgus.at[rows], lsem.at[1, b]),
        )

    def run(b, action):
        for copy in load(b):
            getattr(copy, action)()
        return 0

    lax.fori_loop(0, blocks, lambda b, _: run(b, "start"), 0)
    lax.fori_loop(0, blocks, lambda b, _: run(b, "wait"), 0)
    gradient_tiles(blocks, x, dgus, in_grad, acc, stage, ssem, False)
    drain_tiles(in_grad, acc, stage, ssem)


def first_in_grad(seqs, starts, x_all, dgu):
    rows, width = x_all.shape[1:]
    dma = pltpu.SemaphoreType.DMA
    return pl.pallas_call(
        functools.partial(in_grad_kernel, seqs),
        out_shape=sds((width, dgu.shape[1]), BF16),
        grid_spec=pltpu.PrefetchScalarGridSpec(
            num_scalar_prefetch=1,
            grid=(1,),
            in_specs=[AN, AN],
            out_specs=AN,
            scratch_shapes=[
                pltpu.VMEM((rows, width), BF16),
                pltpu.VMEM(dgu.shape, BF16),
                pltpu.VMEM((512, 2048), F32),
                pltpu.VMEM((2, 512, 2048), BF16),
                dma((2, rows // BLOCK)),
                dma((2,)),
            ],
        ),
        compiler_params=pltpu.CompilerParams(dimension_semantics=("arbitrary",), vmem_limit_bytes=60 << 20),
        cost_estimate=pl.CostEstimate(flops=10**10, bytes_accessed=2 * 10**7, transcendentals=0),
        name="first_in_grad",
    )(starts, x_all, dgu)


def second_kernel(
    seqs, starts, x_all, dy_all, w_in, w_out, act, dgu, out_grad, in_grad,
    x, dy, wi, wo, acts, dgus, acc, stage, wsem, lsem, ssem, rsem,
):
    blocks = (starts[1, seqs] + BLOCK - 1) // BLOCK
    loads = [pltpu.make_async_copy(w_in.at[1], wi, wsem.at[0]), pltpu.make_async_copy(w_out.at[1], wo, wsem.at[1])]

    def load(b, action):
        rows = pl.ds(pl.multiple_of(b * BLOCK, BLOCK), BLOCK)
        for copy in (
            pltpu.make_async_copy(x_all.at[1, rows], x.at[rows], lsem.at[0, b]),
            pltpu.make_async_copy(dy_all.at[rows], dy.at[rows], lsem.at[1, b]),
        ):
            getattr(copy, action)()
        return 0

    for copy in loads:
        copy.start()
    lax.fori_loop(0, blocks, lambda b, _: load(b, "start"), 0)
    for copy in loads:
        copy.wait()
    lax.fori_loop(0, blocks, lambda b, _: load(b, "wait"), 0)
    forward_blocks(blocks, x, dy, wi, wo, acts, dgus)
    saves = [pltpu.make_async_copy(acts, act, rsem.at[0]), pltpu.make_async_copy(dgus, dgu, rsem.at[1])]
    for copy in saves:
        copy.start()
    gradient_tiles(blocks, x, dgus, in_grad, acc, stage, ssem, False)
    gradient_tiles(blocks, acts, dy, out_grad, acc, stage, ssem, True)
    drain_tiles(out_grad, acc, stage, ssem)
    for copy in saves:
        copy.wait()


def expert_second(seqs, starts, x_all, dy_all, w_in, w_out):
    rows, width = dy_all.shape
    hidden = w_out.shape[1]
    dma = pltpu.SemaphoreType.DMA
    return pl.pallas_call(
        functools.partial(second_kernel, seqs),
        out_shape=(
            sds((rows, hidden), BF16),
            sds((rows, 2 * hidden), BF16),
            sds((hidden, width), BF16),
            sds((width, 2 * hidden), BF16),
        ),
        grid_spec=pltpu.PrefetchScalarGridSpec(
            num_scalar_prefetch=1,
            grid=(1,),
            in_specs=[AN] * 4,
            out_specs=(AN, AN, AN, AN),
            scratch_shapes=[
                pltpu.VMEM((rows, width), BF16),
                pltpu.VMEM((rows, width), BF16),
                pltpu.VMEM(w_in.shape[1:], BF16),
                pltpu.VMEM(w_out.shape[1:], BF16),
                pltpu.VMEM((rows, hidden), BF16),
                pltpu.VMEM((rows, 2 * hidden), BF16),
                pltpu.VMEM((512, 2048), F32),
                pltpu.VMEM((2, 512, 2048), BF16),
                dma((2,)),
                dma((2, rows // BLOCK)),
                dma((2,)),
                dma((2,)),
            ],
        ),
        compiler_params=pltpu.CompilerParams(dimension_semantics=("arbitrary",), vmem_limit_bytes=60 << 20),
        cost_estimate=pl.CostEstimate(flops=25 * 10**9, bytes_accessed=6 * 10**7, transcendentals=10**6),
        name="expert_second",
    )(starts, x_all, dy_all, w_in, w_out)


def tail_kernel(j, seqs, starts, act, dgu, w_in, w_out, produced, dx):
    @pl.when(pl.program_id(0) * BLOCK < starts[j, seqs])
    def _():
        produced[...] = dot(act[...], w_out[...], 1, 0).astype(BF16)
        dx[...] = dot(dgu[...], w_in[...], 1, 1).astype(BF16)


def expert_tail(j, seqs, starts, act, dgu, w_in, w_out):
    rows, hidden = act.shape
    width = w_in.shape[1]
    block = lambda i, st: (jnp.maximum(jnp.minimum(i, (st[j, seqs] + BLOCK - 1) // BLOCK - 1), 0), 0)
    return pl.pallas_call(
        functools.partial(tail_kernel, j, seqs),
        out_shape=(sds((rows, width), BF16), sds((rows, width), BF16)),
        grid_spec=pltpu.PrefetchScalarGridSpec(
            num_scalar_prefetch=1,
            grid=(rows // BLOCK,),
            in_specs=[
                pl.BlockSpec((BLOCK, hidden), block),
                pl.BlockSpec((BLOCK, 2 * hidden), block),
                pl.BlockSpec((None,) + w_in.shape[1:], lambda i, *_: (j, 0, 0)),
                pl.BlockSpec((None,) + w_out.shape[1:], lambda i, *_: (j, 0, 0)),
            ],
            out_specs=(pl.BlockSpec((BLOCK, width), block), pl.BlockSpec((BLOCK, width), block)),
        ),
        compiler_params=pltpu.CompilerParams(dimension_semantics=("arbitrary",), vmem_limit_bytes=60 << 20),
        cost_estimate=pl.CostEstimate(flops=12 * 10**9, bytes_accessed=3 * 10**7, transcendentals=0),
        name="expert_tail",
    )(starts, act, dgu, w_in, w_out)


def combine_kernel(capacity, local, *refs):
    s = pl.program_id(0)
    starts = refs[0]
    slots = refs[1 : 1 + local]
    produced = refs[1 + local : 1 + 2 * local]
    dx = refs[1 + 2 * local : 1 + 3 * local]
    out_part, grad_part = refs[1 + 3 * local :]
    out_sum, grad_sum = None, None
    for j in range(local):
        length = slots[j].shape[2]
        column = lax.broadcasted_iota(jnp.int32, (capacity, length), 0).astype(F32)
        place = column == slots[j][0, 0:1]
        span = pl.ds(pl.multiple_of(starts[j, s], 16), capacity)
        held = lax.broadcasted_iota(jnp.int32, (capacity, 1), 0) < starts[j, s + 1] - starts[j, s]
        rows = jnp.where(held, produced[j][span], 0.0).astype(BF16)
        grads = jnp.where(held, dx[j][span], 0.0).astype(BF16)
        out = dot(jnp.where(place, slots[j][0, 8:9], 0.0).astype(BF16), rows, 0, 0)
        grad = dot(jnp.where(place, 1.0, 0.0).astype(BF16), grads, 0, 0)
        out_sum = out if out_sum is None else out_sum + out
        grad_sum = grad if grad_sum is None else grad_sum + grad
    out_part[0] = out_sum.astype(BF16)
    grad_part[0] = grad_sum.astype(BF16)


def combine(starts, slots, produced, dx, capacity):
    local = len(slots)
    seqs, _, length = slots[0].shape
    width = produced[0].shape[1]
    seq = lambda i, *_: (i, 0, 0)
    two = lambda i, *_: (0, 0)
    rows = pl.BlockSpec(produced[0].shape, two)
    return pl.pallas_call(
        functools.partial(combine_kernel, capacity, local),
        out_shape=(sds((seqs, length, width), BF16), sds((seqs, length, width), BF16)),
        grid_spec=pltpu.PrefetchScalarGridSpec(
            num_scalar_prefetch=1,
            grid=(seqs,),
            in_specs=[pl.BlockSpec((1, 16, length), seq)] * local + [rows] * (2 * local),
            out_specs=(pl.BlockSpec((1, length, width), seq), pl.BlockSpec((1, length, width), seq)),
        ),
        compiler_params=pltpu.CompilerParams(dimension_semantics=("arbitrary",), vmem_limit_bytes=60 << 20),
        cost_estimate=pl.CostEstimate(flops=3 * 10**9, bytes_accessed=4 * 10**7, transcendentals=0),
        name="combine",
    )(starts, *slots, *produced, *dx)


def shards(
    tokens, cotangent, gate_weights, expert_ids, seq_lengths, query_weight, key_weight, value_weight,
    output_weight, attn_gain, ffn_gain, query_gain, key_gain, expert_in, expert_out,
):
    ep = lax.axis_size("ep")
    me = lax.axis_index("ep")
    seqs, rows, _ = tokens.shape
    length = rows * ep
    top = gate_weights.shape[2]
    local = expert_in.shape[0]
    experts = local * ep
    capacity = -(-(length * top * 9 // (8 * experts)) // 16) * 16

    gains = jnp.concatenate([attn_gain, ffn_gain]).astype(F32).reshape(-1, 128)
    few = [query_gain.astype(F32), key_gain.astype(F32), seq_lengths.astype(F32)]
    few = jnp.stack([jnp.pad(v, (0, 128 - v.shape[0])) for v in few])
    packet = jnp.concatenate([gains, few], axis=0)
    packet = jnp.pad(packet, ((0, -packet.shape[0] % 8), (0, 0)))
    share = gains.shape[0] // 2

    full, weights, cot_full, gains, small_in = front(
        tokens, cotangent, expert_ids.transpose(0, 2, 1), gate_weights.transpose(0, 2, 1),
        query_weight, key_weight, value_weight, packet,
    )

    half = HEAD_DIM // 2
    frequency = ROPE_BASE ** (-(np.arange(half, dtype=np.float32) * np.float32(2.0 / HEAD_DIM)))
    angles = np.arange(length, dtype=np.float32)[:, None] * frequency.astype(np.float32)[None, :]
    cos = jnp.asarray(np.concatenate([np.cos(angles)] * 2, axis=-1), F32)
    sin = jnp.asarray(np.concatenate([-np.sin(angles), np.sin(angles)], axis=-1), F32)

    if ep == 8 and lax.axis_size("rep") == 4:
        normed, pre, low, ctx, middle, mixed, cot_full, slots0, slots1, starts = attend_mix(
            top, local, full, weights, output_weight, gains, small_in, cos, sin, tokens, cotangent, cot_full
        )
    else:
        number = (me * local).astype(jnp.int32)[None]
        normed, pre, low, ctx, part, slots0, slots1, starts = attend(
            top, number, full, weights, output_weight, gains, small_in, cos, sin
        )
        starts = starts.astype(jnp.int32)
        middle, mixed = mix(part, tokens, small_in, gains)

    act0, dgu0, x_all, dy_all, out_grad0 = expert_first(
        starts, mixed, cot_full, (slots0, slots1), expert_in, expert_out, capacity
    )

    def over_rep(value):
        return lax.psum_scatter(value, "rep", scatter_dimension=0, tiled=True)

    out0 = over_rep(out_grad0)
    in_grad0 = first_in_grad(seqs, starts, x_all, dgu0)
    in0 = over_rep(in_grad0)
    x_all, _ = lax.optimization_barrier((x_all, in_grad0))
    act1, dgu1, out_grad1, in_grad1 = expert_second(seqs, starts, x_all, dy_all, expert_in, expert_out)
    in1 = over_rep(in_grad1)
    out1 = over_rep(out_grad1)
    produced0, dx0 = expert_tail(0, seqs, starts, act0, dgu0, expert_in, expert_out)
    produced1, dx1 = expert_tail(1, seqs, starts, act1, dgu1, expert_in, expert_out)
    out_part, grad_part = combine(starts, (slots0, slots1), (produced0, produced1), (dx0, dx1), capacity)

    mgrad, ffn_back, agrad = back(grad_part, middle, cotangent, small_in, gains)
    npart, wgrad, wograd, qk_back = attend_back(
        agrad, normed, pre, low, ctx, weights, output_weight, small_in, cos, sin
    )

    def widen(into, value, j):
        return lax.dynamic_update_slice(into, value.astype(F32)[None], (j, 0, 0))

    in_all = widen(jnp.zeros((local,) + in0.shape, F32), in0, 0)
    out_all = widen(jnp.zeros((local,) + out0.shape, F32), out0, 0)
    npart, in_all, out_all = lax.optimization_barrier((npart, in_all, out_all))
    sums, small, result, token_grad = finish(
        wgrad, wograd, npart, out_part, tokens, middle, mgrad, gains, ffn_back, qk_back
    )

    def head_share(vector):
        return lax.dynamic_slice_in_dim(vector, me * (HEAD_DIM // ep), HEAD_DIM // ep)

    return (
        result,
        token_grad,
        sums[1].astype(F32),
        sums[2].astype(F32),
        sums[3].astype(F32),
        sums[0].astype(F32),
        small[:share].reshape(-1),
        small[share : 2 * share].reshape(-1),
        head_share(small[2 * share]),
        head_share(small[2 * share + 1]),
        widen(in_all, in1, 1),
        widen(out_all, out1, 1),
    )


def solution(mesh):
    seq = P("rep", "ep", None)
    row, gain, expert = P("ep", None), P("ep"), P("ep", None, None)
    split = P("ep", "rep", None)

    return jax.shard_map(
        shards,
        mesh=mesh,
        in_specs=(seq, seq, seq, seq, P(("rep", "ep")), row, row, row, row, gain, gain, gain, gain, expert, expert),
        out_specs=(seq, seq, row, row, row, row, gain, gain, gain, gain, split, split),
        check_vma=False,
    )
```

```python
import functools

import jax
import jax.numpy as jnp
import numpy as np
from jax import lax
from jax.experimental import pallas as pl
from jax.experimental.pallas import tpu as pltpu
from jax.sharding import PartitionSpec as P

HEAD_DIM = 128
EPS = 1e-06
ROPE_BASE = 50000.0
MESH = pl.DeviceIdType.MESH
F32 = jnp.float32
BF16 = jnp.bfloat16


def sds(shape, dtype):
    return jax.ShapeDtypeStruct(shape, dtype)


VM = pl.BlockSpec(memory_space=pltpu.VMEM)
AN = pl.BlockSpec(memory_space=pl.ANY)


def inverse_rms(v):
    return lax.rsqrt(jnp.mean(v * v, axis=-1, keepdims=True) + EPS)


def rms_back(v, r, ug):
    return r * ug - v * (r * r * r * jnp.mean(ug * v, axis=-1, keepdims=True))


def mix_rows(total, tok, living, gain):
    middle = tok.astype(F32) + living * total
    mixed = middle * inverse_rms(middle) * gain
    return middle, mixed.astype(BF16)


def ffn_back_rows(mixed_grad, middle, cot, living, gain):
    r = inverse_rms(middle)
    middle_grad = cot.astype(F32) + rms_back(middle, r, mixed_grad * gain)
    return middle_grad, (living * middle_grad).astype(BF16), mixed_grad * middle * r


def attn_back_rows(normed_grad, tok, middle_grad, gain):
    v = tok.astype(F32)
    r = inverse_rms(v)
    return (middle_grad + rms_back(v, r, normed_grad * gain)).astype(BF16), normed_grad * v * r


def seq_len(small, s):
    lane = lax.broadcasted_iota(jnp.int32, (1, 128), 1)
    return jnp.sum(jnp.where(lane == s, small[2:3, :], 0.0), axis=1, keepdims=True)


def live_rows(small, s, me, rows):
    place = (lax.broadcasted_iota(jnp.int32, (rows, 1), 0) + me * rows).astype(F32)
    return jnp.where(place < seq_len(small, s), 1.0, 0.0)


class Place:
    def __init__(self):
        me = lax.axis_index("ep")
        core, x, y = lax.rem(me, 2), lax.rem(me // 2, 2), me // 4
        self.rep = lax.axis_index("rep")
        self.me = me
        self.sb = me + 1 - 2 * core
        self.dx = 2 - 4 * x
        self.dy = 4 - 8 * y
        self.xn = me + self.dx
        self.yn = me + self.dy
        self.dg = me + self.dx + self.dy

    def push(self, src, dst, send, recv, dev):
        return pltpu.make_async_remote_copy(
            src_ref=src, dst_ref=dst, send_sem=send, recv_sem=recv, device_id=(self.rep, dev), device_id_type=MESH
        )

    def peers(self):
        sb, dx, dy = self.sb, self.dx, self.dy
        return (self.xn, self.yn, self.dg, sb, sb + dx, sb + dy, sb + dx + dy)

    def greet(self, peers):
        barrier = pltpu.get_barrier_semaphore()
        for peer in peers:
            pl.semaphore_signal(barrier, inc=1, device_id=(self.rep, peer), device_id_type=MESH)
        pl.semaphore_wait(barrier, len(peers))


class Gather:
    sems = 3

    def __init__(self, at, own, full, ssem, rsem, lsem):
        self.at, self.own, self.full, self.ssem, self.rsem, self.lsem = at, own, full, ssem, rsem, lsem
        self.rows = own.shape[1]

    @staticmethod
    def scratch(seqs):
        return [pltpu.SemaphoreType.DMA((7, seqs)), pltpu.SemaphoreType.DMA((8, seqs)), pltpu.SemaphoreType.DMA((seqs,))]

    def block(self, s, dev):
        return self.full.at[s, pl.ds(pl.multiple_of(dev * self.rows, self.rows), self.rows)]

    def copy(self, s, dev, kind, slot, to, src=None):
        block = self.block(s, dev)
        return self.at.push(block if src is None else src, block, self.ssem.at[kind, s], self.rsem.at[slot, s], to)

    def start(self, s):
        at, own = self.at, self.own.at[s]
        self.copy(s, at.me, 0, 2, at.xn, own).start()
        self.copy(s, at.me, 1, 4, at.yn, own).start()
        self.copy(s, at.me, 2, 1, at.sb, own).start()
        pltpu.make_async_copy(own, self.block(s, at.me), self.lsem.at[s]).start()

    def relay(self, s, by_y):
        at = self.at
        self.copy(s, at.xn, 0, 2, at.xn).wait_recv()
        if by_y:
            self.copy(s, at.xn, 3, 6, at.yn).start()
        self.copy(s, at.xn, 4, 3, at.sb).start()
        self.copy(s, at.yn, 1, 4, at.yn).wait_recv()
        if not by_y:
            self.copy(s, at.yn, 3, 6, at.xn).start()
        self.copy(s, at.yn, 5, 5, at.sb).start()

    def relay_far(self, s):
        at = self.at
        self.copy(s, at.dg, 3, 6, at.yn).wait_recv()
        self.copy(s, at.dg, 6, 7, at.sb).start()

    def finish(self, s):
        at = self.at
        for dev, slot in ((at.sb, 1), (at.sb + at.dx, 3), (at.sb + at.dy, 5), (at.sb + at.dx + at.dy, 7)):
            self.copy(s, dev, 0, slot, at.sb).wait_recv()
        for kind in range(7):
            self.copy(s, at.me, kind, 0, at.sb).wait_send()
        pltpu.make_async_copy(self.own.at[s], self.block(s, at.me), self.lsem.at[s]).wait()


def gather_tail(gather, low, high):
    def relay(i, _):
        gather.relay(low + 2 * i, True)
        gather.relay(low + 2 * i + 1, False)
        return 0

    lax.fori_loop(0, (high - low) // 2, relay, 0)
    each(high, gather.relay_far, low=low)
    each(high, gather.finish, low=low)


class Reduce:
    def __init__(self, at, part, held, mine, x1, y1, x2, y2, ms, hs, hr, d1s, d1r, d2s, d2r):
        self.at, self.part, self.held, self.mine = at, part, held, mine
        self.x1, self.y1, self.x2, self.y2 = x1, y1, x2, y2
        self.ms, self.hs, self.hr, self.d1s, self.d1r, self.d2s, self.d2r = ms, hs, hr, d1s, d1r, d2s, d2r
        self.half = part.shape[2] // 2

    @staticmethod
    def scratch(part):
        s, _, t, d = part.shape
        dma = pltpu.SemaphoreType.DMA
        return [
            pltpu.VMEM((s, 4, t, d), BF16),
            pltpu.VMEM((s, 4, t, d), BF16),
            pltpu.VMEM((s, t // 2, d), BF16),
            pltpu.VMEM((s, t // 2, d), BF16),
            pltpu.VMEM((s, t, d), BF16),
            pltpu.VMEM((s, t, d), BF16),
            dma((4, s)),
            dma((4, s)),
            dma((4, s)),
            dma((2, s)),
            dma((2, s)),
            dma((2, s)),
            dma((2, s)),
        ]

    sems = 13

    def core_copy(self, s, k):
        at = self.at
        dest = (at.sb, at.sb + at.dx, at.sb + at.dy, at.sb + at.dx + at.dy)[k]
        return at.push(self.part.at[s, dest], self.held.at[s, k], self.hs.at[k, s], self.hr.at[k, s], at.sb)

    def load(self, s, k):
        at = self.at
        dest = (at.me, at.xn, at.yn, at.dg)[k]
        return pltpu.make_async_copy(self.part.at[s, dest], self.mine.at[s, k], self.ms.at[k, s])

    def first(self, s, k):
        at, h = self.at, self.half
        src = self.held.at[s, 3, pl.ds(k * h, h)]
        return at.push(src, (self.x1, self.y1)[k].at[s], self.d1s.at[k, s], self.d1r.at[k, s], (at.xn, at.yn)[k])

    def second(self, s, k):
        at = self.at
        src = self.held.at[s, 1 + k]
        return at.push(src, (self.x2, self.y2)[k].at[s], self.d2s.at[k, s], self.d2r.at[k, s], (at.xn, at.yn)[k])

    def start(self, s):
        for k in (3, 1, 2, 0):
            self.core_copy(s, k).start()
            self.load(s, k).start()

    def hop1(self, s):
        self.core_copy(s, 3).wait_recv()
        self.load(s, 3).wait()
        self.held[s, 3] = (self.held[s, 3].astype(F32) + self.mine[s, 3].astype(F32)).astype(BF16)
        self.first(s, 0).start()
        self.first(s, 1).start()

    def hop2(self, s):
        h = self.half
        for k, extra, rows, rest in (
            (0, self.y1, pl.ds(h, h), pl.ds(0, h)),
            (1, self.x1, pl.ds(0, h), pl.ds(h, h)),
        ):
            self.core_copy(s, 1 + k).wait_recv()
            self.load(s, 1 + k).wait()
            self.first(s, 1 - k).wait_recv()
            held, mine = self.held.at[s, 1 + k], self.mine.at[s, 1 + k]
            held[rows] = (held[rows].astype(F32) + mine[rows].astype(F32) + extra[s].astype(F32)).astype(BF16)
            held[rest] = (held[rest].astype(F32) + mine[rest].astype(F32)).astype(BF16)
            self.second(s, k).start()

    def total(self, s):
        self.core_copy(s, 0).wait_recv()
        self.load(s, 0).wait()
        self.second(s, 0).wait_recv()
        self.second(s, 1).wait_recv()
        return (
            self.mine[s, 0].astype(F32)
            + self.held[s, 0].astype(F32)
            + self.x2[s].astype(F32)
            + self.y2[s].astype(F32)
        )

    def finish(self, s):
        for k in range(4):
            self.core_copy(s, k).wait_send()
        for k in range(2):
            self.first(s, k).wait_send()
            self.second(s, k).wait_send()


def each(n, *steps, low=0):
    def run(s, _):
        for step in steps:
            step(s)
        return 0

    lax.fori_loop(low, n, run, 0)


COMM = dict(has_side_effects=True, vmem_limit_bytes=60 << 20)


def front_kernel(
    tok, cot, ids, gates, wq, wk, wv, pk, full, weights, cot_full, gains, small,
    packets, own, gsend, grecv, glocal, csend, crecv, clocal,
    wsend, wrecv, psend, precv, rsend, rrecv, lsend, lrecv, local,
):
    at = Place()
    z = at.rep
    gather = Gather(at, own, full, gsend, grecv, glocal)
    cot_gather = Gather(at, cot, cot_full, csend, crecv, clocal)
    seqs, _, width = tok.shape
    top = ids.shape[1]
    block, cols = wq.shape[0], weights.shape[2]
    quarter = block // 4
    peers = at.peers()
    barrier = pltpu.get_barrier_semaphore()
    line = [lax.rem(z + k, 4) for k in range(1, 4)]
    for dev in line:
        pl.semaphore_signal(barrier, inc=1, device_id=(dev, at.me), device_id_type=MESH)
    for dev in peers:
        pl.semaphore_signal(barrier, inc=1, device_id=(z, dev), device_id_type=MESH)
    pl.semaphore_wait(barrier, 10)

    def packet_copy(m, dev):
        return at.push(pk, packets.at[at.me], psend.at[m], precv.at[m], dev)

    def weight_copy(m, j, dev):
        theirs = pl.ds(pl.multiple_of(dev * cols, cols), cols)
        src = (wq, wk, wv)[j].at[pl.ds(pl.multiple_of(z * quarter, quarter), quarter), theirs]
        dst = weights.at[j, pl.ds(pl.multiple_of(at.me * block + z * quarter, quarter), quarter)]
        return at.push(src, dst, wsend.at[m, j], wrecv.at[m, j], dev)

    def weight_landed(m, j, dev):
        dst = weights.at[j, pl.ds(pl.multiple_of(dev * block + z * quarter, quarter), quarter)]
        return at.push(dst, dst, wsend.at[m, j], wrecv.at[m, j], dev)

    def walk(m, q, right):
        part = weights.at[:, pl.ds(pl.multiple_of(peers[m] * block + q * quarter, quarter), quarter)]
        send, recv, dev = (rsend, rrecv, z + 1) if right else (lsend, lrecv, z - 1)
        return pltpu.make_async_remote_copy(
            src_ref=part, dst_ref=part, send_sem=send.at[m, q], recv_sem=recv.at[m, q],
            device_id=(dev, at.me), device_id_type=MESH,
        )

    for m, dev in enumerate(peers):
        packet_copy(m, dev).start()
        for j in range(3):
            weight_copy(m, j, dev).start()

    place = lax.broadcasted_iota(jnp.int32, (top, 128), 0)
    lane = lax.broadcasted_iota(jnp.int32, (top, 128), 1)
    first = jnp.where(lane == place, 1.0, 0.0).astype(BF16)
    second = jnp.where(lane == place + top, 1.0, 0.0).astype(BF16)

    def join(s):
        own[s, :, 0:width] = tok[s]
        table = dot(ids[s].astype(F32).astype(BF16), first, 0, 0) + dot(gates[s], second, 0, 0)
        own[s, :, width : width + 128] = table.astype(BF16)

    each(seqs, join)
    each(seqs, gather.start)
    own_cols = pl.ds(pl.multiple_of(at.me * cols, cols), cols)
    mine = pl.ds(pl.multiple_of(at.me * block, block), block)
    own_weights = [
        pltpu.make_async_copy(w.at[:, own_cols], weights.at[j, mine], local.at[j]) for j, w in enumerate((wq, wk, wv))
    ]
    for copy in own_weights:
        copy.start()
    early = seqs // 2
    each(early, cot_gather.start)

    for m, dev in enumerate(peers):
        for j in range(3):
            weight_landed(m, j, dev).wait_recv()

        @pl.when(z < 3)
        def _():
            walk(m, z, True).start()

        @pl.when(z > 0)
        def _():
            walk(m, z, False).start()

    def pass_on(d):
        @pl.when(z - d >= 0)
        def _():
            for m in range(7):
                walk(m, z - d, True).wait_recv()

                @pl.when(z < 3)
                def _():
                    walk(m, z - d, True).start()

        @pl.when(z + d <= 3)
        def _():
            for m in range(7):
                walk(m, z + d, False).wait_recv()

                @pl.when(z > 0)
                def _():
                    walk(m, z + d, False).start()

    def relay(i, _):
        gather.relay(2 * i, True)
        gather.relay(2 * i + 1, False)
        return 0

    def cot_relay(i, _):
        cot_gather.relay(2 * i, True)
        cot_gather.relay(2 * i + 1, False)
        return 0

    pairs = seqs // 2
    lax.fori_loop(0, pairs // 2, relay, 0)
    pass_on(1)
    lax.fori_loop(pairs // 2, pairs, relay, 0)
    pass_on(2)
    lax.fori_loop(0, early // 2, cot_relay, 0)
    each(seqs, gather.relay_far)
    each(early, cot_gather.relay_far)
    for m, dev in enumerate(peers):
        packet_copy(m, dev).wait_recv()
    packets[at.me] = pk[...]
    devices = packets.shape[0]
    share = width // (128 * devices)
    heads = HEAD_DIM // devices
    gains[...] = jnp.zeros_like(gains)
    small[...] = jnp.zeros_like(small)
    for o in range(devices):
        for k in range(share):
            lanes = pl.ds((o * share + k) * 128, 128)
            gains[0:1, lanes] = packets[o, k : k + 1]
            gains[1:2, lanes] = packets[o, share + k : share + k + 1]
        base = 2 * share
        small[0:1] += pltpu.roll(packets[o, base : base + 1], o * heads, 1)
        small[1:2] += pltpu.roll(packets[o, base + 1 : base + 2], o * heads, 1)
        small[2:3] += pltpu.roll(packets[o, base + 2 : base + 3], o, 1)
    each(seqs, gather.finish)
    each(early, cot_gather.finish)
    pass_on(3)

    def sent(q, going, right):
        @pl.when(going)
        def _():
            for m in range(7):
                walk(m, q, right).wait_send()

    for q in range(4):
        sent(q, jnp.logical_and(q <= z, z < 3), True)
        sent(q, jnp.logical_and(q >= z, z > 0), False)
    for m, dev in enumerate(peers):
        packet_copy(m, dev).wait_send()
        for j in range(3):
            weight_copy(m, j, dev).wait_send()
    for copy in own_weights:
        copy.wait()


def front(tokens, cotangent, ids, gates, wq, wk, wv, packet):
    seqs, rows, width = tokens.shape
    ep = lax.axis_size("ep")
    cols = wq.shape[1] // ep
    top = ids.shape[1]
    if ep != 8 or lax.axis_size("rep") != 4:
        routes = jnp.concatenate([ids.astype(BF16), gates], axis=1).transpose(0, 2, 1)
        routes = jnp.pad(routes, ((0, 0), (0, 0), (0, 128 - 2 * top)))
        full = lax.all_gather(jnp.concatenate([tokens, routes], axis=-1), "ep", axis=1, tiled=True)
        weights = [lax.all_to_all(w, "ep", split_axis=1, concat_axis=0, tiled=True) for w in (wq, wk, wv)]
        packets = lax.all_gather(packet, "ep", axis=0)
        share, heads = width // (128 * ep), HEAD_DIM // ep
        gains = jnp.stack([packets[:, :share].reshape(width), packets[:, share : 2 * share].reshape(width)])
        lens = jnp.pad(packets[:, 2 * share + 2, 0], (0, 128 - ep))
        few = [packets[:, 2 * share + k, :heads].reshape(HEAD_DIM) for k in range(2)] + [lens]
        return (
            full, jnp.stack(weights), lax.all_gather(cotangent, "ep", axis=1, tiled=True),
            jnp.pad(gains, ((0, 6), (0, 0))), jnp.pad(jnp.stack(few), ((0, 5), (0, 0))),
        )
    dma = pltpu.SemaphoreType.DMA
    return pl.pallas_call(
        front_kernel,
        out_shape=(
            sds((seqs, rows * ep, width + 128), BF16),
            sds((3, wq.shape[0] * ep, cols), BF16),
            sds((seqs, rows * ep, width), BF16),
            sds((8, width), F32),
            sds((8, 128), F32),
        ),
        in_specs=[VM] * 8,
        out_specs=(AN, AN, AN, VM, VM),
        scratch_shapes=[pltpu.VMEM((ep,) + packet.shape, F32), pltpu.VMEM((seqs, rows, width + 128), BF16)]
        + Gather.scratch(seqs)
        + Gather.scratch(seqs)
        + [dma((7, 3)), dma((7, 3)), dma((7,)), dma((7,))]
        + [dma((7, 4))] * 4
        + [dma((3,))],
        compiler_params=pltpu.CompilerParams(collective_id=1, **COMM),
        name="front",
    )(tokens, cotangent, ids, gates, wq, wk, wv, packet)


def plain_living(small, seqs, rows):
    place = (jnp.arange(rows) + lax.axis_index("ep") * rows).astype(F32)
    return (place[None] < small[2, :seqs, None]).astype(F32)[..., None]


def mix(part, tokens, small, gains):
    seqs, rows, _ = tokens.shape
    total = lax.psum_scatter(part, "ep", scatter_dimension=1, tiled=True).astype(F32)
    middle, mixed = mix_rows(total, tokens, plain_living(small, seqs, rows), gains[1])
    return middle, lax.all_gather(mixed, "ep", axis=1, tiled=True)


def back_kernel(gpart, middle, cot, small, gains, mgrad, ggrad, full, own, *scratch):
    at = Place()
    seqs = cot.shape[0]
    n = Reduce.sems
    rg = Reduce(at, gpart, *scratch[:n])
    gather = Gather(at, own, full, *scratch[n:])
    at.greet((at.xn, at.yn, at.sb))
    each(seqs, rg.start)
    each(seqs, rg.hop1)
    each(seqs, rg.hop2)
    ggrad[...] = jnp.zeros_like(ggrad)

    def rows(s):
        living = live_rows(small, s, at.me, cot.shape[1])
        mg, ag, back = ffn_back_rows(rg.total(s), middle[s], cot[s], living, gains[1:2])
        mgrad[s] = mg
        own[s] = ag
        ggrad[...] += jnp.sum(back, axis=0, keepdims=True)
        gather.start(s)

    each(seqs, rows)
    gather_tail(gather, 0, seqs)
    each(seqs, rg.finish)


def back(gpart, middle, cot, small, gains):
    seqs, rows, width = cot.shape
    ep = lax.axis_size("ep")
    if ep != 8:
        mixed_grad = lax.psum_scatter(gpart, "ep", scatter_dimension=1, tiled=True).astype(F32)
        mg, ag, backs = ffn_back_rows(mixed_grad, middle, cot, plain_living(small, seqs, rows), gains[1])
        full = lax.all_gather(ag, "ep", axis=1, tiled=True)
        return mg, jnp.sum(backs, axis=(0, 1))[None], full
    gpart = gpart.reshape(seqs, ep, rows, width)
    return pl.pallas_call(
        back_kernel,
        out_shape=(
            sds(cot.shape, F32),
            sds((1, width), F32),
            sds((seqs, rows * ep, width), BF16),
        ),
        in_specs=[AN] + [VM] * 4,
        out_specs=(VM, VM, AN),
        scratch_shapes=[pltpu.VMEM(cot.shape, BF16)] + Reduce.scratch(gpart) + Gather.scratch(seqs),
        compiler_params=pltpu.CompilerParams(collective_id=3, **COMM),
        name="back",
    )(gpart, middle, cot, small, gains)


def finish_kernel(
    wgrad, wograd, npart, opart, tok, middle, mgrad, gains, others,
    out, small_out, result, tgrad,
    own, held, met, ggrad, parcel, landed, spare,
    wsend, wrecv, local, gsend, grecv, os, or_, ps, pr, qs, qr, fs, fr, ss, sr, *scratch,
):
    at = Place()
    z, me = at.rep, at.me
    n = Reduce.sems
    normed_sum = Reduce(at, npart, *scratch[:n])
    result_sum = Reduce(at, opart, *scratch[n:])
    seqs = tok.shape[0]
    parts, pieces = own.shape[:2]
    chunks = parts * pieces
    width = wgrad.shape[3]
    peers = at.peers()
    barrier = pltpu.get_barrier_semaphore()
    line = [lax.rem(z + k, 4) for k in range(1, 4)]
    for dev in line:
        pl.semaphore_signal(barrier, inc=1, device_id=(dev, me), device_id_type=MESH)
    for dev in peers:
        pl.semaphore_signal(barrier, inc=1, device_id=(z, dev), device_id_type=MESH)
    pl.semaphore_wait(barrier, 10)
    inner = jnp.logical_and(z > 0, z < 3)
    outer_end, partner, outer = 1 + z // 3, 3 - z, 3 * (z - 1)
    cols = pl.ds(pl.multiple_of(me * width, width), width)

    def column_copy(m, j, dev):
        rows = pl.ds(pl.multiple_of(dev * pieces, pieces), pieces)
        return at.push(wgrad.at[j, rows], own.at[1 + j, :, :, cols], wsend.at[m, j], wrecv.at[m, j], dev)

    mine_rows = pl.ds(pl.multiple_of(me * pieces, pieces), pieces)
    locals_ = [pltpu.make_async_copy(wgrad.at[j, mine_rows], own.at[1 + j, :, :, cols], local.at[j]) for j in range(3)]
    locals_.append(pltpu.make_async_copy(wograd, own.at[0], local.at[3]))
    for copy in locals_:
        copy.start()
    for j in range(3):
        for m, dev in enumerate(peers):
            column_copy(m, j, dev).start()
    each(seqs, normed_sum.start)
    each(seqs, result_sum.start)
    ggrad[...] = jnp.zeros_like(ggrad)

    def piece(ref, c):
        return ref.at[c // pieces, lax.rem(c, pieces)]

    def line_push(src, dst, send, recv, dev):
        return pltpu.make_async_remote_copy(
            src_ref=src, dst_ref=dst, send_sem=send, recv_sem=recv, device_id=(dev, me), device_id_type=MESH
        )

    def inward(c):
        return line_push(piece(own, c), piece(held, c), os.at[c], or_.at[c], outer_end)

    def across(c):
        return line_push(piece(held, c), met.at[c // 2], ps.at[c], pr.at[c], partner)

    def share(c):
        return line_push(piece(out, c), piece(out, c), qs.at[c], qr.at[c], partner)

    def outward(c):
        return line_push(piece(out, c), piece(out, c), fs.at[c], fr.at[c], outer)

    def mine(c):
        return 1 + lax.rem(c, 2) == z

    def ready(part):
        for j in range(parts):

            @pl.when(part == j)
            def _():
                locals_[(3, 0, 1, 2)[j]].wait()
                if j > 0:
                    for m, dev in enumerate(peers):
                        column_copy(m, j - 1, dev).wait_recv()

    def step(c):
        @pl.when(lax.rem(c, pieces) == 0)
        def _():
            ready(c // pieces)

        @pl.when(jnp.logical_not(inner))
        def _():
            inward(c).start()

        @pl.when(inner)
        def _():
            inward(c).wait_recv()
            here = piece(held, c)
            here[...] = (here[...].astype(F32) + piece(own, c)[...].astype(F32)).astype(BF16)

            @pl.when(jnp.logical_not(mine(c)))
            def _():
                across(c).start()

    def settle(c):
        @pl.when(jnp.logical_and(inner, mine(c)))
        def _():
            across(c).wait_recv()
            piece(out, c)[...] = (piece(held, c)[...].astype(F32) + met[c // 2].astype(F32)).astype(BF16)
            share(c).start()
            outward(c).start()

    def forward(c):
        @pl.when(jnp.logical_and(inner, jnp.logical_not(mine(c))))
        def _():
            share(c).wait_recv()
            outward(c).start()

    def token_rows(s):
        tg, back = attn_back_rows(normed_sum.total(s), tok[s], mgrad[s], gains[0:1])
        tgrad[s] = tg
        ggrad[...] += jnp.sum(back, axis=0, keepdims=True)

    def out_rows(s):
        result[s] = (middle[s] + result_sum.total(s)).astype(BF16)

    jobs = (
        (step, 0, chunks), (settle, 1, chunks), (forward, 2, chunks),
        (normed_sum.hop1, 2, seqs), (normed_sum.hop2, 6, seqs), (token_rows, 10, seqs),
        (result_sum.hop1, 6, seqs), (result_sum.hop2, 10, seqs), (out_rows, 14, seqs),
    )

    def tick(i, _):
        for job, lag, count in jobs:

            @pl.when(jnp.logical_and(i >= lag, i < lag + count))
            def _():
                job(i - lag)

        return 0

    lax.fori_loop(0, max(lag + count for _, lag, count in jobs), tick, 0)

    parcel[...] = jnp.zeros_like(parcel)
    devices = parcel.shape[0]
    rows_of = ggrad.shape[1] // (128 * devices)
    for dev in range(devices):
        for k in range(rows_of):
            lanes = pl.ds((dev * rows_of + k) * 128, 128)
            parcel[dev, k : k + 1] = ggrad[:, lanes]
            parcel[dev, rows_of + k : rows_of + k + 1] = others[0:1, lanes]
        parcel[dev, 2 * rows_of : 2 * rows_of + 2] = others[1:3, 0:128]

    def parcel_copy(m, dev):
        return at.push(parcel.at[dev], landed.at[m], gsend.at[m], grecv.at[m], dev)

    for m, dev in enumerate(peers):
        parcel_copy(m, dev).start()
    total = parcel[me]
    for m, dev in enumerate(peers):
        parcel_copy(m, dev).wait_recv()
        total = total + landed[m]
    spare[0] = total

    def small_copy(k):
        return line_push(spare.at[0], spare.at[1 + k], ss.at[k], sr.at[k], line[k])

    for k in range(3):
        small_copy(k).start()

    @pl.when(jnp.logical_not(inner))
    def _():
        each(chunks, lambda c: outward(c).wait_recv())
        each(chunks, lambda c: inward(c).wait_send())

    @pl.when(inner)
    def _():
        def sent(c):
            outward(c).wait_send()

            @pl.when(mine(c))
            def _():
                share(c).wait_send()

            @pl.when(jnp.logical_not(mine(c)))
            def _():
                across(c).wait_send()

        each(chunks, sent)

    each(seqs, normed_sum.finish, result_sum.finish)
    for m, dev in enumerate(peers):
        parcel_copy(m, dev).wait_send()
        for j in range(3):
            column_copy(m, j, dev).wait_send()
    total = spare[0]
    for k in range(3):
        small_copy(k).wait()
        total = total + spare[1 + k]
    small_out[...] = total


def finish(wgrad, wograd, npart, opart, tokens, middle, mgrad, gains, ffn_back, qk_back):
    seqs, rows, width = tokens.shape
    ep = lax.axis_size("ep")
    if ep != 8 or lax.axis_size("rep") != 4:
        normed_grad = lax.psum_scatter(npart, "ep", scatter_dimension=1, tiled=True).astype(F32)
        moe = lax.psum_scatter(opart, "ep", scatter_dimension=1, tiled=True).astype(F32)
        tg, backs = attn_back_rows(normed_grad, tokens, mgrad, gains[0])
        wrows = lax.all_to_all(wgrad, "ep", split_axis=1, concat_axis=2, tiled=True)
        share = width // ep
        small = jnp.concatenate([jnp.sum(backs, axis=(0, 1)), ffn_back[0], qk_back[0], qk_back[1]])
        small = lax.psum(small, ("ep", "rep"))
        mine = lax.axis_index("ep") * share
        cut = [lax.dynamic_slice_in_dim(small, k * width + mine, share).reshape(-1, 128) for k in range(2)]
        small = jnp.concatenate(cut + [small[2 * width :].reshape(2, HEAD_DIM)], axis=0)
        big = lax.psum(jnp.concatenate([wograd[None], wrows], axis=0), "rep")
        return big, jnp.pad(small, ((0, 8 - small.shape[0]), (0, 0))), (middle + moe).astype(BF16), tg
    others = jnp.concatenate([ffn_back, jnp.pad(qk_back[:2], ((0, 0), (0, width - HEAD_DIM)))], axis=0)
    npart, opart = (p.reshape(seqs, ep, rows, width) for p in (npart, opart))
    pieces = 4
    block = wograd.shape[0] // pieces
    wgrad = wgrad.reshape(3, wgrad.shape[1] // block, block, wgrad.shape[2])
    wograd = wograd.reshape(pieces, block, width)
    whole = (4, pieces, block, width)
    dma = pltpu.SemaphoreType.DMA
    chunks = 4 * pieces
    out, small, result, tgrad = pl.pallas_call(
        finish_kernel,
        out_shape=(sds(whole, BF16), sds((8, 128), F32), sds(tokens.shape, BF16), sds(tokens.shape, BF16)),
        in_specs=[VM, VM, AN, AN] + [VM] * 5,
        out_specs=(VM, VM, VM, VM),
        scratch_shapes=[
            pltpu.VMEM(whole, BF16),
            pltpu.VMEM(whole, BF16),
            pltpu.VMEM((chunks // 2, block, width), BF16),
            pltpu.VMEM((1, width), F32),
            pltpu.VMEM((ep, 8, 128), F32),
            pltpu.VMEM((7, 8, 128), F32),
            pltpu.VMEM((4, 8, 128), F32),
        ]
        + [dma((7, 3)), dma((7, 3)), dma((4,)), dma((7,)), dma((7,))]
        + [dma((chunks,))] * 8
        + [dma((3,))] * 2
        + 2 * Reduce.scratch(npart),
        compiler_params=pltpu.CompilerParams(collective_id=4, has_side_effects=True, vmem_limit_bytes=61 << 20),
        name="finish",
    )(wgrad, wograd, npart, opart, tokens, middle, mgrad, gains, others)
    return out.reshape(4, pieces * block, width), small, result, tgrad


def dot(a, b, ca, cb):
    return lax.dot_general(a, b, (((ca,), (cb,)), ((), ())), preferred_element_type=F32)


def rope_tables(table):
    half = HEAD_DIM // 2
    values = table[...]
    turned = pltpu.roll(values, half, 1)
    first = lax.broadcasted_iota(jnp.int32, values.shape, 1) < half
    return jnp.where(first, values, turned), jnp.where(first, -turned, values)


def rope(v, cos, sin_turn):
    return v * cos + pltpu.roll(v, HEAD_DIM // 2, 1) * sin_turn


def probabilities(q, k, length):
    scores = dot(q, k, 1, 1) * HEAD_DIM**-0.5
    column = lax.broadcasted_iota(jnp.int32, (1, scores.shape[1]), 1).astype(F32)
    scores = jnp.where(column < length, scores, -1e9)
    p = jnp.exp(scores - jnp.max(scores, axis=-1, keepdims=True))
    return p * (1.0 / jnp.sum(p, axis=-1, keepdims=True))


def packed_slots(number, table, length_live, top):
    tab = table.astype(F32)
    length = tab.shape[0]
    lane = lax.broadcasted_iota(jnp.int32, tab.shape, 1)
    row = lax.broadcasted_iota(jnp.int32, (length, 1), 0).astype(F32)
    chosen = jnp.logical_and(jnp.logical_and(tab == number, lane < top), row < length_live)
    gates = jnp.where(chosen, pltpu.roll(tab, 128 - top, 1), 0.0).astype(BF16)
    chosen = jnp.where(chosen, 1.0, 0.0).astype(BF16)
    ones = jnp.ones((8, 128), BF16)
    hit = dot(ones, chosen, 1, 1)
    weight = dot(ones, gates, 1, 1)
    earlier = lax.broadcasted_iota(jnp.int32, (length, length), 0)
    later = lax.broadcasted_iota(jnp.int32, (length, length), 1)
    rank = dot(hit.astype(BF16), jnp.where(earlier < later, 1.0, 0.0).astype(BF16), 1, 0)
    return jnp.where(hit > 0.5, rank, -1.0), weight, jnp.sum(hit[0:1], axis=1, keepdims=True)


def attend_rows(top, number, s, block, w, wo, gains, small, table, normed, pre, low, ctx, part, slots, starts):
    width = normed.shape[1]
    length = seq_len(small, s)
    cos, sin = rope_tables(table)
    v = block[:, 0:width].astype(F32)
    x = (v * inverse_rms(v) * gains[0:1]).astype(BF16)
    normed[...] = x
    q_pre, k_pre = dot(x, w[0], 1, 0), dot(x, w[1], 1, 0)
    value = dot(x, w[2], 1, 0).astype(BF16)
    pre[0], pre[1] = q_pre, k_pre
    low[2] = value
    for h in range(q_pre.shape[1] // HEAD_DIM):
        cols = slice(h * HEAD_DIM, (h + 1) * HEAD_DIM)
        rot = []
        for i, (u, g) in enumerate(((q_pre[:, cols], small[0:1]), (k_pre[:, cols], small[1:2]))):
            rot.append(rope(u * inverse_rms(u) * g, cos, sin).astype(BF16))
            low[i, :, cols] = rot[i]
        attention = probabilities(rot[0], rot[1], length).astype(BF16)
        ctx[:, cols] = dot(attention, value[:, cols], 1, 0).astype(BF16)
    part[...] = dot(ctx[...], wo[...], 1, 0).astype(BF16).reshape(part.shape)
    routes = block[:, width : width + 128]
    lane = lax.broadcasted_iota(jnp.int32, (1, 128), 1)
    for j, ref in enumerate(slots):
        slot, weight, count = packed_slots(number + j, routes, length, top)
        ref[0:8] = slot
        ref[8:16] = weight
        row = starts[j : j + 1]
        after = jnp.sum(jnp.where(lane == s, row, 0.0), axis=1, keepdims=True) + 16.0 * jnp.floor((count + 15.0) * 0.0625)
        starts[j : j + 1] = jnp.where(lane == s + 1, after, row)


def attend_kernel(top, number, full, w, wo, gains, small, table, normed, pre, low, ctx, part, slots0, slots1, starts):
    s = pl.program_id(0)

    @pl.when(s == 0)
    def _():
        starts[...] = jnp.zeros_like(starts)

    attend_rows(
        top, number[0].astype(F32), s, full.at[0], w, wo, gains, small, table,
        normed.at[0], pre.at[:, 0], low.at[:, 0], ctx.at[0], part.at[0], (slots0.at[0], slots1.at[0]), starts,
    )


def attend(top, number, full, weights, wo, gains, small, table):
    seqs, length, wide = full.shape
    width = wide - 128
    cols = weights.shape[2]
    row = lambda i, *_: (i, 0, 0)
    row2 = lambda i, *_: (0, i, 0, 0)
    two = lambda i, *_: (0, 0)
    slot = pl.BlockSpec((1, 16, length), row)
    return pl.pallas_call(
        functools.partial(attend_kernel, top),
        out_shape=(
            sds((seqs, length, width), BF16),
            sds((2, seqs, length, cols), F32),
            sds((3, seqs, length, cols), BF16),
            sds((seqs, length, cols), BF16),
            sds((seqs, length, width), BF16),
            sds((seqs, 16, length), F32),
            sds((seqs, 16, length), F32),
            sds((8, 128), F32),
        ),
        grid_spec=pltpu.PrefetchScalarGridSpec(
            num_scalar_prefetch=1,
            grid=(seqs,),
            in_specs=[
                pl.BlockSpec((1, length, wide), row),
                pl.BlockSpec(weights.shape, lambda i, *_: (0, 0, 0)),
                pl.BlockSpec(wo.shape, two),
                pl.BlockSpec((8, width), two),
                pl.BlockSpec((8, 128), two),
                pl.BlockSpec((length, HEAD_DIM), two),
            ],
            out_specs=(
                pl.BlockSpec((1, length, width), row),
                pl.BlockSpec((2, 1, length, cols), row2),
                pl.BlockSpec((3, 1, length, cols), row2),
                pl.BlockSpec((1, length, cols), row),
                pl.BlockSpec((1, length, width), row),
                slot,
                slot,
                pl.BlockSpec((8, 128), two),
            ),
        ),
        compiler_params=pltpu.CompilerParams(dimension_semantics=("arbitrary",), vmem_limit_bytes=60 << 20),
        cost_estimate=pl.CostEstimate(flops=10**10, bytes_accessed=4 * 10**7, transcendentals=10**6),
        name="attend",
    )(number, full, weights, wo, gains, small, table)


def attend_mix_kernel(
    top, local, full, w, wo, gains, small, table, tok, cot, _cot_early,
    normed, pre, low, ctx, middle, mixed, cot_full, slots0, slots1, starts,
    own, blocks, nbuf, pbuf, lbuf, cbuf, part, begins, tsem, ssem, *scratch,
):
    at = Place()
    seqs = tok.shape[0]
    n = Reduce.sems
    reduce = Reduce(at, part, *scratch[:n])
    gather = Gather(at, own, mixed, *scratch[n : n + 3])
    cot_gather = Gather(at, cot, cot_full, *scratch[n + 3 :])
    number = (at.me * local).astype(F32)
    early = seqs // 2
    at.greet((at.xn, at.yn, at.sb))
    each(seqs, cot_gather.start, low=early)
    begins[...] = jnp.zeros_like(begins)

    def load(s):
        return pltpu.make_async_copy(full.at[s], blocks.at[lax.rem(s, 2)], tsem.at[lax.rem(s, 2)])

    def stores(s):
        k = lax.rem(s, 2)
        pairs = ((nbuf.at[k], normed.at[s]), (pbuf.at[k], pre.at[:, s]), (lbuf.at[k], low.at[:, s]), (cbuf.at[k], ctx.at[s]))
        return [pltpu.make_async_copy(src, dst, ssem.at[i, k]) for i, (src, dst) in enumerate(pairs)]

    load(0).start()

    def sequence(s):
        k = lax.rem(s, 2)
        load(s).wait()

        @pl.when(s + 1 < seqs)
        def _():
            load(s + 1).start()

        @pl.when(s >= 2)
        def _():
            for copy in stores(s - 2):
                copy.wait()

        attend_rows(
            top, number, s, blocks.at[k], w, wo, gains, small, table,
            nbuf.at[k], pbuf.at[k], lbuf.at[k], cbuf.at[k], part.at[s], (slots0.at[s], slots1.at[s]), begins,
        )
        for copy in stores(s):
            copy.start()
        reduce.start(s)

    def rows(s):
        living = live_rows(small, s, at.me, tok.shape[1])
        mid, out = mix_rows(reduce.total(s), tok[s], living, gains[1:2])
        middle[s] = mid
        own[s] = out
        gather.start(s)

    def cot_pair(p):
        @pl.when(lax.rem(p, 2) == 0)
        def _():
            cot_gather.relay(early + p, True)
            cot_gather.relay(early + p + 1, False)

    jobs = (
        (sequence, 0, seqs), (reduce.hop1, 1, seqs), (cot_pair, 3, early), (reduce.hop2, 3, seqs),
        (lambda s: cot_gather.relay_far(early + s), 7, early), (rows, 5, seqs),
    )

    def tick(i, _):
        for job, lag, count in jobs:

            @pl.when(jnp.logical_and(i >= lag, i < lag + count))
            def _():
                job(i - lag)

        return 0

    lax.fori_loop(0, max(lag + count for _, lag, count in jobs), tick, 0)
    starts[...] = begins[...].astype(jnp.int32)
    each(seqs, cot_gather.finish, low=early)
    gather_tail(gather, 0, seqs)
    for s in (seqs - 2, seqs - 1):
        for copy in stores(s):
            copy.wait()
    each(seqs, reduce.finish)


def attend_mix(top, local, full, weights, wo, gains, small, table, tokens, cotangent, cot_early):
    seqs, rows, width = tokens.shape
    length = full.shape[1]
    cols = weights.shape[2]
    part = sds((seqs, 8, rows, width), BF16)
    dma = pltpu.SemaphoreType.DMA
    return pl.pallas_call(
        functools.partial(attend_mix_kernel, top, local),
        out_shape=(
            sds((seqs, length, width), BF16),
            sds((2, seqs, length, cols), F32),
            sds((3, seqs, length, cols), BF16),
            sds((seqs, length, cols), BF16),
            sds(tokens.shape, F32),
            sds((seqs, length, width), BF16),
            sds((seqs, length, width), BF16),
            sds((seqs, 16, length), F32),
            sds((seqs, 16, length), F32),
            sds((8, 128), jnp.int32),
        ),
        in_specs=[AN] + [VM] * 7 + [AN],
        out_specs=(AN, AN, AN, AN, VM, AN, AN, VM, VM, VM),
        input_output_aliases={8: 6},
        scratch_shapes=[
            pltpu.VMEM(tokens.shape, BF16),
            pltpu.VMEM((2,) + full.shape[1:], BF16),
            pltpu.VMEM((2, length, width), BF16),
            pltpu.VMEM((2, 2, length, cols), F32),
            pltpu.VMEM((2, 3, length, cols), BF16),
            pltpu.VMEM((2, length, cols), BF16),
            pltpu.VMEM(part.shape, BF16),
            pltpu.VMEM((8, 128), F32),
            dma((2,)),
            dma((4, 2)),
        ]
        + Reduce.scratch(part)
        + Gather.scratch(seqs)
        + Gather.scratch(seqs),
        compiler_params=pltpu.CompilerParams(collective_id=2, **COMM),
        name="attend_mix",
    )(full, weights, wo, gains, small, table, tokens, cotangent, cot_early)


def attend_back_kernel(
    agrad, normed, pre, low, ctx, w, wo, small, table, part, wgrad, wograd, gains, wacc, woacc,
    gbuf, total,
):
    s = pl.program_id(0)
    length = seq_len(small, s)
    cos, sin = rope_tables(table)

    @pl.when(s == 0)
    def _():
        wacc[...] = jnp.zeros_like(wacc)
        woacc[...] = jnp.zeros_like(woacc)
        gains[...] = jnp.zeros_like(gains)

    ag = agrad[0]
    woacc[...] += dot(ctx[0], ag, 0, 0)
    cg_all = dot(ag, wo[...], 1, 1).astype(BF16)
    scale = HEAD_DIM**-0.5
    half = HEAD_DIM // 2
    grads = ([], [], [])
    for h in range(cg_all.shape[1] // HEAD_DIM):
        cols = slice(h * HEAD_DIM, (h + 1) * HEAD_DIM)
        q, k, value, cg = low[0, 0, :, cols], low[1, 0, :, cols], low[2, 0, :, cols], cg_all[:, cols]
        attention = probabilities(q, k, length)
        grads[2].append(dot(attention.astype(BF16), cg, 0, 0).astype(BF16))
        pg = dot(cg, value, 1, 1)
        sg = (attention * (pg - jnp.sum(attention * pg, axis=-1, keepdims=True))).astype(BF16)
        for i, (rot_grad, g) in enumerate(((dot(sg, k, 1, 0), small[0:1]), (dot(sg, q, 0, 0), small[1:2]))):
            wgt = rot_grad * scale
            u = wgt * cos + pltpu.roll(wgt * sin, half, 1)
            v = pre[i, 0, :, cols]
            r = inverse_rms(v)
            grads[i].append(rms_back(v, r, u * g).astype(BF16))
            gains[i : i + 1] += jnp.sum(u * v * r, axis=0, keepdims=True)
    for i in range(3):
        for h, g in enumerate(grads[i]):
            gbuf[i, :, h * HEAD_DIM : (h + 1) * HEAD_DIM] = g

    def project(i, _):
        g = gbuf[i]
        wacc[i] += dot(normed[0], g, 0, 0)
        piece = dot(g, w[i], 1, 1)

        @pl.when(i == 0)
        def _():
            total[...] = piece

        @pl.when(i > 0)
        def _():
            total[...] += piece

        return 0

    lax.fori_loop(0, 3, project, 0)
    part[0] = total[...].astype(BF16)

    @pl.when(s == pl.num_programs(0) - 1)
    def _():
        wgrad[...] = wacc[...].astype(BF16)
        wograd[...] = woacc[...].astype(BF16)


def attend_back(agrad, normed, pre, low, ctx, weights, wo, small, table):
    seqs, length, width = agrad.shape
    cols = weights.shape[2]
    row = lambda i, *_: (i, 0, 0)
    row2 = lambda i, *_: (0, i, 0, 0)
    two = lambda i, *_: (0, 0)
    three = lambda i, *_: (0, 0, 0)
    return pl.pallas_call(
        attend_back_kernel,
        out_shape=(
            sds(agrad.shape, BF16),
            sds(weights.shape, BF16),
            sds(wo.shape, BF16),
            sds((8, HEAD_DIM), F32),
        ),
        grid_spec=pltpu.PrefetchScalarGridSpec(
            num_scalar_prefetch=0,
            grid=(seqs,),
            in_specs=[
                pl.BlockSpec((1, length, width), row),
                pl.BlockSpec((1, length, width), row),
                pl.BlockSpec((2, 1, length, cols), row2),
                pl.BlockSpec((3, 1, length, cols), row2),
                pl.BlockSpec((1, length, cols), row),
                pl.BlockSpec(weights.shape, three),
                pl.BlockSpec(wo.shape, two),
                pl.BlockSpec((8, 128), two),
                pl.BlockSpec((length, HEAD_DIM), two),
            ],
            out_specs=(
                pl.BlockSpec((1, length, width), row),
                pl.BlockSpec(weights.shape, three),
                pl.BlockSpec(wo.shape, two),
                pl.BlockSpec((8, HEAD_DIM), two),
            ),
            scratch_shapes=[
                pltpu.VMEM(weights.shape, F32),
                pltpu.VMEM(wo.shape, F32),
                pltpu.VMEM((3, length, cols), BF16),
                pltpu.VMEM((length, width), F32),
            ],
        ),
        compiler_params=pltpu.CompilerParams(dimension_semantics=("arbitrary",), vmem_limit_bytes=60 << 20),
        cost_estimate=pl.CostEstimate(flops=2 * 10**10, bytes_accessed=4 * 10**7, transcendentals=10**6),
        name="attend_back",
    )(agrad, normed, pre, low, ctx, weights, wo, small, table)


BLOCK = 256


def pack_rows(seqs, capacity):
    return -(-seqs * capacity // BLOCK) * BLOCK


def each_block(blocks, hidden, job):
    part = min(hidden, 512)
    parts = hidden // part

    def run(i, _):
        b, h = i // parts, lax.rem(i, parts)
        rows = pl.ds(pl.multiple_of(b * BLOCK, BLOCK), BLOCK)
        low = pl.multiple_of(h * part, part)
        job(rows, pl.ds(low, part), pl.ds(pl.multiple_of(hidden + low, part), part))
        return 0

    lax.fori_loop(0, blocks * parts, run, 0)


def swiglu_back(gate, up, dact):
    sig = 1.0 / (1.0 + jnp.exp(-gate))
    return dact * up * sig * (1.0 + gate * (1.0 - sig)), dact * (gate * sig)


def gradient_tiles(blocks, left, right, result, acc, stage, ssem, busy):
    tr, tc = acc.shape
    down, across = result.shape[0] // tr, result.shape[1] // tc

    def tile(t, _):
        rt, ct = t // across, lax.rem(t, across)
        left_cols = pl.ds(pl.multiple_of(rt * tr, tr), tr)
        right_cols = pl.ds(pl.multiple_of(ct * tc, tc), tc)

        def step(b, _):
            rows = pl.ds(pl.multiple_of(b * BLOCK, BLOCK), BLOCK)
            piece = dot(left[rows, left_cols], right[rows, right_cols], 0, 0)

            @pl.when(b == 0)
            def _():
                acc[...] = piece

            @pl.when(b > 0)
            def _():
                acc[...] += piece

            return 0

        @pl.when(blocks == 0)
        def _():
            acc[...] = jnp.zeros_like(acc)

        lax.fori_loop(0, blocks, step, 0)
        k = lax.rem(t, 2)
        out = pltpu.make_async_copy(stage.at[k], result.at[left_cols, right_cols], ssem.at[k])

        @pl.when(jnp.logical_or(t >= 2, busy))
        def _():
            out.wait()

        stage[k] = acc[...].astype(BF16)
        out.start()
        return 0

    lax.fori_loop(0, down * across, tile, 0)


def drain_tiles(result, acc, stage, ssem):
    tr, tc = acc.shape
    for k in range(2):
        pltpu.make_async_copy(stage.at[k], result.at[pl.ds(0, tr), pl.ds(0, tc)], ssem.at[k]).wait()


def first_kernel(
    capacity, starts, mixed, cot, slots0, slots1, w_in,
    act, pair, x_all, dy_all, out_grad,
    x, dy, wi, acts, pairs, acc, stage, wsem, ssem, rsem,
):
    step = pl.program_id(0)
    steps = pl.num_programs(0)
    together = mixed.shape[0]
    seqs = steps * together
    width = mixed.shape[2]
    hidden = acts.shape[1]
    load = pltpu.make_async_copy(w_in.at[0], wi, wsem)

    @pl.when(step == 0)
    def _():
        load.start()

    packed = []
    for k in range(together):
        spread, gate_spread = [], []
        for slots in (slots0, slots1):
            column = lax.broadcasted_iota(jnp.int32, (capacity, slots.shape[2]), 0).astype(F32)
            place = column == slots[k, 0:1]
            spread.append(jnp.where(place, 1.0, 0.0).astype(BF16))
            gate_spread.append(jnp.where(place, slots[k, 8:9], 0.0).astype(BF16))
        packed.append(
            (
                dot(jnp.concatenate(spread, axis=0), mixed[k], 1, 0).astype(BF16),
                dot(jnp.concatenate(gate_spread, axis=0), cot[k], 1, 0).astype(BF16),
            )
        )
    for k, (x_rows, dy_rows) in enumerate(packed):
        s = step * together + k
        for j in range(2):
            start = pl.multiple_of(starts[j, s], 16)
            x[j, pl.ds(start, capacity)] = x_rows[j * capacity : (j + 1) * capacity]
            dy[j, pl.ds(start, capacity)] = dy_rows[j * capacity : (j + 1) * capacity]

    @pl.when(step == steps - 1)
    def _():
        for j in range(2):
            past = (starts[j, seqs - 1] + capacity) // 16
            end = (starts[j, seqs] + BLOCK - 1) // BLOCK * (BLOCK // 16)

            def clear(i, _):
                rows = pl.ds(pl.multiple_of(i * 16, 16), 16)
                x[j, rows] = jnp.zeros((16, width), BF16)
                dy[j, rows] = jnp.zeros((16, width), BF16)
                return 0

            lax.fori_loop(past, end, clear, 0)
        saves = [pltpu.make_async_copy(x, x_all, rsem.at[0]), pltpu.make_async_copy(dy, dy_all, rsem.at[1])]
        for copy in saves:
            copy.start()
        blocks = (starts[0, seqs] + BLOCK - 1) // BLOCK
        load.wait()

        def forward(rows, gcols, ucols):
            gate = dot(x[0, rows], wi[:, gcols], 1, 0)
            up = dot(x[0, rows], wi[:, ucols], 1, 0)
            acts[rows, gcols] = (gate * (1.0 / (1.0 + jnp.exp(-gate))) * up).astype(BF16)
            pairs[rows, gcols] = gate.astype(BF16)
            pairs[rows, ucols] = up.astype(BF16)

        each_block(blocks, hidden, forward)
        saves += [pltpu.make_async_copy(acts, act.at[0], rsem.at[2]), pltpu.make_async_copy(pairs, pair, rsem.at[3])]
        for copy in saves[2:]:
            copy.start()
        gradient_tiles(blocks, acts, dy.at[0], out_grad, acc, stage, ssem, False)
        drain_tiles(out_grad, acc, stage, ssem)
        for copy in saves:
            copy.wait()


def expert_first(starts, mixed, cot, slots, w_in, hidden, capacity):
    seqs, length, width = mixed.shape
    rows = pack_rows(seqs, capacity)
    dma = pltpu.SemaphoreType.DMA
    seq = lambda i, *_: (i, 0, 0)
    together = 2
    slot_spec = pl.BlockSpec((together, 16, length), seq)
    return pl.pallas_call(
        functools.partial(first_kernel, capacity),
        out_shape=(
            sds((2, rows, hidden), BF16),
            sds((rows, 2 * hidden), BF16),
            sds((2, rows, width), BF16),
            sds((2, rows, width), BF16),
            sds((hidden, width), BF16),
        ),
        grid_spec=pltpu.PrefetchScalarGridSpec(
            num_scalar_prefetch=1,
            grid=(seqs // together,),
            in_specs=[
                pl.BlockSpec((together, length, width), seq),
                pl.BlockSpec((together, length, width), seq),
                slot_spec,
                slot_spec,
                AN,
            ],
            out_specs=(AN, AN, AN, AN, AN),
            scratch_shapes=[
                pltpu.VMEM((2, rows, width), BF16),
                pltpu.VMEM((2, rows, width), BF16),
                pltpu.VMEM(w_in.shape[1:], BF16),
                pltpu.VMEM((rows, hidden), BF16),
                pltpu.VMEM((rows, 2 * hidden), BF16),
                pltpu.VMEM((512, 1024), F32),
                pltpu.VMEM((2, 512, 1024), BF16),
                dma,
                dma((2,)),
                dma((4,)),
            ],
        ),
        compiler_params=pltpu.CompilerParams(dimension_semantics=("arbitrary",), vmem_limit_bytes=62 << 20),
        cost_estimate=pl.CostEstimate(flops=2 * 10**10, bytes_accessed=6 * 10**7, transcendentals=10**6),
        name="expert_first",
    )(starts, mixed, cot, *slots, w_in)


def in_grad_kernel(
    seqs, starts, x_all, dy_all, pair, w_out, dgu, in_grad, x, dy, wo, pairs, dgus, acc, stage, lsem, wsem, ssem, rsem
):
    blocks = (starts[0, seqs] + BLOCK - 1) // BLOCK
    hidden = wo.shape[0]
    weights = pltpu.make_async_copy(w_out.at[0], wo, wsem)
    weights.start()

    def run(b, action):
        rows = pl.ds(pl.multiple_of(b * BLOCK, BLOCK), BLOCK)
        for copy in (
            pltpu.make_async_copy(dy_all.at[0, rows], dy.at[rows], lsem.at[0, b]),
            pltpu.make_async_copy(pair.at[rows], pairs.at[rows], lsem.at[1, b]),
            pltpu.make_async_copy(x_all.at[0, rows], x.at[rows], lsem.at[2, b]),
        ):
            getattr(copy, action)()
        return 0

    lax.fori_loop(0, blocks, lambda b, _: run(b, "start"), 0)
    weights.wait()
    lax.fori_loop(0, blocks, lambda b, _: run(b, "wait"), 0)

    def backward(rows, gcols, ucols):
        dact = dot(dy[rows], wo[gcols], 1, 1)
        dgate, dup = swiglu_back(pairs[rows, gcols].astype(F32), pairs[rows, ucols].astype(F32), dact)
        dgus[rows, gcols] = dgate.astype(BF16)
        dgus[rows, ucols] = dup.astype(BF16)

    each_block(blocks, hidden, backward)
    save = pltpu.make_async_copy(dgus, dgu.at[0], rsem)
    save.start()
    gradient_tiles(blocks, x, dgus, in_grad.at[0], acc, stage, ssem, False)
    drain_tiles(in_grad.at[0], acc, stage, ssem)
    save.wait()


def first_in_grad(seqs, starts, x_all, dy_all, pair, w_out):
    rows, width = x_all.shape[1:]
    hidden = w_out.shape[1]
    dma = pltpu.SemaphoreType.DMA
    return pl.pallas_call(
        functools.partial(in_grad_kernel, seqs),
        out_shape=(sds((2, rows, 2 * hidden), BF16), sds((2, width, 2 * hidden), BF16)),
        grid_spec=pltpu.PrefetchScalarGridSpec(
            num_scalar_prefetch=1,
            grid=(1,),
            in_specs=[AN] * 4,
            out_specs=(AN, AN),
            scratch_shapes=[
                pltpu.VMEM((rows, width), BF16),
                pltpu.VMEM((rows, width), BF16),
                pltpu.VMEM(w_out.shape[1:], BF16),
                pltpu.VMEM((rows, 2 * hidden), BF16),
                pltpu.VMEM((rows, 2 * hidden), BF16),
                pltpu.VMEM((512, 2048), F32),
                pltpu.VMEM((2, 512, 2048), BF16),
                dma((3, rows // BLOCK)),
                dma,
                dma((2,)),
                dma,
            ],
        ),
        compiler_params=pltpu.CompilerParams(dimension_semantics=("arbitrary",), vmem_limit_bytes=60 << 20),
        cost_estimate=pl.CostEstimate(flops=10**10, bytes_accessed=2 * 10**7, transcendentals=0),
        name="first_in_grad",
    )(starts, x_all, dy_all, pair, w_out)


def second_kernel(
    seqs, starts, x_all, dy_all, w_in, w_out, _act, _dgu, _in_grad, act, dgu, in_grad, out_grad,
    x, dy, wi, wo, acts, dgus, acc, stage, wsem, lsem, ssem, rsem,
):
    blocks = (starts[1, seqs] + BLOCK - 1) // BLOCK
    hidden = wo.shape[0]
    loads = [pltpu.make_async_copy(w_in.at[1], wi, wsem.at[0]), pltpu.make_async_copy(w_out.at[1], wo, wsem.at[1])]

    def load(b, action):
        rows = pl.ds(pl.multiple_of(b * BLOCK, BLOCK), BLOCK)
        for copy in (
            pltpu.make_async_copy(x_all.at[1, rows], x.at[rows], lsem.at[0, b]),
            pltpu.make_async_copy(dy_all.at[1, rows], dy.at[rows], lsem.at[1, b]),
        ):
            getattr(copy, action)()
        return 0

    for copy in loads:
        copy.start()
    lax.fori_loop(0, blocks, lambda b, _: load(b, "start"), 0)
    for copy in loads:
        copy.wait()
    lax.fori_loop(0, blocks, lambda b, _: load(b, "wait"), 0)

    def both(rows, gcols, ucols):
        gate = dot(x[rows], wi[:, gcols], 1, 0)
        up = dot(x[rows], wi[:, ucols], 1, 0)
        dact = dot(dy[rows], wo[gcols], 1, 1)
        acts[rows, gcols] = (gate * (1.0 / (1.0 + jnp.exp(-gate))) * up).astype(BF16)
        dgate, dup = swiglu_back(gate, up, dact)
        dgus[rows, gcols] = dgate.astype(BF16)
        dgus[rows, ucols] = dup.astype(BF16)

    each_block(blocks, hidden, both)
    saves = [pltpu.make_async_copy(acts, act.at[1], rsem.at[0]), pltpu.make_async_copy(dgus, dgu.at[1], rsem.at[1])]
    for copy in saves:
        copy.start()
    gradient_tiles(blocks, x, dgus, in_grad.at[1], acc, stage, ssem, False)
    gradient_tiles(blocks, acts, dy, out_grad, acc, stage, ssem, True)
    drain_tiles(out_grad, acc, stage, ssem)
    for copy in saves:
        copy.wait()


def expert_second(seqs, starts, x_all, dy_all, w_in, w_out, act, dgu, in_grad):
    rows, width = dy_all.shape[1:]
    hidden = w_out.shape[1]
    dma = pltpu.SemaphoreType.DMA
    return pl.pallas_call(
        functools.partial(second_kernel, seqs),
        out_shape=(sds(act.shape, BF16), sds(dgu.shape, BF16), sds(in_grad.shape, BF16), sds((hidden, width), BF16)),
        input_output_aliases={5: 0, 6: 1, 7: 2},
        grid_spec=pltpu.PrefetchScalarGridSpec(
            num_scalar_prefetch=1,
            grid=(1,),
            in_specs=[AN] * 7,
            out_specs=(AN, AN, AN, AN),
            scratch_shapes=[
                pltpu.VMEM((rows, width), BF16),
                pltpu.VMEM((rows, width), BF16),
                pltpu.VMEM(w_in.shape[1:], BF16),
                pltpu.VMEM(w_out.shape[1:], BF16),
                pltpu.VMEM((rows, hidden), BF16),
                pltpu.VMEM((rows, 2 * hidden), BF16),
                pltpu.VMEM((512, 2048), F32),
                pltpu.VMEM((2, 512, 2048), BF16),
                dma((2,)),
                dma((2, rows // BLOCK)),
                dma((2,)),
                dma((2,)),
            ],
        ),
        compiler_params=pltpu.CompilerParams(dimension_semantics=("arbitrary",), vmem_limit_bytes=60 << 20),
        cost_estimate=pl.CostEstimate(flops=25 * 10**9, bytes_accessed=6 * 10**7, transcendentals=10**6),
        name="expert_second",
    )(starts, x_all, dy_all, w_in, w_out, act, dgu, in_grad)


def tail_kernel(seqs, starts, act, dgu, w_in, w_out, produced, dx):
    @pl.when(pl.program_id(1) * BLOCK < starts[pl.program_id(0), seqs])
    def _():
        part = min(produced.shape[1], 256)

        def run(i, _):
            cols = pl.ds(pl.multiple_of(i * part, part), part)
            produced[:, cols] = dot(act[...], w_out[:, cols], 1, 0).astype(BF16)
            dx[:, cols] = dot(dgu[...], w_in[cols], 1, 1).astype(BF16)
            return 0

        lax.fori_loop(0, produced.shape[1] // part, run, 0)


def expert_tails(seqs, starts, act, dgu, w_in, w_out):
    _, rows, hidden = act.shape
    width = w_in.shape[1]

    def block(j, i, st):
        return j, jnp.maximum(jnp.minimum(i, (st[j, seqs] + BLOCK - 1) // BLOCK - 1), 0), 0

    out = pl.BlockSpec((None, BLOCK, width), block)
    return pl.pallas_call(
        functools.partial(tail_kernel, seqs),
        out_shape=(sds((2, rows, width), BF16), sds((2, rows, width), BF16)),
        grid_spec=pltpu.PrefetchScalarGridSpec(
            num_scalar_prefetch=1,
            grid=(2, rows // BLOCK),
            in_specs=[
                pl.BlockSpec((None, BLOCK, hidden), block),
                pl.BlockSpec((None, BLOCK, 2 * hidden), block),
                pl.BlockSpec((None,) + w_in.shape[1:], lambda j, i, *_: (j, 0, 0)),
                pl.BlockSpec((None,) + w_out.shape[1:], lambda j, i, *_: (j, 0, 0)),
            ],
            out_specs=(out, out),
        ),
        compiler_params=pltpu.CompilerParams(dimension_semantics=("arbitrary", "arbitrary"), vmem_limit_bytes=60 << 20),
        cost_estimate=pl.CostEstimate(flops=24 * 10**9, bytes_accessed=6 * 10**7, transcendentals=0),
        name="expert_tails",
    )(starts, act, dgu, w_in, w_out)


def combine_kernel(capacity, local, *refs):
    s = pl.program_id(0)
    starts = refs[0]
    slots = refs[1 : 1 + local]
    produced, dx, out_part, grad_part = refs[1 + local :]
    out_sum, grad_sum = None, None
    for j in range(local):
        length = slots[j].shape[2]
        column = lax.broadcasted_iota(jnp.int32, (capacity, length), 0).astype(F32)
        place = column == slots[j][0, 0:1]
        span = pl.ds(pl.multiple_of(starts[j, s], 16), capacity)
        held = lax.broadcasted_iota(jnp.int32, (capacity, 1), 0) < starts[j, s + 1] - starts[j, s]
        rows = jnp.where(held, produced[j, span], 0.0).astype(BF16)
        grads = jnp.where(held, dx[j, span], 0.0).astype(BF16)
        out = dot(jnp.where(place, slots[j][0, 8:9], 0.0).astype(BF16), rows, 0, 0)
        grad = dot(jnp.where(place, 1.0, 0.0).astype(BF16), grads, 0, 0)
        out_sum = out if out_sum is None else out_sum + out
        grad_sum = grad if grad_sum is None else grad_sum + grad
    out_part[0] = out_sum.astype(BF16)
    grad_part[0] = grad_sum.astype(BF16)


def combine(starts, slots, produced, dx, capacity):
    local = len(slots)
    seqs, _, length = slots[0].shape
    width = produced.shape[2]
    seq = lambda i, *_: (i, 0, 0)
    rows = pl.BlockSpec(produced.shape, lambda i, *_: (0, 0, 0))
    return pl.pallas_call(
        functools.partial(combine_kernel, capacity, local),
        out_shape=(sds((seqs, length, width), BF16), sds((seqs, length, width), BF16)),
        grid_spec=pltpu.PrefetchScalarGridSpec(
            num_scalar_prefetch=1,
            grid=(seqs,),
            in_specs=[pl.BlockSpec((1, 16, length), seq)] * local + [rows] * 2,
            out_specs=(pl.BlockSpec((1, length, width), seq), pl.BlockSpec((1, length, width), seq)),
        ),
        compiler_params=pltpu.CompilerParams(dimension_semantics=("arbitrary",), vmem_limit_bytes=60 << 20),
        cost_estimate=pl.CostEstimate(flops=3 * 10**9, bytes_accessed=4 * 10**7, transcendentals=0),
        name="combine",
    )(starts, *slots, produced, dx)


def shards(
    tokens, cotangent, gate_weights, expert_ids, seq_lengths, query_weight, key_weight, value_weight,
    output_weight, attn_gain, ffn_gain, query_gain, key_gain, expert_in, expert_out,
):
    ep = lax.axis_size("ep")
    me = lax.axis_index("ep")
    seqs, rows, _ = tokens.shape
    length = rows * ep
    top = gate_weights.shape[2]
    local = expert_in.shape[0]
    hidden = expert_out.shape[1]
    experts = local * ep
    capacity = -(-(length * top * 9 // (8 * experts)) // 16) * 16

    gains = jnp.concatenate([attn_gain, ffn_gain]).astype(F32).reshape(-1, 128)
    few = [query_gain.astype(F32), key_gain.astype(F32), seq_lengths.astype(F32)]
    few = jnp.stack([jnp.pad(v, (0, 128 - v.shape[0])) for v in few])
    packet = jnp.concatenate([gains, few], axis=0)
    packet = jnp.pad(packet, ((0, -packet.shape[0] % 8), (0, 0)))
    share = gains.shape[0] // 2

    full, weights, cot_full, gains, small_in = front(
        tokens, cotangent, expert_ids.transpose(0, 2, 1), gate_weights.transpose(0, 2, 1),
        query_weight, key_weight, value_weight, packet,
    )

    half = HEAD_DIM // 2
    frequency = ROPE_BASE ** (-(np.arange(half, dtype=np.float32) * np.float32(2.0 / HEAD_DIM)))
    angles = np.arange(length, dtype=np.float32)[:, None] * frequency.astype(np.float32)[None, :]
    table = jnp.asarray(np.concatenate([np.cos(angles), np.sin(angles)], axis=-1), F32)

    if ep == 8 and lax.axis_size("rep") == 4:
        normed, pre, low, ctx, middle, mixed, cot_full, slots0, slots1, starts = attend_mix(
            top, local, full, weights, output_weight, gains, small_in, table, tokens, cotangent, cot_full
        )
    else:
        number = (me * local).astype(jnp.int32)[None]
        normed, pre, low, ctx, part, slots0, slots1, starts = attend(
            top, number, full, weights, output_weight, gains, small_in, table
        )
        starts = starts.astype(jnp.int32)
        middle, mixed = mix(part, tokens, small_in, gains)

    act, pair, x_all, dy_all, out_grad0 = expert_first(
        starts, mixed, cot_full, (slots0, slots1), expert_in, hidden, capacity
    )

    def over_rep(value, axis):
        return lax.psum_scatter(value, "rep", scatter_dimension=axis, tiled=True)

    out0 = over_rep(out_grad0, 0)
    dgu, in_grad = first_in_grad(seqs, starts, x_all, dy_all, pair, expert_out)
    act, dgu, in_grad, out_grad1 = expert_second(
        seqs, starts, x_all, dy_all, expert_in, expert_out, act, dgu, in_grad
    )
    in_both = over_rep(in_grad, 1)
    out1 = over_rep(out_grad1, 0)
    produced, dx = expert_tails(seqs, starts, act, dgu, expert_in, expert_out)
    out_part, grad_part = combine(starts, (slots0, slots1), produced, dx, capacity)

    mgrad, ffn_back, agrad = back(grad_part, middle, cotangent, small_in, gains)
    npart, wgrad, wograd, qk_back = attend_back(
        agrad, normed, pre, low, ctx, weights, output_weight, small_in, table
    )

    def widen(into, value, j):
        return lax.dynamic_update_slice(into, value.astype(F32)[None], (j, 0, 0))

    out_all = widen(jnp.zeros((local,) + out0.shape, F32), out0, 0)
    npart, out_all = lax.optimization_barrier((npart, out_all))
    sums, small, result, token_grad = finish(
        wgrad, wograd, npart, out_part, tokens, middle, mgrad, gains, ffn_back, qk_back
    )

    def head_share(vector):
        return lax.dynamic_slice_in_dim(vector, me * (HEAD_DIM // ep), HEAD_DIM // ep)

    return (
        result,
        token_grad,
        sums[1].astype(F32),
        sums[2].astype(F32),
        sums[3].astype(F32),
        sums[0].astype(F32),
        small[:share].reshape(-1),
        small[share : 2 * share].reshape(-1),
        head_share(small[2 * share]),
        head_share(small[2 * share + 1]),
        in_both.astype(F32),
        widen(out_all, out1, 1),
    )


def solution(mesh):
    seq = P("rep", "ep", None)
    row, gain, expert = P("ep", None), P("ep"), P("ep", None, None)
    split = P("ep", "rep", None)

    return jax.shard_map(
        shards,
        mesh=mesh,
        in_specs=(seq, seq, seq, seq, P(("rep", "ep")), row, row, row, row, gain, gain, gain, gain, expert, expert),
        out_specs=(seq, seq, row, row, row, row, gain, gain, gain, gain, split, split),
        check_vma=False,
    )
```

```python
import functools

import jax
import jax.numpy as jnp
import numpy as np
from jax import lax
from jax.experimental import pallas as pl
from jax.experimental.pallas import tpu as pltpu
from jax.sharding import PartitionSpec as P

HEAD_DIM = 128
EPS = 1e-06
ROPE_BASE = 50000.0
MESH = pl.DeviceIdType.MESH
F32 = jnp.float32
BF16 = jnp.bfloat16


def sds(shape, dtype):
    return jax.ShapeDtypeStruct(shape, dtype)


VM = pl.BlockSpec(memory_space=pltpu.VMEM)
AN = pl.BlockSpec(memory_space=pl.ANY)


def inverse_rms(v):
    return lax.rsqrt(jnp.mean(v * v, axis=-1, keepdims=True) + EPS)


def rms_back(v, r, ug):
    return r * ug - v * (r * r * r * jnp.mean(ug * v, axis=-1, keepdims=True))


def mix_rows(total, tok, living, gain):
    middle = tok.astype(F32) + living * total
    mixed = middle * inverse_rms(middle) * gain
    return middle, mixed.astype(BF16)


def ffn_back_rows(mixed_grad, middle, cot, living, gain):
    r = inverse_rms(middle)
    middle_grad = cot.astype(F32) + rms_back(middle, r, mixed_grad * gain)
    return middle_grad, (living * middle_grad).astype(BF16), mixed_grad * middle * r


def attn_back_rows(normed_grad, tok, middle_grad, gain):
    v = tok.astype(F32)
    r = inverse_rms(v)
    return (middle_grad + rms_back(v, r, normed_grad * gain)).astype(BF16), normed_grad * v * r


def seq_len(small, s):
    lane = lax.broadcasted_iota(jnp.int32, (1, 128), 1)
    return jnp.sum(jnp.where(lane == s, small[2:3, :], 0.0), axis=1, keepdims=True)


def live_rows(small, s, me, rows):
    place = (lax.broadcasted_iota(jnp.int32, (rows, 1), 0) + me * rows).astype(F32)
    return jnp.where(place < seq_len(small, s), 1.0, 0.0)


class Place:
    def __init__(self):
        me = lax.axis_index("ep")
        core, x, y = lax.rem(me, 2), lax.rem(me // 2, 2), me // 4
        self.rep = lax.axis_index("rep")
        self.me = me
        self.sb = me + 1 - 2 * core
        self.dx = 2 - 4 * x
        self.dy = 4 - 8 * y
        self.xn = me + self.dx
        self.yn = me + self.dy
        self.dg = me + self.dx + self.dy

    def push(self, src, dst, send, recv, dev):
        return pltpu.make_async_remote_copy(
            src_ref=src, dst_ref=dst, send_sem=send, recv_sem=recv, device_id=(self.rep, dev), device_id_type=MESH
        )

    def peers(self):
        sb, dx, dy = self.sb, self.dx, self.dy
        return (self.xn, self.yn, self.dg, sb, sb + dx, sb + dy, sb + dx + dy)

    def greet(self, peers):
        barrier = pltpu.get_barrier_semaphore()
        for peer in peers:
            pl.semaphore_signal(barrier, inc=1, device_id=(self.rep, peer), device_id_type=MESH)
        pl.semaphore_wait(barrier, len(peers))


class Gather:
    sems = 3

    def __init__(self, at, own, full, ssem, rsem, lsem):
        self.at, self.own, self.full, self.ssem, self.rsem, self.lsem = at, own, full, ssem, rsem, lsem
        self.rows = own.shape[1]

    @staticmethod
    def scratch(seqs):
        return [pltpu.SemaphoreType.DMA((7, seqs)), pltpu.SemaphoreType.DMA((8, seqs)), pltpu.SemaphoreType.DMA((seqs,))]

    def block(self, s, dev):
        return self.full.at[s, pl.ds(pl.multiple_of(dev * self.rows, self.rows), self.rows)]

    def copy(self, s, dev, kind, slot, to, src=None):
        block = self.block(s, dev)
        return self.at.push(block if src is None else src, block, self.ssem.at[kind, s], self.rsem.at[slot, s], to)

    def start(self, s):
        at, own = self.at, self.own.at[s]
        self.copy(s, at.me, 0, 2, at.xn, own).start()
        self.copy(s, at.me, 1, 4, at.yn, own).start()
        self.copy(s, at.me, 2, 1, at.sb, own).start()
        pltpu.make_async_copy(own, self.block(s, at.me), self.lsem.at[s]).start()

    def relay(self, s, by_y):
        at = self.at
        self.copy(s, at.xn, 0, 2, at.xn).wait_recv()
        if by_y:
            self.copy(s, at.xn, 3, 6, at.yn).start()
        self.copy(s, at.xn, 4, 3, at.sb).start()
        self.copy(s, at.yn, 1, 4, at.yn).wait_recv()
        if not by_y:
            self.copy(s, at.yn, 3, 6, at.xn).start()
        self.copy(s, at.yn, 5, 5, at.sb).start()

    def relay_far(self, s):
        at = self.at
        self.copy(s, at.dg, 3, 6, at.yn).wait_recv()
        self.copy(s, at.dg, 6, 7, at.sb).start()

    def finish(self, s):
        at = self.at
        for dev, slot in ((at.sb, 1), (at.sb + at.dx, 3), (at.sb + at.dy, 5), (at.sb + at.dx + at.dy, 7)):
            self.copy(s, dev, 0, slot, at.sb).wait_recv()
        for kind in range(7):
            self.copy(s, at.me, kind, 0, at.sb).wait_send()
        pltpu.make_async_copy(self.own.at[s], self.block(s, at.me), self.lsem.at[s]).wait()


def gather_tail(gather, low, high):
    def relay(i, _):
        gather.relay(low + 2 * i, True)
        gather.relay(low + 2 * i + 1, False)
        return 0

    lax.fori_loop(0, (high - low) // 2, relay, 0)
    each(high, gather.relay_far, low=low)
    each(high, gather.finish, low=low)


class Reduce:
    def __init__(self, at, part, held, mine, x1, y1, x2, y2, ms, hs, hr, d1s, d1r, d2s, d2r):
        self.at, self.part, self.held, self.mine = at, part, held, mine
        self.x1, self.y1, self.x2, self.y2 = x1, y1, x2, y2
        self.ms, self.hs, self.hr, self.d1s, self.d1r, self.d2s, self.d2r = ms, hs, hr, d1s, d1r, d2s, d2r
        self.half = part.shape[2] // 2

    @staticmethod
    def scratch(part):
        s, _, t, d = part.shape
        dma = pltpu.SemaphoreType.DMA
        return [
            pltpu.VMEM((s, 4, t, d), BF16),
            pltpu.VMEM((s, 4, t, d), BF16),
            pltpu.VMEM((s, t // 2, d), BF16),
            pltpu.VMEM((s, t // 2, d), BF16),
            pltpu.VMEM((s, t, d), BF16),
            pltpu.VMEM((s, t, d), BF16),
            dma((4, s)),
            dma((4, s)),
            dma((4, s)),
            dma((2, s)),
            dma((2, s)),
            dma((2, s)),
            dma((2, s)),
        ]

    sems = 13

    def core_copy(self, s, k):
        at = self.at
        dest = (at.sb, at.sb + at.dx, at.sb + at.dy, at.sb + at.dx + at.dy)[k]
        return at.push(self.part.at[s, dest], self.held.at[s, k], self.hs.at[k, s], self.hr.at[k, s], at.sb)

    def load(self, s, k):
        at = self.at
        dest = (at.me, at.xn, at.yn, at.dg)[k]
        return pltpu.make_async_copy(self.part.at[s, dest], self.mine.at[s, k], self.ms.at[k, s])

    def first(self, s, k):
        at, h = self.at, self.half
        src = self.held.at[s, 3, pl.ds(k * h, h)]
        return at.push(src, (self.x1, self.y1)[k].at[s], self.d1s.at[k, s], self.d1r.at[k, s], (at.xn, at.yn)[k])

    def second(self, s, k):
        at = self.at
        src = self.held.at[s, 1 + k]
        return at.push(src, (self.x2, self.y2)[k].at[s], self.d2s.at[k, s], self.d2r.at[k, s], (at.xn, at.yn)[k])

    def start(self, s):
        for k in (3, 1, 2, 0):
            self.core_copy(s, k).start()
            self.load(s, k).start()

    def hop1(self, s):
        self.core_copy(s, 3).wait_recv()
        self.load(s, 3).wait()
        self.held[s, 3] = (self.held[s, 3].astype(F32) + self.mine[s, 3].astype(F32)).astype(BF16)
        self.first(s, 0).start()
        self.first(s, 1).start()

    def hop2(self, s):
        h = self.half
        for k, extra, rows, rest in (
            (0, self.y1, pl.ds(h, h), pl.ds(0, h)),
            (1, self.x1, pl.ds(0, h), pl.ds(h, h)),
        ):
            self.core_copy(s, 1 + k).wait_recv()
            self.load(s, 1 + k).wait()
            self.first(s, 1 - k).wait_recv()
            held, mine = self.held.at[s, 1 + k], self.mine.at[s, 1 + k]
            held[rows] = (held[rows].astype(F32) + mine[rows].astype(F32) + extra[s].astype(F32)).astype(BF16)
            held[rest] = (held[rest].astype(F32) + mine[rest].astype(F32)).astype(BF16)
            self.second(s, k).start()

    def total(self, s):
        self.core_copy(s, 0).wait_recv()
        self.load(s, 0).wait()
        self.second(s, 0).wait_recv()
        self.second(s, 1).wait_recv()
        return (
            self.mine[s, 0].astype(F32)
            + self.held[s, 0].astype(F32)
            + self.x2[s].astype(F32)
            + self.y2[s].astype(F32)
        )

    def finish(self, s):
        for k in range(4):
            self.core_copy(s, k).wait_send()
        for k in range(2):
            self.first(s, k).wait_send()
            self.second(s, k).wait_send()


def each(n, *steps, low=0):
    def run(s, _):
        for step in steps:
            step(s)
        return 0

    lax.fori_loop(low, n, run, 0)


COMM = dict(has_side_effects=True, vmem_limit_bytes=60 << 20)


def front_kernel(
    tok, cot, ids, gates, wq, wk, wv, pk, full, weights, cot_full, gains, small,
    packets, own, gsend, grecv, glocal, csend, crecv, clocal,
    wsend, wrecv, psend, precv, rsend, rrecv, lsend, lrecv, local,
):
    at = Place()
    z = at.rep
    gather = Gather(at, own, full, gsend, grecv, glocal)
    cot_gather = Gather(at, cot, cot_full, csend, crecv, clocal)
    seqs, _, width = tok.shape
    top = ids.shape[1]
    block, cols = wq.shape[0], weights.shape[2]
    quarter = block // 4
    peers = at.peers()
    barrier = pltpu.get_barrier_semaphore()
    line = [lax.rem(z + k, 4) for k in range(1, 4)]
    for dev in line:
        pl.semaphore_signal(barrier, inc=1, device_id=(dev, at.me), device_id_type=MESH)
    for dev in peers:
        pl.semaphore_signal(barrier, inc=1, device_id=(z, dev), device_id_type=MESH)
    pl.semaphore_wait(barrier, 10)

    def packet_copy(m, dev):
        return at.push(pk, packets.at[at.me], psend.at[m], precv.at[m], dev)

    def weight_copy(m, j, dev):
        theirs = pl.ds(pl.multiple_of(dev * cols, cols), cols)
        src = (wq, wk, wv)[j].at[pl.ds(pl.multiple_of(z * quarter, quarter), quarter), theirs]
        dst = weights.at[j, pl.ds(pl.multiple_of(at.me * block + z * quarter, quarter), quarter)]
        return at.push(src, dst, wsend.at[m, j], wrecv.at[m, j], dev)

    def weight_landed(m, j, dev):
        dst = weights.at[j, pl.ds(pl.multiple_of(dev * block + z * quarter, quarter), quarter)]
        return at.push(dst, dst, wsend.at[m, j], wrecv.at[m, j], dev)

    def walk(m, q, right):
        part = weights.at[:, pl.ds(pl.multiple_of(peers[m] * block + q * quarter, quarter), quarter)]
        send, recv, dev = (rsend, rrecv, z + 1) if right else (lsend, lrecv, z - 1)
        return pltpu.make_async_remote_copy(
            src_ref=part, dst_ref=part, send_sem=send.at[m, q], recv_sem=recv.at[m, q],
            device_id=(dev, at.me), device_id_type=MESH,
        )

    for m, dev in enumerate(peers):
        packet_copy(m, dev).start()
        for j in range(3):
            weight_copy(m, j, dev).start()

    place = lax.broadcasted_iota(jnp.int32, (top, 128), 0)
    lane = lax.broadcasted_iota(jnp.int32, (top, 128), 1)
    first = jnp.where(lane == place, 1.0, 0.0).astype(BF16)
    second = jnp.where(lane == place + top, 1.0, 0.0).astype(BF16)

    def join(s):
        own[s, :, 0:width] = tok[s]
        table = dot(ids[s].astype(F32).astype(BF16), first, 0, 0) + dot(gates[s], second, 0, 0)
        own[s, :, width : width + 128] = table.astype(BF16)

    each(seqs, join)
    each(seqs, gather.start)
    own_cols = pl.ds(pl.multiple_of(at.me * cols, cols), cols)
    mine = pl.ds(pl.multiple_of(at.me * block, block), block)
    own_weights = [
        pltpu.make_async_copy(w.at[:, own_cols], weights.at[j, mine], local.at[j]) for j, w in enumerate((wq, wk, wv))
    ]
    for copy in own_weights:
        copy.start()
    early = seqs // 2
    each(early, cot_gather.start)

    for m, dev in enumerate(peers):
        for j in range(3):
            weight_landed(m, j, dev).wait_recv()

        @pl.when(z < 3)
        def _():
            walk(m, z, True).start()

        @pl.when(z > 0)
        def _():
            walk(m, z, False).start()

    def pass_on(d):
        @pl.when(z - d >= 0)
        def _():
            for m in range(7):
                walk(m, z - d, True).wait_recv()

                @pl.when(z < 3)
                def _():
                    walk(m, z - d, True).start()

        @pl.when(z + d <= 3)
        def _():
            for m in range(7):
                walk(m, z + d, False).wait_recv()

                @pl.when(z > 0)
                def _():
                    walk(m, z + d, False).start()

    def relay(i, _):
        gather.relay(2 * i, True)
        gather.relay(2 * i + 1, False)
        return 0

    def cot_relay(i, _):
        cot_gather.relay(2 * i, True)
        cot_gather.relay(2 * i + 1, False)
        return 0

    pairs = seqs // 2
    lax.fori_loop(0, pairs // 2, relay, 0)
    pass_on(1)
    lax.fori_loop(pairs // 2, pairs, relay, 0)
    pass_on(2)
    lax.fori_loop(0, early // 2, cot_relay, 0)
    each(seqs, gather.relay_far)
    each(early, cot_gather.relay_far)
    for m, dev in enumerate(peers):
        packet_copy(m, dev).wait_recv()
    packets[at.me] = pk[...]
    devices = packets.shape[0]
    share = width // (128 * devices)
    heads = HEAD_DIM // devices
    gains[...] = jnp.zeros_like(gains)
    small[...] = jnp.zeros_like(small)
    for o in range(devices):
        for k in range(share):
            lanes = pl.ds((o * share + k) * 128, 128)
            gains[0:1, lanes] = packets[o, k : k + 1]
            gains[1:2, lanes] = packets[o, share + k : share + k + 1]
        base = 2 * share
        small[0:1] += pltpu.roll(packets[o, base : base + 1], o * heads, 1)
        small[1:2] += pltpu.roll(packets[o, base + 1 : base + 2], o * heads, 1)
        small[2:3] += pltpu.roll(packets[o, base + 2 : base + 3], o, 1)
    each(seqs, gather.finish)
    each(early, cot_gather.finish)
    pass_on(3)

    def sent(q, going, right):
        @pl.when(going)
        def _():
            for m in range(7):
                walk(m, q, right).wait_send()

    for q in range(4):
        sent(q, jnp.logical_and(q <= z, z < 3), True)
        sent(q, jnp.logical_and(q >= z, z > 0), False)
    for m, dev in enumerate(peers):
        packet_copy(m, dev).wait_send()
        for j in range(3):
            weight_copy(m, j, dev).wait_send()
    for copy in own_weights:
        copy.wait()


def front(tokens, cotangent, ids, gates, wq, wk, wv, packet):
    seqs, rows, width = tokens.shape
    ep = lax.axis_size("ep")
    cols = wq.shape[1] // ep
    top = ids.shape[1]
    if ep != 8 or lax.axis_size("rep") != 4:
        routes = jnp.concatenate([ids.astype(BF16), gates], axis=1).transpose(0, 2, 1)
        routes = jnp.pad(routes, ((0, 0), (0, 0), (0, 128 - 2 * top)))
        full = lax.all_gather(jnp.concatenate([tokens, routes], axis=-1), "ep", axis=1, tiled=True)
        weights = [lax.all_to_all(w, "ep", split_axis=1, concat_axis=0, tiled=True) for w in (wq, wk, wv)]
        packets = lax.all_gather(packet, "ep", axis=0)
        share, heads = width // (128 * ep), HEAD_DIM // ep
        gains = jnp.stack([packets[:, :share].reshape(width), packets[:, share : 2 * share].reshape(width)])
        lens = jnp.pad(packets[:, 2 * share + 2, 0], (0, 128 - ep))
        few = [packets[:, 2 * share + k, :heads].reshape(HEAD_DIM) for k in range(2)] + [lens]
        return (
            full, jnp.stack(weights), lax.all_gather(cotangent, "ep", axis=1, tiled=True),
            jnp.pad(gains, ((0, 6), (0, 0))), jnp.pad(jnp.stack(few), ((0, 5), (0, 0))),
        )
    dma = pltpu.SemaphoreType.DMA
    return pl.pallas_call(
        front_kernel,
        out_shape=(
            sds((seqs, rows * ep, width + 128), BF16),
            sds((3, wq.shape[0] * ep, cols), BF16),
            sds((seqs, rows * ep, width), BF16),
            sds((8, width), F32),
            sds((8, 128), F32),
        ),
        in_specs=[VM] * 8,
        out_specs=(AN, AN, AN, VM, VM),
        scratch_shapes=[pltpu.VMEM((ep,) + packet.shape, F32), pltpu.VMEM((seqs, rows, width + 128), BF16)]
        + Gather.scratch(seqs)
        + Gather.scratch(seqs)
        + [dma((7, 3)), dma((7, 3)), dma((7,)), dma((7,))]
        + [dma((7, 4))] * 4
        + [dma((3,))],
        compiler_params=pltpu.CompilerParams(collective_id=1, **COMM),
        name="front",
    )(tokens, cotangent, ids, gates, wq, wk, wv, packet)


def plain_living(small, seqs, rows):
    place = (jnp.arange(rows) + lax.axis_index("ep") * rows).astype(F32)
    return (place[None] < small[2, :seqs, None]).astype(F32)[..., None]


def mix(part, tokens, small, gains):
    seqs, rows, _ = tokens.shape
    total = lax.psum_scatter(part, "ep", scatter_dimension=1, tiled=True).astype(F32)
    middle, mixed = mix_rows(total, tokens, plain_living(small, seqs, rows), gains[1])
    return middle, lax.all_gather(mixed, "ep", axis=1, tiled=True)


def back_kernel(gpart, middle, cot, small, gains, mgrad, ggrad, full, own, *scratch):
    at = Place()
    seqs = cot.shape[0]
    n = Reduce.sems
    rg = Reduce(at, gpart, *scratch[:n])
    gather = Gather(at, own, full, *scratch[n:])
    at.greet((at.xn, at.yn, at.sb))
    each(seqs, rg.start)
    each(seqs, rg.hop1)
    each(seqs, rg.hop2)
    ggrad[...] = jnp.zeros_like(ggrad)

    def rows(s):
        living = live_rows(small, s, at.me, cot.shape[1])
        mg, ag, back = ffn_back_rows(rg.total(s), middle[s], cot[s], living, gains[1:2])
        mgrad[s] = mg
        own[s] = ag
        ggrad[...] += jnp.sum(back, axis=0, keepdims=True)
        gather.start(s)

    each(seqs, rows)
    gather_tail(gather, 0, seqs)
    each(seqs, rg.finish)


def back(gpart, middle, cot, small, gains):
    seqs, rows, width = cot.shape
    ep = lax.axis_size("ep")
    if ep != 8:
        mixed_grad = lax.psum_scatter(gpart, "ep", scatter_dimension=1, tiled=True).astype(F32)
        mg, ag, backs = ffn_back_rows(mixed_grad, middle, cot, plain_living(small, seqs, rows), gains[1])
        full = lax.all_gather(ag, "ep", axis=1, tiled=True)
        return mg, jnp.sum(backs, axis=(0, 1))[None], full
    gpart = gpart.reshape(seqs, ep, rows, width)
    return pl.pallas_call(
        back_kernel,
        out_shape=(
            sds(cot.shape, F32),
            sds((1, width), F32),
            sds((seqs, rows * ep, width), BF16),
        ),
        in_specs=[AN] + [VM] * 4,
        out_specs=(VM, VM, AN),
        scratch_shapes=[pltpu.VMEM(cot.shape, BF16)] + Reduce.scratch(gpart) + Gather.scratch(seqs),
        compiler_params=pltpu.CompilerParams(collective_id=3, **COMM),
        name="back",
    )(gpart, middle, cot, small, gains)


def finish_kernel(
    wgrad, wograd, npart, opart, tok, middle, mgrad, gains, others,
    out, small_out, result, tgrad,
    own, held, met, ggrad, parcel, landed, spare,
    wsend, wrecv, local, gsend, grecv, os, or_, ps, pr, qs, qr, fs, fr, ss, sr, *scratch,
):
    at = Place()
    z, me = at.rep, at.me
    n = Reduce.sems
    normed_sum = Reduce(at, npart, *scratch[:n])
    result_sum = Reduce(at, opart, *scratch[n:])
    seqs = tok.shape[0]
    parts, pieces = own.shape[:2]
    chunks = parts * pieces
    width = wgrad.shape[3]
    peers = at.peers()
    barrier = pltpu.get_barrier_semaphore()
    line = [lax.rem(z + k, 4) for k in range(1, 4)]
    for dev in line:
        pl.semaphore_signal(barrier, inc=1, device_id=(dev, me), device_id_type=MESH)
    for dev in peers:
        pl.semaphore_signal(barrier, inc=1, device_id=(z, dev), device_id_type=MESH)
    pl.semaphore_wait(barrier, 10)
    inner = jnp.logical_and(z > 0, z < 3)
    outer_end, partner, outer = 1 + z // 3, 3 - z, 3 * (z - 1)
    cols = pl.ds(pl.multiple_of(me * width, width), width)

    def column_copy(m, j, dev):
        rows = pl.ds(pl.multiple_of(dev * pieces, pieces), pieces)
        return at.push(wgrad.at[j, rows], own.at[1 + j, :, :, cols], wsend.at[m, j], wrecv.at[m, j], dev)

    mine_rows = pl.ds(pl.multiple_of(me * pieces, pieces), pieces)
    locals_ = [pltpu.make_async_copy(wgrad.at[j, mine_rows], own.at[1 + j, :, :, cols], local.at[j]) for j in range(3)]
    locals_.append(pltpu.make_async_copy(wograd, own.at[0], local.at[3]))
    for copy in locals_:
        copy.start()
    for j in range(3):
        for m, dev in enumerate(peers):
            column_copy(m, j, dev).start()
    each(seqs, normed_sum.start)
    each(seqs, result_sum.start)
    ggrad[...] = jnp.zeros_like(ggrad)

    def piece(ref, c):
        return ref.at[c // pieces, lax.rem(c, pieces)]

    def line_push(src, dst, send, recv, dev):
        return pltpu.make_async_remote_copy(
            src_ref=src, dst_ref=dst, send_sem=send, recv_sem=recv, device_id=(dev, me), device_id_type=MESH
        )

    def inward(c):
        return line_push(piece(own, c), piece(held, c), os.at[c], or_.at[c], outer_end)

    def across(c):
        return line_push(piece(held, c), met.at[c // 2], ps.at[c], pr.at[c], partner)

    def share(c):
        return line_push(piece(out, c), piece(out, c), qs.at[c], qr.at[c], partner)

    def outward(c):
        return line_push(piece(out, c), piece(out, c), fs.at[c], fr.at[c], outer)

    def mine(c):
        return 1 + lax.rem(c, 2) == z

    def ready(part):
        for j in range(parts):

            @pl.when(part == j)
            def _():
                locals_[(3, 0, 1, 2)[j]].wait()
                if j > 0:
                    for m, dev in enumerate(peers):
                        column_copy(m, j - 1, dev).wait_recv()

    def step(c):
        @pl.when(lax.rem(c, pieces) == 0)
        def _():
            ready(c // pieces)

        @pl.when(jnp.logical_not(inner))
        def _():
            inward(c).start()

        @pl.when(inner)
        def _():
            inward(c).wait_recv()
            here = piece(held, c)
            here[...] = (here[...].astype(F32) + piece(own, c)[...].astype(F32)).astype(BF16)

            @pl.when(jnp.logical_not(mine(c)))
            def _():
                across(c).start()

    def settle(c):
        @pl.when(jnp.logical_and(inner, mine(c)))
        def _():
            across(c).wait_recv()
            piece(out, c)[...] = (piece(held, c)[...].astype(F32) + met[c // 2].astype(F32)).astype(BF16)
            share(c).start()
            outward(c).start()

    def forward(c):
        @pl.when(jnp.logical_and(inner, jnp.logical_not(mine(c))))
        def _():
            share(c).wait_recv()
            outward(c).start()

    def token_rows(s):
        tg, back = attn_back_rows(normed_sum.total(s), tok[s], mgrad[s], gains[0:1])
        tgrad[s] = tg
        ggrad[...] += jnp.sum(back, axis=0, keepdims=True)

    def out_rows(s):
        result[s] = (middle[s] + result_sum.total(s)).astype(BF16)

    jobs = (
        (step, 0, chunks), (settle, 1, chunks), (forward, 2, chunks),
        (normed_sum.hop1, 2, seqs), (normed_sum.hop2, 6, seqs), (token_rows, 10, seqs),
        (result_sum.hop1, 6, seqs), (result_sum.hop2, 10, seqs), (out_rows, 14, seqs),
    )

    def tick(i, _):
        for job, lag, count in jobs:

            @pl.when(jnp.logical_and(i >= lag, i < lag + count))
            def _():
                job(i - lag)

        return 0

    lax.fori_loop(0, max(lag + count for _, lag, count in jobs), tick, 0)

    parcel[...] = jnp.zeros_like(parcel)
    devices = parcel.shape[0]
    rows_of = ggrad.shape[1] // (128 * devices)
    for dev in range(devices):
        for k in range(rows_of):
            lanes = pl.ds((dev * rows_of + k) * 128, 128)
            parcel[dev, k : k + 1] = ggrad[:, lanes]
            parcel[dev, rows_of + k : rows_of + k + 1] = others[0:1, lanes]
        parcel[dev, 2 * rows_of : 2 * rows_of + 2] = others[1:3, 0:128]

    def parcel_copy(m, dev):
        return at.push(parcel.at[dev], landed.at[m], gsend.at[m], grecv.at[m], dev)

    for m, dev in enumerate(peers):
        parcel_copy(m, dev).start()
    total = parcel[me]
    for m, dev in enumerate(peers):
        parcel_copy(m, dev).wait_recv()
        total = total + landed[m]
    spare[0] = total

    def small_copy(k):
        return line_push(spare.at[0], spare.at[1 + k], ss.at[k], sr.at[k], line[k])

    for k in range(3):
        small_copy(k).start()

    @pl.when(jnp.logical_not(inner))
    def _():
        each(chunks, lambda c: outward(c).wait_recv())
        each(chunks, lambda c: inward(c).wait_send())

    @pl.when(inner)
    def _():
        def sent(c):
            outward(c).wait_send()

            @pl.when(mine(c))
            def _():
                share(c).wait_send()

            @pl.when(jnp.logical_not(mine(c)))
            def _():
                across(c).wait_send()

        each(chunks, sent)

    each(seqs, normed_sum.finish, result_sum.finish)
    for m, dev in enumerate(peers):
        parcel_copy(m, dev).wait_send()
        for j in range(3):
            column_copy(m, j, dev).wait_send()
    total = spare[0]
    for k in range(3):
        small_copy(k).wait()
        total = total + spare[1 + k]
    small_out[...] = total


def finish(wgrad, wograd, npart, opart, tokens, middle, mgrad, gains, ffn_back, qk_back):
    seqs, rows, width = tokens.shape
    ep = lax.axis_size("ep")
    if ep != 8 or lax.axis_size("rep") != 4:
        normed_grad = lax.psum_scatter(npart, "ep", scatter_dimension=1, tiled=True).astype(F32)
        moe = lax.psum_scatter(opart, "ep", scatter_dimension=1, tiled=True).astype(F32)
        tg, backs = attn_back_rows(normed_grad, tokens, mgrad, gains[0])
        wrows = lax.all_to_all(wgrad, "ep", split_axis=1, concat_axis=2, tiled=True)
        share = width // ep
        small = jnp.concatenate([jnp.sum(backs, axis=(0, 1)), ffn_back[0], qk_back[0], qk_back[1]])
        small = lax.psum(small, ("ep", "rep"))
        mine = lax.axis_index("ep") * share
        cut = [lax.dynamic_slice_in_dim(small, k * width + mine, share).reshape(-1, 128) for k in range(2)]
        small = jnp.concatenate(cut + [small[2 * width :].reshape(2, HEAD_DIM)], axis=0)
        big = lax.psum(jnp.concatenate([wograd[None], wrows], axis=0), "rep")
        return big, jnp.pad(small, ((0, 8 - small.shape[0]), (0, 0))), (middle + moe).astype(BF16), tg
    others = jnp.concatenate([ffn_back, jnp.pad(qk_back[:2], ((0, 0), (0, width - HEAD_DIM)))], axis=0)
    npart, opart = (p.reshape(seqs, ep, rows, width) for p in (npart, opart))
    pieces = 4
    block = wograd.shape[0] // pieces
    wgrad = wgrad.reshape(3, wgrad.shape[1] // block, block, wgrad.shape[2])
    wograd = wograd.reshape(pieces, block, width)
    whole = (4, pieces, block, width)
    dma = pltpu.SemaphoreType.DMA
    chunks = 4 * pieces
    out, small, result, tgrad = pl.pallas_call(
        finish_kernel,
        out_shape=(sds(whole, BF16), sds((8, 128), F32), sds(tokens.shape, BF16), sds(tokens.shape, BF16)),
        in_specs=[VM, VM, AN, AN] + [VM] * 5,
        out_specs=(VM, VM, VM, VM),
        scratch_shapes=[
            pltpu.VMEM(whole, BF16),
            pltpu.VMEM(whole, BF16),
            pltpu.VMEM((chunks // 2, block, width), BF16),
            pltpu.VMEM((1, width), F32),
            pltpu.VMEM((ep, 8, 128), F32),
            pltpu.VMEM((7, 8, 128), F32),
            pltpu.VMEM((4, 8, 128), F32),
        ]
        + [dma((7, 3)), dma((7, 3)), dma((4,)), dma((7,)), dma((7,))]
        + [dma((chunks,))] * 8
        + [dma((3,))] * 2
        + 2 * Reduce.scratch(npart),
        compiler_params=pltpu.CompilerParams(collective_id=4, has_side_effects=True, vmem_limit_bytes=61 << 20),
        name="finish",
    )(wgrad, wograd, npart, opart, tokens, middle, mgrad, gains, others)
    return out.reshape(4, pieces * block, width), small, result, tgrad


def dot(a, b, ca, cb):
    return lax.dot_general(a, b, (((ca,), (cb,)), ((), ())), preferred_element_type=F32)


def rope_tables(table):
    half = HEAD_DIM // 2
    values = table[...]
    turned = pltpu.roll(values, half, 1)
    first = lax.broadcasted_iota(jnp.int32, values.shape, 1) < half
    return jnp.where(first, values, turned), jnp.where(first, -turned, values)


def rope(v, cos, sin_turn):
    return v * cos + pltpu.roll(v, HEAD_DIM // 2, 1) * sin_turn


def probabilities(q, k, length):
    scores = dot(q, k, 1, 1) * HEAD_DIM**-0.5
    column = lax.broadcasted_iota(jnp.int32, (1, scores.shape[1]), 1).astype(F32)
    scores = jnp.where(column < length, scores, -1e9)
    p = jnp.exp(scores - jnp.max(scores, axis=-1, keepdims=True))
    return p * (1.0 / jnp.sum(p, axis=-1, keepdims=True))


def packed_slots(number, table, length_live, top):
    tab = table.astype(F32)
    length = tab.shape[0]
    lane = lax.broadcasted_iota(jnp.int32, tab.shape, 1)
    row = lax.broadcasted_iota(jnp.int32, (length, 1), 0).astype(F32)
    chosen = jnp.logical_and(jnp.logical_and(tab == number, lane < top), row < length_live)
    gates = jnp.where(chosen, pltpu.roll(tab, 128 - top, 1), 0.0).astype(BF16)
    chosen = jnp.where(chosen, 1.0, 0.0).astype(BF16)
    ones = jnp.ones((8, 128), BF16)
    hit = dot(ones, chosen, 1, 1)
    weight = dot(ones, gates, 1, 1)
    earlier = lax.broadcasted_iota(jnp.int32, (length, length), 0)
    later = lax.broadcasted_iota(jnp.int32, (length, length), 1)
    rank = dot(hit.astype(BF16), jnp.where(earlier < later, 1.0, 0.0).astype(BF16), 1, 0)
    return jnp.where(hit > 0.5, rank, -1.0), weight, jnp.sum(hit[0:1], axis=1, keepdims=True)


def attend_rows(top, number, s, block, w, wo, gains, small, table, normed, pre, low, ctx, part, slots, starts):
    width = normed.shape[1]
    length = seq_len(small, s)
    cos, sin = rope_tables(table)
    v = block[:, 0:width].astype(F32)
    x = (v * inverse_rms(v) * gains[0:1]).astype(BF16)
    normed[...] = x
    q_pre, k_pre = dot(x, w[0], 1, 0), dot(x, w[1], 1, 0)
    value = dot(x, w[2], 1, 0).astype(BF16)
    pre[0], pre[1] = q_pre, k_pre
    low[2] = value
    for h in range(q_pre.shape[1] // HEAD_DIM):
        cols = slice(h * HEAD_DIM, (h + 1) * HEAD_DIM)
        rot = []
        for i, (u, g) in enumerate(((q_pre[:, cols], small[0:1]), (k_pre[:, cols], small[1:2]))):
            rot.append(rope(u * inverse_rms(u) * g, cos, sin).astype(BF16))
            low[i, :, cols] = rot[i]
        attention = probabilities(rot[0], rot[1], length).astype(BF16)
        ctx[:, cols] = dot(attention, value[:, cols], 1, 0).astype(BF16)
    part[...] = dot(ctx[...], wo[...], 1, 0).astype(BF16).reshape(part.shape)
    routes = block[:, width : width + 128]
    lane = lax.broadcasted_iota(jnp.int32, (1, 128), 1)
    for j, ref in enumerate(slots):
        slot, weight, count = packed_slots(number + j, routes, length, top)
        ref[0:8] = slot
        ref[8:16] = weight
        row = starts[j : j + 1]
        after = jnp.sum(jnp.where(lane == s, row, 0.0), axis=1, keepdims=True) + 16.0 * jnp.floor((count + 15.0) * 0.0625)
        starts[j : j + 1] = jnp.where(lane == s + 1, after, row)


def attend_kernel(top, number, full, w, wo, gains, small, table, normed, pre, low, ctx, part, slots0, slots1, starts):
    s = pl.program_id(0)

    @pl.when(s == 0)
    def _():
        starts[...] = jnp.zeros_like(starts)

    attend_rows(
        top, number[0].astype(F32), s, full.at[0], w, wo, gains, small, table,
        normed.at[0], pre.at[:, 0], low.at[:, 0], ctx.at[0], part.at[0], (slots0.at[0], slots1.at[0]), starts,
    )


def attend(top, number, full, weights, wo, gains, small, table):
    seqs, length, wide = full.shape
    width = wide - 128
    cols = weights.shape[2]
    row = lambda i, *_: (i, 0, 0)
    row2 = lambda i, *_: (0, i, 0, 0)
    two = lambda i, *_: (0, 0)
    slot = pl.BlockSpec((1, 16, length), row)
    return pl.pallas_call(
        functools.partial(attend_kernel, top),
        out_shape=(
            sds((seqs, length, width), BF16),
            sds((2, seqs, length, cols), F32),
            sds((3, seqs, length, cols), BF16),
            sds((seqs, length, cols), BF16),
            sds((seqs, length, width), BF16),
            sds((seqs, 16, length), F32),
            sds((seqs, 16, length), F32),
            sds((8, 128), F32),
        ),
        grid_spec=pltpu.PrefetchScalarGridSpec(
            num_scalar_prefetch=1,
            grid=(seqs,),
            in_specs=[
                pl.BlockSpec((1, length, wide), row),
                pl.BlockSpec(weights.shape, lambda i, *_: (0, 0, 0)),
                pl.BlockSpec(wo.shape, two),
                pl.BlockSpec((8, width), two),
                pl.BlockSpec((8, 128), two),
                pl.BlockSpec((length, HEAD_DIM), two),
            ],
            out_specs=(
                pl.BlockSpec((1, length, width), row),
                pl.BlockSpec((2, 1, length, cols), row2),
                pl.BlockSpec((3, 1, length, cols), row2),
                pl.BlockSpec((1, length, cols), row),
                pl.BlockSpec((1, length, width), row),
                slot,
                slot,
                pl.BlockSpec((8, 128), two),
            ),
        ),
        compiler_params=pltpu.CompilerParams(dimension_semantics=("arbitrary",), vmem_limit_bytes=60 << 20),
        cost_estimate=pl.CostEstimate(flops=10**10, bytes_accessed=4 * 10**7, transcendentals=10**6),
        name="attend",
    )(number, full, weights, wo, gains, small, table)


def attend_mix_kernel(
    top, local, full, w, wo, gains, small, table, tok, cot, _cot_early,
    normed, pre, low, ctx, middle, mixed, cot_full, slots0, slots1, starts,
    own, blocks, nbuf, pbuf, lbuf, cbuf, part, begins, tsem, ssem, *scratch,
):
    at = Place()
    seqs = tok.shape[0]
    n = Reduce.sems
    reduce = Reduce(at, part, *scratch[:n])
    gather = Gather(at, own, mixed, *scratch[n : n + 3])
    cot_gather = Gather(at, cot, cot_full, *scratch[n + 3 :])
    number = (at.me * local).astype(F32)
    early = seqs // 2
    at.greet((at.xn, at.yn, at.sb))
    each(seqs, cot_gather.start, low=early)
    begins[...] = jnp.zeros_like(begins)

    def load(s):
        return pltpu.make_async_copy(full.at[s], blocks.at[lax.rem(s, 2)], tsem.at[lax.rem(s, 2)])

    def stores(s):
        k = lax.rem(s, 2)
        pairs = ((nbuf.at[k], normed.at[s]), (pbuf.at[k], pre.at[:, s]), (lbuf.at[k], low.at[:, s]), (cbuf.at[k], ctx.at[s]))
        return [pltpu.make_async_copy(src, dst, ssem.at[i, k]) for i, (src, dst) in enumerate(pairs)]

    load(0).start()

    def sequence(s):
        k = lax.rem(s, 2)
        load(s).wait()

        @pl.when(s + 1 < seqs)
        def _():
            load(s + 1).start()

        @pl.when(s >= 2)
        def _():
            for copy in stores(s - 2):
                copy.wait()

        attend_rows(
            top, number, s, blocks.at[k], w, wo, gains, small, table,
            nbuf.at[k], pbuf.at[k], lbuf.at[k], cbuf.at[k], part.at[s], (slots0.at[s], slots1.at[s]), begins,
        )
        for copy in stores(s):
            copy.start()
        reduce.start(s)

    def rows(s):
        living = live_rows(small, s, at.me, tok.shape[1])
        mid, out = mix_rows(reduce.total(s), tok[s], living, gains[1:2])
        middle[s] = mid
        own[s] = out
        gather.start(s)

    def cot_pair(p):
        @pl.when(lax.rem(p, 2) == 0)
        def _():
            cot_gather.relay(early + p, True)
            cot_gather.relay(early + p + 1, False)

    jobs = (
        (sequence, 0, seqs), (reduce.hop1, 1, seqs), (cot_pair, 3, early), (reduce.hop2, 3, seqs),
        (lambda s: cot_gather.relay_far(early + s), 7, early), (rows, 5, seqs),
    )

    def tick(i, _):
        for job, lag, count in jobs:

            @pl.when(jnp.logical_and(i >= lag, i < lag + count))
            def _():
                job(i - lag)

        return 0

    lax.fori_loop(0, max(lag + count for _, lag, count in jobs), tick, 0)
    starts[...] = begins[...].astype(jnp.int32)
    each(seqs, cot_gather.finish, low=early)
    gather_tail(gather, 0, seqs)
    for s in (seqs - 2, seqs - 1):
        for copy in stores(s):
            copy.wait()
    each(seqs, reduce.finish)


def attend_mix(top, local, full, weights, wo, gains, small, table, tokens, cotangent, cot_early):
    seqs, rows, width = tokens.shape
    length = full.shape[1]
    cols = weights.shape[2]
    part = sds((seqs, 8, rows, width), BF16)
    dma = pltpu.SemaphoreType.DMA
    return pl.pallas_call(
        functools.partial(attend_mix_kernel, top, local),
        out_shape=(
            sds((seqs, length, width), BF16),
            sds((2, seqs, length, cols), F32),
            sds((3, seqs, length, cols), BF16),
            sds((seqs, length, cols), BF16),
            sds(tokens.shape, F32),
            sds((seqs, length, width), BF16),
            sds((seqs, length, width), BF16),
            sds((seqs, 16, length), F32),
            sds((seqs, 16, length), F32),
            sds((8, 128), jnp.int32),
        ),
        in_specs=[AN] + [VM] * 7 + [AN],
        out_specs=(AN, AN, AN, AN, VM, AN, AN, VM, VM, VM),
        input_output_aliases={8: 6},
        scratch_shapes=[
            pltpu.VMEM(tokens.shape, BF16),
            pltpu.VMEM((2,) + full.shape[1:], BF16),
            pltpu.VMEM((2, length, width), BF16),
            pltpu.VMEM((2, 2, length, cols), F32),
            pltpu.VMEM((2, 3, length, cols), BF16),
            pltpu.VMEM((2, length, cols), BF16),
            pltpu.VMEM(part.shape, BF16),
            pltpu.VMEM((8, 128), F32),
            dma((2,)),
            dma((4, 2)),
        ]
        + Reduce.scratch(part)
        + Gather.scratch(seqs)
        + Gather.scratch(seqs),
        compiler_params=pltpu.CompilerParams(collective_id=2, **COMM),
        name="attend_mix",
    )(full, weights, wo, gains, small, table, tokens, cotangent, cot_early)


def attend_back_kernel(
    agrad, normed, pre, low, ctx, w, wo, small, table, part, wgrad, wograd, gains, wacc, woacc,
):
    s = pl.program_id(0)
    length = seq_len(small, s)
    cos, sin = rope_tables(table)

    @pl.when(s == 0)
    def _():
        wacc[...] = jnp.zeros_like(wacc)
        woacc[...] = jnp.zeros_like(woacc)
        gains[...] = jnp.zeros_like(gains)

    ag = agrad[0]
    woacc[...] += dot(ctx[0], ag, 0, 0)
    cg_all = dot(ag, wo[...], 1, 1).astype(BF16)
    scale = HEAD_DIM**-0.5
    half = HEAD_DIM // 2
    grads = ([], [], [])
    for h in range(cg_all.shape[1] // HEAD_DIM):
        cols = slice(h * HEAD_DIM, (h + 1) * HEAD_DIM)
        q, k, value, cg = low[0, 0, :, cols], low[1, 0, :, cols], low[2, 0, :, cols], cg_all[:, cols]
        attention = probabilities(q, k, length)
        grads[2].append(dot(attention.astype(BF16), cg, 0, 0).astype(BF16))
        pg = dot(cg, value, 1, 1)
        sg = (attention * (pg - jnp.sum(attention * pg, axis=-1, keepdims=True))).astype(BF16)
        for i, (rot_grad, g) in enumerate(((dot(sg, k, 1, 0), small[0:1]), (dot(sg, q, 0, 0), small[1:2]))):
            wgt = rot_grad * scale
            u = wgt * cos + pltpu.roll(wgt * sin, half, 1)
            v = pre[i, 0, :, cols]
            r = inverse_rms(v)
            grads[i].append(rms_back(v, r, u * g).astype(BF16))
            gains[i : i + 1] += jnp.sum(u * v * r, axis=0, keepdims=True)
    total = None
    for i in range(3):
        g = grads[i][0] if len(grads[i]) == 1 else jnp.concatenate(grads[i], axis=1)
        wacc[i] += dot(normed[0], g, 0, 0)
        piece = dot(g, w[i], 1, 1)
        total = piece if total is None else total + piece
    part[0] = total.astype(BF16)

    @pl.when(s == pl.num_programs(0) - 1)
    def _():
        wgrad[...] = wacc[...].astype(BF16)
        wograd[...] = woacc[...].astype(BF16)


def attend_back(agrad, normed, pre, low, ctx, weights, wo, small, table):
    seqs, length, width = agrad.shape
    cols = weights.shape[2]
    row = lambda i, *_: (i, 0, 0)
    row2 = lambda i, *_: (0, i, 0, 0)
    two = lambda i, *_: (0, 0)
    three = lambda i, *_: (0, 0, 0)
    return pl.pallas_call(
        attend_back_kernel,
        out_shape=(
            sds(agrad.shape, BF16),
            sds(weights.shape, BF16),
            sds(wo.shape, BF16),
            sds((8, HEAD_DIM), F32),
        ),
        grid_spec=pltpu.PrefetchScalarGridSpec(
            num_scalar_prefetch=0,
            grid=(seqs,),
            in_specs=[
                pl.BlockSpec((1, length, width), row),
                pl.BlockSpec((1, length, width), row),
                pl.BlockSpec((2, 1, length, cols), row2),
                pl.BlockSpec((3, 1, length, cols), row2),
                pl.BlockSpec((1, length, cols), row),
                pl.BlockSpec(weights.shape, three),
                pl.BlockSpec(wo.shape, two),
                pl.BlockSpec((8, 128), two),
                pl.BlockSpec((length, HEAD_DIM), two),
            ],
            out_specs=(
                pl.BlockSpec((1, length, width), row),
                pl.BlockSpec(weights.shape, three),
                pl.BlockSpec(wo.shape, two),
                pl.BlockSpec((8, HEAD_DIM), two),
            ),
            scratch_shapes=[
                pltpu.VMEM(weights.shape, F32),
                pltpu.VMEM(wo.shape, F32),
            ],
        ),
        compiler_params=pltpu.CompilerParams(dimension_semantics=("arbitrary",), vmem_limit_bytes=60 << 20),
        cost_estimate=pl.CostEstimate(flops=2 * 10**10, bytes_accessed=4 * 10**7, transcendentals=10**6),
        name="attend_back",
    )(agrad, normed, pre, low, ctx, weights, wo, small, table)


BLOCK = 256


def pack_rows(seqs, capacity):
    return -(-seqs * capacity // BLOCK) * BLOCK


def each_block(blocks, hidden, job):
    part = min(hidden, 512)
    parts = hidden // part

    def run(i, _):
        b, h = i // parts, lax.rem(i, parts)
        rows = pl.ds(pl.multiple_of(b * BLOCK, BLOCK), BLOCK)
        low = pl.multiple_of(h * part, part)
        job(rows, pl.ds(low, part), pl.ds(pl.multiple_of(hidden + low, part), part))
        return 0

    lax.fori_loop(0, blocks * parts, run, 0)


def forward_blocks(blocks, x, dy, wi, wo, acts, dgus):
    def job(rows, gcols, ucols):
        gate = dot(x[rows], wi[:, gcols], 1, 0)
        up = dot(x[rows], wi[:, ucols], 1, 0)
        dact = dot(dy[rows], wo[gcols], 1, 1)
        sig = 1.0 / (1.0 + jnp.exp(-gate))
        silu = gate * sig
        acts[rows, gcols] = (silu * up).astype(BF16)
        dgus[rows, gcols] = (dact * up * sig * (1.0 + gate * (1.0 - sig))).astype(BF16)
        dgus[rows, ucols] = (dact * silu).astype(BF16)

    each_block(blocks, wo.shape[0], job)


def gradient_tiles(blocks, left, right, result, acc, stage, ssem, busy):
    tr, tc = acc.shape
    down, across = result.shape[0] // tr, result.shape[1] // tc

    def tile(t, _):
        rt, ct = t // across, lax.rem(t, across)
        left_cols = pl.ds(pl.multiple_of(rt * tr, tr), tr)
        right_cols = pl.ds(pl.multiple_of(ct * tc, tc), tc)

        def step(b, _):
            rows = pl.ds(pl.multiple_of(b * BLOCK, BLOCK), BLOCK)
            piece = dot(left[rows, left_cols], right[rows, right_cols], 0, 0)

            @pl.when(b == 0)
            def _():
                acc[...] = piece

            @pl.when(b > 0)
            def _():
                acc[...] += piece

            return 0

        @pl.when(blocks == 0)
        def _():
            acc[...] = jnp.zeros_like(acc)

        lax.fori_loop(0, blocks, step, 0)
        k = lax.rem(t, 2)
        out = pltpu.make_async_copy(stage.at[k], result.at[left_cols, right_cols], ssem.at[k])

        @pl.when(jnp.logical_or(t >= 2, busy))
        def _():
            out.wait()

        stage[k] = acc[...].astype(BF16)
        out.start()
        return 0

    lax.fori_loop(0, down * across, tile, 0)


def drain_tiles(result, acc, stage, ssem):
    tr, tc = acc.shape
    for k in range(2):
        pltpu.make_async_copy(stage.at[k], result.at[pl.ds(0, tr), pl.ds(0, tc)], ssem.at[k]).wait()


def first_kernel(
    capacity, starts, mixed, cot, slots0, slots1, w_in, w_out,
    act, dgu, x_all, dy_all, out_grad,
    x, dy, wi, wo, acts, dgus, acc, stage, wsem, ssem, rsem,
):
    step = pl.program_id(0)
    steps = pl.num_programs(0)
    together = mixed.shape[0]
    seqs = steps * together
    width = mixed.shape[2]
    loads = [pltpu.make_async_copy(w_in.at[0], wi, wsem.at[0]), pltpu.make_async_copy(w_out.at[0], wo, wsem.at[1])]

    @pl.when(step == 0)
    def _():
        for copy in loads:
            copy.start()

    packed = []
    for k in range(together):
        spread, gate_spread = [], []
        for slots in (slots0, slots1):
            column = lax.broadcasted_iota(jnp.int32, (capacity, slots.shape[2]), 0).astype(F32)
            place = column == slots[k, 0:1]
            spread.append(jnp.where(place, 1.0, 0.0).astype(BF16))
            gate_spread.append(jnp.where(place, slots[k, 8:9], 0.0).astype(BF16))
        packed.append(
            (
                dot(jnp.concatenate(spread, axis=0), mixed[k], 1, 0).astype(BF16),
                dot(jnp.concatenate(gate_spread, axis=0), cot[k], 1, 0).astype(BF16),
            )
        )
    for k, (x_rows, dy_rows) in enumerate(packed):
        s = step * together + k
        for j in range(2):
            start = pl.multiple_of(starts[j, s], 16)
            x[j, pl.ds(start, capacity)] = x_rows[j * capacity : (j + 1) * capacity]
            dy[j, pl.ds(start, capacity)] = dy_rows[j * capacity : (j + 1) * capacity]

    @pl.when(step == steps - 1)
    def _():
        for j in range(2):
            past = (starts[j, seqs - 1] + capacity) // 16
            end = (starts[j, seqs] + BLOCK - 1) // BLOCK * (BLOCK // 16)

            def clear(i, _):
                rows = pl.ds(pl.multiple_of(i * 16, 16), 16)
                x[j, rows] = jnp.zeros((16, width), BF16)
                dy[j, rows] = jnp.zeros((16, width), BF16)
                return 0

            lax.fori_loop(past, end, clear, 0)
        saves = [pltpu.make_async_copy(x, x_all, rsem.at[0]), pltpu.make_async_copy(dy.at[1], dy_all, rsem.at[1])]
        for copy in saves:
            copy.start()
        blocks = (starts[0, seqs] + BLOCK - 1) // BLOCK
        for copy in loads:
            copy.wait()
        forward_blocks(blocks, x.at[0], dy.at[0], wi, wo, acts, dgus)
        saves += [pltpu.make_async_copy(acts, act.at[0], rsem.at[2]), pltpu.make_async_copy(dgus, dgu.at[0], rsem.at[3])]
        for copy in saves[2:]:
            copy.start()
        gradient_tiles(blocks, acts, dy.at[0], out_grad, acc, stage, ssem, False)
        drain_tiles(out_grad, acc, stage, ssem)
        for copy in saves:
            copy.wait()


def expert_first(starts, mixed, cot, slots, w_in, w_out, capacity):
    seqs, length, width = mixed.shape
    hidden = w_out.shape[1]
    rows = pack_rows(seqs, capacity)
    dma = pltpu.SemaphoreType.DMA
    seq = lambda i, *_: (i, 0, 0)
    together = 2
    slot_spec = pl.BlockSpec((together, 16, length), seq)
    return pl.pallas_call(
        functools.partial(first_kernel, capacity),
        out_shape=(
            sds((2, rows, hidden), BF16),
            sds((2, rows, 2 * hidden), BF16),
            sds((2, rows, width), BF16),
            sds((rows, width), BF16),
            sds((hidden, width), BF16),
        ),
        grid_spec=pltpu.PrefetchScalarGridSpec(
            num_scalar_prefetch=1,
            grid=(seqs // together,),
            in_specs=[
                pl.BlockSpec((together, length, width), seq),
                pl.BlockSpec((together, length, width), seq),
                slot_spec,
                slot_spec,
                AN,
                AN,
            ],
            out_specs=(AN, AN, AN, AN, AN),
            scratch_shapes=[
                pltpu.VMEM((2, rows, width), BF16),
                pltpu.VMEM((2, rows, width), BF16),
                pltpu.VMEM(w_in.shape[1:], BF16),
                pltpu.VMEM(w_out.shape[1:], BF16),
                pltpu.VMEM((rows, hidden), BF16),
                pltpu.VMEM((rows, 2 * hidden), BF16),
                pltpu.VMEM((256, 1024), F32),
                pltpu.VMEM((2, 256, 1024), BF16),
                dma((2,)),
                dma((2,)),
                dma((4,)),
            ],
        ),
        compiler_params=pltpu.CompilerParams(dimension_semantics=("arbitrary",), vmem_limit_bytes=63 << 20),
        cost_estimate=pl.CostEstimate(flops=2 * 10**10, bytes_accessed=6 * 10**7, transcendentals=10**6),
        name="expert_first",
    )(starts, mixed, cot, *slots, w_in, w_out)


def in_grad_kernel(seqs, starts, x_all, dgu, in_grad, x, dgus, acc, stage, lsem, ssem):
    blocks = (starts[0, seqs] + BLOCK - 1) // BLOCK

    def load(b):
        rows = pl.ds(pl.multiple_of(b * BLOCK, BLOCK), BLOCK)
        return (
            pltpu.make_async_copy(x_all.at[0, rows], x.at[rows], lsem.at[0, b]),
            pltpu.make_async_copy(dgu.at[0, rows], dgus.at[rows], lsem.at[1, b]),
        )

    def run(b, action):
        for copy in load(b):
            getattr(copy, action)()
        return 0

    lax.fori_loop(0, blocks, lambda b, _: run(b, "start"), 0)
    lax.fori_loop(0, blocks, lambda b, _: run(b, "wait"), 0)
    gradient_tiles(blocks, x, dgus, in_grad, acc, stage, ssem, False)
    drain_tiles(in_grad, acc, stage, ssem)


def first_in_grad(seqs, starts, x_all, dgu):
    rows, width = x_all.shape[1:]
    dma = pltpu.SemaphoreType.DMA
    return pl.pallas_call(
        functools.partial(in_grad_kernel, seqs),
        out_shape=sds((width, dgu.shape[2]), BF16),
        grid_spec=pltpu.PrefetchScalarGridSpec(
            num_scalar_prefetch=1,
            grid=(1,),
            in_specs=[AN, AN],
            out_specs=AN,
            scratch_shapes=[
                pltpu.VMEM((rows, width), BF16),
                pltpu.VMEM(dgu.shape[1:], BF16),
                pltpu.VMEM((512, 2048), F32),
                pltpu.VMEM((2, 512, 2048), BF16),
                dma((2, rows // BLOCK)),
                dma((2,)),
            ],
        ),
        compiler_params=pltpu.CompilerParams(dimension_semantics=("arbitrary",), vmem_limit_bytes=60 << 20),
        cost_estimate=pl.CostEstimate(flops=10**10, bytes_accessed=2 * 10**7, transcendentals=0),
        name="first_in_grad",
    )(starts, x_all, dgu)


def second_kernel(
    seqs, starts, x_all, dy_all, w_in, w_out, _act, _dgu, act, dgu, in_grad, out_grad,
    x, dy, wi, wo, acts, dgus, acc, stage, wsem, lsem, ssem, rsem,
):
    blocks = (starts[1, seqs] + BLOCK - 1) // BLOCK
    loads = [pltpu.make_async_copy(w_in.at[1], wi, wsem.at[0]), pltpu.make_async_copy(w_out.at[1], wo, wsem.at[1])]

    def load(b, action):
        rows = pl.ds(pl.multiple_of(b * BLOCK, BLOCK), BLOCK)
        for copy in (
            pltpu.make_async_copy(x_all.at[1, rows], x.at[rows], lsem.at[0, b]),
            pltpu.make_async_copy(dy_all.at[rows], dy.at[rows], lsem.at[1, b]),
        ):
            getattr(copy, action)()
        return 0

    for copy in loads:
        copy.start()
    lax.fori_loop(0, blocks, lambda b, _: load(b, "start"), 0)
    for copy in loads:
        copy.wait()
    lax.fori_loop(0, blocks, lambda b, _: load(b, "wait"), 0)

    forward_blocks(blocks, x, dy, wi, wo, acts, dgus)
    saves = [pltpu.make_async_copy(acts, act.at[1], rsem.at[0]), pltpu.make_async_copy(dgus, dgu.at[1], rsem.at[1])]
    for copy in saves:
        copy.start()
    gradient_tiles(blocks, x, dgus, in_grad, acc, stage, ssem, False)
    gradient_tiles(blocks, acts, dy, out_grad, acc, stage, ssem, True)
    drain_tiles(out_grad, acc, stage, ssem)
    for copy in saves:
        copy.wait()


def expert_second(seqs, starts, x_all, dy_all, w_in, w_out, act, dgu):
    rows, width = dy_all.shape
    hidden = w_out.shape[1]
    dma = pltpu.SemaphoreType.DMA
    return pl.pallas_call(
        functools.partial(second_kernel, seqs),
        out_shape=(
            sds(act.shape, BF16), sds(dgu.shape, BF16), sds((width, 2 * hidden), BF16), sds((hidden, width), BF16)
        ),
        input_output_aliases={5: 0, 6: 1},
        grid_spec=pltpu.PrefetchScalarGridSpec(
            num_scalar_prefetch=1,
            grid=(1,),
            in_specs=[AN] * 6,
            out_specs=(AN, AN, AN, AN),
            scratch_shapes=[
                pltpu.VMEM((rows, width), BF16),
                pltpu.VMEM((rows, width), BF16),
                pltpu.VMEM(w_in.shape[1:], BF16),
                pltpu.VMEM(w_out.shape[1:], BF16),
                pltpu.VMEM((rows, hidden), BF16),
                pltpu.VMEM((rows, 2 * hidden), BF16),
                pltpu.VMEM((512, 2048), F32),
                pltpu.VMEM((2, 512, 2048), BF16),
                dma((2,)),
                dma((2, rows // BLOCK)),
                dma((2,)),
                dma((2,)),
            ],
        ),
        compiler_params=pltpu.CompilerParams(dimension_semantics=("arbitrary",), vmem_limit_bytes=60 << 20),
        cost_estimate=pl.CostEstimate(flops=25 * 10**9, bytes_accessed=6 * 10**7, transcendentals=10**6),
        name="expert_second",
    )(starts, x_all, dy_all, w_in, w_out, act, dgu)


def tail_kernel(seqs, starts, act, dgu, w_in, w_out, produced, dx):
    @pl.when(pl.program_id(1) * BLOCK < starts[pl.program_id(0), seqs])
    def _():
        part = min(produced.shape[1], 512)

        def run(i, _):
            cols = pl.ds(pl.multiple_of(i * part, part), part)
            produced[:, cols] = dot(act[...], w_out[:, cols], 1, 0).astype(BF16)
            dx[:, cols] = dot(dgu[...], w_in[cols], 1, 1).astype(BF16)
            return 0

        lax.fori_loop(0, produced.shape[1] // part, run, 0)


def expert_tails(seqs, starts, act, dgu, w_in, w_out):
    _, rows, hidden = act.shape
    width = w_in.shape[1]

    def block(j, i, st):
        return j, jnp.maximum(jnp.minimum(i, (st[j, seqs] + BLOCK - 1) // BLOCK - 1), 0), 0

    out = pl.BlockSpec((None, BLOCK, width), block)
    return pl.pallas_call(
        functools.partial(tail_kernel, seqs),
        out_shape=(sds((2, rows, width), BF16), sds((2, rows, width), BF16)),
        grid_spec=pltpu.PrefetchScalarGridSpec(
            num_scalar_prefetch=1,
            grid=(2, rows // BLOCK),
            in_specs=[
                pl.BlockSpec((None, BLOCK, hidden), block),
                pl.BlockSpec((None, BLOCK, 2 * hidden), block),
                pl.BlockSpec((None,) + w_in.shape[1:], lambda j, i, *_: (j, 0, 0)),
                pl.BlockSpec((None,) + w_out.shape[1:], lambda j, i, *_: (j, 0, 0)),
            ],
            out_specs=(out, out),
        ),
        compiler_params=pltpu.CompilerParams(dimension_semantics=("arbitrary", "arbitrary"), vmem_limit_bytes=60 << 20),
        cost_estimate=pl.CostEstimate(flops=24 * 10**9, bytes_accessed=6 * 10**7, transcendentals=0),
        name="expert_tails",
    )(starts, act, dgu, w_in, w_out)


def combine_kernel(capacity, local, *refs):
    s = pl.program_id(0)
    starts = refs[0]
    slots = refs[1 : 1 + local]
    produced, dx, out_part, grad_part = refs[1 + local :]
    out_sum, grad_sum = None, None
    for j in range(local):
        length = slots[j].shape[2]
        column = lax.broadcasted_iota(jnp.int32, (capacity, length), 0).astype(F32)
        place = column == slots[j][0, 0:1]
        span = pl.ds(pl.multiple_of(starts[j, s], 16), capacity)
        held = lax.broadcasted_iota(jnp.int32, (capacity, 1), 0) < starts[j, s + 1] - starts[j, s]
        rows = jnp.where(held, produced[j, span], 0.0).astype(BF16)
        grads = jnp.where(held, dx[j, span], 0.0).astype(BF16)
        out = dot(jnp.where(place, slots[j][0, 8:9], 0.0).astype(BF16), rows, 0, 0)
        grad = dot(jnp.where(place, 1.0, 0.0).astype(BF16), grads, 0, 0)
        out_sum = out if out_sum is None else out_sum + out
        grad_sum = grad if grad_sum is None else grad_sum + grad
    out_part[0] = out_sum.astype(BF16)
    grad_part[0] = grad_sum.astype(BF16)


def combine(starts, slots, produced, dx, capacity):
    local = len(slots)
    seqs, _, length = slots[0].shape
    width = produced.shape[2]
    seq = lambda i, *_: (i, 0, 0)
    rows = pl.BlockSpec(produced.shape, lambda i, *_: (0, 0, 0))
    return pl.pallas_call(
        functools.partial(combine_kernel, capacity, local),
        out_shape=(sds((seqs, length, width), BF16), sds((seqs, length, width), BF16)),
        grid_spec=pltpu.PrefetchScalarGridSpec(
            num_scalar_prefetch=1,
            grid=(seqs,),
            in_specs=[pl.BlockSpec((1, 16, length), seq)] * local + [rows] * 2,
            out_specs=(pl.BlockSpec((1, length, width), seq), pl.BlockSpec((1, length, width), seq)),
        ),
        compiler_params=pltpu.CompilerParams(dimension_semantics=("arbitrary",), vmem_limit_bytes=60 << 20),
        cost_estimate=pl.CostEstimate(flops=3 * 10**9, bytes_accessed=4 * 10**7, transcendentals=0),
        name="combine",
    )(starts, *slots, produced, dx)


def shards(
    tokens, cotangent, gate_weights, expert_ids, seq_lengths, query_weight, key_weight, value_weight,
    output_weight, attn_gain, ffn_gain, query_gain, key_gain, expert_in, expert_out,
):
    ep = lax.axis_size("ep")
    me = lax.axis_index("ep")
    seqs, rows, _ = tokens.shape
    length = rows * ep
    top = gate_weights.shape[2]
    local = expert_in.shape[0]
    experts = local * ep
    capacity = -(-(length * top * 9 // (8 * experts)) // 16) * 16

    gains = jnp.concatenate([attn_gain, ffn_gain]).astype(F32).reshape(-1, 128)
    few = [query_gain.astype(F32), key_gain.astype(F32), seq_lengths.astype(F32)]
    few = jnp.stack([jnp.pad(v, (0, 128 - v.shape[0])) for v in few])
    packet = jnp.concatenate([gains, few], axis=0)
    packet = jnp.pad(packet, ((0, -packet.shape[0] % 8), (0, 0)))
    share = gains.shape[0] // 2

    full, weights, cot_full, gains, small_in = front(
        tokens, cotangent, expert_ids.transpose(0, 2, 1), gate_weights.transpose(0, 2, 1),
        query_weight, key_weight, value_weight, packet,
    )

    half = HEAD_DIM // 2
    frequency = ROPE_BASE ** (-(np.arange(half, dtype=np.float32) * np.float32(2.0 / HEAD_DIM)))
    angles = np.arange(length, dtype=np.float32)[:, None] * frequency.astype(np.float32)[None, :]
    table = jnp.asarray(np.concatenate([np.cos(angles), np.sin(angles)], axis=-1), F32)

    if ep == 8 and lax.axis_size("rep") == 4:
        normed, pre, low, ctx, middle, mixed, cot_full, slots0, slots1, starts = attend_mix(
            top, local, full, weights, output_weight, gains, small_in, table, tokens, cotangent, cot_full
        )
    else:
        number = (me * local).astype(jnp.int32)[None]
        normed, pre, low, ctx, part, slots0, slots1, starts = attend(
            top, number, full, weights, output_weight, gains, small_in, table
        )
        starts = starts.astype(jnp.int32)
        middle, mixed = mix(part, tokens, small_in, gains)

    act, dgu, x_all, dy_all, out_grad0 = expert_first(
        starts, mixed, cot_full, (slots0, slots1), expert_in, expert_out, capacity
    )

    def over_rep(value):
        return lax.psum_scatter(value, "rep", scatter_dimension=0, tiled=True)

    out0 = over_rep(out_grad0)
    in_grad0 = first_in_grad(seqs, starts, x_all, dgu)
    in0 = over_rep(in_grad0)
    x_all, _ = lax.optimization_barrier((x_all, in_grad0))
    act, dgu, in_grad1, out_grad1 = expert_second(seqs, starts, x_all, dy_all, expert_in, expert_out, act, dgu)
    in1 = over_rep(in_grad1)
    out1 = over_rep(out_grad1)
    produced, dx = expert_tails(seqs, starts, act, dgu, expert_in, expert_out)
    out_part, grad_part = combine(starts, (slots0, slots1), produced, dx, capacity)

    mgrad, ffn_back, agrad = back(grad_part, middle, cotangent, small_in, gains)
    npart, wgrad, wograd, qk_back = attend_back(
        agrad, normed, pre, low, ctx, weights, output_weight, small_in, table
    )
    sums, small, result, token_grad = finish(
        wgrad, wograd, npart, out_part, tokens, middle, mgrad, gains, ffn_back, qk_back
    )

    def head_share(vector):
        return lax.dynamic_slice_in_dim(vector, me * (HEAD_DIM // ep), HEAD_DIM // ep)

    return (
        result,
        token_grad,
        sums[1].astype(F32),
        sums[2].astype(F32),
        sums[3].astype(F32),
        sums[0].astype(F32),
        small[:share].reshape(-1),
        small[share : 2 * share].reshape(-1),
        head_share(small[2 * share]),
        head_share(small[2 * share + 1]),
        jnp.stack([in0, in1]).astype(F32),
        jnp.stack([out0, out1]).astype(F32),
    )


def solution(mesh):
    seq = P("rep", "ep", None)
    row, gain, expert = P("ep", None), P("ep"), P("ep", None, None)
    split = P("ep", "rep", None)

    return jax.shard_map(
        shards,
        mesh=mesh,
        in_specs=(seq, seq, seq, seq, P(("rep", "ep")), row, row, row, row, gain, gain, gain, gain, expert, expert),
        out_specs=(seq, seq, row, row, row, row, gain, gain, gain, gain, split, split),
        check_vma=False,
    )
```

```python
import functools

import jax
import jax.numpy as jnp
import numpy as np
from jax import lax
from jax.experimental import pallas as pl
from jax.experimental.pallas import tpu as pltpu
from jax.sharding import PartitionSpec as P

HEAD_DIM = 128
EPS = 1e-06
ROPE_BASE = 50000.0
MESH = pl.DeviceIdType.MESH
F32 = jnp.float32
BF16 = jnp.bfloat16


def sds(shape, dtype):
    return jax.ShapeDtypeStruct(shape, dtype)


VM = pl.BlockSpec(memory_space=pltpu.VMEM)
AN = pl.BlockSpec(memory_space=pl.ANY)


def inverse_rms(v):
    return lax.rsqrt(jnp.mean(v * v, axis=-1, keepdims=True) + EPS)


def rms_back(v, r, ug):
    return r * ug - v * (r * r * r * jnp.mean(ug * v, axis=-1, keepdims=True))


def mix_rows(total, tok, living, gain):
    middle = tok.astype(F32) + living * total
    mixed = middle * inverse_rms(middle) * gain
    return middle, mixed.astype(BF16)


def ffn_back_rows(mixed_grad, middle, cot, living, gain):
    r = inverse_rms(middle)
    middle_grad = cot.astype(F32) + rms_back(middle, r, mixed_grad * gain)
    return middle_grad, (living * middle_grad).astype(BF16), mixed_grad * middle * r


def attn_back_rows(normed_grad, tok, middle_grad, gain):
    v = tok.astype(F32)
    r = inverse_rms(v)
    return (middle_grad + rms_back(v, r, normed_grad * gain)).astype(BF16), normed_grad * v * r


def seq_len(small, s):
    lane = lax.broadcasted_iota(jnp.int32, (1, 128), 1)
    return jnp.sum(jnp.where(lane == s, small[2:3, :], 0.0), axis=1, keepdims=True)


def live_rows(small, s, me, rows):
    place = (lax.broadcasted_iota(jnp.int32, (rows, 1), 0) + me * rows).astype(F32)
    return jnp.where(place < seq_len(small, s), 1.0, 0.0)


class Place:
    def __init__(self):
        me = lax.axis_index("ep")
        core, x, y = lax.rem(me, 2), lax.rem(me // 2, 2), me // 4
        self.rep = lax.axis_index("rep")
        self.me = me
        self.sb = me + 1 - 2 * core
        self.dx = 2 - 4 * x
        self.dy = 4 - 8 * y
        self.xn = me + self.dx
        self.yn = me + self.dy
        self.dg = me + self.dx + self.dy

    def push(self, src, dst, send, recv, dev):
        return pltpu.make_async_remote_copy(
            src_ref=src, dst_ref=dst, send_sem=send, recv_sem=recv, device_id=(self.rep, dev), device_id_type=MESH
        )

    def peer(self, m):
        k = m + 1
        return self.me + (k % 2) * (self.sb - self.me) + (k // 2 % 2) * self.dx + (k // 4) * self.dy

    def greet(self, peers):
        barrier = pltpu.get_barrier_semaphore()
        for peer in peers:
            pl.semaphore_signal(barrier, inc=1, device_id=(self.rep, peer), device_id_type=MESH)
        pl.semaphore_wait(barrier, len(peers))


class Gather:
    sems = 3

    def __init__(self, at, own, full, ssem, rsem, lsem):
        self.at, self.own, self.full, self.ssem, self.rsem, self.lsem = at, own, full, ssem, rsem, lsem
        self.rows = own.shape[1]

    @staticmethod
    def scratch(seqs):
        return [pltpu.SemaphoreType.DMA((7, seqs)), pltpu.SemaphoreType.DMA((8, seqs)), pltpu.SemaphoreType.DMA((seqs,))]

    def block(self, s, dev):
        return self.full.at[s, pl.ds(pl.multiple_of(dev * self.rows, self.rows), self.rows)]

    def copy(self, s, dev, kind, slot, to, src=None):
        block = self.block(s, dev)
        return self.at.push(block if src is None else src, block, self.ssem.at[kind, s], self.rsem.at[slot, s], to)

    def start(self, s):
        at, own = self.at, self.own.at[s]
        self.copy(s, at.me, 0, 2, at.xn, own).start()
        self.copy(s, at.me, 1, 4, at.yn, own).start()
        self.copy(s, at.me, 2, 1, at.sb, own).start()
        pltpu.make_async_copy(own, self.block(s, at.me), self.lsem.at[s]).start()

    def relay(self, s, by_y):
        at = self.at
        self.copy(s, at.xn, 0, 2, at.xn).wait_recv()
        if by_y:
            self.copy(s, at.xn, 3, 6, at.yn).start()
        self.copy(s, at.xn, 4, 3, at.sb).start()
        self.copy(s, at.yn, 1, 4, at.yn).wait_recv()
        if not by_y:
            self.copy(s, at.yn, 3, 6, at.xn).start()
        self.copy(s, at.yn, 5, 5, at.sb).start()

    def relay_far(self, s):
        at = self.at
        self.copy(s, at.dg, 3, 6, at.yn).wait_recv()
        self.copy(s, at.dg, 6, 7, at.sb).start()

    def finish(self, s):
        at = self.at
        for dev, slot in ((at.sb, 1), (at.sb + at.dx, 3), (at.sb + at.dy, 5), (at.sb + at.dx + at.dy, 7)):
            self.copy(s, dev, 0, slot, at.sb).wait_recv()
        for kind in range(7):
            self.copy(s, at.me, kind, 0, at.sb).wait_send()
        pltpu.make_async_copy(self.own.at[s], self.block(s, at.me), self.lsem.at[s]).wait()


def gather_tail(gather, low, high):
    def relay(i, _):
        gather.relay(low + 2 * i, True)
        gather.relay(low + 2 * i + 1, False)
        return 0

    lax.fori_loop(0, (high - low) // 2, relay, 0)
    each(high, gather.relay_far, low=low)
    each(high, gather.finish, low=low)


class Reduce:
    def __init__(self, at, part, held, mine, x1, y1, x2, y2, ms, hs, hr, d1s, d1r, d2s, d2r):
        self.at, self.part, self.held, self.mine = at, part, held, mine
        self.x1, self.y1, self.x2, self.y2 = x1, y1, x2, y2
        self.ms, self.hs, self.hr, self.d1s, self.d1r, self.d2s, self.d2r = ms, hs, hr, d1s, d1r, d2s, d2r
        self.half = part.shape[2] // 2

    @staticmethod
    def scratch(part):
        s, _, t, d = part.shape
        dma = pltpu.SemaphoreType.DMA
        return [
            pltpu.VMEM((s, 4, t, d), BF16),
            pltpu.VMEM((s, 4, t, d), BF16),
            pltpu.VMEM((s, t // 2, d), BF16),
            pltpu.VMEM((s, t // 2, d), BF16),
            pltpu.VMEM((s, t, d), BF16),
            pltpu.VMEM((s, t, d), BF16),
            dma((4, s)),
            dma((4, s)),
            dma((4, s)),
            dma((2, s)),
            dma((2, s)),
            dma((2, s)),
            dma((2, s)),
        ]

    sems = 13

    def core_copy(self, s, k):
        at = self.at
        dest = (at.sb, at.sb + at.dx, at.sb + at.dy, at.sb + at.dx + at.dy)[k]
        return at.push(self.part.at[s, dest], self.held.at[s, k], self.hs.at[k, s], self.hr.at[k, s], at.sb)

    def load(self, s, k):
        at = self.at
        dest = (at.me, at.xn, at.yn, at.dg)[k]
        return pltpu.make_async_copy(self.part.at[s, dest], self.mine.at[s, k], self.ms.at[k, s])

    def first(self, s, k):
        at, h = self.at, self.half
        src = self.held.at[s, 3, pl.ds(k * h, h)]
        return at.push(src, (self.x1, self.y1)[k].at[s], self.d1s.at[k, s], self.d1r.at[k, s], (at.xn, at.yn)[k])

    def second(self, s, k):
        at = self.at
        src = self.held.at[s, 1 + k]
        return at.push(src, (self.x2, self.y2)[k].at[s], self.d2s.at[k, s], self.d2r.at[k, s], (at.xn, at.yn)[k])

    def start(self, s):
        for k in (3, 1, 2, 0):
            self.core_copy(s, k).start()
            self.load(s, k).start()

    def hop1(self, s):
        self.core_copy(s, 3).wait_recv()
        self.load(s, 3).wait()
        self.held[s, 3] = (self.held[s, 3].astype(F32) + self.mine[s, 3].astype(F32)).astype(BF16)
        self.first(s, 0).start()
        self.first(s, 1).start()

    def hop2(self, s):
        h = self.half
        for k, extra, rows, rest in (
            (0, self.y1, pl.ds(h, h), pl.ds(0, h)),
            (1, self.x1, pl.ds(0, h), pl.ds(h, h)),
        ):
            self.core_copy(s, 1 + k).wait_recv()
            self.load(s, 1 + k).wait()
            self.first(s, 1 - k).wait_recv()
            held, mine = self.held.at[s, 1 + k], self.mine.at[s, 1 + k]
            held[rows] = (held[rows].astype(F32) + mine[rows].astype(F32) + extra[s].astype(F32)).astype(BF16)
            held[rest] = (held[rest].astype(F32) + mine[rest].astype(F32)).astype(BF16)
            self.second(s, k).start()

    def total(self, s):
        self.core_copy(s, 0).wait_recv()
        self.load(s, 0).wait()
        self.second(s, 0).wait_recv()
        self.second(s, 1).wait_recv()
        return (
            self.mine[s, 0].astype(F32)
            + self.held[s, 0].astype(F32)
            + self.x2[s].astype(F32)
            + self.y2[s].astype(F32)
        )

    def finish(self, s):
        for k in range(4):
            self.core_copy(s, k).wait_send()
        for k in range(2):
            self.first(s, k).wait_send()
            self.second(s, k).wait_send()


def each(n, *steps, low=0):
    def run(s, _):
        for step in steps:
            step(s)
        return 0

    lax.fori_loop(low, n, run, 0)


COMM = dict(has_side_effects=True, vmem_limit_bytes=60 << 20)


def front_kernel(
    tok, cot, ids, gates, wq, wk, wv, pk, full, weights, cot_full, gains, small,
    packets, own, gsend, grecv, glocal, csend, crecv, clocal,
    wsend, wrecv, psend, precv, rsend, rrecv, lsend, lrecv, local,
):
    at = Place()
    z = at.rep
    gather = Gather(at, own, full, gsend, grecv, glocal)
    cot_gather = Gather(at, cot, cot_full, csend, crecv, clocal)
    seqs, _, width = tok.shape
    top = ids.shape[1]
    block, cols = wq.shape[0], weights.shape[2]
    quarter = block // 4
    barrier = pltpu.get_barrier_semaphore()
    line = [lax.rem(z + k, 4) for k in range(1, 4)]
    for dev in line:
        pl.semaphore_signal(barrier, inc=1, device_id=(dev, at.me), device_id_type=MESH)
    each(7, lambda m: pl.semaphore_signal(barrier, inc=1, device_id=(z, at.peer(m)), device_id_type=MESH))
    pl.semaphore_wait(barrier, 10)

    def packet_copy(m):
        return at.push(pk, packets.at[at.me], psend.at[m], precv.at[m], at.peer(m))

    def weight_copy(m, j):
        dev = at.peer(m)
        theirs = pl.ds(pl.multiple_of(dev * cols, cols), cols)
        src = (wq, wk, wv)[j].at[pl.ds(pl.multiple_of(z * quarter, quarter), quarter), theirs]
        dst = weights.at[j, pl.ds(pl.multiple_of(at.me * block + z * quarter, quarter), quarter)]
        return at.push(src, dst, wsend.at[m, j], wrecv.at[m, j], dev)

    def weight_landed(m, j):
        dev = at.peer(m)
        dst = weights.at[j, pl.ds(pl.multiple_of(dev * block + z * quarter, quarter), quarter)]
        return at.push(dst, dst, wsend.at[m, j], wrecv.at[m, j], dev)

    def walk(m, q, right):
        part = weights.at[:, pl.ds(pl.multiple_of(at.peer(m) * block + q * quarter, quarter), quarter)]
        send, recv, dev = (rsend, rrecv, z + 1) if right else (lsend, lrecv, z - 1)
        return pltpu.make_async_remote_copy(
            src_ref=part, dst_ref=part, send_sem=send.at[m, q], recv_sem=recv.at[m, q],
            device_id=(dev, at.me), device_id_type=MESH,
        )

    def send_weights(m):
        packet_copy(m).start()
        for j in range(3):
            weight_copy(m, j).start()

    each(7, send_weights)

    place = lax.broadcasted_iota(jnp.int32, (top, 128), 0)
    lane = lax.broadcasted_iota(jnp.int32, (top, 128), 1)
    first = jnp.where(lane == place, 1.0, 0.0).astype(BF16)
    second = jnp.where(lane == place + top, 1.0, 0.0).astype(BF16)

    def join(s):
        own[s, :, 0:width] = tok[s]
        table = dot(ids[s].astype(F32).astype(BF16), first, 0, 0) + dot(gates[s], second, 0, 0)
        own[s, :, width : width + 128] = table.astype(BF16)

    each(seqs, join)
    each(seqs, gather.start)
    own_cols = pl.ds(pl.multiple_of(at.me * cols, cols), cols)
    mine = pl.ds(pl.multiple_of(at.me * block, block), block)
    own_weights = [
        pltpu.make_async_copy(w.at[:, own_cols], weights.at[j, mine], local.at[j]) for j, w in enumerate((wq, wk, wv))
    ]
    for copy in own_weights:
        copy.start()
    early = seqs // 2
    each(early, cot_gather.start)

    def set_out(m):
        for j in range(3):
            weight_landed(m, j).wait_recv()

        @pl.when(z < 3)
        def _():
            walk(m, z, True).start()

        @pl.when(z > 0)
        def _():
            walk(m, z, False).start()

    each(7, set_out)

    def pass_on(d):
        def step(m):
            @pl.when(z - d >= 0)
            def _():
                walk(m, z - d, True).wait_recv()

                @pl.when(z < 3)
                def _():
                    walk(m, z - d, True).start()

            @pl.when(z + d <= 3)
            def _():
                walk(m, z + d, False).wait_recv()

                @pl.when(z > 0)
                def _():
                    walk(m, z + d, False).start()

        each(7, step)

    def relay(i, _):
        gather.relay(2 * i, True)
        gather.relay(2 * i + 1, False)
        return 0

    def cot_relay(i, _):
        cot_gather.relay(2 * i, True)
        cot_gather.relay(2 * i + 1, False)
        return 0

    pairs = seqs // 2
    lax.fori_loop(0, pairs // 2, relay, 0)
    pass_on(1)
    lax.fori_loop(pairs // 2, pairs, relay, 0)
    pass_on(2)
    lax.fori_loop(0, early // 2, cot_relay, 0)
    each(seqs, gather.relay_far)
    each(early, cot_gather.relay_far)
    each(7, lambda m: packet_copy(m).wait_recv())
    packets[at.me] = pk[...]
    devices = packets.shape[0]
    share = width // (128 * devices)
    heads = HEAD_DIM // devices
    gains[...] = jnp.zeros_like(gains)
    small[...] = jnp.zeros_like(small)
    for o in range(devices):
        for k in range(share):
            lanes = pl.ds((o * share + k) * 128, 128)
            gains[0:1, lanes] = packets[o, k : k + 1]
            gains[1:2, lanes] = packets[o, share + k : share + k + 1]
        base = 2 * share
        small[0:1] += pltpu.roll(packets[o, base : base + 1], o * heads, 1)
        small[1:2] += pltpu.roll(packets[o, base + 1 : base + 2], o * heads, 1)
        small[2:3] += pltpu.roll(packets[o, base + 2 : base + 3], o, 1)
    each(seqs, gather.finish)
    each(early, cot_gather.finish)
    pass_on(3)

    def sent(m):
        for q in range(4):

            @pl.when(jnp.logical_and(q <= z, z < 3))
            def _():
                walk(m, q, True).wait_send()

            @pl.when(jnp.logical_and(q >= z, z > 0))
            def _():
                walk(m, q, False).wait_send()

        packet_copy(m).wait_send()
        for j in range(3):
            weight_copy(m, j).wait_send()

    each(7, sent)
    for copy in own_weights:
        copy.wait()


def front(tokens, cotangent, ids, gates, wq, wk, wv, packet):
    seqs, rows, width = tokens.shape
    ep = lax.axis_size("ep")
    cols = wq.shape[1] // ep
    top = ids.shape[1]
    if ep != 8 or lax.axis_size("rep") != 4:
        routes = jnp.concatenate([ids.astype(BF16), gates], axis=1).transpose(0, 2, 1)
        routes = jnp.pad(routes, ((0, 0), (0, 0), (0, 128 - 2 * top)))
        full = lax.all_gather(jnp.concatenate([tokens, routes], axis=-1), "ep", axis=1, tiled=True)
        weights = [lax.all_to_all(w, "ep", split_axis=1, concat_axis=0, tiled=True) for w in (wq, wk, wv)]
        packets = lax.all_gather(packet, "ep", axis=0)
        share, heads = width // (128 * ep), HEAD_DIM // ep
        gains = jnp.stack([packets[:, :share].reshape(width), packets[:, share : 2 * share].reshape(width)])
        lens = jnp.pad(packets[:, 2 * share + 2, 0], (0, 128 - ep))
        few = [packets[:, 2 * share + k, :heads].reshape(HEAD_DIM) for k in range(2)] + [lens]
        return (
            full, jnp.stack(weights), lax.all_gather(cotangent, "ep", axis=1, tiled=True),
            jnp.pad(gains, ((0, 6), (0, 0))), jnp.pad(jnp.stack(few), ((0, 5), (0, 0))),
        )
    dma = pltpu.SemaphoreType.DMA
    return pl.pallas_call(
        front_kernel,
        out_shape=(
            sds((seqs, rows * ep, width + 128), BF16),
            sds((3, wq.shape[0] * ep, cols), BF16),
            sds((seqs, rows * ep, width), BF16),
            sds((8, width), F32),
            sds((8, 128), F32),
        ),
        in_specs=[VM] * 8,
        out_specs=(AN, AN, AN, VM, VM),
        scratch_shapes=[pltpu.VMEM((ep,) + packet.shape, F32), pltpu.VMEM((seqs, rows, width + 128), BF16)]
        + Gather.scratch(seqs)
        + Gather.scratch(seqs)
        + [dma((7, 3)), dma((7, 3)), dma((7,)), dma((7,))]
        + [dma((7, 4))] * 4
        + [dma((3,))],
        compiler_params=pltpu.CompilerParams(collective_id=1, **COMM),
        name="front",
    )(tokens, cotangent, ids, gates, wq, wk, wv, packet)


def plain_living(small, seqs, rows):
    place = (jnp.arange(rows) + lax.axis_index("ep") * rows).astype(F32)
    return (place[None] < small[2, :seqs, None]).astype(F32)[..., None]


def mix(part, tokens, small, gains):
    seqs, rows, _ = tokens.shape
    total = lax.psum_scatter(part, "ep", scatter_dimension=1, tiled=True).astype(F32)
    middle, mixed = mix_rows(total, tokens, plain_living(small, seqs, rows), gains[1])
    return middle, lax.all_gather(mixed, "ep", axis=1, tiled=True)


def back_kernel(gpart, middle, cot, small, gains, mgrad, ggrad, full, own, *scratch):
    at = Place()
    seqs = cot.shape[0]
    n = Reduce.sems
    rg = Reduce(at, gpart, *scratch[:n])
    gather = Gather(at, own, full, *scratch[n:])
    at.greet((at.xn, at.yn, at.sb))
    each(seqs, rg.start)
    each(seqs, rg.hop1)
    each(seqs, rg.hop2)
    ggrad[...] = jnp.zeros_like(ggrad)

    def rows(s):
        living = live_rows(small, s, at.me, cot.shape[1])
        mg, ag, back = ffn_back_rows(rg.total(s), middle[s], cot[s], living, gains[1:2])
        mgrad[s] = mg
        own[s] = ag
        ggrad[...] += jnp.sum(back, axis=0, keepdims=True)
        gather.start(s)

    each(seqs, rows)
    gather_tail(gather, 0, seqs)
    each(seqs, rg.finish)


def back(gpart, middle, cot, small, gains):
    seqs, rows, width = cot.shape
    ep = lax.axis_size("ep")
    if ep != 8:
        mixed_grad = lax.psum_scatter(gpart, "ep", scatter_dimension=1, tiled=True).astype(F32)
        mg, ag, backs = ffn_back_rows(mixed_grad, middle, cot, plain_living(small, seqs, rows), gains[1])
        full = lax.all_gather(ag, "ep", axis=1, tiled=True)
        return mg, jnp.sum(backs, axis=(0, 1))[None], full
    gpart = gpart.reshape(seqs, ep, rows, width)
    return pl.pallas_call(
        back_kernel,
        out_shape=(
            sds(cot.shape, F32),
            sds((1, width), F32),
            sds((seqs, rows * ep, width), BF16),
        ),
        in_specs=[AN] + [VM] * 4,
        out_specs=(VM, VM, AN),
        scratch_shapes=[pltpu.VMEM(cot.shape, BF16)] + Reduce.scratch(gpart) + Gather.scratch(seqs),
        compiler_params=pltpu.CompilerParams(collective_id=3, **COMM),
        name="back",
    )(gpart, middle, cot, small, gains)


def finish_kernel(
    wgrad, wograd, npart, opart, tok, middle, mgrad, gains, others,
    out, small_out, result, tgrad,
    own, held, met, ggrad, parcel, landed, spare,
    wsend, wrecv, local, gsend, grecv, os, or_, ps, pr, qs, qr, fs, fr, ss, sr, *scratch,
):
    at = Place()
    z, me = at.rep, at.me
    n = Reduce.sems
    normed_sum = Reduce(at, npart, *scratch[:n])
    result_sum = Reduce(at, opart, *scratch[n:])
    seqs = tok.shape[0]
    parts, pieces = own.shape[:2]
    chunks = parts * pieces
    width = wgrad.shape[3]
    barrier = pltpu.get_barrier_semaphore()
    line = [lax.rem(z + k, 4) for k in range(1, 4)]
    for dev in line:
        pl.semaphore_signal(barrier, inc=1, device_id=(dev, me), device_id_type=MESH)
    each(7, lambda m: pl.semaphore_signal(barrier, inc=1, device_id=(z, at.peer(m)), device_id_type=MESH))
    pl.semaphore_wait(barrier, 10)
    inner = jnp.logical_and(z > 0, z < 3)
    outer_end, partner, outer = 1 + z // 3, 3 - z, 3 * (z - 1)
    cols = pl.ds(pl.multiple_of(me * width, width), width)

    def column_copy(m, j):
        dev = at.peer(m)
        rows = pl.ds(pl.multiple_of(dev * pieces, pieces), pieces)
        return at.push(wgrad.at[j, rows], own.at[1 + j, :, :, cols], wsend.at[m, j], wrecv.at[m, j], dev)

    mine_rows = pl.ds(pl.multiple_of(me * pieces, pieces), pieces)
    locals_ = [pltpu.make_async_copy(wgrad.at[j, mine_rows], own.at[1 + j, :, :, cols], local.at[j]) for j in range(3)]
    locals_.append(pltpu.make_async_copy(wograd, own.at[0], local.at[3]))
    for copy in locals_:
        copy.start()
    for j in range(3):
        each(7, lambda m, j=j: column_copy(m, j).start())
    each(seqs, normed_sum.start)
    each(seqs, result_sum.start)
    ggrad[...] = jnp.zeros_like(ggrad)

    def piece(ref, c):
        return ref.at[c // pieces, lax.rem(c, pieces)]

    def line_push(src, dst, send, recv, dev):
        return pltpu.make_async_remote_copy(
            src_ref=src, dst_ref=dst, send_sem=send, recv_sem=recv, device_id=(dev, me), device_id_type=MESH
        )

    def inward(c):
        return line_push(piece(own, c), piece(held, c), os.at[c], or_.at[c], outer_end)

    def across(c):
        return line_push(piece(held, c), met.at[c // 2], ps.at[c], pr.at[c], partner)

    def share(c):
        return line_push(piece(out, c), piece(out, c), qs.at[c], qr.at[c], partner)

    def outward(c):
        return line_push(piece(out, c), piece(out, c), fs.at[c], fr.at[c], outer)

    def mine(c):
        return 1 + lax.rem(c, 2) == z

    def ready(part):
        for j in range(parts):

            @pl.when(part == j)
            def _():
                locals_[(3, 0, 1, 2)[j]].wait()
                if j > 0:
                    each(7, lambda m: column_copy(m, j - 1).wait_recv())

    def step(c):
        @pl.when(lax.rem(c, pieces) == 0)
        def _():
            ready(c // pieces)

        @pl.when(jnp.logical_not(inner))
        def _():
            inward(c).start()

        @pl.when(inner)
        def _():
            inward(c).wait_recv()
            here = piece(held, c)
            here[...] = (here[...].astype(F32) + piece(own, c)[...].astype(F32)).astype(BF16)

            @pl.when(jnp.logical_not(mine(c)))
            def _():
                across(c).start()

    def settle(c):
        @pl.when(jnp.logical_and(inner, mine(c)))
        def _():
            across(c).wait_recv()
            piece(out, c)[...] = (piece(held, c)[...].astype(F32) + met[c // 2].astype(F32)).astype(BF16)
            share(c).start()
            outward(c).start()

    def forward(c):
        @pl.when(jnp.logical_and(inner, jnp.logical_not(mine(c))))
        def _():
            share(c).wait_recv()
            outward(c).start()

    def token_rows(s):
        tg, back = attn_back_rows(normed_sum.total(s), tok[s], mgrad[s], gains[0:1])
        tgrad[s] = tg
        ggrad[...] += jnp.sum(back, axis=0, keepdims=True)

    def out_rows(s):
        result[s] = (middle[s] + result_sum.total(s)).astype(BF16)

    jobs = (
        (step, 0, chunks), (settle, 1, chunks), (forward, 2, chunks),
        (normed_sum.hop1, 2, seqs), (normed_sum.hop2, 6, seqs), (token_rows, 10, seqs),
        (result_sum.hop1, 6, seqs), (result_sum.hop2, 10, seqs), (out_rows, 14, seqs),
    )

    def tick(i, _):
        for job, lag, count in jobs:

            @pl.when(jnp.logical_and(i >= lag, i < lag + count))
            def _():
                job(i - lag)

        return 0

    lax.fori_loop(0, max(lag + count for _, lag, count in jobs), tick, 0)

    parcel[...] = jnp.zeros_like(parcel)
    devices = parcel.shape[0]
    rows_of = ggrad.shape[1] // (128 * devices)
    for dev in range(devices):
        for k in range(rows_of):
            lanes = pl.ds((dev * rows_of + k) * 128, 128)
            parcel[dev, k : k + 1] = ggrad[:, lanes]
            parcel[dev, rows_of + k : rows_of + k + 1] = others[0:1, lanes]
        parcel[dev, 2 * rows_of : 2 * rows_of + 2] = others[1:3, 0:128]

    def parcel_copy(m):
        dev = at.peer(m)
        return at.push(parcel.at[dev], landed.at[m], gsend.at[m], grecv.at[m], dev)

    each(7, lambda m: parcel_copy(m).start())
    spare[0] = parcel[me]

    def add_parcel(m):
        parcel_copy(m).wait_recv()
        spare[0] += landed[m]

    each(7, add_parcel)

    def small_copy(k):
        return line_push(spare.at[0], spare.at[1 + k], ss.at[k], sr.at[k], line[k])

    for k in range(3):
        small_copy(k).start()

    @pl.when(jnp.logical_not(inner))
    def _():
        each(chunks, lambda c: outward(c).wait_recv())
        each(chunks, lambda c: inward(c).wait_send())

    @pl.when(inner)
    def _():
        def sent(c):
            outward(c).wait_send()

            @pl.when(mine(c))
            def _():
                share(c).wait_send()

            @pl.when(jnp.logical_not(mine(c)))
            def _():
                across(c).wait_send()

        each(chunks, sent)

    each(seqs, normed_sum.finish, result_sum.finish)

    def all_sent(m):
        parcel_copy(m).wait_send()
        for j in range(3):
            column_copy(m, j).wait_send()

    each(7, all_sent)
    total = spare[0]
    for k in range(3):
        small_copy(k).wait()
        total = total + spare[1 + k]
    small_out[...] = total


def finish(wgrad, wograd, npart, opart, tokens, middle, mgrad, gains, ffn_back, qk_back):
    seqs, rows, width = tokens.shape
    ep = lax.axis_size("ep")
    if ep != 8 or lax.axis_size("rep") != 4:
        normed_grad = lax.psum_scatter(npart, "ep", scatter_dimension=1, tiled=True).astype(F32)
        moe = lax.psum_scatter(opart, "ep", scatter_dimension=1, tiled=True).astype(F32)
        tg, backs = attn_back_rows(normed_grad, tokens, mgrad, gains[0])
        wrows = lax.all_to_all(wgrad, "ep", split_axis=1, concat_axis=2, tiled=True)
        share = width // ep
        small = jnp.concatenate([jnp.sum(backs, axis=(0, 1)), ffn_back[0], qk_back[0], qk_back[1]])
        small = lax.psum(small, ("ep", "rep"))
        mine = lax.axis_index("ep") * share
        cut = [lax.dynamic_slice_in_dim(small, k * width + mine, share).reshape(-1, 128) for k in range(2)]
        small = jnp.concatenate(cut + [small[2 * width :].reshape(2, HEAD_DIM)], axis=0)
        big = lax.psum(jnp.concatenate([wograd[None], wrows], axis=0), "rep")
        return big, jnp.pad(small, ((0, 8 - small.shape[0]), (0, 0))), (middle + moe).astype(BF16), tg
    others = jnp.concatenate([ffn_back, jnp.pad(qk_back[:2], ((0, 0), (0, width - HEAD_DIM)))], axis=0)
    npart, opart = (p.reshape(seqs, ep, rows, width) for p in (npart, opart))
    pieces = 4
    block = wograd.shape[0] // pieces
    wgrad = wgrad.reshape(3, wgrad.shape[1] // block, block, wgrad.shape[2])
    wograd = wograd.reshape(pieces, block, width)
    whole = (4, pieces, block, width)
    dma = pltpu.SemaphoreType.DMA
    chunks = 4 * pieces
    out, small, result, tgrad = pl.pallas_call(
        finish_kernel,
        out_shape=(sds(whole, BF16), sds((8, 128), F32), sds(tokens.shape, BF16), sds(tokens.shape, BF16)),
        in_specs=[VM, VM, AN, AN] + [VM] * 5,
        out_specs=(VM, VM, VM, VM),
        scratch_shapes=[
            pltpu.VMEM(whole, BF16),
            pltpu.VMEM(whole, BF16),
            pltpu.VMEM((chunks // 2, block, width), BF16),
            pltpu.VMEM((1, width), F32),
            pltpu.VMEM((ep, 8, 128), F32),
            pltpu.VMEM((7, 8, 128), F32),
            pltpu.VMEM((4, 8, 128), F32),
        ]
        + [dma((7, 3)), dma((7, 3)), dma((4,)), dma((7,)), dma((7,))]
        + [dma((chunks,))] * 8
        + [dma((3,))] * 2
        + 2 * Reduce.scratch(npart),
        compiler_params=pltpu.CompilerParams(collective_id=4, has_side_effects=True, vmem_limit_bytes=61 << 20),
        name="finish",
    )(wgrad, wograd, npart, opart, tokens, middle, mgrad, gains, others)
    return out.reshape(4, pieces * block, width), small, result, tgrad


def dot(a, b, ca, cb):
    return lax.dot_general(a, b, (((ca,), (cb,)), ((), ())), preferred_element_type=F32)


def rope_tables(table):
    half = HEAD_DIM // 2
    values = table[...]
    turned = pltpu.roll(values, half, 1)
    first = lax.broadcasted_iota(jnp.int32, values.shape, 1) < half
    return jnp.where(first, values, turned), jnp.where(first, -turned, values)


def rope(v, cos, sin_turn):
    return v * cos + pltpu.roll(v, HEAD_DIM // 2, 1) * sin_turn


def probabilities(q, k, length):
    scores = dot(q, k, 1, 1) * HEAD_DIM**-0.5
    column = lax.broadcasted_iota(jnp.int32, (1, scores.shape[1]), 1).astype(F32)
    scores = jnp.where(column < length, scores, -1e9)
    p = jnp.exp(scores - jnp.max(scores, axis=-1, keepdims=True))
    return p * (1.0 / jnp.sum(p, axis=-1, keepdims=True))


def packed_slots(number, table, length_live, top):
    tab = table.astype(F32)
    length = tab.shape[0]
    lane = lax.broadcasted_iota(jnp.int32, tab.shape, 1)
    row = lax.broadcasted_iota(jnp.int32, (length, 1), 0).astype(F32)
    chosen = jnp.logical_and(jnp.logical_and(tab == number, lane < top), row < length_live)
    gates = jnp.where(chosen, pltpu.roll(tab, 128 - top, 1), 0.0).astype(BF16)
    chosen = jnp.where(chosen, 1.0, 0.0).astype(BF16)
    ones = jnp.ones((8, 128), BF16)
    hit = dot(ones, chosen, 1, 1)
    weight = dot(ones, gates, 1, 1)
    earlier = lax.broadcasted_iota(jnp.int32, (length, length), 0)
    later = lax.broadcasted_iota(jnp.int32, (length, length), 1)
    rank = dot(hit.astype(BF16), jnp.where(earlier < later, 1.0, 0.0).astype(BF16), 1, 0)
    return jnp.where(hit > 0.5, rank, -1.0), weight, jnp.sum(hit[0:1], axis=1, keepdims=True)


def attend_rows(top, number, s, block, w, wo, gains, small, table, normed, pre, low, ctx, part, slots, starts):
    width = normed.shape[1]
    length = seq_len(small, s)
    cos, sin = rope_tables(table)
    v = block[:, 0:width].astype(F32)
    x = (v * inverse_rms(v) * gains[0:1]).astype(BF16)
    normed[...] = x
    q_pre, k_pre = dot(x, w[0], 1, 0), dot(x, w[1], 1, 0)
    value = dot(x, w[2], 1, 0).astype(BF16)
    pre[0], pre[1] = q_pre, k_pre
    low[2] = value
    for h in range(q_pre.shape[1] // HEAD_DIM):
        cols = slice(h * HEAD_DIM, (h + 1) * HEAD_DIM)
        rot = []
        for i, (u, g) in enumerate(((q_pre[:, cols], small[0:1]), (k_pre[:, cols], small[1:2]))):
            rot.append(rope(u * inverse_rms(u) * g, cos, sin).astype(BF16))
            low[i, :, cols] = rot[i]
        attention = probabilities(rot[0], rot[1], length).astype(BF16)
        ctx[:, cols] = dot(attention, value[:, cols], 1, 0).astype(BF16)
    part[...] = dot(ctx[...], wo[...], 1, 0).astype(BF16).reshape(part.shape)
    routes = block[:, width : width + 128]
    lane = lax.broadcasted_iota(jnp.int32, (1, 128), 1)
    for j, ref in enumerate(slots):
        slot, weight, count = packed_slots(number + j, routes, length, top)
        ref[0:8] = slot
        ref[8:16] = weight
        row = starts[j : j + 1]
        after = jnp.sum(jnp.where(lane == s, row, 0.0), axis=1, keepdims=True) + 16.0 * jnp.floor((count + 15.0) * 0.0625)
        starts[j : j + 1] = jnp.where(lane == s + 1, after, row)


def attend_kernel(top, number, full, w, wo, gains, small, table, normed, pre, low, ctx, part, slots0, slots1, starts):
    s = pl.program_id(0)

    @pl.when(s == 0)
    def _():
        starts[...] = jnp.zeros_like(starts)

    attend_rows(
        top, number[0].astype(F32), s, full.at[0], w, wo, gains, small, table,
        normed.at[0], pre.at[:, 0], low.at[:, 0], ctx.at[0], part.at[0], (slots0.at[0], slots1.at[0]), starts,
    )


def attend(top, number, full, weights, wo, gains, small, table):
    seqs, length, wide = full.shape
    width = wide - 128
    cols = weights.shape[2]
    row = lambda i, *_: (i, 0, 0)
    row2 = lambda i, *_: (0, i, 0, 0)
    two = lambda i, *_: (0, 0)
    slot = pl.BlockSpec((1, 16, length), row)
    return pl.pallas_call(
        functools.partial(attend_kernel, top),
        out_shape=(
            sds((seqs, length, width), BF16),
            sds((2, seqs, length, cols), F32),
            sds((3, seqs, length, cols), BF16),
            sds((seqs, length, cols), BF16),
            sds((seqs, length, width), BF16),
            sds((seqs, 16, length), F32),
            sds((seqs, 16, length), F32),
            sds((8, 128), F32),
        ),
        grid_spec=pltpu.PrefetchScalarGridSpec(
            num_scalar_prefetch=1,
            grid=(seqs,),
            in_specs=[
                pl.BlockSpec((1, length, wide), row),
                pl.BlockSpec(weights.shape, lambda i, *_: (0, 0, 0)),
                pl.BlockSpec(wo.shape, two),
                pl.BlockSpec((8, width), two),
                pl.BlockSpec((8, 128), two),
                pl.BlockSpec((length, HEAD_DIM), two),
            ],
            out_specs=(
                pl.BlockSpec((1, length, width), row),
                pl.BlockSpec((2, 1, length, cols), row2),
                pl.BlockSpec((3, 1, length, cols), row2),
                pl.BlockSpec((1, length, cols), row),
                pl.BlockSpec((1, length, width), row),
                slot,
                slot,
                pl.BlockSpec((8, 128), two),
            ),
        ),
        compiler_params=pltpu.CompilerParams(dimension_semantics=("arbitrary",), vmem_limit_bytes=60 << 20),
        cost_estimate=pl.CostEstimate(flops=10**10, bytes_accessed=4 * 10**7, transcendentals=10**6),
        name="attend",
    )(number, full, weights, wo, gains, small, table)


def attend_mix_kernel(
    top, local, full, w, wo, gains, small, table, tok, cot, _cot_early,
    normed, pre, low, ctx, middle, mixed, cot_full, slots0, slots1, starts,
    own, blocks, nbuf, pbuf, lbuf, cbuf, part, begins, tsem, ssem, *scratch,
):
    at = Place()
    seqs = tok.shape[0]
    n = Reduce.sems
    reduce = Reduce(at, part, *scratch[:n])
    gather = Gather(at, own, mixed, *scratch[n : n + 3])
    cot_gather = Gather(at, cot, cot_full, *scratch[n + 3 :])
    number = (at.me * local).astype(F32)
    early = seqs // 2
    at.greet((at.xn, at.yn, at.sb))
    each(seqs, cot_gather.start, low=early)
    begins[...] = jnp.zeros_like(begins)

    def load(s):
        return pltpu.make_async_copy(full.at[s], blocks.at[lax.rem(s, 2)], tsem.at[lax.rem(s, 2)])

    def stores(s):
        k = lax.rem(s, 2)
        pairs = ((nbuf.at[k], normed.at[s]), (pbuf.at[k], pre.at[:, s]), (lbuf.at[k], low.at[:, s]), (cbuf.at[k], ctx.at[s]))
        return [pltpu.make_async_copy(src, dst, ssem.at[i, k]) for i, (src, dst) in enumerate(pairs)]

    load(0).start()

    def sequence(s):
        k = lax.rem(s, 2)
        load(s).wait()

        @pl.when(s + 1 < seqs)
        def _():
            load(s + 1).start()

        @pl.when(s >= 2)
        def _():
            for copy in stores(s - 2):
                copy.wait()

        attend_rows(
            top, number, s, blocks.at[k], w, wo, gains, small, table,
            nbuf.at[k], pbuf.at[k], lbuf.at[k], cbuf.at[k], part.at[s], (slots0.at[s], slots1.at[s]), begins,
        )
        for copy in stores(s):
            copy.start()
        reduce.start(s)

    def rows(s):
        living = live_rows(small, s, at.me, tok.shape[1])
        mid, out = mix_rows(reduce.total(s), tok[s], living, gains[1:2])
        middle[s] = mid
        own[s] = out
        gather.start(s)

    def cot_pair(p):
        @pl.when(lax.rem(p, 2) == 0)
        def _():
            cot_gather.relay(early + p, True)
            cot_gather.relay(early + p + 1, False)

    jobs = (
        (sequence, 0, seqs), (reduce.hop1, 1, seqs), (cot_pair, 3, early), (reduce.hop2, 3, seqs),
        (lambda s: cot_gather.relay_far(early + s), 7, early), (rows, 5, seqs),
    )

    def tick(i, _):
        for job, lag, count in jobs:

            @pl.when(jnp.logical_and(i >= lag, i < lag + count))
            def _():
                job(i - lag)

        return 0

    lax.fori_loop(0, max(lag + count for _, lag, count in jobs), tick, 0)
    starts[...] = begins[...].astype(jnp.int32)
    each(seqs, cot_gather.finish, low=early)
    gather_tail(gather, 0, seqs)
    for s in (seqs - 2, seqs - 1):
        for copy in stores(s):
            copy.wait()
    each(seqs, reduce.finish)


def attend_mix(top, local, full, weights, wo, gains, small, table, tokens, cotangent, cot_early):
    seqs, rows, width = tokens.shape
    length = full.shape[1]
    cols = weights.shape[2]
    part = sds((seqs, 8, rows, width), BF16)
    dma = pltpu.SemaphoreType.DMA
    return pl.pallas_call(
        functools.partial(attend_mix_kernel, top, local),
        out_shape=(
            sds((seqs, length, width), BF16),
            sds((2, seqs, length, cols), F32),
            sds((3, seqs, length, cols), BF16),
            sds((seqs, length, cols), BF16),
            sds(tokens.shape, F32),
            sds((seqs, length, width), BF16),
            sds((seqs, length, width), BF16),
            sds((seqs, 16, length), F32),
            sds((seqs, 16, length), F32),
            sds((8, 128), jnp.int32),
        ),
        in_specs=[AN] + [VM] * 7 + [AN],
        out_specs=(AN, AN, AN, AN, VM, AN, AN, VM, VM, VM),
        input_output_aliases={8: 6},
        scratch_shapes=[
            pltpu.VMEM(tokens.shape, BF16),
            pltpu.VMEM((2,) + full.shape[1:], BF16),
            pltpu.VMEM((2, length, width), BF16),
            pltpu.VMEM((2, 2, length, cols), F32),
            pltpu.VMEM((2, 3, length, cols), BF16),
            pltpu.VMEM((2, length, cols), BF16),
            pltpu.VMEM(part.shape, BF16),
            pltpu.VMEM((8, 128), F32),
            dma((2,)),
            dma((4, 2)),
        ]
        + Reduce.scratch(part)
        + Gather.scratch(seqs)
        + Gather.scratch(seqs),
        compiler_params=pltpu.CompilerParams(collective_id=2, **COMM),
        name="attend_mix",
    )(full, weights, wo, gains, small, table, tokens, cotangent, cot_early)


def attend_back_kernel(
    agrad, normed, pre, low, ctx, w, wo, small, table, part, wgrad, wograd, gains, wacc, woacc,
):
    s = pl.program_id(0)
    length = seq_len(small, s)
    cos, sin = rope_tables(table)

    @pl.when(s == 0)
    def _():
        wacc[...] = jnp.zeros_like(wacc)
        woacc[...] = jnp.zeros_like(woacc)
        gains[...] = jnp.zeros_like(gains)

    ag = agrad[0]
    woacc[...] += dot(ctx[0], ag, 0, 0)
    cg_all = dot(ag, wo[...], 1, 1).astype(BF16)
    scale = HEAD_DIM**-0.5
    half = HEAD_DIM // 2
    grads = ([], [], [])
    for h in range(cg_all.shape[1] // HEAD_DIM):
        cols = slice(h * HEAD_DIM, (h + 1) * HEAD_DIM)
        q, k, value, cg = low[0, 0, :, cols], low[1, 0, :, cols], low[2, 0, :, cols], cg_all[:, cols]
        attention = probabilities(q, k, length)
        grads[2].append(dot(attention.astype(BF16), cg, 0, 0).astype(BF16))
        pg = dot(cg, value, 1, 1)
        sg = (attention * (pg - jnp.sum(attention * pg, axis=-1, keepdims=True))).astype(BF16)
        for i, (rot_grad, g) in enumerate(((dot(sg, k, 1, 0), small[0:1]), (dot(sg, q, 0, 0), small[1:2]))):
            wgt = rot_grad * scale
            u = wgt * cos + pltpu.roll(wgt * sin, half, 1)
            v = pre[i, 0, :, cols]
            r = inverse_rms(v)
            grads[i].append(rms_back(v, r, u * g).astype(BF16))
            gains[i : i + 1] += jnp.sum(u * v * r, axis=0, keepdims=True)
    total = None
    for i in range(3):
        g = grads[i][0] if len(grads[i]) == 1 else jnp.concatenate(grads[i], axis=1)
        wacc[i] += dot(normed[0], g, 0, 0)
        piece = dot(g, w[i], 1, 1)
        total = piece if total is None else total + piece
    part[0] = total.astype(BF16)

    @pl.when(s == pl.num_programs(0) - 1)
    def _():
        wgrad[...] = wacc[...].astype(BF16)
        wograd[...] = woacc[...].astype(BF16)


def attend_back(agrad, normed, pre, low, ctx, weights, wo, small, table):
    seqs, length, width = agrad.shape
    cols = weights.shape[2]
    row = lambda i, *_: (i, 0, 0)
    row2 = lambda i, *_: (0, i, 0, 0)
    two = lambda i, *_: (0, 0)
    three = lambda i, *_: (0, 0, 0)
    return pl.pallas_call(
        attend_back_kernel,
        out_shape=(
            sds(agrad.shape, BF16),
            sds(weights.shape, BF16),
            sds(wo.shape, BF16),
            sds((8, HEAD_DIM), F32),
        ),
        grid_spec=pltpu.PrefetchScalarGridSpec(
            num_scalar_prefetch=0,
            grid=(seqs,),
            in_specs=[
                pl.BlockSpec((1, length, width), row),
                pl.BlockSpec((1, length, width), row),
                pl.BlockSpec((2, 1, length, cols), row2),
                pl.BlockSpec((3, 1, length, cols), row2),
                pl.BlockSpec((1, length, cols), row),
                pl.BlockSpec(weights.shape, three),
                pl.BlockSpec(wo.shape, two),
                pl.BlockSpec((8, 128), two),
                pl.BlockSpec((length, HEAD_DIM), two),
            ],
            out_specs=(
                pl.BlockSpec((1, length, width), row),
                pl.BlockSpec(weights.shape, three),
                pl.BlockSpec(wo.shape, two),
                pl.BlockSpec((8, HEAD_DIM), two),
            ),
            scratch_shapes=[
                pltpu.VMEM(weights.shape, F32),
                pltpu.VMEM(wo.shape, F32),
            ],
        ),
        compiler_params=pltpu.CompilerParams(dimension_semantics=("arbitrary",), vmem_limit_bytes=60 << 20),
        cost_estimate=pl.CostEstimate(flops=2 * 10**10, bytes_accessed=4 * 10**7, transcendentals=10**6),
        name="attend_back",
    )(agrad, normed, pre, low, ctx, weights, wo, small, table)


BLOCK = 256
FIRST_TILE = (256, 1024)


def pack_rows(seqs, capacity):
    return -(-seqs * capacity // BLOCK) * BLOCK


def each_block(blocks, hidden, job):
    part = min(hidden, 512)
    parts = hidden // part

    def run(i, _):
        b, h = i // parts, lax.rem(i, parts)
        rows = pl.ds(pl.multiple_of(b * BLOCK, BLOCK), BLOCK)
        low = pl.multiple_of(h * part, part)
        job(rows, pl.ds(low, part), pl.ds(pl.multiple_of(hidden + low, part), part))
        return 0

    lax.fori_loop(0, blocks * parts, run, 0)


def swiglu_back(gate, up, dact):
    sig = 1.0 / (1.0 + jnp.exp(-gate))
    return dact * up * sig * (1.0 + gate * (1.0 - sig)), dact * (gate * sig)


def forward_blocks(blocks, x, dy, wi, wo, acts, dgus):
    def job(rows, gcols, ucols):
        gate = dot(x[rows], wi[:, gcols], 1, 0)
        up = dot(x[rows], wi[:, ucols], 1, 0)
        dact = dot(dy[rows], wo[gcols], 1, 1)
        acts[rows, gcols] = (gate * (1.0 / (1.0 + jnp.exp(-gate))) * up).astype(BF16)
        dgate, dup = swiglu_back(gate, up, dact)
        dgus[rows, gcols] = dgate.astype(BF16)
        dgus[rows, ucols] = dup.astype(BF16)

    each_block(blocks, wo.shape[0], job)


def gradient_tiles(blocks, left, right, result, acc, stage, ssem, busy):
    tr, tc = acc.shape
    down, across = result.shape[0] // tr, result.shape[1] // tc

    def tile(t, _):
        rt, ct = t // across, lax.rem(t, across)
        left_cols = pl.ds(pl.multiple_of(rt * tr, tr), tr)
        right_cols = pl.ds(pl.multiple_of(ct * tc, tc), tc)

        def step(b, _):
            rows = pl.ds(pl.multiple_of(b * BLOCK, BLOCK), BLOCK)
            piece = dot(left[rows, left_cols], right[rows, right_cols], 0, 0)

            @pl.when(b == 0)
            def _():
                acc[...] = piece

            @pl.when(b > 0)
            def _():
                acc[...] += piece

            return 0

        @pl.when(blocks == 0)
        def _():
            acc[...] = jnp.zeros_like(acc)

        lax.fori_loop(0, blocks, step, 0)
        k = lax.rem(t, 2)
        out = pltpu.make_async_copy(stage.at[k], result.at[left_cols, right_cols], ssem.at[k])

        @pl.when(jnp.logical_or(t >= 2, busy))
        def _():
            out.wait()

        stage[k] = acc[...].astype(BF16)
        out.start()
        return 0

    lax.fori_loop(0, down * across, tile, 0)


def drain_tiles(result, acc, stage, ssem):
    tr, tc = acc.shape
    for k in range(2):
        pltpu.make_async_copy(stage.at[k], result.at[pl.ds(0, tr), pl.ds(0, tc)], ssem.at[k]).wait()


def first_kernel(
    capacity, starts, mixed, cot, slots0, slots1, w_in,
    act, pair, x_all, dy_all, out_grad,
    x, dy, wi, acts, pairs, acc, stage, wsem, ssem, rsem,
):
    step = pl.program_id(0)
    steps = pl.num_programs(0)
    together = mixed.shape[0]
    seqs = steps * together
    width = mixed.shape[2]
    hidden = acts.shape[1]
    load = pltpu.make_async_copy(w_in.at[0], wi, wsem)

    @pl.when(step == 0)
    def _():
        load.start()

    packed = []
    for k in range(together):
        spread, gate_spread = [], []
        for slots in (slots0, slots1):
            column = lax.broadcasted_iota(jnp.int32, (capacity, slots.shape[2]), 0).astype(F32)
            place = column == slots[k, 0:1]
            spread.append(jnp.where(place, 1.0, 0.0).astype(BF16))
            gate_spread.append(jnp.where(place, slots[k, 8:9], 0.0).astype(BF16))
        packed.append(
            (
                dot(jnp.concatenate(spread, axis=0), mixed[k], 1, 0).astype(BF16),
                dot(jnp.concatenate(gate_spread, axis=0), cot[k], 1, 0).astype(BF16),
            )
        )
    for k, (x_rows, dy_rows) in enumerate(packed):
        s = step * together + k
        for j in range(2):
            start = pl.multiple_of(starts[j, s], 16)
            x[j, pl.ds(start, capacity)] = x_rows[j * capacity : (j + 1) * capacity]
            dy[j, pl.ds(start, capacity)] = dy_rows[j * capacity : (j + 1) * capacity]

    @pl.when(step == steps - 1)
    def _():
        for j in range(2):
            past = (starts[j, seqs - 1] + capacity) // 16
            end = (starts[j, seqs] + BLOCK - 1) // BLOCK * (BLOCK // 16)

            def clear(i, _):
                rows = pl.ds(pl.multiple_of(i * 16, 16), 16)
                x[j, rows] = jnp.zeros((16, width), BF16)
                dy[j, rows] = jnp.zeros((16, width), BF16)
                return 0

            lax.fori_loop(past, end, clear, 0)
        saves = [pltpu.make_async_copy(x, x_all, rsem.at[0]), pltpu.make_async_copy(dy, dy_all, rsem.at[1])]
        for copy in saves:
            copy.start()
        blocks = (starts[0, seqs] + BLOCK - 1) // BLOCK
        load.wait()

        def forward(rows, gcols, ucols):
            gate = dot(x[0, rows], wi[:, gcols], 1, 0)
            up = dot(x[0, rows], wi[:, ucols], 1, 0)
            acts[rows, gcols] = (gate * (1.0 / (1.0 + jnp.exp(-gate))) * up).astype(BF16)
            pairs[rows, gcols] = gate.astype(BF16)
            pairs[rows, ucols] = up.astype(BF16)

        each_block(blocks, hidden, forward)
        saves += [pltpu.make_async_copy(acts, act.at[0], rsem.at[2]), pltpu.make_async_copy(pairs, pair, rsem.at[3])]
        for copy in saves[2:]:
            copy.start()
        gradient_tiles(blocks, acts, dy.at[0], out_grad, acc, stage, ssem, False)
        drain_tiles(out_grad, acc, stage, ssem)
        for copy in saves:
            copy.wait()


def expert_first(starts, mixed, cot, slots, w_in, hidden, capacity):
    seqs, length, width = mixed.shape
    rows = pack_rows(seqs, capacity)
    dma = pltpu.SemaphoreType.DMA
    seq = lambda i, *_: (i, 0, 0)
    together = 2
    slot_spec = pl.BlockSpec((together, 16, length), seq)
    return pl.pallas_call(
        functools.partial(first_kernel, capacity),
        out_shape=(
            sds((2, rows, hidden), BF16),
            sds((rows, 2 * hidden), BF16),
            sds((2, rows, width), BF16),
            sds((2, rows, width), BF16),
            sds((hidden, width), BF16),
        ),
        grid_spec=pltpu.PrefetchScalarGridSpec(
            num_scalar_prefetch=1,
            grid=(seqs // together,),
            in_specs=[
                pl.BlockSpec((together, length, width), seq),
                pl.BlockSpec((together, length, width), seq),
                slot_spec,
                slot_spec,
                AN,
            ],
            out_specs=(AN, AN, AN, AN, AN),
            scratch_shapes=[
                pltpu.VMEM((2, rows, width), BF16),
                pltpu.VMEM((2, rows, width), BF16),
                pltpu.VMEM(w_in.shape[1:], BF16),
                pltpu.VMEM((rows, hidden), BF16),
                pltpu.VMEM((rows, 2 * hidden), BF16),
                pltpu.VMEM(FIRST_TILE, F32),
                pltpu.VMEM((2,) + FIRST_TILE, BF16),
                dma,
                dma((2,)),
                dma((4,)),
            ],
        ),
        compiler_params=pltpu.CompilerParams(dimension_semantics=("arbitrary",), vmem_limit_bytes=62 << 20),
        cost_estimate=pl.CostEstimate(flops=2 * 10**10, bytes_accessed=6 * 10**7, transcendentals=10**6),
        name="expert_first",
    )(starts, mixed, cot, *slots, w_in)


def in_grad_kernel(
    seqs, starts, x_all, dy_all, pair, w_out, dgu, in_grad, x, dy, wo, pairs, dgus, acc, stage, lsem, wsem, ssem, rsem
):
    blocks = (starts[0, seqs] + BLOCK - 1) // BLOCK
    hidden = wo.shape[0]
    weights = pltpu.make_async_copy(w_out.at[0], wo, wsem)
    weights.start()

    def run(b, action):
        rows = pl.ds(pl.multiple_of(b * BLOCK, BLOCK), BLOCK)
        for copy in (
            pltpu.make_async_copy(dy_all.at[0, rows], dy.at[rows], lsem.at[0, b]),
            pltpu.make_async_copy(pair.at[rows], pairs.at[rows], lsem.at[1, b]),
            pltpu.make_async_copy(x_all.at[0, rows], x.at[rows], lsem.at[2, b]),
        ):
            getattr(copy, action)()
        return 0

    lax.fori_loop(0, blocks, lambda b, _: run(b, "start"), 0)
    weights.wait()
    lax.fori_loop(0, blocks, lambda b, _: run(b, "wait"), 0)

    def backward(rows, gcols, ucols):
        dact = dot(dy[rows], wo[gcols], 1, 1)
        dgate, dup = swiglu_back(pairs[rows, gcols].astype(F32), pairs[rows, ucols].astype(F32), dact)
        dgus[rows, gcols] = dgate.astype(BF16)
        dgus[rows, ucols] = dup.astype(BF16)

    each_block(blocks, hidden, backward)
    save = pltpu.make_async_copy(dgus, dgu.at[0], rsem)
    save.start()
    gradient_tiles(blocks, x, dgus, in_grad, acc, stage, ssem, False)
    drain_tiles(in_grad, acc, stage, ssem)
    save.wait()


def first_in_grad(seqs, starts, x_all, dy_all, pair, w_out):
    rows, width = x_all.shape[1:]
    hidden = w_out.shape[1]
    dma = pltpu.SemaphoreType.DMA
    return pl.pallas_call(
        functools.partial(in_grad_kernel, seqs),
        out_shape=(sds((2, rows, 2 * hidden), BF16), sds((width, 2 * hidden), BF16)),
        grid_spec=pltpu.PrefetchScalarGridSpec(
            num_scalar_prefetch=1,
            grid=(1,),
            in_specs=[AN] * 4,
            out_specs=(AN, AN),
            scratch_shapes=[
                pltpu.VMEM((rows, width), BF16),
                pltpu.VMEM((rows, width), BF16),
                pltpu.VMEM(w_out.shape[1:], BF16),
                pltpu.VMEM((rows, 2 * hidden), BF16),
                pltpu.VMEM((rows, 2 * hidden), BF16),
                pltpu.VMEM((512, 2048), F32),
                pltpu.VMEM((2, 512, 2048), BF16),
                dma((3, rows // BLOCK)),
                dma,
                dma((2,)),
                dma,
            ],
        ),
        compiler_params=pltpu.CompilerParams(dimension_semantics=("arbitrary",), vmem_limit_bytes=60 << 20),
        cost_estimate=pl.CostEstimate(flops=10**10, bytes_accessed=2 * 10**7, transcendentals=0),
        name="first_in_grad",
    )(starts, x_all, dy_all, pair, w_out)


def second_kernel(
    seqs, starts, x_all, dy_all, w_in, w_out, _act, _dgu, act, dgu, in_grad, out_grad,
    x, dy, wi, wo, acts, dgus, acc, stage, wsem, lsem, ssem, rsem,
):
    blocks = (starts[1, seqs] + BLOCK - 1) // BLOCK
    loads = [pltpu.make_async_copy(w_in.at[1], wi, wsem.at[0]), pltpu.make_async_copy(w_out.at[1], wo, wsem.at[1])]

    def load(b, action):
        rows = pl.ds(pl.multiple_of(b * BLOCK, BLOCK), BLOCK)
        for copy in (
            pltpu.make_async_copy(x_all.at[1, rows], x.at[rows], lsem.at[0, b]),
            pltpu.make_async_copy(dy_all.at[1, rows], dy.at[rows], lsem.at[1, b]),
        ):
            getattr(copy, action)()
        return 0

    for copy in loads:
        copy.start()
    lax.fori_loop(0, blocks, lambda b, _: load(b, "start"), 0)
    for copy in loads:
        copy.wait()
    lax.fori_loop(0, blocks, lambda b, _: load(b, "wait"), 0)

    forward_blocks(blocks, x, dy, wi, wo, acts, dgus)
    saves = [pltpu.make_async_copy(acts, act.at[1], rsem.at[0]), pltpu.make_async_copy(dgus, dgu.at[1], rsem.at[1])]
    for copy in saves:
        copy.start()
    gradient_tiles(blocks, x, dgus, in_grad, acc, stage, ssem, False)
    gradient_tiles(blocks, acts, dy, out_grad, acc, stage, ssem, True)
    drain_tiles(out_grad, acc, stage, ssem)
    for copy in saves:
        copy.wait()


def expert_second(seqs, starts, x_all, dy_all, w_in, w_out, act, dgu):
    rows, width = dy_all.shape[1:]
    hidden = w_out.shape[1]
    dma = pltpu.SemaphoreType.DMA
    return pl.pallas_call(
        functools.partial(second_kernel, seqs),
        out_shape=(
            sds(act.shape, BF16), sds(dgu.shape, BF16), sds((width, 2 * hidden), BF16), sds((hidden, width), BF16)
        ),
        input_output_aliases={5: 0, 6: 1},
        grid_spec=pltpu.PrefetchScalarGridSpec(
            num_scalar_prefetch=1,
            grid=(1,),
            in_specs=[AN] * 6,
            out_specs=(AN, AN, AN, AN),
            scratch_shapes=[
                pltpu.VMEM((rows, width), BF16),
                pltpu.VMEM((rows, width), BF16),
                pltpu.VMEM(w_in.shape[1:], BF16),
                pltpu.VMEM(w_out.shape[1:], BF16),
                pltpu.VMEM((rows, hidden), BF16),
                pltpu.VMEM((rows, 2 * hidden), BF16),
                pltpu.VMEM((512, 2048), F32),
                pltpu.VMEM((2, 512, 2048), BF16),
                dma((2,)),
                dma((2, rows // BLOCK)),
                dma((2,)),
                dma((2,)),
            ],
        ),
        compiler_params=pltpu.CompilerParams(dimension_semantics=("arbitrary",), vmem_limit_bytes=60 << 20),
        cost_estimate=pl.CostEstimate(flops=25 * 10**9, bytes_accessed=6 * 10**7, transcendentals=10**6),
        name="expert_second",
    )(starts, x_all, dy_all, w_in, w_out, act, dgu)


def tail_kernel(seqs, starts, act, dgu, w_in, w_out, produced, dx):
    @pl.when(pl.program_id(1) * BLOCK < starts[pl.program_id(0), seqs])
    def _():
        part = min(produced.shape[1], 512)

        def run(i, _):
            cols = pl.ds(pl.multiple_of(i * part, part), part)
            produced[:, cols] = dot(act[...], w_out[:, cols], 1, 0).astype(BF16)
            dx[:, cols] = dot(dgu[...], w_in[cols], 1, 1).astype(BF16)
            return 0

        lax.fori_loop(0, produced.shape[1] // part, run, 0)


def expert_tails(seqs, starts, act, dgu, w_in, w_out):
    _, rows, hidden = act.shape
    width = w_in.shape[1]

    def block(j, i, st):
        return j, jnp.maximum(jnp.minimum(i, (st[j, seqs] + BLOCK - 1) // BLOCK - 1), 0), 0

    out = pl.BlockSpec((None, BLOCK, width), block)
    return pl.pallas_call(
        functools.partial(tail_kernel, seqs),
        out_shape=(sds((2, rows, width), BF16), sds((2, rows, width), BF16)),
        grid_spec=pltpu.PrefetchScalarGridSpec(
            num_scalar_prefetch=1,
            grid=(2, rows // BLOCK),
            in_specs=[
                pl.BlockSpec((None, BLOCK, hidden), block),
                pl.BlockSpec((None, BLOCK, 2 * hidden), block),
                pl.BlockSpec((None,) + w_in.shape[1:], lambda j, i, *_: (j, 0, 0)),
                pl.BlockSpec((None,) + w_out.shape[1:], lambda j, i, *_: (j, 0, 0)),
            ],
            out_specs=(out, out),
        ),
        compiler_params=pltpu.CompilerParams(dimension_semantics=("arbitrary", "arbitrary"), vmem_limit_bytes=60 << 20),
        cost_estimate=pl.CostEstimate(flops=24 * 10**9, bytes_accessed=6 * 10**7, transcendentals=0),
        name="expert_tails",
    )(starts, act, dgu, w_in, w_out)


def combine_kernel(capacity, local, *refs):
    s = pl.program_id(0)
    starts = refs[0]
    slots = refs[1 : 1 + local]
    produced, dx, out_part, grad_part = refs[1 + local :]
    out_sum, grad_sum = None, None
    for j in range(local):
        length = slots[j].shape[2]
        column = lax.broadcasted_iota(jnp.int32, (capacity, length), 0).astype(F32)
        place = column == slots[j][0, 0:1]
        span = pl.ds(pl.multiple_of(starts[j, s], 16), capacity)
        held = lax.broadcasted_iota(jnp.int32, (capacity, 1), 0) < starts[j, s + 1] - starts[j, s]
        rows = jnp.where(held, produced[j, span], 0.0).astype(BF16)
        grads = jnp.where(held, dx[j, span], 0.0).astype(BF16)
        out = dot(jnp.where(place, slots[j][0, 8:9], 0.0).astype(BF16), rows, 0, 0)
        grad = dot(jnp.where(place, 1.0, 0.0).astype(BF16), grads, 0, 0)
        out_sum = out if out_sum is None else out_sum + out
        grad_sum = grad if grad_sum is None else grad_sum + grad
    out_part[0] = out_sum.astype(BF16)
    grad_part[0] = grad_sum.astype(BF16)


def combine(starts, slots, produced, dx, capacity):
    local = len(slots)
    seqs, _, length = slots[0].shape
    width = produced.shape[2]
    seq = lambda i, *_: (i, 0, 0)
    rows = pl.BlockSpec(produced.shape, lambda i, *_: (0, 0, 0))
    return pl.pallas_call(
        functools.partial(combine_kernel, capacity, local),
        out_shape=(sds((seqs, length, width), BF16), sds((seqs, length, width), BF16)),
        grid_spec=pltpu.PrefetchScalarGridSpec(
            num_scalar_prefetch=1,
            grid=(seqs,),
            in_specs=[pl.BlockSpec((1, 16, length), seq)] * local + [rows] * 2,
            out_specs=(pl.BlockSpec((1, length, width), seq), pl.BlockSpec((1, length, width), seq)),
        ),
        compiler_params=pltpu.CompilerParams(dimension_semantics=("arbitrary",), vmem_limit_bytes=60 << 20),
        cost_estimate=pl.CostEstimate(flops=3 * 10**9, bytes_accessed=4 * 10**7, transcendentals=0),
        name="combine",
    )(starts, *slots, produced, dx)


def shards(
    tokens, cotangent, gate_weights, expert_ids, seq_lengths, query_weight, key_weight, value_weight,
    output_weight, attn_gain, ffn_gain, query_gain, key_gain, expert_in, expert_out,
):
    ep = lax.axis_size("ep")
    me = lax.axis_index("ep")
    seqs, rows, _ = tokens.shape
    length = rows * ep
    top = gate_weights.shape[2]
    local = expert_in.shape[0]
    hidden = expert_out.shape[1]
    experts = local * ep
    capacity = -(-(length * top * 9 // (8 * experts)) // 16) * 16

    gains = jnp.concatenate([attn_gain, ffn_gain]).astype(F32).reshape(-1, 128)
    few = [query_gain.astype(F32), key_gain.astype(F32), seq_lengths.astype(F32)]
    few = jnp.stack([jnp.pad(v, (0, 128 - v.shape[0])) for v in few])
    packet = jnp.concatenate([gains, few], axis=0)
    packet = jnp.pad(packet, ((0, -packet.shape[0] % 8), (0, 0)))
    share = gains.shape[0] // 2

    full, weights, cot_full, gains, small_in = front(
        tokens, cotangent, expert_ids.transpose(0, 2, 1), gate_weights.transpose(0, 2, 1),
        query_weight, key_weight, value_weight, packet,
    )

    half = HEAD_DIM // 2
    frequency = ROPE_BASE ** (-(np.arange(half, dtype=np.float32) * np.float32(2.0 / HEAD_DIM)))
    angles = np.arange(length, dtype=np.float32)[:, None] * frequency.astype(np.float32)[None, :]
    table = jnp.asarray(np.concatenate([np.cos(angles), np.sin(angles)], axis=-1), F32)

    if ep == 8 and lax.axis_size("rep") == 4:
        normed, pre, low, ctx, middle, mixed, cot_full, slots0, slots1, starts = attend_mix(
            top, local, full, weights, output_weight, gains, small_in, table, tokens, cotangent, cot_full
        )
    else:
        number = (me * local).astype(jnp.int32)[None]
        normed, pre, low, ctx, part, slots0, slots1, starts = attend(
            top, number, full, weights, output_weight, gains, small_in, table
        )
        starts = starts.astype(jnp.int32)
        middle, mixed = mix(part, tokens, small_in, gains)

    act, pair, x_all, dy_all, out_grad0 = expert_first(
        starts, mixed, cot_full, (slots0, slots1), expert_in, hidden, capacity
    )

    def over_rep(value):
        return lax.psum_scatter(value, "rep", scatter_dimension=0, tiled=True)

    out0 = over_rep(out_grad0)
    dgu, in_grad0 = first_in_grad(seqs, starts, x_all, dy_all, pair, expert_out)
    in0 = over_rep(in_grad0)
    x_all, _ = lax.optimization_barrier((x_all, in_grad0))
    act, dgu, in_grad1, out_grad1 = expert_second(seqs, starts, x_all, dy_all, expert_in, expert_out, act, dgu)
    in1 = over_rep(in_grad1)
    out1 = over_rep(out_grad1)
    produced, dx = expert_tails(seqs, starts, act, dgu, expert_in, expert_out)
    out_part, grad_part = combine(starts, (slots0, slots1), produced, dx, capacity)

    mgrad, ffn_back, agrad = back(grad_part, middle, cotangent, small_in, gains)
    npart, wgrad, wograd, qk_back = attend_back(
        agrad, normed, pre, low, ctx, weights, output_weight, small_in, table
    )
    sums, small, result, token_grad = finish(
        wgrad, wograd, npart, out_part, tokens, middle, mgrad, gains, ffn_back, qk_back
    )

    def widen(into, value, j):
        return lax.dynamic_update_slice(into, value.astype(F32)[None], (j, 0, 0))

    small, out0 = lax.optimization_barrier((small, out0))
    out_all = widen(jnp.zeros((local,) + out0.shape, F32), out0, 0)
    small, out_all = lax.optimization_barrier((small, out_all))

    def head_share(vector):
        return lax.dynamic_slice_in_dim(vector, me * (HEAD_DIM // ep), HEAD_DIM // ep)

    return (
        result,
        token_grad,
        sums[1].astype(F32),
        sums[2].astype(F32),
        sums[3].astype(F32),
        sums[0].astype(F32),
        small[:share].reshape(-1),
        small[share : 2 * share].reshape(-1),
        head_share(small[2 * share]),
        head_share(small[2 * share + 1]),
        jnp.stack([in0, in1]).astype(F32),
        widen(out_all, out1, 1),
    )


def solution(mesh):
    seq = P("rep", "ep", None)
    row, gain, expert = P("ep", None), P("ep"), P("ep", None, None)
    split = P("ep", "rep", None)

    return jax.shard_map(
        shards,
        mesh=mesh,
        in_specs=(seq, seq, seq, seq, P(("rep", "ep")), row, row, row, row, gain, gain, gain, gain, expert, expert),
        out_specs=(seq, seq, row, row, row, row, gain, gain, gain, gain, split, split),
        check_vma=False,
    )
```

```python
import functools

import jax
import jax.numpy as jnp
import numpy as np
from jax import lax
from jax.experimental import pallas as pl
from jax.experimental.pallas import tpu as pltpu
from jax.sharding import PartitionSpec as P

HEAD_DIM = 128
EPS = 1e-06
ROPE_BASE = 50000.0
MESH = pl.DeviceIdType.MESH
F32 = jnp.float32
BF16 = jnp.bfloat16


def sds(shape, dtype):
    return jax.ShapeDtypeStruct(shape, dtype)


VM = pl.BlockSpec(memory_space=pltpu.VMEM)
AN = pl.BlockSpec(memory_space=pl.ANY)


def inverse_rms(v):
    return lax.rsqrt(jnp.mean(v * v, axis=-1, keepdims=True) + EPS)


def rms_back(v, r, ug):
    return r * ug - v * (r * r * r * jnp.mean(ug * v, axis=-1, keepdims=True))


def mix_rows(total, tok, living, gain):
    middle = tok.astype(F32) + living * total
    mixed = middle * inverse_rms(middle) * gain
    return middle, mixed.astype(BF16)


def ffn_back_rows(mixed_grad, middle, cot, living, gain):
    r = inverse_rms(middle)
    middle_grad = cot.astype(F32) + rms_back(middle, r, mixed_grad * gain)
    return middle_grad, (living * middle_grad).astype(BF16), mixed_grad * middle * r


def attn_back_rows(normed_grad, tok, middle_grad, gain):
    v = tok.astype(F32)
    r = inverse_rms(v)
    return (middle_grad + rms_back(v, r, normed_grad * gain)).astype(BF16), normed_grad * v * r


def seq_len(small, s):
    lane = lax.broadcasted_iota(jnp.int32, (1, 128), 1)
    return jnp.sum(jnp.where(lane == s, small[2:3, :], 0.0), axis=1, keepdims=True)


def live_rows(small, s, me, rows):
    place = (lax.broadcasted_iota(jnp.int32, (rows, 1), 0) + me * rows).astype(F32)
    return jnp.where(place < seq_len(small, s), 1.0, 0.0)


class Place:
    def __init__(self):
        me = lax.axis_index("ep")
        core, x, y = lax.rem(me, 2), lax.rem(me // 2, 2), me // 4
        self.rep = lax.axis_index("rep")
        self.me = me
        self.sb = me + 1 - 2 * core
        self.dx = 2 - 4 * x
        self.dy = 4 - 8 * y
        self.xn = me + self.dx
        self.yn = me + self.dy
        self.dg = me + self.dx + self.dy

    def push(self, src, dst, send, recv, dev):
        return pltpu.make_async_remote_copy(
            src_ref=src, dst_ref=dst, send_sem=send, recv_sem=recv, device_id=(self.rep, dev), device_id_type=MESH
        )

    def peer(self, m):
        k = m + 1
        return self.me + (k % 2) * (self.sb - self.me) + (k // 2 % 2) * self.dx + (k // 4) * self.dy

    def greet(self, peers):
        barrier = pltpu.get_barrier_semaphore()
        for peer in peers:
            pl.semaphore_signal(barrier, inc=1, device_id=(self.rep, peer), device_id_type=MESH)
        pl.semaphore_wait(barrier, len(peers))


class Gather:
    sems = 3

    def __init__(self, at, own, full, ssem, rsem, lsem):
        self.at, self.own, self.full, self.ssem, self.rsem, self.lsem = at, own, full, ssem, rsem, lsem
        self.rows = own.shape[1]

    @staticmethod
    def scratch(seqs):
        return [pltpu.SemaphoreType.DMA((7, seqs)), pltpu.SemaphoreType.DMA((8, seqs)), pltpu.SemaphoreType.DMA((seqs,))]

    def block(self, s, dev):
        return self.full.at[s, pl.ds(pl.multiple_of(dev * self.rows, self.rows), self.rows)]

    def copy(self, s, dev, kind, slot, to, src=None):
        block = self.block(s, dev)
        return self.at.push(block if src is None else src, block, self.ssem.at[kind, s], self.rsem.at[slot, s], to)

    def start(self, s):
        at, own = self.at, self.own.at[s]
        self.copy(s, at.me, 0, 2, at.xn, own).start()
        self.copy(s, at.me, 1, 4, at.yn, own).start()
        self.copy(s, at.me, 2, 1, at.sb, own).start()
        pltpu.make_async_copy(own, self.block(s, at.me), self.lsem.at[s]).start()

    def relay(self, s, by_y):
        at = self.at
        self.copy(s, at.xn, 0, 2, at.xn).wait_recv()
        if by_y:
            self.copy(s, at.xn, 3, 6, at.yn).start()
        self.copy(s, at.xn, 4, 3, at.sb).start()
        self.copy(s, at.yn, 1, 4, at.yn).wait_recv()
        if not by_y:
            self.copy(s, at.yn, 3, 6, at.xn).start()
        self.copy(s, at.yn, 5, 5, at.sb).start()

    def relay_far(self, s):
        at = self.at
        self.copy(s, at.dg, 3, 6, at.yn).wait_recv()
        self.copy(s, at.dg, 6, 7, at.sb).start()

    def finish(self, s):
        at = self.at
        for dev, slot in ((at.sb, 1), (at.sb + at.dx, 3), (at.sb + at.dy, 5), (at.sb + at.dx + at.dy, 7)):
            self.copy(s, dev, 0, slot, at.sb).wait_recv()
        for kind in range(7):
            self.copy(s, at.me, kind, 0, at.sb).wait_send()
        pltpu.make_async_copy(self.own.at[s], self.block(s, at.me), self.lsem.at[s]).wait()


def gather_tail(gather, low, high):
    def relay(i, _):
        gather.relay(low + 2 * i, True)
        gather.relay(low + 2 * i + 1, False)
        return 0

    lax.fori_loop(0, (high - low) // 2, relay, 0)
    each(high, gather.relay_far, low=low)
    each(high, gather.finish, low=low)


class Reduce:
    def __init__(self, at, part, held, mine, x1, y1, x2, y2, ms, hs, hr, d1s, d1r, d2s, d2r):
        self.at, self.part, self.held, self.mine = at, part, held, mine
        self.x1, self.y1, self.x2, self.y2 = x1, y1, x2, y2
        self.ms, self.hs, self.hr, self.d1s, self.d1r, self.d2s, self.d2r = ms, hs, hr, d1s, d1r, d2s, d2r
        self.half = part.shape[2] // 2

    @staticmethod
    def scratch(part):
        s, _, t, d = part.shape
        dma = pltpu.SemaphoreType.DMA
        return [
            pltpu.VMEM((s, 4, t, d), BF16),
            pltpu.VMEM((s, 4, t, d), BF16),
            pltpu.VMEM((s, t // 2, d), BF16),
            pltpu.VMEM((s, t // 2, d), BF16),
            pltpu.VMEM((s, t, d), BF16),
            pltpu.VMEM((s, t, d), BF16),
            dma((4, s)),
            dma((4, s)),
            dma((4, s)),
            dma((2, s)),
            dma((2, s)),
            dma((2, s)),
            dma((2, s)),
        ]

    sems = 13

    def core_copy(self, s, k):
        at = self.at
        dest = (at.sb, at.sb + at.dx, at.sb + at.dy, at.sb + at.dx + at.dy)[k]
        return at.push(self.part.at[s, dest], self.held.at[s, k], self.hs.at[k, s], self.hr.at[k, s], at.sb)

    def load(self, s, k):
        at = self.at
        dest = (at.me, at.xn, at.yn, at.dg)[k]
        return pltpu.make_async_copy(self.part.at[s, dest], self.mine.at[s, k], self.ms.at[k, s])

    def first(self, s, k):
        at, h = self.at, self.half
        src = self.held.at[s, 3, pl.ds(k * h, h)]
        return at.push(src, (self.x1, self.y1)[k].at[s], self.d1s.at[k, s], self.d1r.at[k, s], (at.xn, at.yn)[k])

    def second(self, s, k):
        at = self.at
        src = self.held.at[s, 1 + k]
        return at.push(src, (self.x2, self.y2)[k].at[s], self.d2s.at[k, s], self.d2r.at[k, s], (at.xn, at.yn)[k])

    def start(self, s):
        for k in (3, 1, 2, 0):
            self.core_copy(s, k).start()
            self.load(s, k).start()

    def hop1(self, s):
        self.core_copy(s, 3).wait_recv()
        self.load(s, 3).wait()
        self.held[s, 3] = (self.held[s, 3].astype(F32) + self.mine[s, 3].astype(F32)).astype(BF16)
        self.first(s, 0).start()
        self.first(s, 1).start()

    def hop2(self, s):
        h = self.half
        for k, extra, rows, rest in (
            (0, self.y1, pl.ds(h, h), pl.ds(0, h)),
            (1, self.x1, pl.ds(0, h), pl.ds(h, h)),
        ):
            self.core_copy(s, 1 + k).wait_recv()
            self.load(s, 1 + k).wait()
            self.first(s, 1 - k).wait_recv()
            held, mine = self.held.at[s, 1 + k], self.mine.at[s, 1 + k]
            held[rows] = (held[rows].astype(F32) + mine[rows].astype(F32) + extra[s].astype(F32)).astype(BF16)
            held[rest] = (held[rest].astype(F32) + mine[rest].astype(F32)).astype(BF16)
            self.second(s, k).start()

    def total(self, s):
        self.core_copy(s, 0).wait_recv()
        self.load(s, 0).wait()
        self.second(s, 0).wait_recv()
        self.second(s, 1).wait_recv()
        return (
            self.mine[s, 0].astype(F32)
            + self.held[s, 0].astype(F32)
            + self.x2[s].astype(F32)
            + self.y2[s].astype(F32)
        )

    def finish(self, s):
        for k in range(4):
            self.core_copy(s, k).wait_send()
        for k in range(2):
            self.first(s, k).wait_send()
            self.second(s, k).wait_send()


def each(n, *steps, low=0):
    def run(s, _):
        for step in steps:
            step(s)
        return 0

    lax.fori_loop(low, n, run, 0)


COMM = dict(has_side_effects=True, vmem_limit_bytes=60 << 20)


def front_kernel(
    tok, cot, ids, gates, wq, wk, wv, pk, full, weights, cot_full, gains, small,
    packets, own, gsend, grecv, glocal, csend, crecv, clocal,
    wsend, wrecv, psend, precv, rsend, rrecv, lsend, lrecv, local,
):
    at = Place()
    z = at.rep
    gather = Gather(at, own, full, gsend, grecv, glocal)
    cot_gather = Gather(at, cot, cot_full, csend, crecv, clocal)
    seqs, _, width = tok.shape
    top = ids.shape[1]
    block, cols = wq.shape[0], weights.shape[2]
    quarter = block // 4
    barrier = pltpu.get_barrier_semaphore()
    line = [lax.rem(z + k, 4) for k in range(1, 4)]
    for dev in line:
        pl.semaphore_signal(barrier, inc=1, device_id=(dev, at.me), device_id_type=MESH)
    each(7, lambda m: pl.semaphore_signal(barrier, inc=1, device_id=(z, at.peer(m)), device_id_type=MESH))
    pl.semaphore_wait(barrier, 10)

    def packet_copy(m):
        return at.push(pk, packets.at[at.me], psend.at[m], precv.at[m], at.peer(m))

    def weight_copy(m, j):
        dev = at.peer(m)
        theirs = pl.ds(pl.multiple_of(dev * cols, cols), cols)
        src = (wq, wk, wv)[j].at[pl.ds(pl.multiple_of(z * quarter, quarter), quarter), theirs]
        dst = weights.at[j, pl.ds(pl.multiple_of(at.me * block + z * quarter, quarter), quarter)]
        return at.push(src, dst, wsend.at[m, j], wrecv.at[m, j], dev)

    def weight_landed(m, j):
        dev = at.peer(m)
        dst = weights.at[j, pl.ds(pl.multiple_of(dev * block + z * quarter, quarter), quarter)]
        return at.push(dst, dst, wsend.at[m, j], wrecv.at[m, j], dev)

    def walk(m, q, right):
        part = weights.at[:, pl.ds(pl.multiple_of(at.peer(m) * block + q * quarter, quarter), quarter)]
        send, recv, dev = (rsend, rrecv, z + 1) if right else (lsend, lrecv, z - 1)
        return pltpu.make_async_remote_copy(
            src_ref=part, dst_ref=part, send_sem=send.at[m, q], recv_sem=recv.at[m, q],
            device_id=(dev, at.me), device_id_type=MESH,
        )

    def send_weights(m):
        packet_copy(m).start()
        for j in range(3):
            weight_copy(m, j).start()

    each(7, send_weights)

    place = lax.broadcasted_iota(jnp.int32, (top, 128), 0)
    lane = lax.broadcasted_iota(jnp.int32, (top, 128), 1)
    first = jnp.where(lane == place, 1.0, 0.0).astype(BF16)
    second = jnp.where(lane == place + top, 1.0, 0.0).astype(BF16)

    def join(s):
        own[s, :, 0:width] = tok[s]
        table = dot(ids[s].astype(F32).astype(BF16), first, 0, 0) + dot(gates[s], second, 0, 0)
        own[s, :, width : width + 128] = table.astype(BF16)

    each(seqs, join)
    each(seqs, gather.start)
    own_cols = pl.ds(pl.multiple_of(at.me * cols, cols), cols)
    mine = pl.ds(pl.multiple_of(at.me * block, block), block)
    own_weights = [
        pltpu.make_async_copy(w.at[:, own_cols], weights.at[j, mine], local.at[j]) for j, w in enumerate((wq, wk, wv))
    ]
    for copy in own_weights:
        copy.start()
    early = seqs // 2
    each(early, cot_gather.start)

    def set_out(m):
        for j in range(3):
            weight_landed(m, j).wait_recv()

        @pl.when(z < 3)
        def _():
            walk(m, z, True).start()

        @pl.when(z > 0)
        def _():
            walk(m, z, False).start()

    each(7, set_out)

    def pass_on(d):
        def step(m):
            @pl.when(z - d >= 0)
            def _():
                walk(m, z - d, True).wait_recv()

                @pl.when(z < 3)
                def _():
                    walk(m, z - d, True).start()

            @pl.when(z + d <= 3)
            def _():
                walk(m, z + d, False).wait_recv()

                @pl.when(z > 0)
                def _():
                    walk(m, z + d, False).start()

        each(7, step)

    def relay(i, _):
        gather.relay(2 * i, True)
        gather.relay(2 * i + 1, False)
        return 0

    def cot_relay(i, _):
        cot_gather.relay(2 * i, True)
        cot_gather.relay(2 * i + 1, False)
        return 0

    pairs = seqs // 2
    lax.fori_loop(0, pairs // 2, relay, 0)
    pass_on(1)
    lax.fori_loop(pairs // 2, pairs, relay, 0)
    pass_on(2)
    lax.fori_loop(0, early // 2, cot_relay, 0)
    each(seqs, gather.relay_far)
    each(early, cot_gather.relay_far)
    each(7, lambda m: packet_copy(m).wait_recv())
    packets[at.me] = pk[...]
    devices = packets.shape[0]
    share = width // (128 * devices)
    heads = HEAD_DIM // devices
    gains[...] = jnp.zeros_like(gains)
    small[...] = jnp.zeros_like(small)
    for o in range(devices):
        for k in range(share):
            lanes = pl.ds((o * share + k) * 128, 128)
            gains[0:1, lanes] = packets[o, k : k + 1]
            gains[1:2, lanes] = packets[o, share + k : share + k + 1]
        base = 2 * share
        small[0:1] += pltpu.roll(packets[o, base : base + 1], o * heads, 1)
        small[1:2] += pltpu.roll(packets[o, base + 1 : base + 2], o * heads, 1)
        small[2:3] += pltpu.roll(packets[o, base + 2 : base + 3], o, 1)
    each(seqs, gather.finish)
    each(early, cot_gather.finish)
    pass_on(3)

    def sent(m):
        for q in range(4):

            @pl.when(jnp.logical_and(q <= z, z < 3))
            def _():
                walk(m, q, True).wait_send()

            @pl.when(jnp.logical_and(q >= z, z > 0))
            def _():
                walk(m, q, False).wait_send()

        packet_copy(m).wait_send()
        for j in range(3):
            weight_copy(m, j).wait_send()

    each(7, sent)
    for copy in own_weights:
        copy.wait()


def front(tokens, cotangent, ids, gates, wq, wk, wv, packet):
    seqs, rows, width = tokens.shape
    ep = lax.axis_size("ep")
    cols = wq.shape[1] // ep
    top = ids.shape[1]
    if ep != 8 or lax.axis_size("rep") != 4:
        routes = jnp.concatenate([ids.astype(BF16), gates], axis=1).transpose(0, 2, 1)
        routes = jnp.pad(routes, ((0, 0), (0, 0), (0, 128 - 2 * top)))
        full = lax.all_gather(jnp.concatenate([tokens, routes], axis=-1), "ep", axis=1, tiled=True)
        weights = [lax.all_to_all(w, "ep", split_axis=1, concat_axis=0, tiled=True) for w in (wq, wk, wv)]
        packets = lax.all_gather(packet, "ep", axis=0)
        share, heads = width // (128 * ep), HEAD_DIM // ep
        gains = jnp.stack([packets[:, :share].reshape(width), packets[:, share : 2 * share].reshape(width)])
        lens = jnp.pad(packets[:, 2 * share + 2, 0], (0, 128 - ep))
        few = [packets[:, 2 * share + k, :heads].reshape(HEAD_DIM) for k in range(2)] + [lens]
        return (
            full, jnp.stack(weights), lax.all_gather(cotangent, "ep", axis=1, tiled=True),
            jnp.pad(gains, ((0, 6), (0, 0))), jnp.pad(jnp.stack(few), ((0, 5), (0, 0))),
        )
    dma = pltpu.SemaphoreType.DMA
    return pl.pallas_call(
        front_kernel,
        out_shape=(
            sds((seqs, rows * ep, width + 128), BF16),
            sds((3, wq.shape[0] * ep, cols), BF16),
            sds((seqs, rows * ep, width), BF16),
            sds((8, width), F32),
            sds((8, 128), F32),
        ),
        in_specs=[VM] * 8,
        out_specs=(AN, AN, AN, VM, VM),
        scratch_shapes=[pltpu.VMEM((ep,) + packet.shape, F32), pltpu.VMEM((seqs, rows, width + 128), BF16)]
        + Gather.scratch(seqs)
        + Gather.scratch(seqs)
        + [dma((7, 3)), dma((7, 3)), dma((7,)), dma((7,))]
        + [dma((7, 4))] * 4
        + [dma((3,))],
        compiler_params=pltpu.CompilerParams(collective_id=1, **COMM),
        name="front",
    )(tokens, cotangent, ids, gates, wq, wk, wv, packet)


def plain_living(small, seqs, rows):
    place = (jnp.arange(rows) + lax.axis_index("ep") * rows).astype(F32)
    return (place[None] < small[2, :seqs, None]).astype(F32)[..., None]


def mix(part, tokens, small, gains):
    seqs, rows, _ = tokens.shape
    total = lax.psum_scatter(part, "ep", scatter_dimension=1, tiled=True).astype(F32)
    middle, mixed = mix_rows(total, tokens, plain_living(small, seqs, rows), gains[1])
    return middle, lax.all_gather(mixed, "ep", axis=1, tiled=True)


def back_kernel(gpart, middle, cot, small, gains, mgrad, ggrad, full, own, *scratch):
    at = Place()
    seqs = cot.shape[0]
    n = Reduce.sems
    rg = Reduce(at, gpart, *scratch[:n])
    gather = Gather(at, own, full, *scratch[n:])
    at.greet((at.xn, at.yn, at.sb))
    each(seqs, rg.start)
    each(seqs, rg.hop1)
    each(seqs, rg.hop2)
    ggrad[...] = jnp.zeros_like(ggrad)

    def rows(s):
        living = live_rows(small, s, at.me, cot.shape[1])
        mg, ag, back = ffn_back_rows(rg.total(s), middle[s], cot[s], living, gains[1:2])
        mgrad[s] = mg
        own[s] = ag
        ggrad[...] += jnp.sum(back, axis=0, keepdims=True)
        gather.start(s)

    each(seqs, rows)
    gather_tail(gather, 0, seqs)
    each(seqs, rg.finish)


def back(gpart, middle, cot, small, gains):
    seqs, rows, width = cot.shape
    ep = lax.axis_size("ep")
    if ep != 8:
        mixed_grad = lax.psum_scatter(gpart, "ep", scatter_dimension=1, tiled=True).astype(F32)
        mg, ag, backs = ffn_back_rows(mixed_grad, middle, cot, plain_living(small, seqs, rows), gains[1])
        full = lax.all_gather(ag, "ep", axis=1, tiled=True)
        return mg, jnp.sum(backs, axis=(0, 1))[None], full
    gpart = gpart.reshape(seqs, ep, rows, width)
    return pl.pallas_call(
        back_kernel,
        out_shape=(
            sds(cot.shape, F32),
            sds((1, width), F32),
            sds((seqs, rows * ep, width), BF16),
        ),
        in_specs=[AN] + [VM] * 4,
        out_specs=(VM, VM, AN),
        scratch_shapes=[pltpu.VMEM(cot.shape, BF16)] + Reduce.scratch(gpart) + Gather.scratch(seqs),
        compiler_params=pltpu.CompilerParams(collective_id=3, **COMM),
        name="back",
    )(gpart, middle, cot, small, gains)


def finish_kernel(
    wgrad, wograd, npart, opart, tok, middle, mgrad, gains, others,
    out, small_out, result, tgrad,
    own, held, met, ggrad, parcel, landed, spare,
    wsend, wrecv, local, gsend, grecv, os, or_, ps, pr, qs, qr, fs, fr, ss, sr, *scratch,
):
    at = Place()
    z, me = at.rep, at.me
    n = Reduce.sems
    normed_sum = Reduce(at, npart, *scratch[:n])
    result_sum = Reduce(at, opart, *scratch[n:])
    seqs = tok.shape[0]
    parts, pieces = own.shape[:2]
    chunks = parts * pieces
    width = wgrad.shape[3]
    barrier = pltpu.get_barrier_semaphore()
    line = [lax.rem(z + k, 4) for k in range(1, 4)]
    for dev in line:
        pl.semaphore_signal(barrier, inc=1, device_id=(dev, me), device_id_type=MESH)
    each(7, lambda m: pl.semaphore_signal(barrier, inc=1, device_id=(z, at.peer(m)), device_id_type=MESH))
    pl.semaphore_wait(barrier, 10)
    inner = jnp.logical_and(z > 0, z < 3)
    outer_end, partner, outer = 1 + z // 3, 3 - z, 3 * (z - 1)
    cols = pl.ds(pl.multiple_of(me * width, width), width)

    def column_copy(m, j):
        dev = at.peer(m)
        rows = pl.ds(pl.multiple_of(dev * pieces, pieces), pieces)
        return at.push(wgrad.at[j, rows], own.at[1 + j, :, :, cols], wsend.at[m, j], wrecv.at[m, j], dev)

    mine_rows = pl.ds(pl.multiple_of(me * pieces, pieces), pieces)
    locals_ = [pltpu.make_async_copy(wgrad.at[j, mine_rows], own.at[1 + j, :, :, cols], local.at[j]) for j in range(3)]
    locals_.append(pltpu.make_async_copy(wograd, own.at[0], local.at[3]))
    for copy in locals_:
        copy.start()
    for j in range(3):
        each(7, lambda m, j=j: column_copy(m, j).start())
    each(seqs, normed_sum.start)
    each(seqs, result_sum.start)
    ggrad[...] = jnp.zeros_like(ggrad)

    def piece(ref, c):
        return ref.at[c // pieces, lax.rem(c, pieces)]

    def line_push(src, dst, send, recv, dev):
        return pltpu.make_async_remote_copy(
            src_ref=src, dst_ref=dst, send_sem=send, recv_sem=recv, device_id=(dev, me), device_id_type=MESH
        )

    def inward(c):
        return line_push(piece(own, c), piece(held, c), os.at[c], or_.at[c], outer_end)

    def across(c):
        return line_push(piece(held, c), met.at[c // 2], ps.at[c], pr.at[c], partner)

    def share(c):
        return line_push(piece(out, c), piece(out, c), qs.at[c], qr.at[c], partner)

    def outward(c):
        return line_push(piece(out, c), piece(out, c), fs.at[c], fr.at[c], outer)

    def mine(c):
        return 1 + lax.rem(c, 2) == z

    def ready(part):
        for j in range(parts):

            @pl.when(part == j)
            def _():
                locals_[(3, 0, 1, 2)[j]].wait()
                if j > 0:
                    each(7, lambda m: column_copy(m, j - 1).wait_recv())

    def step(c):
        @pl.when(lax.rem(c, pieces) == 0)
        def _():
            ready(c // pieces)

        @pl.when(jnp.logical_not(inner))
        def _():
            inward(c).start()

        @pl.when(inner)
        def _():
            inward(c).wait_recv()
            here = piece(held, c)
            here[...] = (here[...].astype(F32) + piece(own, c)[...].astype(F32)).astype(BF16)

            @pl.when(jnp.logical_not(mine(c)))
            def _():
                across(c).start()

    def settle(c):
        @pl.when(jnp.logical_and(inner, mine(c)))
        def _():
            across(c).wait_recv()
            piece(out, c)[...] = (piece(held, c)[...].astype(F32) + met[c // 2].astype(F32)).astype(BF16)
            share(c).start()
            outward(c).start()

    def forward(c):
        @pl.when(jnp.logical_and(inner, jnp.logical_not(mine(c))))
        def _():
            share(c).wait_recv()
            outward(c).start()

    def token_rows(s):
        tg, back = attn_back_rows(normed_sum.total(s), tok[s], mgrad[s], gains[0:1])
        tgrad[s] = tg
        ggrad[...] += jnp.sum(back, axis=0, keepdims=True)

    def out_rows(s):
        result[s] = (middle[s] + result_sum.total(s)).astype(BF16)

    jobs = (
        (step, 0, chunks), (settle, 1, chunks), (forward, 2, chunks),
        (normed_sum.hop1, 2, seqs), (normed_sum.hop2, 6, seqs), (token_rows, 10, seqs),
        (result_sum.hop1, 6, seqs), (result_sum.hop2, 10, seqs), (out_rows, 14, seqs),
    )

    def tick(i, _):
        for job, lag, count in jobs:

            @pl.when(jnp.logical_and(i >= lag, i < lag + count))
            def _():
                job(i - lag)

        return 0

    lax.fori_loop(0, max(lag + count for _, lag, count in jobs), tick, 0)

    parcel[...] = jnp.zeros_like(parcel)
    devices = parcel.shape[0]
    rows_of = ggrad.shape[1] // (128 * devices)
    for dev in range(devices):
        for k in range(rows_of):
            lanes = pl.ds((dev * rows_of + k) * 128, 128)
            parcel[dev, k : k + 1] = ggrad[:, lanes]
            parcel[dev, rows_of + k : rows_of + k + 1] = others[0:1, lanes]
        parcel[dev, 2 * rows_of : 2 * rows_of + 2] = others[1:3, 0:128]

    def parcel_copy(m):
        dev = at.peer(m)
        return at.push(parcel.at[dev], landed.at[m], gsend.at[m], grecv.at[m], dev)

    each(7, lambda m: parcel_copy(m).start())
    spare[0] = parcel[me]

    def add_parcel(m):
        parcel_copy(m).wait_recv()
        spare[0] += landed[m]

    each(7, add_parcel)

    def small_copy(k):
        return line_push(spare.at[0], spare.at[1 + k], ss.at[k], sr.at[k], line[k])

    for k in range(3):
        small_copy(k).start()

    @pl.when(jnp.logical_not(inner))
    def _():
        each(chunks, lambda c: outward(c).wait_recv())
        each(chunks, lambda c: inward(c).wait_send())

    @pl.when(inner)
    def _():
        def sent(c):
            outward(c).wait_send()

            @pl.when(mine(c))
            def _():
                share(c).wait_send()

            @pl.when(jnp.logical_not(mine(c)))
            def _():
                across(c).wait_send()

        each(chunks, sent)

    each(seqs, normed_sum.finish, result_sum.finish)

    def all_sent(m):
        parcel_copy(m).wait_send()
        for j in range(3):
            column_copy(m, j).wait_send()

    each(7, all_sent)
    total = spare[0]
    for k in range(3):
        small_copy(k).wait()
        total = total + spare[1 + k]
    small_out[...] = total
    few = total[2 * rows_of : 2 * rows_of + 2]
    heads = HEAD_DIM // devices
    moved = jnp.zeros_like(few)
    for k in range(devices):
        moved += jnp.where(me == k, pltpu.roll(few, (128 - k * heads) % 128, 1), 0.0)
    small_out[2 * rows_of : 2 * rows_of + 2] = moved


def finish(wgrad, wograd, npart, opart, tokens, middle, mgrad, gains, ffn_back, qk_back):
    seqs, rows, width = tokens.shape
    ep = lax.axis_size("ep")
    if ep != 8 or lax.axis_size("rep") != 4:
        normed_grad = lax.psum_scatter(npart, "ep", scatter_dimension=1, tiled=True).astype(F32)
        moe = lax.psum_scatter(opart, "ep", scatter_dimension=1, tiled=True).astype(F32)
        tg, backs = attn_back_rows(normed_grad, tokens, mgrad, gains[0])
        wrows = lax.all_to_all(wgrad, "ep", split_axis=1, concat_axis=2, tiled=True)
        share = width // ep
        small = jnp.concatenate([jnp.sum(backs, axis=(0, 1)), ffn_back[0], qk_back[0], qk_back[1]])
        small = lax.psum(small, ("ep", "rep"))
        mine = lax.axis_index("ep") * share
        cut = [lax.dynamic_slice_in_dim(small, k * width + mine, share).reshape(-1, 128) for k in range(2)]
        few = small[2 * width :].reshape(2, HEAD_DIM)
        few = jnp.roll(few, -lax.axis_index("ep") * (HEAD_DIM // ep), axis=1)
        small = jnp.concatenate(cut + [few], axis=0)
        big = lax.psum(jnp.concatenate([wograd[None], wrows], axis=0), "rep")
        return big, jnp.pad(small, ((0, 8 - small.shape[0]), (0, 0))), (middle + moe).astype(BF16), tg
    others = jnp.concatenate([ffn_back, jnp.pad(qk_back[:2], ((0, 0), (0, width - HEAD_DIM)))], axis=0)
    npart, opart = (p.reshape(seqs, ep, rows, width) for p in (npart, opart))
    pieces = 4
    block = wograd.shape[0] // pieces
    wgrad = wgrad.reshape(3, wgrad.shape[1] // block, block, wgrad.shape[2])
    wograd = wograd.reshape(pieces, block, width)
    whole = (4, pieces, block, width)
    dma = pltpu.SemaphoreType.DMA
    chunks = 4 * pieces
    out, small, result, tgrad = pl.pallas_call(
        finish_kernel,
        out_shape=(sds(whole, BF16), sds((8, 128), F32), sds(tokens.shape, BF16), sds(tokens.shape, BF16)),
        in_specs=[VM, VM, AN, AN] + [VM] * 5,
        out_specs=(VM, VM, VM, VM),
        scratch_shapes=[
            pltpu.VMEM(whole, BF16),
            pltpu.VMEM(whole, BF16),
            pltpu.VMEM((chunks // 2, block, width), BF16),
            pltpu.VMEM((1, width), F32),
            pltpu.VMEM((ep, 8, 128), F32),
            pltpu.VMEM((7, 8, 128), F32),
            pltpu.VMEM((4, 8, 128), F32),
        ]
        + [dma((7, 3)), dma((7, 3)), dma((4,)), dma((7,)), dma((7,))]
        + [dma((chunks,))] * 8
        + [dma((3,))] * 2
        + 2 * Reduce.scratch(npart),
        compiler_params=pltpu.CompilerParams(collective_id=4, has_side_effects=True, vmem_limit_bytes=61 << 20),
        name="finish",
    )(wgrad, wograd, npart, opart, tokens, middle, mgrad, gains, others)
    return out.reshape(4, pieces * block, width), small, result, tgrad


def dot(a, b, ca, cb):
    return lax.dot_general(a, b, (((ca,), (cb,)), ((), ())), preferred_element_type=F32)


def rope_tables(table):
    half = HEAD_DIM // 2
    values = table[...]
    turned = pltpu.roll(values, half, 1)
    first = lax.broadcasted_iota(jnp.int32, values.shape, 1) < half
    return jnp.where(first, values, turned), jnp.where(first, -turned, values)


def rope(v, cos, sin_turn):
    return v * cos + pltpu.roll(v, HEAD_DIM // 2, 1) * sin_turn


def probabilities(q, k, length):
    scores = dot(q, k, 1, 1) * HEAD_DIM**-0.5
    column = lax.broadcasted_iota(jnp.int32, (1, scores.shape[1]), 1).astype(F32)
    scores = jnp.where(column < length, scores, -1e9)
    p = jnp.exp(scores - jnp.max(scores, axis=-1, keepdims=True))
    return p * (1.0 / jnp.sum(p, axis=-1, keepdims=True))


def packed_slots(number, table, length_live, top):
    tab = table.astype(F32)
    length = tab.shape[0]
    lane = lax.broadcasted_iota(jnp.int32, tab.shape, 1)
    row = lax.broadcasted_iota(jnp.int32, (length, 1), 0).astype(F32)
    chosen = jnp.logical_and(jnp.logical_and(tab == number, lane < top), row < length_live)
    gates = jnp.where(chosen, pltpu.roll(tab, 128 - top, 1), 0.0).astype(BF16)
    chosen = jnp.where(chosen, 1.0, 0.0).astype(BF16)
    ones = jnp.ones((8, 128), BF16)
    hit = dot(ones, chosen, 1, 1)
    weight = dot(ones, gates, 1, 1)
    earlier = lax.broadcasted_iota(jnp.int32, (length, length), 0)
    later = lax.broadcasted_iota(jnp.int32, (length, length), 1)
    rank = dot(hit.astype(BF16), jnp.where(earlier < later, 1.0, 0.0).astype(BF16), 1, 0)
    return jnp.where(hit > 0.5, rank, -1.0), weight, jnp.sum(hit[0:1], axis=1, keepdims=True)


def attend_rows(top, number, s, block, w, wo, gains, small, table, normed, pre, low, ctx, part, slots, starts):
    width = normed.shape[1]
    length = seq_len(small, s)
    cos, sin = rope_tables(table)
    v = block[:, 0:width].astype(F32)
    x = (v * inverse_rms(v) * gains[0:1]).astype(BF16)
    normed[...] = x
    q_pre, k_pre = dot(x, w[0], 1, 0), dot(x, w[1], 1, 0)
    value = dot(x, w[2], 1, 0).astype(BF16)
    pre[0], pre[1] = q_pre, k_pre
    low[2] = value
    for h in range(q_pre.shape[1] // HEAD_DIM):
        cols = slice(h * HEAD_DIM, (h + 1) * HEAD_DIM)
        rot = []
        for i, (u, g) in enumerate(((q_pre[:, cols], small[0:1]), (k_pre[:, cols], small[1:2]))):
            rot.append(rope(u * inverse_rms(u) * g, cos, sin).astype(BF16))
            low[i, :, cols] = rot[i]
        attention = probabilities(rot[0], rot[1], length).astype(BF16)
        ctx[:, cols] = dot(attention, value[:, cols], 1, 0).astype(BF16)
    part[...] = dot(ctx[...], wo[...], 1, 0).astype(BF16).reshape(part.shape)
    routes = block[:, width : width + 128]
    lane = lax.broadcasted_iota(jnp.int32, (1, 128), 1)
    for j, ref in enumerate(slots):
        slot, weight, count = packed_slots(number + j, routes, length, top)
        ref[0:8] = slot
        ref[8:16] = weight
        row = starts[j : j + 1]
        after = jnp.sum(jnp.where(lane == s, row, 0.0), axis=1, keepdims=True) + 16.0 * jnp.floor((count + 15.0) * 0.0625)
        starts[j : j + 1] = jnp.where(lane == s + 1, after, row)


def attend_kernel(top, number, full, w, wo, gains, small, table, normed, pre, low, ctx, part, slots0, slots1, starts):
    s = pl.program_id(0)

    @pl.when(s == 0)
    def _():
        starts[...] = jnp.zeros_like(starts)

    attend_rows(
        top, number[0].astype(F32), s, full.at[0], w, wo, gains, small, table,
        normed.at[0], pre.at[:, 0], low.at[:, 0], ctx.at[0], part.at[0], (slots0.at[0], slots1.at[0]), starts,
    )


def attend(top, number, full, weights, wo, gains, small, table):
    seqs, length, wide = full.shape
    width = wide - 128
    cols = weights.shape[2]
    row = lambda i, *_: (i, 0, 0)
    row2 = lambda i, *_: (0, i, 0, 0)
    two = lambda i, *_: (0, 0)
    slot = pl.BlockSpec((1, 16, length), row)
    return pl.pallas_call(
        functools.partial(attend_kernel, top),
        out_shape=(
            sds((seqs, length, width), BF16),
            sds((2, seqs, length, cols), F32),
            sds((3, seqs, length, cols), BF16),
            sds((seqs, length, cols), BF16),
            sds((seqs, length, width), BF16),
            sds((seqs, 16, length), F32),
            sds((seqs, 16, length), F32),
            sds((8, 128), F32),
        ),
        grid_spec=pltpu.PrefetchScalarGridSpec(
            num_scalar_prefetch=1,
            grid=(seqs,),
            in_specs=[
                pl.BlockSpec((1, length, wide), row),
                pl.BlockSpec(weights.shape, lambda i, *_: (0, 0, 0)),
                pl.BlockSpec(wo.shape, two),
                pl.BlockSpec((8, width), two),
                pl.BlockSpec((8, 128), two),
                pl.BlockSpec((length, HEAD_DIM), two),
            ],
            out_specs=(
                pl.BlockSpec((1, length, width), row),
                pl.BlockSpec((2, 1, length, cols), row2),
                pl.BlockSpec((3, 1, length, cols), row2),
                pl.BlockSpec((1, length, cols), row),
                pl.BlockSpec((1, length, width), row),
                slot,
                slot,
                pl.BlockSpec((8, 128), two),
            ),
        ),
        compiler_params=pltpu.CompilerParams(dimension_semantics=("arbitrary",), vmem_limit_bytes=60 << 20),
        cost_estimate=pl.CostEstimate(flops=10**10, bytes_accessed=4 * 10**7, transcendentals=10**6),
        name="attend",
    )(number, full, weights, wo, gains, small, table)


def attend_mix_kernel(
    top, local, full, w, wo, gains, small, table, tok, cot, _cot_early,
    normed, pre, low, ctx, middle, mixed, cot_full, slots0, slots1, starts,
    own, blocks, nbuf, pbuf, lbuf, cbuf, part, begins, tsem, ssem, *scratch,
):
    at = Place()
    seqs = tok.shape[0]
    n = Reduce.sems
    reduce = Reduce(at, part, *scratch[:n])
    gather = Gather(at, own, mixed, *scratch[n : n + 3])
    cot_gather = Gather(at, cot, cot_full, *scratch[n + 3 :])
    number = (at.me * local).astype(F32)
    early = seqs // 2
    at.greet((at.xn, at.yn, at.sb))
    each(seqs, cot_gather.start, low=early)
    begins[...] = jnp.zeros_like(begins)

    def load(s):
        return pltpu.make_async_copy(full.at[s], blocks.at[lax.rem(s, 2)], tsem.at[lax.rem(s, 2)])

    def stores(s):
        k = lax.rem(s, 2)
        pairs = ((nbuf.at[k], normed.at[s]), (pbuf.at[k], pre.at[:, s]), (lbuf.at[k], low.at[:, s]), (cbuf.at[k], ctx.at[s]))
        return [pltpu.make_async_copy(src, dst, ssem.at[i, k]) for i, (src, dst) in enumerate(pairs)]

    load(0).start()

    def sequence(s):
        k = lax.rem(s, 2)
        load(s).wait()

        @pl.when(s + 1 < seqs)
        def _():
            load(s + 1).start()

        @pl.when(s >= 2)
        def _():
            for copy in stores(s - 2):
                copy.wait()

        attend_rows(
            top, number, s, blocks.at[k], w, wo, gains, small, table,
            nbuf.at[k], pbuf.at[k], lbuf.at[k], cbuf.at[k], part.at[s], (slots0.at[s], slots1.at[s]), begins,
        )
        for copy in stores(s):
            copy.start()
        reduce.start(s)

    def rows(s):
        living = live_rows(small, s, at.me, tok.shape[1])
        mid, out = mix_rows(reduce.total(s), tok[s], living, gains[1:2])
        middle[s] = mid
        own[s] = out
        gather.start(s)

    def cot_pair(p):
        @pl.when(lax.rem(p, 2) == 0)
        def _():
            cot_gather.relay(early + p, True)
            cot_gather.relay(early + p + 1, False)

    jobs = (
        (sequence, 0, seqs), (reduce.hop1, 1, seqs), (cot_pair, 3, early), (reduce.hop2, 3, seqs),
        (lambda s: cot_gather.relay_far(early + s), 7, early), (rows, 5, seqs),
    )

    def tick(i, _):
        for job, lag, count in jobs:

            @pl.when(jnp.logical_and(i >= lag, i < lag + count))
            def _():
                job(i - lag)

        return 0

    lax.fori_loop(0, max(lag + count for _, lag, count in jobs), tick, 0)
    starts[...] = begins[...].astype(jnp.int32)
    each(seqs, cot_gather.finish, low=early)
    gather_tail(gather, 0, seqs)
    for s in (seqs - 2, seqs - 1):
        for copy in stores(s):
            copy.wait()
    each(seqs, reduce.finish)


def attend_mix(top, local, full, weights, wo, gains, small, table, tokens, cotangent, cot_early):
    seqs, rows, width = tokens.shape
    length = full.shape[1]
    cols = weights.shape[2]
    part = sds((seqs, 8, rows, width), BF16)
    dma = pltpu.SemaphoreType.DMA
    return pl.pallas_call(
        functools.partial(attend_mix_kernel, top, local),
        out_shape=(
            sds((seqs, length, width), BF16),
            sds((2, seqs, length, cols), F32),
            sds((3, seqs, length, cols), BF16),
            sds((seqs, length, cols), BF16),
            sds(tokens.shape, F32),
            sds((seqs, length, width), BF16),
            sds((seqs, length, width), BF16),
            sds((seqs, 16, length), F32),
            sds((seqs, 16, length), F32),
            sds((8, 128), jnp.int32),
        ),
        in_specs=[AN] + [VM] * 7 + [AN],
        out_specs=(AN, AN, AN, AN, VM, AN, AN, VM, VM, VM),
        input_output_aliases={8: 6},
        scratch_shapes=[
            pltpu.VMEM(tokens.shape, BF16),
            pltpu.VMEM((2,) + full.shape[1:], BF16),
            pltpu.VMEM((2, length, width), BF16),
            pltpu.VMEM((2, 2, length, cols), F32),
            pltpu.VMEM((2, 3, length, cols), BF16),
            pltpu.VMEM((2, length, cols), BF16),
            pltpu.VMEM(part.shape, BF16),
            pltpu.VMEM((8, 128), F32),
            dma((2,)),
            dma((4, 2)),
        ]
        + Reduce.scratch(part)
        + Gather.scratch(seqs)
        + Gather.scratch(seqs),
        compiler_params=pltpu.CompilerParams(collective_id=2, **COMM),
        name="attend_mix",
    )(full, weights, wo, gains, small, table, tokens, cotangent, cot_early)


def attend_back_kernel(
    agrad, normed, pre, low, ctx, w, wo, small, table, part, wgrad, wograd, gains, wacc, woacc,
):
    s = pl.program_id(0)
    length = seq_len(small, s)
    cos, sin = rope_tables(table)

    @pl.when(s == 0)
    def _():
        wacc[...] = jnp.zeros_like(wacc)
        woacc[...] = jnp.zeros_like(woacc)
        gains[...] = jnp.zeros_like(gains)

    ag = agrad[0]
    woacc[...] += dot(ctx[0], ag, 0, 0)
    cg_all = dot(ag, wo[...], 1, 1).astype(BF16)
    scale = HEAD_DIM**-0.5
    half = HEAD_DIM // 2
    grads = ([], [], [])
    for h in range(cg_all.shape[1] // HEAD_DIM):
        cols = slice(h * HEAD_DIM, (h + 1) * HEAD_DIM)
        q, k, value, cg = low[0, 0, :, cols], low[1, 0, :, cols], low[2, 0, :, cols], cg_all[:, cols]
        attention = probabilities(q, k, length)
        grads[2].append(dot(attention.astype(BF16), cg, 0, 0).astype(BF16))
        pg = dot(cg, value, 1, 1)
        sg = (attention * (pg - jnp.sum(attention * pg, axis=-1, keepdims=True))).astype(BF16)
        for i, (rot_grad, g) in enumerate(((dot(sg, k, 1, 0), small[0:1]), (dot(sg, q, 0, 0), small[1:2]))):
            wgt = rot_grad * scale
            u = wgt * cos + pltpu.roll(wgt * sin, half, 1)
            v = pre[i, 0, :, cols]
            r = inverse_rms(v)
            grads[i].append(rms_back(v, r, u * g).astype(BF16))
            gains[i : i + 1] += jnp.sum(u * v * r, axis=0, keepdims=True)
    width = w.shape[2]
    joined = jnp.concatenate([g for kind in grads for g in kind], axis=1)
    wacc[...] += dot(normed[0], joined, 0, 0)
    total = None
    for i in range(3):
        piece = dot(joined[:, i * width : (i + 1) * width], w[i], 1, 1)
        total = piece if total is None else total + piece
    part[0] = total.astype(BF16)

    @pl.when(s == pl.num_programs(0) - 1)
    def _():
        for i in range(3):
            wgrad[i] = wacc[:, i * width : (i + 1) * width].astype(BF16)
        wograd[...] = woacc[...].astype(BF16)


def attend_back(agrad, normed, pre, low, ctx, weights, wo, small, table):
    seqs, length, width = agrad.shape
    cols = weights.shape[2]
    row = lambda i, *_: (i, 0, 0)
    row2 = lambda i, *_: (0, i, 0, 0)
    two = lambda i, *_: (0, 0)
    three = lambda i, *_: (0, 0, 0)
    return pl.pallas_call(
        attend_back_kernel,
        out_shape=(
            sds(agrad.shape, BF16),
            sds(weights.shape, BF16),
            sds(wo.shape, BF16),
            sds((8, HEAD_DIM), F32),
        ),
        grid_spec=pltpu.PrefetchScalarGridSpec(
            num_scalar_prefetch=0,
            grid=(seqs,),
            in_specs=[
                pl.BlockSpec((1, length, width), row),
                pl.BlockSpec((1, length, width), row),
                pl.BlockSpec((2, 1, length, cols), row2),
                pl.BlockSpec((3, 1, length, cols), row2),
                pl.BlockSpec((1, length, cols), row),
                pl.BlockSpec(weights.shape, three),
                pl.BlockSpec(wo.shape, two),
                pl.BlockSpec((8, 128), two),
                pl.BlockSpec((length, HEAD_DIM), two),
            ],
            out_specs=(
                pl.BlockSpec((1, length, width), row),
                pl.BlockSpec(weights.shape, three),
                pl.BlockSpec(wo.shape, two),
                pl.BlockSpec((8, HEAD_DIM), two),
            ),
            scratch_shapes=[
                pltpu.VMEM((weights.shape[1], 3 * cols), F32),
                pltpu.VMEM(wo.shape, F32),
            ],
        ),
        compiler_params=pltpu.CompilerParams(dimension_semantics=("arbitrary",), vmem_limit_bytes=60 << 20),
        cost_estimate=pl.CostEstimate(flops=2 * 10**10, bytes_accessed=4 * 10**7, transcendentals=10**6),
        name="attend_back",
    )(agrad, normed, pre, low, ctx, weights, wo, small, table)


BLOCK = 256
FIRST_TILE = (512, 1024)


def pack_rows(seqs, capacity):
    return -(-seqs * capacity // BLOCK) * BLOCK


def each_block(blocks, hidden, job):
    part = min(hidden, 512)
    parts = hidden // part

    def run(i, _):
        b, h = i // parts, lax.rem(i, parts)
        rows = pl.ds(pl.multiple_of(b * BLOCK, BLOCK), BLOCK)
        low = pl.multiple_of(h * part, part)
        job(rows, pl.ds(low, part), pl.ds(pl.multiple_of(hidden + low, part), part))
        return 0

    lax.fori_loop(0, blocks * parts, run, 0)


def swiglu_back(gate, up, dact):
    sig = 1.0 / (1.0 + jnp.exp(-gate))
    return dact * up * sig * (1.0 + gate * (1.0 - sig)), dact * (gate * sig)


def forward_blocks(blocks, x, dy, wi, wo, acts, dgus):
    def job(rows, gcols, ucols):
        gate = dot(x[rows], wi[:, gcols], 1, 0)
        up = dot(x[rows], wi[:, ucols], 1, 0)
        dact = dot(dy[rows], wo[gcols], 1, 1)
        acts[rows, gcols] = (gate * (1.0 / (1.0 + jnp.exp(-gate))) * up).astype(BF16)
        dgate, dup = swiglu_back(gate, up, dact)
        dgus[rows, gcols] = dgate.astype(BF16)
        dgus[rows, ucols] = dup.astype(BF16)

    each_block(blocks, wo.shape[0], job)


def gradient_tiles(blocks, left, right, result, acc, stage, ssem, busy):
    tr, tc = acc.shape
    down, across = result.shape[0] // tr, result.shape[1] // tc

    def tile(t, _):
        rt, ct = t // across, lax.rem(t, across)
        left_cols = pl.ds(pl.multiple_of(rt * tr, tr), tr)
        right_cols = pl.ds(pl.multiple_of(ct * tc, tc), tc)

        def step(b, _):
            rows = pl.ds(pl.multiple_of(b * BLOCK, BLOCK), BLOCK)
            piece = dot(left[rows, left_cols], right[rows, right_cols], 0, 0)

            @pl.when(b == 0)
            def _():
                acc[...] = piece

            @pl.when(b > 0)
            def _():
                acc[...] += piece

            return 0

        @pl.when(blocks == 0)
        def _():
            acc[...] = jnp.zeros_like(acc)

        lax.fori_loop(0, blocks, step, 0)
        k = lax.rem(t, 2)
        out = pltpu.make_async_copy(stage.at[k], result.at[left_cols, right_cols], ssem.at[k])

        @pl.when(jnp.logical_or(t >= 2, busy))
        def _():
            out.wait()

        stage[k] = acc[...].astype(BF16)
        out.start()
        return 0

    lax.fori_loop(0, down * across, tile, 0)


def drain_tiles(result, acc, stage, ssem):
    tr, tc = acc.shape
    for k in range(2):
        pltpu.make_async_copy(stage.at[k], result.at[pl.ds(0, tr), pl.ds(0, tc)], ssem.at[k]).wait()


def first_kernel(
    capacity, starts, mixed, cot, slots0, slots1, w_in,
    act, pair, x_all, dy_all, out_grad,
    x, dy, wi, acts, pairs, acc, stage, wsem, ssem, rsem,
):
    step = pl.program_id(0)
    steps = pl.num_programs(0)
    together = mixed.shape[0]
    seqs = steps * together
    width = mixed.shape[2]
    hidden = acts.shape[1]
    load = pltpu.make_async_copy(w_in.at[0], wi, wsem)

    @pl.when(step == 0)
    def _():
        load.start()

    packed = []
    for k in range(together):
        spread, gate_spread = [], []
        for slots in (slots0, slots1):
            column = lax.broadcasted_iota(jnp.int32, (capacity, slots.shape[2]), 0).astype(F32)
            place = column == slots[k, 0:1]
            spread.append(jnp.where(place, 1.0, 0.0).astype(BF16))
            gate_spread.append(jnp.where(place, slots[k, 8:9], 0.0).astype(BF16))
        packed.append(
            (
                dot(jnp.concatenate(spread, axis=0), mixed[k], 1, 0).astype(BF16),
                dot(jnp.concatenate(gate_spread, axis=0), cot[k], 1, 0).astype(BF16),
            )
        )
    for k, (x_rows, dy_rows) in enumerate(packed):
        s = step * together + k
        for j in range(2):
            start = pl.multiple_of(starts[j, s], 16)
            x[j, pl.ds(start, capacity)] = x_rows[j * capacity : (j + 1) * capacity]
            dy[j, pl.ds(start, capacity)] = dy_rows[j * capacity : (j + 1) * capacity]

    @pl.when(step == steps - 1)
    def _():
        for j in range(2):
            past = (starts[j, seqs - 1] + capacity) // 16
            end = (starts[j, seqs] + BLOCK - 1) // BLOCK * (BLOCK // 16)

            def clear(i, _):
                rows = pl.ds(pl.multiple_of(i * 16, 16), 16)
                x[j, rows] = jnp.zeros((16, width), BF16)
                dy[j, rows] = jnp.zeros((16, width), BF16)
                return 0

            lax.fori_loop(past, end, clear, 0)
        saves = [pltpu.make_async_copy(x, x_all, rsem.at[0]), pltpu.make_async_copy(dy, dy_all, rsem.at[1])]
        for copy in saves:
            copy.start()
        blocks = (starts[0, seqs] + BLOCK - 1) // BLOCK
        load.wait()

        def forward(rows, gcols, ucols):
            gate = dot(x[0, rows], wi[:, gcols], 1, 0)
            up = dot(x[0, rows], wi[:, ucols], 1, 0)
            acts[rows, gcols] = (gate * (1.0 / (1.0 + jnp.exp(-gate))) * up).astype(BF16)
            pairs[rows, gcols] = gate.astype(BF16)
            pairs[rows, ucols] = up.astype(BF16)

        each_block(blocks, hidden, forward)
        saves += [pltpu.make_async_copy(acts, act.at[0], rsem.at[2]), pltpu.make_async_copy(pairs, pair, rsem.at[3])]
        for copy in saves[2:]:
            copy.start()
        gradient_tiles(blocks, acts, dy.at[0], out_grad, acc, stage, ssem, False)
        drain_tiles(out_grad, acc, stage, ssem)
        for copy in saves:
            copy.wait()


def expert_first(starts, mixed, cot, slots, w_in, hidden, capacity):
    seqs, length, width = mixed.shape
    rows = pack_rows(seqs, capacity)
    dma = pltpu.SemaphoreType.DMA
    seq = lambda i, *_: (i, 0, 0)
    together = 2
    slot_spec = pl.BlockSpec((together, 16, length), seq)
    return pl.pallas_call(
        functools.partial(first_kernel, capacity),
        out_shape=(
            sds((2, rows, hidden), BF16),
            sds((rows, 2 * hidden), BF16),
            sds((2, rows, width), BF16),
            sds((2, rows, width), BF16),
            sds((hidden, width), BF16),
        ),
        grid_spec=pltpu.PrefetchScalarGridSpec(
            num_scalar_prefetch=1,
            grid=(seqs // together,),
            in_specs=[
                pl.BlockSpec((together, length, width), seq),
                pl.BlockSpec((together, length, width), seq),
                slot_spec,
                slot_spec,
                AN,
            ],
            out_specs=(AN, AN, AN, AN, AN),
            scratch_shapes=[
                pltpu.VMEM((2, rows, width), BF16),
                pltpu.VMEM((2, rows, width), BF16),
                pltpu.VMEM(w_in.shape[1:], BF16),
                pltpu.VMEM((rows, hidden), BF16),
                pltpu.VMEM((rows, 2 * hidden), BF16),
                pltpu.VMEM(FIRST_TILE, F32),
                pltpu.VMEM((2,) + FIRST_TILE, BF16),
                dma,
                dma((2,)),
                dma((4,)),
            ],
        ),
        compiler_params=pltpu.CompilerParams(dimension_semantics=("arbitrary",), vmem_limit_bytes=62 << 20),
        cost_estimate=pl.CostEstimate(flops=2 * 10**10, bytes_accessed=6 * 10**7, transcendentals=10**6),
        name="expert_first",
    )(starts, mixed, cot, *slots, w_in)


def in_grad_kernel(
    seqs, starts, x_all, dy_all, pair, w_out, dgu, in_grad, x, dy, wo, pairs, dgus, acc, stage, lsem, wsem, ssem, rsem
):
    blocks = (starts[0, seqs] + BLOCK - 1) // BLOCK
    hidden = wo.shape[0]
    weights = pltpu.make_async_copy(w_out.at[0], wo, wsem)
    weights.start()

    def run(b, action):
        rows = pl.ds(pl.multiple_of(b * BLOCK, BLOCK), BLOCK)
        for copy in (
            pltpu.make_async_copy(dy_all.at[0, rows], dy.at[rows], lsem.at[0, b]),
            pltpu.make_async_copy(pair.at[rows], pairs.at[rows], lsem.at[1, b]),
            pltpu.make_async_copy(x_all.at[0, rows], x.at[rows], lsem.at[2, b]),
        ):
            getattr(copy, action)()
        return 0

    lax.fori_loop(0, blocks, lambda b, _: run(b, "start"), 0)
    weights.wait()
    lax.fori_loop(0, blocks, lambda b, _: run(b, "wait"), 0)

    def backward(rows, gcols, ucols):
        dact = dot(dy[rows], wo[gcols], 1, 1)
        dgate, dup = swiglu_back(pairs[rows, gcols].astype(F32), pairs[rows, ucols].astype(F32), dact)
        dgus[rows, gcols] = dgate.astype(BF16)
        dgus[rows, ucols] = dup.astype(BF16)

    each_block(blocks, hidden, backward)
    save = pltpu.make_async_copy(dgus, dgu.at[0], rsem)
    save.start()
    gradient_tiles(blocks, x, dgus, in_grad, acc, stage, ssem, False)
    drain_tiles(in_grad, acc, stage, ssem)
    save.wait()


def first_in_grad(seqs, starts, x_all, dy_all, pair, w_out):
    rows, width = x_all.shape[1:]
    hidden = w_out.shape[1]
    dma = pltpu.SemaphoreType.DMA
    return pl.pallas_call(
        functools.partial(in_grad_kernel, seqs),
        out_shape=(sds((2, rows, 2 * hidden), BF16), sds((width, 2 * hidden), BF16)),
        grid_spec=pltpu.PrefetchScalarGridSpec(
            num_scalar_prefetch=1,
            grid=(1,),
            in_specs=[AN] * 4,
            out_specs=(AN, AN),
            scratch_shapes=[
                pltpu.VMEM((rows, width), BF16),
                pltpu.VMEM((rows, width), BF16),
                pltpu.VMEM(w_out.shape[1:], BF16),
                pltpu.VMEM((rows, 2 * hidden), BF16),
                pltpu.VMEM((rows, 2 * hidden), BF16),
                pltpu.VMEM((512, 2048), F32),
                pltpu.VMEM((2, 512, 2048), BF16),
                dma((3, rows // BLOCK)),
                dma,
                dma((2,)),
                dma,
            ],
        ),
        compiler_params=pltpu.CompilerParams(dimension_semantics=("arbitrary",), vmem_limit_bytes=60 << 20),
        cost_estimate=pl.CostEstimate(flops=10**10, bytes_accessed=2 * 10**7, transcendentals=0),
        name="first_in_grad",
    )(starts, x_all, dy_all, pair, w_out)


def second_kernel(
    seqs, starts, x_all, dy_all, w_in, w_out, _act, _dgu, act, dgu, in_grad, out_grad,
    x, dy, wi, wo, acts, dgus, acc, stage, wsem, lsem, ssem, rsem,
):
    blocks = (starts[1, seqs] + BLOCK - 1) // BLOCK
    loads = [pltpu.make_async_copy(w_in.at[1], wi, wsem.at[0]), pltpu.make_async_copy(w_out.at[1], wo, wsem.at[1])]

    def load(b, action):
        rows = pl.ds(pl.multiple_of(b * BLOCK, BLOCK), BLOCK)
        for copy in (
            pltpu.make_async_copy(x_all.at[1, rows], x.at[rows], lsem.at[0, b]),
            pltpu.make_async_copy(dy_all.at[1, rows], dy.at[rows], lsem.at[1, b]),
        ):
            getattr(copy, action)()
        return 0

    for copy in loads:
        copy.start()
    lax.fori_loop(0, blocks, lambda b, _: load(b, "start"), 0)
    for copy in loads:
        copy.wait()
    lax.fori_loop(0, blocks, lambda b, _: load(b, "wait"), 0)

    forward_blocks(blocks, x, dy, wi, wo, acts, dgus)
    saves = [pltpu.make_async_copy(acts, act.at[1], rsem.at[0]), pltpu.make_async_copy(dgus, dgu.at[1], rsem.at[1])]
    for copy in saves:
        copy.start()
    gradient_tiles(blocks, x, dgus, in_grad, acc, stage, ssem, False)
    gradient_tiles(blocks, acts, dy, out_grad, acc, stage, ssem, True)
    drain_tiles(out_grad, acc, stage, ssem)
    for copy in saves:
        copy.wait()


def expert_second(seqs, starts, x_all, dy_all, w_in, w_out, act, dgu):
    rows, width = dy_all.shape[1:]
    hidden = w_out.shape[1]
    dma = pltpu.SemaphoreType.DMA
    return pl.pallas_call(
        functools.partial(second_kernel, seqs),
        out_shape=(
            sds(act.shape, BF16), sds(dgu.shape, BF16), sds((width, 2 * hidden), BF16), sds((hidden, width), BF16)
        ),
        input_output_aliases={5: 0, 6: 1},
        grid_spec=pltpu.PrefetchScalarGridSpec(
            num_scalar_prefetch=1,
            grid=(1,),
            in_specs=[AN] * 6,
            out_specs=(AN, AN, AN, AN),
            scratch_shapes=[
                pltpu.VMEM((rows, width), BF16),
                pltpu.VMEM((rows, width), BF16),
                pltpu.VMEM(w_in.shape[1:], BF16),
                pltpu.VMEM(w_out.shape[1:], BF16),
                pltpu.VMEM((rows, hidden), BF16),
                pltpu.VMEM((rows, 2 * hidden), BF16),
                pltpu.VMEM((256, 2048), F32),
                pltpu.VMEM((2, 256, 2048), BF16),
                dma((2,)),
                dma((2, rows // BLOCK)),
                dma((2,)),
                dma((2,)),
            ],
        ),
        compiler_params=pltpu.CompilerParams(dimension_semantics=("arbitrary",), vmem_limit_bytes=60 << 20),
        cost_estimate=pl.CostEstimate(flops=25 * 10**9, bytes_accessed=6 * 10**7, transcendentals=10**6),
        name="expert_second",
    )(starts, x_all, dy_all, w_in, w_out, act, dgu)


def tail_kernel(seqs, starts, act, dgu, w_in, w_out, produced, dx):
    @pl.when(pl.program_id(1) * BLOCK < starts[pl.program_id(0), seqs])
    def _():
        part = min(produced.shape[1], 512)

        def run(i, _):
            cols = pl.ds(pl.multiple_of(i * part, part), part)
            produced[:, cols] = dot(act[...], w_out[:, cols], 1, 0).astype(BF16)
            dx[:, cols] = dot(dgu[...], w_in[cols], 1, 1).astype(BF16)
            return 0

        lax.fori_loop(0, produced.shape[1] // part, run, 0)


def expert_tails(seqs, starts, act, dgu, w_in, w_out):
    _, rows, hidden = act.shape
    width = w_in.shape[1]

    def block(j, i, st):
        return j, jnp.maximum(jnp.minimum(i, (st[j, seqs] + BLOCK - 1) // BLOCK - 1), 0), 0

    out = pl.BlockSpec((None, BLOCK, width), block)
    return pl.pallas_call(
        functools.partial(tail_kernel, seqs),
        out_shape=(sds((2, rows, width), BF16), sds((2, rows, width), BF16)),
        grid_spec=pltpu.PrefetchScalarGridSpec(
            num_scalar_prefetch=1,
            grid=(2, rows // BLOCK),
            in_specs=[
                pl.BlockSpec((None, BLOCK, hidden), block),
                pl.BlockSpec((None, BLOCK, 2 * hidden), block),
                pl.BlockSpec((None,) + w_in.shape[1:], lambda j, i, *_: (j, 0, 0)),
                pl.BlockSpec((None,) + w_out.shape[1:], lambda j, i, *_: (j, 0, 0)),
            ],
            out_specs=(out, out),
        ),
        compiler_params=pltpu.CompilerParams(dimension_semantics=("arbitrary", "arbitrary"), vmem_limit_bytes=60 << 20),
        cost_estimate=pl.CostEstimate(flops=24 * 10**9, bytes_accessed=6 * 10**7, transcendentals=0),
        name="expert_tails",
    )(starts, act, dgu, w_in, w_out)


def combine_kernel(capacity, local, *refs):
    s = pl.program_id(0)
    starts = refs[0]
    slots = refs[1 : 1 + local]
    produced, dx, out_part, grad_part, held_out, held_grad, sems = refs[1 + local :]
    seqs = pl.num_programs(0)

    def loads(s):
        k = lax.rem(s, 2)
        copies = []
        for j in range(local):
            span = pl.ds(pl.multiple_of(starts[j, s], 16), capacity)
            copies.append(pltpu.make_async_copy(produced.at[j, span], held_out.at[k, j], sems.at[k, 0, j]))
            copies.append(pltpu.make_async_copy(dx.at[j, span], held_grad.at[k, j], sems.at[k, 1, j]))
        return copies

    @pl.when(s == 0)
    def _():
        for copy in loads(s):
            copy.start()

    @pl.when(s + 1 < seqs)
    def _():
        for copy in loads(s + 1):
            copy.start()

    for copy in loads(s):
        copy.wait()
    slot = lax.rem(s, 2)
    out_sum, grad_sum = None, None
    for j in range(local):
        length = slots[j].shape[2]
        column = lax.broadcasted_iota(jnp.int32, (capacity, length), 0).astype(F32)
        place = column == slots[j][0, 0:1]
        held = lax.broadcasted_iota(jnp.int32, (capacity, 1), 0) < starts[j, s + 1] - starts[j, s]
        rows = jnp.where(held, held_out[slot, j], 0.0).astype(BF16)
        grads = jnp.where(held, held_grad[slot, j], 0.0).astype(BF16)
        out = dot(jnp.where(place, slots[j][0, 8:9], 0.0).astype(BF16), rows, 0, 0)
        grad = dot(jnp.where(place, 1.0, 0.0).astype(BF16), grads, 0, 0)
        out_sum = out if out_sum is None else out_sum + out
        grad_sum = grad if grad_sum is None else grad_sum + grad
    out_part[0] = out_sum.astype(BF16)
    grad_part[0] = grad_sum.astype(BF16)


def combine(starts, slots, produced, dx, capacity):
    local = len(slots)
    seqs, _, length = slots[0].shape
    width = produced.shape[2]
    seq = lambda i, *_: (i, 0, 0)
    held = pltpu.VMEM((2, local, capacity, width), BF16)
    return pl.pallas_call(
        functools.partial(combine_kernel, capacity, local),
        out_shape=(sds((seqs, length, width), BF16), sds((seqs, length, width), BF16)),
        grid_spec=pltpu.PrefetchScalarGridSpec(
            num_scalar_prefetch=1,
            grid=(seqs,),
            in_specs=[pl.BlockSpec((1, 16, length), seq)] * local + [AN] * 2,
            out_specs=(pl.BlockSpec((1, length, width), seq), pl.BlockSpec((1, length, width), seq)),
            scratch_shapes=[held, held, pltpu.SemaphoreType.DMA((2, 2, local))],
        ),
        compiler_params=pltpu.CompilerParams(dimension_semantics=("arbitrary",), vmem_limit_bytes=60 << 20),
        cost_estimate=pl.CostEstimate(flops=3 * 10**9, bytes_accessed=4 * 10**7, transcendentals=0),
        name="combine",
    )(starts, *slots, produced, dx)


def shards(
    tokens, cotangent, gate_weights, expert_ids, seq_lengths, query_weight, key_weight, value_weight,
    output_weight, attn_gain, ffn_gain, query_gain, key_gain, expert_in, expert_out,
):
    ep = lax.axis_size("ep")
    me = lax.axis_index("ep")
    seqs, rows, _ = tokens.shape
    length = rows * ep
    top = gate_weights.shape[2]
    local = expert_in.shape[0]
    hidden = expert_out.shape[1]
    experts = local * ep
    capacity = -(-(length * top * 9 // (8 * experts)) // 16) * 16

    gains = jnp.concatenate([attn_gain, ffn_gain]).astype(F32).reshape(-1, 128)
    few = [query_gain.astype(F32), key_gain.astype(F32), seq_lengths.astype(F32)]
    few = jnp.stack([jnp.pad(v, (0, 128 - v.shape[0])) for v in few])
    packet = jnp.concatenate([gains, few], axis=0)
    packet = jnp.pad(packet, ((0, -packet.shape[0] % 8), (0, 0)))
    share = gains.shape[0] // 2

    full, weights, cot_full, gains, small_in = front(
        tokens, cotangent, expert_ids.transpose(0, 2, 1), gate_weights.transpose(0, 2, 1),
        query_weight, key_weight, value_weight, packet,
    )

    half = HEAD_DIM // 2
    frequency = ROPE_BASE ** (-(np.arange(half, dtype=np.float32) * np.float32(2.0 / HEAD_DIM)))
    angles = np.arange(length, dtype=np.float32)[:, None] * frequency.astype(np.float32)[None, :]
    table = jnp.asarray(np.concatenate([np.cos(angles), np.sin(angles)], axis=-1), F32)

    if ep == 8 and lax.axis_size("rep") == 4:
        normed, pre, low, ctx, middle, mixed, cot_full, slots0, slots1, starts = attend_mix(
            top, local, full, weights, output_weight, gains, small_in, table, tokens, cotangent, cot_full
        )
    else:
        number = (me * local).astype(jnp.int32)[None]
        normed, pre, low, ctx, part, slots0, slots1, starts = attend(
            top, number, full, weights, output_weight, gains, small_in, table
        )
        starts = starts.astype(jnp.int32)
        middle, mixed = mix(part, tokens, small_in, gains)

    act, pair, x_all, dy_all, out_grad0 = expert_first(
        starts, mixed, cot_full, (slots0, slots1), expert_in, hidden, capacity
    )

    def over_rep(value):
        return lax.psum_scatter(value, "rep", scatter_dimension=0, tiled=True)

    out0 = over_rep(out_grad0)
    dgu, in_grad0 = first_in_grad(seqs, starts, x_all, dy_all, pair, expert_out)
    in0 = over_rep(in_grad0)
    x_all, _ = lax.optimization_barrier((x_all, in_grad0))
    act, dgu, in_grad1, out_grad1 = expert_second(seqs, starts, x_all, dy_all, expert_in, expert_out, act, dgu)
    in1 = over_rep(in_grad1)
    out1 = over_rep(out_grad1)
    produced, dx = expert_tails(seqs, starts, act, dgu, expert_in, expert_out)
    out_part, grad_part = combine(starts, (slots0, slots1), produced, dx, capacity)

    mgrad, ffn_back, agrad = back(grad_part, middle, cotangent, small_in, gains)
    npart, wgrad, wograd, qk_back = attend_back(
        agrad, normed, pre, low, ctx, weights, output_weight, small_in, table
    )
    sums, small, result, token_grad = finish(
        wgrad, wograd, npart, out_part, tokens, middle, mgrad, gains, ffn_back, qk_back
    )

    def widen(into, value, j):
        return lax.dynamic_update_slice(into, value.astype(F32)[None], (j, 0, 0))

    small, out0 = lax.optimization_barrier((small, out0))
    out_all = widen(jnp.zeros((local,) + out0.shape, F32), out0, 0)
    small, out_all = lax.optimization_barrier((small, out_all))

    heads = HEAD_DIM // ep
    return (
        result,
        token_grad,
        sums[1].astype(F32),
        sums[2].astype(F32),
        sums[3].astype(F32),
        sums[0].astype(F32),
        small[:share].reshape(-1),
        small[share : 2 * share].reshape(-1),
        small[2 * share, :heads],
        small[2 * share + 1, :heads],
        jnp.stack([in0, in1]).astype(F32),
        widen(out_all, out1, 1),
    )


def solution(mesh):
    seq = P("rep", "ep", None)
    row, gain, expert = P("ep", None), P("ep"), P("ep", None, None)
    split = P("ep", "rep", None)

    return jax.shard_map(
        shards,
        mesh=mesh,
        in_specs=(seq, seq, seq, seq, P(("rep", "ep")), row, row, row, row, gain, gain, gain, gain, expert, expert),
        out_specs=(seq, seq, row, row, row, row, gain, gain, gain, gain, split, split),
        check_vma=False,
    )
```

```python
import functools

import jax
import jax.numpy as jnp
import numpy as np
from jax import lax
from jax.experimental import pallas as pl
from jax.experimental.pallas import tpu as pltpu
from jax.sharding import PartitionSpec as P

HEAD_DIM = 128
EPS = 1e-06
ROPE_BASE = 50000.0
MESH = pl.DeviceIdType.MESH
F32 = jnp.float32
BF16 = jnp.bfloat16


def sds(shape, dtype):
    return jax.ShapeDtypeStruct(shape, dtype)


VM = pl.BlockSpec(memory_space=pltpu.VMEM)
AN = pl.BlockSpec(memory_space=pl.ANY)


def inverse_rms(v):
    return lax.rsqrt(jnp.mean(v * v, axis=-1, keepdims=True) + EPS)


def rms_back(v, r, ug):
    return r * ug - v * (r * r * r * jnp.mean(ug * v, axis=-1, keepdims=True))


def mix_rows(total, tok, living, gain):
    middle = tok.astype(F32) + living * total
    mixed = middle * inverse_rms(middle) * gain
    return middle, mixed.astype(BF16)


def ffn_back_rows(mixed_grad, middle, cot, living, gain):
    r = inverse_rms(middle)
    middle_grad = cot.astype(F32) + rms_back(middle, r, mixed_grad * gain)
    return middle_grad, (living * middle_grad).astype(BF16), mixed_grad * middle * r


def attn_back_rows(normed_grad, tok, middle_grad, gain):
    v = tok.astype(F32)
    r = inverse_rms(v)
    return (middle_grad + rms_back(v, r, normed_grad * gain)).astype(BF16), normed_grad * v * r


def seq_len(small, s):
    lane = lax.broadcasted_iota(jnp.int32, (1, 128), 1)
    return jnp.sum(jnp.where(lane == s, small[2:3, :], 0.0), axis=1, keepdims=True)


def live_rows(small, s, me, rows):
    place = (lax.broadcasted_iota(jnp.int32, (rows, 1), 0) + me * rows).astype(F32)
    return jnp.where(place < seq_len(small, s), 1.0, 0.0)


class Place:
    def __init__(self):
        me = lax.axis_index("ep")
        core, x, y = lax.rem(me, 2), lax.rem(me // 2, 2), me // 4
        self.rep = lax.axis_index("rep")
        self.me = me
        self.sb = me + 1 - 2 * core
        self.dx = 2 - 4 * x
        self.dy = 4 - 8 * y
        self.xn = me + self.dx
        self.yn = me + self.dy
        self.dg = me + self.dx + self.dy

    def push(self, src, dst, send, recv, dev):
        return pltpu.make_async_remote_copy(
            src_ref=src, dst_ref=dst, send_sem=send, recv_sem=recv, device_id=(self.rep, dev), device_id_type=MESH
        )

    def peer(self, m):
        k = m + 1
        return self.me + (k % 2) * (self.sb - self.me) + (k // 2 % 2) * self.dx + (k // 4) * self.dy

    def greet(self, peers):
        barrier = pltpu.get_barrier_semaphore()
        for peer in peers:
            pl.semaphore_signal(barrier, inc=1, device_id=(self.rep, peer), device_id_type=MESH)
        pl.semaphore_wait(barrier, len(peers))


class Gather:
    sems = 3

    def __init__(self, at, own, full, ssem, rsem, lsem):
        self.at, self.own, self.full, self.ssem, self.rsem, self.lsem = at, own, full, ssem, rsem, lsem
        self.rows = own.shape[1]

    @staticmethod
    def scratch(seqs):
        return [pltpu.SemaphoreType.DMA((7, seqs)), pltpu.SemaphoreType.DMA((8, seqs)), pltpu.SemaphoreType.DMA((seqs,))]

    def block(self, s, dev):
        return self.full.at[s, pl.ds(pl.multiple_of(dev * self.rows, self.rows), self.rows)]

    def copy(self, s, dev, kind, slot, to, src=None):
        block = self.block(s, dev)
        return self.at.push(block if src is None else src, block, self.ssem.at[kind, s], self.rsem.at[slot, s], to)

    def start(self, s):
        at, own = self.at, self.own.at[s]
        self.copy(s, at.me, 0, 2, at.xn, own).start()
        self.copy(s, at.me, 1, 4, at.yn, own).start()
        self.copy(s, at.me, 2, 1, at.sb, own).start()
        pltpu.make_async_copy(own, self.block(s, at.me), self.lsem.at[s]).start()

    def relay(self, s, by_y):
        at = self.at
        self.copy(s, at.xn, 0, 2, at.xn).wait_recv()
        if by_y:
            self.copy(s, at.xn, 3, 6, at.yn).start()
        self.copy(s, at.xn, 4, 3, at.sb).start()
        self.copy(s, at.yn, 1, 4, at.yn).wait_recv()
        if not by_y:
            self.copy(s, at.yn, 3, 6, at.xn).start()
        self.copy(s, at.yn, 5, 5, at.sb).start()

    def relay_far(self, s):
        at = self.at
        self.copy(s, at.dg, 3, 6, at.yn).wait_recv()
        self.copy(s, at.dg, 6, 7, at.sb).start()

    def finish(self, s):
        at = self.at
        for dev, slot in ((at.sb, 1), (at.sb + at.dx, 3), (at.sb + at.dy, 5), (at.sb + at.dx + at.dy, 7)):
            self.copy(s, dev, 0, slot, at.sb).wait_recv()
        for kind in range(7):
            self.copy(s, at.me, kind, 0, at.sb).wait_send()
        pltpu.make_async_copy(self.own.at[s], self.block(s, at.me), self.lsem.at[s]).wait()


def gather_tail(gather, low, high):
    def relay(i, _):
        gather.relay(low + 2 * i, True)
        gather.relay(low + 2 * i + 1, False)
        return 0

    lax.fori_loop(0, (high - low) // 2, relay, 0)
    each(high, gather.relay_far, low=low)
    each(high, gather.finish, low=low)


class Reduce:
    def __init__(self, at, part, held, mine, x1, y1, x2, y2, ms, hs, hr, d1s, d1r, d2s, d2r):
        self.at, self.part, self.held, self.mine = at, part, held, mine
        self.x1, self.y1, self.x2, self.y2 = x1, y1, x2, y2
        self.ms, self.hs, self.hr, self.d1s, self.d1r, self.d2s, self.d2r = ms, hs, hr, d1s, d1r, d2s, d2r
        self.half = part.shape[2] // 2

    @staticmethod
    def scratch(part):
        s, _, t, d = part.shape
        dma = pltpu.SemaphoreType.DMA
        return [
            pltpu.VMEM((s, 4, t, d), BF16),
            pltpu.VMEM((s, 4, t, d), BF16),
            pltpu.VMEM((s, t // 2, d), BF16),
            pltpu.VMEM((s, t // 2, d), BF16),
            pltpu.VMEM((s, t, d), BF16),
            pltpu.VMEM((s, t, d), BF16),
            dma((4, s)),
            dma((4, s)),
            dma((4, s)),
            dma((2, s)),
            dma((2, s)),
            dma((2, s)),
            dma((2, s)),
        ]

    sems = 13

    def core_copy(self, s, k):
        at = self.at
        dest = (at.sb, at.sb + at.dx, at.sb + at.dy, at.sb + at.dx + at.dy)[k]
        return at.push(self.part.at[s, dest], self.held.at[s, k], self.hs.at[k, s], self.hr.at[k, s], at.sb)

    def load(self, s, k):
        at = self.at
        dest = (at.me, at.xn, at.yn, at.dg)[k]
        return pltpu.make_async_copy(self.part.at[s, dest], self.mine.at[s, k], self.ms.at[k, s])

    def first(self, s, k):
        at, h = self.at, self.half
        src = self.held.at[s, 3, pl.ds(k * h, h)]
        return at.push(src, (self.x1, self.y1)[k].at[s], self.d1s.at[k, s], self.d1r.at[k, s], (at.xn, at.yn)[k])

    def second(self, s, k):
        at = self.at
        src = self.held.at[s, 1 + k]
        return at.push(src, (self.x2, self.y2)[k].at[s], self.d2s.at[k, s], self.d2r.at[k, s], (at.xn, at.yn)[k])

    def start(self, s):
        for k in (3, 1, 2, 0):
            self.core_copy(s, k).start()
            self.load(s, k).start()

    def hop1(self, s):
        self.core_copy(s, 3).wait_recv()
        self.load(s, 3).wait()
        self.held[s, 3] = (self.held[s, 3].astype(F32) + self.mine[s, 3].astype(F32)).astype(BF16)
        self.first(s, 0).start()
        self.first(s, 1).start()

    def hop2(self, s):
        h = self.half
        for k, extra, rows, rest in (
            (0, self.y1, pl.ds(h, h), pl.ds(0, h)),
            (1, self.x1, pl.ds(0, h), pl.ds(h, h)),
        ):
            self.core_copy(s, 1 + k).wait_recv()
            self.load(s, 1 + k).wait()
            self.first(s, 1 - k).wait_recv()
            held, mine = self.held.at[s, 1 + k], self.mine.at[s, 1 + k]
            held[rows] = (held[rows].astype(F32) + mine[rows].astype(F32) + extra[s].astype(F32)).astype(BF16)
            held[rest] = (held[rest].astype(F32) + mine[rest].astype(F32)).astype(BF16)
            self.second(s, k).start()

    def total(self, s):
        self.core_copy(s, 0).wait_recv()
        self.load(s, 0).wait()
        self.second(s, 0).wait_recv()
        self.second(s, 1).wait_recv()
        return (
            self.mine[s, 0].astype(F32)
            + self.held[s, 0].astype(F32)
            + self.x2[s].astype(F32)
            + self.y2[s].astype(F32)
        )

    def finish(self, s):
        for k in range(4):
            self.core_copy(s, k).wait_send()
        for k in range(2):
            self.first(s, k).wait_send()
            self.second(s, k).wait_send()


def each(n, *steps, low=0):
    def run(s, _):
        for step in steps:
            step(s)
        return 0

    lax.fori_loop(low, n, run, 0)


COMM = dict(has_side_effects=True, vmem_limit_bytes=60 << 20)


def front(tokens, cotangent, ids, gates, wq, wk, wv, packet):
    _, _, width = tokens.shape
    ep = lax.axis_size("ep")
    top = ids.shape[1]
    routes = jnp.concatenate([ids.astype(BF16), gates], axis=1).transpose(0, 2, 1)
    routes = jnp.pad(routes, ((0, 0), (0, 0), (0, 128 - 2 * top)))
    full = lax.all_gather(jnp.concatenate([tokens, routes], axis=-1), "ep", axis=1, tiled=True)
    weights = [lax.all_to_all(w, "ep", split_axis=1, concat_axis=0, tiled=True) for w in (wq, wk, wv)]
    packets = lax.all_gather(packet, "ep", axis=0)
    share, heads = width // (128 * ep), HEAD_DIM // ep
    gains = jnp.stack([packets[:, :share].reshape(width), packets[:, share : 2 * share].reshape(width)])
    lens = jnp.pad(packets[:, 2 * share + 2, 0], (0, 128 - ep))
    few = [packets[:, 2 * share + k, :heads].reshape(HEAD_DIM) for k in range(2)] + [lens]
    return (
        full, jnp.stack(weights), lax.all_gather(cotangent, "ep", axis=1, tiled=True),
        jnp.pad(gains, ((0, 6), (0, 0))), jnp.pad(jnp.stack(few), ((0, 5), (0, 0))),
    )


def plain_living(small, seqs, rows):
    place = (jnp.arange(rows) + lax.axis_index("ep") * rows).astype(F32)
    return (place[None] < small[2, :seqs, None]).astype(F32)[..., None]


def mix(part, tokens, small, gains):
    seqs, rows, _ = tokens.shape
    total = lax.psum_scatter(part, "ep", scatter_dimension=1, tiled=True).astype(F32)
    middle, mixed = mix_rows(total, tokens, plain_living(small, seqs, rows), gains[1])
    return middle, lax.all_gather(mixed, "ep", axis=1, tiled=True)


def back_kernel(gpart, middle, cot, small, gains, mgrad, ggrad, full, own, *scratch):
    at = Place()
    seqs = cot.shape[0]
    n = Reduce.sems
    rg = Reduce(at, gpart, *scratch[:n])
    gather = Gather(at, own, full, *scratch[n:])
    at.greet((at.xn, at.yn, at.sb))
    each(seqs, rg.start)
    each(seqs, rg.hop1)
    each(seqs, rg.hop2)
    ggrad[...] = jnp.zeros_like(ggrad)

    def rows(s):
        living = live_rows(small, s, at.me, cot.shape[1])
        mg, ag, back = ffn_back_rows(rg.total(s), middle[s], cot[s], living, gains[1:2])
        mgrad[s] = mg
        own[s] = ag
        ggrad[...] += jnp.sum(back, axis=0, keepdims=True)
        gather.start(s)

    each(seqs, rows)
    gather_tail(gather, 0, seqs)
    each(seqs, rg.finish)


def back(gpart, middle, cot, small, gains):
    seqs, rows, width = cot.shape
    ep = lax.axis_size("ep")
    if ep != 8:
        mixed_grad = lax.psum_scatter(gpart, "ep", scatter_dimension=1, tiled=True).astype(F32)
        mg, ag, backs = ffn_back_rows(mixed_grad, middle, cot, plain_living(small, seqs, rows), gains[1])
        full = lax.all_gather(ag, "ep", axis=1, tiled=True)
        return mg, jnp.sum(backs, axis=(0, 1))[None], full
    gpart = gpart.reshape(seqs, ep, rows, width)
    return pl.pallas_call(
        back_kernel,
        out_shape=(
            sds(cot.shape, F32),
            sds((1, width), F32),
            sds((seqs, rows * ep, width), BF16),
        ),
        in_specs=[AN] + [VM] * 4,
        out_specs=(VM, VM, AN),
        scratch_shapes=[pltpu.VMEM(cot.shape, BF16)] + Reduce.scratch(gpart) + Gather.scratch(seqs),
        compiler_params=pltpu.CompilerParams(collective_id=3, **COMM),
        name="back",
    )(gpart, middle, cot, small, gains)


def finish_kernel(
    wgrad, wograd, npart, opart, tok, middle, mgrad, gains, others,
    out, small_out, result, tgrad,
    own, held, met, ggrad, parcel, landed, spare,
    wsend, wrecv, local, gsend, grecv, os, or_, ps, pr, qs, qr, fs, fr, ss, sr, *scratch,
):
    at = Place()
    z, me = at.rep, at.me
    n = Reduce.sems
    normed_sum = Reduce(at, npart, *scratch[:n])
    result_sum = Reduce(at, opart, *scratch[n:])
    seqs = tok.shape[0]
    parts, pieces = own.shape[:2]
    chunks = parts * pieces
    width = wgrad.shape[3]
    barrier = pltpu.get_barrier_semaphore()
    line = [lax.rem(z + k, 4) for k in range(1, 4)]
    for dev in line:
        pl.semaphore_signal(barrier, inc=1, device_id=(dev, me), device_id_type=MESH)
    each(7, lambda m: pl.semaphore_signal(barrier, inc=1, device_id=(z, at.peer(m)), device_id_type=MESH))
    pl.semaphore_wait(barrier, 10)
    inner = jnp.logical_and(z > 0, z < 3)
    outer_end, partner, outer = 1 + z // 3, 3 - z, 3 * (z - 1)
    cols = pl.ds(pl.multiple_of(me * width, width), width)

    def column_copy(m, j):
        dev = at.peer(m)
        rows = pl.ds(pl.multiple_of(dev * pieces, pieces), pieces)
        return at.push(wgrad.at[j, rows], own.at[1 + j, :, :, cols], wsend.at[m, j], wrecv.at[m, j], dev)

    mine_rows = pl.ds(pl.multiple_of(me * pieces, pieces), pieces)
    locals_ = [pltpu.make_async_copy(wgrad.at[j, mine_rows], own.at[1 + j, :, :, cols], local.at[j]) for j in range(3)]
    locals_.append(pltpu.make_async_copy(wograd, own.at[0], local.at[3]))
    for copy in locals_:
        copy.start()
    for j in range(3):
        each(7, lambda m, j=j: column_copy(m, j).start())
    each(seqs, normed_sum.start)
    each(seqs, result_sum.start)
    ggrad[...] = jnp.zeros_like(ggrad)

    def piece(ref, c):
        return ref.at[c // pieces, lax.rem(c, pieces)]

    def line_push(src, dst, send, recv, dev):
        return pltpu.make_async_remote_copy(
            src_ref=src, dst_ref=dst, send_sem=send, recv_sem=recv, device_id=(dev, me), device_id_type=MESH
        )

    def inward(c):
        return line_push(piece(own, c), piece(held, c), os.at[c], or_.at[c], outer_end)

    def across(c):
        return line_push(piece(held, c), met.at[c // 2], ps.at[c], pr.at[c], partner)

    def share(c):
        return line_push(piece(out, c), piece(out, c), qs.at[c], qr.at[c], partner)

    def outward(c):
        return line_push(piece(out, c), piece(out, c), fs.at[c], fr.at[c], outer)

    def mine(c):
        return 1 + lax.rem(c, 2) == z

    def ready(part):
        for j in range(parts):

            @pl.when(part == j)
            def _():
                locals_[(3, 0, 1, 2)[j]].wait()
                if j > 0:
                    each(7, lambda m: column_copy(m, j - 1).wait_recv())

    def step(c):
        @pl.when(lax.rem(c, pieces) == 0)
        def _():
            ready(c // pieces)

        @pl.when(jnp.logical_not(inner))
        def _():
            inward(c).start()

        @pl.when(inner)
        def _():
            inward(c).wait_recv()
            here = piece(held, c)
            here[...] = (here[...].astype(F32) + piece(own, c)[...].astype(F32)).astype(BF16)

            @pl.when(jnp.logical_not(mine(c)))
            def _():
                across(c).start()

    def settle(c):
        @pl.when(jnp.logical_and(inner, mine(c)))
        def _():
            across(c).wait_recv()
            piece(out, c)[...] = (piece(held, c)[...].astype(F32) + met[c // 2].astype(F32)).astype(BF16)
            share(c).start()
            outward(c).start()

    def forward(c):
        @pl.when(jnp.logical_and(inner, jnp.logical_not(mine(c))))
        def _():
            share(c).wait_recv()
            outward(c).start()

    def token_rows(s):
        tg, back = attn_back_rows(normed_sum.total(s), tok[s], mgrad[s], gains[0:1])
        tgrad[s] = tg
        ggrad[...] += jnp.sum(back, axis=0, keepdims=True)

    def out_rows(s):
        result[s] = (middle[s] + result_sum.total(s)).astype(BF16)

    jobs = (
        (step, 0, chunks), (settle, 1, chunks), (forward, 2, chunks),
        (normed_sum.hop1, 2, seqs), (normed_sum.hop2, 6, seqs), (token_rows, 10, seqs),
        (result_sum.hop1, 6, seqs), (result_sum.hop2, 10, seqs), (out_rows, 14, seqs),
    )

    def tick(i, _):
        for job, lag, count in jobs:

            @pl.when(jnp.logical_and(i >= lag, i < lag + count))
            def _():
                job(i - lag)

        return 0

    lax.fori_loop(0, max(lag + count for _, lag, count in jobs), tick, 0)

    parcel[...] = jnp.zeros_like(parcel)
    devices = parcel.shape[0]
    rows_of = ggrad.shape[1] // (128 * devices)
    for dev in range(devices):
        for k in range(rows_of):
            lanes = pl.ds((dev * rows_of + k) * 128, 128)
            parcel[dev, k : k + 1] = ggrad[:, lanes]
            parcel[dev, rows_of + k : rows_of + k + 1] = others[0:1, lanes]
        parcel[dev, 2 * rows_of : 2 * rows_of + 2] = others[1:3, 0:128]

    def parcel_copy(m):
        dev = at.peer(m)
        return at.push(parcel.at[dev], landed.at[m], gsend.at[m], grecv.at[m], dev)

    each(7, lambda m: parcel_copy(m).start())
    spare[0] = parcel[me]

    def add_parcel(m):
        parcel_copy(m).wait_recv()
        spare[0] += landed[m]

    each(7, add_parcel)

    def small_copy(k):
        return line_push(spare.at[0], spare.at[1 + k], ss.at[k], sr.at[k], line[k])

    for k in range(3):
        small_copy(k).start()

    @pl.when(jnp.logical_not(inner))
    def _():
        each(chunks, lambda c: outward(c).wait_recv())
        each(chunks, lambda c: inward(c).wait_send())

    @pl.when(inner)
    def _():
        def sent(c):
            outward(c).wait_send()

            @pl.when(mine(c))
            def _():
                share(c).wait_send()

            @pl.when(jnp.logical_not(mine(c)))
            def _():
                across(c).wait_send()

        each(chunks, sent)

    each(seqs, normed_sum.finish, result_sum.finish)

    def all_sent(m):
        parcel_copy(m).wait_send()
        for j in range(3):
            column_copy(m, j).wait_send()

    each(7, all_sent)
    total = spare[0]
    for k in range(3):
        small_copy(k).wait()
        total = total + spare[1 + k]
    small_out[...] = total
    few = total[2 * rows_of : 2 * rows_of + 2]
    heads = HEAD_DIM // devices
    moved = jnp.zeros_like(few)
    for k in range(devices):
        moved += jnp.where(me == k, pltpu.roll(few, (128 - k * heads) % 128, 1), 0.0)
    small_out[2 * rows_of : 2 * rows_of + 2] = moved


def finish(wgrad, wograd, npart, opart, tokens, middle, mgrad, gains, ffn_back, qk_back):
    seqs, rows, width = tokens.shape
    ep = lax.axis_size("ep")
    if ep != 8 or lax.axis_size("rep") != 4:
        normed_grad = lax.psum_scatter(npart, "ep", scatter_dimension=1, tiled=True).astype(F32)
        moe = lax.psum_scatter(opart, "ep", scatter_dimension=1, tiled=True).astype(F32)
        tg, backs = attn_back_rows(normed_grad, tokens, mgrad, gains[0])
        wrows = lax.all_to_all(wgrad, "ep", split_axis=1, concat_axis=2, tiled=True)
        share = width // ep
        small = jnp.concatenate([jnp.sum(backs, axis=(0, 1)), ffn_back[0], qk_back[0], qk_back[1]])
        small = lax.psum(small, ("ep", "rep"))
        mine = lax.axis_index("ep") * share
        cut = [lax.dynamic_slice_in_dim(small, k * width + mine, share).reshape(-1, 128) for k in range(2)]
        few = small[2 * width :].reshape(2, HEAD_DIM)
        few = jnp.roll(few, -lax.axis_index("ep") * (HEAD_DIM // ep), axis=1)
        small = jnp.concatenate(cut + [few], axis=0)
        big = lax.psum(jnp.concatenate([wograd[None], wrows], axis=0), "rep")
        return big, jnp.pad(small, ((0, 8 - small.shape[0]), (0, 0))), (middle + moe).astype(BF16), tg
    others = jnp.concatenate([ffn_back, jnp.pad(qk_back[:2], ((0, 0), (0, width - HEAD_DIM)))], axis=0)
    npart, opart = (p.reshape(seqs, ep, rows, width) for p in (npart, opart))
    pieces = 4
    block = wograd.shape[0] // pieces
    wgrad = wgrad.reshape(3, wgrad.shape[1] // block, block, wgrad.shape[2])
    wograd = wograd.reshape(pieces, block, width)
    whole = (4, pieces, block, width)
    dma = pltpu.SemaphoreType.DMA
    chunks = 4 * pieces
    out, small, result, tgrad = pl.pallas_call(
        finish_kernel,
        out_shape=(sds(whole, BF16), sds((8, 128), F32), sds(tokens.shape, BF16), sds(tokens.shape, BF16)),
        in_specs=[VM, VM, AN, AN] + [VM] * 5,
        out_specs=(VM, VM, VM, VM),
        scratch_shapes=[
            pltpu.VMEM(whole, BF16),
            pltpu.VMEM(whole, BF16),
            pltpu.VMEM((chunks // 2, block, width), BF16),
            pltpu.VMEM((1, width), F32),
            pltpu.VMEM((ep, 8, 128), F32),
            pltpu.VMEM((7, 8, 128), F32),
            pltpu.VMEM((4, 8, 128), F32),
        ]
        + [dma((7, 3)), dma((7, 3)), dma((4,)), dma((7,)), dma((7,))]
        + [dma((chunks,))] * 8
        + [dma((3,))] * 2
        + 2 * Reduce.scratch(npart),
        compiler_params=pltpu.CompilerParams(collective_id=4, has_side_effects=True, vmem_limit_bytes=61 << 20),
        name="finish",
    )(wgrad, wograd, npart, opart, tokens, middle, mgrad, gains, others)
    return out.reshape(4, pieces * block, width), small, result, tgrad


def dot(a, b, ca, cb):
    return lax.dot_general(a, b, (((ca,), (cb,)), ((), ())), preferred_element_type=F32)


def rope_tables(table):
    half = HEAD_DIM // 2
    values = table[...]
    turned = pltpu.roll(values, half, 1)
    first = lax.broadcasted_iota(jnp.int32, values.shape, 1) < half
    return jnp.where(first, values, turned), jnp.where(first, -turned, values)


def rope(v, cos, sin_turn):
    return v * cos + pltpu.roll(v, HEAD_DIM // 2, 1) * sin_turn


def probabilities(q, k, length):
    scores = dot(q, k, 1, 1) * HEAD_DIM**-0.5
    column = lax.broadcasted_iota(jnp.int32, (1, scores.shape[1]), 1).astype(F32)
    scores = jnp.where(column < length, scores, -1e9)
    p = jnp.exp(scores - jnp.max(scores, axis=-1, keepdims=True))
    return p * (1.0 / jnp.sum(p, axis=-1, keepdims=True))


def packed_slots(number, table, length_live, top):
    tab = table.astype(F32)
    length = tab.shape[0]
    lane = lax.broadcasted_iota(jnp.int32, tab.shape, 1)
    row = lax.broadcasted_iota(jnp.int32, (length, 1), 0).astype(F32)
    chosen = jnp.logical_and(jnp.logical_and(tab == number, lane < top), row < length_live)
    gates = jnp.where(chosen, pltpu.roll(tab, 128 - top, 1), 0.0).astype(BF16)
    chosen = jnp.where(chosen, 1.0, 0.0).astype(BF16)
    ones = jnp.ones((8, 128), BF16)
    hit = dot(ones, chosen, 1, 1)
    weight = dot(ones, gates, 1, 1)
    earlier = lax.broadcasted_iota(jnp.int32, (length, length), 0)
    later = lax.broadcasted_iota(jnp.int32, (length, length), 1)
    rank = dot(hit.astype(BF16), jnp.where(earlier < later, 1.0, 0.0).astype(BF16), 1, 0)
    return jnp.where(hit > 0.5, rank, -1.0), weight, jnp.sum(hit[0:1], axis=1, keepdims=True)


def attend_rows(top, number, s, block, w, wo, gains, small, table, normed, pre, low, ctx, part, slots, starts):
    width = normed.shape[1]
    length = seq_len(small, s)
    cos, sin = rope_tables(table)
    v = block[:, 0:width].astype(F32)
    x = (v * inverse_rms(v) * gains[0:1]).astype(BF16)
    normed[...] = x
    q_pre, k_pre = dot(x, w[0], 1, 0), dot(x, w[1], 1, 0)
    value = dot(x, w[2], 1, 0).astype(BF16)
    pre[0], pre[1] = q_pre, k_pre
    low[2] = value
    for h in range(q_pre.shape[1] // HEAD_DIM):
        cols = slice(h * HEAD_DIM, (h + 1) * HEAD_DIM)
        rot = []
        for i, (u, g) in enumerate(((q_pre[:, cols], small[0:1]), (k_pre[:, cols], small[1:2]))):
            rot.append(rope(u * inverse_rms(u) * g, cos, sin).astype(BF16))
            low[i, :, cols] = rot[i]
        attention = probabilities(rot[0], rot[1], length).astype(BF16)
        ctx[:, cols] = dot(attention, value[:, cols], 1, 0).astype(BF16)
    part[...] = dot(ctx[...], wo[...], 1, 0).astype(BF16).reshape(part.shape)
    routes = block[:, width : width + 128]
    lane = lax.broadcasted_iota(jnp.int32, (1, 128), 1)
    for j, ref in enumerate(slots):
        slot, weight, count = packed_slots(number + j, routes, length, top)
        ref[0:8] = slot
        ref[8:16] = weight
        row = starts[j : j + 1]
        after = jnp.sum(jnp.where(lane == s, row, 0.0), axis=1, keepdims=True) + 16.0 * jnp.floor((count + 15.0) * 0.0625)
        starts[j : j + 1] = jnp.where(lane == s + 1, after, row)


def attend_kernel(top, number, full, w, wo, gains, small, table, normed, pre, low, ctx, part, slots0, slots1, starts):
    s = pl.program_id(0)

    @pl.when(s == 0)
    def _():
        starts[...] = jnp.zeros_like(starts)

    attend_rows(
        top, number[0].astype(F32), s, full.at[0], w, wo, gains, small, table,
        normed.at[0], pre.at[:, 0], low.at[:, 0], ctx.at[0], part.at[0], (slots0.at[0], slots1.at[0]), starts,
    )


def attend(top, number, full, weights, wo, gains, small, table):
    seqs, length, wide = full.shape
    width = wide - 128
    cols = weights.shape[2]
    row = lambda i, *_: (i, 0, 0)
    row2 = lambda i, *_: (0, i, 0, 0)
    two = lambda i, *_: (0, 0)
    slot = pl.BlockSpec((1, 16, length), row)
    return pl.pallas_call(
        functools.partial(attend_kernel, top),
        out_shape=(
            sds((seqs, length, width), BF16),
            sds((2, seqs, length, cols), F32),
            sds((3, seqs, length, cols), BF16),
            sds((seqs, length, cols), BF16),
            sds((seqs, length, width), BF16),
            sds((seqs, 16, length), F32),
            sds((seqs, 16, length), F32),
            sds((8, 128), F32),
        ),
        grid_spec=pltpu.PrefetchScalarGridSpec(
            num_scalar_prefetch=1,
            grid=(seqs,),
            in_specs=[
                pl.BlockSpec((1, length, wide), row),
                pl.BlockSpec(weights.shape, lambda i, *_: (0, 0, 0)),
                pl.BlockSpec(wo.shape, two),
                pl.BlockSpec((8, width), two),
                pl.BlockSpec((8, 128), two),
                pl.BlockSpec((length, HEAD_DIM), two),
            ],
            out_specs=(
                pl.BlockSpec((1, length, width), row),
                pl.BlockSpec((2, 1, length, cols), row2),
                pl.BlockSpec((3, 1, length, cols), row2),
                pl.BlockSpec((1, length, cols), row),
                pl.BlockSpec((1, length, width), row),
                slot,
                slot,
                pl.BlockSpec((8, 128), two),
            ),
        ),
        compiler_params=pltpu.CompilerParams(dimension_semantics=("arbitrary",), vmem_limit_bytes=60 << 20),
        cost_estimate=pl.CostEstimate(flops=10**10, bytes_accessed=4 * 10**7, transcendentals=10**6),
        name="attend",
    )(number, full, weights, wo, gains, small, table)


def forward_kernel(
    top, experts, tok, cot, ids, gates, wq, wk, wv, pk, wo, table,
    weights_out, gains, small, normed, pre, low, ctx, middle, mixed, cot_full, slots0, slots1, starts,
    weights, full, packets, own, mixed_own, nbuf, pbuf, lbuf, cbuf, part, begins, ssem,
    wsend, wrecv, psend, precv, rsend, rrecv, lsend, lrecv, local, *scratch,
):
    at = Place()
    z = at.rep
    n = Reduce.sems
    reduce = Reduce(at, part, *scratch[:n])
    gather = Gather(at, own, full, *scratch[n : n + 3])
    cot_gather = Gather(at, cot, cot_full, *scratch[n + 3 : n + 6])
    mixed_gather = Gather(at, mixed_own, mixed, *scratch[n + 6 :])
    seqs, rows, width = tok.shape
    top = ids.shape[1]
    block, cols = wq.shape[0], weights.shape[2]
    quarter = block // 4
    barrier = pltpu.get_barrier_semaphore()
    line = [lax.rem(z + k, 4) for k in range(1, 4)]
    for dev in line:
        pl.semaphore_signal(barrier, inc=1, device_id=(dev, at.me), device_id_type=MESH)
    each(7, lambda m: pl.semaphore_signal(barrier, inc=1, device_id=(z, at.peer(m)), device_id_type=MESH))
    pl.semaphore_wait(barrier, 10)

    def packet_copy(m):
        return at.push(pk, packets.at[at.me], psend.at[m], precv.at[m], at.peer(m))

    def weight_copy(m, j):
        dev = at.peer(m)
        theirs = pl.ds(pl.multiple_of(dev * cols, cols), cols)
        src = (wq, wk, wv)[j].at[pl.ds(pl.multiple_of(z * quarter, quarter), quarter), theirs]
        dst = weights.at[j, pl.ds(pl.multiple_of(at.me * block + z * quarter, quarter), quarter)]
        return at.push(src, dst, wsend.at[m, j], wrecv.at[m, j], dev)

    def weight_landed(m, j):
        dev = at.peer(m)
        dst = weights.at[j, pl.ds(pl.multiple_of(dev * block + z * quarter, quarter), quarter)]
        return at.push(dst, dst, wsend.at[m, j], wrecv.at[m, j], dev)

    def walk(m, q, right):
        part = weights.at[:, pl.ds(pl.multiple_of(at.peer(m) * block + q * quarter, quarter), quarter)]
        send, recv, dev = (rsend, rrecv, z + 1) if right else (lsend, lrecv, z - 1)
        return pltpu.make_async_remote_copy(
            src_ref=part, dst_ref=part, send_sem=send.at[m, q], recv_sem=recv.at[m, q],
            device_id=(dev, at.me), device_id_type=MESH,
        )

    def send_weights(m):
        packet_copy(m).start()
        for j in range(3):
            weight_copy(m, j).start()

    each(7, send_weights)

    place = lax.broadcasted_iota(jnp.int32, (top, 128), 0)
    lane = lax.broadcasted_iota(jnp.int32, (top, 128), 1)
    first = jnp.where(lane == place, 1.0, 0.0).astype(BF16)
    second = jnp.where(lane == place + top, 1.0, 0.0).astype(BF16)

    def join(s):
        own[s, :, 0:width] = tok[s]
        table = dot(ids[s].astype(F32).astype(BF16), first, 0, 0) + dot(gates[s], second, 0, 0)
        own[s, :, width : width + 128] = table.astype(BF16)

    each(seqs, join)
    each(seqs, gather.start)
    own_cols = pl.ds(pl.multiple_of(at.me * cols, cols), cols)
    mine = pl.ds(pl.multiple_of(at.me * block, block), block)
    own_weights = [
        pltpu.make_async_copy(w.at[:, own_cols], weights.at[j, mine], local.at[j]) for j, w in enumerate((wq, wk, wv))
    ]
    for copy in own_weights:
        copy.start()
    early = seqs // 2
    each(early, cot_gather.start)

    def set_out(m):
        for j in range(3):
            weight_landed(m, j).wait_recv()

        @pl.when(z < 3)
        def _():
            walk(m, z, True).start()

        @pl.when(z > 0)
        def _():
            walk(m, z, False).start()

    each(7, set_out)

    def pass_on(d):
        def step(m):
            @pl.when(z - d >= 0)
            def _():
                walk(m, z - d, True).wait_recv()

                @pl.when(z < 3)
                def _():
                    walk(m, z - d, True).start()

            @pl.when(z + d <= 3)
            def _():
                walk(m, z + d, False).wait_recv()

                @pl.when(z > 0)
                def _():
                    walk(m, z + d, False).start()

        each(7, step)

    def relay(i, _):
        gather.relay(2 * i, True)
        gather.relay(2 * i + 1, False)
        return 0

    pairs = seqs // 2
    lax.fori_loop(0, pairs // 2, relay, 0)
    pass_on(1)
    lax.fori_loop(pairs // 2, pairs, relay, 0)
    pass_on(2)
    each(seqs, gather.relay_far)
    each(7, lambda m: packet_copy(m).wait_recv())
    packets[at.me] = pk[...]
    devices = packets.shape[0]
    share = width // (128 * devices)
    heads = HEAD_DIM // devices
    gains[...] = jnp.zeros_like(gains)
    small[...] = jnp.zeros_like(small)
    for o in range(devices):
        for k in range(share):
            lanes = pl.ds((o * share + k) * 128, 128)
            gains[0:1, lanes] = packets[o, k : k + 1]
            gains[1:2, lanes] = packets[o, share + k : share + k + 1]
        base = 2 * share
        small[0:1] += pltpu.roll(packets[o, base : base + 1], o * heads, 1)
        small[1:2] += pltpu.roll(packets[o, base + 1 : base + 2], o * heads, 1)
        small[2:3] += pltpu.roll(packets[o, base + 2 : base + 3], o, 1)
    each(seqs, gather.finish)
    pass_on(3)

    def sent(m):
        for q in range(4):

            @pl.when(jnp.logical_and(q <= z, z < 3))
            def _():
                walk(m, q, True).wait_send()

            @pl.when(jnp.logical_and(q >= z, z > 0))
            def _():
                walk(m, q, False).wait_send()

        packet_copy(m).wait_send()
        for j in range(3):
            weight_copy(m, j).wait_send()

    for copy in own_weights:
        copy.wait()
    keep = pltpu.make_async_copy(weights, weights_out, local.at[3])
    keep.start()
    each(seqs, cot_gather.start, low=early)
    number = (at.me * experts).astype(F32)
    begins[...] = jnp.zeros_like(begins)

    def stores(s):
        k = lax.rem(s, 2)
        pairs = ((nbuf.at[k], normed.at[s]), (pbuf.at[k], pre.at[:, s]), (lbuf.at[k], low.at[:, s]), (cbuf.at[k], ctx.at[s]))
        return [pltpu.make_async_copy(src, dst, ssem.at[i, k]) for i, (src, dst) in enumerate(pairs)]

    def sequence(s):
        k = lax.rem(s, 2)

        @pl.when(s >= 2)
        def _():
            for copy in stores(s - 2):
                copy.wait()

        attend_rows(
            top, number, s, full.at[s], weights, wo, gains, small, table,
            nbuf.at[k], pbuf.at[k], lbuf.at[k], cbuf.at[k], part.at[s], (slots0.at[s], slots1.at[s]), begins,
        )
        for copy in stores(s):
            copy.start()
        reduce.start(s)

    def rows(s):
        living = live_rows(small, s, at.me, tok.shape[1])
        mid, out = mix_rows(reduce.total(s), tok[s], living, gains[1:2])
        middle[s] = mid
        mixed_own[s] = out
        mixed_gather.start(s)

    def cot_pair(p):
        @pl.when(lax.rem(p, 2) == 0)
        def _():
            cot_gather.relay(p, True)
            cot_gather.relay(p + 1, False)

    jobs = (
        (sequence, 0, seqs), (reduce.hop1, 1, seqs), (cot_pair, 0, seqs), (reduce.hop2, 3, seqs),
        (cot_gather.relay_far, 4, seqs), (rows, 5, seqs),
    )

    def tick(i, _):
        for job, lag, count in jobs:

            @pl.when(jnp.logical_and(i >= lag, i < lag + count))
            def _():
                job(i - lag)

        return 0

    lax.fori_loop(0, max(lag + count for _, lag, count in jobs), tick, 0)
    starts[...] = begins[...].astype(jnp.int32)
    each(seqs, cot_gather.finish)
    gather_tail(mixed_gather, 0, seqs)
    for s in (seqs - 2, seqs - 1):
        for copy in stores(s):
            copy.wait()
    each(seqs, reduce.finish)
    each(7, sent)
    keep.wait()


def forward(top, experts, tokens, cotangent, ids, gates, wq, wk, wv, packet, wo, table):
    seqs, rows, width = tokens.shape
    length, cols = rows * 8, wq.shape[1] // 8
    part = sds((seqs, 8, rows, width), BF16)
    weights = (3, wq.shape[0] * 8, cols)
    dma = pltpu.SemaphoreType.DMA
    return pl.pallas_call(
        functools.partial(forward_kernel, top, experts),
        out_shape=(
            sds(weights, BF16),
            sds((8, width), F32),
            sds((8, 128), F32),
            sds((seqs, length, width), BF16),
            sds((2, seqs, length, cols), F32),
            sds((3, seqs, length, cols), BF16),
            sds((seqs, length, cols), BF16),
            sds(tokens.shape, F32),
            sds((seqs, length, width), BF16),
            sds((seqs, length, width), BF16),
            sds((seqs, 16, length), F32),
            sds((seqs, 16, length), F32),
            sds((8, 128), jnp.int32),
        ),
        in_specs=[VM] * 10,
        out_specs=(AN, VM, VM, AN, AN, AN, AN, VM, AN, AN, VM, VM, VM),
        scratch_shapes=[
            pltpu.VMEM(weights, BF16),
            pltpu.VMEM((seqs, length, width + 128), BF16),
            pltpu.VMEM((8,) + packet.shape, F32),
            pltpu.VMEM((seqs, rows, width + 128), BF16),
            pltpu.VMEM(tokens.shape, BF16),
            pltpu.VMEM((2, length, width), BF16),
            pltpu.VMEM((2, 2, length, cols), F32),
            pltpu.VMEM((2, 3, length, cols), BF16),
            pltpu.VMEM((2, length, cols), BF16),
            pltpu.VMEM(part.shape, BF16),
            pltpu.VMEM((8, 128), F32),
            dma((4, 2)),
        ]
        + [dma((7, 3)), dma((7, 3)), dma((7,)), dma((7,))]
        + [dma((7, 4))] * 4
        + [dma((4,))]
        + Reduce.scratch(part)
        + 3 * Gather.scratch(seqs),
        compiler_params=pltpu.CompilerParams(collective_id=1, **COMM),
        name="forward",
    )(tokens, cotangent, ids, gates, wq, wk, wv, packet, wo, table)


def attend_back_kernel(
    agrad, normed, pre, low, ctx, w, wo, small, table, part, wgrad, wograd, gains, wacc, woacc,
):
    s = pl.program_id(0)
    length = seq_len(small, s)
    cos, sin = rope_tables(table)

    @pl.when(s == 0)
    def _():
        wacc[...] = jnp.zeros_like(wacc)
        woacc[...] = jnp.zeros_like(woacc)
        gains[...] = jnp.zeros_like(gains)

    ag = agrad[0]
    woacc[...] += dot(ctx[0], ag, 0, 0)
    cg_all = dot(ag, wo[...], 1, 1).astype(BF16)
    scale = HEAD_DIM**-0.5
    half = HEAD_DIM // 2
    grads = ([], [], [])
    for h in range(cg_all.shape[1] // HEAD_DIM):
        cols = slice(h * HEAD_DIM, (h + 1) * HEAD_DIM)
        q, k, value, cg = low[0, 0, :, cols], low[1, 0, :, cols], low[2, 0, :, cols], cg_all[:, cols]
        attention = probabilities(q, k, length)
        grads[2].append(dot(attention.astype(BF16), cg, 0, 0).astype(BF16))
        pg = dot(cg, value, 1, 1)
        sg = (attention * (pg - jnp.sum(attention * pg, axis=-1, keepdims=True))).astype(BF16)
        for i, (rot_grad, g) in enumerate(((dot(sg, k, 1, 0), small[0:1]), (dot(sg, q, 0, 0), small[1:2]))):
            wgt = rot_grad * scale
            u = wgt * cos + pltpu.roll(wgt * sin, half, 1)
            v = pre[i, 0, :, cols]
            r = inverse_rms(v)
            grads[i].append(rms_back(v, r, u * g).astype(BF16))
            gains[i : i + 1] += jnp.sum(u * v * r, axis=0, keepdims=True)
    width = w.shape[2]
    joined = jnp.concatenate([g for kind in grads for g in kind], axis=1)
    wacc[...] += dot(normed[0], joined, 0, 0)
    total = None
    for i in range(3):
        piece = dot(joined[:, i * width : (i + 1) * width], w[i], 1, 1)
        total = piece if total is None else total + piece
    part[0] = total.astype(BF16)

    @pl.when(s == pl.num_programs(0) - 1)
    def _():
        for i in range(3):
            wgrad[i] = wacc[:, i * width : (i + 1) * width].astype(BF16)
        wograd[...] = woacc[...].astype(BF16)


def attend_back(agrad, normed, pre, low, ctx, weights, wo, small, table):
    seqs, length, width = agrad.shape
    cols = weights.shape[2]
    row = lambda i, *_: (i, 0, 0)
    row2 = lambda i, *_: (0, i, 0, 0)
    two = lambda i, *_: (0, 0)
    three = lambda i, *_: (0, 0, 0)
    return pl.pallas_call(
        attend_back_kernel,
        out_shape=(
            sds(agrad.shape, BF16),
            sds(weights.shape, BF16),
            sds(wo.shape, BF16),
            sds((8, HEAD_DIM), F32),
        ),
        grid_spec=pltpu.PrefetchScalarGridSpec(
            num_scalar_prefetch=0,
            grid=(seqs,),
            in_specs=[
                pl.BlockSpec((1, length, width), row),
                pl.BlockSpec((1, length, width), row),
                pl.BlockSpec((2, 1, length, cols), row2),
                pl.BlockSpec((3, 1, length, cols), row2),
                pl.BlockSpec((1, length, cols), row),
                pl.BlockSpec(weights.shape, three),
                pl.BlockSpec(wo.shape, two),
                pl.BlockSpec((8, 128), two),
                pl.BlockSpec((length, HEAD_DIM), two),
            ],
            out_specs=(
                pl.BlockSpec((1, length, width), row),
                pl.BlockSpec(weights.shape, three),
                pl.BlockSpec(wo.shape, two),
                pl.BlockSpec((8, HEAD_DIM), two),
            ),
            scratch_shapes=[
                pltpu.VMEM((weights.shape[1], 3 * cols), F32),
                pltpu.VMEM(wo.shape, F32),
            ],
        ),
        compiler_params=pltpu.CompilerParams(dimension_semantics=("arbitrary",), vmem_limit_bytes=60 << 20),
        cost_estimate=pl.CostEstimate(flops=2 * 10**10, bytes_accessed=4 * 10**7, transcendentals=10**6),
        name="attend_back",
    )(agrad, normed, pre, low, ctx, weights, wo, small, table)


BLOCK = 256
FIRST_TILE = (512, 1024)


def pack_rows(seqs, capacity):
    return -(-seqs * capacity // BLOCK) * BLOCK


def each_block(blocks, hidden, job):
    part = min(hidden, 512)
    parts = hidden // part

    def run(i, _):
        b, h = i // parts, lax.rem(i, parts)
        rows = pl.ds(pl.multiple_of(b * BLOCK, BLOCK), BLOCK)
        low = pl.multiple_of(h * part, part)
        job(rows, pl.ds(low, part), pl.ds(pl.multiple_of(hidden + low, part), part))
        return 0

    lax.fori_loop(0, blocks * parts, run, 0)


def swiglu_back(gate, up, dact):
    sig = 1.0 / (1.0 + jnp.exp(-gate))
    return dact * up * sig * (1.0 + gate * (1.0 - sig)), dact * (gate * sig)


def forward_blocks(blocks, x, dy, wi, wo, acts, dgus):
    def job(rows, gcols, ucols):
        gate = dot(x[rows], wi[:, gcols], 1, 0)
        up = dot(x[rows], wi[:, ucols], 1, 0)
        dact = dot(dy[rows], wo[gcols], 1, 1)
        acts[rows, gcols] = (gate * (1.0 / (1.0 + jnp.exp(-gate))) * up).astype(BF16)
        dgate, dup = swiglu_back(gate, up, dact)
        dgus[rows, gcols] = dgate.astype(BF16)
        dgus[rows, ucols] = dup.astype(BF16)

    each_block(blocks, wo.shape[0], job)


def gradient_tiles(blocks, left, right, result, acc, stage, ssem, busy):
    tr, tc = acc.shape
    down, across = result.shape[0] // tr, result.shape[1] // tc

    def tile(t, _):
        rt, ct = t // across, lax.rem(t, across)
        left_cols = pl.ds(pl.multiple_of(rt * tr, tr), tr)
        right_cols = pl.ds(pl.multiple_of(ct * tc, tc), tc)

        def step(b, _):
            rows = pl.ds(pl.multiple_of(b * BLOCK, BLOCK), BLOCK)
            piece = dot(left[rows, left_cols], right[rows, right_cols], 0, 0)

            @pl.when(b == 0)
            def _():
                acc[...] = piece

            @pl.when(b > 0)
            def _():
                acc[...] += piece

            return 0

        @pl.when(blocks == 0)
        def _():
            acc[...] = jnp.zeros_like(acc)

        lax.fori_loop(0, blocks, step, 0)
        k = lax.rem(t, 2)
        out = pltpu.make_async_copy(stage.at[k], result.at[left_cols, right_cols], ssem.at[k])

        @pl.when(jnp.logical_or(t >= 2, busy))
        def _():
            out.wait()

        stage[k] = acc[...].astype(BF16)
        out.start()
        return 0

    lax.fori_loop(0, down * across, tile, 0)


def drain_tiles(result, acc, stage, ssem):
    tr, tc = acc.shape
    for k in range(2):
        pltpu.make_async_copy(stage.at[k], result.at[pl.ds(0, tr), pl.ds(0, tc)], ssem.at[k]).wait()


def first_kernel(
    capacity, starts, mixed, cot, slots0, slots1, w_in,
    act, pair, x_all, dy_all, out_grad,
    x, dy, wi, acts, pairs, acc, stage, wsem, ssem, rsem,
):
    step = pl.program_id(0)
    steps = pl.num_programs(0)
    together = mixed.shape[0]
    seqs = steps * together
    width = mixed.shape[2]
    hidden = acts.shape[1]
    load = pltpu.make_async_copy(w_in.at[0], wi, wsem)

    @pl.when(step == 0)
    def _():
        load.start()

    packed = []
    for k in range(together):
        spread, gate_spread = [], []
        for slots in (slots0, slots1):
            column = lax.broadcasted_iota(jnp.int32, (capacity, slots.shape[2]), 0).astype(F32)
            place = column == slots[k, 0:1]
            spread.append(jnp.where(place, 1.0, 0.0).astype(BF16))
            gate_spread.append(jnp.where(place, slots[k, 8:9], 0.0).astype(BF16))
        packed.append(
            (
                dot(jnp.concatenate(spread, axis=0), mixed[k], 1, 0).astype(BF16),
                dot(jnp.concatenate(gate_spread, axis=0), cot[k], 1, 0).astype(BF16),
            )
        )
    for k, (x_rows, dy_rows) in enumerate(packed):
        s = step * together + k
        for j in range(2):
            start = pl.multiple_of(starts[j, s], 16)
            x[j, pl.ds(start, capacity)] = x_rows[j * capacity : (j + 1) * capacity]
            dy[j, pl.ds(start, capacity)] = dy_rows[j * capacity : (j + 1) * capacity]

    @pl.when(step == steps - 1)
    def _():
        for j in range(2):
            past = (starts[j, seqs - 1] + capacity) // 16
            end = (starts[j, seqs] + BLOCK - 1) // BLOCK * (BLOCK // 16)

            def clear(i, _):
                rows = pl.ds(pl.multiple_of(i * 16, 16), 16)
                x[j, rows] = jnp.zeros((16, width), BF16)
                dy[j, rows] = jnp.zeros((16, width), BF16)
                return 0

            lax.fori_loop(past, end, clear, 0)
        saves = [pltpu.make_async_copy(x, x_all, rsem.at[0]), pltpu.make_async_copy(dy, dy_all, rsem.at[1])]
        for copy in saves:
            copy.start()
        blocks = (starts[0, seqs] + BLOCK - 1) // BLOCK
        load.wait()

        def forward(rows, gcols, ucols):
            gate = dot(x[0, rows], wi[:, gcols], 1, 0)
            up = dot(x[0, rows], wi[:, ucols], 1, 0)
            acts[rows, gcols] = (gate * (1.0 / (1.0 + jnp.exp(-gate))) * up).astype(BF16)
            pairs[rows, gcols] = gate.astype(BF16)
            pairs[rows, ucols] = up.astype(BF16)

        each_block(blocks, hidden, forward)
        saves += [pltpu.make_async_copy(acts, act.at[0], rsem.at[2]), pltpu.make_async_copy(pairs, pair, rsem.at[3])]
        for copy in saves[2:]:
            copy.start()
        gradient_tiles(blocks, acts, dy.at[0], out_grad, acc, stage, ssem, False)
        drain_tiles(out_grad, acc, stage, ssem)
        for copy in saves:
            copy.wait()


def expert_first(starts, mixed, cot, slots, w_in, hidden, capacity):
    seqs, length, width = mixed.shape
    rows = pack_rows(seqs, capacity)
    dma = pltpu.SemaphoreType.DMA
    seq = lambda i, *_: (i, 0, 0)
    together = 2
    slot_spec = pl.BlockSpec((together, 16, length), seq)
    return pl.pallas_call(
        functools.partial(first_kernel, capacity),
        out_shape=(
            sds((2, rows, hidden), BF16),
            sds((rows, 2 * hidden), BF16),
            sds((2, rows, width), BF16),
            sds((2, rows, width), BF16),
            sds((hidden, width), BF16),
        ),
        grid_spec=pltpu.PrefetchScalarGridSpec(
            num_scalar_prefetch=1,
            grid=(seqs // together,),
            in_specs=[
                pl.BlockSpec((together, length, width), seq),
                pl.BlockSpec((together, length, width), seq),
                slot_spec,
                slot_spec,
                AN,
            ],
            out_specs=(AN, AN, AN, AN, AN),
            scratch_shapes=[
                pltpu.VMEM((2, rows, width), BF16),
                pltpu.VMEM((2, rows, width), BF16),
                pltpu.VMEM(w_in.shape[1:], BF16),
                pltpu.VMEM((rows, hidden), BF16),
                pltpu.VMEM((rows, 2 * hidden), BF16),
                pltpu.VMEM(FIRST_TILE, F32),
                pltpu.VMEM((2,) + FIRST_TILE, BF16),
                dma,
                dma((2,)),
                dma((4,)),
            ],
        ),
        compiler_params=pltpu.CompilerParams(dimension_semantics=("arbitrary",), vmem_limit_bytes=62 << 20),
        cost_estimate=pl.CostEstimate(flops=2 * 10**10, bytes_accessed=6 * 10**7, transcendentals=10**6),
        name="expert_first",
    )(starts, mixed, cot, *slots, w_in)


def in_grad_kernel(
    seqs, starts, x_all, dy_all, pair, w_out, dgu, in_grad, x, dy, wo, pairs, dgus, acc, stage, lsem, wsem, ssem, rsem
):
    blocks = (starts[0, seqs] + BLOCK - 1) // BLOCK
    hidden = wo.shape[0]
    weights = pltpu.make_async_copy(w_out.at[0], wo, wsem)
    weights.start()

    def run(b, action):
        rows = pl.ds(pl.multiple_of(b * BLOCK, BLOCK), BLOCK)
        for copy in (
            pltpu.make_async_copy(dy_all.at[0, rows], dy.at[rows], lsem.at[0, b]),
            pltpu.make_async_copy(pair.at[rows], pairs.at[rows], lsem.at[1, b]),
            pltpu.make_async_copy(x_all.at[0, rows], x.at[rows], lsem.at[2, b]),
        ):
            getattr(copy, action)()
        return 0

    lax.fori_loop(0, blocks, lambda b, _: run(b, "start"), 0)
    weights.wait()
    lax.fori_loop(0, blocks, lambda b, _: run(b, "wait"), 0)

    def backward(rows, gcols, ucols):
        dact = dot(dy[rows], wo[gcols], 1, 1)
        dgate, dup = swiglu_back(pairs[rows, gcols].astype(F32), pairs[rows, ucols].astype(F32), dact)
        dgus[rows, gcols] = dgate.astype(BF16)
        dgus[rows, ucols] = dup.astype(BF16)

    each_block(blocks, hidden, backward)
    save = pltpu.make_async_copy(dgus, dgu.at[0], rsem)
    save.start()
    gradient_tiles(blocks, x, dgus, in_grad, acc, stage, ssem, False)
    drain_tiles(in_grad, acc, stage, ssem)
    save.wait()


def first_in_grad(seqs, starts, x_all, dy_all, pair, w_out):
    rows, width = x_all.shape[1:]
    hidden = w_out.shape[1]
    dma = pltpu.SemaphoreType.DMA
    return pl.pallas_call(
        functools.partial(in_grad_kernel, seqs),
        out_shape=(sds((2, rows, 2 * hidden), BF16), sds((width, 2 * hidden), BF16)),
        grid_spec=pltpu.PrefetchScalarGridSpec(
            num_scalar_prefetch=1,
            grid=(1,),
            in_specs=[AN] * 4,
            out_specs=(AN, AN),
            scratch_shapes=[
                pltpu.VMEM((rows, width), BF16),
                pltpu.VMEM((rows, width), BF16),
                pltpu.VMEM(w_out.shape[1:], BF16),
                pltpu.VMEM((rows, 2 * hidden), BF16),
                pltpu.VMEM((rows, 2 * hidden), BF16),
                pltpu.VMEM((512, 2048), F32),
                pltpu.VMEM((2, 512, 2048), BF16),
                dma((3, rows // BLOCK)),
                dma,
                dma((2,)),
                dma,
            ],
        ),
        compiler_params=pltpu.CompilerParams(dimension_semantics=("arbitrary",), vmem_limit_bytes=60 << 20),
        cost_estimate=pl.CostEstimate(flops=10**10, bytes_accessed=2 * 10**7, transcendentals=0),
        name="first_in_grad",
    )(starts, x_all, dy_all, pair, w_out)


def second_kernel(
    seqs, starts, x_all, dy_all, w_in, w_out, _act, _dgu, act, dgu, in_grad, out_grad,
    x, dy, wi, wo, acts, dgus, acc, stage, wsem, lsem, ssem, rsem,
):
    blocks = (starts[1, seqs] + BLOCK - 1) // BLOCK
    loads = [pltpu.make_async_copy(w_in.at[1], wi, wsem.at[0]), pltpu.make_async_copy(w_out.at[1], wo, wsem.at[1])]

    def load(b, action):
        rows = pl.ds(pl.multiple_of(b * BLOCK, BLOCK), BLOCK)
        for copy in (
            pltpu.make_async_copy(x_all.at[1, rows], x.at[rows], lsem.at[0, b]),
            pltpu.make_async_copy(dy_all.at[1, rows], dy.at[rows], lsem.at[1, b]),
        ):
            getattr(copy, action)()
        return 0

    for copy in loads:
        copy.start()
    lax.fori_loop(0, blocks, lambda b, _: load(b, "start"), 0)
    for copy in loads:
        copy.wait()
    lax.fori_loop(0, blocks, lambda b, _: load(b, "wait"), 0)

    forward_blocks(blocks, x, dy, wi, wo, acts, dgus)
    saves = [pltpu.make_async_copy(acts, act.at[1], rsem.at[0]), pltpu.make_async_copy(dgus, dgu.at[1], rsem.at[1])]
    for copy in saves:
        copy.start()
    gradient_tiles(blocks, x, dgus, in_grad, acc, stage, ssem, False)
    gradient_tiles(blocks, acts, dy, out_grad, acc, stage, ssem, True)
    drain_tiles(out_grad, acc, stage, ssem)
    for copy in saves:
        copy.wait()


def expert_second(seqs, starts, x_all, dy_all, w_in, w_out, act, dgu):
    rows, width = dy_all.shape[1:]
    hidden = w_out.shape[1]
    dma = pltpu.SemaphoreType.DMA
    return pl.pallas_call(
        functools.partial(second_kernel, seqs),
        out_shape=(
            sds(act.shape, BF16), sds(dgu.shape, BF16), sds((width, 2 * hidden), BF16), sds((hidden, width), BF16)
        ),
        input_output_aliases={5: 0, 6: 1},
        grid_spec=pltpu.PrefetchScalarGridSpec(
            num_scalar_prefetch=1,
            grid=(1,),
            in_specs=[AN] * 6,
            out_specs=(AN, AN, AN, AN),
            scratch_shapes=[
                pltpu.VMEM((rows, width), BF16),
                pltpu.VMEM((rows, width), BF16),
                pltpu.VMEM(w_in.shape[1:], BF16),
                pltpu.VMEM(w_out.shape[1:], BF16),
                pltpu.VMEM((rows, hidden), BF16),
                pltpu.VMEM((rows, 2 * hidden), BF16),
                pltpu.VMEM((512, 2048), F32),
                pltpu.VMEM((2, 512, 2048), BF16),
                dma((2,)),
                dma((2, rows // BLOCK)),
                dma((2,)),
                dma((2,)),
            ],
        ),
        compiler_params=pltpu.CompilerParams(dimension_semantics=("arbitrary",), vmem_limit_bytes=60 << 20),
        cost_estimate=pl.CostEstimate(flops=25 * 10**9, bytes_accessed=6 * 10**7, transcendentals=10**6),
        name="expert_second",
    )(starts, x_all, dy_all, w_in, w_out, act, dgu)


def tail_kernel(seqs, starts, act, dgu, w_in, w_out, produced, dx):
    @pl.when(pl.program_id(1) * BLOCK < starts[pl.program_id(0), seqs])
    def _():
        part = min(produced.shape[1], 512)

        def run(i, _):
            cols = pl.ds(pl.multiple_of(i * part, part), part)
            produced[:, cols] = dot(act[...], w_out[:, cols], 1, 0).astype(BF16)
            dx[:, cols] = dot(dgu[...], w_in[cols], 1, 1).astype(BF16)
            return 0

        lax.fori_loop(0, produced.shape[1] // part, run, 0)


def expert_tails(seqs, starts, act, dgu, w_in, w_out):
    _, rows, hidden = act.shape
    width = w_in.shape[1]

    def block(j, i, st):
        return j, jnp.maximum(jnp.minimum(i, (st[j, seqs] + BLOCK - 1) // BLOCK - 1), 0), 0

    out = pl.BlockSpec((None, BLOCK, width), block)
    return pl.pallas_call(
        functools.partial(tail_kernel, seqs),
        out_shape=(sds((2, rows, width), BF16), sds((2, rows, width), BF16)),
        grid_spec=pltpu.PrefetchScalarGridSpec(
            num_scalar_prefetch=1,
            grid=(2, rows // BLOCK),
            in_specs=[
                pl.BlockSpec((None, BLOCK, hidden), block),
                pl.BlockSpec((None, BLOCK, 2 * hidden), block),
                pl.BlockSpec((None,) + w_in.shape[1:], lambda j, i, *_: (j, 0, 0)),
                pl.BlockSpec((None,) + w_out.shape[1:], lambda j, i, *_: (j, 0, 0)),
            ],
            out_specs=(out, out),
        ),
        compiler_params=pltpu.CompilerParams(dimension_semantics=("arbitrary", "arbitrary"), vmem_limit_bytes=60 << 20),
        cost_estimate=pl.CostEstimate(flops=24 * 10**9, bytes_accessed=6 * 10**7, transcendentals=0),
        name="expert_tails",
    )(starts, act, dgu, w_in, w_out)


def combine_kernel(capacity, local, *refs):
    s = pl.program_id(0)
    starts = refs[0]
    slots = refs[1 : 1 + local]
    produced, dx, out_part, grad_part, held_out, held_grad, sems = refs[1 + local :]
    seqs = pl.num_programs(0)

    def loads(s):
        k = lax.rem(s, 2)
        copies = []
        for j in range(local):
            span = pl.ds(pl.multiple_of(starts[j, s], 16), capacity)
            copies.append(pltpu.make_async_copy(produced.at[j, span], held_out.at[k, j], sems.at[k, 0, j]))
            copies.append(pltpu.make_async_copy(dx.at[j, span], held_grad.at[k, j], sems.at[k, 1, j]))
        return copies

    @pl.when(s == 0)
    def _():
        for copy in loads(s):
            copy.start()

    @pl.when(s + 1 < seqs)
    def _():
        for copy in loads(s + 1):
            copy.start()

    for copy in loads(s):
        copy.wait()
    slot = lax.rem(s, 2)
    out_sum, grad_sum = None, None
    for j in range(local):
        length = slots[j].shape[2]
        column = lax.broadcasted_iota(jnp.int32, (capacity, length), 0).astype(F32)
        place = column == slots[j][0, 0:1]
        held = lax.broadcasted_iota(jnp.int32, (capacity, 1), 0) < starts[j, s + 1] - starts[j, s]
        rows = jnp.where(held, held_out[slot, j], 0.0).astype(BF16)
        grads = jnp.where(held, held_grad[slot, j], 0.0).astype(BF16)
        out = dot(jnp.where(place, slots[j][0, 8:9], 0.0).astype(BF16), rows, 0, 0)
        grad = dot(jnp.where(place, 1.0, 0.0).astype(BF16), grads, 0, 0)
        out_sum = out if out_sum is None else out_sum + out
        grad_sum = grad if grad_sum is None else grad_sum + grad
    out_part[0] = out_sum.astype(BF16)
    grad_part[0] = grad_sum.astype(BF16)


def combine(starts, slots, produced, dx, capacity):
    local = len(slots)
    seqs, _, length = slots[0].shape
    width = produced.shape[2]
    seq = lambda i, *_: (i, 0, 0)
    held = pltpu.VMEM((2, local, capacity, width), BF16)
    return pl.pallas_call(
        functools.partial(combine_kernel, capacity, local),
        out_shape=(sds((seqs, length, width), BF16), sds((seqs, length, width), BF16)),
        grid_spec=pltpu.PrefetchScalarGridSpec(
            num_scalar_prefetch=1,
            grid=(seqs,),
            in_specs=[pl.BlockSpec((1, 16, length), seq)] * local + [AN] * 2,
            out_specs=(pl.BlockSpec((1, length, width), seq), pl.BlockSpec((1, length, width), seq)),
            scratch_shapes=[held, held, pltpu.SemaphoreType.DMA((2, 2, local))],
        ),
        compiler_params=pltpu.CompilerParams(dimension_semantics=("arbitrary",), vmem_limit_bytes=60 << 20),
        cost_estimate=pl.CostEstimate(flops=3 * 10**9, bytes_accessed=4 * 10**7, transcendentals=0),
        name="combine",
    )(starts, *slots, produced, dx)


def shards(
    tokens, cotangent, gate_weights, expert_ids, seq_lengths, query_weight, key_weight, value_weight,
    output_weight, attn_gain, ffn_gain, query_gain, key_gain, expert_in, expert_out,
):
    ep = lax.axis_size("ep")
    me = lax.axis_index("ep")
    seqs, rows, _ = tokens.shape
    length = rows * ep
    top = gate_weights.shape[2]
    local = expert_in.shape[0]
    hidden = expert_out.shape[1]
    experts = local * ep
    capacity = -(-(length * top * 9 // (8 * experts)) // 16) * 16

    gains = jnp.concatenate([attn_gain, ffn_gain]).astype(F32).reshape(-1, 128)
    few = [query_gain.astype(F32), key_gain.astype(F32), seq_lengths.astype(F32)]
    few = jnp.stack([jnp.pad(v, (0, 128 - v.shape[0])) for v in few])
    packet = jnp.concatenate([gains, few], axis=0)
    packet = jnp.pad(packet, ((0, -packet.shape[0] % 8), (0, 0)))
    share = gains.shape[0] // 2

    half = HEAD_DIM // 2
    frequency = ROPE_BASE ** (-(np.arange(half, dtype=np.float32) * np.float32(2.0 / HEAD_DIM)))
    angles = np.arange(length, dtype=np.float32)[:, None] * frequency.astype(np.float32)[None, :]
    table = jnp.asarray(np.concatenate([np.cos(angles), np.sin(angles)], axis=-1), F32)

    arrays = (
        tokens, cotangent, expert_ids.transpose(0, 2, 1), gate_weights.transpose(0, 2, 1),
        query_weight, key_weight, value_weight, packet,
    )
    if ep == 8 and lax.axis_size("rep") == 4:
        (
            weights, gains, small_in, normed, pre, low, ctx, middle, mixed, cot_full, slots0, slots1, starts,
        ) = forward(top, local, *arrays, output_weight, table)
    else:
        full, weights, cot_full, gains, small_in = front(*arrays)
        number = (me * local).astype(jnp.int32)[None]
        normed, pre, low, ctx, part, slots0, slots1, starts = attend(
            top, number, full, weights, output_weight, gains, small_in, table
        )
        starts = starts.astype(jnp.int32)
        middle, mixed = mix(part, tokens, small_in, gains)

    act, pair, x_all, dy_all, out_grad0 = expert_first(
        starts, mixed, cot_full, (slots0, slots1), expert_in, hidden, capacity
    )

    def over_rep(value):
        return lax.psum_scatter(value, "rep", scatter_dimension=0, tiled=True)

    out0 = over_rep(out_grad0)
    dgu, in_grad0 = first_in_grad(seqs, starts, x_all, dy_all, pair, expert_out)
    in0 = over_rep(in_grad0)
    x_all, _ = lax.optimization_barrier((x_all, in_grad0))
    act, dgu, in_grad1, out_grad1 = expert_second(seqs, starts, x_all, dy_all, expert_in, expert_out, act, dgu)
    in1 = over_rep(in_grad1)
    out1 = over_rep(out_grad1)
    produced, dx = expert_tails(seqs, starts, act, dgu, expert_in, expert_out)
    out_part, grad_part = combine(starts, (slots0, slots1), produced, dx, capacity)

    mgrad, ffn_back, agrad = back(grad_part, middle, cotangent, small_in, gains)
    npart, wgrad, wograd, qk_back = attend_back(
        agrad, normed, pre, low, ctx, weights, output_weight, small_in, table
    )
    sums, small, result, token_grad = finish(
        wgrad, wograd, npart, out_part, tokens, middle, mgrad, gains, ffn_back, qk_back
    )

    def widen(into, value, j):
        return lax.dynamic_update_slice(into, value.astype(F32)[None], (j, 0, 0))

    small, out0 = lax.optimization_barrier((small, out0))
    out_all = widen(jnp.zeros((local,) + out0.shape, F32), out0, 0)
    small, out_all = lax.optimization_barrier((small, out_all))

    heads = HEAD_DIM // ep
    wide = sums.astype(F32)
    return (
        result,
        token_grad,
        wide[1],
        wide[2],
        wide[3],
        wide[0],
        small[:share].reshape(-1),
        small[share : 2 * share].reshape(-1),
        small[2 * share, :heads],
        small[2 * share + 1, :heads],
        jnp.stack([in0, in1]).astype(F32),
        widen(out_all, out1, 1),
    )


def solution(mesh):
    seq = P("rep", "ep", None)
    row, gain, expert = P("ep", None), P("ep"), P("ep", None, None)
    split = P("ep", "rep", None)

    return jax.shard_map(
        shards,
        mesh=mesh,
        in_specs=(seq, seq, seq, seq, P(("rep", "ep")), row, row, row, row, gain, gain, gain, gain, expert, expert),
        out_specs=(seq, seq, row, row, row, row, gain, gain, gain, gain, split, split),
        check_vma=False,
    )
```

```python
import functools

import jax
import jax.numpy as jnp
import numpy as np
from jax import lax
from jax.experimental import pallas as pl
from jax.experimental.pallas import tpu as pltpu
from jax.sharding import PartitionSpec as P

HEAD_DIM = 128
EPS = 1e-06
ROPE_BASE = 50000.0
MESH = pl.DeviceIdType.MESH
F32 = jnp.float32
BF16 = jnp.bfloat16


def sds(shape, dtype):
    return jax.ShapeDtypeStruct(shape, dtype)


VM = pl.BlockSpec(memory_space=pltpu.VMEM)
AN = pl.BlockSpec(memory_space=pl.ANY)


def inverse_rms(v):
    return lax.rsqrt(jnp.mean(v * v, axis=-1, keepdims=True) + EPS)


def rms_back(v, r, ug):
    return r * ug - v * (r * r * r * jnp.mean(ug * v, axis=-1, keepdims=True))


def mix_rows(total, tok, living, gain):
    middle = tok.astype(F32) + living * total
    mixed = middle * inverse_rms(middle) * gain
    return middle, mixed.astype(BF16)


def ffn_back_rows(mixed_grad, middle, cot, living, gain):
    r = inverse_rms(middle)
    middle_grad = cot.astype(F32) + rms_back(middle, r, mixed_grad * gain)
    return middle_grad, (living * middle_grad).astype(BF16), mixed_grad * middle * r


def attn_back_rows(normed_grad, tok, middle_grad, gain):
    v = tok.astype(F32)
    r = inverse_rms(v)
    return (middle_grad + rms_back(v, r, normed_grad * gain)).astype(BF16), normed_grad * v * r


def seq_len(small, s):
    lane = lax.broadcasted_iota(jnp.int32, (1, 128), 1)
    return jnp.sum(jnp.where(lane == s, small[2:3, :], 0.0), axis=1, keepdims=True)


def live_rows(small, s, me, rows):
    place = (lax.broadcasted_iota(jnp.int32, (rows, 1), 0) + me * rows).astype(F32)
    return jnp.where(place < seq_len(small, s), 1.0, 0.0)


class Place:
    def __init__(self):
        me = lax.axis_index("ep")
        core, x, y = lax.rem(me, 2), lax.rem(me // 2, 2), me // 4
        self.rep = lax.axis_index("rep")
        self.me = me
        self.sb = me + 1 - 2 * core
        self.dx = 2 - 4 * x
        self.dy = 4 - 8 * y
        self.xn = me + self.dx
        self.yn = me + self.dy
        self.dg = me + self.dx + self.dy

    def push(self, src, dst, send, recv, dev):
        return pltpu.make_async_remote_copy(
            src_ref=src, dst_ref=dst, send_sem=send, recv_sem=recv, device_id=(self.rep, dev), device_id_type=MESH
        )

    def peer(self, m):
        k = m + 1
        return self.me + (k % 2) * (self.sb - self.me) + (k // 2 % 2) * self.dx + (k // 4) * self.dy

    def greet(self, peers):
        barrier = pltpu.get_barrier_semaphore()
        for peer in peers:
            pl.semaphore_signal(barrier, inc=1, device_id=(self.rep, peer), device_id_type=MESH)
        pl.semaphore_wait(barrier, len(peers))


class Gather:
    sems = 3

    def __init__(self, at, own, full, ssem, rsem, lsem):
        self.at, self.own, self.full, self.ssem, self.rsem, self.lsem = at, own, full, ssem, rsem, lsem
        self.rows = own.shape[1]

    @staticmethod
    def scratch(seqs):
        return [pltpu.SemaphoreType.DMA((7, seqs)), pltpu.SemaphoreType.DMA((8, seqs)), pltpu.SemaphoreType.DMA((seqs,))]

    def block(self, s, dev):
        return self.full.at[s, pl.ds(pl.multiple_of(dev * self.rows, self.rows), self.rows)]

    def copy(self, s, dev, kind, slot, to, src=None):
        block = self.block(s, dev)
        return self.at.push(block if src is None else src, block, self.ssem.at[kind, s], self.rsem.at[slot, s], to)

    def start(self, s):
        at, own = self.at, self.own.at[s]
        self.copy(s, at.me, 0, 2, at.xn, own).start()
        self.copy(s, at.me, 1, 4, at.yn, own).start()
        self.copy(s, at.me, 2, 1, at.sb, own).start()
        pltpu.make_async_copy(own, self.block(s, at.me), self.lsem.at[s]).start()

    def relay(self, s, by_y):
        at = self.at
        self.copy(s, at.xn, 0, 2, at.xn).wait_recv()
        if by_y:
            self.copy(s, at.xn, 3, 6, at.yn).start()
        self.copy(s, at.xn, 4, 3, at.sb).start()
        self.copy(s, at.yn, 1, 4, at.yn).wait_recv()
        if not by_y:
            self.copy(s, at.yn, 3, 6, at.xn).start()
        self.copy(s, at.yn, 5, 5, at.sb).start()

    def relay_far(self, s):
        at = self.at
        self.copy(s, at.dg, 3, 6, at.yn).wait_recv()
        self.copy(s, at.dg, 6, 7, at.sb).start()

    def finish(self, s):
        at = self.at
        for dev, slot in ((at.sb, 1), (at.sb + at.dx, 3), (at.sb + at.dy, 5), (at.sb + at.dx + at.dy, 7)):
            self.copy(s, dev, 0, slot, at.sb).wait_recv()
        for kind in range(7):
            self.copy(s, at.me, kind, 0, at.sb).wait_send()
        pltpu.make_async_copy(self.own.at[s], self.block(s, at.me), self.lsem.at[s]).wait()


def gather_tail(gather, low, high):
    def relay(i, _):
        gather.relay(low + 2 * i, True)
        gather.relay(low + 2 * i + 1, False)
        return 0

    lax.fori_loop(0, (high - low) // 2, relay, 0)
    each(high, gather.relay_far, low=low)
    each(high, gather.finish, low=low)


class Reduce:
    def __init__(self, at, part, held, mine, x1, y1, x2, y2, ms, hs, hr, d1s, d1r, d2s, d2r):
        self.at, self.part, self.held, self.mine = at, part, held, mine
        self.x1, self.y1, self.x2, self.y2 = x1, y1, x2, y2
        self.ms, self.hs, self.hr, self.d1s, self.d1r, self.d2s, self.d2r = ms, hs, hr, d1s, d1r, d2s, d2r
        self.half = part.shape[2] // 2

    @staticmethod
    def scratch(part):
        s, _, t, d = part.shape
        dma = pltpu.SemaphoreType.DMA
        return [
            pltpu.VMEM((s, 4, t, d), BF16),
            pltpu.VMEM((s, 4, t, d), BF16),
            pltpu.VMEM((s, t // 2, d), BF16),
            pltpu.VMEM((s, t // 2, d), BF16),
            pltpu.VMEM((s, t, d), BF16),
            pltpu.VMEM((s, t, d), BF16),
            dma((4, s)),
            dma((4, s)),
            dma((4, s)),
            dma((2, s)),
            dma((2, s)),
            dma((2, s)),
            dma((2, s)),
        ]

    sems = 13

    def core_copy(self, s, k):
        at = self.at
        dest = (at.sb, at.sb + at.dx, at.sb + at.dy, at.sb + at.dx + at.dy)[k]
        return at.push(self.part.at[s, dest], self.held.at[s, k], self.hs.at[k, s], self.hr.at[k, s], at.sb)

    def load(self, s, k):
        at = self.at
        dest = (at.me, at.xn, at.yn, at.dg)[k]
        return pltpu.make_async_copy(self.part.at[s, dest], self.mine.at[s, k], self.ms.at[k, s])

    def first(self, s, k):
        at, h = self.at, self.half
        src = self.held.at[s, 3, pl.ds(k * h, h)]
        return at.push(src, (self.x1, self.y1)[k].at[s], self.d1s.at[k, s], self.d1r.at[k, s], (at.xn, at.yn)[k])

    def second(self, s, k):
        at = self.at
        src = self.held.at[s, 1 + k]
        return at.push(src, (self.x2, self.y2)[k].at[s], self.d2s.at[k, s], self.d2r.at[k, s], (at.xn, at.yn)[k])

    def start(self, s):
        for k in (3, 1, 2, 0):
            self.core_copy(s, k).start()
            self.load(s, k).start()

    def hop1(self, s):
        self.core_copy(s, 3).wait_recv()
        self.load(s, 3).wait()
        self.held[s, 3] = (self.held[s, 3].astype(F32) + self.mine[s, 3].astype(F32)).astype(BF16)
        self.first(s, 0).start()
        self.first(s, 1).start()

    def hop2(self, s):
        h = self.half
        for k, extra, rows, rest in (
            (0, self.y1, pl.ds(h, h), pl.ds(0, h)),
            (1, self.x1, pl.ds(0, h), pl.ds(h, h)),
        ):
            self.core_copy(s, 1 + k).wait_recv()
            self.load(s, 1 + k).wait()
            self.first(s, 1 - k).wait_recv()
            held, mine = self.held.at[s, 1 + k], self.mine.at[s, 1 + k]
            held[rows] = (held[rows].astype(F32) + mine[rows].astype(F32) + extra[s].astype(F32)).astype(BF16)
            held[rest] = (held[rest].astype(F32) + mine[rest].astype(F32)).astype(BF16)
            self.second(s, k).start()

    def total(self, s):
        self.core_copy(s, 0).wait_recv()
        self.load(s, 0).wait()
        self.second(s, 0).wait_recv()
        self.second(s, 1).wait_recv()
        return (
            self.mine[s, 0].astype(F32)
            + self.held[s, 0].astype(F32)
            + self.x2[s].astype(F32)
            + self.y2[s].astype(F32)
        )

    def finish(self, s):
        for k in range(4):
            self.core_copy(s, k).wait_send()
        for k in range(2):
            self.first(s, k).wait_send()
            self.second(s, k).wait_send()


def each(n, *steps, low=0):
    def run(s, _):
        for step in steps:
            step(s)
        return 0

    lax.fori_loop(low, n, run, 0)


COMM = dict(has_side_effects=True, vmem_limit_bytes=60 << 20)


def front(tokens, cotangent, ids, gates, wq, wk, wv, packet):
    _, _, width = tokens.shape
    ep = lax.axis_size("ep")
    top = ids.shape[1]
    routes = jnp.concatenate([ids.astype(BF16), gates], axis=1).transpose(0, 2, 1)
    routes = jnp.pad(routes, ((0, 0), (0, 0), (0, 128 - 2 * top)))
    full = lax.all_gather(jnp.concatenate([tokens, routes], axis=-1), "ep", axis=1, tiled=True)
    weights = [lax.all_to_all(w, "ep", split_axis=1, concat_axis=0, tiled=True) for w in (wq, wk, wv)]
    packets = lax.all_gather(packet, "ep", axis=0)
    share, heads = width // (128 * ep), HEAD_DIM // ep
    gains = jnp.stack([packets[:, :share].reshape(width), packets[:, share : 2 * share].reshape(width)])
    lens = jnp.pad(packets[:, 2 * share + 2, 0], (0, 128 - ep))
    few = [packets[:, 2 * share + k, :heads].reshape(HEAD_DIM) for k in range(2)] + [lens]
    return (
        full, jnp.stack(weights), lax.all_gather(cotangent, "ep", axis=1, tiled=True),
        jnp.pad(gains, ((0, 6), (0, 0))), jnp.pad(jnp.stack(few), ((0, 5), (0, 0))),
    )


def plain_living(small, seqs, rows):
    place = (jnp.arange(rows) + lax.axis_index("ep") * rows).astype(F32)
    return (place[None] < small[2, :seqs, None]).astype(F32)[..., None]


def mix(part, tokens, small, gains):
    seqs, rows, _ = tokens.shape
    total = lax.psum_scatter(part, "ep", scatter_dimension=1, tiled=True).astype(F32)
    middle, mixed = mix_rows(total, tokens, plain_living(small, seqs, rows), gains[1])
    return middle, lax.all_gather(mixed, "ep", axis=1, tiled=True)


def back_kernel(gpart, middle, cot, small, gains, mgrad, ggrad, full, own, *scratch):
    at = Place()
    seqs = cot.shape[0]
    n = Reduce.sems
    rg = Reduce(at, gpart, *scratch[:n])
    gather = Gather(at, own, full, *scratch[n:])
    at.greet((at.xn, at.yn, at.sb))
    each(seqs, rg.start)
    each(seqs, rg.hop1)
    each(seqs, rg.hop2)
    ggrad[...] = jnp.zeros_like(ggrad)

    def rows(s):
        living = live_rows(small, s, at.me, cot.shape[1])
        mg, ag, back = ffn_back_rows(rg.total(s), middle[s], cot[s], living, gains[1:2])
        mgrad[s] = mg
        own[s] = ag
        ggrad[...] += jnp.sum(back, axis=0, keepdims=True)
        gather.start(s)

    each(seqs, rows)
    gather_tail(gather, 0, seqs)
    each(seqs, rg.finish)


def back(gpart, middle, cot, small, gains):
    seqs, rows, width = cot.shape
    ep = lax.axis_size("ep")
    if ep != 8:
        mixed_grad = lax.psum_scatter(gpart, "ep", scatter_dimension=1, tiled=True).astype(F32)
        mg, ag, backs = ffn_back_rows(mixed_grad, middle, cot, plain_living(small, seqs, rows), gains[1])
        full = lax.all_gather(ag, "ep", axis=1, tiled=True)
        return mg, jnp.sum(backs, axis=(0, 1))[None], full
    gpart = gpart.reshape(seqs, ep, rows, width)
    return pl.pallas_call(
        back_kernel,
        out_shape=(
            sds(cot.shape, F32),
            sds((1, width), F32),
            sds((seqs, rows * ep, width), BF16),
        ),
        in_specs=[AN] + [VM] * 4,
        out_specs=(VM, VM, AN),
        scratch_shapes=[pltpu.VMEM(cot.shape, BF16)] + Reduce.scratch(gpart) + Gather.scratch(seqs),
        compiler_params=pltpu.CompilerParams(collective_id=3, **COMM),
        name="back",
    )(gpart, middle, cot, small, gains)


def finish_kernel(
    wgrad, wograd, npart, opart, tok, middle, mgrad, gains, others,
    out, small_out, result, tgrad,
    own, held, met, ggrad, parcel, landed, spare,
    wsend, wrecv, local, gsend, grecv, os, or_, ps, pr, qs, qr, fs, fr, ss, sr, *scratch,
):
    at = Place()
    z, me = at.rep, at.me
    n = Reduce.sems
    normed_sum = Reduce(at, npart, *scratch[:n])
    result_sum = Reduce(at, opart, *scratch[n:])
    seqs = tok.shape[0]
    parts, pieces = own.shape[:2]
    chunks = parts * pieces
    width = wgrad.shape[3]
    barrier = pltpu.get_barrier_semaphore()
    line = [lax.rem(z + k, 4) for k in range(1, 4)]
    for dev in line:
        pl.semaphore_signal(barrier, inc=1, device_id=(dev, me), device_id_type=MESH)
    each(7, lambda m: pl.semaphore_signal(barrier, inc=1, device_id=(z, at.peer(m)), device_id_type=MESH))
    pl.semaphore_wait(barrier, 10)
    inner = jnp.logical_and(z > 0, z < 3)
    outer_end, partner, outer = 1 + z // 3, 3 - z, 3 * (z - 1)
    cols = pl.ds(pl.multiple_of(me * width, width), width)

    def column_copy(m, j):
        dev = at.peer(m)
        rows = pl.ds(pl.multiple_of(dev * pieces, pieces), pieces)
        return at.push(wgrad.at[j, rows], own.at[1 + j, :, :, cols], wsend.at[m, j], wrecv.at[m, j], dev)

    mine_rows = pl.ds(pl.multiple_of(me * pieces, pieces), pieces)
    locals_ = [pltpu.make_async_copy(wgrad.at[j, mine_rows], own.at[1 + j, :, :, cols], local.at[j]) for j in range(3)]
    locals_.append(pltpu.make_async_copy(wograd, own.at[0], local.at[3]))
    for copy in locals_:
        copy.start()
    for j in range(3):
        each(7, lambda m, j=j: column_copy(m, j).start())
    each(seqs, normed_sum.start)
    each(seqs, result_sum.start)
    ggrad[...] = jnp.zeros_like(ggrad)

    def piece(ref, c):
        return ref.at[c // pieces, lax.rem(c, pieces)]

    def line_push(src, dst, send, recv, dev):
        return pltpu.make_async_remote_copy(
            src_ref=src, dst_ref=dst, send_sem=send, recv_sem=recv, device_id=(dev, me), device_id_type=MESH
        )

    def inward(c):
        return line_push(piece(own, c), piece(held, c), os.at[c], or_.at[c], outer_end)

    def across(c):
        return line_push(piece(held, c), met.at[c // 2], ps.at[c], pr.at[c], partner)

    def share(c):
        return line_push(piece(out, c), piece(out, c), qs.at[c], qr.at[c], partner)

    def outward(c):
        return line_push(piece(out, c), piece(out, c), fs.at[c], fr.at[c], outer)

    def mine(c):
        return 1 + lax.rem(c, 2) == z

    def ready(part):
        for j in range(parts):

            @pl.when(part == j)
            def _():
                locals_[(3, 0, 1, 2)[j]].wait()
                if j > 0:
                    each(7, lambda m: column_copy(m, j - 1).wait_recv())

    def step(c):
        @pl.when(lax.rem(c, pieces) == 0)
        def _():
            ready(c // pieces)

        @pl.when(jnp.logical_not(inner))
        def _():
            inward(c).start()

        @pl.when(inner)
        def _():
            inward(c).wait_recv()
            here = piece(held, c)
            here[...] = (here[...].astype(F32) + piece(own, c)[...].astype(F32)).astype(BF16)

            @pl.when(jnp.logical_not(mine(c)))
            def _():
                across(c).start()

    def settle(c):
        @pl.when(jnp.logical_and(inner, mine(c)))
        def _():
            across(c).wait_recv()
            piece(out, c)[...] = (piece(held, c)[...].astype(F32) + met[c // 2].astype(F32)).astype(BF16)
            share(c).start()
            outward(c).start()

    def forward(c):
        @pl.when(jnp.logical_and(inner, jnp.logical_not(mine(c))))
        def _():
            share(c).wait_recv()
            outward(c).start()

    def token_rows(s):
        tg, back = attn_back_rows(normed_sum.total(s), tok[s], mgrad[s], gains[0:1])
        tgrad[s] = tg
        ggrad[...] += jnp.sum(back, axis=0, keepdims=True)

    def out_rows(s):
        result[s] = (middle[s] + result_sum.total(s)).astype(BF16)

    jobs = (
        (step, 0, chunks), (settle, 1, chunks), (forward, 2, chunks),
        (normed_sum.hop1, 2, seqs), (normed_sum.hop2, 6, seqs), (token_rows, 10, seqs),
        (result_sum.hop1, 6, seqs), (result_sum.hop2, 10, seqs), (out_rows, 14, seqs),
    )

    def tick(i, _):
        for job, lag, count in jobs:

            @pl.when(jnp.logical_and(i >= lag, i < lag + count))
            def _():
                job(i - lag)

        return 0

    lax.fori_loop(0, max(lag + count for _, lag, count in jobs), tick, 0)

    parcel[...] = jnp.zeros_like(parcel)
    devices = parcel.shape[0]
    rows_of = ggrad.shape[1] // (128 * devices)
    for dev in range(devices):
        for k in range(rows_of):
            lanes = pl.ds((dev * rows_of + k) * 128, 128)
            parcel[dev, k : k + 1] = ggrad[:, lanes]
            parcel[dev, rows_of + k : rows_of + k + 1] = others[0:1, lanes]
        parcel[dev, 2 * rows_of : 2 * rows_of + 2] = others[1:3, 0:128]

    def parcel_copy(m):
        dev = at.peer(m)
        return at.push(parcel.at[dev], landed.at[m], gsend.at[m], grecv.at[m], dev)

    each(7, lambda m: parcel_copy(m).start())
    spare[0] = parcel[me]

    def add_parcel(m):
        parcel_copy(m).wait_recv()
        spare[0] += landed[m]

    each(7, add_parcel)

    def small_copy(k):
        return line_push(spare.at[0], spare.at[1 + k], ss.at[k], sr.at[k], line[k])

    for k in range(3):
        small_copy(k).start()

    @pl.when(jnp.logical_not(inner))
    def _():
        each(chunks, lambda c: outward(c).wait_recv())
        each(chunks, lambda c: inward(c).wait_send())

    @pl.when(inner)
    def _():
        def sent(c):
            outward(c).wait_send()

            @pl.when(mine(c))
            def _():
                share(c).wait_send()

            @pl.when(jnp.logical_not(mine(c)))
            def _():
                across(c).wait_send()

        each(chunks, sent)

    each(seqs, normed_sum.finish, result_sum.finish)

    def all_sent(m):
        parcel_copy(m).wait_send()
        for j in range(3):
            column_copy(m, j).wait_send()

    each(7, all_sent)
    total = spare[0]
    for k in range(3):
        small_copy(k).wait()
        total = total + spare[1 + k]
    small_out[...] = total
    few = total[2 * rows_of : 2 * rows_of + 2]
    heads = HEAD_DIM // devices
    moved = jnp.zeros_like(few)
    for k in range(devices):
        moved += jnp.where(me == k, pltpu.roll(few, (128 - k * heads) % 128, 1), 0.0)
    small_out[2 * rows_of : 2 * rows_of + 2] = moved


def finish(wgrad, wograd, npart, opart, tokens, middle, mgrad, gains, ffn_back, qk_back):
    seqs, rows, width = tokens.shape
    ep = lax.axis_size("ep")
    if ep != 8 or lax.axis_size("rep") != 4:
        normed_grad = lax.psum_scatter(npart, "ep", scatter_dimension=1, tiled=True).astype(F32)
        moe = lax.psum_scatter(opart, "ep", scatter_dimension=1, tiled=True).astype(F32)
        tg, backs = attn_back_rows(normed_grad, tokens, mgrad, gains[0])
        wrows = lax.all_to_all(wgrad, "ep", split_axis=1, concat_axis=2, tiled=True)
        share = width // ep
        small = jnp.concatenate([jnp.sum(backs, axis=(0, 1)), ffn_back[0], qk_back[0], qk_back[1]])
        small = lax.psum(small, ("ep", "rep"))
        mine = lax.axis_index("ep") * share
        cut = [lax.dynamic_slice_in_dim(small, k * width + mine, share).reshape(-1, 128) for k in range(2)]
        few = small[2 * width :].reshape(2, HEAD_DIM)
        few = jnp.roll(few, -lax.axis_index("ep") * (HEAD_DIM // ep), axis=1)
        small = jnp.concatenate(cut + [few], axis=0)
        big = lax.psum(jnp.concatenate([wograd[None], wrows], axis=0), "rep")
        return big, jnp.pad(small, ((0, 8 - small.shape[0]), (0, 0))), (middle + moe).astype(BF16), tg
    others = jnp.concatenate([ffn_back, jnp.pad(qk_back[:2], ((0, 0), (0, width - HEAD_DIM)))], axis=0)
    npart, opart = (p.reshape(seqs, ep, rows, width) for p in (npart, opart))
    pieces = 4
    block = wograd.shape[0] // pieces
    wgrad = wgrad.reshape(3, wgrad.shape[1] // block, block, wgrad.shape[2])
    wograd = wograd.reshape(pieces, block, width)
    whole = (4, pieces, block, width)
    dma = pltpu.SemaphoreType.DMA
    chunks = 4 * pieces
    out, small, result, tgrad = pl.pallas_call(
        finish_kernel,
        out_shape=(sds(whole, BF16), sds((8, 128), F32), sds(tokens.shape, BF16), sds(tokens.shape, BF16)),
        in_specs=[VM, VM, AN, AN] + [VM] * 5,
        out_specs=(VM, VM, VM, VM),
        scratch_shapes=[
            pltpu.VMEM(whole, BF16),
            pltpu.VMEM(whole, BF16),
            pltpu.VMEM((chunks // 2, block, width), BF16),
            pltpu.VMEM((1, width), F32),
            pltpu.VMEM((ep, 8, 128), F32),
            pltpu.VMEM((7, 8, 128), F32),
            pltpu.VMEM((4, 8, 128), F32),
        ]
        + [dma((7, 3)), dma((7, 3)), dma((4,)), dma((7,)), dma((7,))]
        + [dma((chunks,))] * 8
        + [dma((3,))] * 2
        + 2 * Reduce.scratch(npart),
        compiler_params=pltpu.CompilerParams(collective_id=4, has_side_effects=True, vmem_limit_bytes=61 << 20),
        name="finish",
    )(wgrad, wograd, npart, opart, tokens, middle, mgrad, gains, others)
    return out.reshape(4, pieces * block, width), small, result, tgrad


def dot(a, b, ca, cb):
    return lax.dot_general(a, b, (((ca,), (cb,)), ((), ())), preferred_element_type=F32)


def rope_tables(table):
    half = HEAD_DIM // 2
    values = table[...]
    turned = pltpu.roll(values, half, 1)
    first = lax.broadcasted_iota(jnp.int32, values.shape, 1) < half
    return jnp.where(first, values, turned), jnp.where(first, -turned, values)


def rope(v, cos, sin_turn):
    return v * cos + pltpu.roll(v, HEAD_DIM // 2, 1) * sin_turn


def probabilities(q, k, length):
    scores = dot(q, k, 1, 1) * HEAD_DIM**-0.5
    column = lax.broadcasted_iota(jnp.int32, (1, scores.shape[1]), 1).astype(F32)
    scores = jnp.where(column < length, scores, -1e9)
    p = jnp.exp(scores - jnp.max(scores, axis=-1, keepdims=True))
    return p * (1.0 / jnp.sum(p, axis=-1, keepdims=True))


def packed_slots(number, table, length_live, top):
    tab = table.astype(F32)
    length = tab.shape[0]
    lane = lax.broadcasted_iota(jnp.int32, tab.shape, 1)
    row = lax.broadcasted_iota(jnp.int32, (length, 1), 0).astype(F32)
    chosen = jnp.logical_and(jnp.logical_and(tab == number, lane < top), row < length_live)
    gates = jnp.where(chosen, pltpu.roll(tab, 128 - top, 1), 0.0).astype(BF16)
    chosen = jnp.where(chosen, 1.0, 0.0).astype(BF16)
    ones = jnp.ones((8, 128), BF16)
    hit = dot(ones, chosen, 1, 1)
    weight = dot(ones, gates, 1, 1)
    earlier = lax.broadcasted_iota(jnp.int32, (length, length), 0)
    later = lax.broadcasted_iota(jnp.int32, (length, length), 1)
    rank = dot(hit.astype(BF16), jnp.where(earlier < later, 1.0, 0.0).astype(BF16), 1, 0)
    return jnp.where(hit > 0.5, rank, -1.0), weight, jnp.sum(hit[0:1], axis=1, keepdims=True)


def attend_rows(top, number, s, block, w, wo, gains, small, table, normed, pre, low, ctx, part, slots, starts):
    width = normed.shape[1]
    length = seq_len(small, s)
    cos, sin = rope_tables(table)
    v = block[:, 0:width].astype(F32)
    x = (v * inverse_rms(v) * gains[0:1]).astype(BF16)
    normed[...] = x
    q_pre, k_pre = dot(x, w[0], 1, 0), dot(x, w[1], 1, 0)
    value = dot(x, w[2], 1, 0).astype(BF16)
    pre[0], pre[1] = q_pre, k_pre
    low[2] = value
    for h in range(q_pre.shape[1] // HEAD_DIM):
        cols = slice(h * HEAD_DIM, (h + 1) * HEAD_DIM)
        rot = []
        for i, (u, g) in enumerate(((q_pre[:, cols], small[0:1]), (k_pre[:, cols], small[1:2]))):
            rot.append(rope(u * inverse_rms(u) * g, cos, sin).astype(BF16))
            low[i, :, cols] = rot[i]
        attention = probabilities(rot[0], rot[1], length).astype(BF16)
        ctx[:, cols] = dot(attention, value[:, cols], 1, 0).astype(BF16)
    part[...] = dot(ctx[...], wo[...], 1, 0).astype(BF16).reshape(part.shape)
    routes = block[:, width : width + 128]
    lane = lax.broadcasted_iota(jnp.int32, (1, 128), 1)
    for j, ref in enumerate(slots):
        slot, weight, count = packed_slots(number + j, routes, length, top)
        ref[0:8] = slot
        ref[8:16] = weight
        row = starts[j : j + 1]
        after = jnp.sum(jnp.where(lane == s, row, 0.0), axis=1, keepdims=True) + 16.0 * jnp.floor((count + 15.0) * 0.0625)
        starts[j : j + 1] = jnp.where(lane == s + 1, after, row)


def attend_kernel(top, number, full, w, wo, gains, small, table, normed, pre, low, ctx, part, slots0, slots1, starts):
    s = pl.program_id(0)

    @pl.when(s == 0)
    def _():
        starts[...] = jnp.zeros_like(starts)

    attend_rows(
        top, number[0].astype(F32), s, full.at[0], w, wo, gains, small, table,
        normed.at[0], pre.at[:, 0], low.at[:, 0], ctx.at[0], part.at[0], (slots0.at[0], slots1.at[0]), starts,
    )


def attend(top, number, full, weights, wo, gains, small, table):
    seqs, length, wide = full.shape
    width = wide - 128
    cols = weights.shape[2]
    row = lambda i, *_: (i, 0, 0)
    row2 = lambda i, *_: (0, i, 0, 0)
    two = lambda i, *_: (0, 0)
    slot = pl.BlockSpec((1, 16, length), row)
    return pl.pallas_call(
        functools.partial(attend_kernel, top),
        out_shape=(
            sds((seqs, length, width), BF16),
            sds((2, seqs, length, cols), F32),
            sds((3, seqs, length, cols), BF16),
            sds((seqs, length, cols), BF16),
            sds((seqs, length, width), BF16),
            sds((seqs, 16, length), F32),
            sds((seqs, 16, length), F32),
            sds((8, 128), F32),
        ),
        grid_spec=pltpu.PrefetchScalarGridSpec(
            num_scalar_prefetch=1,
            grid=(seqs,),
            in_specs=[
                pl.BlockSpec((1, length, wide), row),
                pl.BlockSpec(weights.shape, lambda i, *_: (0, 0, 0)),
                pl.BlockSpec(wo.shape, two),
                pl.BlockSpec((8, width), two),
                pl.BlockSpec((8, 128), two),
                pl.BlockSpec((length, HEAD_DIM), two),
            ],
            out_specs=(
                pl.BlockSpec((1, length, width), row),
                pl.BlockSpec((2, 1, length, cols), row2),
                pl.BlockSpec((3, 1, length, cols), row2),
                pl.BlockSpec((1, length, cols), row),
                pl.BlockSpec((1, length, width), row),
                slot,
                slot,
                pl.BlockSpec((8, 128), two),
            ),
        ),
        compiler_params=pltpu.CompilerParams(dimension_semantics=("arbitrary",), vmem_limit_bytes=60 << 20),
        cost_estimate=pl.CostEstimate(flops=10**10, bytes_accessed=4 * 10**7, transcendentals=10**6),
        name="attend",
    )(number, full, weights, wo, gains, small, table)


def forward_kernel(
    top, experts, capacity, tok, cot, ids, gates, wq, wk, wv, pk, wo, table,
    weights_out, gains, small, normed, pre, low, ctx, middle, mixed, cot_full, slots0, slots1, starts, packed,
    weights, full, packets, cot_rows, packed_rows, csem, dsem, own, mixed_own, nbuf, pbuf, lbuf, cbuf, part, begins, ssem,
    wsend, wrecv, psend, precv, rsend, rrecv, lsend, lrecv, local, *scratch,
):
    at = Place()
    z = at.rep
    n = Reduce.sems
    reduce = Reduce(at, part, *scratch[:n])
    gather = Gather(at, own, full, *scratch[n : n + 3])
    cot_gather = Gather(at, cot, cot_full, *scratch[n + 3 : n + 6])
    mixed_gather = Gather(at, mixed_own, mixed, *scratch[n + 6 :])
    seqs, rows, width = tok.shape
    top = ids.shape[1]
    block, cols = wq.shape[0], weights.shape[2]
    quarter = block // 4
    barrier = pltpu.get_barrier_semaphore()
    line = [lax.rem(z + k, 4) for k in range(1, 4)]
    for dev in line:
        pl.semaphore_signal(barrier, inc=1, device_id=(dev, at.me), device_id_type=MESH)
    each(7, lambda m: pl.semaphore_signal(barrier, inc=1, device_id=(z, at.peer(m)), device_id_type=MESH))
    pl.semaphore_wait(barrier, 10)

    def packet_copy(m):
        return at.push(pk, packets.at[at.me], psend.at[m], precv.at[m], at.peer(m))

    def weight_copy(m, j):
        dev = at.peer(m)
        theirs = pl.ds(pl.multiple_of(dev * cols, cols), cols)
        src = (wq, wk, wv)[j].at[pl.ds(pl.multiple_of(z * quarter, quarter), quarter), theirs]
        dst = weights.at[j, pl.ds(pl.multiple_of(at.me * block + z * quarter, quarter), quarter)]
        return at.push(src, dst, wsend.at[m, j], wrecv.at[m, j], dev)

    def weight_landed(m, j):
        dev = at.peer(m)
        dst = weights.at[j, pl.ds(pl.multiple_of(dev * block + z * quarter, quarter), quarter)]
        return at.push(dst, dst, wsend.at[m, j], wrecv.at[m, j], dev)

    def walk(m, q, right):
        part = weights.at[:, pl.ds(pl.multiple_of(at.peer(m) * block + q * quarter, quarter), quarter)]
        send, recv, dev = (rsend, rrecv, z + 1) if right else (lsend, lrecv, z - 1)
        return pltpu.make_async_remote_copy(
            src_ref=part, dst_ref=part, send_sem=send.at[m, q], recv_sem=recv.at[m, q],
            device_id=(dev, at.me), device_id_type=MESH,
        )

    def send_weights(m):
        packet_copy(m).start()
        for j in range(3):
            weight_copy(m, j).start()

    each(7, send_weights)

    place = lax.broadcasted_iota(jnp.int32, (top, 128), 0)
    lane = lax.broadcasted_iota(jnp.int32, (top, 128), 1)
    first = jnp.where(lane == place, 1.0, 0.0).astype(BF16)
    second = jnp.where(lane == place + top, 1.0, 0.0).astype(BF16)

    def join(s):
        own[s, :, 0:width] = tok[s]
        table = dot(ids[s].astype(F32).astype(BF16), first, 0, 0) + dot(gates[s], second, 0, 0)
        own[s, :, width : width + 128] = table.astype(BF16)

    each(seqs, join)
    each(seqs, gather.start)
    own_cols = pl.ds(pl.multiple_of(at.me * cols, cols), cols)
    mine = pl.ds(pl.multiple_of(at.me * block, block), block)
    own_weights = [
        pltpu.make_async_copy(w.at[:, own_cols], weights.at[j, mine], local.at[j]) for j, w in enumerate((wq, wk, wv))
    ]
    for copy in own_weights:
        copy.start()
    early = seqs // 2
    each(early, cot_gather.start)

    def set_out(m):
        for j in range(3):
            weight_landed(m, j).wait_recv()

        @pl.when(z < 3)
        def _():
            walk(m, z, True).start()

        @pl.when(z > 0)
        def _():
            walk(m, z, False).start()

    each(7, set_out)

    def pass_on(d):
        def step(m):
            @pl.when(z - d >= 0)
            def _():
                walk(m, z - d, True).wait_recv()

                @pl.when(z < 3)
                def _():
                    walk(m, z - d, True).start()

            @pl.when(z + d <= 3)
            def _():
                walk(m, z + d, False).wait_recv()

                @pl.when(z > 0)
                def _():
                    walk(m, z + d, False).start()

        each(7, step)

    def relay(i, _):
        gather.relay(2 * i, True)
        gather.relay(2 * i + 1, False)
        return 0

    pairs = seqs // 2
    lax.fori_loop(0, pairs // 2, relay, 0)
    pass_on(1)
    lax.fori_loop(pairs // 2, pairs, relay, 0)
    pass_on(2)
    each(seqs, gather.relay_far)
    each(7, lambda m: packet_copy(m).wait_recv())
    packets[at.me] = pk[...]
    devices = packets.shape[0]
    share = width // (128 * devices)
    heads = HEAD_DIM // devices
    gains[...] = jnp.zeros_like(gains)
    small[...] = jnp.zeros_like(small)
    for o in range(devices):
        for k in range(share):
            lanes = pl.ds((o * share + k) * 128, 128)
            gains[0:1, lanes] = packets[o, k : k + 1]
            gains[1:2, lanes] = packets[o, share + k : share + k + 1]
        base = 2 * share
        small[0:1] += pltpu.roll(packets[o, base : base + 1], o * heads, 1)
        small[1:2] += pltpu.roll(packets[o, base + 1 : base + 2], o * heads, 1)
        small[2:3] += pltpu.roll(packets[o, base + 2 : base + 3], o, 1)
    each(seqs, gather.finish)
    pass_on(3)

    def sent(m):
        for q in range(4):

            @pl.when(jnp.logical_and(q <= z, z < 3))
            def _():
                walk(m, q, True).wait_send()

            @pl.when(jnp.logical_and(q >= z, z > 0))
            def _():
                walk(m, q, False).wait_send()

        packet_copy(m).wait_send()
        for j in range(3):
            weight_copy(m, j).wait_send()

    for copy in own_weights:
        copy.wait()
    keep = pltpu.make_async_copy(weights, weights_out, local.at[3])
    keep.start()
    each(seqs, cot_gather.start, low=early)
    number = (at.me * experts).astype(F32)
    begins[...] = jnp.zeros_like(begins)

    def stores(s):
        k = lax.rem(s, 2)
        pairs = ((nbuf.at[k], normed.at[s]), (pbuf.at[k], pre.at[:, s]), (lbuf.at[k], low.at[:, s]), (cbuf.at[k], ctx.at[s]))
        return [pltpu.make_async_copy(src, dst, ssem.at[i, k]) for i, (src, dst) in enumerate(pairs)]

    def sequence(s):
        k = lax.rem(s, 2)

        @pl.when(s >= 2)
        def _():
            for copy in stores(s - 2):
                copy.wait()

        attend_rows(
            top, number, s, full.at[s], weights, wo, gains, small, table,
            nbuf.at[k], pbuf.at[k], lbuf.at[k], cbuf.at[k], part.at[s], (slots0.at[s], slots1.at[s]), begins,
        )
        for copy in stores(s):
            copy.start()
        reduce.start(s)

    def rows(s):
        living = live_rows(small, s, at.me, tok.shape[1])
        mid, out = mix_rows(reduce.total(s), tok[s], living, gains[1:2])
        middle[s] = mid
        mixed_own[s] = out
        mixed_gather.start(s)

    def cot_pair(p):
        @pl.when(lax.rem(p, 2) == 0)
        def _():
            cot_gather.relay(p, True)
            cot_gather.relay(p + 1, False)

    jobs = (
        (sequence, 0, seqs), (reduce.hop1, 1, seqs), (cot_pair, 0, seqs), (reduce.hop2, 3, seqs),
        (cot_gather.relay_far, 4, seqs), (rows, 5, seqs),
    )

    def tick(i, _):
        for job, lag, count in jobs:

            @pl.when(jnp.logical_and(i >= lag, i < lag + count))
            def _():
                job(i - lag)

        return 0

    lax.fori_loop(0, max(lag + count for _, lag, count in jobs), tick, 0)
    starts[...] = begins[...].astype(jnp.int32)
    each(seqs, cot_gather.finish)

    def cot_load(s):
        k = lax.rem(s, 2)
        return pltpu.make_async_copy(cot_full.at[s], cot_rows.at[k], csem.at[k])

    def pack_store(s):
        k = lax.rem(s, 2)
        return pltpu.make_async_copy(packed_rows.at[k], packed.at[s], dsem.at[k])

    def pack(s):
        k = lax.rem(s, 2)
        cot_load(s).wait()

        @pl.when(s + 1 < seqs)
        def _():
            cot_load(s + 1).start()

        @pl.when(s >= 2)
        def _():
            pack_store(s - 2).wait()

        spread = []
        for slots in (slots0, slots1):
            place = lax.broadcasted_iota(jnp.int32, (capacity, length), 0).astype(F32) == slots[s, 0:1]
            spread.append(jnp.where(place, slots[s, 8:9], 0.0).astype(BF16))
        packed_rows[k] = dot(jnp.concatenate(spread, axis=0), cot_rows[k], 1, 0).astype(BF16)
        pack_store(s).start()

    length = cot_full.shape[1]
    cot_load(0).start()

    def relay_and_pack(i, _):
        mixed_gather.relay(2 * i, True)
        mixed_gather.relay(2 * i + 1, False)
        pack(2 * i)
        pack(2 * i + 1)
        return 0

    lax.fori_loop(0, seqs // 2, relay_and_pack, 0)
    each(seqs, mixed_gather.relay_far)
    each(seqs, mixed_gather.finish)
    pack_store(seqs - 2).wait()
    pack_store(seqs - 1).wait()
    for s in (seqs - 2, seqs - 1):
        for copy in stores(s):
            copy.wait()
    each(seqs, reduce.finish)
    each(7, sent)
    keep.wait()


def forward(top, experts, capacity, tokens, cotangent, ids, gates, wq, wk, wv, packet, wo, table):
    seqs, rows, width = tokens.shape
    length, cols = rows * 8, wq.shape[1] // 8
    part = sds((seqs, 8, rows, width), BF16)
    weights = (3, wq.shape[0] * 8, cols)
    dma = pltpu.SemaphoreType.DMA
    return pl.pallas_call(
        functools.partial(forward_kernel, top, experts, capacity),
        out_shape=(
            sds(weights, BF16),
            sds((8, width), F32),
            sds((8, 128), F32),
            sds((seqs, length, width), BF16),
            sds((2, seqs, length, cols), F32),
            sds((3, seqs, length, cols), BF16),
            sds((seqs, length, cols), BF16),
            sds(tokens.shape, F32),
            sds((seqs, length, width), BF16),
            sds((seqs, length, width), BF16),
            sds((seqs, 16, length), F32),
            sds((seqs, 16, length), F32),
            sds((8, 128), jnp.int32),
            sds((seqs, 2 * capacity, width), BF16),
        ),
        in_specs=[VM] * 10,
        out_specs=(AN, VM, VM, AN, AN, AN, AN, VM, AN, AN, VM, VM, VM, AN),
        scratch_shapes=[
            pltpu.VMEM(weights, BF16),
            pltpu.VMEM((seqs, length, width + 128), BF16),
            pltpu.VMEM((8,) + packet.shape, F32),
            pltpu.VMEM((2, length, width), BF16),
            pltpu.VMEM((2, 2 * capacity, width), BF16),
            dma((2,)),
            dma((2,)),
            pltpu.VMEM((seqs, rows, width + 128), BF16),
            pltpu.VMEM(tokens.shape, BF16),
            pltpu.VMEM((2, length, width), BF16),
            pltpu.VMEM((2, 2, length, cols), F32),
            pltpu.VMEM((2, 3, length, cols), BF16),
            pltpu.VMEM((2, length, cols), BF16),
            pltpu.VMEM(part.shape, BF16),
            pltpu.VMEM((8, 128), F32),
            dma((4, 2)),
        ]
        + [dma((7, 3)), dma((7, 3)), dma((7,)), dma((7,))]
        + [dma((7, 4))] * 4
        + [dma((4,))]
        + Reduce.scratch(part)
        + 3 * Gather.scratch(seqs),
        compiler_params=pltpu.CompilerParams(collective_id=1, **COMM),
        name="forward",
    )(tokens, cotangent, ids, gates, wq, wk, wv, packet, wo, table)


def attend_back_kernel(
    agrad, normed, pre, low, ctx, w, wo, small, table, part, wgrad, wograd, gains, wacc, woacc,
):
    s = pl.program_id(0)
    length = seq_len(small, s)
    cos, sin = rope_tables(table)

    @pl.when(s == 0)
    def _():
        wacc[...] = jnp.zeros_like(wacc)
        woacc[...] = jnp.zeros_like(woacc)
        gains[...] = jnp.zeros_like(gains)

    ag = agrad[0]
    woacc[...] += dot(ctx[0], ag, 0, 0)
    cg_all = dot(ag, wo[...], 1, 1).astype(BF16)
    scale = HEAD_DIM**-0.5
    half = HEAD_DIM // 2
    grads = ([], [], [])
    for h in range(cg_all.shape[1] // HEAD_DIM):
        cols = slice(h * HEAD_DIM, (h + 1) * HEAD_DIM)
        q, k, value, cg = low[0, 0, :, cols], low[1, 0, :, cols], low[2, 0, :, cols], cg_all[:, cols]
        attention = probabilities(q, k, length)
        grads[2].append(dot(attention.astype(BF16), cg, 0, 0).astype(BF16))
        pg = dot(cg, value, 1, 1)
        sg = (attention * (pg - jnp.sum(attention * pg, axis=-1, keepdims=True))).astype(BF16)
        for i, (rot_grad, g) in enumerate(((dot(sg, k, 1, 0), small[0:1]), (dot(sg, q, 0, 0), small[1:2]))):
            wgt = rot_grad * scale
            u = wgt * cos + pltpu.roll(wgt * sin, half, 1)
            v = pre[i, 0, :, cols]
            r = inverse_rms(v)
            grads[i].append(rms_back(v, r, u * g).astype(BF16))
            gains[i : i + 1] += jnp.sum(u * v * r, axis=0, keepdims=True)
    width = w.shape[2]
    joined = jnp.concatenate([g for kind in grads for g in kind], axis=1)
    wacc[...] += dot(normed[0], joined, 0, 0)
    total = None
    for i in range(3):
        piece = dot(joined[:, i * width : (i + 1) * width], w[i], 1, 1)
        total = piece if total is None else total + piece
    part[0] = total.astype(BF16)

    @pl.when(s == pl.num_programs(0) - 1)
    def _():
        for i in range(3):
            wgrad[i] = wacc[:, i * width : (i + 1) * width].astype(BF16)
        wograd[...] = woacc[...].astype(BF16)


def attend_back(agrad, normed, pre, low, ctx, weights, wo, small, table):
    seqs, length, width = agrad.shape
    cols = weights.shape[2]
    row = lambda i, *_: (i, 0, 0)
    row2 = lambda i, *_: (0, i, 0, 0)
    two = lambda i, *_: (0, 0)
    three = lambda i, *_: (0, 0, 0)
    return pl.pallas_call(
        attend_back_kernel,
        out_shape=(
            sds(agrad.shape, BF16),
            sds(weights.shape, BF16),
            sds(wo.shape, BF16),
            sds((8, HEAD_DIM), F32),
        ),
        grid_spec=pltpu.PrefetchScalarGridSpec(
            num_scalar_prefetch=0,
            grid=(seqs,),
            in_specs=[
                pl.BlockSpec((1, length, width), row),
                pl.BlockSpec((1, length, width), row),
                pl.BlockSpec((2, 1, length, cols), row2),
                pl.BlockSpec((3, 1, length, cols), row2),
                pl.BlockSpec((1, length, cols), row),
                pl.BlockSpec(weights.shape, three),
                pl.BlockSpec(wo.shape, two),
                pl.BlockSpec((8, 128), two),
                pl.BlockSpec((length, HEAD_DIM), two),
            ],
            out_specs=(
                pl.BlockSpec((1, length, width), row),
                pl.BlockSpec(weights.shape, three),
                pl.BlockSpec(wo.shape, two),
                pl.BlockSpec((8, HEAD_DIM), two),
            ),
            scratch_shapes=[
                pltpu.VMEM((weights.shape[1], 3 * cols), F32),
                pltpu.VMEM(wo.shape, F32),
            ],
        ),
        compiler_params=pltpu.CompilerParams(dimension_semantics=("arbitrary",), vmem_limit_bytes=60 << 20),
        cost_estimate=pl.CostEstimate(flops=2 * 10**10, bytes_accessed=4 * 10**7, transcendentals=10**6),
        name="attend_back",
    )(agrad, normed, pre, low, ctx, weights, wo, small, table)


BLOCK = 256
FIRST_TILE = (512, 1024)


def pack_rows(seqs, capacity):
    return -(-seqs * capacity // BLOCK) * BLOCK


def each_block(blocks, hidden, job):
    part = min(hidden, 512)
    parts = hidden // part

    def run(i, _):
        b, h = i // parts, lax.rem(i, parts)
        rows = pl.ds(pl.multiple_of(b * BLOCK, BLOCK), BLOCK)
        low = pl.multiple_of(h * part, part)
        job(rows, pl.ds(low, part), pl.ds(pl.multiple_of(hidden + low, part), part))
        return 0

    lax.fori_loop(0, blocks * parts, run, 0)


def swiglu_back(gate, up, dact):
    sig = 1.0 / (1.0 + jnp.exp(-gate))
    return dact * up * sig * (1.0 + gate * (1.0 - sig)), dact * (gate * sig)


def forward_blocks(blocks, x, dy, wi, wo, acts, dgus):
    def job(rows, gcols, ucols):
        gate = dot(x[rows], wi[:, gcols], 1, 0)
        up = dot(x[rows], wi[:, ucols], 1, 0)
        dact = dot(dy[rows], wo[gcols], 1, 1)
        acts[rows, gcols] = (gate * (1.0 / (1.0 + jnp.exp(-gate))) * up).astype(BF16)
        dgate, dup = swiglu_back(gate, up, dact)
        dgus[rows, gcols] = dgate.astype(BF16)
        dgus[rows, ucols] = dup.astype(BF16)

    each_block(blocks, wo.shape[0], job)


def gradient_tiles(blocks, left, right, result, acc, stage, ssem, busy):
    tr, tc = acc.shape
    down, across = result.shape[0] // tr, result.shape[1] // tc

    def tile(t, _):
        rt, ct = t // across, lax.rem(t, across)
        left_cols = pl.ds(pl.multiple_of(rt * tr, tr), tr)
        right_cols = pl.ds(pl.multiple_of(ct * tc, tc), tc)

        def step(b, _):
            rows = pl.ds(pl.multiple_of(b * BLOCK, BLOCK), BLOCK)
            piece = dot(left[rows, left_cols], right[rows, right_cols], 0, 0)

            @pl.when(b == 0)
            def _():
                acc[...] = piece

            @pl.when(b > 0)
            def _():
                acc[...] += piece

            return 0

        @pl.when(blocks == 0)
        def _():
            acc[...] = jnp.zeros_like(acc)

        lax.fori_loop(0, blocks, step, 0)
        k = lax.rem(t, 2)
        out = pltpu.make_async_copy(stage.at[k], result.at[left_cols, right_cols], ssem.at[k])

        @pl.when(jnp.logical_or(t >= 2, busy))
        def _():
            out.wait()

        stage[k] = acc[...].astype(BF16)
        out.start()
        return 0

    lax.fori_loop(0, down * across, tile, 0)


def drain_tiles(result, acc, stage, ssem):
    tr, tc = acc.shape
    for k in range(2):
        pltpu.make_async_copy(stage.at[k], result.at[pl.ds(0, tr), pl.ds(0, tc)], ssem.at[k]).wait()


def first_kernel(
    capacity, starts, mixed, weighted, slots0, slots1, w_in,
    act, pair, x_all, dy_all, out_grad,
    x, dy, wi, acts, pairs, acc, stage, wsem, ssem, rsem,
):
    step = pl.program_id(0)
    steps = pl.num_programs(0)
    together = mixed.shape[0]
    seqs = steps * together
    width = mixed.shape[2]
    hidden = acts.shape[1]
    load = pltpu.make_async_copy(w_in.at[0], wi, wsem)

    @pl.when(step == 0)
    def _():
        load.start()

    rows_of = []
    for k in range(together):
        spread = []
        for slots in (slots0, slots1):
            place = lax.broadcasted_iota(jnp.int32, (capacity, slots.shape[2]), 0).astype(F32) == slots[k, 0:1]
            spread.append(jnp.where(place, 1.0, 0.0).astype(BF16))
        rows_of.append(dot(jnp.concatenate(spread, axis=0), mixed[k], 1, 0).astype(BF16))
    for k, x_rows in enumerate(rows_of):
        s = step * together + k
        for j in range(2):
            start = pl.multiple_of(starts[j, s], 16)
            x[j, pl.ds(start, capacity)] = x_rows[j * capacity : (j + 1) * capacity]
            dy[j, pl.ds(start, capacity)] = weighted[k, j * capacity : (j + 1) * capacity]

    @pl.when(step == steps - 1)
    def _():
        for j in range(2):
            past = (starts[j, seqs - 1] + capacity) // 16
            end = (starts[j, seqs] + BLOCK - 1) // BLOCK * (BLOCK // 16)

            def clear(i, _):
                rows = pl.ds(pl.multiple_of(i * 16, 16), 16)
                x[j, rows] = jnp.zeros((16, width), BF16)
                dy[j, rows] = jnp.zeros((16, width), BF16)
                return 0

            lax.fori_loop(past, end, clear, 0)
        saves = [pltpu.make_async_copy(x, x_all, rsem.at[0]), pltpu.make_async_copy(dy, dy_all, rsem.at[1])]
        for copy in saves:
            copy.start()
        blocks = (starts[0, seqs] + BLOCK - 1) // BLOCK
        load.wait()

        def forward(rows, gcols, ucols):
            gate = dot(x[0, rows], wi[:, gcols], 1, 0)
            up = dot(x[0, rows], wi[:, ucols], 1, 0)
            acts[rows, gcols] = (gate * (1.0 / (1.0 + jnp.exp(-gate))) * up).astype(BF16)
            pairs[rows, gcols] = gate.astype(BF16)
            pairs[rows, ucols] = up.astype(BF16)

        each_block(blocks, hidden, forward)
        saves += [pltpu.make_async_copy(acts, act.at[0], rsem.at[2]), pltpu.make_async_copy(pairs, pair, rsem.at[3])]
        for copy in saves[2:]:
            copy.start()
        gradient_tiles(blocks, acts, dy.at[0], out_grad, acc, stage, ssem, False)
        drain_tiles(out_grad, acc, stage, ssem)
        for copy in saves:
            copy.wait()


def expert_first(starts, mixed, weighted, slots, w_in, hidden, capacity):
    seqs, length, width = mixed.shape
    rows = pack_rows(seqs, capacity)
    dma = pltpu.SemaphoreType.DMA
    seq = lambda i, *_: (i, 0, 0)
    together = 2
    slot_spec = pl.BlockSpec((together, 16, length), seq)
    return pl.pallas_call(
        functools.partial(first_kernel, capacity),
        out_shape=(
            sds((2, rows, hidden), BF16),
            sds((rows, 2 * hidden), BF16),
            sds((2, rows, width), BF16),
            sds((2, rows, width), BF16),
            sds((hidden, width), BF16),
        ),
        grid_spec=pltpu.PrefetchScalarGridSpec(
            num_scalar_prefetch=1,
            grid=(seqs // together,),
            in_specs=[
                pl.BlockSpec((together, length, width), seq),
                pl.BlockSpec((together, 2 * capacity, width), seq),
                slot_spec,
                slot_spec,
                AN,
            ],
            out_specs=(AN, AN, AN, AN, AN),
            scratch_shapes=[
                pltpu.VMEM((2, rows, width), BF16),
                pltpu.VMEM((2, rows, width), BF16),
                pltpu.VMEM(w_in.shape[1:], BF16),
                pltpu.VMEM((rows, hidden), BF16),
                pltpu.VMEM((rows, 2 * hidden), BF16),
                pltpu.VMEM(FIRST_TILE, F32),
                pltpu.VMEM((2,) + FIRST_TILE, BF16),
                dma,
                dma((2,)),
                dma((4,)),
            ],
        ),
        compiler_params=pltpu.CompilerParams(dimension_semantics=("arbitrary",), vmem_limit_bytes=62 << 20),
        cost_estimate=pl.CostEstimate(flops=2 * 10**10, bytes_accessed=6 * 10**7, transcendentals=10**6),
        name="expert_first",
    )(starts, mixed, weighted, *slots, w_in)


def in_grad_kernel(
    seqs, starts, x_all, dy_all, pair, w_out, dgu, in_grad, x, dy, wo, pairs, dgus, acc, stage, lsem, wsem, ssem, rsem
):
    blocks = (starts[0, seqs] + BLOCK - 1) // BLOCK
    hidden = wo.shape[0]
    weights = pltpu.make_async_copy(w_out.at[0], wo, wsem)
    weights.start()

    def run(b, action):
        rows = pl.ds(pl.multiple_of(b * BLOCK, BLOCK), BLOCK)
        for copy in (
            pltpu.make_async_copy(dy_all.at[0, rows], dy.at[rows], lsem.at[0, b]),
            pltpu.make_async_copy(pair.at[rows], pairs.at[rows], lsem.at[1, b]),
            pltpu.make_async_copy(x_all.at[0, rows], x.at[rows], lsem.at[2, b]),
        ):
            getattr(copy, action)()
        return 0

    lax.fori_loop(0, blocks, lambda b, _: run(b, "start"), 0)
    weights.wait()
    lax.fori_loop(0, blocks, lambda b, _: run(b, "wait"), 0)

    def backward(rows, gcols, ucols):
        dact = dot(dy[rows], wo[gcols], 1, 1)
        dgate, dup = swiglu_back(pairs[rows, gcols].astype(F32), pairs[rows, ucols].astype(F32), dact)
        dgus[rows, gcols] = dgate.astype(BF16)
        dgus[rows, ucols] = dup.astype(BF16)

    each_block(blocks, hidden, backward)
    save = pltpu.make_async_copy(dgus, dgu.at[0], rsem)
    save.start()
    gradient_tiles(blocks, x, dgus, in_grad, acc, stage, ssem, False)
    drain_tiles(in_grad, acc, stage, ssem)
    save.wait()


def first_in_grad(seqs, starts, x_all, dy_all, pair, w_out):
    rows, width = x_all.shape[1:]
    hidden = w_out.shape[1]
    dma = pltpu.SemaphoreType.DMA
    return pl.pallas_call(
        functools.partial(in_grad_kernel, seqs),
        out_shape=(sds((2, rows, 2 * hidden), BF16), sds((width, 2 * hidden), BF16)),
        grid_spec=pltpu.PrefetchScalarGridSpec(
            num_scalar_prefetch=1,
            grid=(1,),
            in_specs=[AN] * 4,
            out_specs=(AN, AN),
            scratch_shapes=[
                pltpu.VMEM((rows, width), BF16),
                pltpu.VMEM((rows, width), BF16),
                pltpu.VMEM(w_out.shape[1:], BF16),
                pltpu.VMEM((rows, 2 * hidden), BF16),
                pltpu.VMEM((rows, 2 * hidden), BF16),
                pltpu.VMEM((512, 2048), F32),
                pltpu.VMEM((2, 512, 2048), BF16),
                dma((3, rows // BLOCK)),
                dma,
                dma((2,)),
                dma,
            ],
        ),
        compiler_params=pltpu.CompilerParams(dimension_semantics=("arbitrary",), vmem_limit_bytes=60 << 20),
        cost_estimate=pl.CostEstimate(flops=10**10, bytes_accessed=2 * 10**7, transcendentals=0),
        name="first_in_grad",
    )(starts, x_all, dy_all, pair, w_out)


def second_kernel(
    seqs, starts, x_all, dy_all, w_in, w_out, _act, _dgu, act, dgu, in_grad, out_grad,
    x, dy, wi, wo, acts, dgus, acc, stage, wsem, lsem, ssem, rsem,
):
    blocks = (starts[1, seqs] + BLOCK - 1) // BLOCK
    loads = [pltpu.make_async_copy(w_in.at[1], wi, wsem.at[0]), pltpu.make_async_copy(w_out.at[1], wo, wsem.at[1])]

    def load(b, action):
        rows = pl.ds(pl.multiple_of(b * BLOCK, BLOCK), BLOCK)
        for copy in (
            pltpu.make_async_copy(x_all.at[1, rows], x.at[rows], lsem.at[0, b]),
            pltpu.make_async_copy(dy_all.at[1, rows], dy.at[rows], lsem.at[1, b]),
        ):
            getattr(copy, action)()
        return 0

    for copy in loads:
        copy.start()
    lax.fori_loop(0, blocks, lambda b, _: load(b, "start"), 0)
    for copy in loads:
        copy.wait()
    lax.fori_loop(0, blocks, lambda b, _: load(b, "wait"), 0)

    forward_blocks(blocks, x, dy, wi, wo, acts, dgus)
    saves = [pltpu.make_async_copy(acts, act.at[1], rsem.at[0]), pltpu.make_async_copy(dgus, dgu.at[1], rsem.at[1])]
    for copy in saves:
        copy.start()
    gradient_tiles(blocks, x, dgus, in_grad, acc, stage, ssem, False)
    gradient_tiles(blocks, acts, dy, out_grad, acc, stage, ssem, True)
    drain_tiles(out_grad, acc, stage, ssem)
    for copy in saves:
        copy.wait()


def expert_second(seqs, starts, x_all, dy_all, w_in, w_out, act, dgu):
    rows, width = dy_all.shape[1:]
    hidden = w_out.shape[1]
    dma = pltpu.SemaphoreType.DMA
    return pl.pallas_call(
        functools.partial(second_kernel, seqs),
        out_shape=(
            sds(act.shape, BF16), sds(dgu.shape, BF16), sds((width, 2 * hidden), BF16), sds((hidden, width), BF16)
        ),
        input_output_aliases={5: 0, 6: 1},
        grid_spec=pltpu.PrefetchScalarGridSpec(
            num_scalar_prefetch=1,
            grid=(1,),
            in_specs=[AN] * 6,
            out_specs=(AN, AN, AN, AN),
            scratch_shapes=[
                pltpu.VMEM((rows, width), BF16),
                pltpu.VMEM((rows, width), BF16),
                pltpu.VMEM(w_in.shape[1:], BF16),
                pltpu.VMEM(w_out.shape[1:], BF16),
                pltpu.VMEM((rows, hidden), BF16),
                pltpu.VMEM((rows, 2 * hidden), BF16),
                pltpu.VMEM((512, 2048), F32),
                pltpu.VMEM((2, 512, 2048), BF16),
                dma((2,)),
                dma((2, rows // BLOCK)),
                dma((2,)),
                dma((2,)),
            ],
        ),
        compiler_params=pltpu.CompilerParams(dimension_semantics=("arbitrary",), vmem_limit_bytes=60 << 20),
        cost_estimate=pl.CostEstimate(flops=25 * 10**9, bytes_accessed=6 * 10**7, transcendentals=10**6),
        name="expert_second",
    )(starts, x_all, dy_all, w_in, w_out, act, dgu)


def tail_kernel(seqs, starts, act, dgu, w_in, w_out, produced, dx):
    @pl.when(pl.program_id(1) * BLOCK < starts[pl.program_id(0), seqs])
    def _():
        part = min(produced.shape[1], 512)

        def run(i, _):
            cols = pl.ds(pl.multiple_of(i * part, part), part)
            produced[:, cols] = dot(act[...], w_out[:, cols], 1, 0).astype(BF16)
            dx[:, cols] = dot(dgu[...], w_in[cols], 1, 1).astype(BF16)
            return 0

        lax.fori_loop(0, produced.shape[1] // part, run, 0)


def expert_tails(seqs, starts, act, dgu, w_in, w_out):
    _, rows, hidden = act.shape
    width = w_in.shape[1]

    def block(j, i, st):
        return j, jnp.maximum(jnp.minimum(i, (st[j, seqs] + BLOCK - 1) // BLOCK - 1), 0), 0

    out = pl.BlockSpec((None, BLOCK, width), block)
    return pl.pallas_call(
        functools.partial(tail_kernel, seqs),
        out_shape=(sds((2, rows, width), BF16), sds((2, rows, width), BF16)),
        grid_spec=pltpu.PrefetchScalarGridSpec(
            num_scalar_prefetch=1,
            grid=(2, rows // BLOCK),
            in_specs=[
                pl.BlockSpec((None, BLOCK, hidden), block),
                pl.BlockSpec((None, BLOCK, 2 * hidden), block),
                pl.BlockSpec((None,) + w_in.shape[1:], lambda j, i, *_: (j, 0, 0)),
                pl.BlockSpec((None,) + w_out.shape[1:], lambda j, i, *_: (j, 0, 0)),
            ],
            out_specs=(out, out),
        ),
        compiler_params=pltpu.CompilerParams(dimension_semantics=("arbitrary", "arbitrary"), vmem_limit_bytes=60 << 20),
        cost_estimate=pl.CostEstimate(flops=24 * 10**9, bytes_accessed=6 * 10**7, transcendentals=0),
        name="expert_tails",
    )(starts, act, dgu, w_in, w_out)


def combine_kernel(capacity, local, *refs):
    s = pl.program_id(0)
    starts = refs[0]
    slots = refs[1 : 1 + local]
    produced, dx, out_part, grad_part, held_out, held_grad, sems = refs[1 + local :]
    seqs = pl.num_programs(0)

    def loads(s):
        k = lax.rem(s, 2)
        copies = []
        for j in range(local):
            span = pl.ds(pl.multiple_of(starts[j, s], 16), capacity)
            copies.append(pltpu.make_async_copy(produced.at[j, span], held_out.at[k, j], sems.at[k, 0, j]))
            copies.append(pltpu.make_async_copy(dx.at[j, span], held_grad.at[k, j], sems.at[k, 1, j]))
        return copies

    @pl.when(s == 0)
    def _():
        for copy in loads(s):
            copy.start()

    @pl.when(s + 1 < seqs)
    def _():
        for copy in loads(s + 1):
            copy.start()

    for copy in loads(s):
        copy.wait()
    slot = lax.rem(s, 2)
    out_sum, grad_sum = None, None
    for j in range(local):
        length = slots[j].shape[2]
        column = lax.broadcasted_iota(jnp.int32, (capacity, length), 0).astype(F32)
        place = column == slots[j][0, 0:1]
        held = lax.broadcasted_iota(jnp.int32, (capacity, 1), 0) < starts[j, s + 1] - starts[j, s]
        rows = jnp.where(held, held_out[slot, j], 0.0).astype(BF16)
        grads = jnp.where(held, held_grad[slot, j], 0.0).astype(BF16)
        out = dot(jnp.where(place, slots[j][0, 8:9], 0.0).astype(BF16), rows, 0, 0)
        grad = dot(jnp.where(place, 1.0, 0.0).astype(BF16), grads, 0, 0)
        out_sum = out if out_sum is None else out_sum + out
        grad_sum = grad if grad_sum is None else grad_sum + grad
    out_part[0] = out_sum.astype(BF16)
    grad_part[0] = grad_sum.astype(BF16)


def combine(starts, slots, produced, dx, capacity):
    local = len(slots)
    seqs, _, length = slots[0].shape
    width = produced.shape[2]
    seq = lambda i, *_: (i, 0, 0)
    held = pltpu.VMEM((2, local, capacity, width), BF16)
    return pl.pallas_call(
        functools.partial(combine_kernel, capacity, local),
        out_shape=(sds((seqs, length, width), BF16), sds((seqs, length, width), BF16)),
        grid_spec=pltpu.PrefetchScalarGridSpec(
            num_scalar_prefetch=1,
            grid=(seqs,),
            in_specs=[pl.BlockSpec((1, 16, length), seq)] * local + [AN] * 2,
            out_specs=(pl.BlockSpec((1, length, width), seq), pl.BlockSpec((1, length, width), seq)),
            scratch_shapes=[held, held, pltpu.SemaphoreType.DMA((2, 2, local))],
        ),
        compiler_params=pltpu.CompilerParams(dimension_semantics=("arbitrary",), vmem_limit_bytes=60 << 20),
        cost_estimate=pl.CostEstimate(flops=3 * 10**9, bytes_accessed=4 * 10**7, transcendentals=0),
        name="combine",
    )(starts, *slots, produced, dx)


def shards(
    tokens, cotangent, gate_weights, expert_ids, seq_lengths, query_weight, key_weight, value_weight,
    output_weight, attn_gain, ffn_gain, query_gain, key_gain, expert_in, expert_out,
):
    ep = lax.axis_size("ep")
    me = lax.axis_index("ep")
    seqs, rows, _ = tokens.shape
    length = rows * ep
    top = gate_weights.shape[2]
    local = expert_in.shape[0]
    hidden = expert_out.shape[1]
    experts = local * ep
    capacity = -(-(length * top * 9 // (8 * experts)) // 16) * 16

    gains = jnp.concatenate([attn_gain, ffn_gain]).astype(F32).reshape(-1, 128)
    few = [query_gain.astype(F32), key_gain.astype(F32), seq_lengths.astype(F32)]
    few = jnp.stack([jnp.pad(v, (0, 128 - v.shape[0])) for v in few])
    packet = jnp.concatenate([gains, few], axis=0)
    packet = jnp.pad(packet, ((0, -packet.shape[0] % 8), (0, 0)))
    share = gains.shape[0] // 2

    half = HEAD_DIM // 2
    frequency = ROPE_BASE ** (-(np.arange(half, dtype=np.float32) * np.float32(2.0 / HEAD_DIM)))
    angles = np.arange(length, dtype=np.float32)[:, None] * frequency.astype(np.float32)[None, :]
    table = jnp.asarray(np.concatenate([np.cos(angles), np.sin(angles)], axis=-1), F32)

    arrays = (
        tokens, cotangent, expert_ids.transpose(0, 2, 1), gate_weights.transpose(0, 2, 1),
        query_weight, key_weight, value_weight, packet,
    )
    if ep == 8 and lax.axis_size("rep") == 4:
        (
            weights, gains, small_in, normed, pre, low, ctx, middle, mixed, cot_full, slots0, slots1, starts, weighted,
        ) = forward(top, local, capacity, *arrays, output_weight, table)
    else:
        full, weights, cot_full, gains, small_in = front(*arrays)
        number = (me * local).astype(jnp.int32)[None]
        normed, pre, low, ctx, part, slots0, slots1, starts = attend(
            top, number, full, weights, output_weight, gains, small_in, table
        )
        starts = starts.astype(jnp.int32)
        middle, mixed = mix(part, tokens, small_in, gains)
        column = jnp.arange(capacity, dtype=F32)[None, :, None]
        spread = [jnp.where(column == t[:, 0:1], t[:, 8:9], 0.0).astype(BF16) for t in (slots0, slots1)]
        weighted = jnp.einsum(
            "srt,std->srd", jnp.concatenate(spread, axis=1), cot_full, preferred_element_type=F32
        ).astype(BF16)

    act, pair, x_all, dy_all, out_grad0 = expert_first(
        starts, mixed, weighted, (slots0, slots1), expert_in, hidden, capacity
    )

    def over_rep(value):
        return lax.psum_scatter(value, "rep", scatter_dimension=0, tiled=True)

    out0 = over_rep(out_grad0)
    dgu, in_grad0 = first_in_grad(seqs, starts, x_all, dy_all, pair, expert_out)
    in0 = over_rep(in_grad0)
    x_all, _ = lax.optimization_barrier((x_all, in_grad0))
    act, dgu, in_grad1, out_grad1 = expert_second(seqs, starts, x_all, dy_all, expert_in, expert_out, act, dgu)
    in1 = over_rep(in_grad1)
    out1 = over_rep(out_grad1)
    produced, dx = expert_tails(seqs, starts, act, dgu, expert_in, expert_out)
    out_part, grad_part = combine(starts, (slots0, slots1), produced, dx, capacity)

    mgrad, ffn_back, agrad = back(grad_part, middle, cotangent, small_in, gains)
    npart, wgrad, wograd, qk_back = attend_back(
        agrad, normed, pre, low, ctx, weights, output_weight, small_in, table
    )
    sums, small, result, token_grad = finish(
        wgrad, wograd, npart, out_part, tokens, middle, mgrad, gains, ffn_back, qk_back
    )

    heads = HEAD_DIM // ep
    wide = sums.astype(F32)
    return (
        result,
        token_grad,
        wide[1],
        wide[2],
        wide[3],
        wide[0],
        small[:share].reshape(-1),
        small[share : 2 * share].reshape(-1),
        small[2 * share, :heads],
        small[2 * share + 1, :heads],
        jnp.stack([in0, in1]).astype(F32),
        jnp.stack([out0, out1]).astype(F32),
    )


def solution(mesh):
    seq = P("rep", "ep", None)
    row, gain, expert = P("ep", None), P("ep"), P("ep", None, None)
    split = P("ep", "rep", None)

    return jax.shard_map(
        shards,
        mesh=mesh,
        in_specs=(seq, seq, seq, seq, P(("rep", "ep")), row, row, row, row, gain, gain, gain, gain, expert, expert),
        out_specs=(seq, seq, row, row, row, row, gain, gain, gain, gain, split, split),
        check_vma=False,
    )
```
